32 devices in a mesh: dp: 8 (over z, x), seq: 4 (over y, core).
Axes of the slice: x: 2, y: 2, z: 4, core: 2. Of those that a mesh axis runs over, the one named last changes fastest.
Arguments:
- tokens: bfloat16 [16, 2048, 768], P('dp', 'seq'), may hold values from -6 to 6
- segment_ids: int32 [16, 2048], P('dp'), may hold values from 0 to 3, never falling along the last dimension, each value on 1 to 1024 neighbouring positions
- w_query: float32 [768, 768], P('dp'), may hold values from -0.3125 to 0.3125
- w_key: float32 [768, 768], P('dp'), may hold values from -0.3125 to 0.3125
- w_value: float32 [768, 768], P('dp'), may hold values from -0.21875 to 0.21875
- w_output: float32 [768, 768], P('dp'), may hold values from -0.875 to 0.875
- b_query: float32 [768], P('dp'), may hold values from -3 to 3
- b_value: float32 [768], P('dp'), may hold values from -3 to 3
- b_output: float32 [768], P('dp'), may hold values from -3 to 3
- first_gain: float32 [768], P('dp'), may hold values from 0.5 to 1.5
- first_shift: float32 [768], P('dp'), may hold values from -3 to 3
- w_inner: float32 [768, 3072], P('dp'), may hold values from -0.21875 to 0.21875
- b_inner: float32 [3072], P('dp'), may hold values from -3 to 3
- w_outer: float32 [3072, 768], P('dp'), may hold values from -0.109375 to 0.109375
- b_outer: float32 [768], P('dp'), may hold values from -3 to 3
- second_gain: float32 [768], P('dp'), may hold values from 0.5 to 1.5
- second_shift: float32 [768], P('dp'), may hold values from -3 to 3
- cotangent: bfloat16 [16, 2048, 768], P('dp', 'seq'), may hold values from -6 to 6
Outputs:
- mixed: bfloat16 [16, 2048, 768], P('dp', 'seq')
- grad_tokens: float32 [16, 2048, 768], P('dp', 'seq')
- grad_w_query: float32 [768, 768], P('dp')
- grad_w_key: float32 [768, 768], P('dp')
- grad_w_value: float32 [768, 768], P('dp')
- grad_w_output: float32 [768, 768], P('dp')
- grad_b_query: float32 [768], P('dp')
- grad_b_value: float32 [768], P('dp')
- grad_b_output: float32 [768], P('dp')
- grad_first_gain: float32 [768], P('dp')
- grad_first_shift: float32 [768], P('dp')
- grad_w_inner: float32 [768, 3072], P('dp')
- grad_b_inner: float32 [3072], P('dp')
- grad_w_outer: float32 [3072, 768], P('dp')
- grad_b_outer: float32 [768], P('dp')
- grad_second_gain: float32 [768], P('dp')
- grad_second_shift: float32 [768], P('dp')
The draws below stay inside these ranges and needn't reach their ends.
Inputs may be any that keep to these rules, and one draw needn't show every extreme that they name: `segment_ids`: within each sequence the segment numbers never fall, and each of the 4 numbers covers 1 to 1024 positions.
All inputs are finite; a program needn't handle non-finite values.
Results may differ from the reference program's by a relative error of at most 0.017.
The reference program's roundings to bfloat16 on the way count: a program that leaves them out, or rounds other values in their place, can miss the bound.
Values may be sent and summed in bfloat16 or wider, within the bound.
A program may use at most 192 MiB of HBM per device.

```python
import math
import jax
import jax.numpy as jnp
import numpy as np
from jax import lax

D = 768
H = 12
HD = 64
FF = 3072
L = 2048
DOCS = 4
SEQS = 16


def spiked(drawn, rng, source, target, shards_of, factor):
    def block_of(position):
        return (jnp.arange(drawn.shape[position]) // (drawn.shape[position] // shards_of)).reshape((-1,) + (1,) * (drawn.ndim - 1 - position))

    near = jax.random.permutation(rng, shards_of)[block_of(target)]
    far = (block_of(target) + shards_of // 2) % shards_of
    return jnp.where((block_of(source) == near) | (block_of(source) == far), factor * drawn, drawn)


def block_scale(rng, extent, split, smallest, top_value):
    def one(position, shards_of):
        steps = jax.random.uniform(jax.random.fold_in(jax.random.fold_in(rng, 6), position), (shards_of,), jnp.float32, smallest / len(split), top_value / len(split))
        return jnp.repeat(jnp.exp(steps), extent[position] // shards_of).reshape((-1,) + (1,) * (len(extent) - position - 1))

    gain = one(*split[0])
    for cut in split[1:]:
        gain = gain * one(*cut)
    return gain


def profile(amount, total, limit, skew):
    loads = [(1 << 20) // math.isqrt(grade ** skew) + 1 for grade in range(2, amount + 1)]
    rest, counts = total - limit - (amount - 1), [1] * (amount - 1)
    while rest > 0:
        candidates = [i for i in range(amount - 1) if counts[i] < limit]
        pool, budget = sum([loads[i] for i in candidates]), rest
        for i in candidates:
            extra = min(limit - counts[i], max(1, budget * loads[i] // pool), rest)
            counts[i] = counts[i] + extra
            rest = rest - extra
    return np.array([limit] + counts)


def uneven(rng, number_of, total, most, skew):
    if number_of == 2:
        one = jax.random.randint(rng, (), max(1, total - most), min(most, total - 1) + 1)
        return jnp.stack([one, total - one])
    tallies = jnp.asarray(profile(number_of, total, most, skew), jnp.int32)
    twos = (number_of - 1) // 2
    giver, receiver = tallies[1:1 + 2 * twos:2], tallies[2:2 + 2 * twos:2]
    margin = jnp.minimum(giver - 1, most - receiver)
    passed = jax.random.randint(jax.random.fold_in(rng, 1), (twos,), 0, 1 << 20) % (margin + 1)
    tallies = tallies.at[1:1 + 2 * twos:2].set(giver - passed).at[2:2 + 2 * twos:2].set(receiver + passed)
    return tallies[jax.random.permutation(jax.random.fold_in(rng, 2), number_of)]


def noise(own_key, shape, spread, reach, shards=(), dtype=jnp.bfloat16):
    entries = jax.random.normal(own_key, shape, jnp.float32) * spread
    if len(shards) > 0:
        entries = block_scale(own_key, shape, shards, -0.22, 0.18) * entries
    return jnp.clip(entries, min=-reach, max=reach).astype(dtype)


def bell_draw_with(stream_key, extent, scale, most, split, heavy, dtype=jnp.bfloat16):
    array = scale * jax.random.normal(stream_key, extent, jnp.float32)
    if split:
        array = array * block_scale(stream_key, extent, split, -0.22, 0.18)
    return jnp.clip(spiked(array, jax.random.fold_in(stream_key, 3), *heavy), -most, most).astype(dtype)


def setup_inputs(seed: int = 0) -> dict:
    key_of = jax.random.split(jax.random.key(seed), 19)
    return {
        "tokens": noise(key_of[0], (SEQS, L, D), 1.0, 6.0, ((0, 8), (1, 4))),
        "segment_ids": jax.vmap(lambda own: jnp.searchsorted(jnp.cumsum(uneven(own, DOCS, L, L // 2, 0)), jnp.arange(L), side="right"))(jax.random.split(key_of[1], SEQS)).reshape((SEQS, L)).astype(jnp.int32),
        "w_query": noise(key_of[2], (D, D), (D // 2) ** -0.5, 0.3125, ((0, 8),), jnp.float32),
        "w_key": noise(key_of[3], (D, D), (D // 2) ** -0.5, 0.3125, ((0, 8),), jnp.float32),
        "w_value": noise(key_of[4], (D, D), D ** -0.5, 0.21875, ((0, 8),), jnp.float32),
        "w_output": noise(key_of[5], (D, D), (D // 16) ** -0.5, 0.875, ((0, 8),), jnp.float32),
        "b_query": noise(key_of[6], (D,), 0.5, 3.0, ((0, 8),), jnp.float32),
        "b_value": noise(key_of[7], (D,), 0.5, 3.0, ((0, 8),), jnp.float32),
        "b_output": noise(key_of[8], (D,), 0.5, 3.0, ((0, 8),), jnp.float32),
        "first_gain": jnp.clip(1.0 + 0.1 * jax.random.normal(key_of[9], (D,), jnp.float32), 0.5, 1.5),
        "first_shift": noise(key_of[10], (D,), 0.5, 3.0, ((0, 8),), jnp.float32),
        "w_inner": noise(key_of[11], (D, FF), D ** -0.5, 0.21875, ((0, 8),), jnp.float32),
        "b_inner": noise(key_of[12], (FF,), 0.5, 3.0, ((0, 8),), jnp.float32),
        "w_outer": noise(key_of[13], (FF, D), FF ** -0.5, 0.109375, ((0, 8),), jnp.float32),
        "b_outer": noise(key_of[14], (D,), 0.5, 3.0, ((0, 8),), jnp.float32),
        "second_gain": jnp.clip(1.0 + 0.1 * jax.random.normal(key_of[15], (D,), jnp.float32), 0.5, 1.5),
        "second_shift": noise(key_of[16], (D,), 0.5, 3.0, ((0, 8),), jnp.float32),
        "cotangent": bell_draw_with(key_of[17], (SEQS, L, D), 1.0, 6.0, ((0, 8), (1, 4)), (0, 2, 8, 2.0)),
    }


@jax.custom_vjp
def low(v):
    return lax.optimization_barrier(v.astype(jnp.bfloat16)).astype(jnp.float32)

@jax.custom_vjp
def low_back(v):
    return v

def low_keep(v):
    return (low(v), None)

def low_pass(kept, grad):
    return (grad,)

def back_keep(v):
    return (v, None)

def back_low(kept, grad):
    return (low(grad),)
low.defvjp(low_keep, low_pass)
low_back.defvjp(back_keep, back_low)
EPS = 1e-12
MASKED = -1000000000.0
ROOT_HALF = 0.7071067811865476

def highest(left, right):
    return jnp.dot(left, right, precision=lax.Precision.HIGHEST, preferred_element_type=jnp.float32)

def normalize(hidden, norm_gain, norm_shift):
    centred = hidden - lax.optimization_barrier(jnp.mean(hidden, axis=-1, keepdims=True))
    variance = lax.optimization_barrier(jnp.mean(centred * centred, axis=-1, keepdims=True))
    return centred * lax.rsqrt(variance + EPS) * norm_gain + norm_shift

def gelu_value(values_in):
    return 0.5 * values_in * (1.0 + lax.erf(values_in * ROOT_HALF))

def layer(params, inputs, segments):
    q_weight, k_weight, v_weight, o_weight, q_bias, v_bias, o_bias, gain_first, shift_first, inner_weight, inner_bias, outer_weight, outer_bias, gain_second, shift_second = tuple((low(piece) for piece in params))
    positions = inputs.shape[0]
    queries = low(low_back(highest(inputs, q_weight) + q_bias))
    key_rows = low(low_back(highest(inputs, k_weight)))
    value_rows = low(low_back(highest(inputs, v_weight) + v_bias))

    def split_heads(matrix):
        return matrix.reshape(positions, H, HD)
    products = jnp.einsum('qhd,khd->hqk', split_heads(queries), split_heads(key_rows), precision=lax.Precision.HIGHEST) * HD ** (-0.5)
    same_doc = segments[:, None] == segments[None, :]
    scores = low_back(jnp.where(same_doc[None], products, MASKED))
    largest = lax.optimization_barrier(jnp.max(scores, axis=-1, keepdims=True))
    exponent = jnp.exp(scores - largest)
    weights = low(exponent / lax.optimization_barrier(jnp.sum(exponent, axis=-1, keepdims=True)))
    context = jnp.einsum('hqk,khd->qhd', weights, split_heads(value_rows), precision=lax.Precision.HIGHEST).reshape(positions, H * HD)
    context = low(low_back(context))
    attended = low_back(highest(context, o_weight) + o_bias)
    first = normalize(inputs + attended, gain_first, shift_first)
    inner = low_back(highest(low(first), inner_weight) + inner_bias)
    active = low(gelu_value(inner))
    outer = low_back(highest(active, outer_weight) + outer_bias)
    return normalize(first + outer, gain_second, shift_second)

def reference(tokens, segment_ids, w_query, w_key, w_value, w_output, b_query, b_value, b_output, first_gain, first_shift, w_inner, b_inner, w_outer, b_outer, second_gain, second_shift, cotangent):
    params = (w_query, w_key, w_value, w_output, b_query, b_value, b_output, first_gain, first_shift, w_inner, b_inner, w_outer, b_outer, second_gain, second_shift)
    token_values = tokens.astype(jnp.float32)
    upstream = cotangent.astype(jnp.float32)

    def one_sequence(totals, item):
        inputs, segments, seq_grad = item
        output, pullback = jax.vjp(lambda pr, xs: layer(pr, xs, segments), params, inputs)
        param_grads, input_grad = pullback(seq_grad)
        totals = jax.tree.map(lambda acc, new: acc + new, totals, param_grads)
        return (totals, (output.astype(jnp.bfloat16), input_grad))
    zeros = tuple((jnp.zeros_like(piece) for piece in params))
    totals, (outputs, input_grads) = lax.scan(one_sequence, zeros, (token_values, segment_ids, upstream))
    return (outputs, input_grads, totals[0], totals[1], totals[2], totals[3], totals[4], totals[5], totals[6], totals[7], totals[8], totals[9], totals[10], totals[11], totals[12], totals[13], totals[14])
```

```python
import jax
import jax.numpy as jnp
from jax import lax
from jax.experimental import pallas as pl
from jax.experimental.pallas import tpu as pltpu
from jax.sharding import Mesh
from jax.sharding import PartitionSpec as P

BLK = 256
BIG = -1.0e9

def dot_nt(a, b):
    return lax.dot_general(a, b, (((1,), (1,)), ((), ())), preferred_element_type=jnp.float32)

def dot_nn(a, b):
    return jnp.dot(a, b, preferred_element_type=jnp.float32)

def half_lanes(rows):
    return lax.broadcasted_iota(jnp.int32, (rows, 128), 1) < 64

def part_rows(place_ref, part, rows):
    return pl.ds(pl.multiple_of(place_ref[part], 128), rows)

def forward_kernel(place_ref, start_ref, count_ref, qkv_ref, ohq_ref, nohk_ref, ctx_ref, lse_ref, q2, k2, vt, acc, top, tot):
    length = qkv_ref.shape[0]
    blocks = length // BLK
    part = length // 4
    low = half_lanes(part)
    for b in range(4):
        src = part_rows(place_ref, b, part)
        dst = slice(b * part, (b + 1) * part)
        q, k = qkv_ref[src, 0:128], qkv_ref[src, 128:256]
        ohq, nohk = ohq_ref[dst, :], nohk_ref[dst, :]
        q2[0, dst, :] = jnp.where(low, q, ohq)
        q2[1, dst, :] = jnp.where(low, ohq, q)
        k2[0, dst, :] = jnp.where(low, k, nohk)
        k2[1, dst, :] = jnp.where(low, nohk, k)
        vt[:, dst] = qkv_ref[src, 256:384].T
    lse_ref[...] = jnp.zeros_like(lse_ref)

    def row(qb, _):
        qs = pl.ds(pl.multiple_of(qb * BLK, BLK), BLK)
        acc[...] = jnp.zeros_like(acc)
        top[...] = jnp.full_like(top, -1.0e30)
        tot[...] = jnp.zeros_like(tot)
        start, count = start_ref[qb], count_ref[qb]

        def tiles(first, number):
            spans = [pl.ds(pl.multiple_of(first + i * BLK, 128), BLK) for i in range(number)]
            for h in range(2):
                rows = slice(64 * h, 64 * h + 64)
                sts = [dot_nt(k2[h, ks, :], q2[h, qs, :]) for ks in spans]
                before = top[h : h + 1, :]
                after = before
                for st in sts:
                    after = jnp.maximum(after, jnp.max(st, axis=0, keepdims=True))
                alpha = jnp.exp(before - after)
                total = tot[h : h + 1, :] * alpha
                result = acc[rows, :] * alpha
                for ks, st in zip(spans, sts):
                    p = jnp.exp(st - after)
                    total = total + jnp.sum(p, axis=0, keepdims=True)
                    result = result + dot_nn(vt[rows, ks], p.astype(jnp.bfloat16))
                top[h : h + 1, :] = after
                tot[h : h + 1, :] = total
                acc[rows, :] = result

        def two(i, _):
            tiles(start + i * (2 * BLK), 2)
            return 0

        lax.fori_loop(0, count // 2, two, 0)

        @pl.when(count % 2 == 1)
        def _():
            tiles(start + (count - 1) * BLK, 1)

        for h in range(2):
            rows = slice(64 * h, 64 * h + 64)
            total = tot[h : h + 1, :]
            acc[rows, :] = acc[rows, :] / total
            lse_ref[h : h + 1, qs] = top[h : h + 1, :] + jnp.log(total)
        where = pl.ds(pl.multiple_of(place_ref[qb * BLK // part] + qb * BLK % part, BLK), BLK)
        ctx_ref[where, :] = acc[...].T.astype(jnp.bfloat16)
        return 0

    lax.fori_loop(0, blocks, row, 0)

def attention(place, start, count, qkv, ohq, nohk):
    length, width = qkv.shape
    pairs = width // 384
    return pl.pallas_call(
        forward_kernel,
        out_shape=(
            jax.ShapeDtypeStruct((length, pairs * 128), jnp.bfloat16),
            jax.ShapeDtypeStruct((pairs * 8, length), jnp.float32),
        ),
        grid_spec=pltpu.PrefetchScalarGridSpec(
            num_scalar_prefetch=3,
            grid=(pairs,),
            in_specs=[
                pl.BlockSpec((length, 384), lambda p, *_: (0, p)),
                pl.BlockSpec((length, 128), lambda p, *_: (0, 0)),
                pl.BlockSpec((length, 128), lambda p, *_: (0, 0)),
            ],
            out_specs=[
                pl.BlockSpec((length, 128), lambda p, *_: (0, p)),
                pl.BlockSpec((8, length), lambda p, *_: (p, 0)),
            ],
            scratch_shapes=[
                pltpu.VMEM((2, length, 128), jnp.bfloat16),
                pltpu.VMEM((2, length, 128), jnp.bfloat16),
                pltpu.VMEM((128, length), jnp.bfloat16),
                pltpu.VMEM((128, BLK), jnp.float32),
                pltpu.VMEM((8, BLK), jnp.float32),
                pltpu.VMEM((8, BLK), jnp.float32),
            ],
        ),
        compiler_params=pltpu.CompilerParams(dimension_semantics=("arbitrary",), vmem_limit_bytes=60 << 20),
        cost_estimate=pl.CostEstimate(flops=pairs * 8_000_000_000, bytes_accessed=pairs * 3_000_000, transcendentals=pairs * 4_000_000),
        name="attention_forward",
    )(place, start, count, qkv, ohq, nohk)

def backward_kernel(place_ref, start_ref, count_ref, qkv_ref, ctx_ref, do_ref, lse_ref, ohq_ref, nohk_ref, out_ref, q2, k2, q0, d0, v0, kt, dk, dv, dqt, delta):
    length = qkv_ref.shape[0]
    blocks = length // BLK
    part = length // 4
    low = half_lanes(part)
    for b in range(4):
        src = part_rows(place_ref, b, part)
        dst = slice(b * part, (b + 1) * part)
        q, k, do = qkv_ref[src, 0:128], qkv_ref[src, 128:256], do_ref[src, :]
        zero = jnp.zeros_like(q)
        ohq, nohk = ohq_ref[dst, :], nohk_ref[dst, :]
        q2[0, dst, :] = jnp.where(low, q, ohq)
        q2[1, dst, :] = jnp.where(low, ohq, q)
        k2[0, dst, :] = jnp.where(low, k, nohk)
        k2[1, dst, :] = jnp.where(low, nohk, k)
        q0[0, dst, :] = jnp.where(low, q, zero)
        q0[1, dst, :] = jnp.where(low, zero, q)
        d0[0, dst, :] = jnp.where(low, do, zero)
        d0[1, dst, :] = jnp.where(low, zero, do)
        v0[dst, :] = qkv_ref[src, 256:384]
        kt[:, dst] = k.T
        prod = (do.astype(jnp.float32) * ctx_ref[src, :].astype(jnp.float32)).T
        delta[0:1, dst] = jnp.sum(prod[0:64], axis=0, keepdims=True)
        delta[1:2, dst] = jnp.sum(prod[64:128], axis=0, keepdims=True)
    dk[...] = jnp.zeros_like(dk)
    dv[...] = jnp.zeros_like(dv)
    dqt[...] = jnp.zeros_like(dqt)

    def row(qb, _):
        qs = pl.ds(pl.multiple_of(qb * BLK, BLK), BLK)
        start, count = start_ref[qb], count_ref[qb]

        def tiles(first, number):
            spans = [pl.ds(pl.multiple_of(first + i * BLK, 128), BLK) for i in range(number)]
            for h in range(2):
                rows = slice(64 * h, 64 * h + 64)
                for ks in spans:
                    st = dot_nt(k2[h, ks, :], q2[h, qs, :])
                    w = jnp.exp(st - lse_ref[h : h + 1, qs])
                    gw = dot_nt(v0[ks, :], d0[h, qs, :])
                    ds = (w * (gw - delta[h : h + 1, qs])).astype(jnp.bfloat16)
                    dv[ks, :] += dot_nn(w.astype(jnp.bfloat16), d0[h, qs, :])
                    dk[ks, :] += dot_nn(ds, q0[h, qs, :])
                    dqt[rows, qs] += dot_nn(kt[rows, ks], ds)

        def two(i, _):
            tiles(start + i * (2 * BLK), 2)
            return 0

        lax.fori_loop(0, count // 2, two, 0)

        @pl.when(count % 2 == 1)
        def _():
            tiles(start + (count - 1) * BLK, 1)
        return 0

    lax.fori_loop(0, blocks, row, 0)
    for b in range(4):
        dst = part_rows(place_ref, b, part)
        src = slice(b * part, (b + 1) * part)
        out_ref[dst, 0:128] = (dqt[:, src].T * 0.125).astype(jnp.bfloat16)
        out_ref[dst, 128:256] = dk[src, :].astype(jnp.bfloat16)
        out_ref[dst, 256:384] = dv[src, :].astype(jnp.bfloat16)

def attention_back(place, start, count, qkv, ctx, do, lse, ohq, nohk):
    length, width = qkv.shape
    pairs = width // 384
    half = lambda: pltpu.VMEM((2, length, 128), jnp.bfloat16)
    return pl.pallas_call(
        backward_kernel,
        out_shape=jax.ShapeDtypeStruct((length, width), jnp.bfloat16),
        grid_spec=pltpu.PrefetchScalarGridSpec(
            num_scalar_prefetch=3,
            grid=(pairs,),
            in_specs=[
                pl.BlockSpec((length, 384), lambda p, *_: (0, p)),
                pl.BlockSpec((length, 128), lambda p, *_: (0, p)),
                pl.BlockSpec((length, 128), lambda p, *_: (0, p)),
                pl.BlockSpec((8, length), lambda p, *_: (p, 0)),
                pl.BlockSpec((length, 128), lambda p, *_: (0, 0)),
                pl.BlockSpec((length, 128), lambda p, *_: (0, 0)),
            ],
            out_specs=pl.BlockSpec((length, 384), lambda p, *_: (0, p)),
            scratch_shapes=[
                half(), half(), half(), half(),
                pltpu.VMEM((length, 128), jnp.bfloat16),
                pltpu.VMEM((128, length), jnp.bfloat16),
                pltpu.VMEM((length, 128), jnp.float32),
                pltpu.VMEM((length, 128), jnp.float32),
                pltpu.VMEM((128, length), jnp.float32),
                pltpu.VMEM((8, length), jnp.float32),
            ],
        ),
        compiler_params=pltpu.CompilerParams(dimension_semantics=("arbitrary",), vmem_limit_bytes=60 << 20),
        cost_estimate=pl.CostEstimate(flops=pairs * 20_000_000_000, bytes_accessed=pairs * 5_000_000, transcendentals=pairs * 4_000_000),
        name="attention_backward",
    )(place, start, count, qkv, ctx, do, lse, ohq, nohk)

def masks_of(segments):
    length = segments.shape[0]
    grid = segments.reshape(length // BLK, BLK)
    lo, hi = grid[:, 0], grid[:, -1]
    below = jnp.sum((segments[None, :] < lo[:, None]).astype(jnp.int32), axis=1)
    upto = jnp.sum((segments[None, :] <= hi[:, None]).astype(jnp.int32), axis=1)
    start = below // 128 * 128
    count = (upto - start + BLK - 1) // BLK
    start = jnp.minimum(start, length - count * BLK)
    lane = jnp.arange(128, dtype=jnp.int32) % 64
    same = lane[None, :] == segments[:, None]
    ohq = same.astype(jnp.bfloat16)
    nohk = jnp.where(jnp.logical_and(lane[None, :] < 4, jnp.logical_not(same)), BIG, 0.0).astype(jnp.bfloat16)
    return start, count, ohq, nohk


HD = 64
EPS = 1e-12
ROOT_HALF = 0.7071067811865476
INV_ROOT_TAU = 0.3989422804014327


def lowered(piece):
    return piece.astype(jnp.bfloat16)


def widen(piece):
    return piece.astype(jnp.float32)


def matmul(left, right):
    return jnp.dot(left, right, preferred_element_type=jnp.float32)


def matmul_tn(left, right):
    return lax.dot_general(
        left, right, (((0,), (0,)), ((), ())), preferred_element_type=jnp.float32
    )


def matmul_nt(left, right):
    return lax.dot_general(
        left, right, (((1,), (1,)), ((), ())), preferred_element_type=jnp.float32
    )


def normalize(hidden, norm_gain, norm_shift):
    centred = hidden - jnp.mean(hidden, axis=-1, keepdims=True)
    reciprocal = lax.rsqrt(jnp.mean(centred * centred, axis=-1, keepdims=True) + EPS)
    normed = centred * reciprocal
    return (normed * norm_gain + norm_shift, normed, reciprocal)


def normalize_back(upstream, normed, reciprocal, norm_gain):
    scaled = upstream * norm_gain
    result = reciprocal * (
        scaled
        - jnp.mean(scaled, axis=-1, keepdims=True)
        - normed * jnp.mean(scaled * normed, axis=-1, keepdims=True)
    )
    return (result, jnp.sum(upstream * normed, axis=0), jnp.sum(upstream, axis=0))


def gelu_value(values_in):
    return 0.5 * values_in * (1.0 + lax.erf(values_in * ROOT_HALF))


def gelu_slope(values_in):
    return (
        0.5 * (1.0 + lax.erf(values_in * ROOT_HALF))
        + values_in * jnp.exp(-0.5 * values_in * values_in) * INV_ROOT_TAU
    )


def shift(piece, axis, step):
    size = lax.axis_size(axis)
    return lax.ppermute(piece, axis, [(i, (i + step) % size) for i in range(size)])


def swap(piece, axis):
    return lax.ppermute(piece, axis, [(0, 1), (1, 0)])


def pick(piece, index, axis=0):
    return lax.dynamic_index_in_dim(piece, index, axis, keepdims=False)


def in_order(first_is_zero, own, other, axis):
    return jnp.where(
        first_is_zero,
        jnp.concatenate([own, other], axis),
        jnp.concatenate([other, own], axis),
    )


def collect(piece):
    size_z, size_x = lax.axis_size("z"), lax.axis_size("x")
    z, x = lax.axis_index("z"), lax.axis_index("x")
    along_z = [piece] + [shift(piece, "z", k) for k in range(1, size_z)]
    whole = jnp.zeros((size_z, size_x) + piece.shape, piece.dtype)
    zeros = (0,) * piece.ndim
    for j in range(size_x):
        for k in range(size_z):
            arrived = along_z[k] if j == 0 else shift(along_z[k], "x", j)
            place = ((z - k) % size_z, (x - j) % size_x) + zeros
            whole = lax.dynamic_update_slice(whole, arrived[None, None], place)
    return whole.reshape((size_z * size_x,) + piece.shape)


def reduce_owned(terms):
    size_z, size_x = lax.axis_size("z"), lax.axis_size("x")
    z, x = lax.axis_index("z"), lax.axis_index("x")
    terms = terms.reshape((size_z, size_x) + terms.shape[1:])
    total = widen(pick(terms, x, 1))
    for j in range(1, size_x):
        total = total + widen(shift(pick(terms, (x + j) % size_x, 1), "x", j))
    terms = lowered(total)
    total = widen(pick(terms, z))
    for k in range(1, size_z):
        total = total + widen(shift(pick(terms, (z + k) % size_z), "z", k))
    terms = lowered(total)
    return widen(terms) + widen(swap(terms, "y"))


def body(
    tokens,
    segment_ids,
    w_query,
    w_key,
    w_value,
    w_output,
    b_query,
    b_value,
    b_output,
    first_gain,
    first_shift,
    w_inner,
    b_inner,
    w_outer,
    b_outer,
    second_gain,
    second_shift,
    cotangent,
):
    core, y = lax.axis_index("core"), lax.axis_index("y")
    shards = lax.axis_size("z") * lax.axis_size("x")
    sequences, part, width = tokens.shape
    half = width // 2
    pairs = half // 128
    hidden = w_inner.shape[1]
    local = 2 * part
    own_rows = w_query.shape[0]
    unit_half = hidden // shards // 2

    def columns(matrix):
        return lowered(lax.dynamic_slice_in_dim(matrix, core * half, half, 1))

    vectors = (b_query, b_value, b_output, first_gain, first_shift, b_inner, b_outer, second_gain, second_shift)
    flat = jnp.concatenate([lowered(v) for v in vectors])
    lanes = 3 * half
    extra = -(-flat.shape[0] // lanes)
    flat = jnp.pad(flat, (0, extra * lanes - flat.shape[0])).reshape(extra, lanes)
    weights = jnp.stack([columns(w).reshape(own_rows, pairs, 128) for w in (w_query, w_key, w_value)], axis=2)
    early = collect(jnp.concatenate([weights.reshape(own_rows, lanes), flat], axis=0))

    mine = pick(tokens, y)
    arrived = swap(pick(tokens, 1 - y), "y")
    mine_other, arrived_other = swap(mine, "core"), swap(arrived, "core")
    inputs_all = jnp.concatenate([mine, arrived, mine_other, arrived_other], axis=0)
    inputs = jnp.concatenate([mine, arrived], axis=0)

    inner_piece = lowered(pick(w_inner.reshape(own_rows, shards, 2, unit_half), core, 2)).reshape(own_rows, hidden // 2)
    late = collect(jnp.concatenate([columns(w_output), inner_piece], axis=1)).reshape(width, half + hidden // 2)
    outer_own = collect(lowered(lax.dynamic_slice_in_dim(w_outer, core * unit_half, unit_half, 0))).reshape(hidden // 2, width)
    output_own, inner_own = late[:, :half], late[:, half:]
    output_other, inner_other, outer_other = swap(output_own, "core"), swap(inner_own, "core"), swap(outer_own, "core")
    full_output = in_order(core == 0, output_own, output_other, 1)
    cotangent_mine = pick(cotangent, y)
    cotangent_arrived = swap(pick(cotangent, 1 - y), "y")

    full_early = early[:, :own_rows].reshape(width, lanes)
    flat_all = early[:, own_rows:].reshape(shards, extra * lanes)
    sizes = [v.shape[0] for v in vectors]
    gathered, at = [], 0
    for size in sizes:
        gathered.append(flat_all[:, at : at + size].reshape(shards * size))
        at += size
    bias_query, bias_value, bias_output, gain_first, shift_first, bias_inner, bias_outer, gain_second, shift_second = [
        widen(v) for v in gathered
    ]
    heads_query = lax.dynamic_slice_in_dim(bias_query, core * half, half).reshape(pairs, 1, 128)
    heads_value = lax.dynamic_slice_in_dim(bias_value, core * half, half).reshape(pairs, 1, 128)
    bias_all = jnp.concatenate([heads_query, jnp.zeros_like(heads_query), heads_value], axis=1).reshape(lanes)
    scale = jnp.tile(jnp.concatenate([jnp.full((128,), HD ** (-0.5)), jnp.ones((256,))]), pairs)
    projected = lowered((matmul(inputs_all, full_early) + bias_all) * scale)

    start, count, mark_query, mark_key = masks_of(pick(segment_ids, y))
    spot = jnp.arange(4, dtype=jnp.int32)
    place = ((spot % 2 != core) * 2 + (spot // 2 != y) * 1) * part
    context_heads, logsum = attention(place, start, count, projected, mark_query, mark_key)
    context = in_order(core == 0, context_heads[:local], swap(context_heads[local:], "core"), 1)

    attended = matmul(context, full_output) + bias_output
    first, first_normed, first_recip = normalize(widen(inputs) + attended, gain_first, shift_first)
    first_low = lowered(first)
    biases = bias_inner.reshape(shards, 2, unit_half)
    halves = ((inner_own, outer_own, pick(biases, core, 1)), (inner_other, outer_other, pick(biases, 1 - core, 1)))
    outer, kept = bias_outer, []
    for inner_weight, outer_weight, bias in halves:
        inner = matmul(first_low, inner_weight) + bias.reshape(hidden // 2)
        active = lowered(gelu_value(inner))
        outer = outer + matmul(active, outer_weight)
        kept.append((inner, active))
    mixed, second_normed, second_recip = normalize(first + outer, gain_second, shift_second)
    mixed = lowered(mixed)

    upstream = widen(jnp.concatenate([cotangent_mine, cotangent_arrived], axis=0))
    pre_second, grad_second_gain, grad_second_shift = normalize_back(upstream, second_normed, second_recip, gain_second)
    grad_outer = lowered(pre_second)
    grad_b_outer = jnp.sum(widen(grad_outer), axis=0)
    grad_first, inner_grads, outer_grads, bias_grads = pre_second, [], [], []
    for (inner, active), (inner_weight, outer_weight, _) in zip(kept, halves):
        grad_inner = lowered(matmul_nt(grad_outer, outer_weight) * gelu_slope(inner))
        outer_grads.append(lowered(matmul_tn(active, grad_outer)))
        inner_grads.append(lowered(matmul_tn(first_low, grad_inner)))
        bias_grads.append(jnp.sum(widen(grad_inner), axis=0).reshape(shards, 1, unit_half))
        grad_first = grad_first + matmul_nt(grad_inner, inner_weight)
    grad_b_inner = in_order(core == 0, bias_grads[0], bias_grads[1], 1).reshape(hidden)
    pre_first, grad_first_gain, grad_first_shift = normalize_back(grad_first, first_normed, first_recip, gain_first)
    grad_attended = lowered(pre_first)
    grad_b_output = jnp.sum(widen(grad_attended), axis=0)
    grad_w_output = lowered(matmul_tn(context, grad_attended))
    grad_context = lowered(matmul_nt(grad_attended, full_output))
    context_mine = lax.dynamic_slice_in_dim(grad_context, core * half, half, 1)
    context_other = lax.dynamic_slice_in_dim(grad_context, (1 - core) * half, half, 1)
    upstream_heads = jnp.concatenate([context_mine, swap(context_other, "core")], axis=0)

    def core_sum(own, other):
        return lowered(widen(own) + widen(swap(other, "core")))

    outer_term = core_sum(*outer_grads)
    inner_term = core_sum(*inner_grads)
    output_term = core_sum(
        lax.dynamic_slice_in_dim(grad_w_output, core * half, half, 1),
        lax.dynamic_slice_in_dim(grad_w_output, (1 - core) * half, half, 1),
    )
    outer_done = reduce_owned(outer_term.reshape(shards, unit_half, width))
    late_done = reduce_owned(jnp.concatenate([output_term, inner_term], axis=1).reshape(shards, own_rows, half + hidden // 2))

    grads = attention_back(place, start, count, projected, context_heads, upstream_heads, logsum, mark_query, mark_key)
    grad_early = lowered(matmul_tn(inputs_all, grads))
    partial = matmul_nt(grads, full_early)
    sums = jnp.sum(widen(grads), axis=0).reshape(pairs, 3, 128)
    blank = jnp.zeros((width,), jnp.float32)
    grad_b_query = lax.dynamic_update_slice(blank, sums[:, 0].reshape(half), (core * half,))
    grad_b_value = lax.dynamic_update_slice(blank, sums[:, 2].reshape(half), (core * half,))
    vector_grads = (
        grad_b_query,
        grad_b_value,
        grad_b_output,
        grad_first_gain,
        grad_first_shift,
        grad_b_inner,
        grad_b_outer,
        grad_second_gain,
        grad_second_shift,
    )
    flat_grads = jnp.concatenate([v.reshape(shards, -1) for v in vector_grads], axis=1)
    flat_grads = jnp.pad(flat_grads, ((0, 0), (0, extra * lanes - flat_grads.shape[1])))
    early_term = jnp.concatenate(
        [grad_early.reshape(shards, own_rows, lanes), lowered(flat_grads).reshape(shards, extra, lanes)], axis=1
    )
    early_done = reduce_owned(early_term)

    grad_inputs = pre_first + partial[:local] + widen(swap(lowered(partial[local:]), "core"))
    returned = widen(swap(lowered(grad_inputs[part:]), "y"))
    grad_tokens = in_order(y == 0, grad_inputs[None, :part], returned[None], 0)
    mixed_out = in_order(y == 0, mixed[None, :part], swap(mixed[part:], "y")[None], 0)

    def both(piece):
        return widen(swap(lowered(piece), "core"))

    early_matrix = early_done[:own_rows]
    early_full = in_order(
        core == 0, early_matrix.reshape(own_rows, pairs, 3, 128)[None], both(early_matrix).reshape(own_rows, pairs, 3, 128)[None], 0
    )
    early_full = early_full.transpose(3, 1, 0, 2, 4).reshape(3, own_rows, width)
    late_other = both(late_done)
    output_full = in_order(core == 0, late_done[:, :half], late_other[:, :half], 1)
    inner_full = in_order(
        core == 0,
        late_done[:, half:].reshape(own_rows, shards, 1, unit_half),
        late_other[:, half:].reshape(own_rows, shards, 1, unit_half),
        2,
    ).reshape(own_rows, hidden)
    outer_full = in_order(core == 0, outer_done, both(outer_done), 0)
    vector_part = early_done[own_rows:]
    vector_sums = (vector_part + swap(vector_part, "core")).reshape(extra * lanes)
    out_vectors, at = [], 0
    for size in sizes:
        out_vectors.append(vector_sums[at : at + size])
        at += size
    (
        done_b_query,
        done_b_value,
        done_b_output,
        done_first_gain,
        done_first_shift,
        done_b_inner,
        done_b_outer,
        done_second_gain,
        done_second_shift,
    ) = out_vectors
    return (
        mixed_out,
        grad_tokens,
        early_full[0],
        early_full[1],
        early_full[2],
        output_full,
        done_b_query,
        done_b_value,
        done_b_output,
        done_first_gain,
        done_first_shift,
        inner_full,
        done_b_inner,
        outer_full,
        done_b_outer,
        done_second_gain,
        done_second_shift,
    )


def solution(mesh):
    outer, inner = mesh.devices.shape
    size_z = 1
    while size_z * size_z < outer:
        size_z *= 2
    split = Mesh(mesh.devices.reshape(size_z, outer // size_z, inner // 2, 2), ("z", "x", "y", "core"))
    dp, seq = ("z", "x"), ("y", "core")
    activation, matrix, vector = P(dp, seq, None), P(dp, None), P(dp)
    return jax.shard_map(
        body,
        mesh=split,
        in_specs=(
            activation,
            matrix,
            matrix,
            matrix,
            matrix,
            matrix,
            vector,
            vector,
            vector,
            vector,
            vector,
            matrix,
            vector,
            matrix,
            vector,
            vector,
            vector,
            activation,
        ),
        out_specs=(
            activation,
            activation,
            matrix,
            matrix,
            matrix,
            matrix,
            vector,
            vector,
            vector,
            vector,
            vector,
            matrix,
            vector,
            matrix,
            vector,
            vector,
            vector,
        ),
        check_vma=False,
    )
```

```python
import jax
import jax.numpy as jnp
from jax import lax
from jax.experimental import pallas as pl
from jax.experimental.pallas import tpu as pltpu
from jax.sharding import Mesh
from jax.sharding import PartitionSpec as P

BLK = 256
BIG = -1.0e9

def dot_nt(a, b):
    return lax.dot_general(a, b, (((1,), (1,)), ((), ())), preferred_element_type=jnp.float32)

def dot_nn(a, b):
    return jnp.dot(a, b, preferred_element_type=jnp.float32)

def half_lanes(rows):
    return lax.broadcasted_iota(jnp.int32, (rows, 128), 1) < 64

def part_rows(place_ref, part, rows):
    return pl.ds(pl.multiple_of(place_ref[part], 128), rows)

def forward_kernel(place_ref, start_ref, count_ref, qkv_ref, ohq_ref, nohk_ref, ctx_ref, lse_ref, q2, k2, vt, acc, top, tot):
    length = qkv_ref.shape[0]
    blocks = length // BLK
    part = length // 4
    low = half_lanes(part)
    for b in range(4):
        src = part_rows(place_ref, b, part)
        dst = slice(b * part, (b + 1) * part)
        q, k = qkv_ref[src, 0:128], qkv_ref[src, 128:256]
        ohq, nohk = ohq_ref[dst, :], nohk_ref[dst, :]
        q2[0, dst, :] = jnp.where(low, q, ohq)
        q2[1, dst, :] = jnp.where(low, ohq, q)
        k2[0, dst, :] = jnp.where(low, k, nohk)
        k2[1, dst, :] = jnp.where(low, nohk, k)
        vt[:, dst] = qkv_ref[src, 256:384].T
    lse_ref[...] = jnp.zeros_like(lse_ref)

    def row(qb, _):
        qs = pl.ds(pl.multiple_of(qb * BLK, BLK), BLK)
        acc[...] = jnp.zeros_like(acc)
        top[...] = jnp.full_like(top, -1.0e30)
        tot[...] = jnp.zeros_like(tot)
        start, count = start_ref[qb], count_ref[qb]

        def tiles(first, number):
            spans = [pl.ds(pl.multiple_of(first + i * BLK, 128), BLK) for i in range(number)]
            for h in range(2):
                rows = slice(64 * h, 64 * h + 64)
                sts = [dot_nt(k2[h, ks, :], q2[h, qs, :]) for ks in spans]
                before = top[h : h + 1, :]
                after = before
                for st in sts:
                    after = jnp.maximum(after, jnp.max(st, axis=0, keepdims=True))
                alpha = jnp.exp(before - after)
                total = tot[h : h + 1, :] * alpha
                result = acc[rows, :] * alpha
                for ks, st in zip(spans, sts):
                    p = jnp.exp(st - after)
                    total = total + jnp.sum(p, axis=0, keepdims=True)
                    result = result + dot_nn(vt[rows, ks], p.astype(jnp.bfloat16))
                top[h : h + 1, :] = after
                tot[h : h + 1, :] = total
                acc[rows, :] = result

        def two(i, _):
            tiles(start + i * (2 * BLK), 2)
            return 0

        lax.fori_loop(0, count // 2, two, 0)

        @pl.when(count % 2 == 1)
        def _():
            tiles(start + (count - 1) * BLK, 1)

        for h in range(2):
            rows = slice(64 * h, 64 * h + 64)
            total = tot[h : h + 1, :]
            acc[rows, :] = acc[rows, :] / total
            lse_ref[h : h + 1, qs] = top[h : h + 1, :] + jnp.log(total)
        where = pl.ds(pl.multiple_of(place_ref[qb * BLK // part] + qb * BLK % part, BLK), BLK)
        ctx_ref[where, :] = acc[...].T.astype(jnp.bfloat16)
        return 0

    lax.fori_loop(0, blocks, row, 0)

def attention(place, start, count, qkv, ohq, nohk):
    length, width = qkv.shape
    pairs = width // 384
    return pl.pallas_call(
        forward_kernel,
        out_shape=(
            jax.ShapeDtypeStruct((length, pairs * 128), jnp.bfloat16),
            jax.ShapeDtypeStruct((pairs * 8, length), jnp.float32),
        ),
        grid_spec=pltpu.PrefetchScalarGridSpec(
            num_scalar_prefetch=3,
            grid=(pairs,),
            in_specs=[
                pl.BlockSpec((length, 384), lambda p, *_: (0, p)),
                pl.BlockSpec((length, 128), lambda p, *_: (0, 0)),
                pl.BlockSpec((length, 128), lambda p, *_: (0, 0)),
            ],
            out_specs=[
                pl.BlockSpec((length, 128), lambda p, *_: (0, p)),
                pl.BlockSpec((8, length), lambda p, *_: (p, 0)),
            ],
            scratch_shapes=[
                pltpu.VMEM((2, length, 128), jnp.bfloat16),
                pltpu.VMEM((2, length, 128), jnp.bfloat16),
                pltpu.VMEM((128, length), jnp.bfloat16),
                pltpu.VMEM((128, BLK), jnp.float32),
                pltpu.VMEM((8, BLK), jnp.float32),
                pltpu.VMEM((8, BLK), jnp.float32),
            ],
        ),
        compiler_params=pltpu.CompilerParams(dimension_semantics=("arbitrary",), vmem_limit_bytes=60 << 20),
        cost_estimate=pl.CostEstimate(flops=pairs * 8_000_000_000, bytes_accessed=pairs * 3_000_000, transcendentals=pairs * 4_000_000),
        name="attention_forward",
    )(place, start, count, qkv, ohq, nohk)

def backward_kernel(place_ref, start_ref, count_ref, qkv_ref, ctx_ref, do_ref, lse_ref, ohq_ref, nohk_ref, out_ref, q2, k2, q0, d0, v0, kt, dk, dv, dqt, delta):
    length = qkv_ref.shape[0]
    blocks = length // BLK
    part = length // 4
    low = half_lanes(part)
    for b in range(4):
        src = part_rows(place_ref, b, part)
        dst = slice(b * part, (b + 1) * part)
        q, k, do = qkv_ref[src, 0:128], qkv_ref[src, 128:256], do_ref[src, :]
        zero = jnp.zeros_like(q)
        ohq, nohk = ohq_ref[dst, :], nohk_ref[dst, :]
        q2[0, dst, :] = jnp.where(low, q, ohq)
        q2[1, dst, :] = jnp.where(low, ohq, q)
        k2[0, dst, :] = jnp.where(low, k, nohk)
        k2[1, dst, :] = jnp.where(low, nohk, k)
        q0[0, dst, :] = jnp.where(low, q, zero)
        q0[1, dst, :] = jnp.where(low, zero, q)
        d0[0, dst, :] = jnp.where(low, do, zero)
        d0[1, dst, :] = jnp.where(low, zero, do)
        v0[dst, :] = qkv_ref[src, 256:384]
        kt[:, dst] = k.T
        prod = (do.astype(jnp.float32) * ctx_ref[src, :].astype(jnp.float32)).T
        delta[0:1, dst] = jnp.sum(prod[0:64], axis=0, keepdims=True)
        delta[1:2, dst] = jnp.sum(prod[64:128], axis=0, keepdims=True)
    dk[...] = jnp.zeros_like(dk)
    dv[...] = jnp.zeros_like(dv)
    dqt[...] = jnp.zeros_like(dqt)

    def row(qb, _):
        qs = pl.ds(pl.multiple_of(qb * BLK, BLK), BLK)
        start, count = start_ref[qb], count_ref[qb]

        def tiles(first, number):
            spans = [pl.ds(pl.multiple_of(first + i * BLK, 128), BLK) for i in range(number)]
            for h in range(2):
                rows = slice(64 * h, 64 * h + 64)
                for ks in spans:
                    st = dot_nt(k2[h, ks, :], q2[h, qs, :])
                    w = jnp.exp(st - lse_ref[h : h + 1, qs])
                    gw = dot_nt(v0[ks, :], d0[h, qs, :])
                    ds = (w * (gw - delta[h : h + 1, qs])).astype(jnp.bfloat16)
                    dv[ks, :] += dot_nn(w.astype(jnp.bfloat16), d0[h, qs, :])
                    dk[ks, :] += dot_nn(ds, q0[h, qs, :])
                    dqt[rows, qs] += dot_nn(kt[rows, ks], ds)

        def two(i, _):
            tiles(start + i * (2 * BLK), 2)
            return 0

        lax.fori_loop(0, count // 2, two, 0)

        @pl.when(count % 2 == 1)
        def _():
            tiles(start + (count - 1) * BLK, 1)
        return 0

    lax.fori_loop(0, blocks, row, 0)
    for b in range(4):
        dst = part_rows(place_ref, b, part)
        src = slice(b * part, (b + 1) * part)
        out_ref[dst, 0:128] = (dqt[:, src].T * 0.125).astype(jnp.bfloat16)
        out_ref[dst, 128:256] = dk[src, :].astype(jnp.bfloat16)
        out_ref[dst, 256:384] = dv[src, :].astype(jnp.bfloat16)

def attention_back(place, start, count, qkv, ctx, do, lse, ohq, nohk):
    length, width = qkv.shape
    pairs = width // 384
    half = lambda: pltpu.VMEM((2, length, 128), jnp.bfloat16)
    return pl.pallas_call(
        backward_kernel,
        out_shape=jax.ShapeDtypeStruct((length, width), jnp.bfloat16),
        grid_spec=pltpu.PrefetchScalarGridSpec(
            num_scalar_prefetch=3,
            grid=(pairs,),
            in_specs=[
                pl.BlockSpec((length, 384), lambda p, *_: (0, p)),
                pl.BlockSpec((length, 128), lambda p, *_: (0, p)),
                pl.BlockSpec((length, 128), lambda p, *_: (0, p)),
                pl.BlockSpec((8, length), lambda p, *_: (p, 0)),
                pl.BlockSpec((length, 128), lambda p, *_: (0, 0)),
                pl.BlockSpec((length, 128), lambda p, *_: (0, 0)),
            ],
            out_specs=pl.BlockSpec((length, 384), lambda p, *_: (0, p)),
            scratch_shapes=[
                half(), half(), half(), half(),
                pltpu.VMEM((length, 128), jnp.bfloat16),
                pltpu.VMEM((128, length), jnp.bfloat16),
                pltpu.VMEM((length, 128), jnp.float32),
                pltpu.VMEM((length, 128), jnp.float32),
                pltpu.VMEM((128, length), jnp.float32),
                pltpu.VMEM((8, length), jnp.float32),
            ],
        ),
        compiler_params=pltpu.CompilerParams(dimension_semantics=("arbitrary",), vmem_limit_bytes=60 << 20),
        cost_estimate=pl.CostEstimate(flops=pairs * 20_000_000_000, bytes_accessed=pairs * 5_000_000, transcendentals=pairs * 4_000_000),
        name="attention_backward",
    )(place, start, count, qkv, ctx, do, lse, ohq, nohk)

def masks_of(segments):
    length = segments.shape[0]
    grid = segments.reshape(length // BLK, BLK)
    lo, hi = grid[:, 0], grid[:, -1]
    below = jnp.sum((segments[None, :] < lo[:, None]).astype(jnp.int32), axis=1)
    upto = jnp.sum((segments[None, :] <= hi[:, None]).astype(jnp.int32), axis=1)
    start = below // 128 * 128
    count = (upto - start + BLK - 1) // BLK
    start = jnp.minimum(start, length - count * BLK)
    lane = jnp.arange(128, dtype=jnp.int32) % 64
    same = lane[None, :] == segments[:, None]
    ohq = same.astype(jnp.bfloat16)
    nohk = jnp.where(jnp.logical_and(lane[None, :] < 4, jnp.logical_not(same)), BIG, 0.0).astype(jnp.bfloat16)
    return start, count, ohq, nohk


MESH_ID = pl.DeviceIdType.MESH


def place_of():
    return tuple(lax.axis_index(name) for name in ("z", "x", "y", "core"))


def sizes_of():
    return lax.axis_size("z"), lax.axis_size("x")


def partner(**moved):
    z, x, y, core = place_of()
    return (moved.get("z", z), moved.get("x", x), moved.get("y", y), moved.get("core", core))


def greet(with_grid):
    z, x, y, core = place_of()
    size_z, size_x = sizes_of()
    peers = [partner(y=1 - y), partner(core=1 - core)]
    if with_grid:
        peers += [partner(z=lax.rem(z + k, size_z)) for k in range(1, size_z)]
        peers += [partner(x=lax.rem(x + j, size_x)) for j in range(1, size_x)]
    barrier = pltpu.get_barrier_semaphore()
    for peer in peers:
        pl.semaphore_signal(barrier, inc=1, device_id=peer, device_id_type=MESH_ID)
    pl.semaphore_wait(barrier, len(peers))


def remote(src, dst, send, recv, peer):
    return pltpu.make_async_remote_copy(
        src_ref=src, dst_ref=dst, send_sem=send, recv_sem=recv, device_id=peer, device_id_type=MESH_ID
    )


def entry_kernel(size_z, size_x, count, *refs):
    tokens, wq, wk, wv = refs[:4]
    vectors = refs[4 : 4 + count]
    tokens_all, weights_all, vectors_all = refs[4 + count : 7 + count]
    stage, pack, vpack, local_sem, tsend, trecv, zsend, zrecv, xsend, xrecv = refs[7 + count :]
    z, x, y, core = place_of()
    half = pack.shape[1] // 3
    pairs = half // 128
    me = z * size_x + x

    load = pltpu.make_async_copy(tokens.at[y], stage, local_sem.at[0])
    load.start()
    vpack[...] = jnp.zeros_like(vpack)
    for i, vector in enumerate(vectors):
        vpack[i : i + 1, 0 : vector.shape[1]] = vector[...].astype(jnp.bfloat16).astype(jnp.float32)
    for i, weight in enumerate((wq, wk, wv)):
        for p in range(pairs):
            lanes = pl.ds(pl.multiple_of(core * half + p * 128, 128), 128)
            pack[:, (3 * p + i) * 128 : (3 * p + i + 1) * 128] = weight[:, lanes].astype(jnp.bfloat16)
    greet(True)
    across = remote(tokens.at[1 - y], tokens_all.at[1], tsend.at[0], trecv.at[0], partner(y=1 - y))
    across.start()
    along = []
    for k in range(1, size_z):
        peer = partner(z=lax.rem(z + k, size_z))
        along.append(
            (
                remote(pack, weights_all.at[me], zsend.at[0, k - 1], zrecv.at[0, k - 1], peer),
                remote(vpack, vectors_all.at[me], zsend.at[1, k - 1], zrecv.at[1, k - 1], peer),
            )
        )
    beside = remote(tokens.at[y], tokens_all.at[2], tsend.at[1], trecv.at[1], partner(core=1 - core))
    sideways = []

    def forward(k, weights_src, vectors_src):
        slot = lax.rem(z - k + size_z, size_z) * size_x + x
        for j in range(1, size_x):
            peer = partner(x=lax.rem(x + j, size_x))
            first = remote(weights_src, weights_all.at[slot], xsend.at[0, k, j - 1], xrecv.at[0, k, j - 1], peer)
            second = remote(vectors_src, vectors_all.at[slot], xsend.at[1, k, j - 1], xrecv.at[1, k, j - 1], peer)
            first.start()
            second.start()
            sideways.append((first, second))

    forward(0, pack, vpack)
    for first, second in along:
        first.start()
        second.start()
    beside.start()
    keep_weights = pltpu.make_async_copy(pack, weights_all.at[me], local_sem.at[1])
    keep_vectors = pltpu.make_async_copy(vpack, vectors_all.at[me], local_sem.at[2])
    keep_weights.start()
    keep_vectors.start()
    load.wait()
    keep_tokens = pltpu.make_async_copy(stage, tokens_all.at[0], local_sem.at[3])
    keep_tokens.start()
    order = sorted(range(1, size_z), key=lambda k: min(k, size_z - k))
    for k in order:
        first, second = along[k - 1]
        first.wait_recv()
        second.wait_recv()
        slot = lax.rem(z - k + size_z, size_z) * size_x + x
        forward(k, weights_all.at[slot], vectors_all.at[slot])
    across.wait_recv()
    onward = remote(tokens_all.at[1], tokens_all.at[3], tsend.at[2], trecv.at[2], partner(core=1 - core))
    onward.start()
    for first, second in sideways:
        first.wait()
        second.wait()
    for first, second in along:
        first.wait_send()
        second.wait_send()
    across.wait_send()
    beside.wait()
    onward.wait()
    keep_weights.wait()
    keep_vectors.wait()
    keep_tokens.wait()


def entry(size_z, size_x, tokens, wq, wk, wv, vectors):
    _, part, width = tokens.shape
    rows = wq.shape[0]
    lanes = wq.shape[1] // 2 * 3
    longest = max(v.shape[0] for v in vectors)
    shards = size_z * size_x
    anywhere, vmem = pl.BlockSpec(memory_space=pl.ANY), pl.BlockSpec(memory_space=pltpu.VMEM)
    dma = pltpu.SemaphoreType.DMA
    return pl.pallas_call(
        lambda *refs: entry_kernel(size_z, size_x, len(vectors), *refs),
        out_shape=(
            jax.ShapeDtypeStruct((4, part, width), tokens.dtype),
            jax.ShapeDtypeStruct((shards, rows, lanes), jnp.bfloat16),
            jax.ShapeDtypeStruct((shards, 16, longest), jnp.float32),
        ),
        in_specs=[anywhere] + [vmem] * (3 + len(vectors)),
        out_specs=(anywhere, anywhere, anywhere),
        scratch_shapes=[
            pltpu.VMEM((part, width), tokens.dtype),
            pltpu.VMEM((rows, lanes), jnp.bfloat16),
            pltpu.VMEM((16, longest), jnp.float32),
            dma((4,)),
            dma((3,)),
            dma((3,)),
            dma((2, size_z - 1)),
            dma((2, size_z - 1)),
            dma((2, size_z, max(size_x - 1, 1))),
            dma((2, size_z, max(size_x - 1, 1))),
        ],
        compiler_params=pltpu.CompilerParams(collective_id=0, has_side_effects=True, vmem_limit_bytes=20 << 20),
        name="entry",
    )(tokens, wq, wk, wv, *[v.reshape(1, -1) for v in vectors])


def exit_kernel(size_z, size_x, terms, output_term, vector_terms, own_rows, other_rows, *refs):
    token_grads, grad_query, grad_key, grad_value, grad_output, vector_sums = refs[:6]
    refs = refs[6:]
    recv_rows, send_rows, far_rows, odd, xbuf, xvec, zout, zvout, zbuf, zvec, ybuf, yvec, cbuf, cvec = refs[:14]
    tsend, trecv, osend, orecv, xsend, xrecv, zsend, zrecv, ysend, yrecv, csend, crecv = refs[14:]
    z, x, y, core = place_of()
    shards, rows, lanes = terms.shape
    half = output_term.shape[2] // 2
    pairs = half // 128
    part = token_grads.shape[1]
    mine = pl.ds(pl.multiple_of(core * half, 128), half)
    theirs = pl.ds(pl.multiple_of((1 - core) * half, 128), half)
    order = sorted(range(size_z), key=lambda k: -min(k, size_z - k))
    greet(True)

    outputs = remote(output_term.at[:, :, theirs], odd, osend, orecv, partner(core=1 - core))
    outputs.start()
    halves = remote(other_rows, recv_rows, tsend.at[0], trecv.at[0], partner(core=1 - core))
    halves.start()
    sideways = {}

    def send_side(n, k, src, dst):
        for j in range(1, size_x):
            column = lax.rem(x + j, size_x)
            slot = lax.rem(z + k, size_z) * size_x + column
            if n == 1:
                odd[slot] = (odd[slot].astype(jnp.float32) + output_term[slot, :, mine].astype(jnp.float32)).astype(jnp.bfloat16)
            move = remote(src.at[slot], dst(j), xsend.at[n, k, j - 1], xrecv.at[n, k, j - 1], partner(x=column))
            move.start()
            sideways.setdefault((k, j), []).append(move)

    for k in order:
        send_side(0, k, terms, lambda j: xbuf.at[j - 1, k, :, 0:lanes])
        send_side(2, k, vector_terms, lambda j: xvec.at[j - 1, k])
        if k == order[0]:
            outputs.wait()
        send_side(1, k, odd, lambda j: xbuf.at[j - 1, k, :, lanes : lanes + half])

    halves.wait()
    for i in (1, 0):
        block = slice(i * part, (i + 1) * part)
        summed = own_rows[block, :] + recv_rows[block, :].astype(jnp.float32)
        if i == 1:
            send_rows[...] = summed.astype(jnp.bfloat16)
            back = remote(send_rows, far_rows, tsend.at[1], trecv.at[1], partner(y=1 - y))
            back.start()
        else:
            token_grads[y] = summed

    along = {}
    kept = None
    for k in order:
        target = lax.rem(z + k, size_z)
        slot = target * size_x + x
        total = terms[slot].astype(jnp.float32)
        total_out = odd[slot].astype(jnp.float32) + output_term[slot, :, mine].astype(jnp.float32)
        total_vec = vector_terms[slot]
        for j in range(1, size_x):
            for move in sideways[k, j]:
                move.wait()
            total = total + xbuf[j - 1, k, :, 0:lanes].astype(jnp.float32)
            total_out = total_out + xbuf[j - 1, k, :, lanes : lanes + half].astype(jnp.float32)
            total_vec = total_vec + xvec[j - 1, k]
        if k == 0:
            kept = (total, total_out, total_vec)
            continue
        zout[k - 1, :, 0:lanes] = total.astype(jnp.bfloat16)
        zout[k - 1, :, lanes : lanes + half] = total_out.astype(jnp.bfloat16)
        zvout[k - 1] = total_vec
        peer = partner(z=target)
        moves = (
            remote(zout.at[k - 1], zbuf.at[k - 1], zsend.at[0, k - 1], zrecv.at[0, k - 1], peer),
            remote(zvout.at[k - 1], zvec.at[k - 1], zsend.at[1, k - 1], zrecv.at[1, k - 1], peer),
        )
        for move in moves:
            move.start()
        along[k] = moves

    total, total_out, total_vec = kept
    for k in reversed(order):
        if k == 0:
            continue
        for move in along[k]:
            move.wait()
        total = total + zbuf[k - 1, :, 0:lanes].astype(jnp.float32)
        total_out = total_out + zbuf[k - 1, :, lanes : lanes + half].astype(jnp.float32)
        total_vec = total_vec + zvec[k - 1]
    ybuf[0, :, 0:lanes] = total.astype(jnp.bfloat16)
    ybuf[0, :, lanes : lanes + half] = total_out.astype(jnp.bfloat16)
    yvec[0] = total_vec
    moves = (
        remote(ybuf.at[0], ybuf.at[1], ysend.at[0], yrecv.at[0], partner(y=1 - y)),
        remote(yvec.at[0], yvec.at[1], ysend.at[1], yrecv.at[1], partner(y=1 - y)),
    )
    for move in moves:
        move.start()
    for move in moves:
        move.wait()
    cbuf[0] = ybuf[0].astype(jnp.float32) + ybuf[1].astype(jnp.float32)
    cvec[0] = yvec[0] + yvec[1]
    moves = (
        remote(cbuf.at[0], cbuf.at[1], csend.at[0], crecv.at[0], partner(core=1 - core)),
        remote(cvec.at[0], cvec.at[1], csend.at[1], crecv.at[1], partner(core=1 - core)),
    )
    for move in moves:
        move.start()
    back.wait()
    token_grads[1 - y] = far_rows[...].astype(jnp.float32)
    for move in moves:
        move.wait()
    for i in range(2):
        owner = core if i == 0 else 1 - core
        for p in range(pairs):
            place = pl.ds(pl.multiple_of(owner * half + p * 128, 128), 128)
            for n, out in enumerate((grad_query, grad_key, grad_value)):
                out[:, place] = cbuf[i, :, (3 * p + n) * 128 : (3 * p + n + 1) * 128]
        grad_output[:, pl.ds(pl.multiple_of(owner * half, 128), half)] = cbuf[i, :, lanes : lanes + half]
    vector_sums[...] = cvec[0] + cvec[1]


def exit_call(size_z, size_x, terms, output_term, vector_terms, own_rows, other_rows):
    shards, rows, lanes = terms.shape
    width = output_term.shape[2]
    half = width // 2
    part = own_rows.shape[0] // 2
    vrows, vlanes = vector_terms.shape[1:]
    vmem = pl.BlockSpec(memory_space=pltpu.VMEM)
    dma = pltpu.SemaphoreType.DMA
    full = lanes + half
    side = max(size_x - 1, 1)
    low, high = jnp.bfloat16, jnp.float32
    matrix = jax.ShapeDtypeStruct((rows, width), high)
    return pl.pallas_call(
        lambda *refs: exit_kernel(size_z, size_x, *refs),
        out_shape=(
            jax.ShapeDtypeStruct((2, part, width), high),
            matrix,
            matrix,
            matrix,
            matrix,
            jax.ShapeDtypeStruct((vrows, vlanes), high),
        ),
        in_specs=[vmem] * 5,
        out_specs=(vmem,) * 6,
        scratch_shapes=[
            pltpu.VMEM((2 * part, width), low),
            pltpu.VMEM((part, width), low),
            pltpu.VMEM((part, width), low),
            pltpu.VMEM((shards, rows, half), low),
            pltpu.VMEM((side, size_z, rows, full), low),
            pltpu.VMEM((side, size_z, vrows, vlanes), high),
            pltpu.VMEM((size_z - 1, rows, full), low),
            pltpu.VMEM((size_z - 1, vrows, vlanes), high),
            pltpu.VMEM((size_z - 1, rows, full), low),
            pltpu.VMEM((size_z - 1, vrows, vlanes), high),
            pltpu.VMEM((2, rows, full), low),
            pltpu.VMEM((2, vrows, vlanes), high),
            pltpu.VMEM((2, rows, full), high),
            pltpu.VMEM((2, vrows, vlanes), high),
            dma((2,)),
            dma((2,)),
            dma,
            dma,
            dma((3, size_z, side)),
            dma((3, size_z, side)),
            dma((2, size_z - 1)),
            dma((2, size_z - 1)),
            dma((2,)),
            dma((2,)),
            dma((2,)),
            dma((2,)),
        ],
        compiler_params=pltpu.CompilerParams(collective_id=1, has_side_effects=True, vmem_limit_bytes=60 << 20),
        name="exit",
    )(terms, output_term, vector_terms, own_rows, other_rows)


def finish_kernel(inner, outer, grad_inner, grad_outer, ybuf, yvuf, cbuf, cvuf, ysend, yrecv, csend, crecv):
    z, x, y, core = place_of()
    greet(False)
    moves = (
        remote(inner, ybuf, ysend.at[0], yrecv.at[0], partner(y=1 - y)),
        remote(outer, yvuf, ysend.at[1], yrecv.at[1], partner(y=1 - y)),
    )
    for move in moves:
        move.start()
    sources = ((inner, ybuf, cbuf, grad_inner), (outer, yvuf, cvuf, grad_outer))
    onward = []
    for i, (own, far, swap_buf, out) in enumerate(sources):
        moves[i].wait()
        swap_buf[0] = own[...].astype(jnp.float32) + far[...].astype(jnp.float32)
        move = remote(swap_buf.at[0], swap_buf.at[1], csend.at[i], crecv.at[i], partner(core=1 - core))
        move.start()
        onward.append(move)
    for i, (own, far, swap_buf, out) in enumerate(sources):
        onward[i].wait()
        rows = own.shape[0]
        first = core == 0
        out[0:rows, :] = jnp.where(first, swap_buf[0], swap_buf[1])
        out[rows : 2 * rows, :] = jnp.where(first, swap_buf[1], swap_buf[0])


def finish(inner, outer):
    vmem = pl.BlockSpec(memory_space=pltpu.VMEM)
    dma = pltpu.SemaphoreType.DMA
    low, high = jnp.bfloat16, jnp.float32
    return pl.pallas_call(
        finish_kernel,
        out_shape=tuple(jax.ShapeDtypeStruct((2 * a.shape[0], a.shape[1]), high) for a in (inner, outer)),
        in_specs=[vmem] * 2,
        out_specs=(vmem,) * 2,
        scratch_shapes=[
            pltpu.VMEM(inner.shape, low),
            pltpu.VMEM(outer.shape, low),
            pltpu.VMEM((2,) + inner.shape, high),
            pltpu.VMEM((2,) + outer.shape, high),
            dma((2,)),
            dma((2,)),
            dma((2,)),
            dma((2,)),
        ],
        compiler_params=pltpu.CompilerParams(collective_id=2, has_side_effects=True, vmem_limit_bytes=30 << 20),
        name="finish",
    )(inner, outer)


HD = 64
EPS = 1e-12
ROOT_HALF = 0.7071067811865476
INV_ROOT_TAU = 0.3989422804014327


def lowered(piece):
    return piece.astype(jnp.bfloat16)


def widen(piece):
    return piece.astype(jnp.float32)


def matmul(left, right):
    return jnp.dot(left, right, preferred_element_type=jnp.float32)


def matmul_tn(left, right):
    return lax.dot_general(
        left, right, (((0,), (0,)), ((), ())), preferred_element_type=jnp.float32
    )


def matmul_nt(left, right):
    return lax.dot_general(
        left, right, (((1,), (1,)), ((), ())), preferred_element_type=jnp.float32
    )


def normalize(hidden, norm_gain, norm_shift):
    centred = hidden - jnp.mean(hidden, axis=-1, keepdims=True)
    reciprocal = lax.rsqrt(jnp.mean(centred * centred, axis=-1, keepdims=True) + EPS)
    normed = centred * reciprocal
    return (normed * norm_gain + norm_shift, normed, reciprocal)


def normalize_back(upstream, normed, reciprocal, norm_gain):
    scaled = upstream * norm_gain
    result = reciprocal * (
        scaled
        - jnp.mean(scaled, axis=-1, keepdims=True)
        - normed * jnp.mean(scaled * normed, axis=-1, keepdims=True)
    )
    return (result, jnp.sum(upstream * normed, axis=0), jnp.sum(upstream, axis=0))


def gelu_value(values_in):
    return 0.5 * values_in * (1.0 + lax.erf(values_in * ROOT_HALF))


def gelu_slope(values_in):
    return (
        0.5 * (1.0 + lax.erf(values_in * ROOT_HALF))
        + values_in * jnp.exp(-0.5 * values_in * values_in) * INV_ROOT_TAU
    )


def swap(piece, axis):
    return lax.ppermute(piece, axis, [(0, 1), (1, 0)])


def pick(piece, index, axis=0):
    return lax.dynamic_index_in_dim(piece, index, axis, keepdims=False)


def in_order(first_is_zero, own, other, axis):
    return jnp.where(
        first_is_zero,
        jnp.concatenate([own, other], axis),
        jnp.concatenate([other, own], axis),
    )


def body(
    tokens,
    segment_ids,
    w_query,
    w_key,
    w_value,
    w_output,
    b_query,
    b_value,
    b_output,
    first_gain,
    first_shift,
    w_inner,
    b_inner,
    w_outer,
    b_outer,
    second_gain,
    second_shift,
    cotangent,
):
    core, y = lax.axis_index("core"), lax.axis_index("y")
    size_z, size_x = lax.axis_size("z"), lax.axis_size("x")
    shards = size_z * size_x
    everyone = ("z", "x", "core")
    sequences, part, width = tokens.shape
    half = width // 2
    pairs = half // 128
    hidden = w_inner.shape[1]
    local = 2 * part
    own_rows = w_query.shape[0]
    lanes = 3 * half

    def core_rows(matrix):
        rows = matrix.shape[0] // 2
        return lowered(lax.dynamic_slice_in_dim(matrix, core * rows, rows, 0))

    dense = lax.all_gather(jnp.concatenate([core_rows(w_inner), core_rows(w_output)], axis=1), everyone, axis=0, tiled=True)
    full_outer = lax.all_gather(core_rows(w_outer), everyone, axis=0, tiled=True)
    full_inner, full_output = dense[:, :hidden], dense[:, hidden:]

    vectors = (b_query, b_value, b_output, first_gain, first_shift, b_inner, b_outer, second_gain, second_shift)
    sizes = [v.shape[0] for v in vectors]
    tokens_all, early, vectors_all = entry(size_z, size_x, tokens, w_query, w_key, w_value, vectors)
    inputs_all = tokens_all.reshape(4 * part, width)
    full_early = early.reshape(width, lanes)
    inputs = inputs_all[:local]
    cotangent_mine = pick(cotangent, y)
    cotangent_arrived = swap(pick(cotangent, 1 - y), "y")
    bias_query, bias_value, bias_output, gain_first, shift_first, bias_inner, bias_outer, gain_second, shift_second = [
        vectors_all[:, i, :size].reshape(shards * size) for i, size in enumerate(sizes)
    ]
    heads_query = lax.dynamic_slice_in_dim(bias_query, core * half, half).reshape(pairs, 1, 128)
    heads_value = lax.dynamic_slice_in_dim(bias_value, core * half, half).reshape(pairs, 1, 128)
    bias_all = jnp.concatenate([heads_query, jnp.zeros_like(heads_query), heads_value], axis=1).reshape(lanes)
    scale = jnp.tile(jnp.concatenate([jnp.full((128,), HD ** (-0.5)), jnp.ones((256,))]), pairs)
    projected = lowered((matmul(inputs_all, full_early) + bias_all) * scale)

    start, count, mark_query, mark_key = masks_of(pick(segment_ids, y))
    spot = jnp.arange(4, dtype=jnp.int32)
    place = ((spot % 2 != core) * 2 + (spot // 2 != y) * 1) * part
    context_heads, logsum = attention(place, start, count, projected, mark_query, mark_key)
    context = in_order(core == 0, context_heads[:local], swap(context_heads[local:], "core"), 1)

    attended = matmul(context, full_output) + bias_output
    first, first_normed, first_recip = normalize(widen(inputs) + attended, gain_first, shift_first)
    first_low = lowered(first)
    inner = matmul(first_low, full_inner) + bias_inner
    active = lowered(gelu_value(inner))
    outer = matmul(active, full_outer) + bias_outer
    mixed, second_normed, second_recip = normalize(first + outer, gain_second, shift_second)
    mixed = lowered(mixed)

    upstream = widen(jnp.concatenate([cotangent_mine, cotangent_arrived], axis=0))
    pre_second, grad_second_gain, grad_second_shift = normalize_back(upstream, second_normed, second_recip, gain_second)
    grad_outer = lowered(pre_second)
    grad_b_outer = jnp.sum(widen(grad_outer), axis=0)
    outer_done = lax.psum_scatter(lowered(matmul_tn(active, grad_outer)), everyone, scatter_dimension=0, tiled=True)
    grad_inner = lowered(matmul_nt(grad_outer, full_outer) * gelu_slope(inner))
    grad_b_inner = jnp.sum(widen(grad_inner), axis=0)
    inner_done = lax.psum_scatter(lowered(matmul_tn(first_low, grad_inner)), everyone, scatter_dimension=0, tiled=True)
    grad_first = pre_second + matmul_nt(grad_inner, full_inner)
    pre_first, grad_first_gain, grad_first_shift = normalize_back(grad_first, first_normed, first_recip, gain_first)
    grad_attended = lowered(pre_first)
    grad_b_output = jnp.sum(widen(grad_attended), axis=0)
    grad_w_output = lowered(matmul_tn(context, grad_attended))
    grad_context = lowered(matmul_nt(grad_attended, full_output))
    context_mine = lax.dynamic_slice_in_dim(grad_context, core * half, half, 1)
    context_other = lax.dynamic_slice_in_dim(grad_context, (1 - core) * half, half, 1)
    upstream_heads = jnp.concatenate([context_mine, swap(context_other, "core")], axis=0)
    mixed_out = in_order(y == 0, mixed[None, :part], swap(mixed[part:], "y")[None], 0)

    grads = attention_back(place, start, count, projected, context_heads, upstream_heads, logsum, mark_query, mark_key)
    grad_early = lowered(matmul_tn(inputs_all, grads)).reshape(shards, own_rows, lanes)
    own_partial = pre_first + matmul_nt(grads[:local], full_early)
    other_partial = lowered(matmul_nt(grads[local:], full_early))
    sums = jnp.sum(widen(grads), axis=0).reshape(pairs, 3, 128)
    blank = jnp.zeros((width,), jnp.float32)
    grad_b_query = lax.dynamic_update_slice(blank, sums[:, 0].reshape(half), (core * half,))
    grad_b_value = lax.dynamic_update_slice(blank, sums[:, 2].reshape(half), (core * half,))
    vector_grads = (
        grad_b_query,
        grad_b_value,
        grad_b_output,
        grad_first_gain,
        grad_first_shift,
        grad_b_inner,
        grad_b_outer,
        grad_second_gain,
        grad_second_shift,
    )
    longest = vectors_all.shape[2]
    rows = [jnp.pad(v.reshape(shards, 1, -1), ((0, 0), (0, 0), (0, longest - v.shape[0] // shards))) for v in vector_grads]
    rows.append(jnp.zeros((shards, vectors_all.shape[1] - len(rows), longest), jnp.float32))
    vector_terms = jnp.concatenate(rows, axis=1)
    grad_tokens, grad_query, grad_key, grad_value, grad_output, vector_sums = exit_call(
        size_z, size_x, grad_early, grad_w_output.reshape(shards, own_rows, width), vector_terms, own_partial, other_partial
    )
    grad_inner_full, grad_outer_full = finish(inner_done, outer_done)
    done = [vector_sums[i, :size] for i, size in enumerate(sizes)]
    return (
        mixed_out,
        grad_tokens,
        grad_query,
        grad_key,
        grad_value,
        grad_output,
        done[0],
        done[1],
        done[2],
        done[3],
        done[4],
        grad_inner_full,
        done[5],
        grad_outer_full,
        done[6],
        done[7],
        done[8],
    )


def solution(mesh):
    outer, inner = mesh.devices.shape
    size_z = 1
    while size_z * size_z < outer:
        size_z *= 2
    split = Mesh(mesh.devices.reshape(size_z, outer // size_z, inner // 2, 2), ("z", "x", "y", "core"))
    dp, seq = ("z", "x"), ("y", "core")
    activation, matrix, vector = P(dp, seq, None), P(dp, None), P(dp)
    return jax.shard_map(
        body,
        mesh=split,
        in_specs=(
            activation,
            matrix,
            matrix,
            matrix,
            matrix,
            matrix,
            vector,
            vector,
            vector,
            vector,
            vector,
            matrix,
            vector,
            matrix,
            vector,
            vector,
            vector,
            activation,
        ),
        out_specs=(
            activation,
            activation,
            matrix,
            matrix,
            matrix,
            matrix,
            vector,
            vector,
            vector,
            vector,
            vector,
            matrix,
            vector,
            matrix,
            vector,
            vector,
            vector,
        ),
        check_vma=False,
    )
```

```python
import jax
import jax.numpy as jnp
from jax import lax
from jax.experimental import pallas as pl
from jax.experimental.pallas import tpu as pltpu
from jax.sharding import Mesh
from jax.sharding import PartitionSpec as P

BLK = 256
BIG = -1.0e9
DOCUMENTS = 4


def dot_nn(a, b):
    return jnp.dot(a, b, preferred_element_type=jnp.float32)


def part_rows(place_ref, part, rows):
    return pl.ds(pl.multiple_of(place_ref[part], 128), rows)


def find_bounds(segment_ref, bound_ref):
    length = segment_ref.shape[0]
    bound_ref[0] = 0
    bound_ref[DOCUMENTS] = length
    for d in range(1, DOCUMENTS):

        def halve(_, span):
            low, high = span
            middle = (low + high) // 2
            below = segment_ref[jnp.minimum(middle, length - 1)] < d
            inside = low < high
            return (
                jnp.where(jnp.logical_and(inside, below), middle + 1, low),
                jnp.where(jnp.logical_and(inside, jnp.logical_not(below)), middle, high),
            )

        low, _ = lax.fori_loop(0, length.bit_length(), halve, (0, length))
        bound_ref[d] = low


def find_window(segment_ref, bound_ref, qb):
    length = segment_ref.shape[0]
    first = segment_ref[qb * BLK]
    last = segment_ref[qb * BLK + BLK - 1]
    start = bound_ref[first] // 128 * 128
    count = (bound_ref[last + 1] - start + BLK - 1) // BLK
    return jnp.minimum(start, length - count * BLK), count


def make_marks(row_ref, mark_query, mark_key):
    length = mark_query.shape[0]
    step = 512
    for b in range(length // step):
        rows = slice(b * step, (b + 1) * step)
        column = jnp.broadcast_to(row_ref[0:1, rows], (128, step)).T
        lane = lax.broadcasted_iota(jnp.int32, (step, 128), 1) % 64
        same = lane == column
        mark_query[rows, :] = jnp.where(same, 1.0, 0.0).astype(jnp.bfloat16)
        apart = jnp.logical_and(lane < DOCUMENTS, jnp.logical_not(same))
        mark_key[rows, :] = jnp.where(apart, BIG, 0.0).astype(jnp.bfloat16)


def forward_kernel(
    place_ref, segment_ref, qkv_ref, row_ref, mine_ref, other_ref, lse_ref, q2, k2, vt, acc, top, tot, keep, mark_query, mark_key, bound_ref
):
    length = qkv_ref.shape[0]
    blocks = length // BLK
    part = length // 4

    @pl.when(pl.program_id(0) == 0)
    def _():
        find_bounds(segment_ref, bound_ref)
        make_marks(row_ref, mark_query, mark_key)

    low = lax.broadcasted_iota(jnp.int32, (part, 128), 1) < 64
    for b in range(4):
        src = part_rows(place_ref, b, part)
        dst = slice(b * part, (b + 1) * part)
        q, k = qkv_ref[src, 0:128], qkv_ref[src, 128:256]
        ohq, nohk = mark_query[dst, :], mark_key[dst, :]
        q2[0, :, dst] = jnp.where(low, q, ohq).T
        q2[1, :, dst] = jnp.where(low, ohq, q).T
        k2[0, dst, :] = jnp.where(low, k, nohk)
        k2[1, dst, :] = jnp.where(low, nohk, k)
        vt[:, dst] = qkv_ref[src, 256:384].T
    lse_ref[...] = jnp.zeros_like(lse_ref)

    def row(qb, _):
        qs = pl.ds(pl.multiple_of(qb * BLK, BLK), BLK)
        start, count = find_window(segment_ref, bound_ref, qb)
        top[...] = jnp.full_like(top, -1.0e30)

        def span(i):
            return pl.ds(pl.multiple_of(start + i * BLK, 128), BLK)

        def fold(tile, function):
            return function(tile.reshape(BLK // 8, 8, BLK), axis=0)

        def highest(i):
            for h in range(2):
                st = dot_nn(k2[h, span(i), :], q2[h, :, qs])
                keep[h, pl.ds(pl.multiple_of(i * BLK, BLK), BLK), :] = st
                top[h] = jnp.maximum(top[h], fold(st, jnp.max))

        def weigh(i, largest):
            for h in range(2):
                rows = slice(64 * h, 64 * h + 64)
                st = keep[h, pl.ds(pl.multiple_of(i * BLK, BLK), BLK), :]
                p = jnp.exp(st - largest[h])
                tot[h] = tot[h] + fold(p, jnp.sum)
                acc[rows, :] = acc[rows, :] + dot_nn(vt[rows, span(i)], p.astype(jnp.bfloat16))

        def paired(step):
            def two(i, _):
                step(2 * i)
                step(2 * i + 1)
                return 0

            lax.fori_loop(0, count // 2, two, 0)

            @pl.when(count % 2 == 1)
            def _():
                step(count - 1)

        paired(highest)
        largest = [jnp.max(top[h], axis=0, keepdims=True) for h in range(2)]
        acc[...] = jnp.zeros_like(acc)
        tot[...] = jnp.zeros_like(tot)
        paired(lambda i: weigh(i, largest))
        for h in range(2):
            rows = slice(64 * h, 64 * h + 64)
            total = jnp.sum(tot[h], axis=0, keepdims=True)
            acc[rows, :] = acc[rows, :] / total
            lse_ref[h : h + 1, qs] = largest[h] + jnp.log(total)
        where = place_ref[qb * BLK // part] + qb * BLK % part
        result = acc[...].T.astype(jnp.bfloat16)

        @pl.when(where < 2 * part)
        def _():
            mine_ref[pl.ds(pl.multiple_of(where, BLK), BLK), :] = result

        @pl.when(where >= 2 * part)
        def _():
            other_ref[pl.ds(pl.multiple_of(where - 2 * part, BLK), BLK), :] = result

        return 0

    lax.fori_loop(0, blocks, row, 0)


def attention(place, segments, qkv):
    length, width = qkv.shape
    pairs = width // 384
    rows = length // 2
    return pl.pallas_call(
        forward_kernel,
        out_shape=(
            jax.ShapeDtypeStruct((rows, pairs * 128), jnp.bfloat16),
            jax.ShapeDtypeStruct((rows, pairs * 128), jnp.bfloat16),
            jax.ShapeDtypeStruct((pairs * 8, length), jnp.float32),
        ),
        grid_spec=pltpu.PrefetchScalarGridSpec(
            num_scalar_prefetch=2,
            grid=(pairs,),
            in_specs=[
                pl.BlockSpec((length, 384), lambda p, *_: (0, p)),
                pl.BlockSpec((1, length), lambda p, *_: (0, 0)),
            ],
            out_specs=[
                pl.BlockSpec((rows, 128), lambda p, *_: (0, p)),
                pl.BlockSpec((rows, 128), lambda p, *_: (0, p)),
                pl.BlockSpec((8, length), lambda p, *_: (p, 0)),
            ],
            scratch_shapes=[
                pltpu.VMEM((2, 128, length), jnp.bfloat16),
                pltpu.VMEM((2, length, 128), jnp.bfloat16),
                pltpu.VMEM((128, length), jnp.bfloat16),
                pltpu.VMEM((128, BLK), jnp.float32),
                pltpu.VMEM((2, 8, BLK), jnp.float32),
                pltpu.VMEM((2, 8, BLK), jnp.float32),
                pltpu.VMEM((2, length, BLK), jnp.float32),
                pltpu.VMEM((length, 128), jnp.bfloat16),
                pltpu.VMEM((length, 128), jnp.bfloat16),
                pltpu.SMEM((DOCUMENTS + 1,), jnp.int32),
            ],
        ),
        compiler_params=pltpu.CompilerParams(dimension_semantics=("arbitrary",), vmem_limit_bytes=60 << 20),
        cost_estimate=pl.CostEstimate(flops=pairs * 8_000_000_000, bytes_accessed=pairs * 3_000_000, transcendentals=pairs * 4_000_000),
        name="attention_forward",
    )(place, segments, qkv, segments.reshape(1, length))


def backward_kernel(
    place_ref,
    segment_ref,
    qkv_ref,
    ctx_mine_ref,
    ctx_other_ref,
    do_mine_ref,
    do_other_ref,
    lse_ref,
    row_ref,
    out_ref,
    sum_ref,
    q2,
    k2,
    q0,
    d0,
    dt,
    v0,
    kt,
    dk,
    dv,
    dqt,
    delta,
    mark_query,
    mark_key,
    bound_ref,
):
    length = qkv_ref.shape[0]
    blocks = length // BLK
    part = length // 4

    @pl.when(pl.program_id(0) == 0)
    def _():
        find_bounds(segment_ref, bound_ref)
        make_marks(row_ref, mark_query, mark_key)

    low = lax.broadcasted_iota(jnp.int32, (part, 128), 1) < 64

    def prepare(b, do, ctx):
        src = part_rows(place_ref, b, part)
        dst = slice(b * part, (b + 1) * part)
        q, k = qkv_ref[src, 0:128], qkv_ref[src, 128:256]
        zero = jnp.zeros_like(q)
        ohq, nohk = mark_query[dst, :], mark_key[dst, :]
        q2[0, :, dst] = jnp.where(low, q, ohq).T
        q2[1, :, dst] = jnp.where(low, ohq, q).T
        k2[0, dst, :] = jnp.where(low, k, nohk)
        k2[1, dst, :] = jnp.where(low, nohk, k)
        q0[0, dst, :] = jnp.where(low, q, zero)
        q0[1, dst, :] = jnp.where(low, zero, q)
        d0[0, dst, :] = jnp.where(low, do, zero)
        d0[1, dst, :] = jnp.where(low, zero, do)
        dt[0, :, dst] = jnp.where(low, do, zero).T
        dt[1, :, dst] = jnp.where(low, zero, do).T
        v0[dst, :] = qkv_ref[src, 256:384]
        kt[:, dst] = k.T
        prod = (do.astype(jnp.float32) * ctx.astype(jnp.float32)).T
        delta[0:1, dst] = jnp.sum(prod[0:64], axis=0, keepdims=True)
        delta[1:2, dst] = jnp.sum(prod[64:128], axis=0, keepdims=True)

    for b in range(4):

        @pl.when(place_ref[b] < 2 * part)
        def _():
            rows = part_rows(place_ref, b, part)
            prepare(b, do_mine_ref[rows, :], ctx_mine_ref[rows, :])

        @pl.when(place_ref[b] >= 2 * part)
        def _():
            rows = pl.ds(pl.multiple_of(place_ref[b] - 2 * part, 128), part)
            prepare(b, do_other_ref[rows, :], ctx_other_ref[rows, :])

    dk[...] = jnp.zeros_like(dk)
    dv[...] = jnp.zeros_like(dv)
    dqt[...] = jnp.zeros_like(dqt)

    def row(qb, _):
        qs = pl.ds(pl.multiple_of(qb * BLK, BLK), BLK)
        start, count = find_window(segment_ref, bound_ref, qb)

        def tile(i):
            ks = pl.ds(pl.multiple_of(start + i * BLK, 128), BLK)
            for h in range(2):
                rows = slice(64 * h, 64 * h + 64)
                st = dot_nn(k2[h, ks, :], q2[h, :, qs])
                w = jnp.exp(st - lse_ref[h : h + 1, qs])
                gw = dot_nn(v0[ks, :], dt[h, :, qs])
                ds = (w * (gw - delta[h : h + 1, qs])).astype(jnp.bfloat16)
                dv[ks, :] += dot_nn(w.astype(jnp.bfloat16), d0[h, qs, :])
                dk[ks, :] += dot_nn(ds, q0[h, qs, :])
                dqt[rows, qs] += dot_nn(kt[rows, ks], ds)

        def two(i, _):
            tile(2 * i)
            tile(2 * i + 1)
            return 0

        lax.fori_loop(0, count // 2, two, 0)

        @pl.when(count % 2 == 1)
        def _():
            tile(count - 1)

        return 0

    lax.fori_loop(0, blocks, row, 0)
    sums = [jnp.zeros((1, 128), jnp.float32) for _ in range(3)]
    for b in range(4):
        dst = part_rows(place_ref, b, part)
        src = slice(b * part, (b + 1) * part)
        pieces = ((dqt[:, src].T * 0.125).astype(jnp.bfloat16), dk[src, :].astype(jnp.bfloat16), dv[src, :].astype(jnp.bfloat16))
        for i, piece in enumerate(pieces):
            out_ref[dst, 128 * i : 128 * i + 128] = piece
            sums[i] = sums[i] + jnp.sum(piece.astype(jnp.float32), axis=0, keepdims=True)
    sum_ref[...] = jnp.zeros_like(sum_ref)
    for i in range(3):
        sum_ref[0:1, 128 * i : 128 * i + 128] = sums[i]


def attention_back(place, segments, qkv, ctx_mine, ctx_other, do_all, do_other, lse):
    length, width = qkv.shape
    pairs = width // 384
    rows = length // 2
    half = lambda: pltpu.VMEM((2, length, 128), jnp.bfloat16)
    turned = lambda: pltpu.VMEM((2, 128, length), jnp.bfloat16)
    column = pl.BlockSpec((rows, 128), lambda p, *_: (0, p))
    return pl.pallas_call(
        backward_kernel,
        out_shape=(
            jax.ShapeDtypeStruct((length, width), jnp.bfloat16),
            jax.ShapeDtypeStruct((pairs * 8, 384), jnp.float32),
        ),
        grid_spec=pltpu.PrefetchScalarGridSpec(
            num_scalar_prefetch=2,
            grid=(pairs,),
            in_specs=[
                pl.BlockSpec((length, 384), lambda p, *_: (0, p)),
                column,
                column,
                pl.BlockSpec((rows, 128), lambda p, place, seg: (0, place[4] * pairs + p)),
                column,
                pl.BlockSpec((8, length), lambda p, *_: (p, 0)),
                pl.BlockSpec((1, length), lambda p, *_: (0, 0)),
            ],
            out_specs=[
                pl.BlockSpec((length, 384), lambda p, *_: (0, p)),
                pl.BlockSpec((8, 384), lambda p, *_: (p, 0)),
            ],
            scratch_shapes=[
                turned(),
                half(),
                half(),
                half(),
                turned(),
                pltpu.VMEM((length, 128), jnp.bfloat16),
                pltpu.VMEM((128, length), jnp.bfloat16),
                pltpu.VMEM((length, 128), jnp.float32),
                pltpu.VMEM((length, 128), jnp.float32),
                pltpu.VMEM((128, length), jnp.float32),
                pltpu.VMEM((8, length), jnp.float32),
                pltpu.VMEM((length, 128), jnp.bfloat16),
                pltpu.VMEM((length, 128), jnp.bfloat16),
                pltpu.SMEM((DOCUMENTS + 1,), jnp.int32),
            ],
        ),
        compiler_params=pltpu.CompilerParams(dimension_semantics=("arbitrary",), vmem_limit_bytes=60 << 20),
        cost_estimate=pl.CostEstimate(flops=pairs * 20_000_000_000, bytes_accessed=pairs * 5_000_000, transcendentals=pairs * 4_000_000),
        name="attention_backward",
    )(place, segments, qkv, ctx_mine, ctx_other, do_all, do_other, lse, segments.reshape(1, length))


MESH_ID = pl.DeviceIdType.MESH


def place_of():
    return tuple(lax.axis_index(name) for name in ("z", "x", "y", "core"))


def sizes_of():
    return lax.axis_size("z"), lax.axis_size("x")


def partner(**moved):
    z, x, y, core = place_of()
    return (moved.get("z", z), moved.get("x", x), moved.get("y", y), moved.get("core", core))


def greet(with_grid):
    z, x, y, core = place_of()
    size_z, size_x = sizes_of()
    peers = [partner(y=1 - y), partner(core=1 - core)]
    if with_grid:
        peers += [partner(z=lax.rem(z + k, size_z)) for k in range(1, size_z)]
        peers += [partner(x=lax.rem(x + j, size_x)) for j in range(1, size_x)]
    barrier = pltpu.get_barrier_semaphore()
    for peer in peers:
        pl.semaphore_signal(barrier, inc=1, device_id=peer, device_id_type=MESH_ID)
    pl.semaphore_wait(barrier, len(peers))


def remote(src, dst, send, recv, peer):
    return pltpu.make_async_remote_copy(
        src_ref=src, dst_ref=dst, send_sem=send, recv_sem=recv, device_id=peer, device_id_type=MESH_ID
    )


def entry_kernel(size_z, size_x, count, *refs):
    tokens, wq, wk, wv = refs[:4]
    vectors = refs[4 : 4 + count]
    tokens_all, weights_all, vectors_all = refs[4 + count : 7 + count]
    raw = refs[7 + count : 7 + 2 * count]
    stage, wbuf, pack, vpack, local_sem, load_sem, tsend, trecv, zsend, zrecv, xsend, xrecv = refs[7 + 2 * count :]
    z, x, y, core = place_of()
    half = pack.shape[1] // 3
    pairs = half // 128
    me = z * size_x + x

    mine = pl.ds(pl.multiple_of(core * half, 128), half)
    loads = [pltpu.make_async_copy(w.at[:, mine], wbuf.at[i], load_sem.at[i]) for i, w in enumerate((wq, wk, wv))]
    loads += [pltpu.make_async_copy(v, r, load_sem.at[3 + i]) for i, (v, r) in enumerate(zip(vectors, raw))]
    for load in loads:
        load.start()
    load = pltpu.make_async_copy(tokens.at[y], stage, local_sem.at[0])
    load.start()
    vpack[...] = jnp.zeros_like(vpack)
    for copy in loads:
        copy.wait()
    for i, vector in enumerate(raw):
        vpack[i : i + 1, 0 : vector.shape[1]] = vector[...].astype(jnp.bfloat16).astype(jnp.float32)
    for i in range(3):
        for p in range(pairs):
            pack[:, (3 * p + i) * 128 : (3 * p + i + 1) * 128] = wbuf[i, :, p * 128 : (p + 1) * 128].astype(jnp.bfloat16)
    greet(True)
    across = remote(tokens.at[1 - y], tokens_all.at[1], tsend.at[0], trecv.at[0], partner(y=1 - y))
    across.start()
    along = []
    for k in range(1, size_z):
        peer = partner(z=lax.rem(z + k, size_z))
        along.append(
            (
                remote(pack, weights_all.at[me], zsend.at[0, k - 1], zrecv.at[0, k - 1], peer),
                remote(vpack, vectors_all.at[me], zsend.at[1, k - 1], zrecv.at[1, k - 1], peer),
            )
        )
    beside = remote(tokens.at[y], tokens_all.at[2], tsend.at[1], trecv.at[1], partner(core=1 - core))
    sideways = []

    def forward(k, weights_src, vectors_src):
        slot = lax.rem(z - k + size_z, size_z) * size_x + x
        for j in range(1, size_x):
            peer = partner(x=lax.rem(x + j, size_x))
            first = remote(weights_src, weights_all.at[slot], xsend.at[0, k, j - 1], xrecv.at[0, k, j - 1], peer)
            second = remote(vectors_src, vectors_all.at[slot], xsend.at[1, k, j - 1], xrecv.at[1, k, j - 1], peer)
            first.start()
            second.start()
            sideways.append((first, second))

    forward(0, pack, vpack)
    for first, second in along:
        first.start()
        second.start()
    beside.start()
    keep_weights = pltpu.make_async_copy(pack, weights_all.at[me], local_sem.at[1])
    keep_vectors = pltpu.make_async_copy(vpack, vectors_all.at[me], local_sem.at[2])
    keep_weights.start()
    keep_vectors.start()
    load.wait()
    keep_tokens = pltpu.make_async_copy(stage, tokens_all.at[0], local_sem.at[3])
    keep_tokens.start()
    order = sorted(range(1, size_z), key=lambda k: min(k, size_z - k))
    for k in order:
        first, second = along[k - 1]
        first.wait_recv()
        second.wait_recv()
        slot = lax.rem(z - k + size_z, size_z) * size_x + x
        forward(k, weights_all.at[slot], vectors_all.at[slot])
    across.wait_recv()
    onward = remote(tokens_all.at[1], tokens_all.at[3], tsend.at[2], trecv.at[2], partner(core=1 - core))
    onward.start()
    for first, second in sideways:
        first.wait()
        second.wait()
    for first, second in along:
        first.wait_send()
        second.wait_send()
    across.wait_send()
    beside.wait()
    onward.wait()
    keep_weights.wait()
    keep_vectors.wait()
    keep_tokens.wait()


def entry(size_z, size_x, tokens, wq, wk, wv, vectors):
    _, part, width = tokens.shape
    rows = wq.shape[0]
    lanes = wq.shape[1] // 2 * 3
    longest = max(v.shape[0] for v in vectors)
    shards = size_z * size_x
    anywhere = pl.BlockSpec(memory_space=pl.ANY)
    dma = pltpu.SemaphoreType.DMA
    return pl.pallas_call(
        lambda *refs: entry_kernel(size_z, size_x, len(vectors), *refs),
        out_shape=(
            jax.ShapeDtypeStruct((4, part, width), tokens.dtype),
            jax.ShapeDtypeStruct((shards, rows, lanes), jnp.bfloat16),
            jax.ShapeDtypeStruct((shards, 16, longest), jnp.float32),
        ),
        in_specs=[anywhere] * (4 + len(vectors)),
        out_specs=(anywhere, anywhere, anywhere),
        scratch_shapes=[pltpu.VMEM((1, v.shape[0]), v.dtype) for v in vectors]
        + [
            pltpu.VMEM((part, width), tokens.dtype),
            pltpu.VMEM((3, rows, lanes // 3), wq.dtype),
            pltpu.VMEM((rows, lanes), jnp.bfloat16),
            pltpu.VMEM((16, longest), jnp.float32),
            dma((4,)),
            dma((3 + len(vectors),)),
            dma((3,)),
            dma((3,)),
            dma((2, size_z - 1)),
            dma((2, size_z - 1)),
            dma((2, size_z, max(size_x - 1, 1))),
            dma((2, size_z, max(size_x - 1, 1))),
        ],
        compiler_params=pltpu.CompilerParams(collective_id=0, has_side_effects=True, vmem_limit_bytes=20 << 20),
        name="entry",
    )(tokens, wq, wk, wv, *[v.reshape(1, -1) for v in vectors])


def exit_kernel(size_z, size_x, terms, output_term, vector_terms, own_rows, other_rows, *refs):
    token_grads, grad_query, grad_key, grad_value, grad_output, vector_sums = refs[:6]
    refs = refs[6:]
    recv_rows, send_rows, far_rows, odd, xbuf, xvec, zout, zvout, zbuf, zvec, ybuf, yvec, cbuf, cvec = refs[:14]
    tsend, trecv, osend, orecv, xsend, xrecv, zsend, zrecv, ysend, yrecv, csend, crecv = refs[14:]
    z, x, y, core = place_of()
    shards, rows, lanes = terms.shape
    half = output_term.shape[2] // 2
    pairs = half // 128
    part = token_grads.shape[1]
    mine = pl.ds(pl.multiple_of(core * half, 128), half)
    theirs = pl.ds(pl.multiple_of((1 - core) * half, 128), half)
    order = sorted(range(size_z), key=lambda k: -min(k, size_z - k))
    greet(True)

    outputs = remote(output_term.at[:, :, theirs], odd, osend, orecv, partner(core=1 - core))
    outputs.start()
    halves = remote(other_rows, recv_rows, tsend.at[0], trecv.at[0], partner(core=1 - core))
    halves.start()
    sideways = {}

    def send_side(n, k, src, dst):
        for j in range(1, size_x):
            column = lax.rem(x + j, size_x)
            slot = lax.rem(z + k, size_z) * size_x + column
            if n == 1:
                odd[slot] = (odd[slot].astype(jnp.float32) + output_term[slot, :, mine].astype(jnp.float32)).astype(jnp.bfloat16)
            move = remote(src.at[slot], dst(j), xsend.at[n, k, j - 1], xrecv.at[n, k, j - 1], partner(x=column))
            move.start()
            sideways.setdefault((k, j), []).append(move)

    for k in order:
        send_side(0, k, terms, lambda j: xbuf.at[j - 1, k, :, 0:lanes])
        send_side(2, k, vector_terms, lambda j: xvec.at[j - 1, k])
        if k == order[0]:
            outputs.wait()
        send_side(1, k, odd, lambda j: xbuf.at[j - 1, k, :, lanes : lanes + half])

    halves.wait()
    for i in (1, 0):
        block = slice(i * part, (i + 1) * part)
        summed = own_rows[block, :] + recv_rows[block, :].astype(jnp.float32)
        if i == 1:
            send_rows[...] = summed.astype(jnp.bfloat16)
            back = remote(send_rows, far_rows, tsend.at[1], trecv.at[1], partner(y=1 - y))
            back.start()
        else:
            token_grads[y] = summed

    along = {}
    kept = None
    for k in order:
        target = lax.rem(z + k, size_z)
        slot = target * size_x + x
        total = terms[slot].astype(jnp.float32)
        total_out = odd[slot].astype(jnp.float32) + output_term[slot, :, mine].astype(jnp.float32)
        total_vec = vector_terms[slot]
        for j in range(1, size_x):
            for move in sideways[k, j]:
                move.wait()
            total = total + xbuf[j - 1, k, :, 0:lanes].astype(jnp.float32)
            total_out = total_out + xbuf[j - 1, k, :, lanes : lanes + half].astype(jnp.float32)
            total_vec = total_vec + xvec[j - 1, k]
        if k == 0:
            kept = (total, total_out, total_vec)
            continue
        zout[k - 1, :, 0:lanes] = total.astype(jnp.bfloat16)
        zout[k - 1, :, lanes : lanes + half] = total_out.astype(jnp.bfloat16)
        zvout[k - 1] = total_vec
        peer = partner(z=target)
        moves = (
            remote(zout.at[k - 1], zbuf.at[k - 1], zsend.at[0, k - 1], zrecv.at[0, k - 1], peer),
            remote(zvout.at[k - 1], zvec.at[k - 1], zsend.at[1, k - 1], zrecv.at[1, k - 1], peer),
        )
        for move in moves:
            move.start()
        along[k] = moves

    total, total_out, total_vec = kept
    for k in reversed(order):
        if k == 0:
            continue
        for move in along[k]:
            move.wait()
        total = total + zbuf[k - 1, :, 0:lanes].astype(jnp.float32)
        total_out = total_out + zbuf[k - 1, :, lanes : lanes + half].astype(jnp.float32)
        total_vec = total_vec + zvec[k - 1]
    ybuf[0, :, 0:lanes] = total.astype(jnp.bfloat16)
    ybuf[0, :, lanes : lanes + half] = total_out.astype(jnp.bfloat16)
    yvec[0] = total_vec
    moves = (
        remote(ybuf.at[0], ybuf.at[1], ysend.at[0], yrecv.at[0], partner(y=1 - y)),
        remote(yvec.at[0], yvec.at[1], ysend.at[1], yrecv.at[1], partner(y=1 - y)),
    )
    for move in moves:
        move.start()
    for move in moves:
        move.wait()
    cbuf[0] = ybuf[0].astype(jnp.float32) + ybuf[1].astype(jnp.float32)
    cvec[0] = yvec[0] + yvec[1]
    moves = (
        remote(cbuf.at[0], cbuf.at[1], csend.at[0], crecv.at[0], partner(core=1 - core)),
        remote(cvec.at[0], cvec.at[1], csend.at[1], crecv.at[1], partner(core=1 - core)),
    )
    for move in moves:
        move.start()
    back.wait()
    token_grads[1 - y] = far_rows[...].astype(jnp.float32)
    for move in moves:
        move.wait()
    for i in range(2):
        owner = core if i == 0 else 1 - core
        for p in range(pairs):
            place = pl.ds(pl.multiple_of(owner * half + p * 128, 128), 128)
            for n, out in enumerate((grad_query, grad_key, grad_value)):
                out[:, place] = cbuf[i, :, (3 * p + n) * 128 : (3 * p + n + 1) * 128]
        grad_output[:, pl.ds(pl.multiple_of(owner * half, 128), half)] = cbuf[i, :, lanes : lanes + half]
    vector_sums[...] = cvec[0] + cvec[1]


def exit_call(size_z, size_x, terms, output_term, vector_terms, own_rows, other_rows):
    shards, rows, lanes = terms.shape
    width = output_term.shape[2]
    half = width // 2
    part = own_rows.shape[0] // 2
    vrows, vlanes = vector_terms.shape[1:]
    vmem = pl.BlockSpec(memory_space=pltpu.VMEM)
    dma = pltpu.SemaphoreType.DMA
    full = lanes + half
    side = max(size_x - 1, 1)
    low, high = jnp.bfloat16, jnp.float32
    matrix = jax.ShapeDtypeStruct((rows, width), high)
    return pl.pallas_call(
        lambda *refs: exit_kernel(size_z, size_x, *refs),
        out_shape=(
            jax.ShapeDtypeStruct((2, part, width), high),
            matrix,
            matrix,
            matrix,
            matrix,
            jax.ShapeDtypeStruct((vrows, vlanes), high),
        ),
        in_specs=[vmem] * 5,
        out_specs=(vmem,) * 6,
        scratch_shapes=[
            pltpu.VMEM((2 * part, width), low),
            pltpu.VMEM((part, width), low),
            pltpu.VMEM((part, width), low),
            pltpu.VMEM((shards, rows, half), low),
            pltpu.VMEM((side, size_z, rows, full), low),
            pltpu.VMEM((side, size_z, vrows, vlanes), high),
            pltpu.VMEM((size_z - 1, rows, full), low),
            pltpu.VMEM((size_z - 1, vrows, vlanes), high),
            pltpu.VMEM((size_z - 1, rows, full), low),
            pltpu.VMEM((size_z - 1, vrows, vlanes), high),
            pltpu.VMEM((2, rows, full), low),
            pltpu.VMEM((2, vrows, vlanes), high),
            pltpu.VMEM((2, rows, full), high),
            pltpu.VMEM((2, vrows, vlanes), high),
            dma((2,)),
            dma((2,)),
            dma,
            dma,
            dma((3, size_z, side)),
            dma((3, size_z, side)),
            dma((2, size_z - 1)),
            dma((2, size_z - 1)),
            dma((2,)),
            dma((2,)),
            dma((2,)),
            dma((2,)),
        ],
        compiler_params=pltpu.CompilerParams(collective_id=1, has_side_effects=True, vmem_limit_bytes=60 << 20),
        name="exit",
    )(terms, output_term, vector_terms, own_rows, other_rows)


def finish_kernel(inner, outer, grad_inner, grad_outer, ybuf, yvuf, cbuf, cvuf, ysend, yrecv, csend, crecv):
    z, x, y, core = place_of()
    greet(False)
    moves = (
        remote(inner, ybuf, ysend.at[0], yrecv.at[0], partner(y=1 - y)),
        remote(outer, yvuf, ysend.at[1], yrecv.at[1], partner(y=1 - y)),
    )
    for move in moves:
        move.start()
    sources = ((inner, ybuf, cbuf, grad_inner), (outer, yvuf, cvuf, grad_outer))
    onward = []
    for i, (own, far, swap_buf, out) in enumerate(sources):
        moves[i].wait()
        swap_buf[0] = own[...].astype(jnp.float32) + far[...].astype(jnp.float32)
        move = remote(swap_buf.at[0], swap_buf.at[1], csend.at[i], crecv.at[i], partner(core=1 - core))
        move.start()
        onward.append(move)
    for i, (own, far, swap_buf, out) in enumerate(sources):
        onward[i].wait()
        rows = own.shape[0]
        first = core == 0
        out[0:rows, :] = jnp.where(first, swap_buf[0], swap_buf[1])
        out[rows : 2 * rows, :] = jnp.where(first, swap_buf[1], swap_buf[0])


def finish(inner, outer):
    vmem = pl.BlockSpec(memory_space=pltpu.VMEM)
    dma = pltpu.SemaphoreType.DMA
    low, high = jnp.bfloat16, jnp.float32
    return pl.pallas_call(
        finish_kernel,
        out_shape=tuple(jax.ShapeDtypeStruct((2 * a.shape[0], a.shape[1]), high) for a in (inner, outer)),
        in_specs=[vmem] * 2,
        out_specs=(vmem,) * 2,
        scratch_shapes=[
            pltpu.VMEM(inner.shape, low),
            pltpu.VMEM(outer.shape, low),
            pltpu.VMEM((2,) + inner.shape, high),
            pltpu.VMEM((2,) + outer.shape, high),
            dma((2,)),
            dma((2,)),
            dma((2,)),
            dma((2,)),
        ],
        compiler_params=pltpu.CompilerParams(collective_id=2, has_side_effects=True, vmem_limit_bytes=30 << 20),
        name="finish",
    )(inner, outer)


HD = 64
EPS = 1e-12
ROOT_HALF = 0.7071067811865476
INV_ROOT_TAU = 0.3989422804014327


def lowered(piece):
    return piece.astype(jnp.bfloat16)


def widen(piece):
    return piece.astype(jnp.float32)


def matmul(left, right):
    return jnp.dot(left, right, preferred_element_type=jnp.float32)


def matmul_tn(left, right):
    return lax.dot_general(
        left, right, (((0,), (0,)), ((), ())), preferred_element_type=jnp.float32
    )


def matmul_nt(left, right):
    return lax.dot_general(
        left, right, (((1,), (1,)), ((), ())), preferred_element_type=jnp.float32
    )


def normalize(hidden, norm_gain, norm_shift):
    centred = hidden - jnp.mean(hidden, axis=-1, keepdims=True)
    reciprocal = lax.rsqrt(jnp.mean(centred * centred, axis=-1, keepdims=True) + EPS)
    normed = centred * reciprocal
    return (normed * norm_gain + norm_shift, normed, reciprocal)


def normalize_back(upstream, normed, reciprocal, norm_gain):
    scaled = upstream * norm_gain
    result = reciprocal * (
        scaled
        - jnp.mean(scaled, axis=-1, keepdims=True)
        - normed * jnp.mean(scaled * normed, axis=-1, keepdims=True)
    )
    return (result, jnp.sum(upstream * normed, axis=0), jnp.sum(upstream, axis=0))


def gelu_value(values_in):
    return 0.5 * values_in * (1.0 + lax.erf(values_in * ROOT_HALF))


def gelu_slope(values_in):
    return (
        0.5 * (1.0 + lax.erf(values_in * ROOT_HALF))
        + values_in * jnp.exp(-0.5 * values_in * values_in) * INV_ROOT_TAU
    )


def swap(piece, axis):
    return lax.ppermute(piece, axis, [(0, 1), (1, 0)])


def pick(piece, index, axis=0):
    return lax.dynamic_index_in_dim(piece, index, axis, keepdims=False)


def in_order(first_is_zero, own, other, axis):
    return jnp.where(
        first_is_zero,
        jnp.concatenate([own, other], axis),
        jnp.concatenate([other, own], axis),
    )


def body(
    tokens,
    segment_ids,
    w_query,
    w_key,
    w_value,
    w_output,
    b_query,
    b_value,
    b_output,
    first_gain,
    first_shift,
    w_inner,
    b_inner,
    w_outer,
    b_outer,
    second_gain,
    second_shift,
    cotangent,
):
    core, y = lax.axis_index("core"), lax.axis_index("y")
    size_z, size_x = lax.axis_size("z"), lax.axis_size("x")
    shards = size_z * size_x
    everyone = ("z", "x", "core")
    sequences, part, width = tokens.shape
    half = width // 2
    pairs = half // 128
    hidden = w_inner.shape[1]
    local = 2 * part
    own_rows = w_query.shape[0]
    lanes = 3 * half

    stack = hidden // width

    def core_rows(matrix):
        rows = matrix.shape[0] // 2
        return lowered(lax.dynamic_slice_in_dim(matrix, core * rows, rows, 0))

    def side_by_side(matrix, groups):
        rows = matrix.shape[0] // groups // stack
        return matrix.reshape(groups, stack, rows, width).transpose(0, 2, 1, 3).reshape(groups * rows, hidden)

    def stacked(matrix, groups):
        rows = matrix.shape[0] // groups
        return matrix.reshape(groups, rows, stack, width).transpose(0, 2, 1, 3).reshape(groups * rows * stack, width)

    pieces = (core_rows(w_inner), core_rows(w_output), side_by_side(core_rows(w_outer), 1))
    dense = lax.all_gather(jnp.concatenate(pieces, axis=1), everyone, axis=0, tiled=True)
    full_inner, full_output = dense[:, :hidden], dense[:, hidden : hidden + width]
    full_outer = stacked(dense[:, hidden + width :], 2 * shards)

    vectors = (b_query, b_value, b_output, first_gain, first_shift, b_inner, b_outer, second_gain, second_shift)
    sizes = [v.shape[0] for v in vectors]
    tokens_all, early, vectors_all = entry(size_z, size_x, tokens, w_query, w_key, w_value, vectors)
    inputs_all = tokens_all.reshape(4 * part, width)
    full_early = early.reshape(width, lanes)
    inputs = inputs_all[:local]
    cotangent_mine = pick(cotangent, y)
    cotangent_arrived = swap(pick(cotangent, 1 - y), "y")
    bias_query, bias_value, bias_output, gain_first, shift_first, bias_inner, bias_outer, gain_second, shift_second = [
        vectors_all[:, i, :size].reshape(shards * size) for i, size in enumerate(sizes)
    ]
    heads_query = lax.dynamic_slice_in_dim(bias_query, core * half, half).reshape(pairs, 1, 128)
    heads_value = lax.dynamic_slice_in_dim(bias_value, core * half, half).reshape(pairs, 1, 128)
    bias_all = jnp.concatenate([heads_query, jnp.zeros_like(heads_query), heads_value], axis=1).reshape(lanes)
    scale = jnp.tile(jnp.concatenate([jnp.full((128,), HD ** (-0.5)), jnp.ones((256,))]), pairs)
    projected = lowered((matmul(inputs_all, full_early) + bias_all) * scale)

    spot = jnp.arange(5, dtype=jnp.int32)
    place = jnp.where(spot < 4, ((spot % 2 != core) * 2 + (spot // 2 != y) * 1) * part, core)
    segments = pick(segment_ids, y)
    context_mine, context_other, logsum = attention(place, segments, projected)
    context = in_order(core == 0, context_mine, swap(context_other, "core"), 1)

    attended = matmul(context, full_output) + bias_output
    first, first_normed, first_recip = normalize(widen(inputs) + attended, gain_first, shift_first)
    first_low = lowered(first)
    inner = matmul(first_low, full_inner) + bias_inner
    active = lowered(gelu_value(inner))
    outer = matmul(active, full_outer) + bias_outer
    mixed, second_normed, second_recip = normalize(first + outer, gain_second, shift_second)
    mixed = lowered(mixed)

    upstream = widen(jnp.concatenate([cotangent_mine, cotangent_arrived], axis=0))
    pre_second, grad_second_gain, grad_second_shift = normalize_back(upstream, second_normed, second_recip, gain_second)
    grad_outer = lowered(pre_second)
    grad_b_outer = jnp.sum(widen(grad_outer), axis=0)
    outer_term = side_by_side(lowered(matmul_tn(active, grad_outer)), 2 * shards)
    grad_inner = lowered(matmul_nt(grad_outer, full_outer) * gelu_slope(inner))
    grad_b_inner = jnp.sum(widen(grad_inner), axis=0)
    inner_term = lowered(matmul_tn(first_low, grad_inner))
    both_done = lax.psum_scatter(jnp.concatenate([inner_term, outer_term], axis=1), everyone, scatter_dimension=0, tiled=True)
    inner_done, outer_done = both_done[:, :hidden], stacked(both_done[:, hidden:], 1)
    grad_first = pre_second + matmul_nt(grad_inner, full_inner)
    pre_first, grad_first_gain, grad_first_shift = normalize_back(grad_first, first_normed, first_recip, gain_first)
    grad_attended = lowered(pre_first)
    grad_b_output = jnp.sum(widen(grad_attended), axis=0)
    grad_w_output = lowered(matmul_tn(context, grad_attended))
    grad_context = lowered(matmul_nt(grad_attended, full_output))
    context_send = lax.dynamic_slice_in_dim(grad_context, (1 - core) * half, half, 1)
    upstream_other = swap(context_send, "core")
    mixed_out = in_order(y == 0, mixed[None, :part], swap(mixed[part:], "y")[None], 0)

    grads, sums = attention_back(place, segments, projected, context_mine, context_other, grad_context, upstream_other, logsum)
    grad_early = lowered(matmul_tn(inputs_all, grads)).reshape(shards, own_rows, lanes)
    own_partial = pre_first + matmul_nt(grads[:local], full_early)
    other_partial = lowered(matmul_nt(grads[local:], full_early))
    sums = sums.reshape(pairs, 8, 3, 128)[:, 0]
    blank = jnp.zeros((width,), jnp.float32)
    grad_b_query = lax.dynamic_update_slice(blank, sums[:, 0].reshape(half), (core * half,))
    grad_b_value = lax.dynamic_update_slice(blank, sums[:, 2].reshape(half), (core * half,))
    vector_grads = (
        grad_b_query,
        grad_b_value,
        grad_b_output,
        grad_first_gain,
        grad_first_shift,
        grad_b_inner,
        grad_b_outer,
        grad_second_gain,
        grad_second_shift,
    )
    longest = vectors_all.shape[2]
    rows = [jnp.pad(v.reshape(shards, 1, -1), ((0, 0), (0, 0), (0, longest - v.shape[0] // shards))) for v in vector_grads]
    rows.append(jnp.zeros((shards, vectors_all.shape[1] - len(rows), longest), jnp.float32))
    vector_terms = jnp.concatenate(rows, axis=1)
    grad_tokens, grad_query, grad_key, grad_value, grad_output, vector_sums = exit_call(
        size_z, size_x, grad_early, grad_w_output.reshape(shards, own_rows, width), vector_terms, own_partial, other_partial
    )
    grad_inner_full, grad_outer_full = finish(inner_done, outer_done)
    done = [vector_sums[i, :size] for i, size in enumerate(sizes)]
    return (
        mixed_out,
        grad_tokens,
        grad_query,
        grad_key,
        grad_value,
        grad_output,
        done[0],
        done[1],
        done[2],
        done[3],
        done[4],
        grad_inner_full,
        done[5],
        grad_outer_full,
        done[6],
        done[7],
        done[8],
    )


def solution(mesh):
    outer, inner = mesh.devices.shape
    size_z = 1
    while size_z * size_z < outer:
        size_z *= 2
    split = Mesh(mesh.devices.reshape(size_z, outer // size_z, inner // 2, 2), ("z", "x", "y", "core"))
    dp, seq = ("z", "x"), ("y", "core")
    activation, matrix, vector = P(dp, seq, None), P(dp, None), P(dp)
    return jax.shard_map(
        body,
        mesh=split,
        in_specs=(
            activation,
            matrix,
            matrix,
            matrix,
            matrix,
            matrix,
            vector,
            vector,
            vector,
            vector,
            vector,
            matrix,
            vector,
            matrix,
            vector,
            vector,
            vector,
            activation,
        ),
        out_specs=(
            activation,
            activation,
            matrix,
            matrix,
            matrix,
            matrix,
            vector,
            vector,
            vector,
            vector,
            vector,
            matrix,
            vector,
            matrix,
            vector,
            vector,
            vector,
        ),
        check_vma=False,
    )
```

```python
import jax
import jax.numpy as jnp
from jax import lax
from jax.experimental import pallas as pl
from jax.experimental.pallas import tpu as pltpu
from jax.sharding import Mesh
from jax.sharding import PartitionSpec as P


HD = 64
EPS = 1e-12
ROOT_HALF = 0.7071067811865476
INV_ROOT_TAU = 0.3989422804014327

BLK = 256
BIG = -1.0e9
DOCUMENTS = 4


def dot_nn(a, b):
    return jnp.dot(a, b, preferred_element_type=jnp.float32)


def part_rows(place_ref, part, rows):
    return pl.ds(pl.multiple_of(place_ref[part], 128), rows)


def find_bounds(segment_ref, bound_ref):
    length = segment_ref.shape[0]
    bound_ref[0] = 0
    bound_ref[DOCUMENTS] = length
    for d in range(1, DOCUMENTS):

        def halve(_, span):
            low, high = span
            middle = (low + high) // 2
            below = segment_ref[jnp.minimum(middle, length - 1)] < d
            inside = low < high
            return (
                jnp.where(jnp.logical_and(inside, below), middle + 1, low),
                jnp.where(jnp.logical_and(inside, jnp.logical_not(below)), middle, high),
            )

        low, _ = lax.fori_loop(0, length.bit_length(), halve, (0, length))
        bound_ref[d] = low


def find_window(segment_ref, bound_ref, qb):
    length = segment_ref.shape[0]
    first = segment_ref[qb * BLK]
    last = segment_ref[qb * BLK + BLK - 1]
    start = bound_ref[first] // 128 * 128
    count = (bound_ref[last + 1] - start + BLK - 1) // BLK
    return jnp.minimum(start, length - count * BLK), count


def make_marks(row_ref, mark_query, mark_key):
    length = mark_query.shape[0]
    step = 512
    for b in range(length // step):
        rows = slice(b * step, (b + 1) * step)
        column = jnp.broadcast_to(row_ref[0:1, rows], (128, step)).T
        lane = lax.broadcasted_iota(jnp.int32, (step, 128), 1) % 64
        same = lane == column
        mark_query[rows, :] = jnp.where(same, 1.0, 0.0).astype(jnp.bfloat16)
        apart = jnp.logical_and(lane < DOCUMENTS, jnp.logical_not(same))
        mark_key[rows, :] = jnp.where(apart, BIG, 0.0).astype(jnp.bfloat16)


def forward_kernel(
    place_ref, segment_ref, qkv_ref, row_ref, mine_ref, other_ref, lse_ref, q2, k2, vt, acc, top, tot, keep, mark_query, mark_key, bound_ref
):
    length = qkv_ref.shape[0]
    blocks = length // BLK
    part = length // 4

    @pl.when(pl.program_id(0) == 0)
    def _():
        find_bounds(segment_ref, bound_ref)
        make_marks(row_ref, mark_query, mark_key)

    low = lax.broadcasted_iota(jnp.int32, (part, 128), 1) < 64
    for b in range(4):
        src = part_rows(place_ref, b, part)
        dst = slice(b * part, (b + 1) * part)
        q, k = qkv_ref[src, 0:128], qkv_ref[src, 128:256]
        ohq, nohk = mark_query[dst, :], mark_key[dst, :]
        q2[0, :, dst] = jnp.where(low, q, ohq).T
        q2[1, :, dst] = jnp.where(low, ohq, q).T
        k2[0, dst, :] = jnp.where(low, k, nohk)
        k2[1, dst, :] = jnp.where(low, nohk, k)
        vt[:, dst] = qkv_ref[src, 256:384].T
    lse_ref[...] = jnp.zeros_like(lse_ref)

    def row(qb, _):
        qs = pl.ds(pl.multiple_of(qb * BLK, BLK), BLK)
        start, count = find_window(segment_ref, bound_ref, qb)
        top[...] = jnp.full_like(top, -1.0e30)

        def span(i):
            return pl.ds(pl.multiple_of(start + i * BLK, 128), BLK)

        def fold(tile, function):
            return function(tile.reshape(BLK // 8, 8, BLK), axis=0)

        def highest(i):
            for h in range(2):
                st = dot_nn(k2[h, span(i), :], q2[h, :, qs])
                keep[h, pl.ds(pl.multiple_of(i * BLK, BLK), BLK), :] = st
                top[h] = jnp.maximum(top[h], fold(st, jnp.max))

        def weigh(i, largest):
            for h in range(2):
                rows = slice(64 * h, 64 * h + 64)
                st = keep[h, pl.ds(pl.multiple_of(i * BLK, BLK), BLK), :]
                p = jnp.exp(st - largest[h])
                tot[h] = tot[h] + fold(p, jnp.sum)
                acc[rows, :] = acc[rows, :] + dot_nn(vt[rows, span(i)], p.astype(jnp.bfloat16))

        def paired(step):
            def two(i, _):
                step(2 * i)
                step(2 * i + 1)
                return 0

            lax.fori_loop(0, count // 2, two, 0)

            @pl.when(count % 2 == 1)
            def _():
                step(count - 1)

        paired(highest)
        largest = [jnp.max(top[h], axis=0, keepdims=True) for h in range(2)]
        acc[...] = jnp.zeros_like(acc)
        tot[...] = jnp.zeros_like(tot)
        paired(lambda i: weigh(i, largest))
        for h in range(2):
            rows = slice(64 * h, 64 * h + 64)
            total = jnp.sum(tot[h], axis=0, keepdims=True)
            acc[rows, :] = acc[rows, :] / total
            lse_ref[h : h + 1, qs] = largest[h] + jnp.log(total)
        where = place_ref[qb * BLK // part] + qb * BLK % part
        result = acc[...].T.astype(jnp.bfloat16)

        @pl.when(where < 2 * part)
        def _():
            mine_ref[pl.ds(pl.multiple_of(where, BLK), BLK), :] = result

        @pl.when(where >= 2 * part)
        def _():
            other_ref[pl.ds(pl.multiple_of(where - 2 * part, BLK), BLK), :] = result

        return 0

    lax.fori_loop(0, blocks, row, 0)


def attention(place, segments, qkv):
    length, width = qkv.shape
    pairs = width // 384
    rows = length // 2
    return pl.pallas_call(
        forward_kernel,
        out_shape=(
            jax.ShapeDtypeStruct((rows, pairs * 128), jnp.bfloat16),
            jax.ShapeDtypeStruct((rows, pairs * 128), jnp.bfloat16),
            jax.ShapeDtypeStruct((pairs * 8, length), jnp.float32),
        ),
        grid_spec=pltpu.PrefetchScalarGridSpec(
            num_scalar_prefetch=2,
            grid=(pairs,),
            in_specs=[
                pl.BlockSpec((length, 384), lambda p, *_: (0, p)),
                pl.BlockSpec((1, length), lambda p, *_: (0, 0)),
            ],
            out_specs=[
                pl.BlockSpec((rows, 128), lambda p, *_: (0, p)),
                pl.BlockSpec((rows, 128), lambda p, *_: (0, p)),
                pl.BlockSpec((8, length), lambda p, *_: (p, 0)),
            ],
            scratch_shapes=[
                pltpu.VMEM((2, 128, length), jnp.bfloat16),
                pltpu.VMEM((2, length, 128), jnp.bfloat16),
                pltpu.VMEM((128, length), jnp.bfloat16),
                pltpu.VMEM((128, BLK), jnp.float32),
                pltpu.VMEM((2, 8, BLK), jnp.float32),
                pltpu.VMEM((2, 8, BLK), jnp.float32),
                pltpu.VMEM((2, length, BLK), jnp.float32),
                pltpu.VMEM((length, 128), jnp.bfloat16),
                pltpu.VMEM((length, 128), jnp.bfloat16),
                pltpu.SMEM((DOCUMENTS + 1,), jnp.int32),
            ],
        ),
        compiler_params=pltpu.CompilerParams(dimension_semantics=("arbitrary",), vmem_limit_bytes=60 << 20),
        cost_estimate=pl.CostEstimate(flops=pairs * 8_000_000_000, bytes_accessed=pairs * 3_000_000, transcendentals=pairs * 4_000_000),
        name="attention_forward",
    )(place, segments, qkv, segments.reshape(1, length))


def backward_kernel(
    place_ref,
    segment_ref,
    qkv_ref,
    ctx_mine_ref,
    ctx_other_ref,
    do_mine_ref,
    do_other_ref,
    lse_ref,
    row_ref,
    out_ref,
    sum_ref,
    q2,
    k2,
    q0,
    d0,
    dt,
    v0,
    kt,
    dk,
    dv,
    dqt,
    delta,
    mark_query,
    mark_key,
    bound_ref,
):
    length = qkv_ref.shape[0]
    blocks = length // BLK
    part = length // 4

    @pl.when(pl.program_id(0) == 0)
    def _():
        find_bounds(segment_ref, bound_ref)
        make_marks(row_ref, mark_query, mark_key)

    low = lax.broadcasted_iota(jnp.int32, (part, 128), 1) < 64

    def prepare(b, do, ctx):
        src = part_rows(place_ref, b, part)
        dst = slice(b * part, (b + 1) * part)
        q, k = qkv_ref[src, 0:128], qkv_ref[src, 128:256]
        zero = jnp.zeros_like(q)
        ohq, nohk = mark_query[dst, :], mark_key[dst, :]
        q2[0, :, dst] = jnp.where(low, q, ohq).T
        q2[1, :, dst] = jnp.where(low, ohq, q).T
        k2[0, dst, :] = jnp.where(low, k, nohk)
        k2[1, dst, :] = jnp.where(low, nohk, k)
        q0[0, dst, :] = jnp.where(low, q, zero)
        q0[1, dst, :] = jnp.where(low, zero, q)
        d0[0, dst, :] = jnp.where(low, do, zero)
        d0[1, dst, :] = jnp.where(low, zero, do)
        dt[0, :, dst] = jnp.where(low, do, zero).T
        dt[1, :, dst] = jnp.where(low, zero, do).T
        v0[dst, :] = qkv_ref[src, 256:384]
        kt[:, dst] = k.T
        prod = (do.astype(jnp.float32) * ctx.astype(jnp.float32)).T
        delta[0:1, dst] = jnp.sum(prod[0:64], axis=0, keepdims=True)
        delta[1:2, dst] = jnp.sum(prod[64:128], axis=0, keepdims=True)

    for b in range(4):

        @pl.when(place_ref[b] < 2 * part)
        def _():
            rows = part_rows(place_ref, b, part)
            prepare(b, do_mine_ref[rows, :], ctx_mine_ref[rows, :])

        @pl.when(place_ref[b] >= 2 * part)
        def _():
            rows = pl.ds(pl.multiple_of(place_ref[b] - 2 * part, 128), part)
            prepare(b, do_other_ref[rows, :], ctx_other_ref[rows, :])

    dk[...] = jnp.zeros_like(dk)
    dv[...] = jnp.zeros_like(dv)
    dqt[...] = jnp.zeros_like(dqt)

    def row(qb, _):
        qs = pl.ds(pl.multiple_of(qb * BLK, BLK), BLK)
        start, count = find_window(segment_ref, bound_ref, qb)

        def tile(i):
            ks = pl.ds(pl.multiple_of(start + i * BLK, 128), BLK)
            for h in range(2):
                rows = slice(64 * h, 64 * h + 64)
                st = dot_nn(k2[h, ks, :], q2[h, :, qs])
                w = jnp.exp(st - lse_ref[h : h + 1, qs])
                gw = dot_nn(v0[ks, :], dt[h, :, qs])
                ds = (w * (gw - delta[h : h + 1, qs])).astype(jnp.bfloat16)
                dv[ks, :] += dot_nn(w.astype(jnp.bfloat16), d0[h, qs, :])
                dk[ks, :] += dot_nn(ds, q0[h, qs, :])
                dqt[rows, qs] += dot_nn(kt[rows, ks], ds)

        def two(i, _):
            tile(2 * i)
            tile(2 * i + 1)
            return 0

        lax.fori_loop(0, count // 2, two, 0)

        @pl.when(count % 2 == 1)
        def _():
            tile(count - 1)

        return 0

    lax.fori_loop(0, blocks, row, 0)
    sums = [jnp.zeros((1, 128), jnp.float32) for _ in range(3)]
    for b in range(4):
        dst = part_rows(place_ref, b, part)
        src = slice(b * part, (b + 1) * part)
        pieces = ((dqt[:, src].T * 0.125).astype(jnp.bfloat16), dk[src, :].astype(jnp.bfloat16), dv[src, :].astype(jnp.bfloat16))
        for i, piece in enumerate(pieces):
            out_ref[dst, 128 * i : 128 * i + 128] = piece
            sums[i] = sums[i] + jnp.sum(piece.astype(jnp.float32), axis=0, keepdims=True)
    sum_ref[...] = jnp.zeros_like(sum_ref)
    for i in range(3):
        sum_ref[0:1, 128 * i : 128 * i + 128] = sums[i]


def attention_back(place, segments, qkv, ctx_mine, ctx_other, do_mine, do_other, lse):
    length, width = qkv.shape
    pairs = width // 384
    rows = length // 2
    half = lambda: pltpu.VMEM((2, length, 128), jnp.bfloat16)
    turned = lambda: pltpu.VMEM((2, 128, length), jnp.bfloat16)
    column = pl.BlockSpec((rows, 128), lambda p, *_: (0, p))
    return pl.pallas_call(
        backward_kernel,
        out_shape=(
            jax.ShapeDtypeStruct((length, width), jnp.bfloat16),
            jax.ShapeDtypeStruct((pairs * 8, 384), jnp.float32),
        ),
        grid_spec=pltpu.PrefetchScalarGridSpec(
            num_scalar_prefetch=2,
            grid=(pairs,),
            in_specs=[
                pl.BlockSpec((length, 384), lambda p, *_: (0, p)),
                column,
                column,
                column,
                column,
                pl.BlockSpec((8, length), lambda p, *_: (p, 0)),
                pl.BlockSpec((1, length), lambda p, *_: (0, 0)),
            ],
            out_specs=[
                pl.BlockSpec((length, 384), lambda p, *_: (0, p)),
                pl.BlockSpec((8, 384), lambda p, *_: (p, 0)),
            ],
            scratch_shapes=[
                turned(),
                half(),
                half(),
                half(),
                turned(),
                pltpu.VMEM((length, 128), jnp.bfloat16),
                pltpu.VMEM((128, length), jnp.bfloat16),
                pltpu.VMEM((length, 128), jnp.float32),
                pltpu.VMEM((length, 128), jnp.float32),
                pltpu.VMEM((128, length), jnp.float32),
                pltpu.VMEM((8, length), jnp.float32),
                pltpu.VMEM((length, 128), jnp.bfloat16),
                pltpu.VMEM((length, 128), jnp.bfloat16),
                pltpu.SMEM((DOCUMENTS + 1,), jnp.int32),
            ],
        ),
        compiler_params=pltpu.CompilerParams(dimension_semantics=("arbitrary",), vmem_limit_bytes=60 << 20),
        cost_estimate=pl.CostEstimate(flops=pairs * 20_000_000_000, bytes_accessed=pairs * 5_000_000, transcendentals=pairs * 4_000_000),
        name="attention_backward",
    )(place, segments, qkv, ctx_mine, ctx_other, do_mine, do_other, lse, segments.reshape(1, length))


MESH_ID = pl.DeviceIdType.MESH


def place_of():
    return tuple(lax.axis_index(name) for name in ("z", "x", "y", "core"))


def sizes_of():
    return lax.axis_size("z"), lax.axis_size("x")


def partner(**moved):
    z, x, y, core = place_of()
    return (moved.get("z", z), moved.get("x", x), moved.get("y", y), moved.get("core", core))


def greet(with_grid):
    z, x, y, core = place_of()
    size_z, size_x = sizes_of()
    peers = [partner(y=1 - y), partner(core=1 - core)]
    if with_grid:
        peers += [partner(z=lax.rem(z + k, size_z)) for k in range(1, size_z)]
        peers += [partner(x=lax.rem(x + j, size_x)) for j in range(1, size_x)]
    barrier = pltpu.get_barrier_semaphore()
    for peer in peers:
        pl.semaphore_signal(barrier, inc=1, device_id=peer, device_id_type=MESH_ID)
    pl.semaphore_wait(barrier, len(peers))


def remote(src, dst, send, recv, peer):
    return pltpu.make_async_remote_copy(
        src_ref=src, dst_ref=dst, send_sem=send, recv_sem=recv, device_id=peer, device_id_type=MESH_ID
    )


def entry_kernel(size_z, size_x, count, *refs):
    tokens, wq, wk, wv = refs[:4]
    vectors = refs[4 : 4 + count]
    tokens_all, weights_all, vectors_all = refs[4 + count : 7 + count]
    raw = refs[7 + count : 7 + 2 * count]
    stage, wbuf, pack, vpack, local_sem, load_sem, tsend, trecv, zsend, zrecv, xsend, xrecv = refs[7 + 2 * count :]
    z, x, y, core = place_of()
    half = pack.shape[1] // 3
    pairs = half // 128
    me = z * size_x + x

    mine = pl.ds(pl.multiple_of(core * half, 128), half)
    loads = [pltpu.make_async_copy(w.at[:, mine], wbuf.at[i], load_sem.at[i]) for i, w in enumerate((wq, wk, wv))]
    loads += [pltpu.make_async_copy(v, r, load_sem.at[3 + i]) for i, (v, r) in enumerate(zip(vectors, raw))]
    for load in loads:
        load.start()
    load = pltpu.make_async_copy(tokens.at[y], stage, local_sem.at[0])
    load.start()
    vpack[...] = jnp.zeros_like(vpack)
    for copy in loads:
        copy.wait()
    for i, vector in enumerate(raw):
        vpack[i : i + 1, 0 : vector.shape[1]] = vector[...].astype(jnp.bfloat16).astype(jnp.float32)
    for i in range(3):
        for p in range(pairs):
            pack[:, (3 * p + i) * 128 : (3 * p + i + 1) * 128] = wbuf[i, :, p * 128 : (p + 1) * 128].astype(jnp.bfloat16)
    greet(True)
    across = remote(tokens.at[1 - y], tokens_all.at[1], tsend.at[0], trecv.at[0], partner(y=1 - y))
    across.start()
    along = []
    for k in range(1, size_z):
        peer = partner(z=lax.rem(z + k, size_z))
        along.append(
            (
                remote(pack, weights_all.at[me], zsend.at[0, k - 1], zrecv.at[0, k - 1], peer),
                remote(vpack, vectors_all.at[me], zsend.at[1, k - 1], zrecv.at[1, k - 1], peer),
            )
        )
    beside = remote(tokens.at[y], tokens_all.at[2], tsend.at[1], trecv.at[1], partner(core=1 - core))
    sideways = []

    def forward(k, weights_src, vectors_src):
        slot = lax.rem(z - k + size_z, size_z) * size_x + x
        for j in range(1, size_x):
            peer = partner(x=lax.rem(x + j, size_x))
            first = remote(weights_src, weights_all.at[slot], xsend.at[0, k, j - 1], xrecv.at[0, k, j - 1], peer)
            second = remote(vectors_src, vectors_all.at[slot], xsend.at[1, k, j - 1], xrecv.at[1, k, j - 1], peer)
            first.start()
            second.start()
            sideways.append((first, second))

    forward(0, pack, vpack)
    for first, second in along:
        first.start()
        second.start()
    beside.start()
    keep_weights = pltpu.make_async_copy(pack, weights_all.at[me], local_sem.at[1])
    keep_vectors = pltpu.make_async_copy(vpack, vectors_all.at[me], local_sem.at[2])
    keep_weights.start()
    keep_vectors.start()
    load.wait()
    keep_tokens = pltpu.make_async_copy(stage, tokens_all.at[0], local_sem.at[3])
    keep_tokens.start()
    order = sorted(range(1, size_z), key=lambda k: min(k, size_z - k))
    for k in order:
        first, second = along[k - 1]
        first.wait_recv()
        second.wait_recv()
        slot = lax.rem(z - k + size_z, size_z) * size_x + x
        forward(k, weights_all.at[slot], vectors_all.at[slot])
    across.wait_recv()
    onward = remote(tokens_all.at[1], tokens_all.at[3], tsend.at[2], trecv.at[2], partner(core=1 - core))
    onward.start()
    for first, second in sideways:
        first.wait()
        second.wait()
    for first, second in along:
        first.wait_send()
        second.wait_send()
    across.wait_send()
    beside.wait()
    onward.wait()
    keep_weights.wait()
    keep_vectors.wait()
    keep_tokens.wait()


def entry(size_z, size_x, tokens, wq, wk, wv, vectors):
    _, part, width = tokens.shape
    rows = wq.shape[0]
    lanes = wq.shape[1] // 2 * 3
    longest = max(v.shape[0] for v in vectors)
    shards = size_z * size_x
    anywhere = pl.BlockSpec(memory_space=pl.ANY)
    dma = pltpu.SemaphoreType.DMA
    return pl.pallas_call(
        lambda *refs: entry_kernel(size_z, size_x, len(vectors), *refs),
        out_shape=(
            jax.ShapeDtypeStruct((4, part, width), tokens.dtype),
            jax.ShapeDtypeStruct((shards, rows, lanes), jnp.bfloat16),
            jax.ShapeDtypeStruct((shards, 16, longest), jnp.float32),
        ),
        in_specs=[anywhere] * (4 + len(vectors)),
        out_specs=(anywhere, anywhere, anywhere),
        scratch_shapes=[pltpu.VMEM((1, v.shape[0]), v.dtype) for v in vectors]
        + [
            pltpu.VMEM((part, width), tokens.dtype),
            pltpu.VMEM((3, rows, lanes // 3), wq.dtype),
            pltpu.VMEM((rows, lanes), jnp.bfloat16),
            pltpu.VMEM((16, longest), jnp.float32),
            dma((4,)),
            dma((3 + len(vectors),)),
            dma((3,)),
            dma((3,)),
            dma((2, size_z - 1)),
            dma((2, size_z - 1)),
            dma((2, size_z, max(size_x - 1, 1))),
            dma((2, size_z, max(size_x - 1, 1))),
        ],
        compiler_params=pltpu.CompilerParams(collective_id=0, has_side_effects=True, vmem_limit_bytes=20 << 20),
        name="entry",
    )(tokens, wq, wk, wv, *[v.reshape(1, -1) for v in vectors])


def exit_kernel(size_z, size_x, terms, output_term, vector_terms, own_rows, other_rows, *refs):
    token_grads, grad_query, grad_key, grad_value, grad_output, vector_sums = refs[:6]
    refs = refs[6:]
    recv_rows, send_rows, far_rows, odd, xbuf, xvec, zout, zvout, zbuf, zvec, ybuf, yvec, cbuf, cvec = refs[:14]
    tsend, trecv, osend, orecv, xsend, xrecv, zsend, zrecv, ysend, yrecv, csend, crecv = refs[14:]
    z, x, y, core = place_of()
    shards, rows, lanes = terms.shape
    half = output_term.shape[2] // 2
    pairs = half // 128
    part = token_grads.shape[1]
    mine = pl.ds(pl.multiple_of(core * half, 128), half)
    theirs = pl.ds(pl.multiple_of((1 - core) * half, 128), half)
    order = sorted(range(size_z), key=lambda k: -min(k, size_z - k))
    greet(True)

    outputs = remote(output_term.at[:, :, theirs], odd, osend, orecv, partner(core=1 - core))
    outputs.start()
    halves = remote(other_rows, recv_rows, tsend.at[0], trecv.at[0], partner(core=1 - core))
    halves.start()
    sideways = {}

    def send_side(n, k, src, dst):
        for j in range(1, size_x):
            column = lax.rem(x + j, size_x)
            slot = lax.rem(z + k, size_z) * size_x + column
            if n == 1:
                odd[slot] = (odd[slot].astype(jnp.float32) + output_term[slot, :, mine].astype(jnp.float32)).astype(jnp.bfloat16)
            move = remote(src.at[slot], dst(j), xsend.at[n, k, j - 1], xrecv.at[n, k, j - 1], partner(x=column))
            move.start()
            sideways.setdefault((k, j), []).append(move)

    for k in order:
        send_side(0, k, terms, lambda j: xbuf.at[j - 1, k, :, 0:lanes])
        send_side(2, k, vector_terms, lambda j: xvec.at[j - 1, k])
        if k == order[0]:
            outputs.wait()
        send_side(1, k, odd, lambda j: xbuf.at[j - 1, k, :, lanes : lanes + half])

    halves.wait()
    for i in (1, 0):
        block = slice(i * part, (i + 1) * part)
        summed = own_rows[block, :] + recv_rows[block, :].astype(jnp.float32)
        if i == 1:
            send_rows[...] = summed.astype(jnp.bfloat16)
            back = remote(send_rows, far_rows, tsend.at[1], trecv.at[1], partner(y=1 - y))
            back.start()
        else:
            token_grads[y] = summed

    along = {}
    kept = None
    for k in order:
        target = lax.rem(z + k, size_z)
        slot = target * size_x + x
        total = terms[slot].astype(jnp.float32)
        total_out = odd[slot].astype(jnp.float32) + output_term[slot, :, mine].astype(jnp.float32)
        total_vec = vector_terms[slot]
        for j in range(1, size_x):
            for move in sideways[k, j]:
                move.wait()
            total = total + xbuf[j - 1, k, :, 0:lanes].astype(jnp.float32)
            total_out = total_out + xbuf[j - 1, k, :, lanes : lanes + half].astype(jnp.float32)
            total_vec = total_vec + xvec[j - 1, k]
        if k == 0:
            kept = (total, total_out, total_vec)
            continue
        zout[k - 1, :, 0:lanes] = total.astype(jnp.bfloat16)
        zout[k - 1, :, lanes : lanes + half] = total_out.astype(jnp.bfloat16)
        zvout[k - 1] = total_vec
        peer = partner(z=target)
        moves = (
            remote(zout.at[k - 1], zbuf.at[k - 1], zsend.at[0, k - 1], zrecv.at[0, k - 1], peer),
            remote(zvout.at[k - 1], zvec.at[k - 1], zsend.at[1, k - 1], zrecv.at[1, k - 1], peer),
        )
        for move in moves:
            move.start()
        along[k] = moves

    total, total_out, total_vec = kept
    for k in reversed(order):
        if k == 0:
            continue
        for move in along[k]:
            move.wait()
        total = total + zbuf[k - 1, :, 0:lanes].astype(jnp.float32)
        total_out = total_out + zbuf[k - 1, :, lanes : lanes + half].astype(jnp.float32)
        total_vec = total_vec + zvec[k - 1]
    ybuf[0, :, 0:lanes] = total.astype(jnp.bfloat16)
    ybuf[0, :, lanes : lanes + half] = total_out.astype(jnp.bfloat16)
    yvec[0] = total_vec
    moves = (
        remote(ybuf.at[0], ybuf.at[1], ysend.at[0], yrecv.at[0], partner(y=1 - y)),
        remote(yvec.at[0], yvec.at[1], ysend.at[1], yrecv.at[1], partner(y=1 - y)),
    )
    for move in moves:
        move.start()
    for move in moves:
        move.wait()
    cbuf[0] = ybuf[0].astype(jnp.float32) + ybuf[1].astype(jnp.float32)
    cvec[0] = yvec[0] + yvec[1]
    moves = (
        remote(cbuf.at[0], cbuf.at[1], csend.at[0], crecv.at[0], partner(core=1 - core)),
        remote(cvec.at[0], cvec.at[1], csend.at[1], crecv.at[1], partner(core=1 - core)),
    )
    for move in moves:
        move.start()
    back.wait()
    token_grads[1 - y] = far_rows[...].astype(jnp.float32)
    for move in moves:
        move.wait()
    for i in range(2):
        owner = core if i == 0 else 1 - core
        for p in range(pairs):
            place = pl.ds(pl.multiple_of(owner * half + p * 128, 128), 128)
            for n, out in enumerate((grad_query, grad_key, grad_value)):
                out[:, place] = cbuf[i, :, (3 * p + n) * 128 : (3 * p + n + 1) * 128]
        grad_output[:, pl.ds(pl.multiple_of(owner * half, 128), half)] = cbuf[i, :, lanes : lanes + half]
    vector_sums[...] = cvec[0] + cvec[1]


def exit_call(size_z, size_x, terms, output_term, vector_terms, own_rows, other_rows):
    shards, rows, lanes = terms.shape
    width = output_term.shape[2]
    half = width // 2
    part = own_rows.shape[0] // 2
    vrows, vlanes = vector_terms.shape[1:]
    vmem = pl.BlockSpec(memory_space=pltpu.VMEM)
    dma = pltpu.SemaphoreType.DMA
    full = lanes + half
    side = max(size_x - 1, 1)
    low, high = jnp.bfloat16, jnp.float32
    matrix = jax.ShapeDtypeStruct((rows, width), high)
    return pl.pallas_call(
        lambda *refs: exit_kernel(size_z, size_x, *refs),
        out_shape=(
            jax.ShapeDtypeStruct((2, part, width), high),
            matrix,
            matrix,
            matrix,
            matrix,
            jax.ShapeDtypeStruct((vrows, vlanes), high),
        ),
        in_specs=[vmem] * 5,
        out_specs=(vmem,) * 6,
        scratch_shapes=[
            pltpu.VMEM((2 * part, width), low),
            pltpu.VMEM((part, width), low),
            pltpu.VMEM((part, width), low),
            pltpu.VMEM((shards, rows, half), low),
            pltpu.VMEM((side, size_z, rows, full), low),
            pltpu.VMEM((side, size_z, vrows, vlanes), high),
            pltpu.VMEM((size_z - 1, rows, full), low),
            pltpu.VMEM((size_z - 1, vrows, vlanes), high),
            pltpu.VMEM((size_z - 1, rows, full), low),
            pltpu.VMEM((size_z - 1, vrows, vlanes), high),
            pltpu.VMEM((2, rows, full), low),
            pltpu.VMEM((2, vrows, vlanes), high),
            pltpu.VMEM((2, rows, full), high),
            pltpu.VMEM((2, vrows, vlanes), high),
            dma((2,)),
            dma((2,)),
            dma,
            dma,
            dma((3, size_z, side)),
            dma((3, size_z, side)),
            dma((2, size_z - 1)),
            dma((2, size_z - 1)),
            dma((2,)),
            dma((2,)),
            dma((2,)),
            dma((2,)),
        ],
        compiler_params=pltpu.CompilerParams(collective_id=1, has_side_effects=True, vmem_limit_bytes=60 << 20),
        name="exit",
    )(terms, output_term, vector_terms, own_rows, other_rows)


def finish_kernel(inner, outer, grad_inner, grad_outer, ybuf, yvuf, cbuf, cvuf, ysend, yrecv, csend, crecv):
    z, x, y, core = place_of()
    greet(False)
    moves = (
        remote(inner, ybuf, ysend.at[0], yrecv.at[0], partner(y=1 - y)),
        remote(outer, yvuf, ysend.at[1], yrecv.at[1], partner(y=1 - y)),
    )
    for move in moves:
        move.start()
    sources = ((inner, ybuf, cbuf, grad_inner), (outer, yvuf, cvuf, grad_outer))
    onward = []
    for i, (own, far, swap_buf, out) in enumerate(sources):
        moves[i].wait()
        swap_buf[0] = own[...].astype(jnp.float32) + far[...].astype(jnp.float32)
        move = remote(swap_buf.at[0], swap_buf.at[1], csend.at[i], crecv.at[i], partner(core=1 - core))
        move.start()
        onward.append(move)
    for i, (own, far, swap_buf, out) in enumerate(sources):
        onward[i].wait()
        rows = own.shape[0]
        first = core == 0
        out[0:rows, :] = jnp.where(first, swap_buf[0], swap_buf[1])
        out[rows : 2 * rows, :] = jnp.where(first, swap_buf[1], swap_buf[0])


def finish(inner, outer):
    vmem = pl.BlockSpec(memory_space=pltpu.VMEM)
    dma = pltpu.SemaphoreType.DMA
    low, high = jnp.bfloat16, jnp.float32
    return pl.pallas_call(
        finish_kernel,
        out_shape=tuple(jax.ShapeDtypeStruct((2 * a.shape[0], a.shape[1]), high) for a in (inner, outer)),
        in_specs=[vmem] * 2,
        out_specs=(vmem,) * 2,
        scratch_shapes=[
            pltpu.VMEM(inner.shape, low),
            pltpu.VMEM(outer.shape, low),
            pltpu.VMEM((2,) + inner.shape, high),
            pltpu.VMEM((2,) + outer.shape, high),
            dma((2,)),
            dma((2,)),
            dma((2,)),
            dma((2,)),
        ],
        compiler_params=pltpu.CompilerParams(collective_id=2, has_side_effects=True, vmem_limit_bytes=30 << 20),
        name="finish",
    )(inner, outer)


TILE = 256
CHUNK = 768


def dot_nt(a, b):
    return lax.dot_general(a, b, (((1,), (1,)), ((), ())), preferred_element_type=jnp.float32)


def row_mean(value):
    return jnp.sum(value, axis=-1, keepdims=True) * (1.0 / value.shape[-1])


def standardize(hidden):
    centred = hidden - row_mean(hidden)
    reciprocal = lax.rsqrt(row_mean(centred * centred) + EPS)
    return centred * reciprocal, reciprocal


def column_sum(value):
    return jnp.sum(value.reshape(value.shape[0] // 8, 8, value.shape[1]), axis=0)


def dense_kernel(
    direct,
    pieces,
    where_ref,
    tokens_ref,
    mine_ref,
    other_ref,
    cot_ref,
    cot_far_ref,
    vectors_ref,
    bias_inner_ref,
    weights_hbm,
    outer_hbm,
    mixed_ref,
    pre_first_ref,
    grad_mine_ref,
    grad_other_ref,
    sums_ref,
    inner_sum_ref,
    grad_output_ref,
    terms_hbm,
    outer_terms_hbm,
    w_output,
    w_inner,
    w_outer,
    a_output,
    a_inner,
    a_outer,
    stage,
    context,
    first_low,
    turned_low,
    normed,
    first,
    slope,
    active,
    work,
    load_sem,
    outer_sem,
    store_sem,
):
    step, steps = pl.program_id(0), pl.num_programs(0)
    core = where_ref[0]
    width, hidden = w_inner.shape
    half = width // 2
    chunks = hidden // CHUNK
    rows = width // pieces
    ratio = hidden // width

    def load_outer(start):
        if not direct:
            copy = pltpu.make_async_copy(outer_hbm, w_outer, outer_sem)
            copy.start() if start else copy.wait()
            return

        if not start:
            pltpu.make_async_copy(w_outer, w_outer, outer_sem).wait()
            return

        def piece(s, _):
            for q in range(ratio):
                src = weights_hbm.at[
                    pl.ds(pl.multiple_of(s * rows, rows), rows), pl.ds(hidden + width + q * width, width)
                ]
                dst = w_outer.at[pl.ds(pl.multiple_of((s * ratio + q) * rows, rows), rows), :]
                pltpu.make_async_copy(src, dst, outer_sem).start()
            return 0

        lax.fori_loop(0, pieces, piece, 0)

    loads = (
        pltpu.make_async_copy(weights_hbm.at[:, pl.ds(hidden, width)], w_output, load_sem.at[0]),
        pltpu.make_async_copy(weights_hbm.at[:, pl.ds(0, hidden)], w_inner, load_sem.at[1]),
    )

    @pl.when(step == 0)
    def _():
        for load in loads:
            load.start()
        load_outer(True)
        a_output[...] = jnp.zeros_like(a_output)
        a_inner[...] = jnp.zeros_like(a_inner)
        a_outer[...] = jnp.zeros_like(a_outer)
        sums_ref[...] = jnp.zeros_like(sums_ref)
        inner_sum_ref[...] = jnp.zeros_like(inner_sum_ref)

    def vector(i):
        return vectors_ref[i : i + 1, :]

    def add_sum(i, value):
        sums_ref[8 * i : 8 * i + 8, :] += column_sum(value)

    context[:, pl.ds(pl.multiple_of(core * half, 128), half)] = mine_ref[...]
    context[:, pl.ds(pl.multiple_of((1 - core) * half, 128), half)] = other_ref[...]

    @pl.when(step == 0)
    def _():
        loads[0].wait()

    hidden_rows = tokens_ref[...].astype(jnp.float32) + (dot_nn(context[...], w_output[...]) + vector(0))
    normed[...], first_recip = standardize(hidden_rows)
    first[...] = normed[...] * vector(1) + vector(2)
    first_low[...] = first[...].astype(jnp.bfloat16)
    turned_low[...] = first_low[...].T
    work[...] = jnp.broadcast_to(vector(3), work.shape)

    @pl.when(step == 0)
    def _():
        loads[1].wait()
        load_outer(False)

    def part(c):
        return pl.ds(pl.multiple_of(c * CHUNK, CHUNK), CHUNK)

    def forward(c, _):
        u = dot_nn(first_low[...], w_inner[:, part(c)]) + bias_inner_ref[0:1, part(c)]
        cdf = 0.5 * (1.0 + lax.erf(u * ROOT_HALF))
        slope[:, part(c)] = cdf + u * jnp.exp(-0.5 * u * u) * INV_ROOT_TAU
        active[:, part(c)] = (u * cdf).astype(jnp.bfloat16)
        work[...] += dot_nn(active[:, part(c)], w_outer[part(c), :])
        return 0

    lax.fori_loop(0, chunks, forward, 0)
    second, second_recip = standardize(first[...] + work[...])
    mixed_ref[...] = (second * vector(4) + vector(5)).astype(jnp.bfloat16)
    upstream = jnp.where(step < steps // 2, cot_ref[0], cot_far_ref[...]).astype(jnp.float32)
    add_sum(0, upstream * second)
    add_sum(1, upstream)
    scaled = upstream * vector(4)
    pre_second = second_recip * (scaled - row_mean(scaled) - second * row_mean(scaled * second))
    grad_outer = pre_second.astype(jnp.bfloat16)
    add_sum(2, grad_outer.astype(jnp.float32))
    work[...] = pre_second
    stage[0, 0:TILE, :] = grad_outer

    def backward(c, _):
        grad_out = stage[0, 0:TILE, :]
        grad = dot_nt(grad_out, w_outer[part(c), :])
        grad_inner = (grad * slope[:, part(c)]).astype(jnp.bfloat16)
        inner_sum_ref[:, part(c)] += column_sum(grad_inner.astype(jnp.float32))
        a_outer[part(c), :] += dot_nn(active[:, part(c)].T, grad_out)
        a_inner[:, part(c)] += dot_nn(turned_low[...], grad_inner)
        work[...] += dot_nt(grad_inner, w_inner[:, part(c)])
        return 0

    lax.fori_loop(0, chunks, backward, 0)
    grad_first = work[...]
    add_sum(3, grad_first * normed[...])
    add_sum(4, grad_first)
    scaled = grad_first * vector(1)
    pre_first = first_recip * (scaled - row_mean(scaled) - normed[...] * row_mean(scaled * normed[...]))
    pre_first_ref[...] = pre_first
    grad_attended = pre_first.astype(jnp.bfloat16)
    add_sum(5, grad_attended.astype(jnp.float32))
    a_output[...] += dot_nn(context[...].T, grad_attended)
    context[...] = dot_nt(grad_attended, w_output[...]).astype(jnp.bfloat16)
    grad_mine_ref[...] = context[:, pl.ds(pl.multiple_of(core * half, 128), half)]
    grad_other_ref[...] = context[:, pl.ds(pl.multiple_of((1 - core) * half, 128), half)]

    @pl.when(step == steps - 1)
    def _():
        grad_output_ref[...] = a_output[...].astype(jnp.bfloat16)

        def inner_copy(c, slot):
            return pltpu.make_async_copy(stage.at[slot], terms_hbm.at[:, part(c)], store_sem.at[slot])

        def outer_wait(slot):
            pltpu.make_async_copy(stage.at[slot], stage.at[slot], store_sem.at[slot]).wait()

        def outer_start(c, slot):
            if not direct:
                pltpu.make_async_copy(stage.at[slot], outer_terms_hbm.at[part(c), :], store_sem.at[slot]).start()
                return
            groups = CHUNK // (rows * ratio)
            for s in range(groups):
                for q in range(ratio):
                    src = stage.at[slot, pl.ds((s * ratio + q) * rows, rows), :]
                    dst = terms_hbm.at[
                        pl.ds(pl.multiple_of((c * groups + s) * rows, rows), rows), pl.ds(hidden + q * width, width)
                    ]
                    pltpu.make_async_copy(src, dst, store_sem.at[slot]).start()

        for c in range(chunks):
            if c > 0:
                inner_copy(c - 1, 0).wait()
                outer_wait(1)
            stage[0] = a_inner[:, part(c)].astype(jnp.bfloat16)
            inner_copy(c, 0).start()
            stage[1] = a_outer[part(c), :].astype(jnp.bfloat16)
            outer_start(c, 1)
        inner_copy(chunks - 1, 0).wait()
        outer_wait(1)


def dense_layer(where, tokens, mine, other, cotangent, cotangent_far, vectors, bias_inner, weights, outer, pieces, direct):
    local, half = mine.shape
    width = 2 * half
    hidden = bias_inner.shape[1]
    steps = local // TILE
    rows = width // pieces
    low, high = jnp.bfloat16, jnp.float32
    tile = pl.BlockSpec((TILE, width), lambda t, *_: (t, 0))
    half_tile = pl.BlockSpec((TILE, half), lambda t, *_: (t, 0))
    anywhere = pl.BlockSpec(memory_space=pl.ANY)
    halfway = steps // 2

    def whole(shape):
        return pl.BlockSpec(shape, lambda t, *_: (0, 0))

    terms_shape = (width, 2 * hidden if direct else hidden)
    outer_shape = (8, 128) if direct else (hidden, width)
    return pl.pallas_call(
        lambda *refs: dense_kernel(direct, pieces, *refs),
        out_shape=(
            jax.ShapeDtypeStruct((local, width), low),
            jax.ShapeDtypeStruct((local, width), high),
            jax.ShapeDtypeStruct((local, half), low),
            jax.ShapeDtypeStruct((local, half), low),
            jax.ShapeDtypeStruct((48, width), high),
            jax.ShapeDtypeStruct((8, hidden), high),
            jax.ShapeDtypeStruct((width, width), low),
            jax.ShapeDtypeStruct(terms_shape, low),
            jax.ShapeDtypeStruct(outer_shape, low),
        ),
        grid_spec=pltpu.PrefetchScalarGridSpec(
            num_scalar_prefetch=1,
            grid=(steps,),
            in_specs=[
                tile,
                half_tile,
                half_tile,
                pl.BlockSpec((1, TILE, width), lambda t, where: (where[1], jnp.minimum(t, halfway - 1), 0)),
                pl.BlockSpec((TILE, width), lambda t, *_: (jnp.maximum(t - halfway, 0), 0)),
                whole((8, width)),
                whole((1, hidden)),
                anywhere,
                anywhere,
            ],
            out_specs=[
                tile,
                tile,
                half_tile,
                half_tile,
                whole((48, width)),
                whole((8, hidden)),
                whole((width, width)),
                anywhere,
                anywhere,
            ],
            scratch_shapes=[
                pltpu.VMEM((width, width), low),
                pltpu.VMEM((width, hidden), low),
                pltpu.VMEM((hidden, width), low),
                pltpu.VMEM((width, width), high),
                pltpu.VMEM((width, hidden), high),
                pltpu.VMEM((hidden, width), high),
                pltpu.VMEM((2, width, CHUNK), low),
                pltpu.VMEM((TILE, width), low),
                pltpu.VMEM((TILE, width), low),
                pltpu.VMEM((width, TILE), low),
                pltpu.VMEM((TILE, width), high),
                pltpu.VMEM((TILE, width), high),
                pltpu.VMEM((TILE, hidden), high),
                pltpu.VMEM((TILE, hidden), low),
                pltpu.VMEM((TILE, width), high),
                pltpu.SemaphoreType.DMA((2,)),
                pltpu.SemaphoreType.DMA,
                pltpu.SemaphoreType.DMA((2,)),
            ],
        ),
        compiler_params=pltpu.CompilerParams(dimension_semantics=("arbitrary",), vmem_limit_bytes=66_000_000),
        cost_estimate=pl.CostEstimate(flops=32_000_000_000, bytes_accessed=40_000_000, transcendentals=6_000_000),
        name="dense_layer",
    )(where, tokens, mine, other, cotangent, cotangent_far, vectors, bias_inner, weights, outer)


def lowered(piece):
    return piece.astype(jnp.bfloat16)


def widen(piece):
    return piece.astype(jnp.float32)


def matmul(left, right):
    return jnp.dot(left, right, preferred_element_type=jnp.float32)


def matmul_tn(left, right):
    return lax.dot_general(
        left, right, (((0,), (0,)), ((), ())), preferred_element_type=jnp.float32
    )


def matmul_nt(left, right):
    return lax.dot_general(
        left, right, (((1,), (1,)), ((), ())), preferred_element_type=jnp.float32
    )


def swap(piece, axis):
    return lax.ppermute(piece, axis, [(0, 1), (1, 0)])


def pick(piece, index, axis=0):
    return lax.dynamic_index_in_dim(piece, index, axis, keepdims=False)


def in_order(first_is_zero, own, other, axis):
    return jnp.where(
        first_is_zero,
        jnp.concatenate([own, other], axis),
        jnp.concatenate([other, own], axis),
    )


def body(
    tokens,
    segment_ids,
    w_query,
    w_key,
    w_value,
    w_output,
    b_query,
    b_value,
    b_output,
    first_gain,
    first_shift,
    w_inner,
    b_inner,
    w_outer,
    b_outer,
    second_gain,
    second_shift,
    cotangent,
):
    core, y = lax.axis_index("core"), lax.axis_index("y")
    size_z, size_x = lax.axis_size("z"), lax.axis_size("x")
    shards = size_z * size_x
    everyone = ("z", "x", "core")
    sequences, part, width = tokens.shape
    half = width // 2
    pairs = half // 128
    hidden = w_inner.shape[1]
    local = 2 * part
    own_rows = w_query.shape[0]
    lanes = 3 * half

    stack = hidden // width

    def core_rows(matrix):
        rows = matrix.shape[0] // 2
        return lowered(lax.dynamic_slice_in_dim(matrix, core * rows, rows, 0))

    def side_by_side(matrix, groups):
        rows = matrix.shape[0] // groups // stack
        return matrix.reshape(groups, stack, rows, width).transpose(0, 2, 1, 3).reshape(groups * rows, hidden)

    def stacked(matrix, groups):
        rows = matrix.shape[0] // groups
        return matrix.reshape(groups, rows, stack, width).transpose(0, 2, 1, 3).reshape(groups * rows * stack, width)

    pieces = (core_rows(w_inner), core_rows(w_output), side_by_side(core_rows(w_outer), 1))
    dense = lax.all_gather(jnp.concatenate(pieces, axis=1), everyone, axis=0, tiled=True)
    pieces_count = 2 * shards
    direct = (width // pieces_count) % 16 == 0
    if direct:
        full_outer = dense
    else:
        full_outer = stacked(dense[:, hidden + width :], pieces_count)

    vectors = (b_query, b_value, b_output, first_gain, first_shift, b_inner, b_outer, second_gain, second_shift)
    sizes = [v.shape[0] for v in vectors]
    tokens_all, early, vectors_all = entry(size_z, size_x, tokens, w_query, w_key, w_value, vectors)
    inputs_all = tokens_all.reshape(4 * part, width)
    full_early = early.reshape(width, lanes)
    cotangent_far = swap(pick(cotangent, 1 - y), "y")
    bias_query, bias_value, bias_output, gain_first, shift_first, bias_inner, bias_outer, gain_second, shift_second = [
        vectors_all[:, i, :size].reshape(shards * size) for i, size in enumerate(sizes)
    ]
    heads_query = lax.dynamic_slice_in_dim(bias_query, core * half, half).reshape(pairs, 1, 128)
    heads_value = lax.dynamic_slice_in_dim(bias_value, core * half, half).reshape(pairs, 1, 128)
    bias_all = jnp.concatenate([heads_query, jnp.zeros_like(heads_query), heads_value], axis=1).reshape(lanes)
    scale = jnp.tile(jnp.concatenate([jnp.full((128,), HD ** (-0.5)), jnp.ones((256,))]), pairs)
    projected = lowered((matmul(inputs_all, full_early) + bias_all) * scale)

    spot = jnp.arange(5, dtype=jnp.int32)
    place = jnp.where(spot < 4, ((spot % 2 != core) * 2 + (spot // 2 != y) * 1) * part, core)
    segments = pick(segment_ids, y)
    context_mine, context_other, logsum = attention(place, segments, projected)
    norms = jnp.stack([bias_output, gain_first, shift_first, bias_outer, gain_second, shift_second])
    norms = jnp.concatenate([norms, jnp.zeros((2, width), jnp.float32)], axis=0)
    mixed, pre_first, upstream_mine, upstream_send, dense_sums, inner_sums, grad_w_output, terms, outer_terms = dense_layer(
        jnp.stack([core, y]).astype(jnp.int32),
        inputs_all,
        context_mine,
        swap(context_other, "core"),
        cotangent,
        cotangent_far,
        norms,
        bias_inner.reshape(1, hidden),
        dense,
        full_outer,
        pieces_count,
        direct,
    )
    if not direct:
        terms = jnp.concatenate([terms, side_by_side(outer_terms, pieces_count)], axis=1)
    both_done = lax.psum_scatter(terms, everyone, scatter_dimension=0, tiled=True)
    inner_done, outer_done = both_done[:, :hidden], stacked(both_done[:, hidden:], 1)
    upstream_other = swap(upstream_send, "core")
    dense_sums = jnp.sum(dense_sums.reshape(6, 8, width), axis=1)
    grad_second_gain, grad_second_shift, grad_b_outer, grad_first_gain, grad_first_shift, grad_b_output = [
        dense_sums[i] for i in range(6)
    ]
    grad_b_inner = jnp.sum(inner_sums, axis=0)
    mixed_out = in_order(y == 0, mixed[None, :part], swap(mixed[part:], "y")[None], 0)

    grads, sums = attention_back(place, segments, projected, context_mine, context_other, upstream_mine, upstream_other, logsum)
    grad_early = lowered(matmul_tn(inputs_all, grads)).reshape(shards, own_rows, lanes)
    own_partial = pre_first + matmul_nt(grads[:local], full_early)
    other_partial = lowered(matmul_nt(grads[local:], full_early))
    sums = sums.reshape(pairs, 8, 3, 128)[:, 0]
    blank = jnp.zeros((width,), jnp.float32)
    grad_b_query = lax.dynamic_update_slice(blank, sums[:, 0].reshape(half), (core * half,))
    grad_b_value = lax.dynamic_update_slice(blank, sums[:, 2].reshape(half), (core * half,))
    vector_grads = (
        grad_b_query,
        grad_b_value,
        grad_b_output,
        grad_first_gain,
        grad_first_shift,
        grad_b_inner,
        grad_b_outer,
        grad_second_gain,
        grad_second_shift,
    )
    longest = vectors_all.shape[2]
    rows = [jnp.pad(v.reshape(shards, 1, -1), ((0, 0), (0, 0), (0, longest - v.shape[0] // shards))) for v in vector_grads]
    rows.append(jnp.zeros((shards, vectors_all.shape[1] - len(rows), longest), jnp.float32))
    vector_terms = jnp.concatenate(rows, axis=1)
    grad_tokens, grad_query, grad_key, grad_value, grad_output, vector_sums = exit_call(
        size_z, size_x, grad_early, grad_w_output.reshape(shards, own_rows, width), vector_terms, own_partial, other_partial
    )
    grad_inner_full, grad_outer_full = finish(inner_done, outer_done)
    done = [vector_sums[i, :size] for i, size in enumerate(sizes)]
    return (
        mixed_out,
        grad_tokens,
        grad_query,
        grad_key,
        grad_value,
        grad_output,
        done[0],
        done[1],
        done[2],
        done[3],
        done[4],
        grad_inner_full,
        done[5],
        grad_outer_full,
        done[6],
        done[7],
        done[8],
    )


def solution(mesh):
    outer, inner = mesh.devices.shape
    size_z = 1
    while size_z * size_z < outer:
        size_z *= 2
    split = Mesh(mesh.devices.reshape(size_z, outer // size_z, inner // 2, 2), ("z", "x", "y", "core"))
    dp, seq = ("z", "x"), ("y", "core")
    activation, matrix, vector = P(dp, seq, None), P(dp, None), P(dp)
    return jax.shard_map(
        body,
        mesh=split,
        in_specs=(
            activation,
            matrix,
            matrix,
            matrix,
            matrix,
            matrix,
            vector,
            vector,
            vector,
            vector,
            vector,
            matrix,
            vector,
            matrix,
            vector,
            vector,
            vector,
            activation,
        ),
        out_specs=(
            activation,
            activation,
            matrix,
            matrix,
            matrix,
            matrix,
            vector,
            vector,
            vector,
            vector,
            vector,
            matrix,
            vector,
            matrix,
            vector,
            vector,
            vector,
        ),
        check_vma=False,
    )
```

```python
import jax
import jax.numpy as jnp
from jax import lax
from jax.experimental import pallas as pl
from jax.experimental.pallas import tpu as pltpu
from jax.sharding import Mesh
from jax.sharding import PartitionSpec as P


HD = 64
EPS = 1e-12
ROOT_HALF = 0.7071067811865476
INV_ROOT_TAU = 0.3989422804014327

BLK = 256
BIG = -1.0e9
DOCUMENTS = 4


def dot_nn(a, b):
    return jnp.dot(a, b, preferred_element_type=jnp.float32)


def part_rows(place_ref, part, rows):
    return pl.ds(pl.multiple_of(place_ref[part], 128), rows)


def find_bounds(segment_ref, bound_ref):
    length = segment_ref.shape[0]
    bound_ref[0] = 0
    bound_ref[DOCUMENTS] = length
    for d in range(1, DOCUMENTS):

        def halve(_, span):
            low, high = span
            middle = (low + high) // 2
            below = segment_ref[jnp.minimum(middle, length - 1)] < d
            inside = low < high
            return (
                jnp.where(jnp.logical_and(inside, below), middle + 1, low),
                jnp.where(jnp.logical_and(inside, jnp.logical_not(below)), middle, high),
            )

        low, _ = lax.fori_loop(0, length.bit_length(), halve, (0, length))
        bound_ref[d] = low


def find_window(segment_ref, bound_ref, qb):
    length = segment_ref.shape[0]
    first = segment_ref[qb * BLK]
    last = segment_ref[qb * BLK + BLK - 1]
    start = bound_ref[first] // 128 * 128
    count = (bound_ref[last + 1] - start + BLK - 1) // BLK
    return jnp.minimum(start, length - count * BLK), count


def each_tile(count, step):
    def two(i, _):
        step(i * (2 * BLK), 2 * BLK)
        return 0

    lax.fori_loop(0, count // 2, two, 0)

    @pl.when(count % 2 == 1)
    def _():
        step((count - 1) * BLK, BLK)


def make_marks(row_ref, mark_query, mark_key):
    length = mark_key.shape[0]
    step = 512
    for b in range(length // step):
        rows = slice(b * step, (b + 1) * step)
        column = jnp.broadcast_to(row_ref[0:1, rows], (128, step)).T
        lane = lax.broadcasted_iota(jnp.int32, (step, 128), 1) % 64
        same = lane == column
        line = lax.broadcasted_iota(jnp.int32, (128, step), 0) % 64
        mark_query[:, rows] = jnp.where(line == row_ref[0:1, rows], 1.0, 0.0).astype(jnp.bfloat16)
        apart = jnp.logical_and(lane < DOCUMENTS, jnp.logical_not(same))
        mark_key[rows, :] = jnp.where(apart, BIG, 0.0).astype(jnp.bfloat16)


def forward_kernel(
    place_ref, segment_ref, qkv_ref, row_ref, mine_ref, other_ref, lse_ref, q2, k2, vt, acc, top, tot, keep, mark_query, mark_key, bound_ref
):
    length = qkv_ref.shape[0]
    blocks = length // BLK
    part = length // 4

    @pl.when(pl.program_id(0) == 0)
    def _():
        find_bounds(segment_ref, bound_ref)
        make_marks(row_ref, mark_query, mark_key)

    low = lax.broadcasted_iota(jnp.int32, (part, 128), 1) < 64
    for b in range(4):
        src = part_rows(place_ref, b, part)
        dst = slice(b * part, (b + 1) * part)
        k, nohk = qkv_ref[src, 128:256], mark_key[dst, :]
        turned = qkv_ref[src, 0:128].T
        q2[0, 0:64, dst] = turned[0:64]
        q2[0, 64:128, dst] = mark_query[64:128, dst]
        q2[1, 0:64, dst] = mark_query[0:64, dst]
        q2[1, 64:128, dst] = turned[64:128]
        k2[0, dst, :] = jnp.where(low, k, nohk)
        k2[1, dst, :] = jnp.where(low, nohk, k)
        vt[:, dst] = qkv_ref[src, 256:384].T
    lse_ref[...] = jnp.zeros_like(lse_ref)

    def row(qb, _):
        qs = pl.ds(pl.multiple_of(qb * BLK, BLK), BLK)
        start, count = find_window(segment_ref, bound_ref, qb)
        top[...] = jnp.full_like(top, -1.0e30)

        def fold(tile, function):
            return function(tile.reshape(tile.shape[0] // 8, 8, BLK), axis=0)

        def highest(first, size):
            keys = pl.ds(pl.multiple_of(start + first, 128), size)
            for h in range(2):
                st = dot_nn(k2[h, keys, :], q2[h, :, qs])
                keep[h, pl.ds(pl.multiple_of(first, BLK), size), :] = st
                top[h] = jnp.maximum(top[h], fold(st, jnp.max))

        def weigh(first, size, largest):
            keys = pl.ds(pl.multiple_of(start + first, 128), size)
            for h in range(2):
                rows = slice(64 * h, 64 * h + 64)
                st = keep[h, pl.ds(pl.multiple_of(first, BLK), size), :]
                p = jnp.exp(st - largest[h])
                tot[h] = tot[h] + fold(p, jnp.sum)
                acc[rows, :] = acc[rows, :] + dot_nn(vt[rows, keys], p.astype(jnp.bfloat16))

        def paired(step):
            each_tile(count, step)

        paired(highest)
        largest = [jnp.max(top[h], axis=0, keepdims=True) for h in range(2)]
        acc[...] = jnp.zeros_like(acc)
        tot[...] = jnp.zeros_like(tot)
        paired(lambda first, size: weigh(first, size, largest))
        for h in range(2):
            rows = slice(64 * h, 64 * h + 64)
            total = jnp.sum(tot[h], axis=0, keepdims=True)
            acc[rows, :] = acc[rows, :] / total
            lse_ref[h : h + 1, qs] = largest[h] + jnp.log(total)
        where = place_ref[qb * BLK // part] + qb * BLK % part
        result = acc[...].T.astype(jnp.bfloat16)

        @pl.when(where < 2 * part)
        def _():
            mine_ref[pl.ds(pl.multiple_of(where, BLK), BLK), :] = result

        @pl.when(where >= 2 * part)
        def _():
            other_ref[pl.ds(pl.multiple_of(where - 2 * part, BLK), BLK), :] = result

        return 0

    lax.fori_loop(0, blocks, row, 0)


def attention(place, segments, qkv):
    length, width = qkv.shape
    pairs = width // 384
    rows = length // 2
    return pl.pallas_call(
        forward_kernel,
        out_shape=(
            jax.ShapeDtypeStruct((rows, pairs * 128), jnp.bfloat16),
            jax.ShapeDtypeStruct((rows, pairs * 128), jnp.bfloat16),
            jax.ShapeDtypeStruct((pairs * 8, length), jnp.float32),
        ),
        grid_spec=pltpu.PrefetchScalarGridSpec(
            num_scalar_prefetch=2,
            grid=(pairs,),
            in_specs=[
                pl.BlockSpec((length, 384), lambda p, *_: (0, p)),
                pl.BlockSpec((1, length), lambda p, *_: (0, 0)),
            ],
            out_specs=[
                pl.BlockSpec((rows, 128), lambda p, *_: (0, p)),
                pl.BlockSpec((rows, 128), lambda p, *_: (0, p)),
                pl.BlockSpec((8, length), lambda p, *_: (p, 0)),
            ],
            scratch_shapes=[
                pltpu.VMEM((2, 128, length), jnp.bfloat16),
                pltpu.VMEM((2, length, 128), jnp.bfloat16),
                pltpu.VMEM((128, length), jnp.bfloat16),
                pltpu.VMEM((128, BLK), jnp.float32),
                pltpu.VMEM((2, 8, BLK), jnp.float32),
                pltpu.VMEM((2, 8, BLK), jnp.float32),
                pltpu.VMEM((2, length, BLK), jnp.float32),
                pltpu.VMEM((128, length), jnp.bfloat16),
                pltpu.VMEM((length, 128), jnp.bfloat16),
                pltpu.SMEM((DOCUMENTS + 1,), jnp.int32),
            ],
        ),
        compiler_params=pltpu.CompilerParams(dimension_semantics=("arbitrary",), vmem_limit_bytes=60 << 20),
        cost_estimate=pl.CostEstimate(flops=pairs * 8_000_000_000, bytes_accessed=pairs * 3_000_000, transcendentals=pairs * 4_000_000),
        name="attention_forward",
    )(place, segments, qkv, segments.reshape(1, length))


def backward_kernel(
    place_ref,
    segment_ref,
    qkv_ref,
    ctx_mine_ref,
    ctx_other_ref,
    do_mine_ref,
    do_other_ref,
    lse_ref,
    row_ref,
    out_ref,
    sum_ref,
    q2,
    k2,
    q0,
    d0,
    dt,
    v0,
    kt,
    dk,
    dv,
    dqt,
    delta,
    mark_query,
    mark_key,
    bound_ref,
):
    length = qkv_ref.shape[0]
    blocks = length // BLK
    part = length // 4

    @pl.when(pl.program_id(0) == 0)
    def _():
        find_bounds(segment_ref, bound_ref)
        make_marks(row_ref, mark_query, mark_key)

    low = lax.broadcasted_iota(jnp.int32, (part, 128), 1) < 64

    def prepare(b, do, ctx):
        src = part_rows(place_ref, b, part)
        dst = slice(b * part, (b + 1) * part)
        q, k = qkv_ref[src, 0:128], qkv_ref[src, 128:256]
        zero = jnp.zeros_like(q)
        nohk = mark_key[dst, :]
        turned = q.T
        q2[0, 0:64, dst] = turned[0:64]
        q2[0, 64:128, dst] = mark_query[64:128, dst]
        q2[1, 0:64, dst] = mark_query[0:64, dst]
        q2[1, 64:128, dst] = turned[64:128]
        k2[0, dst, :] = jnp.where(low, k, nohk)
        k2[1, dst, :] = jnp.where(low, nohk, k)
        q0[0, dst, :] = jnp.where(low, q, zero)
        q0[1, dst, :] = jnp.where(low, zero, q)
        d0[0, dst, :] = jnp.where(low, do, zero)
        d0[1, dst, :] = jnp.where(low, zero, do)
        turned = do.T
        blank = jnp.zeros((64, part), jnp.bfloat16)
        dt[0, 0:64, dst] = turned[0:64]
        dt[0, 64:128, dst] = blank
        dt[1, 0:64, dst] = blank
        dt[1, 64:128, dst] = turned[64:128]
        v0[dst, :] = qkv_ref[src, 256:384]
        kt[:, dst] = k.T
        prod = turned.astype(jnp.float32) * ctx.T.astype(jnp.float32)
        delta[0:1, dst] = jnp.sum(prod[0:64], axis=0, keepdims=True)
        delta[1:2, dst] = jnp.sum(prod[64:128], axis=0, keepdims=True)

    for b in range(4):

        @pl.when(place_ref[b] < 2 * part)
        def _():
            rows = part_rows(place_ref, b, part)
            prepare(b, do_mine_ref[rows, :], ctx_mine_ref[rows, :])

        @pl.when(place_ref[b] >= 2 * part)
        def _():
            rows = pl.ds(pl.multiple_of(place_ref[b] - 2 * part, 128), part)
            prepare(b, do_other_ref[rows, :], ctx_other_ref[rows, :])

    dk[...] = jnp.zeros_like(dk)
    dv[...] = jnp.zeros_like(dv)
    dqt[...] = jnp.zeros_like(dqt)

    def row(qb, _):
        qs = pl.ds(pl.multiple_of(qb * BLK, BLK), BLK)
        start, count = find_window(segment_ref, bound_ref, qb)

        def tile(first, size):
            ks = pl.ds(pl.multiple_of(start + first, 128), size)
            weights, grads = [], []
            for h in range(2):
                st = dot_nn(k2[h, ks, :], q2[h, :, qs])
                w = jnp.exp(st - lse_ref[h : h + 1, qs])
                gw = dot_nn(v0[ks, :], dt[h, :, qs])
                weights.append(w.astype(jnp.bfloat16))
                grads.append((w * (gw - delta[h : h + 1, qs])).astype(jnp.bfloat16))
            dv[ks, :] += dot_nn(jnp.concatenate(weights, axis=1), jnp.concatenate([d0[0, qs, :], d0[1, qs, :]], axis=0))
            dk[ks, :] += dot_nn(jnp.concatenate(grads, axis=1), jnp.concatenate([q0[0, qs, :], q0[1, qs, :]], axis=0))
            for h in range(2):
                rows = slice(64 * h, 64 * h + 64)
                dqt[rows, qs] += dot_nn(kt[rows, ks], grads[h])

        each_tile(count, tile)
        return 0

    lax.fori_loop(0, blocks, row, 0)
    sums = [jnp.zeros((1, 128), jnp.float32) for _ in range(3)]
    for b in range(4):
        dst = part_rows(place_ref, b, part)
        src = slice(b * part, (b + 1) * part)
        pieces = ((dqt[:, src].T * 0.125).astype(jnp.bfloat16), dk[src, :].astype(jnp.bfloat16), dv[src, :].astype(jnp.bfloat16))
        for i, piece in enumerate(pieces):
            out_ref[dst, 128 * i : 128 * i + 128] = piece
            sums[i] = sums[i] + jnp.sum(piece.astype(jnp.float32), axis=0, keepdims=True)
    sum_ref[...] = jnp.zeros_like(sum_ref)
    for i in range(3):
        sum_ref[0:1, 128 * i : 128 * i + 128] = sums[i]


def attention_back(place, segments, qkv, ctx_mine, ctx_other, do_mine, do_other, lse):
    length, width = qkv.shape
    pairs = width // 384
    rows = length // 2
    half = lambda: pltpu.VMEM((2, length, 128), jnp.bfloat16)
    turned = lambda: pltpu.VMEM((2, 128, length), jnp.bfloat16)
    column = pl.BlockSpec((rows, 128), lambda p, *_: (0, p))
    return pl.pallas_call(
        backward_kernel,
        out_shape=(
            jax.ShapeDtypeStruct((length, width), jnp.bfloat16),
            jax.ShapeDtypeStruct((pairs * 8, 384), jnp.float32),
        ),
        grid_spec=pltpu.PrefetchScalarGridSpec(
            num_scalar_prefetch=2,
            grid=(pairs,),
            in_specs=[
                pl.BlockSpec((length, 384), lambda p, *_: (0, p)),
                column,
                column,
                column,
                column,
                pl.BlockSpec((8, length), lambda p, *_: (p, 0)),
                pl.BlockSpec((1, length), lambda p, *_: (0, 0)),
            ],
            out_specs=[
                pl.BlockSpec((length, 384), lambda p, *_: (0, p)),
                pl.BlockSpec((8, 384), lambda p, *_: (p, 0)),
            ],
            scratch_shapes=[
                turned(),
                half(),
                half(),
                half(),
                turned(),
                pltpu.VMEM((length, 128), jnp.bfloat16),
                pltpu.VMEM((128, length), jnp.bfloat16),
                pltpu.VMEM((length, 128), jnp.float32),
                pltpu.VMEM((length, 128), jnp.float32),
                pltpu.VMEM((128, length), jnp.float32),
                pltpu.VMEM((8, length), jnp.float32),
                pltpu.VMEM((128, length), jnp.bfloat16),
                pltpu.VMEM((length, 128), jnp.bfloat16),
                pltpu.SMEM((DOCUMENTS + 1,), jnp.int32),
            ],
        ),
        compiler_params=pltpu.CompilerParams(dimension_semantics=("arbitrary",), vmem_limit_bytes=60 << 20),
        cost_estimate=pl.CostEstimate(flops=pairs * 20_000_000_000, bytes_accessed=pairs * 5_000_000, transcendentals=pairs * 4_000_000),
        name="attention_backward",
    )(place, segments, qkv, ctx_mine, ctx_other, do_mine, do_other, lse, segments.reshape(1, length))


TILE = 256
CHUNK = 768


def dot_nt(a, b):
    return lax.dot_general(a, b, (((1,), (1,)), ((), ())), preferred_element_type=jnp.float32)


def row_mean(value):
    return jnp.sum(value, axis=-1, keepdims=True) * (1.0 / value.shape[-1])


def standardize(hidden):
    centred = hidden - row_mean(hidden)
    reciprocal = lax.rsqrt(row_mean(centred * centred) + EPS)
    return centred * reciprocal, reciprocal


def column_sum(value):
    return jnp.sum(value.reshape(value.shape[0] // 8, 8, value.shape[1]), axis=0)


def dense_kernel(
    direct,
    pieces,
    where_ref,
    tokens_ref,
    mine_ref,
    other_ref,
    cot_ref,
    cot_far_ref,
    vectors_ref,
    bias_inner_ref,
    weights_hbm,
    outer_hbm,
    mixed_ref,
    pre_first_ref,
    grad_mine_ref,
    grad_other_ref,
    sums_ref,
    inner_sum_ref,
    grad_output_ref,
    terms_hbm,
    outer_terms_hbm,
    w_output,
    w_inner,
    w_outer,
    a_output,
    a_inner,
    a_outer,
    stage,
    context,
    first_low,
    turned_low,
    normed,
    first,
    slope,
    active,
    work,
    load_sem,
    outer_sem,
    store_sem,
):
    step, steps = pl.program_id(0), pl.num_programs(0)
    core = where_ref[0]
    width, hidden = w_inner.shape
    half = width // 2
    chunks = hidden // CHUNK
    rows = width // pieces
    ratio = hidden // width

    def load_outer(start):
        if not direct:
            copy = pltpu.make_async_copy(outer_hbm, w_outer, outer_sem)
            copy.start() if start else copy.wait()
            return

        if not start:
            pltpu.make_async_copy(w_outer, w_outer, outer_sem).wait()
            return

        def piece(s, _):
            for q in range(ratio):
                src = weights_hbm.at[
                    pl.ds(pl.multiple_of(s * rows, rows), rows), pl.ds(hidden + width + q * width, width)
                ]
                dst = w_outer.at[pl.ds(pl.multiple_of((s * ratio + q) * rows, rows), rows), :]
                pltpu.make_async_copy(src, dst, outer_sem).start()
            return 0

        lax.fori_loop(0, pieces, piece, 0)

    loads = (
        pltpu.make_async_copy(weights_hbm.at[:, pl.ds(hidden, width)], w_output, load_sem.at[0]),
        pltpu.make_async_copy(weights_hbm.at[:, pl.ds(0, hidden)], w_inner, load_sem.at[1]),
    )

    @pl.when(step == 0)
    def _():
        for load in loads:
            load.start()
        load_outer(True)
        a_output[...] = jnp.zeros_like(a_output)
        a_inner[...] = jnp.zeros_like(a_inner)
        a_outer[...] = jnp.zeros_like(a_outer)
        sums_ref[...] = jnp.zeros_like(sums_ref)
        inner_sum_ref[...] = jnp.zeros_like(inner_sum_ref)

    def vector(i):
        return vectors_ref[i : i + 1, :]

    def add_sum(i, value):
        sums_ref[8 * i : 8 * i + 8, :] += column_sum(value)

    context[:, pl.ds(pl.multiple_of(core * half, 128), half)] = mine_ref[...]
    context[:, pl.ds(pl.multiple_of((1 - core) * half, 128), half)] = other_ref[...]

    @pl.when(step == 0)
    def _():
        loads[0].wait()

    hidden_rows = tokens_ref[...].astype(jnp.float32) + (dot_nn(context[...], w_output[...]) + vector(0))
    normed[...], first_recip = standardize(hidden_rows)
    first[...] = normed[...] * vector(1) + vector(2)
    first_low[...] = first[...].astype(jnp.bfloat16)
    turned_low[...] = first_low[...].T
    work[...] = jnp.broadcast_to(vector(3), work.shape)

    @pl.when(step == 0)
    def _():
        loads[1].wait()
        load_outer(False)

    def part(c):
        return pl.ds(pl.multiple_of(c * CHUNK, CHUNK), CHUNK)

    def forward(c, _):
        u = dot_nn(first_low[...], w_inner[:, part(c)]) + bias_inner_ref[0:1, part(c)]
        cdf = 0.5 * (1.0 + lax.erf(u * ROOT_HALF))
        slope[:, part(c)] = cdf + u * jnp.exp(-0.5 * u * u) * INV_ROOT_TAU
        active[:, part(c)] = (u * cdf).astype(jnp.bfloat16)
        work[...] += dot_nn(active[:, part(c)], w_outer[part(c), :])
        return 0

    lax.fori_loop(0, chunks, forward, 0)
    second, second_recip = standardize(first[...] + work[...])
    mixed_ref[...] = (second * vector(4) + vector(5)).astype(jnp.bfloat16)
    upstream = jnp.where(step < steps // 2, cot_ref[0], cot_far_ref[...]).astype(jnp.float32)
    add_sum(0, upstream * second)
    add_sum(1, upstream)
    scaled = upstream * vector(4)
    pre_second = second_recip * (scaled - row_mean(scaled) - second * row_mean(scaled * second))
    grad_outer = pre_second.astype(jnp.bfloat16)
    add_sum(2, grad_outer.astype(jnp.float32))
    work[...] = pre_second
    stage[0, 0:TILE, :] = grad_outer

    def backward(c, _):
        grad_out = stage[0, 0:TILE, :]
        grad = dot_nt(grad_out, w_outer[part(c), :])
        grad_inner = (grad * slope[:, part(c)]).astype(jnp.bfloat16)
        inner_sum_ref[:, part(c)] += column_sum(grad_inner.astype(jnp.float32))
        a_outer[part(c), :] += dot_nn(active[:, part(c)].T, grad_out)
        a_inner[:, part(c)] += dot_nn(turned_low[...], grad_inner)
        work[...] += dot_nt(grad_inner, w_inner[:, part(c)])
        return 0

    lax.fori_loop(0, chunks, backward, 0)
    grad_first = work[...]
    add_sum(3, grad_first * normed[...])
    add_sum(4, grad_first)
    scaled = grad_first * vector(1)
    pre_first = first_recip * (scaled - row_mean(scaled) - normed[...] * row_mean(scaled * normed[...]))
    pre_first_ref[...] = pre_first
    grad_attended = pre_first.astype(jnp.bfloat16)
    add_sum(5, grad_attended.astype(jnp.float32))
    a_output[...] += dot_nn(context[...].T, grad_attended)
    context[...] = dot_nt(grad_attended, w_output[...]).astype(jnp.bfloat16)
    grad_mine_ref[...] = context[:, pl.ds(pl.multiple_of(core * half, 128), half)]
    grad_other_ref[...] = context[:, pl.ds(pl.multiple_of((1 - core) * half, 128), half)]

    @pl.when(step == steps - 1)
    def _():
        grad_output_ref[...] = a_output[...].astype(jnp.bfloat16)

        def inner_copy(c, slot):
            return pltpu.make_async_copy(stage.at[slot], terms_hbm.at[:, part(c)], store_sem.at[slot])

        def outer_wait(slot):
            pltpu.make_async_copy(stage.at[slot], stage.at[slot], store_sem.at[slot]).wait()

        def outer_start(c, slot):
            if not direct:
                pltpu.make_async_copy(stage.at[slot], outer_terms_hbm.at[part(c), :], store_sem.at[slot]).start()
                return
            groups = CHUNK // (rows * ratio)
            for s in range(groups):
                for q in range(ratio):
                    src = stage.at[slot, pl.ds((s * ratio + q) * rows, rows), :]
                    dst = terms_hbm.at[
                        pl.ds(pl.multiple_of((c * groups + s) * rows, rows), rows), pl.ds(hidden + q * width, width)
                    ]
                    pltpu.make_async_copy(src, dst, store_sem.at[slot]).start()

        for c in range(chunks):
            if c > 0:
                inner_copy(c - 1, 0).wait()
                outer_wait(1)
            stage[0] = a_inner[:, part(c)].astype(jnp.bfloat16)
            inner_copy(c, 0).start()
            stage[1] = a_outer[part(c), :].astype(jnp.bfloat16)
            outer_start(c, 1)
        inner_copy(chunks - 1, 0).wait()
        outer_wait(1)


def dense_layer(where, tokens, mine, other, cotangent, cotangent_far, vectors, bias_inner, weights, outer, pieces, direct):
    local, half = mine.shape
    width = 2 * half
    hidden = bias_inner.shape[1]
    steps = local // TILE
    rows = width // pieces
    low, high = jnp.bfloat16, jnp.float32
    tile = pl.BlockSpec((TILE, width), lambda t, *_: (t, 0))
    half_tile = pl.BlockSpec((TILE, half), lambda t, *_: (t, 0))
    anywhere = pl.BlockSpec(memory_space=pl.ANY)
    halfway = steps // 2

    def whole(shape):
        return pl.BlockSpec(shape, lambda t, *_: (0, 0))

    terms_shape = (width, 2 * hidden if direct else hidden)
    outer_shape = (8, 128) if direct else (hidden, width)
    return pl.pallas_call(
        lambda *refs: dense_kernel(direct, pieces, *refs),
        out_shape=(
            jax.ShapeDtypeStruct((local, width), low),
            jax.ShapeDtypeStruct((local, width), high),
            jax.ShapeDtypeStruct((local, half), low),
            jax.ShapeDtypeStruct((local, half), low),
            jax.ShapeDtypeStruct((48, width), high),
            jax.ShapeDtypeStruct((8, hidden), high),
            jax.ShapeDtypeStruct((width, width), low),
            jax.ShapeDtypeStruct(terms_shape, low),
            jax.ShapeDtypeStruct(outer_shape, low),
        ),
        grid_spec=pltpu.PrefetchScalarGridSpec(
            num_scalar_prefetch=1,
            grid=(steps,),
            in_specs=[
                tile,
                half_tile,
                half_tile,
                pl.BlockSpec((1, TILE, width), lambda t, where: (where[1], jnp.minimum(t, halfway - 1), 0)),
                pl.BlockSpec((TILE, width), lambda t, *_: (jnp.maximum(t - halfway, 0), 0)),
                whole((8, width)),
                whole((1, hidden)),
                anywhere,
                anywhere,
            ],
            out_specs=[
                tile,
                tile,
                half_tile,
                half_tile,
                whole((48, width)),
                whole((8, hidden)),
                whole((width, width)),
                anywhere,
                anywhere,
            ],
            scratch_shapes=[
                pltpu.VMEM((width, width), low),
                pltpu.VMEM((width, hidden), low),
                pltpu.VMEM((hidden, width), low),
                pltpu.VMEM((width, width), high),
                pltpu.VMEM((width, hidden), high),
                pltpu.VMEM((hidden, width), high),
                pltpu.VMEM((2, width, CHUNK), low),
                pltpu.VMEM((TILE, width), low),
                pltpu.VMEM((TILE, width), low),
                pltpu.VMEM((width, TILE), low),
                pltpu.VMEM((TILE, width), high),
                pltpu.VMEM((TILE, width), high),
                pltpu.VMEM((TILE, hidden), high),
                pltpu.VMEM((TILE, hidden), low),
                pltpu.VMEM((TILE, width), high),
                pltpu.SemaphoreType.DMA((2,)),
                pltpu.SemaphoreType.DMA,
                pltpu.SemaphoreType.DMA((2,)),
            ],
        ),
        compiler_params=pltpu.CompilerParams(dimension_semantics=("arbitrary",), vmem_limit_bytes=66_000_000),
        cost_estimate=pl.CostEstimate(flops=32_000_000_000, bytes_accessed=40_000_000, transcendentals=6_000_000),
        name="dense_layer",
    )(where, tokens, mine, other, cotangent, cotangent_far, vectors, bias_inner, weights, outer)


MESH_ID = pl.DeviceIdType.MESH


def place_of():
    return tuple(lax.axis_index(name) for name in ("z", "x", "y", "core"))


def sizes_of():
    return lax.axis_size("z"), lax.axis_size("x")


def partner(**moved):
    z, x, y, core = place_of()
    return (moved.get("z", z), moved.get("x", x), moved.get("y", y), moved.get("core", core))


def greet(with_grid):
    z, x, y, core = place_of()
    size_z, size_x = sizes_of()
    peers = [partner(y=1 - y), partner(core=1 - core)]
    if with_grid:
        peers += [partner(z=lax.rem(z + k, size_z)) for k in range(1, size_z)]
        peers += [partner(x=lax.rem(x + j, size_x)) for j in range(1, size_x)]
    barrier = pltpu.get_barrier_semaphore()
    for peer in peers:
        pl.semaphore_signal(barrier, inc=1, device_id=peer, device_id_type=MESH_ID)
    pl.semaphore_wait(barrier, len(peers))


def remote(src, dst, send, recv, peer):
    return pltpu.make_async_remote_copy(
        src_ref=src, dst_ref=dst, send_sem=send, recv_sem=recv, device_id=peer, device_id_type=MESH_ID
    )


def entry_kernel(size_z, size_x, count, *refs):
    tokens, cotangent, wq, wk, wv = refs[:5]
    vectors = refs[5 : 5 + count]
    tokens_all, cotangent_far, weights_all, vectors_all = refs[5 + count : 9 + count]
    raw = refs[9 + count : 9 + 2 * count]
    stage, wbuf, pack, vpack, local_sem, load_sem, tsend, trecv, zsend, zrecv, xsend, xrecv = refs[9 + 2 * count :]
    z, x, y, core = place_of()
    half = pack.shape[1] // 3
    pairs = half // 128
    me = z * size_x + x

    mine = pl.ds(pl.multiple_of(core * half, 128), half)
    loads = [pltpu.make_async_copy(w.at[:, mine], wbuf.at[i], load_sem.at[i]) for i, w in enumerate((wq, wk, wv))]
    loads += [pltpu.make_async_copy(v, r, load_sem.at[3 + i]) for i, (v, r) in enumerate(zip(vectors, raw))]
    for load in loads:
        load.start()
    load = pltpu.make_async_copy(tokens.at[y], stage, local_sem.at[0])
    load.start()
    vpack[...] = jnp.zeros_like(vpack)
    for copy in loads:
        copy.wait()
    for i, vector in enumerate(raw):
        vpack[i : i + 1, 0 : vector.shape[1]] = vector[...].astype(jnp.bfloat16).astype(jnp.float32)
    for i in range(3):
        for p in range(pairs):
            pack[:, (3 * p + i) * 128 : (3 * p + i + 1) * 128] = wbuf[i, :, p * 128 : (p + 1) * 128].astype(jnp.bfloat16)
    greet(True)
    across = remote(tokens.at[1 - y], tokens_all.at[1], tsend.at[0], trecv.at[0], partner(y=1 - y))
    across.start()
    along = []
    for k in range(1, size_z):
        peer = partner(z=lax.rem(z + k, size_z))
        along.append(
            (
                remote(pack, weights_all.at[me], zsend.at[0, k - 1], zrecv.at[0, k - 1], peer),
                remote(vpack, vectors_all.at[me], zsend.at[1, k - 1], zrecv.at[1, k - 1], peer),
            )
        )
    beside = remote(tokens.at[y], tokens_all.at[2], tsend.at[1], trecv.at[1], partner(core=1 - core))
    sideways = []

    def forward(k, weights_src, vectors_src):
        slot = lax.rem(z - k + size_z, size_z) * size_x + x
        for j in range(1, size_x):
            peer = partner(x=lax.rem(x + j, size_x))
            first = remote(weights_src, weights_all.at[slot], xsend.at[0, k, j - 1], xrecv.at[0, k, j - 1], peer)
            second = remote(vectors_src, vectors_all.at[slot], xsend.at[1, k, j - 1], xrecv.at[1, k, j - 1], peer)
            first.start()
            second.start()
            sideways.append((first, second))

    forward(0, pack, vpack)
    for first, second in along:
        first.start()
        second.start()
    beside.start()
    keep_weights = pltpu.make_async_copy(pack, weights_all.at[me], local_sem.at[1])
    keep_vectors = pltpu.make_async_copy(vpack, vectors_all.at[me], local_sem.at[2])
    keep_weights.start()
    keep_vectors.start()
    load.wait()
    keep_tokens = pltpu.make_async_copy(stage, tokens_all.at[0], local_sem.at[3])
    keep_tokens.start()
    order = sorted(range(1, size_z), key=lambda k: min(k, size_z - k))
    for k in order:
        first, second = along[k - 1]
        first.wait_recv()
        second.wait_recv()
        slot = lax.rem(z - k + size_z, size_z) * size_x + x
        forward(k, weights_all.at[slot], vectors_all.at[slot])
    across.wait_recv()
    onward = remote(tokens_all.at[1], tokens_all.at[3], tsend.at[2], trecv.at[2], partner(core=1 - core))
    onward.start()
    later = remote(cotangent.at[1 - y], cotangent_far, tsend.at[3], trecv.at[3], partner(y=1 - y))
    later.start()
    for first, second in sideways:
        first.wait()
        second.wait()
    for first, second in along:
        first.wait_send()
        second.wait_send()
    across.wait_send()
    beside.wait()
    onward.wait()
    later.wait()
    keep_weights.wait()
    keep_vectors.wait()
    keep_tokens.wait()


def entry(size_z, size_x, tokens, cotangent, wq, wk, wv, vectors):
    _, part, width = tokens.shape
    rows = wq.shape[0]
    lanes = wq.shape[1] // 2 * 3
    longest = max(v.shape[0] for v in vectors)
    shards = size_z * size_x
    anywhere = pl.BlockSpec(memory_space=pl.ANY)
    dma = pltpu.SemaphoreType.DMA
    return pl.pallas_call(
        lambda *refs: entry_kernel(size_z, size_x, len(vectors), *refs),
        out_shape=(
            jax.ShapeDtypeStruct((4, part, width), tokens.dtype),
            jax.ShapeDtypeStruct((part, width), cotangent.dtype),
            jax.ShapeDtypeStruct((shards, rows, lanes), jnp.bfloat16),
            jax.ShapeDtypeStruct((shards, 16, longest), jnp.float32),
        ),
        in_specs=[anywhere] * (5 + len(vectors)),
        out_specs=(anywhere,) * 4,
        scratch_shapes=[pltpu.VMEM((1, v.shape[0]), v.dtype) for v in vectors]
        + [
            pltpu.VMEM((part, width), tokens.dtype),
            pltpu.VMEM((3, rows, lanes // 3), wq.dtype),
            pltpu.VMEM((rows, lanes), jnp.bfloat16),
            pltpu.VMEM((16, longest), jnp.float32),
            dma((4,)),
            dma((3 + len(vectors),)),
            dma((4,)),
            dma((4,)),
            dma((2, size_z - 1)),
            dma((2, size_z - 1)),
            dma((2, size_z, max(size_x - 1, 1))),
            dma((2, size_z, max(size_x - 1, 1))),
        ],
        compiler_params=pltpu.CompilerParams(collective_id=0, has_side_effects=True, vmem_limit_bytes=20 << 20),
        name="entry",
    )(tokens, cotangent, wq, wk, wv, *[v.reshape(1, -1) for v in vectors])


def exit_kernel(
    size_z,
    size_x,
    direct,
    grads_hbm,
    inputs_hbm,
    weights_hbm,
    base_hbm,
    terms_hbm,
    output_term,
    vector_terms,
    dense_hbm,
    token_grads,
    grad_query,
    grad_key,
    grad_value,
    grad_output,
    grad_inner,
    grad_outer,
    vector_sums,
    grads,
    inputs,
    turned,
    weights,
    base,
    terms,
    other_rows,
    recv_rows,
    send_rows,
    far_rows,
    odd,
    dense_own,
    dense_far,
    dense_core,
    xbuf,
    xvec,
    zout,
    zvout,
    zbuf,
    zvec,
    ybuf,
    yvec,
    cbuf,
    cvec,
    load_sem,
    tsend,
    trecv,
    osend,
    orecv,
    dsend,
    drecv,
    xsend,
    xrecv,
    zsend,
    zrecv,
    ysend,
    yrecv,
    csend,
    crecv,
):
    z, x, y, core = place_of()
    shards, rows, lanes = terms.shape
    width = grads_hbm.shape[1] * 2 // 3
    half = width // 2
    pairs = half // 128
    hidden = grad_inner.shape[1]
    part = token_grads.shape[1]
    local = 2 * part
    mine = pl.ds(pl.multiple_of(core * half, 128), half)
    theirs = pl.ds(pl.multiple_of((1 - core) * half, 128), half)
    order = sorted(range(size_z), key=lambda k: -min(k, size_z - k))
    loads = [
        pltpu.make_async_copy(src, dst, load_sem.at[i])
        for i, (src, dst) in enumerate(
            (
                (inputs_hbm, inputs),
                (grads_hbm, grads),
                (weights_hbm, weights),
                (base_hbm, base),
                (dense_hbm, dense_own),
            )
            + (() if direct else ((terms_hbm, terms),))
        )
    ]
    for load in loads:
        load.start()
    greet(True)

    outputs = remote(output_term.at[:, :, theirs], odd, osend, orecv, partner(core=1 - core))
    outputs.start()
    dense_move = remote(dense_hbm, dense_far, dsend.at[0], drecv.at[0], partner(y=1 - y))
    dense_move.start()
    sideways = {}

    def send_side(n, k, src, dst, lane=None):
        for j in range(1, size_x):
            column = lax.rem(x + j, size_x)
            slot = lax.rem(z + k, size_z) * size_x + column
            view = src.at[slot] if lane is None else src.at[slot, :, lane]
            move = remote(view, dst(j), xsend.at[n, k, j - 1], xrecv.at[n, k, j - 1], partner(x=column))
            move.start()
            sideways.setdefault((k, j), []).append(move)

    for k in order:
        send_side(0, k, vector_terms, lambda j: xvec.at[j - 1, k])
    loads[0].wait()
    if direct:
        for b in range(4):
            turned[:, b * part : (b + 1) * part] = inputs[b * part : (b + 1) * part, :].T
    loads[1].wait()
    group = min(shards, 4)
    for p in range(pairs):
        block = slice(p * 384, (p + 1) * 384)
        if direct:

            def some(m, _):
                value = dot_nn(turned[pl.ds(pl.multiple_of(m * group * rows, group * rows), group * rows), :], grads[:, block])
                terms[pl.ds(m * group, group), :, block] = value.reshape(group, rows, 384).astype(jnp.bfloat16)
                return 0

            lax.fori_loop(0, shards // group, some, 0)
        elif p == 0:
            loads[5].wait()
        for k in order:
            send_side(1 + p, k, terms, lambda j: xbuf.at[j - 1, k, :, block], block)
    outputs.wait()
    for k in order:
        for j in range(1, size_x):
            slot = lax.rem(z + k, size_z) * size_x + lax.rem(x + j, size_x)
            odd[slot] = (odd[slot].astype(jnp.float32) + output_term[slot, :, mine].astype(jnp.float32)).astype(jnp.bfloat16)
        send_side(1 + pairs, k, odd, lambda j: xbuf.at[j - 1, k, :, lanes : lanes + half])

    loads[2].wait()
    strip = 256

    def product(first):
        at = pl.ds(pl.multiple_of(first, strip), strip)
        return dot_nt(grads[at, :], weights[...])

    def other_strip(i, _):
        other_rows[pl.ds(pl.multiple_of(i * strip, strip), strip), :] = product(local + i * strip).astype(jnp.bfloat16)
        return 0

    lax.fori_loop(0, local // strip, other_strip, 0)
    halves = remote(other_rows, recv_rows, tsend.at[0], trecv.at[0], partner(core=1 - core))
    halves.start()
    loads[3].wait()

    def own_strip(i, _):
        at = pl.ds(pl.multiple_of(i * strip, strip), strip)
        base[at, :] = base[at, :] + product(i * strip)
        return 0

    lax.fori_loop(0, local // strip, own_strip, 0)
    halves.wait()
    send_rows[...] = (base[part:local, :] + recv_rows[part:local, :].astype(jnp.float32)).astype(jnp.bfloat16)
    back = remote(send_rows, far_rows, tsend.at[1], trecv.at[1], partner(y=1 - y))
    back.start()
    token_grads[y] = base[0:part, :] + recv_rows[0:part, :].astype(jnp.float32)

    loads[4].wait()
    dense_move.wait()
    dense_core[0] = dense_own[...].astype(jnp.float32) + dense_far[...].astype(jnp.float32)
    dense_swap = remote(dense_core.at[0], dense_core.at[1], dsend.at[1], drecv.at[1], partner(core=1 - core))
    dense_swap.start()

    along = {}
    kept = None
    for k in order:
        target = lax.rem(z + k, size_z)
        slot = target * size_x + x
        total = terms[slot].astype(jnp.float32)
        total_out = odd[slot].astype(jnp.float32) + output_term[slot, :, mine].astype(jnp.float32)
        total_vec = vector_terms[slot]
        for j in range(1, size_x):
            for move in sideways[k, j]:
                move.wait()
            total = total + xbuf[j - 1, k, :, 0:lanes].astype(jnp.float32)
            total_out = total_out + xbuf[j - 1, k, :, lanes : lanes + half].astype(jnp.float32)
            total_vec = total_vec + xvec[j - 1, k]
        if k == 0:
            kept = (total, total_out, total_vec)
            continue
        zout[k - 1, :, 0:lanes] = total.astype(jnp.bfloat16)
        zout[k - 1, :, lanes : lanes + half] = total_out.astype(jnp.bfloat16)
        zvout[k - 1] = total_vec
        peer = partner(z=target)
        moves = (
            remote(zout.at[k - 1], zbuf.at[k - 1], zsend.at[0, k - 1], zrecv.at[0, k - 1], peer),
            remote(zvout.at[k - 1], zvec.at[k - 1], zsend.at[1, k - 1], zrecv.at[1, k - 1], peer),
        )
        for move in moves:
            move.start()
        along[k] = moves

    dense_swap.wait()
    first = core == 0
    ratio = hidden // width
    count = dense_own.shape[0]
    for i in range(2):
        piece = jnp.where(first, dense_core[i], dense_core[1 - i])
        grad_inner[i * count : (i + 1) * count, :] = piece[:, 0:hidden]
        for q in range(ratio):
            at = (i * ratio + q) * count
            grad_outer[at : at + count, :] = piece[:, hidden + q * width : hidden + (q + 1) * width]

    total, total_out, total_vec = kept
    for k in reversed(order):
        if k == 0:
            continue
        for move in along[k]:
            move.wait()
        total = total + zbuf[k - 1, :, 0:lanes].astype(jnp.float32)
        total_out = total_out + zbuf[k - 1, :, lanes : lanes + half].astype(jnp.float32)
        total_vec = total_vec + zvec[k - 1]
    ybuf[0, :, 0:lanes] = total.astype(jnp.bfloat16)
    ybuf[0, :, lanes : lanes + half] = total_out.astype(jnp.bfloat16)
    yvec[0] = total_vec
    moves = (
        remote(ybuf.at[0], ybuf.at[1], ysend.at[0], yrecv.at[0], partner(y=1 - y)),
        remote(yvec.at[0], yvec.at[1], ysend.at[1], yrecv.at[1], partner(y=1 - y)),
    )
    for move in moves:
        move.start()
    back.wait()
    token_grads[1 - y] = far_rows[...].astype(jnp.float32)
    for move in moves:
        move.wait()
    cbuf[0] = ybuf[0].astype(jnp.float32) + ybuf[1].astype(jnp.float32)
    cvec[0] = yvec[0] + yvec[1]
    moves = (
        remote(cbuf.at[0], cbuf.at[1], csend.at[0], crecv.at[0], partner(core=1 - core)),
        remote(cvec.at[0], cvec.at[1], csend.at[1], crecv.at[1], partner(core=1 - core)),
    )
    for move in moves:
        move.start()
    for move in moves:
        move.wait()
    for i in range(2):
        owner = core if i == 0 else 1 - core
        for p in range(pairs):
            place = pl.ds(pl.multiple_of(owner * half + p * 128, 128), 128)
            for n, out in enumerate((grad_query, grad_key, grad_value)):
                out[:, place] = cbuf[i, :, (3 * p + n) * 128 : (3 * p + n + 1) * 128]
        grad_output[:, pl.ds(pl.multiple_of(owner * half, 128), half)] = cbuf[i, :, lanes : lanes + half]
    vector_sums[...] = cvec[0] + cvec[1]


def exit_call(size_z, size_x, direct, hidden, grads, inputs, weights, base, terms, output_term, vector_terms, dense):
    shards, rows, width = output_term.shape
    lanes = grads.shape[1]
    half = width // 2
    pairs = half // 128
    length = inputs.shape[0]
    local = length // 2
    part = local // 2
    vrows, vlanes = vector_terms.shape[1:]
    count = dense.shape[0]
    vmem, anywhere = pl.BlockSpec(memory_space=pltpu.VMEM), pl.BlockSpec(memory_space=pl.ANY)
    dma = pltpu.SemaphoreType.DMA
    full = lanes + half
    side = max(size_x - 1, 1)
    low, high = jnp.bfloat16, jnp.float32
    matrix = jax.ShapeDtypeStruct((rows, width), high)
    return pl.pallas_call(
        lambda *refs: exit_kernel(size_z, size_x, direct, *refs),
        out_shape=(
            jax.ShapeDtypeStruct((2, part, width), high),
            matrix,
            matrix,
            matrix,
            matrix,
            jax.ShapeDtypeStruct((2 * count, hidden), high),
            jax.ShapeDtypeStruct((2 * count * hidden // width, width), high),
            jax.ShapeDtypeStruct((vrows, vlanes), high),
        ),
        in_specs=[anywhere] * 5 + [vmem] * 2 + [anywhere],
        out_specs=(vmem,) * 8,
        scratch_shapes=[
            pltpu.VMEM((length, lanes), low),
            pltpu.VMEM((length, width), low),
            pltpu.VMEM((width, length) if direct else (16, 128), low),
            pltpu.VMEM((width, lanes), low),
            pltpu.VMEM((local, width), high),
            pltpu.VMEM((shards, rows, lanes), low),
            pltpu.VMEM((local, width), low),
            pltpu.VMEM((local, width), low),
            pltpu.VMEM((part, width), low),
            pltpu.VMEM((part, width), low),
            pltpu.VMEM((shards, rows, half), low),
            pltpu.VMEM(dense.shape, low),
            pltpu.VMEM(dense.shape, low),
            pltpu.VMEM((2,) + dense.shape, high),
            pltpu.VMEM((side, size_z, rows, full), low),
            pltpu.VMEM((side, size_z, vrows, vlanes), high),
            pltpu.VMEM((size_z - 1, rows, full), low),
            pltpu.VMEM((size_z - 1, vrows, vlanes), high),
            pltpu.VMEM((size_z - 1, rows, full), low),
            pltpu.VMEM((size_z - 1, vrows, vlanes), high),
            pltpu.VMEM((2, rows, full), low),
            pltpu.VMEM((2, vrows, vlanes), high),
            pltpu.VMEM((2, rows, full), high),
            pltpu.VMEM((2, vrows, vlanes), high),
            dma((6,)),
            dma((2,)),
            dma((2,)),
            dma,
            dma,
            dma((2,)),
            dma((2,)),
            dma((2 + pairs, size_z, side)),
            dma((2 + pairs, size_z, side)),
            dma((2, size_z - 1)),
            dma((2, size_z - 1)),
            dma((2,)),
            dma((2,)),
            dma((2,)),
            dma((2,)),
        ],
        compiler_params=pltpu.CompilerParams(collective_id=1, has_side_effects=True, vmem_limit_bytes=66_000_000),
        name="exit",
    )(grads, inputs, weights, base, terms, output_term, vector_terms, dense)


def lowered(piece):
    return piece.astype(jnp.bfloat16)


def widen(piece):
    return piece.astype(jnp.float32)


def matmul(left, right):
    return jnp.dot(left, right, preferred_element_type=jnp.float32)


def matmul_tn(left, right):
    return lax.dot_general(
        left, right, (((0,), (0,)), ((), ())), preferred_element_type=jnp.float32
    )


def matmul_nt(left, right):
    return lax.dot_general(
        left, right, (((1,), (1,)), ((), ())), preferred_element_type=jnp.float32
    )


def swap(piece, axis):
    return lax.ppermute(piece, axis, [(0, 1), (1, 0)])


def pick(piece, index, axis=0):
    return lax.dynamic_index_in_dim(piece, index, axis, keepdims=False)


def in_order(first_is_zero, own, other, axis):
    return jnp.where(
        first_is_zero,
        jnp.concatenate([own, other], axis),
        jnp.concatenate([other, own], axis),
    )


def body(
    tokens,
    segment_ids,
    w_query,
    w_key,
    w_value,
    w_output,
    b_query,
    b_value,
    b_output,
    first_gain,
    first_shift,
    w_inner,
    b_inner,
    w_outer,
    b_outer,
    second_gain,
    second_shift,
    cotangent,
):
    core, y = lax.axis_index("core"), lax.axis_index("y")
    size_z, size_x = lax.axis_size("z"), lax.axis_size("x")
    shards = size_z * size_x
    everyone = ("z", "x", "core")
    sequences, part, width = tokens.shape
    half = width // 2
    pairs = half // 128
    hidden = w_inner.shape[1]
    local = 2 * part
    own_rows = w_query.shape[0]
    lanes = 3 * half

    stack = hidden // width

    def core_rows(matrix):
        rows = matrix.shape[0] // 2
        return lowered(lax.dynamic_slice_in_dim(matrix, core * rows, rows, 0))

    def side_by_side(matrix, groups):
        rows = matrix.shape[0] // groups // stack
        return matrix.reshape(groups, stack, rows, width).transpose(0, 2, 1, 3).reshape(groups * rows, hidden)

    def stacked(matrix, groups):
        rows = matrix.shape[0] // groups
        return matrix.reshape(groups, rows, stack, width).transpose(0, 2, 1, 3).reshape(groups * rows * stack, width)

    pieces = (core_rows(w_inner), core_rows(w_output), side_by_side(core_rows(w_outer), 1))
    dense = lax.all_gather(jnp.concatenate(pieces, axis=1), everyone, axis=0, tiled=True)
    pieces_count = 2 * shards
    direct = (width // pieces_count) % 16 == 0
    if direct:
        full_outer = dense
    else:
        full_outer = stacked(dense[:, hidden + width :], pieces_count)

    vectors = (b_query, b_value, b_output, first_gain, first_shift, b_inner, b_outer, second_gain, second_shift)
    sizes = [v.shape[0] for v in vectors]
    tokens_all, cotangent_far, early, vectors_all = entry(size_z, size_x, tokens, cotangent, w_query, w_key, w_value, vectors)
    inputs_all = tokens_all.reshape(4 * part, width)
    full_early = early.reshape(width, lanes)
    bias_query, bias_value, bias_output, gain_first, shift_first, bias_inner, bias_outer, gain_second, shift_second = [
        vectors_all[:, i, :size].reshape(shards * size) for i, size in enumerate(sizes)
    ]
    heads_query = lax.dynamic_slice_in_dim(bias_query, core * half, half).reshape(pairs, 1, 128)
    heads_value = lax.dynamic_slice_in_dim(bias_value, core * half, half).reshape(pairs, 1, 128)
    bias_all = jnp.concatenate([heads_query, jnp.zeros_like(heads_query), heads_value], axis=1).reshape(lanes)
    scale = jnp.tile(jnp.concatenate([jnp.full((128,), HD ** (-0.5)), jnp.ones((256,))]), pairs)
    projected = lowered((matmul(inputs_all, full_early) + bias_all) * scale)

    spot = jnp.arange(5, dtype=jnp.int32)
    place = jnp.where(spot < 4, ((spot % 2 != core) * 2 + (spot // 2 != y) * 1) * part, core)
    segments = pick(segment_ids, y)
    context_mine, context_other, logsum = attention(place, segments, projected)
    norms = jnp.stack([bias_output, gain_first, shift_first, bias_outer, gain_second, shift_second])
    norms = jnp.concatenate([norms, jnp.zeros((2, width), jnp.float32)], axis=0)
    mixed, pre_first, upstream_mine, upstream_send, dense_sums, inner_sums, grad_w_output, terms, outer_terms = dense_layer(
        jnp.stack([core, y]).astype(jnp.int32),
        inputs_all,
        context_mine,
        swap(context_other, "core"),
        cotangent,
        cotangent_far,
        norms,
        bias_inner.reshape(1, hidden),
        dense,
        full_outer,
        pieces_count,
        direct,
    )
    if not direct:
        terms = jnp.concatenate([terms, side_by_side(outer_terms, pieces_count)], axis=1)
    both_done = lax.psum_scatter(terms, everyone, scatter_dimension=0, tiled=True)
    upstream_other = swap(upstream_send, "core")
    dense_sums = jnp.sum(dense_sums.reshape(6, 8, width), axis=1)
    grad_second_gain, grad_second_shift, grad_b_outer, grad_first_gain, grad_first_shift, grad_b_output = [
        dense_sums[i] for i in range(6)
    ]
    grad_b_inner = jnp.sum(inner_sums, axis=0)
    mixed_out = in_order(y == 0, mixed[None, :part], swap(mixed[part:], "y")[None], 0)

    grads, sums = attention_back(place, segments, projected, context_mine, context_other, upstream_mine, upstream_other, logsum)
    if direct:
        grad_early = grads
    else:
        grad_early = lowered(matmul_tn(inputs_all, grads)).reshape(shards, own_rows, lanes)
    sums = sums.reshape(pairs, 8, 3, 128)[:, 0]
    blank = jnp.zeros((width,), jnp.float32)
    grad_b_query = lax.dynamic_update_slice(blank, sums[:, 0].reshape(half), (core * half,))
    grad_b_value = lax.dynamic_update_slice(blank, sums[:, 2].reshape(half), (core * half,))
    vector_grads = (
        grad_b_query,
        grad_b_value,
        grad_b_output,
        grad_first_gain,
        grad_first_shift,
        grad_b_inner,
        grad_b_outer,
        grad_second_gain,
        grad_second_shift,
    )
    longest = vectors_all.shape[2]
    rows = [jnp.pad(v.reshape(shards, 1, -1), ((0, 0), (0, 0), (0, longest - v.shape[0] // shards))) for v in vector_grads]
    rows.append(jnp.zeros((shards, vectors_all.shape[1] - len(rows), longest), jnp.float32))
    vector_terms = jnp.concatenate(rows, axis=1)
    grad_tokens, grad_query, grad_key, grad_value, grad_output, grad_inner_full, grad_outer_full, vector_sums = exit_call(
        size_z,
        size_x,
        direct,
        hidden,
        grads,
        inputs_all,
        full_early,
        pre_first,
        grad_early,
        grad_w_output.reshape(shards, own_rows, width),
        vector_terms,
        both_done,
    )
    done = [vector_sums[i, :size] for i, size in enumerate(sizes)]
    return (
        mixed_out,
        grad_tokens,
        grad_query,
        grad_key,
        grad_value,
        grad_output,
        done[0],
        done[1],
        done[2],
        done[3],
        done[4],
        grad_inner_full,
        done[5],
        grad_outer_full,
        done[6],
        done[7],
        done[8],
    )


def solution(mesh):
    outer, inner = mesh.devices.shape
    size_z = 1
    while size_z * size_z < outer:
        size_z *= 2
    split = Mesh(mesh.devices.reshape(size_z, outer // size_z, inner // 2, 2), ("z", "x", "y", "core"))
    dp, seq = ("z", "x"), ("y", "core")
    activation, matrix, vector = P(dp, seq, None), P(dp, None), P(dp)
    return jax.shard_map(
        body,
        mesh=split,
        in_specs=(
            activation,
            matrix,
            matrix,
            matrix,
            matrix,
            matrix,
            vector,
            vector,
            vector,
            vector,
            vector,
            matrix,
            vector,
            matrix,
            vector,
            vector,
            vector,
            activation,
        ),
        out_specs=(
            activation,
            activation,
            matrix,
            matrix,
            matrix,
            matrix,
            vector,
            vector,
            vector,
            vector,
            vector,
            matrix,
            vector,
            matrix,
            vector,
            vector,
            vector,
        ),
        check_vma=False,
    )
```

```python
import jax
import jax.numpy as jnp
from jax import lax
from jax.experimental import pallas as pl
from jax.experimental.pallas import tpu as pltpu
from jax.sharding import Mesh
from jax.sharding import PartitionSpec as P


HD = 64
EPS = 1e-12
ROOT_HALF = 0.7071067811865476
INV_ROOT_TAU = 0.3989422804014327

BLK = 256
BIG = -1.0e9
DOCUMENTS = 4


def dot_nn(a, b):
    return jnp.dot(a, b, preferred_element_type=jnp.float32)


def part_rows(place_ref, part, rows):
    return pl.ds(pl.multiple_of(place_ref[part], 128), rows)


def find_bounds(segment_ref, bound_ref):
    length = segment_ref.shape[0]
    bound_ref[0] = 0
    bound_ref[DOCUMENTS] = length
    for d in range(1, DOCUMENTS):

        def halve(_, span):
            low, high = span
            middle = (low + high) // 2
            below = segment_ref[jnp.minimum(middle, length - 1)] < d
            inside = low < high
            return (
                jnp.where(jnp.logical_and(inside, below), middle + 1, low),
                jnp.where(jnp.logical_and(inside, jnp.logical_not(below)), middle, high),
            )

        low, _ = lax.fori_loop(0, length.bit_length(), halve, (0, length))
        bound_ref[d] = low


def find_window(segment_ref, bound_ref, qb):
    length = segment_ref.shape[0]
    first = segment_ref[qb * BLK]
    last = segment_ref[qb * BLK + BLK - 1]
    start = bound_ref[first] // 128 * 128
    count = (bound_ref[last + 1] - start + BLK - 1) // BLK
    return jnp.minimum(start, length - count * BLK), count


def each_tile(count, step):
    def two(i, _):
        step(i * (2 * BLK), 2 * BLK)
        return 0

    lax.fori_loop(0, count // 2, two, 0)

    @pl.when(count % 2 == 1)
    def _():
        step((count - 1) * BLK, BLK)


def make_marks(row_ref, mark_query, mark_key):
    length = mark_key.shape[0]
    step = 512
    for b in range(length // step):
        rows = slice(b * step, (b + 1) * step)
        column = jnp.broadcast_to(row_ref[0:1, rows], (128, step)).T
        lane = lax.broadcasted_iota(jnp.int32, (step, 128), 1) % 64
        same = lane == column
        line = lax.broadcasted_iota(jnp.int32, (128, step), 0) % 64
        mark_query[:, rows] = jnp.where(line == row_ref[0:1, rows], 1.0, 0.0).astype(jnp.bfloat16)
        apart = jnp.logical_and(lane < DOCUMENTS, jnp.logical_not(same))
        mark_key[rows, :] = jnp.where(apart, BIG, 0.0).astype(jnp.bfloat16)


def forward_kernel(
    place_ref, segment_ref, qkv_ref, row_ref, mine_ref, other_ref, lse_ref, q2, k2, vt, acc, top, tot, keep, mark_query, mark_key, bound_ref
):
    length = qkv_ref.shape[0]
    blocks = length // BLK
    part = length // 4

    @pl.when(pl.program_id(0) == 0)
    def _():
        find_bounds(segment_ref, bound_ref)
        make_marks(row_ref, mark_query, mark_key)

    low = lax.broadcasted_iota(jnp.int32, (part, 128), 1) < 64
    for b in range(4):
        src = part_rows(place_ref, b, part)
        dst = slice(b * part, (b + 1) * part)
        k, nohk = qkv_ref[src, 128:256], mark_key[dst, :]
        turned = qkv_ref[src, 0:128].T
        q2[0, 0:64, dst] = turned[0:64]
        q2[0, 64:128, dst] = mark_query[64:128, dst]
        q2[1, 0:64, dst] = mark_query[0:64, dst]
        q2[1, 64:128, dst] = turned[64:128]
        k2[0, dst, :] = jnp.where(low, k, nohk)
        k2[1, dst, :] = jnp.where(low, nohk, k)
        vt[:, dst] = qkv_ref[src, 256:384].T
    lse_ref[...] = jnp.zeros_like(lse_ref)

    def row(qb, _):
        qs = pl.ds(pl.multiple_of(qb * BLK, BLK), BLK)
        start, count = find_window(segment_ref, bound_ref, qb)
        top[...] = jnp.full_like(top, -1.0e30)

        def fold(tile, function):
            return function(tile.reshape(tile.shape[0] // 8, 8, BLK), axis=0)

        def highest(first, size):
            keys = pl.ds(pl.multiple_of(start + first, 128), size)
            for h in range(2):
                st = dot_nn(k2[h, keys, :], q2[h, :, qs])
                keep[h, pl.ds(pl.multiple_of(first, BLK), size), :] = st
                top[h] = jnp.maximum(top[h], fold(st, jnp.max))

        def weigh(first, size, largest):
            keys = pl.ds(pl.multiple_of(start + first, 128), size)
            for h in range(2):
                rows = slice(64 * h, 64 * h + 64)
                st = keep[h, pl.ds(pl.multiple_of(first, BLK), size), :]
                p = jnp.exp(st - largest[h])
                tot[h] = tot[h] + fold(p, jnp.sum)
                acc[rows, :] = acc[rows, :] + dot_nn(vt[rows, keys], p.astype(jnp.bfloat16))

        def paired(step):
            each_tile(count, step)

        paired(highest)
        largest = [jnp.max(top[h], axis=0, keepdims=True) for h in range(2)]
        acc[...] = jnp.zeros_like(acc)
        tot[...] = jnp.zeros_like(tot)
        paired(lambda first, size: weigh(first, size, largest))
        for h in range(2):
            rows = slice(64 * h, 64 * h + 64)
            total = jnp.sum(tot[h], axis=0, keepdims=True)
            acc[rows, :] = acc[rows, :] / total
            lse_ref[h : h + 1, qs] = largest[h] + jnp.log(total)
        where = place_ref[qb * BLK // part] + qb * BLK % part
        result = acc[...].T.astype(jnp.bfloat16)

        @pl.when(where < 2 * part)
        def _():
            mine_ref[pl.ds(pl.multiple_of(where, BLK), BLK), :] = result

        @pl.when(where >= 2 * part)
        def _():
            other_ref[pl.ds(pl.multiple_of(where - 2 * part, BLK), BLK), :] = result

        return 0

    lax.fori_loop(0, blocks, row, 0)


def attention(place, segments, qkv):
    length, width = qkv.shape
    pairs = width // 384
    rows = length // 2
    return pl.pallas_call(
        forward_kernel,
        out_shape=(
            jax.ShapeDtypeStruct((rows, pairs * 128), jnp.bfloat16),
            jax.ShapeDtypeStruct((rows, pairs * 128), jnp.bfloat16),
            jax.ShapeDtypeStruct((pairs * 8, length), jnp.float32),
        ),
        grid_spec=pltpu.PrefetchScalarGridSpec(
            num_scalar_prefetch=2,
            grid=(pairs,),
            in_specs=[
                pl.BlockSpec((length, 384), lambda p, *_: (0, p)),
                pl.BlockSpec((1, length), lambda p, *_: (0, 0)),
            ],
            out_specs=[
                pl.BlockSpec((rows, 128), lambda p, *_: (0, p)),
                pl.BlockSpec((rows, 128), lambda p, *_: (0, p)),
                pl.BlockSpec((8, length), lambda p, *_: (p, 0)),
            ],
            scratch_shapes=[
                pltpu.VMEM((2, 128, length), jnp.bfloat16),
                pltpu.VMEM((2, length, 128), jnp.bfloat16),
                pltpu.VMEM((128, length), jnp.bfloat16),
                pltpu.VMEM((128, BLK), jnp.float32),
                pltpu.VMEM((2, 8, BLK), jnp.float32),
                pltpu.VMEM((2, 8, BLK), jnp.float32),
                pltpu.VMEM((2, length, BLK), jnp.float32),
                pltpu.VMEM((128, length), jnp.bfloat16),
                pltpu.VMEM((length, 128), jnp.bfloat16),
                pltpu.SMEM((DOCUMENTS + 1,), jnp.int32),
            ],
        ),
        compiler_params=pltpu.CompilerParams(dimension_semantics=("arbitrary",), vmem_limit_bytes=60 << 20),
        cost_estimate=pl.CostEstimate(flops=pairs * 8_000_000_000, bytes_accessed=pairs * 3_000_000, transcendentals=pairs * 4_000_000),
        name="attention_forward",
    )(place, segments, qkv, segments.reshape(1, length))


def backward_kernel(
    place_ref,
    segment_ref,
    qkv_ref,
    ctx_mine_ref,
    ctx_other_ref,
    do_mine_ref,
    do_other_ref,
    lse_ref,
    row_ref,
    out_ref,
    sum_ref,
    q2,
    k2,
    q0,
    d0,
    dt,
    v0,
    kt,
    dk,
    dv,
    dqt,
    delta,
    mark_query,
    mark_key,
    bound_ref,
):
    length = qkv_ref.shape[0]
    blocks = length // BLK
    part = length // 4

    @pl.when(pl.program_id(0) == 0)
    def _():
        find_bounds(segment_ref, bound_ref)
        make_marks(row_ref, mark_query, mark_key)

    low = lax.broadcasted_iota(jnp.int32, (part, 128), 1) < 64

    def prepare(b, do, ctx):
        src = part_rows(place_ref, b, part)
        dst = slice(b * part, (b + 1) * part)
        q, k = qkv_ref[src, 0:128], qkv_ref[src, 128:256]
        zero = jnp.zeros_like(q)
        nohk = mark_key[dst, :]
        turned = q.T
        q2[0, 0:64, dst] = turned[0:64]
        q2[0, 64:128, dst] = mark_query[64:128, dst]
        q2[1, 0:64, dst] = mark_query[0:64, dst]
        q2[1, 64:128, dst] = turned[64:128]
        k2[0, dst, :] = jnp.where(low, k, nohk)
        k2[1, dst, :] = jnp.where(low, nohk, k)
        q0[0, dst, :] = jnp.where(low, q, zero)
        q0[1, dst, :] = jnp.where(low, zero, q)
        d0[0, dst, :] = jnp.where(low, do, zero)
        d0[1, dst, :] = jnp.where(low, zero, do)
        turned = do.T
        blank = jnp.zeros((64, part), jnp.bfloat16)
        dt[0, 0:64, dst] = turned[0:64]
        dt[0, 64:128, dst] = blank
        dt[1, 0:64, dst] = blank
        dt[1, 64:128, dst] = turned[64:128]
        v0[dst, :] = qkv_ref[src, 256:384]
        kt[:, dst] = k.T
        prod = turned.astype(jnp.float32) * ctx.T.astype(jnp.float32)
        delta[0:1, dst] = jnp.sum(prod[0:64], axis=0, keepdims=True)
        delta[1:2, dst] = jnp.sum(prod[64:128], axis=0, keepdims=True)

    for b in range(4):

        @pl.when(place_ref[b] < 2 * part)
        def _():
            rows = part_rows(place_ref, b, part)
            prepare(b, do_mine_ref[rows, :], ctx_mine_ref[rows, :])

        @pl.when(place_ref[b] >= 2 * part)
        def _():
            rows = pl.ds(pl.multiple_of(place_ref[b] - 2 * part, 128), part)
            prepare(b, do_other_ref[rows, :], ctx_other_ref[rows, :])

    dk[...] = jnp.zeros_like(dk)
    dv[...] = jnp.zeros_like(dv)
    dqt[...] = jnp.zeros_like(dqt)

    def row(qb, _):
        qs = pl.ds(pl.multiple_of(qb * BLK, BLK), BLK)
        start, count = find_window(segment_ref, bound_ref, qb)

        def tile(first, size):
            ks = pl.ds(pl.multiple_of(start + first, 128), size)
            weights, grads = [], []
            for h in range(2):
                st = dot_nn(k2[h, ks, :], q2[h, :, qs])
                w = jnp.exp(st - lse_ref[h : h + 1, qs])
                gw = dot_nn(v0[ks, :], dt[h, :, qs])
                weights.append(w.astype(jnp.bfloat16))
                grads.append((w * (gw - delta[h : h + 1, qs])).astype(jnp.bfloat16))
            dv[ks, :] += dot_nn(jnp.concatenate(weights, axis=1), jnp.concatenate([d0[0, qs, :], d0[1, qs, :]], axis=0))
            dk[ks, :] += dot_nn(jnp.concatenate(grads, axis=1), jnp.concatenate([q0[0, qs, :], q0[1, qs, :]], axis=0))
            for h in range(2):
                rows = slice(64 * h, 64 * h + 64)
                dqt[rows, qs] += dot_nn(kt[rows, ks], grads[h])

        each_tile(count, tile)
        return 0

    lax.fori_loop(0, blocks, row, 0)
    sums = [jnp.zeros((1, 128), jnp.float32) for _ in range(3)]
    for b in range(4):
        dst = part_rows(place_ref, b, part)
        src = slice(b * part, (b + 1) * part)
        pieces = ((dqt[:, src].T * 0.125).astype(jnp.bfloat16), dk[src, :].astype(jnp.bfloat16), dv[src, :].astype(jnp.bfloat16))
        for i, piece in enumerate(pieces):
            out_ref[dst, 128 * i : 128 * i + 128] = piece
            sums[i] = sums[i] + jnp.sum(piece.astype(jnp.float32), axis=0, keepdims=True)
    sum_ref[...] = jnp.zeros_like(sum_ref)
    for i in range(3):
        sum_ref[0:1, 128 * i : 128 * i + 128] = sums[i]


def attention_back(place, segments, qkv, ctx_mine, ctx_other, do_mine, do_other, lse):
    length, width = qkv.shape
    pairs = width // 384
    rows = length // 2
    half = lambda: pltpu.VMEM((2, length, 128), jnp.bfloat16)
    turned = lambda: pltpu.VMEM((2, 128, length), jnp.bfloat16)
    column = pl.BlockSpec((rows, 128), lambda p, *_: (0, p))
    return pl.pallas_call(
        backward_kernel,
        out_shape=(
            jax.ShapeDtypeStruct((length, width), jnp.bfloat16),
            jax.ShapeDtypeStruct((pairs * 8, 384), jnp.float32),
        ),
        grid_spec=pltpu.PrefetchScalarGridSpec(
            num_scalar_prefetch=2,
            grid=(pairs,),
            in_specs=[
                pl.BlockSpec((length, 384), lambda p, *_: (0, p)),
                column,
                column,
                column,
                column,
                pl.BlockSpec((8, length), lambda p, *_: (p, 0)),
                pl.BlockSpec((1, length), lambda p, *_: (0, 0)),
            ],
            out_specs=[
                pl.BlockSpec((length, 384), lambda p, *_: (0, p)),
                pl.BlockSpec((8, 384), lambda p, *_: (p, 0)),
            ],
            scratch_shapes=[
                turned(),
                half(),
                half(),
                half(),
                turned(),
                pltpu.VMEM((length, 128), jnp.bfloat16),
                pltpu.VMEM((128, length), jnp.bfloat16),
                pltpu.VMEM((length, 128), jnp.float32),
                pltpu.VMEM((length, 128), jnp.float32),
                pltpu.VMEM((128, length), jnp.float32),
                pltpu.VMEM((8, length), jnp.float32),
                pltpu.VMEM((128, length), jnp.bfloat16),
                pltpu.VMEM((length, 128), jnp.bfloat16),
                pltpu.SMEM((DOCUMENTS + 1,), jnp.int32),
            ],
        ),
        compiler_params=pltpu.CompilerParams(dimension_semantics=("arbitrary",), vmem_limit_bytes=60 << 20),
        cost_estimate=pl.CostEstimate(flops=pairs * 20_000_000_000, bytes_accessed=pairs * 5_000_000, transcendentals=pairs * 4_000_000),
        name="attention_backward",
    )(place, segments, qkv, ctx_mine, ctx_other, do_mine, do_other, lse, segments.reshape(1, length))


MESH_ID = pl.DeviceIdType.MESH


def place_of():
    return tuple(lax.axis_index(name) for name in ("z", "x", "y", "core"))


def sizes_of():
    return lax.axis_size("z"), lax.axis_size("x")


def partner(**moved):
    z, x, y, core = place_of()
    return (moved.get("z", z), moved.get("x", x), moved.get("y", y), moved.get("core", core))


def greet(with_grid):
    z, x, y, core = place_of()
    size_z, size_x = sizes_of()
    peers = [partner(y=1 - y), partner(core=1 - core)]
    if with_grid:
        peers += [partner(z=lax.rem(z + k, size_z)) for k in range(1, size_z)]
        peers += [partner(x=lax.rem(x + j, size_x)) for j in range(1, size_x)]
    barrier = pltpu.get_barrier_semaphore()
    for peer in peers:
        pl.semaphore_signal(barrier, inc=1, device_id=peer, device_id_type=MESH_ID)
    pl.semaphore_wait(barrier, len(peers))


def remote(src, dst, send, recv, peer):
    return pltpu.make_async_remote_copy(
        src_ref=src, dst_ref=dst, send_sem=send, recv_sem=recv, device_id=peer, device_id_type=MESH_ID
    )


def entry_kernel(size_z, size_x, count, *refs):
    tokens, cotangent, wq, wk, wv = refs[:5]
    vectors = refs[5 : 5 + count]
    tokens_all, cotangent_all, weights_all, vectors_all = refs[5 + count : 9 + count]
    raw = refs[9 + count : 9 + 2 * count]
    stage, cot_stage, wbuf, pack, vpack, local_sem, load_sem, tsend, trecv, zsend, zrecv, xsend, xrecv = refs[9 + 2 * count :]
    z, x, y, core = place_of()
    half = pack.shape[1] // 3
    pairs = half // 128
    me = z * size_x + x

    mine = pl.ds(pl.multiple_of(core * half, 128), half)
    loads = [pltpu.make_async_copy(w.at[:, mine], wbuf.at[i], load_sem.at[i]) for i, w in enumerate((wq, wk, wv))]
    loads += [pltpu.make_async_copy(v, r, load_sem.at[3 + i]) for i, (v, r) in enumerate(zip(vectors, raw))]
    for load in loads:
        load.start()
    load = pltpu.make_async_copy(tokens.at[y], stage, local_sem.at[0])
    load.start()
    cot_load = pltpu.make_async_copy(cotangent.at[y], cot_stage, local_sem.at[4])
    cot_load.start()
    vpack[...] = jnp.zeros_like(vpack)
    for copy in loads:
        copy.wait()
    for i, vector in enumerate(raw):
        vpack[i : i + 1, 0 : vector.shape[1]] = vector[...].astype(jnp.bfloat16).astype(jnp.float32)
    for i in range(3):
        for p in range(pairs):
            pack[:, (3 * p + i) * 128 : (3 * p + i + 1) * 128] = wbuf[i, :, p * 128 : (p + 1) * 128].astype(jnp.bfloat16)
    greet(True)
    across = remote(tokens.at[1 - y], tokens_all.at[1], tsend.at[0], trecv.at[0], partner(y=1 - y))
    across.start()
    along = []
    for k in range(1, size_z):
        peer = partner(z=lax.rem(z + k, size_z))
        along.append(
            (
                remote(pack, weights_all.at[me], zsend.at[0, k - 1], zrecv.at[0, k - 1], peer),
                remote(vpack, vectors_all.at[me], zsend.at[1, k - 1], zrecv.at[1, k - 1], peer),
            )
        )
    beside = remote(tokens.at[y], tokens_all.at[2], tsend.at[1], trecv.at[1], partner(core=1 - core))
    sideways = []

    def forward(k, weights_src, vectors_src):
        slot = lax.rem(z - k + size_z, size_z) * size_x + x
        for j in range(1, size_x):
            peer = partner(x=lax.rem(x + j, size_x))
            first = remote(weights_src, weights_all.at[slot], xsend.at[0, k, j - 1], xrecv.at[0, k, j - 1], peer)
            second = remote(vectors_src, vectors_all.at[slot], xsend.at[1, k, j - 1], xrecv.at[1, k, j - 1], peer)
            first.start()
            second.start()
            sideways.append((first, second))

    forward(0, pack, vpack)
    for first, second in along:
        first.start()
        second.start()
    beside.start()
    keep_weights = pltpu.make_async_copy(pack, weights_all.at[me], local_sem.at[1])
    keep_vectors = pltpu.make_async_copy(vpack, vectors_all.at[me], local_sem.at[2])
    keep_weights.start()
    keep_vectors.start()
    load.wait()
    keep_tokens = pltpu.make_async_copy(stage, tokens_all.at[0], local_sem.at[3])
    keep_tokens.start()
    cot_load.wait()
    keep_cot = pltpu.make_async_copy(cot_stage, cotangent_all.at[0], local_sem.at[5])
    keep_cot.start()
    order = sorted(range(1, size_z), key=lambda k: min(k, size_z - k))
    for k in order:
        first, second = along[k - 1]
        first.wait_recv()
        second.wait_recv()
        slot = lax.rem(z - k + size_z, size_z) * size_x + x
        forward(k, weights_all.at[slot], vectors_all.at[slot])
    across.wait_recv()
    onward = remote(tokens_all.at[1], tokens_all.at[3], tsend.at[2], trecv.at[2], partner(core=1 - core))
    onward.start()
    later = remote(cotangent.at[1 - y], cotangent_all.at[1], tsend.at[3], trecv.at[3], partner(y=1 - y))
    later.start()
    for first, second in sideways:
        first.wait()
        second.wait()
    for first, second in along:
        first.wait_send()
        second.wait_send()
    across.wait_send()
    beside.wait()
    onward.wait()
    later.wait()
    keep_weights.wait()
    keep_vectors.wait()
    keep_tokens.wait()
    keep_cot.wait()


def entry(size_z, size_x, tokens, cotangent, wq, wk, wv, vectors):
    _, part, width = tokens.shape
    rows = wq.shape[0]
    lanes = wq.shape[1] // 2 * 3
    longest = max(v.shape[0] for v in vectors)
    shards = size_z * size_x
    anywhere = pl.BlockSpec(memory_space=pl.ANY)
    dma = pltpu.SemaphoreType.DMA
    return pl.pallas_call(
        lambda *refs: entry_kernel(size_z, size_x, len(vectors), *refs),
        out_shape=(
            jax.ShapeDtypeStruct((4, part, width), tokens.dtype),
            jax.ShapeDtypeStruct((2, part, width), cotangent.dtype),
            jax.ShapeDtypeStruct((shards, rows, lanes), jnp.bfloat16),
            jax.ShapeDtypeStruct((shards, 16, longest), jnp.float32),
        ),
        in_specs=[anywhere] * (5 + len(vectors)),
        out_specs=(anywhere,) * 4,
        scratch_shapes=[pltpu.VMEM((1, v.shape[0]), v.dtype) for v in vectors]
        + [
            pltpu.VMEM((part, width), tokens.dtype),
            pltpu.VMEM((part, width), cotangent.dtype),
            pltpu.VMEM((3, rows, lanes // 3), wq.dtype),
            pltpu.VMEM((rows, lanes), jnp.bfloat16),
            pltpu.VMEM((16, longest), jnp.float32),
            dma((6,)),
            dma((3 + len(vectors),)),
            dma((4,)),
            dma((4,)),
            dma((2, size_z - 1)),
            dma((2, size_z - 1)),
            dma((2, size_z, max(size_x - 1, 1))),
            dma((2, size_z, max(size_x - 1, 1))),
        ],
        compiler_params=pltpu.CompilerParams(collective_id=0, has_side_effects=True, vmem_limit_bytes=20 << 20),
        name="entry",
    )(tokens, cotangent, wq, wk, wv, *[v.reshape(1, -1) for v in vectors])


def exit_kernel(size_z, size_x, shapes, *refs):
    z, x, y, core = place_of()
    names = list(shapes)
    grads_hbm, inputs_hbm, weights_hbm, base_hbm, output_term, vector_terms = refs[:6]
    inner_in = refs[6 : 6 + size_z]
    outer_in = refs[6 + size_z : 6 + size_z + size_x]
    refs = refs[6 + size_z + size_x :]
    token_grads, grad_query, grad_key, grad_value, grad_output, grad_inner, grad_outer, vector_sums = refs[:8]
    grads, inputs, turned, weights, base, terms, other_rows, recv_rows, send_rows, far_rows, odd = refs[8:19]
    inner_buf, outer_buf = refs[19:21]
    load_sem, tsend, trecv, osend, orecv = refs[21:26]
    refs = refs[26:]
    xin, xsend, xrecv, xout = {}, {}, {}, {}
    zout, zin, zsend, zrecv = {}, {}, {}, {}
    ybuf, ysend, yrecv, cbuf, csend, crecv = {}, {}, {}, {}, {}, {}
    refs = list(refs)
    for name in names:
        ybuf[name], ysend[name], yrecv[name], cbuf[name], csend[name], crecv[name] = [refs.pop(0) for _ in range(6)]
        if name != "outer":
            xin[name], xsend[name], xrecv[name] = [refs.pop(0) for _ in range(3)]
        if name != "inner":
            zout[name], zin[name], zsend[name], zrecv[name] = [refs.pop(0) for _ in range(4)]
    xout["inner"] = refs.pop(0)

    shards, rows, lanes = terms.shape
    half = lanes // 3
    width = 2 * half
    pairs = half // 128
    hidden = grad_inner.shape[1]
    part = token_grads.shape[1]
    local = 2 * part
    low, high = jnp.bfloat16, jnp.float32
    mine = pl.ds(pl.multiple_of(core * half, 128), half)
    theirs = pl.ds(pl.multiple_of((1 - core) * half, 128), half)
    order = sorted(range(size_z), key=lambda k: -min(k, size_z - k))
    far_order = [k for k in order if k > 0]
    columns = [lax.rem(x + j, size_x) for j in range(size_x)]

    def slot_of(k, j):
        return lax.rem(z + k, size_z) * size_x + columns[j]

    loads = {}
    for i, src in enumerate(inner_in):
        loads["inner", i] = pltpu.make_async_copy(src, inner_buf.at[i], load_sem.at[i])
    for i, src in enumerate(outer_in):
        loads["outer", i] = pltpu.make_async_copy(src, outer_buf.at[i], load_sem.at[size_z + i])
    for i, (name, src, dst) in enumerate(
        (("inputs", inputs_hbm, inputs), ("grads", grads_hbm, grads), ("weights", weights_hbm, weights), ("base", base_hbm, base))
    ):
        loads[name] = pltpu.make_async_copy(src, dst, load_sem.at[size_z + size_x + i])
    for load in loads.values():
        load.start()
    greet(True)

    core_peer, y_peer = partner(core=1 - core), partner(y=1 - y)
    outputs = remote(output_term.at[:, :, theirs], odd, osend, orecv, core_peer)
    outputs.start()
    sideways = {}
    along = {}
    kept = {}

    def send_x(name, n, k, j, src, dst):
        move = remote(src, dst, xsend[name].at[n, k, j - 1], xrecv[name].at[n, k, j - 1], partner(x=columns[j]))
        move.start()
        sideways.setdefault((name, k, j), []).append(move)

    def send_z(name, k):
        move = remote(
            zout[name].at[k - 1],
            zin[name].at[k - 1],
            zsend[name].at[k - 1],
            zrecv[name].at[k - 1],
            partner(z=lax.rem(z + k, size_z)),
        )
        move.start()
        along[name, k] = move

    for k in order:
        for j in range(1, size_x):
            send_x("vec", 0, k, j, vector_terms.at[slot_of(k, j)], xin["vec"].at[j - 1, k])

    for i in range(size_z):
        loads["inner", i].wait()
    for j in range(size_x):
        total = inner_buf[0, columns[j]].astype(high)
        for i in range(1, size_z):
            total = total + inner_buf[i, columns[j]].astype(high)
        if j == 0:
            kept["inner"] = total
        else:
            xout["inner"][j - 1] = total.astype(low)
            send_x("inner", 0, 0, j, xout["inner"].at[j - 1], xin["inner"].at[j - 1, 0])

    for i in range(size_x):
        loads["outer", i].wait()
    for k in order:
        target = lax.rem(z + k, size_z)
        total = outer_buf[0, target].astype(high)
        for i in range(1, size_x):
            total = total + outer_buf[i, target].astype(high)
        if k == 0:
            kept["outer"] = total
        else:
            zout["outer"][k - 1] = total.astype(low)
            send_z("outer", k)

    loads["inputs"].wait()
    for b in range(4):
        turned[:, b * part : (b + 1) * part] = inputs[b * part : (b + 1) * part, :].T
    loads["grads"].wait()
    group = 4
    for p in range(pairs):
        block = slice(p * 384, (p + 1) * 384)

        def some(m, _):
            value = dot_nn(turned[pl.ds(pl.multiple_of(m * group * rows, group * rows), group * rows), :], grads[:, block])
            terms[pl.ds(m * group, group), :, block] = value.reshape(group, rows, 384).astype(low)
            return 0

        lax.fori_loop(0, shards // group, some, 0)
        for k in order:
            for j in range(1, size_x):
                send_x("qkv", p, k, j, terms.at[slot_of(k, j), :, block], xin["qkv"].at[j - 1, k, :, block])

    loads["weights"].wait()
    strip = 256

    def product(first):
        at = pl.ds(pl.multiple_of(first, strip), strip)
        return dot_nt(grads[at, :], weights[...])

    def other_strip(i, _):
        other_rows[pl.ds(pl.multiple_of(i * strip, strip), strip), :] = product(local + i * strip).astype(low)
        return 0

    lax.fori_loop(0, local // strip, other_strip, 0)
    halves = remote(other_rows, recv_rows, tsend.at[0], trecv.at[0], core_peer)
    halves.start()
    outputs.wait()
    for k in order:
        for j in range(1, size_x):
            slot = slot_of(k, j)
            odd[slot] = (odd[slot].astype(high) + output_term[slot, :, mine].astype(high)).astype(low)
            send_x("out", 0, k, j, odd.at[slot], xin["out"].at[j - 1, k])
    loads["base"].wait()

    def own_strip(i, _):
        at = pl.ds(pl.multiple_of(i * strip, strip), strip)
        base[at, :] = base[at, :] + product(i * strip)
        return 0

    lax.fori_loop(0, local // strip, own_strip, 0)
    halves.wait()
    send_rows[...] = (base[part:local, :] + recv_rows[part:local, :].astype(high)).astype(low)
    back = remote(send_rows, far_rows, tsend.at[1], trecv.at[1], y_peer)
    back.start()
    token_grads[y] = base[0:part, :] + recv_rows[0:part, :].astype(high)

    across = {}
    swapped = {}

    def step_y(name):
        move = remote(ybuf[name].at[0], ybuf[name].at[1], ysend[name], yrecv[name], y_peer)
        move.start()
        across[name] = move

    def step_core(name):
        across[name].wait()
        cbuf[name][0] = ybuf[name][0].astype(high) + ybuf[name][1].astype(high)
        move = remote(cbuf[name].at[0], cbuf[name].at[1], csend[name], crecv[name], core_peer)
        move.start()
        swapped[name] = move

    def finish_x(name):
        for k in order:
            slot = slot_of(k, 0)
            if name == "qkv":
                total = terms[slot].astype(high)
            elif name == "out":
                total = odd[slot].astype(high) + output_term[slot, :, mine].astype(high)
            else:
                total = vector_terms[slot]
            for j in range(1, size_x):
                for move in sideways[name, k, j]:
                    move.wait()
                total = total + xin[name][j - 1, k].astype(high)
            if k == 0:
                kept[name] = total
            else:
                zout[name][k - 1] = total.astype(zout[name].dtype)
                send_z(name, k)

    def finish_z(name):
        total = kept[name]
        for k in far_order:
            along[name, k].wait()
            total = total + zin[name][k - 1].astype(high)
        ybuf[name][0] = total.astype(ybuf[name].dtype)
        step_y(name)

    total = kept["inner"]
    for j in range(1, size_x):
        for move in sideways["inner", 0, j]:
            move.wait()
        total = total + xin["inner"][j - 1, 0].astype(high)
    ybuf["inner"][0] = total.astype(low)
    step_y("inner")
    finish_x("vec")
    finish_x("qkv")
    finish_z("outer")
    step_core("inner")
    finish_x("out")
    finish_z("vec")
    step_core("outer")
    finish_z("qkv")
    finish_z("out")
    back.wait()
    token_grads[1 - y] = far_rows[...].astype(high)
    step_core("vec")

    def finish_core(name):
        swapped[name].wait()
        return cbuf[name]

    buf = finish_core("inner")
    chunks = hidden // CHUNK
    for i in range(2):
        owner = core if i == 0 else 1 - core
        for c in range(chunks):
            place = pl.ds(pl.multiple_of(c * CHUNK + owner * half, 128), half)
            grad_inner[:, place] = buf[i, :, c * half : (c + 1) * half]
    buf = finish_core("outer")
    for i in range(2):
        owner = core if i == 0 else 1 - core
        grad_outer[:, pl.ds(pl.multiple_of(owner * half, 128), half)] = buf[i]
    step_core("qkv")
    step_core("out")
    buf = finish_core("vec")
    vector_sums[...] = buf[0] + buf[1]
    buf = finish_core("qkv")
    for i in range(2):
        owner = core if i == 0 else 1 - core
        for p in range(pairs):
            place = pl.ds(pl.multiple_of(owner * half + p * 128, 128), 128)
            for n, out in enumerate((grad_query, grad_key, grad_value)):
                out[:, place] = buf[i, :, (3 * p + n) * 128 : (3 * p + n + 1) * 128]
    buf = finish_core("out")
    for i in range(2):
        owner = core if i == 0 else 1 - core
        grad_output[:, pl.ds(pl.multiple_of(owner * half, 128), half)] = buf[i]


def exit_call(size_z, size_x, grads, inputs, weights, base, output_term, vector_terms, inner_terms, outer_terms):
    shards, rows, width = output_term.shape
    lanes = grads.shape[1]
    half = width // 2
    pairs = half // 128
    length = inputs.shape[0]
    local = length // 2
    part = local // 2
    long = outer_terms[0].shape[1]
    hidden = 2 * inner_terms[0].shape[2]
    vmem, anywhere = pl.BlockSpec(memory_space=pltpu.VMEM), pl.BlockSpec(memory_space=pl.ANY)
    dma = pltpu.SemaphoreType.DMA
    side = size_x - 1
    low, high = jnp.bfloat16, jnp.float32
    shapes = {
        "vec": (vector_terms.shape[1:], high, 1),
        "qkv": ((rows, lanes), low, pairs),
        "out": ((rows, half), low, 1),
        "inner": ((rows, hidden // 2), low, 1),
        "outer": ((long, half), low, 1),
    }
    scratch = [
        pltpu.VMEM((length, lanes), low),
        pltpu.VMEM((length, width), low),
        pltpu.VMEM((width, length), low),
        pltpu.VMEM((width, lanes), low),
        pltpu.VMEM((local, width), high),
        pltpu.VMEM((shards, rows, lanes), low),
        pltpu.VMEM((local, width), low),
        pltpu.VMEM((local, width), low),
        pltpu.VMEM((part, width), low),
        pltpu.VMEM((part, width), low),
        pltpu.VMEM((shards, rows, half), low),
        pltpu.VMEM((size_z,) + inner_terms[0].shape, low),
        pltpu.VMEM((size_x,) + outer_terms[0].shape, low),
        dma((size_z + size_x + 4,)),
        dma((2,)),
        dma((2,)),
        dma,
        dma,
    ]
    for name, (shape, kind, sends) in shapes.items():
        scratch += [pltpu.VMEM((2,) + shape, kind), dma, dma, pltpu.VMEM((2,) + shape, high), dma, dma]
        stages = 1 if name == "inner" else size_z
        if name != "outer":
            scratch += [pltpu.VMEM((side, stages) + shape, kind), dma((sends, stages, side)), dma((sends, stages, side))]
        if name != "inner":
            scratch += [pltpu.VMEM((size_z - 1,) + shape, kind)] * 2 + [dma((size_z - 1,))] * 2
    scratch.append(pltpu.VMEM((side, rows, hidden // 2), low))
    matrix = jax.ShapeDtypeStruct((rows, width), high)
    return pl.pallas_call(
        lambda *refs: exit_kernel(size_z, size_x, shapes, *refs),
        out_shape=(
            jax.ShapeDtypeStruct((2, part, width), high),
            matrix,
            matrix,
            matrix,
            matrix,
            jax.ShapeDtypeStruct((rows, hidden), high),
            jax.ShapeDtypeStruct((long, width), high),
            jax.ShapeDtypeStruct(vector_terms.shape[1:], high),
        ),
        in_specs=[anywhere] * 4 + [vmem] * 2 + [anywhere] * (size_z + size_x),
        out_specs=(vmem,) * 8,
        scratch_shapes=scratch,
        compiler_params=pltpu.CompilerParams(collective_id=1, has_side_effects=True, vmem_limit_bytes=67_000_000),
        name="exit",
    )(grads, inputs, weights, base, output_term, vector_terms, *inner_terms, *outer_terms)


TILE = 256
CHUNK = 768


def dot_nt(a, b):
    return lax.dot_general(a, b, (((1,), (1,)), ((), ())), preferred_element_type=jnp.float32)


def row_mean(value):
    return jnp.sum(value, axis=-1, keepdims=True) * (1.0 / value.shape[-1])


def standardize(hidden):
    centred = hidden - row_mean(hidden)
    reciprocal = lax.rsqrt(row_mean(centred * centred) + EPS)
    return centred * reciprocal, reciprocal


def column_sum(value):
    return jnp.sum(value.reshape(value.shape[0] // 8, 8, value.shape[1]), axis=0)


def dense_kernel(
    size_z,
    size_x,
    tokens_ref,
    mine_ref,
    other_ref,
    cot_ref,
    vectors_ref,
    bias_inner_ref,
    weights_hbm,
    *refs,
):
    mixed_ref, pre_first_ref, grad_mine_ref, grad_other_ref, sums_ref, inner_sum_ref, grad_output_ref = refs[:7]
    inner_terms = refs[7 : 7 + size_z]
    outer_terms = refs[7 + size_z : 7 + size_z + size_x]
    refs = refs[7 + size_z + size_x :]
    w_output, w_inner, w_outer, a_output, a_inner, a_outer, grad_out_buf = refs[:7]
    context, first_low, turned_low, normed, first, slope, active, work = refs[7:15]
    send_inner, send_outer, recv_inner, recv_outer, load_sem, outer_sem, send_sem, recv_sem, store_sem = refs[15:]
    step, steps = pl.program_id(0), pl.num_programs(0)
    core_here = lax.axis_index("core")
    width, hidden = w_inner.shape
    half = width // 2
    chunks = hidden // CHUNK
    shards = size_z * size_x
    pieces = 2 * shards
    rows = width // pieces
    ratio = hidden // width
    z, x, y, _ = place_of()
    twin = partner(core=1 - lax.axis_index("core"))

    def load_outer(start):
        if not start:
            pltpu.make_async_copy(w_outer, w_outer, outer_sem).wait()
            return

        def piece(s, _):
            for q in range(ratio):
                src = weights_hbm.at[
                    pl.ds(pl.multiple_of(s * rows, rows), rows), pl.ds(hidden + width + q * width, width)
                ]
                dst = w_outer.at[pl.ds(pl.multiple_of((s * ratio + q) * rows, rows), rows), :]
                pltpu.make_async_copy(src, dst, outer_sem).start()
            return 0

        lax.fori_loop(0, pieces, piece, 0)

    loads = (
        pltpu.make_async_copy(weights_hbm.at[:, pl.ds(hidden, width)], w_output, load_sem.at[0]),
        pltpu.make_async_copy(weights_hbm.at[:, pl.ds(0, hidden)], w_inner, load_sem.at[1]),
    )

    @pl.when(step == 0)
    def _():
        barrier = pltpu.get_barrier_semaphore()
        pl.semaphore_signal(barrier, inc=1, device_id=twin, device_id_type=MESH_ID)
        pl.semaphore_wait(barrier, 1)
        for load in loads:
            load.start()
        load_outer(True)
        a_output[...] = jnp.zeros_like(a_output)
        a_inner[...] = jnp.zeros_like(a_inner)
        a_outer[...] = jnp.zeros_like(a_outer)
        sums_ref[...] = jnp.zeros_like(sums_ref)
        inner_sum_ref[...] = jnp.zeros_like(inner_sum_ref)

    def vector(i):
        return vectors_ref[i : i + 1, :]

    def add_sum(i, value):
        sums_ref[8 * i : 8 * i + 8, :] += column_sum(value)

    context[:, pl.ds(pl.multiple_of(core_here * half, 128), half)] = mine_ref[...]
    context[:, pl.ds(pl.multiple_of((1 - core_here) * half, 128), half)] = other_ref[...]

    @pl.when(step == 0)
    def _():
        loads[0].wait()

    hidden_rows = tokens_ref[...].astype(jnp.float32) + (dot_nn(context[...], w_output[...]) + vector(0))
    normed[...], first_recip = standardize(hidden_rows)
    first[...] = normed[...] * vector(1) + vector(2)
    first_low[...] = first[...].astype(jnp.bfloat16)
    turned_low[...] = first_low[...].T
    work[...] = jnp.broadcast_to(vector(3), work.shape)

    @pl.when(step == 0)
    def _():
        loads[1].wait()
        load_outer(False)

    def part(c):
        return pl.ds(pl.multiple_of(c * CHUNK, CHUNK), CHUNK)

    def exchange(c):
        return (
            remote(send_inner.at[c], recv_inner.at[c], send_sem.at[0, c], recv_sem.at[0, c], twin),
            remote(send_outer.at[c], recv_outer.at[c], send_sem.at[1, c], recv_sem.at[1, c], twin),
        )

    def forward(c, _):
        u = dot_nn(first_low[...], w_inner[:, part(c)]) + bias_inner_ref[0:1, part(c)]
        cdf = 0.5 * (1.0 + lax.erf(u * ROOT_HALF))
        slope[:, part(c)] = cdf + u * jnp.exp(-0.5 * u * u) * INV_ROOT_TAU
        active[:, part(c)] = (u * cdf).astype(jnp.bfloat16)
        work[...] += dot_nn(active[:, part(c)], w_outer[part(c), :])
        return 0

    lax.fori_loop(0, chunks, forward, 0)
    second, second_recip = standardize(first[...] + work[...])
    mixed_ref[...] = (second * vector(4) + vector(5)).astype(jnp.bfloat16)
    upstream = cot_ref[...].astype(jnp.float32)
    add_sum(0, upstream * second)
    add_sum(1, upstream)
    scaled = upstream * vector(4)
    pre_second = second_recip * (scaled - row_mean(scaled) - second * row_mean(scaled * second))
    grad_outer = pre_second.astype(jnp.bfloat16)
    add_sum(2, grad_outer.astype(jnp.float32))
    work[...] = pre_second
    grad_out_buf[...] = grad_outer

    def backward(c, _):
        grad_out = grad_out_buf[...]
        grad = dot_nt(grad_out, w_outer[part(c), :])
        grad_inner = (grad * slope[:, part(c)]).astype(jnp.bfloat16)
        inner_sum_ref[:, part(c)] += column_sum(grad_inner.astype(jnp.float32))
        a_outer[part(c), :] += dot_nn(active[:, part(c)].T, grad_out)
        a_inner[:, part(c)] += dot_nn(turned_low[...], grad_inner)
        work[...] += dot_nt(grad_inner, w_inner[:, part(c)])

        @pl.when(step == steps - 1)
        def _():
            theirs = pl.multiple_of(c * CHUNK + (1 - core_here) * half, 128)
            send_inner[c] = a_inner[:, pl.ds(theirs, half)].astype(jnp.bfloat16)
            send_outer[c] = a_outer[part(c), pl.ds(pl.multiple_of((1 - core_here) * half, 128), half)].astype(jnp.bfloat16)
            for move in exchange(c):
                move.start()

        return 0

    lax.fori_loop(0, chunks, backward, 0)
    grad_first = work[...]
    add_sum(3, grad_first * normed[...])
    add_sum(4, grad_first)
    scaled = grad_first * vector(1)
    pre_first = first_recip * (scaled - row_mean(scaled) - normed[...] * row_mean(scaled * normed[...]))
    pre_first_ref[...] = pre_first
    grad_attended = pre_first.astype(jnp.bfloat16)
    add_sum(5, grad_attended.astype(jnp.float32))
    a_output[...] += dot_nn(context[...].T, grad_attended)
    context[...] = dot_nt(grad_attended, w_output[...]).astype(jnp.bfloat16)
    grad_mine_ref[...] = context[:, pl.ds(pl.multiple_of(core_here * half, 128), half)]
    grad_other_ref[...] = context[:, pl.ds(pl.multiple_of((1 - core_here) * half, 128), half)]

    @pl.when(step == steps - 1)
    def _():
        grad_output_ref[...] = a_output[...].astype(jnp.bfloat16)

        shard = width // shards
        long = hidden // shards

        def inner_out(c):
            copies = []
            for k in range(size_z):
                for column in range(size_x):
                    slot = lax.rem(z + k, size_z) * size_x + column
                    src = send_inner.at[c, pl.ds(pl.multiple_of(slot * shard, shard), shard), :]
                    copies.append(
                        pltpu.make_async_copy(src, inner_terms[k].at[column, :, pl.ds(c * half, half)], store_sem.at[0, c])
                    )
            return copies

        def outer_out(c):
            copies = []
            group = CHUNK // long // size_x
            for i in range(group):
                for j in range(size_x):
                    src = send_outer.at[c, pl.ds(pl.multiple_of((i * size_x + lax.rem(x + j, size_x)) * long, long), long), :]
                    copies.append(pltpu.make_async_copy(src, outer_terms[j].at[c * group + i], store_sem.at[1, c]))
            return copies

        for c in range(chunks):
            ours = pl.multiple_of(c * CHUNK + core_here * half, 128)
            first_move, second_move = exchange(c)
            first_move.wait()
            send_inner[c] = (a_inner[:, pl.ds(ours, half)] + recv_inner[c].astype(jnp.float32)).astype(jnp.bfloat16)
            for copy in inner_out(c):
                copy.start()
            second_move.wait()
            columns = pl.ds(pl.multiple_of(core_here * half, 128), half)
            send_outer[c] = (a_outer[part(c), columns] + recv_outer[c].astype(jnp.float32)).astype(jnp.bfloat16)
            for copy in outer_out(c):
                copy.start()
        for c in range(chunks):
            pltpu.make_async_copy(send_inner.at[c], send_inner.at[c], store_sem.at[0, c]).wait()
            pltpu.make_async_copy(send_outer.at[c], send_outer.at[c], store_sem.at[1, c]).wait()


def dense_layer(size_z, size_x, tokens, mine, other, cotangent, vectors, bias_inner, weights):
    local, half = mine.shape
    width = 2 * half
    hidden = bias_inner.shape[1]
    steps = local // TILE
    shards = size_z * size_x
    chunks = hidden // CHUNK
    low, high = jnp.bfloat16, jnp.float32
    tile = pl.BlockSpec((TILE, width), lambda t, *_: (t, 0))
    half_tile = pl.BlockSpec((TILE, half), lambda t, *_: (t, 0))
    anywhere = pl.BlockSpec(memory_space=pl.ANY)

    def whole(shape):
        return pl.BlockSpec(shape, lambda t, *_: (0, 0))

    inner_shape = jax.ShapeDtypeStruct((size_x, width // shards, hidden // 2), low)
    outer_shape = jax.ShapeDtypeStruct((size_z, hidden // shards, half), low)
    halves = pltpu.VMEM((chunks, width, half), low)
    dma = pltpu.SemaphoreType.DMA
    return pl.pallas_call(
        lambda *refs: dense_kernel(size_z, size_x, *refs),
        out_shape=(
            jax.ShapeDtypeStruct((local, width), low),
            jax.ShapeDtypeStruct((local, width), high),
            jax.ShapeDtypeStruct((local, half), low),
            jax.ShapeDtypeStruct((local, half), low),
            jax.ShapeDtypeStruct((48, width), high),
            jax.ShapeDtypeStruct((8, hidden), high),
            jax.ShapeDtypeStruct((width, width), low),
        )
        + (inner_shape,) * size_z
        + (outer_shape,) * size_x,
        grid_spec=pltpu.PrefetchScalarGridSpec(
            num_scalar_prefetch=0,
            grid=(steps,),
            in_specs=[
                tile,
                half_tile,
                half_tile,
                tile,
                whole((8, width)),
                whole((1, hidden)),
                anywhere,
            ],
            out_specs=[
                tile,
                tile,
                half_tile,
                half_tile,
                whole((48, width)),
                whole((8, hidden)),
                whole((width, width)),
            ]
            + [anywhere] * (size_z + size_x),
            scratch_shapes=[
                pltpu.VMEM((width, width), low),
                pltpu.VMEM((width, hidden), low),
                pltpu.VMEM((hidden, width), low),
                pltpu.VMEM((width, width), high),
                pltpu.VMEM((width, hidden), high),
                pltpu.VMEM((hidden, width), high),
                pltpu.VMEM((TILE, width), low),
                pltpu.VMEM((TILE, width), low),
                pltpu.VMEM((TILE, width), low),
                pltpu.VMEM((width, TILE), low),
                pltpu.VMEM((TILE, width), high),
                pltpu.VMEM((TILE, width), high),
                pltpu.VMEM((TILE, hidden), high),
                pltpu.VMEM((TILE, hidden), low),
                pltpu.VMEM((TILE, width), high),
                halves,
                halves,
                halves,
                halves,
                dma((2,)),
                dma,
                dma((2, chunks)),
                dma((2, chunks)),
                dma((2, chunks)),
            ],
        ),
        compiler_params=pltpu.CompilerParams(
            dimension_semantics=("arbitrary",), vmem_limit_bytes=67_000_000, collective_id=3, has_side_effects=True
        ),
        cost_estimate=pl.CostEstimate(flops=32_000_000_000, bytes_accessed=40_000_000, transcendentals=6_000_000),
        name="dense_layer",
    )(tokens, mine, other, cotangent, vectors, bias_inner, weights)


def lowered(piece):
    return piece.astype(jnp.bfloat16)


def widen(piece):
    return piece.astype(jnp.float32)


def matmul(left, right):
    return jnp.dot(left, right, preferred_element_type=jnp.float32)


def matmul_tn(left, right):
    return lax.dot_general(
        left, right, (((0,), (0,)), ((), ())), preferred_element_type=jnp.float32
    )


def matmul_nt(left, right):
    return lax.dot_general(
        left, right, (((1,), (1,)), ((), ())), preferred_element_type=jnp.float32
    )


def normalize(hidden, norm_gain, norm_shift):
    centred = hidden - jnp.mean(hidden, axis=-1, keepdims=True)
    reciprocal = lax.rsqrt(jnp.mean(centred * centred, axis=-1, keepdims=True) + EPS)
    normed = centred * reciprocal
    return (normed * norm_gain + norm_shift, normed, reciprocal)


def normalize_back(upstream, normed, reciprocal, norm_gain):
    scaled = upstream * norm_gain
    result = reciprocal * (
        scaled
        - jnp.mean(scaled, axis=-1, keepdims=True)
        - normed * jnp.mean(scaled * normed, axis=-1, keepdims=True)
    )
    return (result, jnp.sum(upstream * normed, axis=0), jnp.sum(upstream, axis=0))


def gelu_value(values_in):
    return 0.5 * values_in * (1.0 + lax.erf(values_in * ROOT_HALF))


def gelu_slope(values_in):
    return (
        0.5 * (1.0 + lax.erf(values_in * ROOT_HALF))
        + values_in * jnp.exp(-0.5 * values_in * values_in) * INV_ROOT_TAU
    )


def shift(piece, axis, step):
    size = lax.axis_size(axis)
    return lax.ppermute(piece, axis, [(i, (i + step) % size) for i in range(size)])


def swap(piece, axis):
    return lax.ppermute(piece, axis, [(0, 1), (1, 0)])


def pick(piece, index, axis=0):
    return lax.dynamic_index_in_dim(piece, index, axis, keepdims=False)


def in_order(first_is_zero, own, other, axis):
    return jnp.where(
        first_is_zero,
        jnp.concatenate([own, other], axis),
        jnp.concatenate([other, own], axis),
    )


def collect(piece):
    size_z, size_x = lax.axis_size("z"), lax.axis_size("x")
    z, x = lax.axis_index("z"), lax.axis_index("x")
    along_z = [piece] + [shift(piece, "z", k) for k in range(1, size_z)]
    whole = jnp.zeros((size_z, size_x) + piece.shape, piece.dtype)
    zeros = (0,) * piece.ndim
    for j in range(size_x):
        for k in range(size_z):
            arrived = along_z[k] if j == 0 else shift(along_z[k], "x", j)
            place = ((z - k) % size_z, (x - j) % size_x) + zeros
            whole = lax.dynamic_update_slice(whole, arrived[None, None], place)
    return whole.reshape((size_z * size_x,) + piece.shape)


def reduce_owned(terms):
    size_z, size_x = lax.axis_size("z"), lax.axis_size("x")
    z, x = lax.axis_index("z"), lax.axis_index("x")
    terms = terms.reshape((size_z, size_x) + terms.shape[1:])
    total = widen(pick(terms, x, 1))
    for j in range(1, size_x):
        total = total + widen(shift(pick(terms, (x + j) % size_x, 1), "x", j))
    terms = lowered(total)
    total = widen(pick(terms, z))
    for k in range(1, size_z):
        total = total + widen(shift(pick(terms, (z + k) % size_z), "z", k))
    terms = lowered(total)
    return widen(terms) + widen(swap(terms, "y"))


def plain_body(
    tokens,
    segment_ids,
    w_query,
    w_key,
    w_value,
    w_output,
    b_query,
    b_value,
    b_output,
    first_gain,
    first_shift,
    w_inner,
    b_inner,
    w_outer,
    b_outer,
    second_gain,
    second_shift,
    cotangent,
):
    core, y = lax.axis_index("core"), lax.axis_index("y")
    shards = lax.axis_size("z") * lax.axis_size("x")
    sequences, part, width = tokens.shape
    half = width // 2
    pairs = half // 128
    hidden = w_inner.shape[1]
    local = 2 * part
    own_rows = w_query.shape[0]
    unit_half = hidden // shards // 2

    def columns(matrix):
        return lowered(lax.dynamic_slice_in_dim(matrix, core * half, half, 1))

    vectors = (b_query, b_value, b_output, first_gain, first_shift, b_inner, b_outer, second_gain, second_shift)
    flat = jnp.concatenate([lowered(v) for v in vectors])
    lanes = 3 * half
    extra = -(-flat.shape[0] // lanes)
    flat = jnp.pad(flat, (0, extra * lanes - flat.shape[0])).reshape(extra, lanes)
    weights = jnp.stack([columns(w).reshape(own_rows, pairs, 128) for w in (w_query, w_key, w_value)], axis=2)
    early = collect(jnp.concatenate([weights.reshape(own_rows, lanes), flat], axis=0))

    mine = pick(tokens, y)
    arrived = swap(pick(tokens, 1 - y), "y")
    mine_other, arrived_other = swap(mine, "core"), swap(arrived, "core")
    inputs_all = jnp.concatenate([mine, arrived, mine_other, arrived_other], axis=0)
    inputs = jnp.concatenate([mine, arrived], axis=0)

    inner_piece = lowered(pick(w_inner.reshape(own_rows, shards, 2, unit_half), core, 2)).reshape(own_rows, hidden // 2)
    late = collect(jnp.concatenate([columns(w_output), inner_piece], axis=1)).reshape(width, half + hidden // 2)
    outer_own = collect(lowered(lax.dynamic_slice_in_dim(w_outer, core * unit_half, unit_half, 0))).reshape(hidden // 2, width)
    output_own, inner_own = late[:, :half], late[:, half:]
    output_other, inner_other, outer_other = swap(output_own, "core"), swap(inner_own, "core"), swap(outer_own, "core")
    full_output = in_order(core == 0, output_own, output_other, 1)
    cotangent_mine = pick(cotangent, y)
    cotangent_arrived = swap(pick(cotangent, 1 - y), "y")

    full_early = early[:, :own_rows].reshape(width, lanes)
    flat_all = early[:, own_rows:].reshape(shards, extra * lanes)
    sizes = [v.shape[0] for v in vectors]
    gathered, at = [], 0
    for size in sizes:
        gathered.append(flat_all[:, at : at + size].reshape(shards * size))
        at += size
    bias_query, bias_value, bias_output, gain_first, shift_first, bias_inner, bias_outer, gain_second, shift_second = [
        widen(v) for v in gathered
    ]
    heads_query = lax.dynamic_slice_in_dim(bias_query, core * half, half).reshape(pairs, 1, 128)
    heads_value = lax.dynamic_slice_in_dim(bias_value, core * half, half).reshape(pairs, 1, 128)
    bias_all = jnp.concatenate([heads_query, jnp.zeros_like(heads_query), heads_value], axis=1).reshape(lanes)
    scale = jnp.tile(jnp.concatenate([jnp.full((128,), HD ** (-0.5)), jnp.ones((256,))]), pairs)
    projected = lowered((matmul(inputs_all, full_early) + bias_all) * scale)

    spot = jnp.arange(5, dtype=jnp.int32)
    place = jnp.where(spot < 4, ((spot % 2 != core) * 2 + (spot // 2 != y) * 1) * part, core)
    segments = pick(segment_ids, y)
    heads_mine, heads_other, logsum = attention(place, segments, projected)
    context = in_order(core == 0, heads_mine, swap(heads_other, "core"), 1)

    attended = matmul(context, full_output) + bias_output
    first, first_normed, first_recip = normalize(widen(inputs) + attended, gain_first, shift_first)
    first_low = lowered(first)
    biases = bias_inner.reshape(shards, 2, unit_half)
    halves = ((inner_own, outer_own, pick(biases, core, 1)), (inner_other, outer_other, pick(biases, 1 - core, 1)))
    outer, kept = bias_outer, []
    for inner_weight, outer_weight, bias in halves:
        inner = matmul(first_low, inner_weight) + bias.reshape(hidden // 2)
        active = lowered(gelu_value(inner))
        outer = outer + matmul(active, outer_weight)
        kept.append((inner, active))
    mixed, second_normed, second_recip = normalize(first + outer, gain_second, shift_second)
    mixed = lowered(mixed)

    upstream = widen(jnp.concatenate([cotangent_mine, cotangent_arrived], axis=0))
    pre_second, grad_second_gain, grad_second_shift = normalize_back(upstream, second_normed, second_recip, gain_second)
    grad_outer = lowered(pre_second)
    grad_b_outer = jnp.sum(widen(grad_outer), axis=0)
    grad_first, inner_grads, outer_grads, bias_grads = pre_second, [], [], []
    for (inner, active), (inner_weight, outer_weight, _) in zip(kept, halves):
        grad_inner = lowered(matmul_nt(grad_outer, outer_weight) * gelu_slope(inner))
        outer_grads.append(lowered(matmul_tn(active, grad_outer)))
        inner_grads.append(lowered(matmul_tn(first_low, grad_inner)))
        bias_grads.append(jnp.sum(widen(grad_inner), axis=0).reshape(shards, 1, unit_half))
        grad_first = grad_first + matmul_nt(grad_inner, inner_weight)
    grad_b_inner = in_order(core == 0, bias_grads[0], bias_grads[1], 1).reshape(hidden)
    pre_first, grad_first_gain, grad_first_shift = normalize_back(grad_first, first_normed, first_recip, gain_first)
    grad_attended = lowered(pre_first)
    grad_b_output = jnp.sum(widen(grad_attended), axis=0)
    grad_w_output = lowered(matmul_tn(context, grad_attended))
    grad_context = lowered(matmul_nt(grad_attended, full_output))
    context_mine = lax.dynamic_slice_in_dim(grad_context, core * half, half, 1)
    context_other = lax.dynamic_slice_in_dim(grad_context, (1 - core) * half, half, 1)
    upstream_other = swap(context_other, "core")

    def core_sum(own, other):
        return lowered(widen(own) + widen(swap(other, "core")))

    outer_term = core_sum(*outer_grads)
    inner_term = core_sum(*inner_grads)
    output_term = core_sum(
        lax.dynamic_slice_in_dim(grad_w_output, core * half, half, 1),
        lax.dynamic_slice_in_dim(grad_w_output, (1 - core) * half, half, 1),
    )
    outer_done = reduce_owned(outer_term.reshape(shards, unit_half, width))
    late_done = reduce_owned(jnp.concatenate([output_term, inner_term], axis=1).reshape(shards, own_rows, half + hidden // 2))

    grads, sums = attention_back(place, segments, projected, heads_mine, heads_other, context_mine, upstream_other, logsum)
    grad_early = lowered(matmul_tn(inputs_all, grads))
    partial = matmul_nt(grads, full_early)
    sums = sums.reshape(pairs, 8, 3, 128)[:, 0]
    blank = jnp.zeros((width,), jnp.float32)
    grad_b_query = lax.dynamic_update_slice(blank, sums[:, 0].reshape(half), (core * half,))
    grad_b_value = lax.dynamic_update_slice(blank, sums[:, 2].reshape(half), (core * half,))
    vector_grads = (
        grad_b_query,
        grad_b_value,
        grad_b_output,
        grad_first_gain,
        grad_first_shift,
        grad_b_inner,
        grad_b_outer,
        grad_second_gain,
        grad_second_shift,
    )
    flat_grads = jnp.concatenate([v.reshape(shards, -1) for v in vector_grads], axis=1)
    flat_grads = jnp.pad(flat_grads, ((0, 0), (0, extra * lanes - flat_grads.shape[1])))
    early_term = jnp.concatenate(
        [grad_early.reshape(shards, own_rows, lanes), lowered(flat_grads).reshape(shards, extra, lanes)], axis=1
    )
    early_done = reduce_owned(early_term)

    grad_inputs = pre_first + partial[:local] + widen(swap(lowered(partial[local:]), "core"))
    returned = widen(swap(lowered(grad_inputs[part:]), "y"))
    grad_tokens = in_order(y == 0, grad_inputs[None, :part], returned[None], 0)
    mixed_out = in_order(y == 0, mixed[None, :part], swap(mixed[part:], "y")[None], 0)

    def both(piece):
        return widen(swap(lowered(piece), "core"))

    early_matrix = early_done[:own_rows]
    early_full = in_order(
        core == 0, early_matrix.reshape(own_rows, pairs, 3, 128)[None], both(early_matrix).reshape(own_rows, pairs, 3, 128)[None], 0
    )
    early_full = early_full.transpose(3, 1, 0, 2, 4).reshape(3, own_rows, width)
    late_other = both(late_done)
    output_full = in_order(core == 0, late_done[:, :half], late_other[:, :half], 1)
    inner_full = in_order(
        core == 0,
        late_done[:, half:].reshape(own_rows, shards, 1, unit_half),
        late_other[:, half:].reshape(own_rows, shards, 1, unit_half),
        2,
    ).reshape(own_rows, hidden)
    outer_full = in_order(core == 0, outer_done, both(outer_done), 0)
    vector_part = early_done[own_rows:]
    vector_sums = (vector_part + swap(vector_part, "core")).reshape(extra * lanes)
    out_vectors, at = [], 0
    for size in sizes:
        out_vectors.append(vector_sums[at : at + size])
        at += size
    (
        done_b_query,
        done_b_value,
        done_b_output,
        done_first_gain,
        done_first_shift,
        done_b_inner,
        done_b_outer,
        done_second_gain,
        done_second_shift,
    ) = out_vectors
    return (
        mixed_out,
        grad_tokens,
        early_full[0],
        early_full[1],
        early_full[2],
        output_full,
        done_b_query,
        done_b_value,
        done_b_output,
        done_first_gain,
        done_first_shift,
        inner_full,
        done_b_inner,
        outer_full,
        done_b_outer,
        done_second_gain,
        done_second_shift,
    )


def body(
    tokens,
    segment_ids,
    w_query,
    w_key,
    w_value,
    w_output,
    b_query,
    b_value,
    b_output,
    first_gain,
    first_shift,
    w_inner,
    b_inner,
    w_outer,
    b_outer,
    second_gain,
    second_shift,
    cotangent,
):
    core, y = lax.axis_index("core"), lax.axis_index("y")
    size_z, size_x = lax.axis_size("z"), lax.axis_size("x")
    shards = size_z * size_x
    everyone = ("z", "x", "core")
    sequences, part, width = tokens.shape
    half = width // 2
    pairs = half // 128
    hidden = w_inner.shape[1]
    local = 2 * part
    own_rows = w_query.shape[0]
    lanes = 3 * half

    stack = hidden // width

    def core_rows(matrix):
        rows = matrix.shape[0] // 2
        return lowered(lax.dynamic_slice_in_dim(matrix, core * rows, rows, 0))

    outer_rows = core_rows(w_outer)
    outer_rows = outer_rows.reshape(stack, own_rows // 2, width).transpose(1, 0, 2).reshape(own_rows // 2, hidden)
    pieces = (core_rows(w_inner), core_rows(w_output), outer_rows)
    dense = lax.all_gather(jnp.concatenate(pieces, axis=1), everyone, axis=0, tiled=True)

    vectors = (b_query, b_value, b_output, first_gain, first_shift, b_inner, b_outer, second_gain, second_shift)
    sizes = [v.shape[0] for v in vectors]
    tokens_all, cotangent_all, early, vectors_all = entry(size_z, size_x, tokens, cotangent, w_query, w_key, w_value, vectors)
    inputs_all = tokens_all.reshape(4 * part, width)
    full_early = early.reshape(width, lanes)
    bias_query, bias_value, bias_output, gain_first, shift_first, bias_inner, bias_outer, gain_second, shift_second = [
        vectors_all[:, i, :size].reshape(shards * size) for i, size in enumerate(sizes)
    ]
    heads_query = lax.dynamic_slice_in_dim(bias_query, core * half, half).reshape(pairs, 1, 128)
    heads_value = lax.dynamic_slice_in_dim(bias_value, core * half, half).reshape(pairs, 1, 128)
    bias_all = jnp.concatenate([heads_query, jnp.zeros_like(heads_query), heads_value], axis=1).reshape(lanes)
    scale = jnp.tile(jnp.concatenate([jnp.full((128,), HD ** (-0.5)), jnp.ones((256,))]), pairs)
    projected = lowered((matmul(inputs_all, full_early) + bias_all) * scale)

    spot = jnp.arange(5, dtype=jnp.int32)
    place = jnp.where(spot < 4, ((spot % 2 != core) * 2 + (spot // 2 != y) * 1) * part, core)
    segments = pick(segment_ids, y)
    context_mine, context_other, logsum = attention(place, segments, projected)
    norms = jnp.stack([bias_output, gain_first, shift_first, bias_outer, gain_second, shift_second])
    norms = jnp.concatenate([norms, jnp.zeros((2, width), jnp.float32)], axis=0)
    made = dense_layer(
        size_z,
        size_x,
        inputs_all,
        context_mine,
        swap(context_other, "core"),
        cotangent_all.reshape(local, width),
        norms,
        bias_inner.reshape(1, hidden),
        dense,
    )
    mixed, pre_first, upstream_mine, upstream_send, dense_sums, inner_sums, grad_w_output = made[:7]
    inner_terms = [made[7]] + [shift(made[7 + k], "z", k) for k in range(1, size_z)]
    outer_terms = [made[7 + size_z]] + [shift(made[7 + size_z + j], "x", j) for j in range(1, size_x)]
    upstream_other = swap(upstream_send, "core")
    dense_sums = jnp.sum(dense_sums.reshape(6, 8, width), axis=1)
    grad_second_gain, grad_second_shift, grad_b_outer, grad_first_gain, grad_first_shift, grad_b_output = [
        dense_sums[i] for i in range(6)
    ]
    grad_b_inner = jnp.sum(inner_sums, axis=0)
    mixed_out = in_order(y == 0, mixed[None, :part], swap(mixed[part:], "y")[None], 0)

    grads, sums = attention_back(place, segments, projected, context_mine, context_other, upstream_mine, upstream_other, logsum)
    sums = sums.reshape(pairs, 8, 3, 128)[:, 0]
    blank = jnp.zeros((width,), jnp.float32)
    grad_b_query = lax.dynamic_update_slice(blank, sums[:, 0].reshape(half), (core * half,))
    grad_b_value = lax.dynamic_update_slice(blank, sums[:, 2].reshape(half), (core * half,))
    vector_grads = (
        grad_b_query,
        grad_b_value,
        grad_b_output,
        grad_first_gain,
        grad_first_shift,
        grad_b_inner,
        grad_b_outer,
        grad_second_gain,
        grad_second_shift,
    )
    longest = vectors_all.shape[2]
    rows = [jnp.pad(v.reshape(shards, 1, -1), ((0, 0), (0, 0), (0, longest - v.shape[0] // shards))) for v in vector_grads]
    rows.append(jnp.zeros((shards, vectors_all.shape[1] - len(rows), longest), jnp.float32))
    vector_terms = jnp.concatenate(rows, axis=1)
    grad_tokens, grad_query, grad_key, grad_value, grad_output, grad_inner_full, grad_outer_full, vector_sums = exit_call(
        size_z,
        size_x,
        grads,
        inputs_all,
        full_early,
        pre_first,
        grad_w_output.reshape(shards, own_rows, width),
        vector_terms,
        inner_terms,
        outer_terms,
    )
    done = [vector_sums[i, :size] for i, size in enumerate(sizes)]
    return (
        mixed_out,
        grad_tokens,
        grad_query,
        grad_key,
        grad_value,
        grad_output,
        done[0],
        done[1],
        done[2],
        done[3],
        done[4],
        grad_inner_full,
        done[5],
        grad_outer_full,
        done[6],
        done[7],
        done[8],
    )


def layer(*arrays):
    if arrays[2].shape[0] % 32 == 0 and lax.axis_size("x") > 1:
        return body(*arrays)
    return plain_body(*arrays)


def solution(mesh):
    outer, inner = mesh.devices.shape
    size_z = 1
    while size_z * size_z < outer:
        size_z *= 2
    split = Mesh(mesh.devices.reshape(size_z, outer // size_z, inner // 2, 2), ("z", "x", "y", "core"))
    dp, seq = ("z", "x"), ("y", "core")
    activation, matrix, vector = P(dp, seq, None), P(dp, None), P(dp)
    return jax.shard_map(
        layer,
        mesh=split,
        in_specs=(
            activation,
            matrix,
            matrix,
            matrix,
            matrix,
            matrix,
            vector,
            vector,
            vector,
            vector,
            vector,
            matrix,
            vector,
            matrix,
            vector,
            vector,
            vector,
            activation,
        ),
        out_specs=(
            activation,
            activation,
            matrix,
            matrix,
            matrix,
            matrix,
            vector,
            vector,
            vector,
            vector,
            vector,
            matrix,
            vector,
            matrix,
            vector,
            vector,
            vector,
        ),
        check_vma=False,
    )
```

```python
import jax
import jax.numpy as jnp
from jax import lax
from jax.experimental import pallas as pl
from jax.experimental.pallas import tpu as pltpu
from jax.sharding import Mesh
from jax.sharding import PartitionSpec as P


HD = 64
EPS = 1e-12
ROOT_HALF = 0.7071067811865476
INV_ROOT_TAU = 0.3989422804014327

BLK = 256
BIG = -1.0e9
DOCUMENTS = 4


def dot_nn(a, b):
    return jnp.dot(a, b, preferred_element_type=jnp.float32)


def part_rows(place_ref, part, rows):
    return pl.ds(pl.multiple_of(place_ref[part], 128), rows)


def find_bounds(segment_ref, bound_ref):
    length = segment_ref.shape[0]
    bound_ref[0] = 0
    bound_ref[DOCUMENTS] = length
    for d in range(1, DOCUMENTS):

        def halve(_, span):
            low, high = span
            middle = (low + high) // 2
            below = segment_ref[jnp.minimum(middle, length - 1)] < d
            inside = low < high
            return (
                jnp.where(jnp.logical_and(inside, below), middle + 1, low),
                jnp.where(jnp.logical_and(inside, jnp.logical_not(below)), middle, high),
            )

        low, _ = lax.fori_loop(0, length.bit_length(), halve, (0, length))
        bound_ref[d] = low


def find_window(segment_ref, bound_ref, qb):
    length = segment_ref.shape[0]
    first = segment_ref[qb * BLK]
    last = segment_ref[qb * BLK + BLK - 1]
    start = bound_ref[first] // 128 * 128
    count = (bound_ref[last + 1] - start + BLK - 1) // BLK
    return jnp.minimum(start, length - count * BLK), count


def each_tile(count, step):
    def two(i, _):
        step(i * (2 * BLK), 2 * BLK)
        return 0

    lax.fori_loop(0, count // 2, two, 0)

    @pl.when(count % 2 == 1)
    def _():
        step((count - 1) * BLK, BLK)


def make_marks(row_ref, mark_query, mark_key):
    length = mark_key.shape[0]
    step = 512
    for b in range(length // step):
        rows = slice(b * step, (b + 1) * step)
        column = jnp.broadcast_to(row_ref[0:1, rows], (128, step)).T
        lane = lax.broadcasted_iota(jnp.int32, (step, 128), 1) % 64
        same = lane == column
        line = lax.broadcasted_iota(jnp.int32, (128, step), 0) % 64
        mark_query[:, rows] = jnp.where(line == row_ref[0:1, rows], 1.0, 0.0).astype(jnp.bfloat16)
        apart = jnp.logical_and(lane < DOCUMENTS, jnp.logical_not(same))
        mark_key[rows, :] = jnp.where(apart, BIG, 0.0).astype(jnp.bfloat16)


def forward_kernel(place_ref, segment_ref, row_ref, tokens_ref, weights_ref, bias_ref, *refs):
    mine_ref, other_ref, lse_ref, qkv_ref, q2, k2, vt, acc, top, tot, keep, mark_query, mark_key, bound_ref = refs
    length = qkv_ref.shape[0]
    blocks = length // BLK
    part = length // 4

    @pl.when(pl.program_id(0) == 0)
    def _():
        find_bounds(segment_ref, bound_ref)
        make_marks(row_ref, mark_query, mark_key)

    low = lax.broadcasted_iota(jnp.int32, (part, 128), 1) < 64
    for b in range(4):
        src = part_rows(place_ref, b, part)
        dst = slice(b * part, (b + 1) * part)
        made = dot_nn(tokens_ref[src, :], weights_ref[...])
        lanes = pl.ds(pl.multiple_of(place_ref[4] * (128 * pl.num_programs(0)) + pl.program_id(0) * 128, 128), 128)
        q = ((made[:, 0:128] + bias_ref[0:1, lanes]) * 0.125).astype(jnp.bfloat16)
        k = made[:, 128:256].astype(jnp.bfloat16)
        v = (made[:, 256:384] + bias_ref[1:2, lanes]).astype(jnp.bfloat16)
        qkv_ref[src, 0:128] = q
        qkv_ref[src, 128:256] = k
        qkv_ref[src, 256:384] = v
        nohk = mark_key[dst, :]
        turned = q.T
        q2[0, 0:64, dst] = turned[0:64]
        q2[0, 64:128, dst] = mark_query[64:128, dst]
        q2[1, 0:64, dst] = mark_query[0:64, dst]
        q2[1, 64:128, dst] = turned[64:128]
        k2[0, dst, :] = jnp.where(low, k, nohk)
        k2[1, dst, :] = jnp.where(low, nohk, k)
        vt[:, dst] = v.T
    lse_ref[...] = jnp.zeros_like(lse_ref)

    def row(qb, _):
        qs = pl.ds(pl.multiple_of(qb * BLK, BLK), BLK)
        start, count = find_window(segment_ref, bound_ref, qb)
        top[...] = jnp.full_like(top, -1.0e30)

        def fold(tile, function):
            return function(tile.reshape(tile.shape[0] // 8, 8, BLK), axis=0)

        def highest(first, size):
            keys = pl.ds(pl.multiple_of(start + first, 128), size)
            for h in range(2):
                st = dot_nn(k2[h, keys, :], q2[h, :, qs])
                keep[h, pl.ds(pl.multiple_of(first, BLK), size), :] = st
                top[h] = jnp.maximum(top[h], fold(st, jnp.max))

        def weigh(first, size, largest):
            keys = pl.ds(pl.multiple_of(start + first, 128), size)
            for h in range(2):
                rows = slice(64 * h, 64 * h + 64)
                st = keep[h, pl.ds(pl.multiple_of(first, BLK), size), :]
                p = jnp.exp(st - largest[h])
                tot[h] = tot[h] + fold(p, jnp.sum)
                acc[rows, :] = acc[rows, :] + dot_nn(vt[rows, keys], p.astype(jnp.bfloat16))

        def paired(step):
            each_tile(count, step)

        paired(highest)
        largest = [jnp.max(top[h], axis=0, keepdims=True) for h in range(2)]
        acc[...] = jnp.zeros_like(acc)
        tot[...] = jnp.zeros_like(tot)
        paired(lambda first, size: weigh(first, size, largest))
        for h in range(2):
            rows = slice(64 * h, 64 * h + 64)
            total = jnp.sum(tot[h], axis=0, keepdims=True)
            acc[rows, :] = acc[rows, :] / total
            lse_ref[h : h + 1, qs] = largest[h] + jnp.log(total)
        where = place_ref[qb * BLK // part] + qb * BLK % part
        result = acc[...].T.astype(jnp.bfloat16)

        @pl.when(where < 2 * part)
        def _():
            mine_ref[pl.ds(pl.multiple_of(where, BLK), BLK), :] = result

        @pl.when(where >= 2 * part)
        def _():
            other_ref[pl.ds(pl.multiple_of(where - 2 * part, BLK), BLK), :] = result

        return 0

    lax.fori_loop(0, blocks, row, 0)


def attention(place, segments, tokens, weights, biases):
    length, depth = tokens.shape
    width = weights.shape[1]
    pairs = width // 384
    rows = length // 2
    return pl.pallas_call(
        forward_kernel,
        out_shape=(
            jax.ShapeDtypeStruct((rows, pairs * 128), jnp.bfloat16),
            jax.ShapeDtypeStruct((rows, pairs * 128), jnp.bfloat16),
            jax.ShapeDtypeStruct((pairs * 8, length), jnp.float32),
            jax.ShapeDtypeStruct((length, width), jnp.bfloat16),
        ),
        grid_spec=pltpu.PrefetchScalarGridSpec(
            num_scalar_prefetch=2,
            grid=(pairs,),
            in_specs=[
                pl.BlockSpec((1, length), lambda p, *_: (0, 0)),
                pl.BlockSpec((length, depth), lambda p, *_: (0, 0)),
                pl.BlockSpec((depth, 384), lambda p, *_: (0, p)),
                pl.BlockSpec(biases.shape, lambda p, *_: (0, 0)),
            ],
            out_specs=[
                pl.BlockSpec((rows, 128), lambda p, *_: (0, p)),
                pl.BlockSpec((rows, 128), lambda p, *_: (0, p)),
                pl.BlockSpec((8, length), lambda p, *_: (p, 0)),
                pl.BlockSpec((length, 384), lambda p, *_: (0, p)),
            ],
            scratch_shapes=[
                pltpu.VMEM((2, 128, length), jnp.bfloat16),
                pltpu.VMEM((2, length, 128), jnp.bfloat16),
                pltpu.VMEM((128, length), jnp.bfloat16),
                pltpu.VMEM((128, BLK), jnp.float32),
                pltpu.VMEM((2, 8, BLK), jnp.float32),
                pltpu.VMEM((2, 8, BLK), jnp.float32),
                pltpu.VMEM((2, length, BLK), jnp.float32),
                pltpu.VMEM((128, length), jnp.bfloat16),
                pltpu.VMEM((length, 128), jnp.bfloat16),
                pltpu.SMEM((DOCUMENTS + 1,), jnp.int32),
            ],
        ),
        compiler_params=pltpu.CompilerParams(dimension_semantics=("arbitrary",), vmem_limit_bytes=60 << 20),
        cost_estimate=pl.CostEstimate(flops=pairs * 8_000_000_000, bytes_accessed=pairs * 3_000_000, transcendentals=pairs * 4_000_000),
        name="attention_forward",
    )(place, segments, segments.reshape(1, length), tokens, weights, biases)


def backward_kernel(
    place_ref,
    segment_ref,
    qkv_ref,
    ctx_mine_ref,
    ctx_other_ref,
    do_mine_ref,
    do_other_ref,
    lse_ref,
    row_ref,
    out_ref,
    sum_ref,
    q2,
    k2,
    q0,
    d0,
    dt,
    v0,
    kt,
    dk,
    dv,
    dqt,
    delta,
    mark_query,
    mark_key,
    bound_ref,
):
    length = qkv_ref.shape[0]
    blocks = length // BLK
    part = length // 4

    @pl.when(pl.program_id(0) == 0)
    def _():
        find_bounds(segment_ref, bound_ref)
        make_marks(row_ref, mark_query, mark_key)

    low = lax.broadcasted_iota(jnp.int32, (part, 128), 1) < 64

    def prepare(b, do, ctx):
        src = part_rows(place_ref, b, part)
        dst = slice(b * part, (b + 1) * part)
        q, k = qkv_ref[src, 0:128], qkv_ref[src, 128:256]
        zero = jnp.zeros_like(q)
        nohk = mark_key[dst, :]
        turned = q.T
        q2[0, 0:64, dst] = turned[0:64]
        q2[0, 64:128, dst] = mark_query[64:128, dst]
        q2[1, 0:64, dst] = mark_query[0:64, dst]
        q2[1, 64:128, dst] = turned[64:128]
        k2[0, dst, :] = jnp.where(low, k, nohk)
        k2[1, dst, :] = jnp.where(low, nohk, k)
        q0[0, dst, :] = jnp.where(low, q, zero)
        q0[1, dst, :] = jnp.where(low, zero, q)
        d0[0, dst, :] = jnp.where(low, do, zero)
        d0[1, dst, :] = jnp.where(low, zero, do)
        turned = do.T
        blank = jnp.zeros((64, part), jnp.bfloat16)
        dt[0, 0:64, dst] = turned[0:64]
        dt[0, 64:128, dst] = blank
        dt[1, 0:64, dst] = blank
        dt[1, 64:128, dst] = turned[64:128]
        v0[dst, :] = qkv_ref[src, 256:384]
        kt[:, dst] = k.T
        prod = turned.astype(jnp.float32) * ctx.T.astype(jnp.float32)
        delta[0:1, dst] = jnp.sum(prod[0:64], axis=0, keepdims=True)
        delta[1:2, dst] = jnp.sum(prod[64:128], axis=0, keepdims=True)

    for b in range(4):

        @pl.when(place_ref[b] < 2 * part)
        def _():
            rows = part_rows(place_ref, b, part)
            prepare(b, do_mine_ref[rows, :], ctx_mine_ref[rows, :])

        @pl.when(place_ref[b] >= 2 * part)
        def _():
            rows = pl.ds(pl.multiple_of(place_ref[b] - 2 * part, 128), part)
            prepare(b, do_other_ref[rows, :], ctx_other_ref[rows, :])

    dk[...] = jnp.zeros_like(dk)
    dv[...] = jnp.zeros_like(dv)
    dqt[...] = jnp.zeros_like(dqt)

    def row(qb, _):
        qs = pl.ds(pl.multiple_of(qb * BLK, BLK), BLK)
        start, count = find_window(segment_ref, bound_ref, qb)

        def tile(first, size):
            ks = pl.ds(pl.multiple_of(start + first, 128), size)
            weights, grads = [], []
            for h in range(2):
                st = dot_nn(k2[h, ks, :], q2[h, :, qs])
                w = jnp.exp(st - lse_ref[h : h + 1, qs])
                gw = dot_nn(v0[ks, :], dt[h, :, qs])
                weights.append(w.astype(jnp.bfloat16))
                grads.append((w * (gw - delta[h : h + 1, qs])).astype(jnp.bfloat16))
            dv[ks, :] += dot_nn(jnp.concatenate(weights, axis=1), jnp.concatenate([d0[0, qs, :], d0[1, qs, :]], axis=0))
            dk[ks, :] += dot_nn(jnp.concatenate(grads, axis=1), jnp.concatenate([q0[0, qs, :], q0[1, qs, :]], axis=0))
            for h in range(2):
                rows = slice(64 * h, 64 * h + 64)
                dqt[rows, qs] += dot_nn(kt[rows, ks], grads[h])

        each_tile(count, tile)
        return 0

    lax.fori_loop(0, blocks, row, 0)
    sums = [jnp.zeros((1, 128), jnp.float32) for _ in range(3)]
    for b in range(4):
        dst = part_rows(place_ref, b, part)
        src = slice(b * part, (b + 1) * part)
        pieces = ((dqt[:, src].T * 0.125).astype(jnp.bfloat16), dk[src, :].astype(jnp.bfloat16), dv[src, :].astype(jnp.bfloat16))
        for i, piece in enumerate(pieces):
            out_ref[dst, 128 * i : 128 * i + 128] = piece
            sums[i] = sums[i] + jnp.sum(piece.astype(jnp.float32), axis=0, keepdims=True)
    sum_ref[...] = jnp.zeros_like(sum_ref)
    for i in range(3):
        sum_ref[0:1, 128 * i : 128 * i + 128] = sums[i]


def attention_back(place, segments, qkv, ctx_mine, ctx_other, do_mine, do_other, lse):
    length, width = qkv.shape
    pairs = width // 384
    rows = length // 2
    half = lambda: pltpu.VMEM((2, length, 128), jnp.bfloat16)
    turned = lambda: pltpu.VMEM((2, 128, length), jnp.bfloat16)
    column = pl.BlockSpec((rows, 128), lambda p, *_: (0, p))
    return pl.pallas_call(
        backward_kernel,
        out_shape=(
            jax.ShapeDtypeStruct((length, width), jnp.bfloat16),
            jax.ShapeDtypeStruct((pairs * 8, 384), jnp.float32),
        ),
        grid_spec=pltpu.PrefetchScalarGridSpec(
            num_scalar_prefetch=2,
            grid=(pairs,),
            in_specs=[
                pl.BlockSpec((length, 384), lambda p, *_: (0, p)),
                column,
                column,
                column,
                column,
                pl.BlockSpec((8, length), lambda p, *_: (p, 0)),
                pl.BlockSpec((1, length), lambda p, *_: (0, 0)),
            ],
            out_specs=[
                pl.BlockSpec((length, 384), lambda p, *_: (0, p)),
                pl.BlockSpec((8, 384), lambda p, *_: (p, 0)),
            ],
            scratch_shapes=[
                turned(),
                half(),
                half(),
                half(),
                turned(),
                pltpu.VMEM((length, 128), jnp.bfloat16),
                pltpu.VMEM((128, length), jnp.bfloat16),
                pltpu.VMEM((length, 128), jnp.float32),
                pltpu.VMEM((length, 128), jnp.float32),
                pltpu.VMEM((128, length), jnp.float32),
                pltpu.VMEM((8, length), jnp.float32),
                pltpu.VMEM((128, length), jnp.bfloat16),
                pltpu.VMEM((length, 128), jnp.bfloat16),
                pltpu.SMEM((DOCUMENTS + 1,), jnp.int32),
            ],
        ),
        compiler_params=pltpu.CompilerParams(dimension_semantics=("arbitrary",), vmem_limit_bytes=60 << 20),
        cost_estimate=pl.CostEstimate(flops=pairs * 20_000_000_000, bytes_accessed=pairs * 5_000_000, transcendentals=pairs * 4_000_000),
        name="attention_backward",
    )(place, segments, qkv, ctx_mine, ctx_other, do_mine, do_other, lse, segments.reshape(1, length))


MESH_ID = pl.DeviceIdType.MESH
WIDE = 5


def place_of():
    return tuple(lax.axis_index(name) for name in ("z", "x", "y", "core"))


def sizes_of():
    return lax.axis_size("z"), lax.axis_size("x")


def partner(**moved):
    z, x, y, core = place_of()
    return (moved.get("z", z), moved.get("x", x), moved.get("y", y), moved.get("core", core))


def greet(with_grid):
    z, x, y, core = place_of()
    size_z, size_x = sizes_of()
    peers = [partner(y=1 - y), partner(core=1 - core)]
    if with_grid:
        peers += [partner(z=lax.rem(z + k, size_z)) for k in range(1, size_z)]
        peers += [partner(x=lax.rem(x + j, size_x)) for j in range(1, size_x)]
    barrier = pltpu.get_barrier_semaphore()
    for peer in peers:
        pl.semaphore_signal(barrier, inc=1, device_id=peer, device_id_type=MESH_ID)
    pl.semaphore_wait(barrier, len(peers))


def remote(src, dst, send, recv, peer):
    return pltpu.make_async_remote_copy(
        src_ref=src, dst_ref=dst, send_sem=send, recv_sem=recv, device_id=peer, device_id_type=MESH_ID
    )


def entry_kernel(size_z, size_x, count, *refs):
    tokens, cotangent, wq, wk, wv = refs[:5]
    vectors = refs[5 : 5 + count]
    tokens_all, cotangent_all, weights_all, rows_out, inner_out = refs[5 + count : 10 + count]
    raw = refs[10 + count : 10 + 2 * count]
    stage, cot_stage, wbuf, pack, vpack, vectors_all, local_sem, load_sem, tsend, trecv, zsend, zrecv, xsend, xrecv = refs[
        10 + 2 * count :
    ]
    z, x, y, core = place_of()
    half = pack.shape[1] // 3
    pairs = half // 128
    me = z * size_x + x

    mine = pl.ds(pl.multiple_of(core * half, 128), half)
    loads = [pltpu.make_async_copy(w.at[:, mine], wbuf.at[i], load_sem.at[i]) for i, w in enumerate((wq, wk, wv))]
    loads += [pltpu.make_async_copy(v, r, load_sem.at[3 + i]) for i, (v, r) in enumerate(zip(vectors, raw))]
    for load in loads:
        load.start()
    load = pltpu.make_async_copy(tokens.at[y], stage, local_sem.at[0])
    load.start()
    cot_load = pltpu.make_async_copy(cotangent.at[y], cot_stage, local_sem.at[4])
    cot_load.start()
    vpack[...] = jnp.zeros_like(vpack)
    for copy in loads:
        copy.wait()
    for i, vector in enumerate(raw):
        vpack[i : i + 1, 0 : vector.shape[1]] = vector[...].astype(jnp.bfloat16).astype(jnp.float32)
    for i in range(3):
        for p in range(pairs):
            pack[:, (3 * p + i) * 128 : (3 * p + i + 1) * 128] = wbuf[i, :, p * 128 : (p + 1) * 128].astype(jnp.bfloat16)
    greet(True)
    across = remote(tokens.at[1 - y], tokens_all.at[1], tsend.at[0], trecv.at[0], partner(y=1 - y))
    across.start()
    along = []
    for k in range(1, size_z):
        peer = partner(z=lax.rem(z + k, size_z))
        along.append(
            (
                remote(pack, weights_all.at[me], zsend.at[0, k - 1], zrecv.at[0, k - 1], peer),
                remote(vpack, vectors_all.at[me], zsend.at[1, k - 1], zrecv.at[1, k - 1], peer),
            )
        )
    beside = remote(tokens.at[y], tokens_all.at[2], tsend.at[1], trecv.at[1], partner(core=1 - core))
    sideways = []

    def forward(k, weights_src, vectors_src):
        slot = lax.rem(z - k + size_z, size_z) * size_x + x
        for j in range(1, size_x):
            peer = partner(x=lax.rem(x + j, size_x))
            first = remote(weights_src, weights_all.at[slot], xsend.at[0, k, j - 1], xrecv.at[0, k, j - 1], peer)
            second = remote(vectors_src, vectors_all.at[slot], xsend.at[1, k, j - 1], xrecv.at[1, k, j - 1], peer)
            first.start()
            second.start()
            sideways.append((first, second))

    forward(0, pack, vpack)
    for first, second in along:
        first.start()
        second.start()
    beside.start()
    keep_weights = pltpu.make_async_copy(pack, weights_all.at[me], local_sem.at[1])
    keep_weights.start()
    vectors_all[me] = vpack[...]
    load.wait()
    keep_tokens = pltpu.make_async_copy(stage, tokens_all.at[0], local_sem.at[3])
    keep_tokens.start()
    cot_load.wait()
    keep_cot = pltpu.make_async_copy(cot_stage, cotangent_all.at[0], local_sem.at[5])
    keep_cot.start()
    order = sorted(range(1, size_z), key=lambda k: min(k, size_z - k))
    for k in order:
        first, second = along[k - 1]
        first.wait_recv()
        second.wait_recv()
        slot = lax.rem(z - k + size_z, size_z) * size_x + x
        forward(k, weights_all.at[slot], vectors_all.at[slot])
    across.wait_recv()
    onward = remote(tokens_all.at[1], tokens_all.at[3], tsend.at[2], trecv.at[2], partner(core=1 - core))
    onward.start()
    later = remote(cotangent.at[1 - y], cotangent_all.at[1], tsend.at[3], trecv.at[3], partner(y=1 - y))
    later.start()
    for first, second in sideways:
        first.wait()
        second.wait()
    for first, second in along:
        first.wait_send()
        second.wait_send()
    short = min(vector.shape[1] for vector in raw)
    longest = vpack.shape[1]
    for s in range(size_z * size_x):
        rows_out[:, s * short : (s + 1) * short] = vectors_all[s, :, 0:short]
        inner_out[:, s * longest : (s + 1) * longest] = vectors_all[s, WIDE : WIDE + 1, :]
    across.wait_send()
    beside.wait()
    onward.wait()
    later.wait()
    keep_weights.wait()
    keep_tokens.wait()
    keep_cot.wait()


def entry(size_z, size_x, tokens, cotangent, wq, wk, wv, vectors):
    _, part, width = tokens.shape
    rows = wq.shape[0]
    lanes = wq.shape[1] // 2 * 3
    longest = max(v.shape[0] for v in vectors)
    shards = size_z * size_x
    anywhere = pl.BlockSpec(memory_space=pl.ANY)
    dma = pltpu.SemaphoreType.DMA
    return pl.pallas_call(
        lambda *refs: entry_kernel(size_z, size_x, len(vectors), *refs),
        out_shape=(
            jax.ShapeDtypeStruct((4, part, width), tokens.dtype),
            jax.ShapeDtypeStruct((2, part, width), cotangent.dtype),
            jax.ShapeDtypeStruct((shards, rows, lanes), jnp.bfloat16),
            jax.ShapeDtypeStruct((16, width), jnp.float32),
            jax.ShapeDtypeStruct((1, shards * longest), jnp.float32),
        ),
        in_specs=[anywhere] * (5 + len(vectors)),
        out_specs=(anywhere,) * 3 + (pl.BlockSpec(memory_space=pltpu.VMEM),) * 2,
        scratch_shapes=[pltpu.VMEM((1, v.shape[0]), v.dtype) for v in vectors]
        + [
            pltpu.VMEM((part, width), tokens.dtype),
            pltpu.VMEM((part, width), cotangent.dtype),
            pltpu.VMEM((3, rows, lanes // 3), wq.dtype),
            pltpu.VMEM((rows, lanes), jnp.bfloat16),
            pltpu.VMEM((16, longest), jnp.float32),
            pltpu.VMEM((shards, 16, longest), jnp.float32),
            dma((6,)),
            dma((3 + len(vectors),)),
            dma((4,)),
            dma((4,)),
            dma((2, size_z - 1)),
            dma((2, size_z - 1)),
            dma((2, size_z, max(size_x - 1, 1))),
            dma((2, size_z, max(size_x - 1, 1))),
        ],
        compiler_params=pltpu.CompilerParams(collective_id=0, has_side_effects=True, vmem_limit_bytes=66_000_000),
        name="entry",
    )(tokens, cotangent, wq, wk, wv, *[v.reshape(1, -1) for v in vectors])


def exit_kernel(size_z, size_x, shapes, *refs):
    z, x, y, core = place_of()
    names = list(shapes)
    grads_hbm, inputs_hbm, weights_hbm, base_hbm, output_term, dense_sums, inner_sums, head_sums = refs[:8]
    inner_in = refs[8 : 8 + size_z]
    outer_in = refs[8 + size_z : 8 + size_z + size_x]
    refs = refs[8 + size_z + size_x :]
    results = refs[:8]
    token_grads, grad_query, grad_key, grad_value, grad_output, grad_inner, grad_outer, vector_sums = refs[8:16]
    grads, inputs, turned, weights, base, terms, other_rows, recv_rows, send_rows, far_rows, odd = refs[16:27]
    inner_buf, outer_buf, vector_rows, vector_terms, store_sem = refs[27:32]
    load_sem, tsend, trecv, osend, orecv = refs[32:37]
    refs = refs[37:]
    made = (token_grads, grad_query, grad_key, grad_value, grad_output, grad_inner, grad_outer, vector_sums)
    stores = [pltpu.make_async_copy(a, b, store_sem.at[i]) for i, (a, b) in enumerate(zip(made, results))]
    xin, xsend, xrecv, xout = {}, {}, {}, {}
    zout, zin, zsend, zrecv = {}, {}, {}, {}
    ybuf, ysend, yrecv, cbuf, csend, crecv = {}, {}, {}, {}, {}, {}
    refs = list(refs)
    for name in names:
        ybuf[name], ysend[name], yrecv[name], cbuf[name], csend[name], crecv[name] = [refs.pop(0) for _ in range(6)]
        if name != "outer":
            xin[name], xsend[name], xrecv[name] = [refs.pop(0) for _ in range(3)]
        if name != "inner":
            zout[name], zin[name], zsend[name], zrecv[name] = [refs.pop(0) for _ in range(4)]
    xout["inner"] = refs.pop(0)

    shards, rows, lanes = terms.shape
    half = lanes // 3
    width = 2 * half
    pairs = half // 128
    hidden = grad_inner.shape[1]
    part = token_grads.shape[1]
    local = 2 * part
    low, high = jnp.bfloat16, jnp.float32
    mine = pl.ds(pl.multiple_of(core * half, 128), half)
    theirs = pl.ds(pl.multiple_of((1 - core) * half, 128), half)
    order = sorted(range(size_z), key=lambda k: -min(k, size_z - k))
    far_order = [k for k in order if k > 0]
    columns = [lax.rem(x + j, size_x) for j in range(size_x)]

    def slot_of(k, j):
        return lax.rem(z + k, size_z) * size_x + columns[j]

    loads = {}
    for i, src in enumerate(inner_in):
        loads["inner", i] = pltpu.make_async_copy(src, inner_buf.at[i], load_sem.at[i])
    for i, src in enumerate(outer_in):
        loads["outer", i] = pltpu.make_async_copy(src, outer_buf.at[i], load_sem.at[size_z + i])
    for i, (name, src, dst) in enumerate(
        (("inputs", inputs_hbm, inputs), ("grads", grads_hbm, grads), ("weights", weights_hbm, weights), ("base", base_hbm, base))
    ):
        loads[name] = pltpu.make_async_copy(src, dst, load_sem.at[size_z + size_x + i])
    for load in loads.values():
        load.start()
    greet(True)

    core_peer, y_peer = partner(core=1 - core), partner(y=1 - y)
    outputs = remote(output_term.at[:, :, theirs], odd, osend, orecv, core_peer)
    outputs.start()
    sideways = {}
    along = {}
    kept = {}

    def send_x(name, n, k, j, src, dst):
        move = remote(src, dst, xsend[name].at[n, k, j - 1], xrecv[name].at[n, k, j - 1], partner(x=columns[j]))
        move.start()
        sideways.setdefault((name, k, j), []).append(move)

    def send_z(name, k):
        move = remote(
            zout[name].at[k - 1],
            zin[name].at[k - 1],
            zsend[name].at[k - 1],
            zrecv[name].at[k - 1],
            partner(z=lax.rem(z + k, size_z)),
        )
        move.start()
        along[name, k] = move

    vector_rows[...] = jnp.zeros_like(vector_rows)
    for i, row in enumerate((7, 8, 6, 3, 4, 2)):
        vector_rows[row : row + 1, :] = jnp.sum(dense_sums[8 * i : 8 * i + 8, :], axis=0, keepdims=True)
    for p in range(pairs):
        place = pl.ds(pl.multiple_of(core * half + p * 128, 128), 128)
        vector_rows[0:1, place] = head_sums[8 * p : 8 * p + 1, 0:128]
        vector_rows[1:2, place] = head_sums[8 * p : 8 * p + 1, 256:384]
    inner_row = jnp.sum(inner_sums[...], axis=0, keepdims=True)
    vector_terms[...] = jnp.zeros_like(vector_terms)
    longest = vector_terms.shape[2]
    for s in range(shards):
        vector_terms[s, :, 0:rows] = vector_rows[:, s * rows : (s + 1) * rows]
        vector_terms[s, WIDE : WIDE + 1, :] = inner_row[:, s * longest : (s + 1) * longest]
    for k in order:
        for j in range(1, size_x):
            send_x("vec", 0, k, j, vector_terms.at[slot_of(k, j)], xin["vec"].at[j - 1, k])

    for i in range(size_z):
        loads["inner", i].wait()
    for j in range(size_x):
        total = inner_buf[0, columns[j]].astype(high)
        for i in range(1, size_z):
            total = total + inner_buf[i, columns[j]].astype(high)
        if j == 0:
            kept["inner"] = total
        else:
            xout["inner"][j - 1] = total.astype(low)
            send_x("inner", 0, 0, j, xout["inner"].at[j - 1], xin["inner"].at[j - 1, 0])

    for i in range(size_x):
        loads["outer", i].wait()
    for k in order:
        target = lax.rem(z + k, size_z)
        total = outer_buf[0, target].astype(high)
        for i in range(1, size_x):
            total = total + outer_buf[i, target].astype(high)
        if k == 0:
            kept["outer"] = total
        else:
            zout["outer"][k - 1] = total.astype(low)
            send_z("outer", k)

    loads["inputs"].wait()
    for b in range(4):
        turned[:, b * part : (b + 1) * part] = inputs[b * part : (b + 1) * part, :].T
    loads["grads"].wait()
    group = 4
    for p in range(pairs):
        block = slice(p * 384, (p + 1) * 384)

        def some(m, _):
            value = dot_nn(turned[pl.ds(pl.multiple_of(m * group * rows, group * rows), group * rows), :], grads[:, block])
            terms[pl.ds(m * group, group), :, block] = value.reshape(group, rows, 384).astype(low)
            return 0

        lax.fori_loop(0, shards // group, some, 0)
        for k in order:
            for j in range(1, size_x):
                send_x("qkv", p, k, j, terms.at[slot_of(k, j), :, block], xin["qkv"].at[j - 1, k, :, block])

    loads["weights"].wait()
    strip = 256

    def product(first):
        at = pl.ds(pl.multiple_of(first, strip), strip)
        return dot_nt(grads[at, :], weights[...])

    def other_strip(i, _):
        other_rows[pl.ds(pl.multiple_of(i * strip, strip), strip), :] = product(local + i * strip).astype(low)
        return 0

    lax.fori_loop(0, local // strip, other_strip, 0)
    halves = remote(other_rows, recv_rows, tsend.at[0], trecv.at[0], core_peer)
    halves.start()
    outputs.wait()
    for k in order:
        for j in range(1, size_x):
            slot = slot_of(k, j)
            odd[slot] = (odd[slot].astype(high) + output_term[slot, :, mine].astype(high)).astype(low)
            send_x("out", 0, k, j, odd.at[slot], xin["out"].at[j - 1, k])
    loads["base"].wait()

    def own_strip(i, _):
        at = pl.ds(pl.multiple_of(i * strip, strip), strip)
        base[at, :] = base[at, :] + product(i * strip)
        return 0

    lax.fori_loop(0, local // strip, own_strip, 0)
    halves.wait()
    send_rows[...] = (base[part:local, :] + recv_rows[part:local, :].astype(high)).astype(low)
    back = remote(send_rows, far_rows, tsend.at[1], trecv.at[1], y_peer)
    back.start()
    token_grads[y] = base[0:part, :] + recv_rows[0:part, :].astype(high)

    across = {}
    swapped = {}

    def step_y(name):
        move = remote(ybuf[name].at[0], ybuf[name].at[1], ysend[name], yrecv[name], y_peer)
        move.start()
        across[name] = move

    def step_core(name):
        across[name].wait()
        cbuf[name][0] = ybuf[name][0].astype(high) + ybuf[name][1].astype(high)
        move = remote(cbuf[name].at[0], cbuf[name].at[1], csend[name], crecv[name], core_peer)
        move.start()
        swapped[name] = move

    def finish_x(name):
        for k in order:
            slot = slot_of(k, 0)
            if name == "qkv":
                total = terms[slot].astype(high)
            elif name == "out":
                total = odd[slot].astype(high) + output_term[slot, :, mine].astype(high)
            else:
                total = vector_terms[slot]
            for j in range(1, size_x):
                for move in sideways[name, k, j]:
                    move.wait()
                total = total + xin[name][j - 1, k].astype(high)
            if k == 0:
                kept[name] = total
            else:
                zout[name][k - 1] = total.astype(zout[name].dtype)
                send_z(name, k)

    def finish_z(name):
        total = kept[name]
        for k in far_order:
            along[name, k].wait()
            total = total + zin[name][k - 1].astype(high)
        ybuf[name][0] = total.astype(ybuf[name].dtype)
        step_y(name)

    total = kept["inner"]
    for j in range(1, size_x):
        for move in sideways["inner", 0, j]:
            move.wait()
        total = total + xin["inner"][j - 1, 0].astype(high)
    ybuf["inner"][0] = total.astype(low)
    step_y("inner")
    finish_x("vec")
    finish_x("qkv")
    finish_z("outer")
    step_core("inner")
    finish_x("out")
    finish_z("vec")
    step_core("outer")
    finish_z("qkv")
    finish_z("out")
    back.wait()
    token_grads[1 - y] = far_rows[...].astype(high)
    stores[0].start()
    step_core("vec")

    def finish_core(name):
        swapped[name].wait()
        return cbuf[name]

    buf = finish_core("inner")
    chunks = hidden // CHUNK
    for i in range(2):
        owner = core if i == 0 else 1 - core
        for c in range(chunks):
            place = pl.ds(pl.multiple_of(c * CHUNK + owner * half, 128), half)
            grad_inner[:, place] = buf[i, :, c * half : (c + 1) * half]
    stores[5].start()
    buf = finish_core("outer")
    for i in range(2):
        owner = core if i == 0 else 1 - core
        grad_outer[:, pl.ds(pl.multiple_of(owner * half, 128), half)] = buf[i]
    stores[6].start()
    step_core("qkv")
    step_core("out")
    buf = finish_core("vec")
    vector_sums[...] = buf[0] + buf[1]
    stores[7].start()
    buf = finish_core("qkv")
    for i in range(2):
        owner = core if i == 0 else 1 - core
        for p in range(pairs):
            place = pl.ds(pl.multiple_of(owner * half + p * 128, 128), 128)
            for n, out in enumerate((grad_query, grad_key, grad_value)):
                out[:, place] = buf[i, :, (3 * p + n) * 128 : (3 * p + n + 1) * 128]
    for i in (1, 2, 3):
        stores[i].start()
    buf = finish_core("out")
    for i in range(2):
        owner = core if i == 0 else 1 - core
        grad_output[:, pl.ds(pl.multiple_of(owner * half, 128), half)] = buf[i]
    stores[4].start()
    for store in stores:
        store.wait()


def deliver_kernel(count, *refs):
    sources, vectors, outs, sem = refs[:count], refs[count], refs[count + 1 : -1], refs[-1]
    copies = [pltpu.make_async_copy(src, dst, sem.at[i]) for i, (src, dst) in enumerate(zip(sources, outs))]
    for copy in copies:
        copy.start()
    for i, out in enumerate(outs[count:]):
        out[...] = vectors[i : i + 1, 0 : out.shape[1]]
    for copy in copies:
        copy.wait()


def deliver(matrices, vectors, sizes):
    count = len(matrices)
    vmem, anywhere = pl.BlockSpec(memory_space=pltpu.VMEM), pl.BlockSpec(memory_space=pl.ANY)
    return pl.pallas_call(
        lambda *refs: deliver_kernel(count, *refs),
        out_shape=tuple(jax.ShapeDtypeStruct(m.shape, m.dtype) for m in matrices)
        + tuple(jax.ShapeDtypeStruct((1, size), jnp.float32) for size in sizes),
        in_specs=[vmem] * (count + 1),
        out_specs=(anywhere,) * count + (vmem,) * len(sizes),
        scratch_shapes=[pltpu.SemaphoreType.DMA((count,))],
        compiler_params=pltpu.CompilerParams(vmem_limit_bytes=60_000_000),
        name="deliver",
    )(*matrices, vectors)


def exit_call(size_z, size_x, grads, inputs, weights, base, output_term, dense_sums, inner_sums, head_sums, inner_terms, outer_terms):
    shards, rows, width = output_term.shape
    lanes = grads.shape[1]
    half = width // 2
    pairs = half // 128
    length = inputs.shape[0]
    local = length // 2
    part = local // 2
    long = outer_terms[0].shape[1]
    hidden = 2 * inner_terms[0].shape[2]
    vmem, anywhere = pl.BlockSpec(memory_space=pltpu.VMEM), pl.BlockSpec(memory_space=pl.ANY)
    dma = pltpu.SemaphoreType.DMA
    side = size_x - 1
    low, high = jnp.bfloat16, jnp.float32
    vector_shape = (16, hidden // shards)
    shapes = {
        "vec": (vector_shape, high, 1),
        "qkv": ((rows, lanes), low, pairs),
        "out": ((rows, half), low, 1),
        "inner": ((rows, hidden // 2), low, 1),
        "outer": ((long, half), low, 1),
    }
    matrix = jax.ShapeDtypeStruct((rows, width), high)
    results = (
        jax.ShapeDtypeStruct((2, part, width), high),
        matrix,
        matrix,
        matrix,
        matrix,
        jax.ShapeDtypeStruct((rows, hidden), high),
        jax.ShapeDtypeStruct((long, width), high),
        jax.ShapeDtypeStruct(vector_shape, high),
    )
    scratch = [pltpu.VMEM(r.shape, r.dtype) for r in results] + [
        pltpu.VMEM((length, lanes), low),
        pltpu.VMEM((length, width), low),
        pltpu.VMEM((width, length), low),
        pltpu.VMEM((width, lanes), low),
        pltpu.VMEM((local, width), high),
        pltpu.VMEM((shards, rows, lanes), low),
        pltpu.VMEM((local, width), low),
        pltpu.VMEM((local, width), low),
        pltpu.VMEM((part, width), low),
        pltpu.VMEM((part, width), low),
        pltpu.VMEM((shards, rows, half), low),
        pltpu.VMEM((size_z,) + inner_terms[0].shape, low),
        pltpu.VMEM((size_x,) + outer_terms[0].shape, low),
        pltpu.VMEM((16, width), high),
        pltpu.VMEM((shards,) + vector_shape, high),
        dma((len(results),)),
        dma((size_z + size_x + 4,)),
        dma((2,)),
        dma((2,)),
        dma,
        dma,
    ]
    for name, (shape, kind, sends) in shapes.items():
        scratch += [pltpu.VMEM((2,) + shape, kind), dma, dma, pltpu.VMEM((2,) + shape, high), dma, dma]
        stages = 1 if name == "inner" else size_z
        if name != "outer":
            scratch += [pltpu.VMEM((side, stages) + shape, kind), dma((sends, stages, side)), dma((sends, stages, side))]
        if name != "inner":
            scratch += [pltpu.VMEM((size_z - 1,) + shape, kind)] * 2 + [dma((size_z - 1,))] * 2
    scratch.append(pltpu.VMEM((side, rows, hidden // 2), low))
    return pl.pallas_call(
        lambda *refs: exit_kernel(size_z, size_x, shapes, *refs),
        out_shape=results,
        in_specs=[anywhere] * 4 + [vmem] * 4 + [anywhere] * (size_z + size_x),
        out_specs=(anywhere,) * len(results),
        scratch_shapes=scratch,
        compiler_params=pltpu.CompilerParams(collective_id=1, has_side_effects=True, vmem_limit_bytes=67_000_000),
        name="exit",
    )(grads, inputs, weights, base, output_term, dense_sums, inner_sums, head_sums, *inner_terms, *outer_terms)


TILE = 256
CHUNK = 768


def dot_nt(a, b):
    return lax.dot_general(a, b, (((1,), (1,)), ((), ())), preferred_element_type=jnp.float32)


def row_mean(value):
    return jnp.sum(value, axis=-1, keepdims=True) * (1.0 / value.shape[-1])


def standardize(hidden):
    centred = hidden - row_mean(hidden)
    reciprocal = lax.rsqrt(row_mean(centred * centred) + EPS)
    return centred * reciprocal, reciprocal


def column_sum(value):
    return jnp.sum(value.reshape(value.shape[0] // 8, 8, value.shape[1]), axis=0)


def dense_kernel(
    size_z,
    size_x,
    tokens_ref,
    mine_ref,
    other_ref,
    cot_ref,
    vectors_ref,
    bias_inner_ref,
    weights_hbm,
    *refs,
):
    mixed_ref, pre_first_ref, grad_mine_ref, grad_other_ref, sums_ref, inner_sum_ref, grad_output_ref = refs[:7]
    inner_terms = refs[7 : 7 + size_z]
    outer_terms = refs[7 + size_z : 7 + size_z + size_x]
    refs = refs[7 + size_z + size_x :]
    w_output, w_inner, w_outer, a_output, a_inner, a_outer, grad_out_buf = refs[:7]
    context, first_low, turned_low, normed, first, slope, active, work = refs[7:15]
    send_inner, send_outer, recv_inner, recv_outer, load_sem, outer_sem, send_sem, recv_sem, store_sem = refs[15:]
    step, steps = pl.program_id(0), pl.num_programs(0)
    core_here = lax.axis_index("core")
    width, hidden = w_inner.shape
    half = width // 2
    chunks = hidden // CHUNK
    shards = size_z * size_x
    pieces = 2 * shards
    rows = width // pieces
    ratio = hidden // width
    z, x, y, _ = place_of()
    twin = partner(core=1 - lax.axis_index("core"))

    def load_outer(start):
        if not start:
            pltpu.make_async_copy(w_outer, w_outer, outer_sem).wait()
            return

        def piece(s, _):
            for q in range(ratio):
                src = weights_hbm.at[
                    pl.ds(pl.multiple_of(s * rows, rows), rows), pl.ds(hidden + width + q * width, width)
                ]
                dst = w_outer.at[pl.ds(pl.multiple_of((s * ratio + q) * rows, rows), rows), :]
                pltpu.make_async_copy(src, dst, outer_sem).start()
            return 0

        lax.fori_loop(0, pieces, piece, 0)

    loads = (
        pltpu.make_async_copy(weights_hbm.at[:, pl.ds(hidden, width)], w_output, load_sem.at[0]),
        pltpu.make_async_copy(weights_hbm.at[:, pl.ds(0, hidden)], w_inner, load_sem.at[1]),
    )

    @pl.when(step == 0)
    def _():
        barrier = pltpu.get_barrier_semaphore()
        pl.semaphore_signal(barrier, inc=1, device_id=twin, device_id_type=MESH_ID)
        pl.semaphore_wait(barrier, 1)
        for load in loads:
            load.start()
        load_outer(True)
        a_output[...] = jnp.zeros_like(a_output)
        a_inner[...] = jnp.zeros_like(a_inner)
        a_outer[...] = jnp.zeros_like(a_outer)
        sums_ref[...] = jnp.zeros_like(sums_ref)
        inner_sum_ref[...] = jnp.zeros_like(inner_sum_ref)

    def vector(i):
        row = (2, 3, 4, 6, 7, 8)[i]
        return vectors_ref[row : row + 1, :]

    def add_sum(i, value):
        sums_ref[8 * i : 8 * i + 8, :] += column_sum(value)

    context[:, pl.ds(pl.multiple_of(core_here * half, 128), half)] = mine_ref[...]
    context[:, pl.ds(pl.multiple_of((1 - core_here) * half, 128), half)] = other_ref[...]

    @pl.when(step == 0)
    def _():
        loads[0].wait()

    hidden_rows = tokens_ref[...].astype(jnp.float32) + (dot_nn(context[...], w_output[...]) + vector(0))
    normed[...], first_recip = standardize(hidden_rows)
    first[...] = normed[...] * vector(1) + vector(2)
    first_low[...] = first[...].astype(jnp.bfloat16)
    turned_low[...] = first_low[...].T
    work[...] = jnp.broadcast_to(vector(3), work.shape)

    @pl.when(step == 0)
    def _():
        loads[1].wait()
        load_outer(False)

    def part(c):
        return pl.ds(pl.multiple_of(c * CHUNK, CHUNK), CHUNK)

    def exchange(c):
        return (
            remote(send_inner.at[c], recv_inner.at[c], send_sem.at[0, c], recv_sem.at[0, c], twin),
            remote(send_outer.at[c], recv_outer.at[c], send_sem.at[1, c], recv_sem.at[1, c], twin),
        )

    def forward(c, _):
        u = dot_nn(first_low[...], w_inner[:, part(c)]) + bias_inner_ref[0:1, part(c)]
        cdf = 0.5 * (1.0 + lax.erf(u * ROOT_HALF))
        slope[:, part(c)] = cdf + u * jnp.exp(-0.5 * u * u) * INV_ROOT_TAU
        active[:, part(c)] = (u * cdf).astype(jnp.bfloat16)
        work[...] += dot_nn(active[:, part(c)], w_outer[part(c), :])
        return 0

    lax.fori_loop(0, chunks, forward, 0)
    second, second_recip = standardize(first[...] + work[...])
    mixed_ref[...] = (second * vector(4) + vector(5)).astype(jnp.bfloat16)
    upstream = cot_ref[...].astype(jnp.float32)
    add_sum(0, upstream * second)
    add_sum(1, upstream)
    scaled = upstream * vector(4)
    pre_second = second_recip * (scaled - row_mean(scaled) - second * row_mean(scaled * second))
    grad_outer = pre_second.astype(jnp.bfloat16)
    add_sum(2, grad_outer.astype(jnp.float32))
    work[...] = pre_second
    grad_out_buf[...] = grad_outer

    def backward(c, _):
        grad_out = grad_out_buf[...]
        grad = dot_nt(grad_out, w_outer[part(c), :])
        grad_inner = (grad * slope[:, part(c)]).astype(jnp.bfloat16)
        inner_sum_ref[:, part(c)] += column_sum(grad_inner.astype(jnp.float32))
        a_outer[part(c), :] += dot_nn(active[:, part(c)].T, grad_out)
        a_inner[:, part(c)] += dot_nn(turned_low[...], grad_inner)
        work[...] += dot_nt(grad_inner, w_inner[:, part(c)])

        @pl.when(step == steps - 1)
        def _():
            theirs = pl.multiple_of(c * CHUNK + (1 - core_here) * half, 128)
            send_inner[c] = a_inner[:, pl.ds(theirs, half)].astype(jnp.bfloat16)
            send_outer[c] = a_outer[part(c), pl.ds(pl.multiple_of((1 - core_here) * half, 128), half)].astype(jnp.bfloat16)
            for move in exchange(c):
                move.start()

        return 0

    lax.fori_loop(0, chunks, backward, 0)
    grad_first = work[...]
    add_sum(3, grad_first * normed[...])
    add_sum(4, grad_first)
    scaled = grad_first * vector(1)
    pre_first = first_recip * (scaled - row_mean(scaled) - normed[...] * row_mean(scaled * normed[...]))
    pre_first_ref[...] = pre_first
    grad_attended = pre_first.astype(jnp.bfloat16)
    add_sum(5, grad_attended.astype(jnp.float32))
    a_output[...] += dot_nn(context[...].T, grad_attended)
    context[...] = dot_nt(grad_attended, w_output[...]).astype(jnp.bfloat16)
    grad_mine_ref[...] = context[:, pl.ds(pl.multiple_of(core_here * half, 128), half)]
    grad_other_ref[...] = context[:, pl.ds(pl.multiple_of((1 - core_here) * half, 128), half)]

    @pl.when(step == steps - 1)
    def _():
        grad_output_ref[...] = a_output[...].astype(jnp.bfloat16)

        shard = width // shards
        long = hidden // shards

        def inner_out(c):
            copies = []
            for k in range(size_z):
                for column in range(size_x):
                    slot = lax.rem(z + k, size_z) * size_x + column
                    src = send_inner.at[c, pl.ds(pl.multiple_of(slot * shard, shard), shard), :]
                    copies.append(
                        pltpu.make_async_copy(src, inner_terms[k].at[column, :, pl.ds(c * half, half)], store_sem.at[0, c])
                    )
            return copies

        def outer_out(c):
            copies = []
            group = CHUNK // long // size_x
            for i in range(group):
                for j in range(size_x):
                    src = send_outer.at[c, pl.ds(pl.multiple_of((i * size_x + lax.rem(x + j, size_x)) * long, long), long), :]
                    copies.append(pltpu.make_async_copy(src, outer_terms[j].at[c * group + i], store_sem.at[1, c]))
            return copies

        for c in range(chunks):
            ours = pl.multiple_of(c * CHUNK + core_here * half, 128)
            first_move, second_move = exchange(c)
            first_move.wait()
            send_inner[c] = (a_inner[:, pl.ds(ours, half)] + recv_inner[c].astype(jnp.float32)).astype(jnp.bfloat16)
            for copy in inner_out(c):
                copy.start()
            second_move.wait()
            columns = pl.ds(pl.multiple_of(core_here * half, 128), half)
            send_outer[c] = (a_outer[part(c), columns] + recv_outer[c].astype(jnp.float32)).astype(jnp.bfloat16)
            for copy in outer_out(c):
                copy.start()
        for c in range(chunks):
            pltpu.make_async_copy(send_inner.at[c], send_inner.at[c], store_sem.at[0, c]).wait()
            pltpu.make_async_copy(send_outer.at[c], send_outer.at[c], store_sem.at[1, c]).wait()


def dense_layer(size_z, size_x, tokens, mine, other, cotangent, vectors, bias_inner, weights):
    local, half = mine.shape
    width = 2 * half
    hidden = bias_inner.shape[1]
    steps = local // TILE
    shards = size_z * size_x
    chunks = hidden // CHUNK
    low, high = jnp.bfloat16, jnp.float32
    tile = pl.BlockSpec((TILE, width), lambda t, *_: (t, 0))
    half_tile = pl.BlockSpec((TILE, half), lambda t, *_: (t, 0))
    anywhere = pl.BlockSpec(memory_space=pl.ANY)

    def whole(shape):
        return pl.BlockSpec(shape, lambda t, *_: (0, 0))

    inner_shape = jax.ShapeDtypeStruct((size_x, width // shards, hidden // 2), low)
    outer_shape = jax.ShapeDtypeStruct((size_z, hidden // shards, half), low)
    halves = pltpu.VMEM((chunks, width, half), low)
    dma = pltpu.SemaphoreType.DMA
    return pl.pallas_call(
        lambda *refs: dense_kernel(size_z, size_x, *refs),
        out_shape=(
            jax.ShapeDtypeStruct((local, width), low),
            jax.ShapeDtypeStruct((local, width), high),
            jax.ShapeDtypeStruct((local, half), low),
            jax.ShapeDtypeStruct((local, half), low),
            jax.ShapeDtypeStruct((48, width), high),
            jax.ShapeDtypeStruct((8, hidden), high),
            jax.ShapeDtypeStruct((width, width), low),
        )
        + (inner_shape,) * size_z
        + (outer_shape,) * size_x,
        grid_spec=pltpu.PrefetchScalarGridSpec(
            num_scalar_prefetch=0,
            grid=(steps,),
            in_specs=[
                tile,
                half_tile,
                half_tile,
                tile,
                whole((16, width)),
                whole((1, hidden)),
                anywhere,
            ],
            out_specs=[
                tile,
                tile,
                half_tile,
                half_tile,
                whole((48, width)),
                whole((8, hidden)),
                whole((width, width)),
            ]
            + [anywhere] * (size_z + size_x),
            scratch_shapes=[
                pltpu.VMEM((width, width), low),
                pltpu.VMEM((width, hidden), low),
                pltpu.VMEM((hidden, width), low),
                pltpu.VMEM((width, width), high),
                pltpu.VMEM((width, hidden), high),
                pltpu.VMEM((hidden, width), high),
                pltpu.VMEM((TILE, width), low),
                pltpu.VMEM((TILE, width), low),
                pltpu.VMEM((TILE, width), low),
                pltpu.VMEM((width, TILE), low),
                pltpu.VMEM((TILE, width), high),
                pltpu.VMEM((TILE, width), high),
                pltpu.VMEM((TILE, hidden), high),
                pltpu.VMEM((TILE, hidden), low),
                pltpu.VMEM((TILE, width), high),
                halves,
                halves,
                halves,
                halves,
                dma((2,)),
                dma,
                dma((2, chunks)),
                dma((2, chunks)),
                dma((2, chunks)),
            ],
        ),
        compiler_params=pltpu.CompilerParams(
            dimension_semantics=("arbitrary",), vmem_limit_bytes=67_000_000, collective_id=3, has_side_effects=True
        ),
        cost_estimate=pl.CostEstimate(flops=32_000_000_000, bytes_accessed=40_000_000, transcendentals=6_000_000),
        name="dense_layer",
    )(tokens, mine, other, cotangent, vectors, bias_inner, weights)


def lowered(piece):
    return piece.astype(jnp.bfloat16)


def widen(piece):
    return piece.astype(jnp.float32)


def matmul(left, right):
    return jnp.dot(left, right, preferred_element_type=jnp.float32)


def matmul_tn(left, right):
    return lax.dot_general(
        left, right, (((0,), (0,)), ((), ())), preferred_element_type=jnp.float32
    )


def matmul_nt(left, right):
    return lax.dot_general(
        left, right, (((1,), (1,)), ((), ())), preferred_element_type=jnp.float32
    )


def normalize(hidden, norm_gain, norm_shift):
    centred = hidden - jnp.mean(hidden, axis=-1, keepdims=True)
    reciprocal = lax.rsqrt(jnp.mean(centred * centred, axis=-1, keepdims=True) + EPS)
    normed = centred * reciprocal
    return (normed * norm_gain + norm_shift, normed, reciprocal)


def normalize_back(upstream, normed, reciprocal, norm_gain):
    scaled = upstream * norm_gain
    result = reciprocal * (
        scaled
        - jnp.mean(scaled, axis=-1, keepdims=True)
        - normed * jnp.mean(scaled * normed, axis=-1, keepdims=True)
    )
    return (result, jnp.sum(upstream * normed, axis=0), jnp.sum(upstream, axis=0))


def gelu_value(values_in):
    return 0.5 * values_in * (1.0 + lax.erf(values_in * ROOT_HALF))


def gelu_slope(values_in):
    return (
        0.5 * (1.0 + lax.erf(values_in * ROOT_HALF))
        + values_in * jnp.exp(-0.5 * values_in * values_in) * INV_ROOT_TAU
    )


def shift(piece, axis, step):
    size = lax.axis_size(axis)
    return lax.ppermute(piece, axis, [(i, (i + step) % size) for i in range(size)])


def swap(piece, axis):
    return lax.ppermute(piece, axis, [(0, 1), (1, 0)])


def pick(piece, index, axis=0):
    return lax.dynamic_index_in_dim(piece, index, axis, keepdims=False)


def in_order(first_is_zero, own, other, axis):
    return jnp.where(
        first_is_zero,
        jnp.concatenate([own, other], axis),
        jnp.concatenate([other, own], axis),
    )


def collect(piece):
    size_z, size_x = lax.axis_size("z"), lax.axis_size("x")
    z, x = lax.axis_index("z"), lax.axis_index("x")
    along_z = [piece] + [shift(piece, "z", k) for k in range(1, size_z)]
    whole = jnp.zeros((size_z, size_x) + piece.shape, piece.dtype)
    zeros = (0,) * piece.ndim
    for j in range(size_x):
        for k in range(size_z):
            arrived = along_z[k] if j == 0 else shift(along_z[k], "x", j)
            place = ((z - k) % size_z, (x - j) % size_x) + zeros
            whole = lax.dynamic_update_slice(whole, arrived[None, None], place)
    return whole.reshape((size_z * size_x,) + piece.shape)


def reduce_owned(terms):
    size_z, size_x = lax.axis_size("z"), lax.axis_size("x")
    z, x = lax.axis_index("z"), lax.axis_index("x")
    terms = terms.reshape((size_z, size_x) + terms.shape[1:])
    total = widen(pick(terms, x, 1))
    for j in range(1, size_x):
        total = total + widen(shift(pick(terms, (x + j) % size_x, 1), "x", j))
    terms = lowered(total)
    total = widen(pick(terms, z))
    for k in range(1, size_z):
        total = total + widen(shift(pick(terms, (z + k) % size_z), "z", k))
    terms = lowered(total)
    return widen(terms) + widen(swap(terms, "y"))


def plain_body(
    tokens,
    segment_ids,
    w_query,
    w_key,
    w_value,
    w_output,
    b_query,
    b_value,
    b_output,
    first_gain,
    first_shift,
    w_inner,
    b_inner,
    w_outer,
    b_outer,
    second_gain,
    second_shift,
    cotangent,
):
    core, y = lax.axis_index("core"), lax.axis_index("y")
    shards = lax.axis_size("z") * lax.axis_size("x")
    sequences, part, width = tokens.shape
    half = width // 2
    pairs = half // 128
    hidden = w_inner.shape[1]
    local = 2 * part
    own_rows = w_query.shape[0]
    unit_half = hidden // shards // 2

    def columns(matrix):
        return lowered(lax.dynamic_slice_in_dim(matrix, core * half, half, 1))

    vectors = (b_query, b_value, b_output, first_gain, first_shift, b_inner, b_outer, second_gain, second_shift)
    flat = jnp.concatenate([lowered(v) for v in vectors])
    lanes = 3 * half
    extra = -(-flat.shape[0] // lanes)
    flat = jnp.pad(flat, (0, extra * lanes - flat.shape[0])).reshape(extra, lanes)
    weights = jnp.stack([columns(w).reshape(own_rows, pairs, 128) for w in (w_query, w_key, w_value)], axis=2)
    early = collect(jnp.concatenate([weights.reshape(own_rows, lanes), flat], axis=0))

    mine = pick(tokens, y)
    arrived = swap(pick(tokens, 1 - y), "y")
    mine_other, arrived_other = swap(mine, "core"), swap(arrived, "core")
    inputs_all = jnp.concatenate([mine, arrived, mine_other, arrived_other], axis=0)
    inputs = jnp.concatenate([mine, arrived], axis=0)

    inner_piece = lowered(pick(w_inner.reshape(own_rows, shards, 2, unit_half), core, 2)).reshape(own_rows, hidden // 2)
    late = collect(jnp.concatenate([columns(w_output), inner_piece], axis=1)).reshape(width, half + hidden // 2)
    outer_own = collect(lowered(lax.dynamic_slice_in_dim(w_outer, core * unit_half, unit_half, 0))).reshape(hidden // 2, width)
    output_own, inner_own = late[:, :half], late[:, half:]
    output_other, inner_other, outer_other = swap(output_own, "core"), swap(inner_own, "core"), swap(outer_own, "core")
    full_output = in_order(core == 0, output_own, output_other, 1)
    cotangent_mine = pick(cotangent, y)
    cotangent_arrived = swap(pick(cotangent, 1 - y), "y")

    full_early = early[:, :own_rows].reshape(width, lanes)
    flat_all = early[:, own_rows:].reshape(shards, extra * lanes)
    sizes = [v.shape[0] for v in vectors]
    gathered, at = [], 0
    for size in sizes:
        gathered.append(flat_all[:, at : at + size].reshape(shards * size))
        at += size
    bias_query, bias_value, bias_output, gain_first, shift_first, bias_inner, bias_outer, gain_second, shift_second = [
        widen(v) for v in gathered
    ]
    spot = jnp.arange(5, dtype=jnp.int32)
    place = jnp.where(spot < 4, ((spot % 2 != core) * 2 + (spot // 2 != y) * 1) * part, core)
    segments = pick(segment_ids, y)
    biases = jnp.concatenate([bias_query[None], bias_value[None], jnp.zeros((14, width), jnp.float32)], axis=0)
    heads_mine, heads_other, logsum, projected = attention(place, segments, inputs_all, full_early, biases)
    context = in_order(core == 0, heads_mine, swap(heads_other, "core"), 1)

    attended = matmul(context, full_output) + bias_output
    first, first_normed, first_recip = normalize(widen(inputs) + attended, gain_first, shift_first)
    first_low = lowered(first)
    biases = bias_inner.reshape(shards, 2, unit_half)
    halves = ((inner_own, outer_own, pick(biases, core, 1)), (inner_other, outer_other, pick(biases, 1 - core, 1)))
    outer, kept = bias_outer, []
    for inner_weight, outer_weight, bias in halves:
        inner = matmul(first_low, inner_weight) + bias.reshape(hidden // 2)
        active = lowered(gelu_value(inner))
        outer = outer + matmul(active, outer_weight)
        kept.append((inner, active))
    mixed, second_normed, second_recip = normalize(first + outer, gain_second, shift_second)
    mixed = lowered(mixed)

    upstream = widen(jnp.concatenate([cotangent_mine, cotangent_arrived], axis=0))
    pre_second, grad_second_gain, grad_second_shift = normalize_back(upstream, second_normed, second_recip, gain_second)
    grad_outer = lowered(pre_second)
    grad_b_outer = jnp.sum(widen(grad_outer), axis=0)
    grad_first, inner_grads, outer_grads, bias_grads = pre_second, [], [], []
    for (inner, active), (inner_weight, outer_weight, _) in zip(kept, halves):
        grad_inner = lowered(matmul_nt(grad_outer, outer_weight) * gelu_slope(inner))
        outer_grads.append(lowered(matmul_tn(active, grad_outer)))
        inner_grads.append(lowered(matmul_tn(first_low, grad_inner)))
        bias_grads.append(jnp.sum(widen(grad_inner), axis=0).reshape(shards, 1, unit_half))
        grad_first = grad_first + matmul_nt(grad_inner, inner_weight)
    grad_b_inner = in_order(core == 0, bias_grads[0], bias_grads[1], 1).reshape(hidden)
    pre_first, grad_first_gain, grad_first_shift = normalize_back(grad_first, first_normed, first_recip, gain_first)
    grad_attended = lowered(pre_first)
    grad_b_output = jnp.sum(widen(grad_attended), axis=0)
    grad_w_output = lowered(matmul_tn(context, grad_attended))
    grad_context = lowered(matmul_nt(grad_attended, full_output))
    context_mine = lax.dynamic_slice_in_dim(grad_context, core * half, half, 1)
    context_other = lax.dynamic_slice_in_dim(grad_context, (1 - core) * half, half, 1)
    upstream_other = swap(context_other, "core")

    def core_sum(own, other):
        return lowered(widen(own) + widen(swap(other, "core")))

    outer_term = core_sum(*outer_grads)
    inner_term = core_sum(*inner_grads)
    output_term = core_sum(
        lax.dynamic_slice_in_dim(grad_w_output, core * half, half, 1),
        lax.dynamic_slice_in_dim(grad_w_output, (1 - core) * half, half, 1),
    )
    outer_done = reduce_owned(outer_term.reshape(shards, unit_half, width))
    late_done = reduce_owned(jnp.concatenate([output_term, inner_term], axis=1).reshape(shards, own_rows, half + hidden // 2))

    grads, sums = attention_back(place, segments, projected, heads_mine, heads_other, context_mine, upstream_other, logsum)
    grad_early = lowered(matmul_tn(inputs_all, grads))
    partial = matmul_nt(grads, full_early)
    sums = sums.reshape(pairs, 8, 3, 128)[:, 0]
    blank = jnp.zeros((width,), jnp.float32)
    grad_b_query = lax.dynamic_update_slice(blank, sums[:, 0].reshape(half), (core * half,))
    grad_b_value = lax.dynamic_update_slice(blank, sums[:, 2].reshape(half), (core * half,))
    vector_grads = (
        grad_b_query,
        grad_b_value,
        grad_b_output,
        grad_first_gain,
        grad_first_shift,
        grad_b_inner,
        grad_b_outer,
        grad_second_gain,
        grad_second_shift,
    )
    flat_grads = jnp.concatenate([v.reshape(shards, -1) for v in vector_grads], axis=1)
    flat_grads = jnp.pad(flat_grads, ((0, 0), (0, extra * lanes - flat_grads.shape[1])))
    early_term = jnp.concatenate(
        [grad_early.reshape(shards, own_rows, lanes), lowered(flat_grads).reshape(shards, extra, lanes)], axis=1
    )
    early_done = reduce_owned(early_term)

    grad_inputs = pre_first + partial[:local] + widen(swap(lowered(partial[local:]), "core"))
    returned = widen(swap(lowered(grad_inputs[part:]), "y"))
    grad_tokens = in_order(y == 0, grad_inputs[None, :part], returned[None], 0)
    mixed_out = in_order(y == 0, mixed[None, :part], swap(mixed[part:], "y")[None], 0)

    def both(piece):
        return widen(swap(lowered(piece), "core"))

    early_matrix = early_done[:own_rows]
    early_full = in_order(
        core == 0, early_matrix.reshape(own_rows, pairs, 3, 128)[None], both(early_matrix).reshape(own_rows, pairs, 3, 128)[None], 0
    )
    early_full = early_full.transpose(3, 1, 0, 2, 4).reshape(3, own_rows, width)
    late_other = both(late_done)
    output_full = in_order(core == 0, late_done[:, :half], late_other[:, :half], 1)
    inner_full = in_order(
        core == 0,
        late_done[:, half:].reshape(own_rows, shards, 1, unit_half),
        late_other[:, half:].reshape(own_rows, shards, 1, unit_half),
        2,
    ).reshape(own_rows, hidden)
    outer_full = in_order(core == 0, outer_done, both(outer_done), 0)
    vector_part = early_done[own_rows:]
    vector_sums = (vector_part + swap(vector_part, "core")).reshape(extra * lanes)
    out_vectors, at = [], 0
    for size in sizes:
        out_vectors.append(vector_sums[at : at + size])
        at += size
    (
        done_b_query,
        done_b_value,
        done_b_output,
        done_first_gain,
        done_first_shift,
        done_b_inner,
        done_b_outer,
        done_second_gain,
        done_second_shift,
    ) = out_vectors
    return (
        mixed_out,
        grad_tokens,
        early_full[0],
        early_full[1],
        early_full[2],
        output_full,
        done_b_query,
        done_b_value,
        done_b_output,
        done_first_gain,
        done_first_shift,
        inner_full,
        done_b_inner,
        outer_full,
        done_b_outer,
        done_second_gain,
        done_second_shift,
    )


def body(
    tokens,
    segment_ids,
    w_query,
    w_key,
    w_value,
    w_output,
    b_query,
    b_value,
    b_output,
    first_gain,
    first_shift,
    w_inner,
    b_inner,
    w_outer,
    b_outer,
    second_gain,
    second_shift,
    cotangent,
):
    core, y = lax.axis_index("core"), lax.axis_index("y")
    size_z, size_x = lax.axis_size("z"), lax.axis_size("x")
    shards = size_z * size_x
    everyone = ("z", "x", "core")
    sequences, part, width = tokens.shape
    half = width // 2
    pairs = half // 128
    hidden = w_inner.shape[1]
    local = 2 * part
    own_rows = w_query.shape[0]
    lanes = 3 * half

    stack = hidden // width

    def core_rows(matrix):
        rows = matrix.shape[0] // 2
        return lowered(lax.dynamic_slice_in_dim(matrix, core * rows, rows, 0))

    outer_rows = core_rows(w_outer)
    outer_rows = outer_rows.reshape(stack, own_rows // 2, width).transpose(1, 0, 2).reshape(own_rows // 2, hidden)
    pieces = (core_rows(w_inner), core_rows(w_output), outer_rows)
    dense = lax.all_gather(jnp.concatenate(pieces, axis=1), everyone, axis=0, tiled=True)

    vectors = (b_query, b_value, b_output, first_gain, first_shift, b_inner, b_outer, second_gain, second_shift)
    sizes = [v.shape[0] for v in vectors]
    tokens_all, cotangent_all, early, rows, inner_row = entry(size_z, size_x, tokens, cotangent, w_query, w_key, w_value, vectors)
    inputs_all = tokens_all.reshape(4 * part, width)
    full_early = early.reshape(width, lanes)
    spot = jnp.arange(5, dtype=jnp.int32)
    place = jnp.where(spot < 4, ((spot % 2 != core) * 2 + (spot // 2 != y) * 1) * part, core)
    segments = pick(segment_ids, y)
    context_mine, context_other, logsum, projected = attention(place, segments, inputs_all, full_early, rows)
    made = dense_layer(
        size_z,
        size_x,
        inputs_all,
        context_mine,
        swap(context_other, "core"),
        cotangent_all.reshape(local, width),
        rows,
        inner_row,
        dense,
    )
    mixed, pre_first, upstream_mine, upstream_send, dense_sums, inner_sums, grad_w_output = made[:7]
    inner_terms = [made[7]] + [shift(made[7 + k], "z", k) for k in range(1, size_z)]
    outer_terms = [made[7 + size_z]] + [shift(made[7 + size_z + j], "x", j) for j in range(1, size_x)]
    upstream_other = swap(upstream_send, "core")
    mixed_out = in_order(y == 0, mixed[None, :part], swap(mixed[part:], "y")[None], 0)

    grads, sums = attention_back(place, segments, projected, context_mine, context_other, upstream_mine, upstream_other, logsum)
    made = exit_call(
        size_z,
        size_x,
        grads,
        inputs_all,
        full_early,
        pre_first,
        grad_w_output.reshape(shards, own_rows, width),
        dense_sums,
        inner_sums,
        sums,
        inner_terms,
        outer_terms,
    )
    grad_tokens, grad_query, grad_key, grad_value, grad_output, grad_inner_full, grad_outer_full, *done = deliver(
        made[:7], made[7], sizes
    )
    done = [v.reshape(size) for v, size in zip(done, sizes)]
    return (
        mixed_out,
        grad_tokens,
        grad_query,
        grad_key,
        grad_value,
        grad_output,
        *done[:5],
        grad_inner_full,
        done[5],
        grad_outer_full,
        *done[6:],
    )


def layer(*arrays):
    if arrays[2].shape[0] % 32 == 0 and lax.axis_size("x") > 1:
        return body(*arrays)
    return plain_body(*arrays)


def solution(mesh):
    outer, inner = mesh.devices.shape
    size_z = 1
    while size_z * size_z < outer:
        size_z *= 2
    split = Mesh(mesh.devices.reshape(size_z, outer // size_z, inner // 2, 2), ("z", "x", "y", "core"))
    dp, seq = ("z", "x"), ("y", "core")
    activation, matrix, vector = P(dp, seq, None), P(dp, None), P(dp)
    return jax.shard_map(
        layer,
        mesh=split,
        in_specs=(
            activation,
            matrix,
            matrix,
            matrix,
            matrix,
            matrix,
            vector,
            vector,
            vector,
            vector,
            vector,
            matrix,
            vector,
            matrix,
            vector,
            vector,
            vector,
            activation,
        ),
        out_specs=(
            activation,
            activation,
            matrix,
            matrix,
            matrix,
            matrix,
            vector,
            vector,
            vector,
            vector,
            vector,
            matrix,
            vector,
            matrix,
            vector,
            vector,
            vector,
        ),
        check_vma=False,
    )
```

```python
import jax
import jax.numpy as jnp
from jax import lax
from jax.experimental import pallas as pl
from jax.experimental.pallas import tpu as pltpu
from jax.sharding import Mesh
from jax.sharding import PartitionSpec as P


HD = 64
EPS = 1e-12
ROOT_HALF = 0.7071067811865476
INV_ROOT_TAU = 0.3989422804014327

BLK = 256
BIG = -1.0e9
DOCUMENTS = 4


def dot_nn(a, b):
    return jnp.dot(a, b, preferred_element_type=jnp.float32)


def part_rows(place_ref, part, rows):
    return pl.ds(pl.multiple_of(place_ref[part], 128), rows)


def find_bounds(segment_ref, bound_ref):
    length = segment_ref.shape[0]
    bound_ref[0] = 0
    bound_ref[DOCUMENTS] = length
    for d in range(1, DOCUMENTS):

        def halve(_, span):
            low, high = span
            middle = (low + high) // 2
            below = segment_ref[jnp.minimum(middle, length - 1)] < d
            inside = low < high
            return (
                jnp.where(jnp.logical_and(inside, below), middle + 1, low),
                jnp.where(jnp.logical_and(inside, jnp.logical_not(below)), middle, high),
            )

        low, _ = lax.fori_loop(0, length.bit_length(), halve, (0, length))
        bound_ref[d] = low


def find_window(segment_ref, bound_ref, qb):
    length = segment_ref.shape[0]
    first = segment_ref[qb * BLK]
    last = segment_ref[qb * BLK + BLK - 1]
    start = bound_ref[first] // 128 * 128
    count = (bound_ref[last + 1] - start + BLK - 1) // BLK
    return jnp.minimum(start, length - count * BLK), count


def each_tile(count, step):
    def two(i, _):
        step(i * (2 * BLK), 2 * BLK)
        return 0

    lax.fori_loop(0, count // 2, two, 0)

    @pl.when(count % 2 == 1)
    def _():
        step((count - 1) * BLK, BLK)


def make_marks(row_ref, mark_query, mark_key):
    length = mark_key.shape[0]
    step = 512
    for b in range(length // step):
        rows = slice(b * step, (b + 1) * step)
        column = jnp.broadcast_to(row_ref[0:1, rows], (128, step)).T
        lane = lax.broadcasted_iota(jnp.int32, (step, 128), 1) % 64
        same = lane == column
        line = lax.broadcasted_iota(jnp.int32, (128, step), 0) % 64
        mark_query[:, rows] = jnp.where(line == row_ref[0:1, rows], 1.0, 0.0).astype(jnp.bfloat16)
        apart = jnp.logical_and(lane < DOCUMENTS, jnp.logical_not(same))
        mark_key[rows, :] = jnp.where(apart, BIG, 0.0).astype(jnp.bfloat16)


def forward_kernel(place_ref, segment_ref, row_ref, tokens_ref, weights_ref, bias_ref, *refs):
    mine_ref, other_ref, lse_ref, qkv_ref, q2, k2, vt, acc, top, tot, keep, mark_query, mark_key, bound_ref = refs
    length = qkv_ref.shape[0]
    blocks = length // BLK
    part = length // 4

    @pl.when(pl.program_id(0) == 0)
    def _():
        find_bounds(segment_ref, bound_ref)
        make_marks(row_ref, mark_query, mark_key)

    low = lax.broadcasted_iota(jnp.int32, (part, 128), 1) < 64
    for b in range(4):
        src = part_rows(place_ref, b, part)
        dst = slice(b * part, (b + 1) * part)
        made = dot_nn(tokens_ref[src, :], weights_ref[...])
        lanes = pl.ds(pl.multiple_of(place_ref[4] * (128 * pl.num_programs(0)) + pl.program_id(0) * 128, 128), 128)
        q = ((made[:, 0:128] + bias_ref[0:1, lanes]) * 0.125).astype(jnp.bfloat16)
        k = made[:, 128:256].astype(jnp.bfloat16)
        v = (made[:, 256:384] + bias_ref[1:2, lanes]).astype(jnp.bfloat16)
        qkv_ref[src, 0:128] = q
        qkv_ref[src, 128:256] = k
        qkv_ref[src, 256:384] = v
        nohk = mark_key[dst, :]
        turned = q.T
        q2[0, 0:64, dst] = turned[0:64]
        q2[0, 64:128, dst] = mark_query[64:128, dst]
        q2[1, 0:64, dst] = mark_query[0:64, dst]
        q2[1, 64:128, dst] = turned[64:128]
        k2[0, dst, :] = jnp.where(low, k, nohk)
        k2[1, dst, :] = jnp.where(low, nohk, k)
        vt[:, dst] = v.T
    lse_ref[...] = jnp.zeros_like(lse_ref)

    def row(qb, _):
        qs = pl.ds(pl.multiple_of(qb * BLK, BLK), BLK)
        start, count = find_window(segment_ref, bound_ref, qb)
        top[...] = jnp.full_like(top, -1.0e30)

        def fold(tile, function):
            return function(tile.reshape(tile.shape[0] // 8, 8, BLK), axis=0)

        def highest(first, size):
            keys = pl.ds(pl.multiple_of(start + first, 128), size)
            for h in range(2):
                st = dot_nn(k2[h, keys, :], q2[h, :, qs])
                keep[h, pl.ds(pl.multiple_of(first, BLK), size), :] = st
                top[h] = jnp.maximum(top[h], fold(st, jnp.max))

        def weigh(first, size, largest):
            keys = pl.ds(pl.multiple_of(start + first, 128), size)
            for h in range(2):
                rows = slice(64 * h, 64 * h + 64)
                st = keep[h, pl.ds(pl.multiple_of(first, BLK), size), :]
                p = jnp.exp(st - largest[h])
                tot[h] = tot[h] + fold(p, jnp.sum)
                acc[rows, :] = acc[rows, :] + dot_nn(vt[rows, keys], p.astype(jnp.bfloat16))

        def paired(step):
            each_tile(count, step)

        paired(highest)
        largest = [jnp.max(top[h], axis=0, keepdims=True) for h in range(2)]
        acc[...] = jnp.zeros_like(acc)
        tot[...] = jnp.zeros_like(tot)
        paired(lambda first, size: weigh(first, size, largest))
        for h in range(2):
            rows = slice(64 * h, 64 * h + 64)
            total = jnp.sum(tot[h], axis=0, keepdims=True)
            acc[rows, :] = acc[rows, :] / total
            lse_ref[h : h + 1, qs] = largest[h] + jnp.log(total)
        where = place_ref[qb * BLK // part] + qb * BLK % part
        result = acc[...].T.astype(jnp.bfloat16)

        @pl.when(where < 2 * part)
        def _():
            mine_ref[pl.ds(pl.multiple_of(where, BLK), BLK), :] = result

        @pl.when(where >= 2 * part)
        def _():
            other_ref[pl.ds(pl.multiple_of(where - 2 * part, BLK), BLK), :] = result

        return 0

    lax.fori_loop(0, blocks, row, 0)


def attention(place, segments, tokens, weights, biases):
    length, depth = tokens.shape
    width = weights.shape[1]
    pairs = width // 384
    rows = length // 2
    return pl.pallas_call(
        forward_kernel,
        out_shape=(
            jax.ShapeDtypeStruct((rows, pairs * 128), jnp.bfloat16),
            jax.ShapeDtypeStruct((rows, pairs * 128), jnp.bfloat16),
            jax.ShapeDtypeStruct((pairs * 8, length), jnp.float32),
            jax.ShapeDtypeStruct((length, width), jnp.bfloat16),
        ),
        grid_spec=pltpu.PrefetchScalarGridSpec(
            num_scalar_prefetch=2,
            grid=(pairs,),
            in_specs=[
                pl.BlockSpec((1, length), lambda p, *_: (0, 0)),
                pl.BlockSpec((length, depth), lambda p, *_: (0, 0)),
                pl.BlockSpec((depth, 384), lambda p, *_: (0, p)),
                pl.BlockSpec(biases.shape, lambda p, *_: (0, 0)),
            ],
            out_specs=[
                pl.BlockSpec((rows, 128), lambda p, *_: (0, p)),
                pl.BlockSpec((rows, 128), lambda p, *_: (0, p)),
                pl.BlockSpec((8, length), lambda p, *_: (p, 0)),
                pl.BlockSpec((length, 384), lambda p, *_: (0, p)),
            ],
            scratch_shapes=[
                pltpu.VMEM((2, 128, length), jnp.bfloat16),
                pltpu.VMEM((2, length, 128), jnp.bfloat16),
                pltpu.VMEM((128, length), jnp.bfloat16),
                pltpu.VMEM((128, BLK), jnp.float32),
                pltpu.VMEM((2, 8, BLK), jnp.float32),
                pltpu.VMEM((2, 8, BLK), jnp.float32),
                pltpu.VMEM((2, length, BLK), jnp.float32),
                pltpu.VMEM((128, length), jnp.bfloat16),
                pltpu.VMEM((length, 128), jnp.bfloat16),
                pltpu.SMEM((DOCUMENTS + 1,), jnp.int32),
            ],
        ),
        compiler_params=pltpu.CompilerParams(dimension_semantics=("arbitrary",), vmem_limit_bytes=60 << 20),
        cost_estimate=pl.CostEstimate(flops=pairs * 8_000_000_000, bytes_accessed=pairs * 3_000_000, transcendentals=pairs * 4_000_000),
        name="attention_forward",
    )(place, segments, segments.reshape(1, length), tokens, weights, biases)


def backward_kernel(
    place_ref,
    segment_ref,
    qkv_ref,
    ctx_mine_ref,
    ctx_other_ref,
    do_mine_ref,
    do_other_ref,
    lse_ref,
    row_ref,
    out_ref,
    sum_ref,
    q2,
    k2,
    q0,
    d0,
    dt,
    v0,
    kt,
    dk,
    dv,
    dqt,
    delta,
    mark_query,
    mark_key,
    bound_ref,
):
    length = qkv_ref.shape[0]
    blocks = length // BLK
    part = length // 4

    @pl.when(pl.program_id(0) == 0)
    def _():
        find_bounds(segment_ref, bound_ref)
        make_marks(row_ref, mark_query, mark_key)

    low = lax.broadcasted_iota(jnp.int32, (part, 128), 1) < 64

    def prepare(b, do, ctx):
        src = part_rows(place_ref, b, part)
        dst = slice(b * part, (b + 1) * part)
        q, k = qkv_ref[src, 0:128], qkv_ref[src, 128:256]
        zero = jnp.zeros_like(q)
        nohk = mark_key[dst, :]
        turned = q.T
        q2[0, 0:64, dst] = turned[0:64]
        q2[0, 64:128, dst] = mark_query[64:128, dst]
        q2[1, 0:64, dst] = mark_query[0:64, dst]
        q2[1, 64:128, dst] = turned[64:128]
        k2[0, dst, :] = jnp.where(low, k, nohk)
        k2[1, dst, :] = jnp.where(low, nohk, k)
        q0[0, dst, :] = jnp.where(low, q, zero)
        q0[1, dst, :] = jnp.where(low, zero, q)
        d0[0, dst, :] = jnp.where(low, do, zero)
        d0[1, dst, :] = jnp.where(low, zero, do)
        turned = do.T
        blank = jnp.zeros((64, part), jnp.bfloat16)
        dt[0, 0:64, dst] = turned[0:64]
        dt[0, 64:128, dst] = blank
        dt[1, 0:64, dst] = blank
        dt[1, 64:128, dst] = turned[64:128]
        v0[dst, :] = qkv_ref[src, 256:384]
        kt[:, dst] = k.T
        prod = turned.astype(jnp.float32) * ctx.T.astype(jnp.float32)
        delta[0:1, dst] = jnp.sum(prod[0:64], axis=0, keepdims=True)
        delta[1:2, dst] = jnp.sum(prod[64:128], axis=0, keepdims=True)

    for b in range(4):

        @pl.when(place_ref[b] < 2 * part)
        def _():
            rows = part_rows(place_ref, b, part)
            prepare(b, do_mine_ref[rows, :], ctx_mine_ref[rows, :])

        @pl.when(place_ref[b] >= 2 * part)
        def _():
            rows = pl.ds(pl.multiple_of(place_ref[b] - 2 * part, 128), part)
            prepare(b, do_other_ref[rows, :], ctx_other_ref[rows, :])

    dk[...] = jnp.zeros_like(dk)
    dv[...] = jnp.zeros_like(dv)
    dqt[...] = jnp.zeros_like(dqt)

    def row(qb, _):
        qs = pl.ds(pl.multiple_of(qb * BLK, BLK), BLK)
        start, count = find_window(segment_ref, bound_ref, qb)

        def tile(first, size):
            ks = pl.ds(pl.multiple_of(start + first, 128), size)
            weights, grads = [], []
            for h in range(2):
                st = dot_nn(k2[h, ks, :], q2[h, :, qs])
                w = jnp.exp(st - lse_ref[h : h + 1, qs])
                gw = dot_nn(v0[ks, :], dt[h, :, qs])
                weights.append(w.astype(jnp.bfloat16))
                grads.append((w * (gw - delta[h : h + 1, qs])).astype(jnp.bfloat16))
            dv[ks, :] += dot_nn(jnp.concatenate(weights, axis=1), jnp.concatenate([d0[0, qs, :], d0[1, qs, :]], axis=0))
            dk[ks, :] += dot_nn(jnp.concatenate(grads, axis=1), jnp.concatenate([q0[0, qs, :], q0[1, qs, :]], axis=0))
            for h in range(2):
                rows = slice(64 * h, 64 * h + 64)
                dqt[rows, qs] += dot_nn(kt[rows, ks], grads[h])

        each_tile(count, tile)
        return 0

    lax.fori_loop(0, blocks, row, 0)
    sums = [jnp.zeros((1, 128), jnp.float32) for _ in range(3)]
    for b in range(4):
        dst = part_rows(place_ref, b, part)
        src = slice(b * part, (b + 1) * part)
        pieces = ((dqt[:, src].T * 0.125).astype(jnp.bfloat16), dk[src, :].astype(jnp.bfloat16), dv[src, :].astype(jnp.bfloat16))
        for i, piece in enumerate(pieces):
            out_ref[dst, 128 * i : 128 * i + 128] = piece
            sums[i] = sums[i] + jnp.sum(piece.astype(jnp.float32), axis=0, keepdims=True)
    sum_ref[...] = jnp.zeros_like(sum_ref)
    for i in range(3):
        sum_ref[0:1, 128 * i : 128 * i + 128] = sums[i]


def attention_back(place, segments, qkv, ctx_mine, ctx_other, do_mine, do_other, lse):
    length, width = qkv.shape
    pairs = width // 384
    rows = length // 2
    half = lambda: pltpu.VMEM((2, length, 128), jnp.bfloat16)
    turned = lambda: pltpu.VMEM((2, 128, length), jnp.bfloat16)
    column = pl.BlockSpec((rows, 128), lambda p, *_: (0, p))
    return pl.pallas_call(
        backward_kernel,
        out_shape=(
            jax.ShapeDtypeStruct((length, width), jnp.bfloat16),
            jax.ShapeDtypeStruct((pairs * 8, 384), jnp.float32),
        ),
        grid_spec=pltpu.PrefetchScalarGridSpec(
            num_scalar_prefetch=2,
            grid=(pairs,),
            in_specs=[
                pl.BlockSpec((length, 384), lambda p, *_: (0, p)),
                column,
                column,
                column,
                column,
                pl.BlockSpec((8, length), lambda p, *_: (p, 0)),
                pl.BlockSpec((1, length), lambda p, *_: (0, 0)),
            ],
            out_specs=[
                pl.BlockSpec((length, 384), lambda p, *_: (0, p)),
                pl.BlockSpec((8, 384), lambda p, *_: (p, 0)),
            ],
            scratch_shapes=[
                turned(),
                half(),
                half(),
                half(),
                turned(),
                pltpu.VMEM((length, 128), jnp.bfloat16),
                pltpu.VMEM((128, length), jnp.bfloat16),
                pltpu.VMEM((length, 128), jnp.float32),
                pltpu.VMEM((length, 128), jnp.float32),
                pltpu.VMEM((128, length), jnp.float32),
                pltpu.VMEM((8, length), jnp.float32),
                pltpu.VMEM((128, length), jnp.bfloat16),
                pltpu.VMEM((length, 128), jnp.bfloat16),
                pltpu.SMEM((DOCUMENTS + 1,), jnp.int32),
            ],
        ),
        compiler_params=pltpu.CompilerParams(dimension_semantics=("arbitrary",), vmem_limit_bytes=60 << 20),
        cost_estimate=pl.CostEstimate(flops=pairs * 20_000_000_000, bytes_accessed=pairs * 5_000_000, transcendentals=pairs * 4_000_000),
        name="attention_backward",
    )(place, segments, qkv, ctx_mine, ctx_other, do_mine, do_other, lse, segments.reshape(1, length))


MESH_ID = pl.DeviceIdType.MESH
WIDE = 5


def place_of():
    return tuple(lax.axis_index(name) for name in ("z", "x", "y", "core"))


def sizes_of():
    return lax.axis_size("z"), lax.axis_size("x")


def partner(**moved):
    z, x, y, core = place_of()
    return (moved.get("z", z), moved.get("x", x), moved.get("y", y), moved.get("core", core))


def greet(with_grid):
    z, x, y, core = place_of()
    size_z, size_x = sizes_of()
    peers = [partner(y=1 - y), partner(core=1 - core)]
    if with_grid:
        peers += [partner(z=lax.rem(z + k, size_z)) for k in range(1, size_z)]
        peers += [partner(x=lax.rem(x + j, size_x)) for j in range(1, size_x)]
    barrier = pltpu.get_barrier_semaphore()
    for peer in peers:
        pl.semaphore_signal(barrier, inc=1, device_id=peer, device_id_type=MESH_ID)
    pl.semaphore_wait(barrier, len(peers))


def remote(src, dst, send, recv, peer):
    return pltpu.make_async_remote_copy(
        src_ref=src, dst_ref=dst, send_sem=send, recv_sem=recv, device_id=peer, device_id_type=MESH_ID
    )


def entry_kernel(size_z, size_x, count, *refs):
    tokens, cotangent, wq, wk, wv, w_inner, w_output, w_outer = refs[:8]
    vectors = refs[8 : 8 + count]
    tokens_all, cotangent_all, weights_all, inner_all, outer_all, rows_out, inner_out = refs[8 + count : 15 + count]
    raw = refs[15 + count : 15 + 2 * count]
    stage, cot_stage, wbuf, ibuf, obuf, pack, ipack, opack, vpack, vectors_all = refs[15 + 2 * count : 25 + 2 * count]
    local_sem, load_sem, tsend, trecv, zsend, zrecv, xsend, xrecv, osend, orecv = refs[25 + 2 * count :]
    z, x, y, core = place_of()
    half = pack.shape[1] // 3
    pairs = half // 128
    chunks = w_inner.shape[1] // CHUNK
    me = z * size_x + x
    columns = [lax.rem(x + j, size_x) for j in range(size_x)]

    mine = pl.ds(pl.multiple_of(core * half, 128), half)
    loads = [pltpu.make_async_copy(w.at[:, mine], wbuf.at[i], load_sem.at[i]) for i, w in enumerate((wq, wk, wv))]
    loads += [pltpu.make_async_copy(v, r, load_sem.at[3 + i]) for i, (v, r) in enumerate(zip(vectors, raw))]
    late = [
        pltpu.make_async_copy(
            w_inner.at[:, pl.ds(pl.multiple_of(c * CHUNK + core * half, 128), half)],
            ibuf.at[:, pl.ds(c * half, half)],
            load_sem.at[3 + count + c],
        )
        for c in range(chunks)
    ]
    late.append(pltpu.make_async_copy(w_output.at[:, mine], ibuf.at[:, pl.ds(chunks * half, half)], load_sem.at[3 + count + chunks]))
    late.append(pltpu.make_async_copy(w_outer.at[:, mine], obuf, load_sem.at[4 + count + chunks]))
    load = pltpu.make_async_copy(tokens.at[y], stage, local_sem.at[0])
    cot_load = pltpu.make_async_copy(cotangent.at[y], cot_stage, local_sem.at[4])
    for copy in loads + late + [load, cot_load]:
        copy.start()
    vpack[...] = jnp.zeros_like(vpack)
    for copy in loads:
        copy.wait()
    for i, vector in enumerate(raw):
        vpack[i : i + 1, 0 : vector.shape[1]] = vector[...].astype(jnp.bfloat16).astype(jnp.float32)
    for i in range(3):
        for p in range(pairs):
            pack[:, (3 * p + i) * 128 : (3 * p + i + 1) * 128] = wbuf[i, :, p * 128 : (p + 1) * 128].astype(jnp.bfloat16)
    vectors_all[me] = vpack[...]
    greet(True)

    across = remote(tokens.at[1 - y], tokens_all.at[1], tsend.at[0], trecv.at[0], partner(y=1 - y))
    across.start()
    beside = remote(tokens.at[y], tokens_all.at[2], tsend.at[1], trecv.at[1], partner(core=1 - core))

    packs = (pack, vpack, ipack)

    def home(stream, origin):
        if stream == 2:
            return inner_all.at[origin]
        return (weights_all, vectors_all)[stream].at[origin * size_x + x]

    def z_move(stream, way, t):
        step = 1 - 2 * way
        origin = z - step * (t - 1)
        src = packs[stream] if t == 1 else home(stream, origin)
        peer = partner(z=lax.rem(z + step + size_z, size_z))
        return remote(src, home(stream, origin), zsend.at[stream, way, t - 1], zrecv.at[stream, way, t - 1], peer)

    def sends(way, t):
        step = 1 - 2 * way
        origin, target = z - step * (t - 1), z + step
        inside = lambda v: jnp.logical_and(v >= 0, v < size_z)
        return jnp.logical_and(inside(origin), inside(target))

    def receives(way, t):
        origin = z - (1 - 2 * way) * t
        return jnp.logical_and(origin >= 0, origin < size_z)

    def x_moves(index, origin, own):
        moves = []
        for j in range(1, size_x):
            for stream in range(2):
                src = packs[stream] if own else home(stream, origin)
                moves.append(
                    remote(
                        src,
                        home(stream, origin),
                        xsend.at[stream, index, j - 1],
                        xrecv.at[stream, index, j - 1],
                        partner(x=columns[j]),
                    )
                )
        return moves

    def start_z(streams, t):
        for way in range(2):

            @pl.when(sends(way, t))
            def _():
                for stream in streams:
                    z_move(stream, way, t).start()

    for move in x_moves(0, z, True):
        move.start()
    start_z((0, 1), 1)
    beside.start()
    for copy in late:
        copy.wait()
    ipack[...] = ibuf[...].astype(jnp.bfloat16)
    opack[...] = obuf[...].astype(jnp.bfloat16)
    start_z((2,), 1)
    outer_moves = [
        remote(opack, outer_all.at[x], osend.at[j - 1], orecv.at[j - 1], partner(x=columns[j])) for j in range(1, size_x)
    ]
    keeps = [
        pltpu.make_async_copy(pack, weights_all.at[me], local_sem.at[1]),
        pltpu.make_async_copy(ipack, inner_all.at[z], local_sem.at[2]),
        pltpu.make_async_copy(opack, outer_all.at[x], local_sem.at[6]),
    ]
    load.wait()
    keeps.append(pltpu.make_async_copy(stage, tokens_all.at[0], local_sem.at[3]))
    cot_load.wait()
    keeps.append(pltpu.make_async_copy(cot_stage, cotangent_all.at[0], local_sem.at[5]))
    for keep in keeps:
        keep.start()

    def arrive(streams, t, sideways):
        for way in range(2):

            @pl.when(receives(way, t))
            def _():
                origin = z - (1 - 2 * way) * t
                for stream in streams:
                    slot = home(stream, origin)
                    remote(
                        slot, slot, zsend.at[stream, way, t - 1], zrecv.at[stream, way, t - 1], partner(core=1 - core)
                    ).wait_recv()
                if sideways:
                    for move in x_moves(1 + way * (size_z - 1) + t - 1, origin, False):
                        move.start()

    onward = remote(tokens_all.at[1], tokens_all.at[3], tsend.at[2], trecv.at[2], partner(core=1 - core))
    later = remote(cotangent.at[1 - y], cotangent_all.at[1], tsend.at[3], trecv.at[3], partner(y=1 - y))
    for t in range(1, size_z):
        arrive((0, 1), t, True)
        if t < size_z - 1:
            start_z((0, 1), t + 1)
        if t == 1:
            for move in outer_moves:
                move.start()
        arrive((2,), t, False)
        if t < size_z - 1:
            start_z((2,), t + 1)
        if t == min(2, size_z - 1):
            across.wait_recv()
            onward.start()
            later.start()

    for move in x_moves(0, z, True):
        move.wait()
    for t in range(1, size_z):
        for way in range(2):

            @pl.when(receives(way, t))
            def _():
                origin = z - (1 - 2 * way) * t
                for move in x_moves(1 + way * (size_z - 1) + t - 1, origin, False):
                    move.wait()

            @pl.when(sends(way, t))
            def _():
                for stream in range(3):
                    z_move(stream, way, t).wait_send()

    short = min(vector.shape[1] for vector in raw)
    longest = vpack.shape[1]
    for s in range(size_z * size_x):
        rows_out[:, s * short : (s + 1) * short] = vectors_all[s, :, 0:short]
        inner_out[:, s * longest : (s + 1) * longest] = vectors_all[s, WIDE : WIDE + 1, :]
    for move in outer_moves:
        move.wait()
    across.wait_send()
    beside.wait()
    onward.wait()
    later.wait()
    for keep in keeps:
        keep.wait()


def entry(size_z, size_x, tokens, cotangent, wq, wk, wv, w_inner, w_output, w_outer, vectors):
    _, part, width = tokens.shape
    rows = wq.shape[0]
    half = width // 2
    lanes = 3 * half
    hidden = w_inner.shape[1]
    long = w_outer.shape[0]
    mixed_lanes = hidden // 2 + half
    chunks = hidden // CHUNK
    longest = max(v.shape[0] for v in vectors)
    shards = size_z * size_x
    count = len(vectors)
    anywhere, vmem = pl.BlockSpec(memory_space=pl.ANY), pl.BlockSpec(memory_space=pltpu.VMEM)
    dma = pltpu.SemaphoreType.DMA
    low, high = jnp.bfloat16, jnp.float32
    side = size_x - 1
    return pl.pallas_call(
        lambda *refs: entry_kernel(size_z, size_x, count, *refs),
        out_shape=(
            jax.ShapeDtypeStruct((4, part, width), low),
            jax.ShapeDtypeStruct((2, part, width), low),
            jax.ShapeDtypeStruct((shards, rows, lanes), low),
            jax.ShapeDtypeStruct((size_z, rows, mixed_lanes), low),
            jax.ShapeDtypeStruct((size_x, long, half), low),
            jax.ShapeDtypeStruct((16, width), high),
            jax.ShapeDtypeStruct((1, shards * longest), high),
        ),
        in_specs=[anywhere] * (8 + count),
        out_specs=(anywhere,) * 5 + (vmem,) * 2,
        scratch_shapes=[pltpu.VMEM((1, v.shape[0]), v.dtype) for v in vectors]
        + [
            pltpu.VMEM((part, width), low),
            pltpu.VMEM((part, width), low),
            pltpu.VMEM((3, rows, half), high),
            pltpu.VMEM((rows, mixed_lanes), high),
            pltpu.VMEM((long, half), high),
            pltpu.VMEM((rows, lanes), low),
            pltpu.VMEM((rows, mixed_lanes), low),
            pltpu.VMEM((long, half), low),
            pltpu.VMEM((16, longest), high),
            pltpu.VMEM((shards, 16, longest), high),
            dma((7,)),
            dma((5 + count + chunks,)),
            dma((4,)),
            dma((4,)),
            dma((3, 2, size_z - 1)),
            dma((3, 2, size_z - 1)),
            dma((2, 2 * size_z - 1, side)),
            dma((2, 2 * size_z - 1, side)),
            dma((side,)),
            dma((side,)),
        ],
        compiler_params=pltpu.CompilerParams(collective_id=0, has_side_effects=True, vmem_limit_bytes=66_000_000),
        name="entry",
    )(tokens, cotangent, wq, wk, wv, w_inner, w_output, w_outer, *[v.reshape(1, -1) for v in vectors])


def exit_kernel(size_z, size_x, shapes, *refs):
    z, x, y, core = place_of()
    names = list(shapes)
    grads_hbm, inputs_hbm, weights_hbm, base_hbm, output_term, dense_sums, inner_sums, head_sums = refs[:8]
    inner_in = refs[8 : 8 + size_z]
    outer_in = refs[8 + size_z : 8 + size_z + size_x]
    refs = refs[8 + size_z + size_x :]
    results = refs[:8]
    token_grads, grad_query, grad_key, grad_value, grad_output, grad_inner, grad_outer, vector_sums = refs[8:16]
    grads, inputs, turned, weights, base, terms, other_rows, recv_rows, send_rows, far_rows, odd = refs[16:27]
    inner_buf, outer_buf, vector_rows, vector_terms, store_sem = refs[27:32]
    load_sem, tsend, trecv, osend, orecv = refs[32:37]
    refs = refs[37:]
    made = (token_grads, grad_query, grad_key, grad_value, grad_output, grad_inner, grad_outer, vector_sums)
    stores = [pltpu.make_async_copy(a, b, store_sem.at[i]) for i, (a, b) in enumerate(zip(made, results))]
    xin, xsend, xrecv, xout = {}, {}, {}, {}
    zout, zin, zsend, zrecv = {}, {}, {}, {}
    ybuf, ysend, yrecv, cbuf, csend, crecv = {}, {}, {}, {}, {}, {}
    refs = list(refs)
    for name in names:
        ybuf[name], ysend[name], yrecv[name], cbuf[name], csend[name], crecv[name] = [refs.pop(0) for _ in range(6)]
        if name != "outer":
            xin[name], xsend[name], xrecv[name] = [refs.pop(0) for _ in range(3)]
        if name != "inner":
            zout[name], zin[name], zsend[name], zrecv[name] = [refs.pop(0) for _ in range(4)]
    xout["inner"] = refs.pop(0)

    shards, rows, lanes = terms.shape
    half = lanes // 3
    width = 2 * half
    pairs = half // 128
    hidden = grad_inner.shape[1]
    part = token_grads.shape[1]
    local = 2 * part
    low, high = jnp.bfloat16, jnp.float32
    mine = pl.ds(pl.multiple_of(core * half, 128), half)
    theirs = pl.ds(pl.multiple_of((1 - core) * half, 128), half)
    order = sorted(range(size_z), key=lambda k: -min(k, size_z - k))
    far_order = [k for k in order if k > 0]
    columns = [lax.rem(x + j, size_x) for j in range(size_x)]

    def slot_of(k, j):
        return lax.rem(z + k, size_z) * size_x + columns[j]

    loads = {}
    for i, src in enumerate(inner_in):
        loads["inner", i] = pltpu.make_async_copy(src, inner_buf.at[i], load_sem.at[i])
    for i, src in enumerate(outer_in):
        loads["outer", i] = pltpu.make_async_copy(src, outer_buf.at[i], load_sem.at[size_z + i])
    for i, (name, src, dst) in enumerate(
        (("inputs", inputs_hbm, inputs), ("grads", grads_hbm, grads), ("weights", weights_hbm, weights), ("base", base_hbm, base))
    ):
        loads[name] = pltpu.make_async_copy(src, dst, load_sem.at[size_z + size_x + i])
    for load in loads.values():
        load.start()
    greet(True)

    core_peer, y_peer = partner(core=1 - core), partner(y=1 - y)
    outputs = remote(output_term.at[:, :, theirs], odd, osend, orecv, core_peer)
    outputs.start()
    sideways = {}
    along = {}
    kept = {}

    def send_x(name, n, k, j, src, dst):
        move = remote(src, dst, xsend[name].at[n, k, j - 1], xrecv[name].at[n, k, j - 1], partner(x=columns[j]))
        move.start()
        sideways.setdefault((name, k, j), []).append(move)

    def send_z(name, k):
        move = remote(
            zout[name].at[k - 1],
            zin[name].at[k - 1],
            zsend[name].at[k - 1],
            zrecv[name].at[k - 1],
            partner(z=lax.rem(z + k, size_z)),
        )
        move.start()
        along[name, k] = move

    vector_rows[...] = jnp.zeros_like(vector_rows)
    for i, row in enumerate((7, 8, 6, 3, 4, 2)):
        vector_rows[row : row + 1, :] = jnp.sum(dense_sums[8 * i : 8 * i + 8, :], axis=0, keepdims=True)
    for p in range(pairs):
        place = pl.ds(pl.multiple_of(core * half + p * 128, 128), 128)
        vector_rows[0:1, place] = head_sums[8 * p : 8 * p + 1, 0:128]
        vector_rows[1:2, place] = head_sums[8 * p : 8 * p + 1, 256:384]
    inner_row = jnp.sum(inner_sums[...], axis=0, keepdims=True)
    vector_terms[...] = jnp.zeros_like(vector_terms)
    longest = vector_terms.shape[2]
    for s in range(shards):
        vector_terms[s, :, 0:rows] = vector_rows[:, s * rows : (s + 1) * rows]
        vector_terms[s, WIDE : WIDE + 1, :] = inner_row[:, s * longest : (s + 1) * longest]
    for k in order:
        for j in range(1, size_x):
            send_x("vec", 0, k, j, vector_terms.at[slot_of(k, j)], xin["vec"].at[j - 1, k])

    for i in range(size_z):
        loads["inner", i].wait()
    for j in range(size_x):
        total = inner_buf[0, columns[j]].astype(high)
        for i in range(1, size_z):
            total = total + inner_buf[i, columns[j]].astype(high)
        if j == 0:
            kept["inner"] = total
        else:
            xout["inner"][j - 1] = total.astype(low)
            send_x("inner", 0, 0, j, xout["inner"].at[j - 1], xin["inner"].at[j - 1, 0])

    for i in range(size_x):
        loads["outer", i].wait()
    for k in order:
        target = lax.rem(z + k, size_z)
        total = outer_buf[0, target].astype(high)
        for i in range(1, size_x):
            total = total + outer_buf[i, target].astype(high)
        if k == 0:
            kept["outer"] = total
        else:
            zout["outer"][k - 1] = total.astype(low)
            send_z("outer", k)

    loads["inputs"].wait()
    for b in range(4):
        turned[:, b * part : (b + 1) * part] = inputs[b * part : (b + 1) * part, :].T
    loads["grads"].wait()
    group = 4
    for p in range(pairs):
        block = slice(p * 384, (p + 1) * 384)

        def some(m, _):
            value = dot_nn(turned[pl.ds(pl.multiple_of(m * group * rows, group * rows), group * rows), :], grads[:, block])
            terms[pl.ds(m * group, group), :, block] = value.reshape(group, rows, 384).astype(low)
            return 0

        lax.fori_loop(0, shards // group, some, 0)
        for k in order:
            for j in range(1, size_x):
                send_x("qkv", p, k, j, terms.at[slot_of(k, j), :, block], xin["qkv"].at[j - 1, k, :, block])

    loads["weights"].wait()
    strip = 256

    def product(first):
        at = pl.ds(pl.multiple_of(first, strip), strip)
        return dot_nt(grads[at, :], weights[...])

    def other_strip(i, _):
        other_rows[pl.ds(pl.multiple_of(i * strip, strip), strip), :] = product(local + i * strip).astype(low)
        return 0

    lax.fori_loop(0, local // strip, other_strip, 0)
    halves = remote(other_rows, recv_rows, tsend.at[0], trecv.at[0], core_peer)
    halves.start()
    outputs.wait()
    for k in order:
        for j in range(1, size_x):
            slot = slot_of(k, j)
            odd[slot] = (odd[slot].astype(high) + output_term[slot, :, mine].astype(high)).astype(low)
            send_x("out", 0, k, j, odd.at[slot], xin["out"].at[j - 1, k])
    loads["base"].wait()

    def own_strip(i, _):
        at = pl.ds(pl.multiple_of(i * strip, strip), strip)
        base[at, :] = base[at, :] + product(i * strip)
        return 0

    lax.fori_loop(0, local // strip, own_strip, 0)
    halves.wait()
    send_rows[...] = (base[part:local, :] + recv_rows[part:local, :].astype(high)).astype(low)
    back = remote(send_rows, far_rows, tsend.at[1], trecv.at[1], y_peer)
    back.start()
    token_grads[y] = base[0:part, :] + recv_rows[0:part, :].astype(high)

    across = {}
    swapped = {}

    def step_y(name):
        move = remote(ybuf[name].at[0], ybuf[name].at[1], ysend[name], yrecv[name], y_peer)
        move.start()
        across[name] = move

    def step_core(name):
        across[name].wait()
        cbuf[name][0] = ybuf[name][0].astype(high) + ybuf[name][1].astype(high)
        move = remote(cbuf[name].at[0], cbuf[name].at[1], csend[name], crecv[name], core_peer)
        move.start()
        swapped[name] = move

    def finish_x(name):
        for k in order:
            slot = slot_of(k, 0)
            if name == "qkv":
                total = terms[slot].astype(high)
            elif name == "out":
                total = odd[slot].astype(high) + output_term[slot, :, mine].astype(high)
            else:
                total = vector_terms[slot]
            for j in range(1, size_x):
                for move in sideways[name, k, j]:
                    move.wait()
                total = total + xin[name][j - 1, k].astype(high)
            if k == 0:
                kept[name] = total
            else:
                zout[name][k - 1] = total.astype(zout[name].dtype)
                send_z(name, k)

    def finish_z(name):
        total = kept[name]
        for k in far_order:
            along[name, k].wait()
            total = total + zin[name][k - 1].astype(high)
        ybuf[name][0] = total.astype(ybuf[name].dtype)
        step_y(name)

    total = kept["inner"]
    for j in range(1, size_x):
        for move in sideways["inner", 0, j]:
            move.wait()
        total = total + xin["inner"][j - 1, 0].astype(high)
    ybuf["inner"][0] = total.astype(low)
    step_y("inner")
    finish_x("vec")
    finish_x("qkv")
    finish_z("outer")
    step_core("inner")
    finish_x("out")
    finish_z("vec")
    step_core("outer")
    finish_z("qkv")
    finish_z("out")
    back.wait()
    token_grads[1 - y] = far_rows[...].astype(high)
    stores[0].start()
    step_core("vec")

    def finish_core(name):
        swapped[name].wait()
        return cbuf[name]

    buf = finish_core("inner")
    chunks = hidden // CHUNK
    for i in range(2):
        owner = core if i == 0 else 1 - core
        for c in range(chunks):
            place = pl.ds(pl.multiple_of(c * CHUNK + owner * half, 128), half)
            grad_inner[:, place] = buf[i, :, c * half : (c + 1) * half]
    stores[5].start()
    buf = finish_core("outer")
    for i in range(2):
        owner = core if i == 0 else 1 - core
        grad_outer[:, pl.ds(pl.multiple_of(owner * half, 128), half)] = buf[i]
    stores[6].start()
    step_core("qkv")
    step_core("out")
    buf = finish_core("vec")
    vector_sums[...] = buf[0] + buf[1]
    stores[7].start()
    buf = finish_core("qkv")
    for i in range(2):
        owner = core if i == 0 else 1 - core
        for p in range(pairs):
            place = pl.ds(pl.multiple_of(owner * half + p * 128, 128), 128)
            for n, out in enumerate((grad_query, grad_key, grad_value)):
                out[:, place] = buf[i, :, (3 * p + n) * 128 : (3 * p + n + 1) * 128]
    for i in (1, 2, 3):
        stores[i].start()
    buf = finish_core("out")
    for i in range(2):
        owner = core if i == 0 else 1 - core
        grad_output[:, pl.ds(pl.multiple_of(owner * half, 128), half)] = buf[i]
    stores[4].start()
    for store in stores:
        store.wait()


def deliver_kernel(count, *refs):
    sources, vectors, outs, sem = refs[:count], refs[count], refs[count + 1 : -1], refs[-1]
    copies = [pltpu.make_async_copy(src, dst, sem.at[i]) for i, (src, dst) in enumerate(zip(sources, outs))]
    for copy in copies:
        copy.start()
    for i, out in enumerate(outs[count:]):
        out[...] = vectors[i : i + 1, 0 : out.shape[1]]
    for copy in copies:
        copy.wait()


def deliver(matrices, vectors, sizes):
    count = len(matrices)
    vmem, anywhere = pl.BlockSpec(memory_space=pltpu.VMEM), pl.BlockSpec(memory_space=pl.ANY)
    return pl.pallas_call(
        lambda *refs: deliver_kernel(count, *refs),
        out_shape=tuple(jax.ShapeDtypeStruct(m.shape, m.dtype) for m in matrices)
        + tuple(jax.ShapeDtypeStruct((1, size), jnp.float32) for size in sizes),
        in_specs=[vmem] * (count + 1),
        out_specs=(anywhere,) * count + (vmem,) * len(sizes),
        scratch_shapes=[pltpu.SemaphoreType.DMA((count,))],
        compiler_params=pltpu.CompilerParams(vmem_limit_bytes=60_000_000),
        name="deliver",
    )(*matrices, vectors)


def exit_call(size_z, size_x, grads, inputs, weights, base, output_term, dense_sums, inner_sums, head_sums, inner_terms, outer_terms):
    shards, rows, width = output_term.shape
    lanes = grads.shape[1]
    half = width // 2
    pairs = half // 128
    length = inputs.shape[0]
    local = length // 2
    part = local // 2
    long = outer_terms[0].shape[1]
    hidden = 2 * inner_terms[0].shape[2]
    vmem, anywhere = pl.BlockSpec(memory_space=pltpu.VMEM), pl.BlockSpec(memory_space=pl.ANY)
    dma = pltpu.SemaphoreType.DMA
    side = size_x - 1
    low, high = jnp.bfloat16, jnp.float32
    vector_shape = (16, hidden // shards)
    shapes = {
        "vec": (vector_shape, high, 1),
        "qkv": ((rows, lanes), low, pairs),
        "out": ((rows, half), low, 1),
        "inner": ((rows, hidden // 2), low, 1),
        "outer": ((long, half), low, 1),
    }
    matrix = jax.ShapeDtypeStruct((rows, width), high)
    results = (
        jax.ShapeDtypeStruct((2, part, width), high),
        matrix,
        matrix,
        matrix,
        matrix,
        jax.ShapeDtypeStruct((rows, hidden), high),
        jax.ShapeDtypeStruct((long, width), high),
        jax.ShapeDtypeStruct(vector_shape, high),
    )
    scratch = [pltpu.VMEM(r.shape, r.dtype) for r in results] + [
        pltpu.VMEM((length, lanes), low),
        pltpu.VMEM((length, width), low),
        pltpu.VMEM((width, length), low),
        pltpu.VMEM((width, lanes), low),
        pltpu.VMEM((local, width), high),
        pltpu.VMEM((shards, rows, lanes), low),
        pltpu.VMEM((local, width), low),
        pltpu.VMEM((local, width), low),
        pltpu.VMEM((part, width), low),
        pltpu.VMEM((part, width), low),
        pltpu.VMEM((shards, rows, half), low),
        pltpu.VMEM((size_z,) + inner_terms[0].shape, low),
        pltpu.VMEM((size_x,) + outer_terms[0].shape, low),
        pltpu.VMEM((16, width), high),
        pltpu.VMEM((shards,) + vector_shape, high),
        dma((len(results),)),
        dma((size_z + size_x + 4,)),
        dma((2,)),
        dma((2,)),
        dma,
        dma,
    ]
    for name, (shape, kind, sends) in shapes.items():
        scratch += [pltpu.VMEM((2,) + shape, kind), dma, dma, pltpu.VMEM((2,) + shape, high), dma, dma]
        stages = 1 if name == "inner" else size_z
        if name != "outer":
            scratch += [pltpu.VMEM((side, stages) + shape, kind), dma((sends, stages, side)), dma((sends, stages, side))]
        if name != "inner":
            scratch += [pltpu.VMEM((size_z - 1,) + shape, kind)] * 2 + [dma((size_z - 1,))] * 2
    scratch.append(pltpu.VMEM((side, rows, hidden // 2), low))
    return pl.pallas_call(
        lambda *refs: exit_kernel(size_z, size_x, shapes, *refs),
        out_shape=results,
        in_specs=[anywhere] * 4 + [vmem] * 4 + [anywhere] * (size_z + size_x),
        out_specs=(anywhere,) * len(results),
        scratch_shapes=scratch,
        compiler_params=pltpu.CompilerParams(collective_id=1, has_side_effects=True, vmem_limit_bytes=67_000_000),
        name="exit",
    )(grads, inputs, weights, base, output_term, dense_sums, inner_sums, head_sums, *inner_terms, *outer_terms)


TILE = 256
CHUNK = 768


def dot_nt(a, b):
    return lax.dot_general(a, b, (((1,), (1,)), ((), ())), preferred_element_type=jnp.float32)


def row_mean(value):
    return jnp.sum(value, axis=-1, keepdims=True) * (1.0 / value.shape[-1])


def standardize(hidden):
    centred = hidden - row_mean(hidden)
    reciprocal = lax.rsqrt(row_mean(centred * centred) + EPS)
    return centred * reciprocal, reciprocal


def column_sum(value):
    return jnp.sum(value.reshape(value.shape[0] // 8, 8, value.shape[1]), axis=0)


def dense_kernel(
    size_z,
    size_x,
    tokens_ref,
    mine_ref,
    other_ref,
    cot_ref,
    vectors_ref,
    bias_inner_ref,
    *refs,
):
    inner_parts, outer_parts = refs[:size_x], refs[size_x : size_x + size_z]
    refs = refs[size_x + size_z :]
    mixed_ref, pre_first_ref, grad_mine_ref, grad_other_ref, sums_ref, inner_sum_ref, grad_output_ref = refs[:7]
    inner_terms = refs[7 : 7 + size_z]
    outer_terms = refs[7 + size_z : 7 + size_z + size_x]
    refs = refs[7 + size_z + size_x :]
    w_output, w_inner, w_outer, a_output, a_inner, a_outer, grad_out_buf = refs[:7]
    context, first_low, turned_low, normed, first, slope, active, work = refs[7:15]
    send_inner, send_outer, recv_inner, recv_outer = refs[15:19]
    load_sem, share_send, share_recv, send_sem, recv_sem, store_sem = refs[19:]
    step, steps = pl.program_id(0), pl.num_programs(0)
    core_here = lax.axis_index("core")
    width, hidden = w_inner.shape
    half = width // 2
    chunks = hidden // CHUNK
    shards = size_z * size_x
    z, x, y, _ = place_of()
    twin = partner(core=1 - lax.axis_index("core"))

    shard = width // shards
    long = hidden // shards
    group = CHUNK // long // size_x

    def columns_of(first, owner):
        return pl.ds(pl.multiple_of(first + owner * half, 128), half)

    def start_piece(i, src, dst):
        pltpu.make_async_copy(src, dst, load_sem.at[i]).start()
        remote(src, dst, share_send.at[i], share_recv.at[i], twin).start()

    def start_rows(i, lane, ref, first):
        for j in range(size_x):
            for at in range(size_z):
                slot = at * size_x + lax.rem(x - j + size_x, size_x)
                rows = pl.ds(pl.multiple_of(slot * shard, shard), shard)
                start_piece(i, inner_parts[j].at[at, :, pl.ds(lane, half)], ref.at[rows, columns_of(first, core_here)])

    def start_loads():
        start_rows(0, hidden // 2, w_output, 0)
        for c in range(chunks):
            start_rows(1 + 2 * c, c * half, w_inner, c * CHUNK)
            for at in range(c * group, (c + 1) * group):
                for k in range(size_z):

                    @pl.when(lax.rem(z - k + size_z, size_z) == at)
                    def _():
                        for column in range(size_x):
                            rows = pl.ds((at * size_x + column) * long, long)
                            start_piece(2 + 2 * c, outer_parts[k].at[column], w_outer.at[rows, columns_of(0, core_here)])

    def wait_load(i, ref, rows, first):
        own, far = ref.at[rows, columns_of(first, core_here)], ref.at[rows, columns_of(first, 1 - core_here)]
        pltpu.make_async_copy(own, own, load_sem.at[i]).wait()
        remote(own, far, share_send.at[i], share_recv.at[i], twin).wait()

    @pl.when(step == 0)
    def _():
        barrier = pltpu.get_barrier_semaphore()
        pl.semaphore_signal(barrier, inc=1, device_id=twin, device_id_type=MESH_ID)
        pl.semaphore_wait(barrier, 1)
        start_loads()
        a_output[...] = jnp.zeros_like(a_output)
        a_inner[...] = jnp.zeros_like(a_inner)
        a_outer[...] = jnp.zeros_like(a_outer)
        sums_ref[...] = jnp.zeros_like(sums_ref)
        inner_sum_ref[...] = jnp.zeros_like(inner_sum_ref)

    def vector(i):
        row = (2, 3, 4, 6, 7, 8)[i]
        return vectors_ref[row : row + 1, :]

    def add_sum(i, value):
        sums_ref[8 * i : 8 * i + 8, :] += column_sum(value)

    context[:, pl.ds(pl.multiple_of(core_here * half, 128), half)] = mine_ref[...]
    context[:, pl.ds(pl.multiple_of((1 - core_here) * half, 128), half)] = other_ref[...]

    @pl.when(step == 0)
    def _():
        wait_load(0, w_output, slice(None), 0)

    hidden_rows = tokens_ref[...].astype(jnp.float32) + (dot_nn(context[...], w_output[...]) + vector(0))
    normed[...], first_recip = standardize(hidden_rows)
    first[...] = normed[...] * vector(1) + vector(2)
    first_low[...] = first[...].astype(jnp.bfloat16)
    turned_low[...] = first_low[...].T
    work[...] = jnp.broadcast_to(vector(3), work.shape)

    def part(c):
        return pl.ds(pl.multiple_of(c * CHUNK, CHUNK), CHUNK)

    def exchange(c):
        return (
            remote(send_inner.at[c], recv_inner.at[c], send_sem.at[0, c], recv_sem.at[0, c], twin),
            remote(send_outer.at[c], recv_outer.at[c], send_sem.at[1, c], recv_sem.at[1, c], twin),
        )

    def forward(c):
        @pl.when(step == 0)
        def _():
            wait_load(1 + 2 * c, w_inner, slice(None), c * CHUNK)

        u = dot_nn(first_low[...], w_inner[:, part(c)]) + bias_inner_ref[0:1, part(c)]
        cdf = 0.5 * (1.0 + lax.erf(u * ROOT_HALF))
        slope[:, part(c)] = cdf + u * jnp.exp(-0.5 * u * u) * INV_ROOT_TAU
        active[:, part(c)] = (u * cdf).astype(jnp.bfloat16)

        @pl.when(step == 0)
        def _():
            wait_load(2 + 2 * c, w_outer, part(c), 0)

        work[...] += dot_nn(active[:, part(c)], w_outer[part(c), :])

    for c in range(chunks):
        forward(c)
    second, second_recip = standardize(first[...] + work[...])
    mixed_ref[...] = (second * vector(4) + vector(5)).astype(jnp.bfloat16)
    upstream = cot_ref[...].astype(jnp.float32)
    add_sum(0, upstream * second)
    add_sum(1, upstream)
    scaled = upstream * vector(4)
    pre_second = second_recip * (scaled - row_mean(scaled) - second * row_mean(scaled * second))
    grad_outer = pre_second.astype(jnp.bfloat16)
    add_sum(2, grad_outer.astype(jnp.float32))
    work[...] = pre_second
    grad_out_buf[...] = grad_outer

    def backward(c, _):
        grad_out = grad_out_buf[...]
        grad = dot_nt(grad_out, w_outer[part(c), :])
        grad_inner = (grad * slope[:, part(c)]).astype(jnp.bfloat16)
        inner_sum_ref[:, part(c)] += column_sum(grad_inner.astype(jnp.float32))
        a_outer[part(c), :] += dot_nn(active[:, part(c)].T, grad_out)
        a_inner[:, part(c)] += dot_nn(turned_low[...], grad_inner)
        work[...] += dot_nt(grad_inner, w_inner[:, part(c)])

        @pl.when(step == steps - 1)
        def _():
            theirs = pl.multiple_of(c * CHUNK + (1 - core_here) * half, 128)
            send_inner[c] = a_inner[:, pl.ds(theirs, half)].astype(jnp.bfloat16)
            send_outer[c] = a_outer[part(c), pl.ds(pl.multiple_of((1 - core_here) * half, 128), half)].astype(jnp.bfloat16)
            for move in exchange(c):
                move.start()

        return 0

    lax.fori_loop(0, chunks, backward, 0)
    grad_first = work[...]
    add_sum(3, grad_first * normed[...])
    add_sum(4, grad_first)
    scaled = grad_first * vector(1)
    pre_first = first_recip * (scaled - row_mean(scaled) - normed[...] * row_mean(scaled * normed[...]))
    pre_first_ref[...] = pre_first
    grad_attended = pre_first.astype(jnp.bfloat16)
    add_sum(5, grad_attended.astype(jnp.float32))
    a_output[...] += dot_nn(context[...].T, grad_attended)
    context[...] = dot_nt(grad_attended, w_output[...]).astype(jnp.bfloat16)
    grad_mine_ref[...] = context[:, pl.ds(pl.multiple_of(core_here * half, 128), half)]
    grad_other_ref[...] = context[:, pl.ds(pl.multiple_of((1 - core_here) * half, 128), half)]

    @pl.when(step == steps - 1)
    def _():
        grad_output_ref[...] = a_output[...].astype(jnp.bfloat16)

        def inner_out(c):
            copies = []
            for k in range(size_z):
                for column in range(size_x):
                    slot = lax.rem(z + k, size_z) * size_x + column
                    src = send_inner.at[c, pl.ds(pl.multiple_of(slot * shard, shard), shard), :]
                    copies.append(
                        pltpu.make_async_copy(src, inner_terms[k].at[column, :, pl.ds(c * half, half)], store_sem.at[0, c])
                    )
            return copies

        def outer_out(c):
            copies = []
            for i in range(group):
                for j in range(size_x):
                    src = send_outer.at[c, pl.ds(pl.multiple_of((i * size_x + lax.rem(x + j, size_x)) * long, long), long), :]
                    copies.append(pltpu.make_async_copy(src, outer_terms[j].at[c * group + i], store_sem.at[1, c]))
            return copies

        for c in range(chunks):
            ours = pl.multiple_of(c * CHUNK + core_here * half, 128)
            first_move, second_move = exchange(c)
            first_move.wait()
            send_inner[c] = (a_inner[:, pl.ds(ours, half)] + recv_inner[c].astype(jnp.float32)).astype(jnp.bfloat16)
            for copy in inner_out(c):
                copy.start()
            second_move.wait()
            columns = pl.ds(pl.multiple_of(core_here * half, 128), half)
            send_outer[c] = (a_outer[part(c), columns] + recv_outer[c].astype(jnp.float32)).astype(jnp.bfloat16)
            for copy in outer_out(c):
                copy.start()
        for c in range(chunks):
            pltpu.make_async_copy(send_inner.at[c], send_inner.at[c], store_sem.at[0, c]).wait()
            pltpu.make_async_copy(send_outer.at[c], send_outer.at[c], store_sem.at[1, c]).wait()


def dense_layer(size_z, size_x, tokens, mine, other, cotangent, vectors, bias_inner, inner_parts, outer_parts):
    local, half = mine.shape
    width = 2 * half
    hidden = bias_inner.shape[1]
    steps = local // TILE
    shards = size_z * size_x
    chunks = hidden // CHUNK
    low, high = jnp.bfloat16, jnp.float32
    tile = pl.BlockSpec((TILE, width), lambda t, *_: (t, 0))
    half_tile = pl.BlockSpec((TILE, half), lambda t, *_: (t, 0))
    anywhere = pl.BlockSpec(memory_space=pl.ANY)

    def whole(shape):
        return pl.BlockSpec(shape, lambda t, *_: (0, 0))

    inner_shape = jax.ShapeDtypeStruct((size_x, width // shards, hidden // 2), low)
    outer_shape = jax.ShapeDtypeStruct((size_z, hidden // shards, half), low)
    halves = pltpu.VMEM((chunks, width, half), low)
    dma = pltpu.SemaphoreType.DMA
    return pl.pallas_call(
        lambda *refs: dense_kernel(size_z, size_x, *refs),
        out_shape=(
            jax.ShapeDtypeStruct((local, width), low),
            jax.ShapeDtypeStruct((local, width), high),
            jax.ShapeDtypeStruct((local, half), low),
            jax.ShapeDtypeStruct((local, half), low),
            jax.ShapeDtypeStruct((48, width), high),
            jax.ShapeDtypeStruct((8, hidden), high),
            jax.ShapeDtypeStruct((width, width), low),
        )
        + (inner_shape,) * size_z
        + (outer_shape,) * size_x,
        grid_spec=pltpu.PrefetchScalarGridSpec(
            num_scalar_prefetch=0,
            grid=(steps,),
            in_specs=[
                tile,
                half_tile,
                half_tile,
                tile,
                whole((16, width)),
                whole((1, hidden)),
            ]
            + [anywhere] * (size_x + size_z),
            out_specs=[
                tile,
                tile,
                half_tile,
                half_tile,
                whole((48, width)),
                whole((8, hidden)),
                whole((width, width)),
            ]
            + [anywhere] * (size_z + size_x),
            scratch_shapes=[
                pltpu.VMEM((width, width), low),
                pltpu.VMEM((width, hidden), low),
                pltpu.VMEM((hidden, width), low),
                pltpu.VMEM((width, width), high),
                pltpu.VMEM((width, hidden), high),
                pltpu.VMEM((hidden, width), high),
                pltpu.VMEM((TILE, width), low),
                pltpu.VMEM((TILE, width), low),
                pltpu.VMEM((TILE, width), low),
                pltpu.VMEM((width, TILE), low),
                pltpu.VMEM((TILE, width), high),
                pltpu.VMEM((TILE, width), high),
                pltpu.VMEM((TILE, hidden), high),
                pltpu.VMEM((TILE, hidden), low),
                pltpu.VMEM((TILE, width), high),
                halves,
                halves,
                halves,
                halves,
                dma((1 + 2 * chunks,)),
                dma((1 + 2 * chunks,)),
                dma((1 + 2 * chunks,)),
                dma((2, chunks)),
                dma((2, chunks)),
                dma((2, chunks)),
            ],
        ),
        compiler_params=pltpu.CompilerParams(
            dimension_semantics=("arbitrary",), vmem_limit_bytes=67_000_000, collective_id=3, has_side_effects=True
        ),
        cost_estimate=pl.CostEstimate(flops=32_000_000_000, bytes_accessed=40_000_000, transcendentals=6_000_000),
        name="dense_layer",
    )(tokens, mine, other, cotangent, vectors, bias_inner, *inner_parts, *outer_parts)


def lowered(piece):
    return piece.astype(jnp.bfloat16)


def widen(piece):
    return piece.astype(jnp.float32)


def matmul(left, right):
    return jnp.dot(left, right, preferred_element_type=jnp.float32)


def matmul_tn(left, right):
    return lax.dot_general(
        left, right, (((0,), (0,)), ((), ())), preferred_element_type=jnp.float32
    )


def matmul_nt(left, right):
    return lax.dot_general(
        left, right, (((1,), (1,)), ((), ())), preferred_element_type=jnp.float32
    )


def normalize(hidden, norm_gain, norm_shift):
    centred = hidden - jnp.mean(hidden, axis=-1, keepdims=True)
    reciprocal = lax.rsqrt(jnp.mean(centred * centred, axis=-1, keepdims=True) + EPS)
    normed = centred * reciprocal
    return (normed * norm_gain + norm_shift, normed, reciprocal)


def normalize_back(upstream, normed, reciprocal, norm_gain):
    scaled = upstream * norm_gain
    result = reciprocal * (
        scaled
        - jnp.mean(scaled, axis=-1, keepdims=True)
        - normed * jnp.mean(scaled * normed, axis=-1, keepdims=True)
    )
    return (result, jnp.sum(upstream * normed, axis=0), jnp.sum(upstream, axis=0))


def gelu_value(values_in):
    return 0.5 * values_in * (1.0 + lax.erf(values_in * ROOT_HALF))


def gelu_slope(values_in):
    return (
        0.5 * (1.0 + lax.erf(values_in * ROOT_HALF))
        + values_in * jnp.exp(-0.5 * values_in * values_in) * INV_ROOT_TAU
    )


def shift(piece, axis, step):
    size = lax.axis_size(axis)
    return lax.ppermute(piece, axis, [(i, (i + step) % size) for i in range(size)])


def swap(piece, axis):
    return lax.ppermute(piece, axis, [(0, 1), (1, 0)])


def pick(piece, index, axis=0):
    return lax.dynamic_index_in_dim(piece, index, axis, keepdims=False)


def in_order(first_is_zero, own, other, axis):
    return jnp.where(
        first_is_zero,
        jnp.concatenate([own, other], axis),
        jnp.concatenate([other, own], axis),
    )


def collect(piece):
    size_z, size_x = lax.axis_size("z"), lax.axis_size("x")
    z, x = lax.axis_index("z"), lax.axis_index("x")
    along_z = [piece] + [shift(piece, "z", k) for k in range(1, size_z)]
    whole = jnp.zeros((size_z, size_x) + piece.shape, piece.dtype)
    zeros = (0,) * piece.ndim
    for j in range(size_x):
        for k in range(size_z):
            arrived = along_z[k] if j == 0 else shift(along_z[k], "x", j)
            place = ((z - k) % size_z, (x - j) % size_x) + zeros
            whole = lax.dynamic_update_slice(whole, arrived[None, None], place)
    return whole.reshape((size_z * size_x,) + piece.shape)


def reduce_owned(terms):
    size_z, size_x = lax.axis_size("z"), lax.axis_size("x")
    z, x = lax.axis_index("z"), lax.axis_index("x")
    terms = terms.reshape((size_z, size_x) + terms.shape[1:])
    total = widen(pick(terms, x, 1))
    for j in range(1, size_x):
        total = total + widen(shift(pick(terms, (x + j) % size_x, 1), "x", j))
    terms = lowered(total)
    total = widen(pick(terms, z))
    for k in range(1, size_z):
        total = total + widen(shift(pick(terms, (z + k) % size_z), "z", k))
    terms = lowered(total)
    return widen(terms) + widen(swap(terms, "y"))


def plain_body(
    tokens,
    segment_ids,
    w_query,
    w_key,
    w_value,
    w_output,
    b_query,
    b_value,
    b_output,
    first_gain,
    first_shift,
    w_inner,
    b_inner,
    w_outer,
    b_outer,
    second_gain,
    second_shift,
    cotangent,
):
    core, y = lax.axis_index("core"), lax.axis_index("y")
    shards = lax.axis_size("z") * lax.axis_size("x")
    sequences, part, width = tokens.shape
    half = width // 2
    pairs = half // 128
    hidden = w_inner.shape[1]
    local = 2 * part
    own_rows = w_query.shape[0]
    unit_half = hidden // shards // 2

    def columns(matrix):
        return lowered(lax.dynamic_slice_in_dim(matrix, core * half, half, 1))

    vectors = (b_query, b_value, b_output, first_gain, first_shift, b_inner, b_outer, second_gain, second_shift)
    flat = jnp.concatenate([lowered(v) for v in vectors])
    lanes = 3 * half
    extra = -(-flat.shape[0] // lanes)
    flat = jnp.pad(flat, (0, extra * lanes - flat.shape[0])).reshape(extra, lanes)
    weights = jnp.stack([columns(w).reshape(own_rows, pairs, 128) for w in (w_query, w_key, w_value)], axis=2)
    early = collect(jnp.concatenate([weights.reshape(own_rows, lanes), flat], axis=0))

    mine = pick(tokens, y)
    arrived = swap(pick(tokens, 1 - y), "y")
    mine_other, arrived_other = swap(mine, "core"), swap(arrived, "core")
    inputs_all = jnp.concatenate([mine, arrived, mine_other, arrived_other], axis=0)
    inputs = jnp.concatenate([mine, arrived], axis=0)

    inner_piece = lowered(pick(w_inner.reshape(own_rows, shards, 2, unit_half), core, 2)).reshape(own_rows, hidden // 2)
    late = collect(jnp.concatenate([columns(w_output), inner_piece], axis=1)).reshape(width, half + hidden // 2)
    outer_own = collect(lowered(lax.dynamic_slice_in_dim(w_outer, core * unit_half, unit_half, 0))).reshape(hidden // 2, width)
    output_own, inner_own = late[:, :half], late[:, half:]
    output_other, inner_other, outer_other = swap(output_own, "core"), swap(inner_own, "core"), swap(outer_own, "core")
    full_output = in_order(core == 0, output_own, output_other, 1)
    cotangent_mine = pick(cotangent, y)
    cotangent_arrived = swap(pick(cotangent, 1 - y), "y")

    full_early = early[:, :own_rows].reshape(width, lanes)
    flat_all = early[:, own_rows:].reshape(shards, extra * lanes)
    sizes = [v.shape[0] for v in vectors]
    gathered, at = [], 0
    for size in sizes:
        gathered.append(flat_all[:, at : at + size].reshape(shards * size))
        at += size
    bias_query, bias_value, bias_output, gain_first, shift_first, bias_inner, bias_outer, gain_second, shift_second = [
        widen(v) for v in gathered
    ]
    spot = jnp.arange(5, dtype=jnp.int32)
    place = jnp.where(spot < 4, ((spot % 2 != core) * 2 + (spot // 2 != y) * 1) * part, core)
    segments = pick(segment_ids, y)
    biases = jnp.concatenate([bias_query[None], bias_value[None], jnp.zeros((14, width), jnp.float32)], axis=0)
    heads_mine, heads_other, logsum, projected = attention(place, segments, inputs_all, full_early, biases)
    context = in_order(core == 0, heads_mine, swap(heads_other, "core"), 1)

    attended = matmul(context, full_output) + bias_output
    first, first_normed, first_recip = normalize(widen(inputs) + attended, gain_first, shift_first)
    first_low = lowered(first)
    biases = bias_inner.reshape(shards, 2, unit_half)
    halves = ((inner_own, outer_own, pick(biases, core, 1)), (inner_other, outer_other, pick(biases, 1 - core, 1)))
    outer, kept = bias_outer, []
    for inner_weight, outer_weight, bias in halves:
        inner = matmul(first_low, inner_weight) + bias.reshape(hidden // 2)
        active = lowered(gelu_value(inner))
        outer = outer + matmul(active, outer_weight)
        kept.append((inner, active))
    mixed, second_normed, second_recip = normalize(first + outer, gain_second, shift_second)
    mixed = lowered(mixed)

    upstream = widen(jnp.concatenate([cotangent_mine, cotangent_arrived], axis=0))
    pre_second, grad_second_gain, grad_second_shift = normalize_back(upstream, second_normed, second_recip, gain_second)
    grad_outer = lowered(pre_second)
    grad_b_outer = jnp.sum(widen(grad_outer), axis=0)
    grad_first, inner_grads, outer_grads, bias_grads = pre_second, [], [], []
    for (inner, active), (inner_weight, outer_weight, _) in zip(kept, halves):
        grad_inner = lowered(matmul_nt(grad_outer, outer_weight) * gelu_slope(inner))
        outer_grads.append(lowered(matmul_tn(active, grad_outer)))
        inner_grads.append(lowered(matmul_tn(first_low, grad_inner)))
        bias_grads.append(jnp.sum(widen(grad_inner), axis=0).reshape(shards, 1, unit_half))
        grad_first = grad_first + matmul_nt(grad_inner, inner_weight)
    grad_b_inner = in_order(core == 0, bias_grads[0], bias_grads[1], 1).reshape(hidden)
    pre_first, grad_first_gain, grad_first_shift = normalize_back(grad_first, first_normed, first_recip, gain_first)
    grad_attended = lowered(pre_first)
    grad_b_output = jnp.sum(widen(grad_attended), axis=0)
    grad_w_output = lowered(matmul_tn(context, grad_attended))
    grad_context = lowered(matmul_nt(grad_attended, full_output))
    context_mine = lax.dynamic_slice_in_dim(grad_context, core * half, half, 1)
    context_other = lax.dynamic_slice_in_dim(grad_context, (1 - core) * half, half, 1)
    upstream_other = swap(context_other, "core")

    def core_sum(own, other):
        return lowered(widen(own) + widen(swap(other, "core")))

    outer_term = core_sum(*outer_grads)
    inner_term = core_sum(*inner_grads)
    output_term = core_sum(
        lax.dynamic_slice_in_dim(grad_w_output, core * half, half, 1),
        lax.dynamic_slice_in_dim(grad_w_output, (1 - core) * half, half, 1),
    )
    outer_done = reduce_owned(outer_term.reshape(shards, unit_half, width))
    late_done = reduce_owned(jnp.concatenate([output_term, inner_term], axis=1).reshape(shards, own_rows, half + hidden // 2))

    grads, sums = attention_back(place, segments, projected, heads_mine, heads_other, context_mine, upstream_other, logsum)
    grad_early = lowered(matmul_tn(inputs_all, grads))
    partial = matmul_nt(grads, full_early)
    sums = sums.reshape(pairs, 8, 3, 128)[:, 0]
    blank = jnp.zeros((width,), jnp.float32)
    grad_b_query = lax.dynamic_update_slice(blank, sums[:, 0].reshape(half), (core * half,))
    grad_b_value = lax.dynamic_update_slice(blank, sums[:, 2].reshape(half), (core * half,))
    vector_grads = (
        grad_b_query,
        grad_b_value,
        grad_b_output,
        grad_first_gain,
        grad_first_shift,
        grad_b_inner,
        grad_b_outer,
        grad_second_gain,
        grad_second_shift,
    )
    flat_grads = jnp.concatenate([v.reshape(shards, -1) for v in vector_grads], axis=1)
    flat_grads = jnp.pad(flat_grads, ((0, 0), (0, extra * lanes - flat_grads.shape[1])))
    early_term = jnp.concatenate(
        [grad_early.reshape(shards, own_rows, lanes), lowered(flat_grads).reshape(shards, extra, lanes)], axis=1
    )
    early_done = reduce_owned(early_term)

    grad_inputs = pre_first + partial[:local] + widen(swap(lowered(partial[local:]), "core"))
    returned = widen(swap(lowered(grad_inputs[part:]), "y"))
    grad_tokens = in_order(y == 0, grad_inputs[None, :part], returned[None], 0)
    mixed_out = in_order(y == 0, mixed[None, :part], swap(mixed[part:], "y")[None], 0)

    def both(piece):
        return widen(swap(lowered(piece), "core"))

    early_matrix = early_done[:own_rows]
    early_full = in_order(
        core == 0, early_matrix.reshape(own_rows, pairs, 3, 128)[None], both(early_matrix).reshape(own_rows, pairs, 3, 128)[None], 0
    )
    early_full = early_full.transpose(3, 1, 0, 2, 4).reshape(3, own_rows, width)
    late_other = both(late_done)
    output_full = in_order(core == 0, late_done[:, :half], late_other[:, :half], 1)
    inner_full = in_order(
        core == 0,
        late_done[:, half:].reshape(own_rows, shards, 1, unit_half),
        late_other[:, half:].reshape(own_rows, shards, 1, unit_half),
        2,
    ).reshape(own_rows, hidden)
    outer_full = in_order(core == 0, outer_done, both(outer_done), 0)
    vector_part = early_done[own_rows:]
    vector_sums = (vector_part + swap(vector_part, "core")).reshape(extra * lanes)
    out_vectors, at = [], 0
    for size in sizes:
        out_vectors.append(vector_sums[at : at + size])
        at += size
    (
        done_b_query,
        done_b_value,
        done_b_output,
        done_first_gain,
        done_first_shift,
        done_b_inner,
        done_b_outer,
        done_second_gain,
        done_second_shift,
    ) = out_vectors
    return (
        mixed_out,
        grad_tokens,
        early_full[0],
        early_full[1],
        early_full[2],
        output_full,
        done_b_query,
        done_b_value,
        done_b_output,
        done_first_gain,
        done_first_shift,
        inner_full,
        done_b_inner,
        outer_full,
        done_b_outer,
        done_second_gain,
        done_second_shift,
    )


def body(
    tokens,
    segment_ids,
    w_query,
    w_key,
    w_value,
    w_output,
    b_query,
    b_value,
    b_output,
    first_gain,
    first_shift,
    w_inner,
    b_inner,
    w_outer,
    b_outer,
    second_gain,
    second_shift,
    cotangent,
):
    core, y = lax.axis_index("core"), lax.axis_index("y")
    size_z, size_x = lax.axis_size("z"), lax.axis_size("x")
    shards = size_z * size_x
    sequences, part, width = tokens.shape
    half = width // 2
    pairs = half // 128
    hidden = w_inner.shape[1]
    local = 2 * part
    own_rows = w_query.shape[0]
    lanes = 3 * half

    vectors = (b_query, b_value, b_output, first_gain, first_shift, b_inner, b_outer, second_gain, second_shift)
    sizes = [v.shape[0] for v in vectors]
    tokens_all, cotangent_all, early, inner_own, outer_own, rows, inner_row = entry(
        size_z, size_x, tokens, cotangent, w_query, w_key, w_value, w_inner, w_output, w_outer, vectors
    )
    inner_parts = [inner_own] + [shift(inner_own, "x", j) for j in range(1, size_x)]
    outer_parts = [outer_own] + [shift(outer_own, "z", k) for k in range(1, size_z)]
    inputs_all = tokens_all.reshape(4 * part, width)
    full_early = early.reshape(width, lanes)
    spot = jnp.arange(5, dtype=jnp.int32)
    place = jnp.where(spot < 4, ((spot % 2 != core) * 2 + (spot // 2 != y) * 1) * part, core)
    segments = pick(segment_ids, y)
    context_mine, context_other, logsum, projected = attention(place, segments, inputs_all, full_early, rows)
    made = dense_layer(
        size_z,
        size_x,
        inputs_all,
        context_mine,
        swap(context_other, "core"),
        cotangent_all.reshape(local, width),
        rows,
        inner_row,
        inner_parts,
        outer_parts,
    )
    mixed, pre_first, upstream_mine, upstream_send, dense_sums, inner_sums, grad_w_output = made[:7]
    inner_terms = [made[7]] + [shift(made[7 + k], "z", k) for k in range(1, size_z)]
    outer_terms = [made[7 + size_z]] + [shift(made[7 + size_z + j], "x", j) for j in range(1, size_x)]
    upstream_other = swap(upstream_send, "core")
    mixed_out = in_order(y == 0, mixed[None, :part], swap(mixed[part:], "y")[None], 0)

    grads, sums = attention_back(place, segments, projected, context_mine, context_other, upstream_mine, upstream_other, logsum)
    made = exit_call(
        size_z,
        size_x,
        grads,
        inputs_all,
        full_early,
        pre_first,
        grad_w_output.reshape(shards, own_rows, width),
        dense_sums,
        inner_sums,
        sums,
        inner_terms,
        outer_terms,
    )
    grad_tokens, grad_query, grad_key, grad_value, grad_output, grad_inner_full, grad_outer_full, *done = deliver(
        made[:7], made[7], sizes
    )
    done = [v.reshape(size) for v, size in zip(done, sizes)]
    return (
        mixed_out,
        grad_tokens,
        grad_query,
        grad_key,
        grad_value,
        grad_output,
        *done[:5],
        grad_inner_full,
        done[5],
        grad_outer_full,
        *done[6:],
    )


def layer(*arrays):
    if arrays[2].shape[0] % 32 == 0 and lax.axis_size("x") > 1:
        return body(*arrays)
    return plain_body(*arrays)


def solution(mesh):
    outer, inner = mesh.devices.shape
    size_z = 1
    while size_z * size_z < outer:
        size_z *= 2
    split = Mesh(mesh.devices.reshape(size_z, outer // size_z, inner // 2, 2), ("z", "x", "y", "core"))
    dp, seq = ("z", "x"), ("y", "core")
    activation, matrix, vector = P(dp, seq, None), P(dp, None), P(dp)
    return jax.shard_map(
        layer,
        mesh=split,
        in_specs=(
            activation,
            matrix,
            matrix,
            matrix,
            matrix,
            matrix,
            vector,
            vector,
            vector,
            vector,
            vector,
            matrix,
            vector,
            matrix,
            vector,
            vector,
            vector,
            activation,
        ),
        out_specs=(
            activation,
            activation,
            matrix,
            matrix,
            matrix,
            matrix,
            vector,
            vector,
            vector,
            vector,
            vector,
            matrix,
            vector,
            matrix,
            vector,
            vector,
            vector,
        ),
        check_vma=False,
    )
```

```python
import jax
import jax.numpy as jnp
from jax import lax
from jax.experimental import pallas as pl
from jax.experimental.pallas import tpu as pltpu
from jax.sharding import Mesh
from jax.sharding import PartitionSpec as P


HD = 64
EPS = 1e-12
ROOT_HALF = 0.7071067811865476
INV_ROOT_TAU = 0.3989422804014327

BLK = 256
BIG = -1.0e9
DOCUMENTS = 4


def dot_nn(a, b):
    return jnp.dot(a, b, preferred_element_type=jnp.float32)


def part_rows(place_ref, part, rows):
    return pl.ds(pl.multiple_of(place_ref[part], 128), rows)


def find_bounds(segment_ref, bound_ref):
    length = segment_ref.shape[0]
    bound_ref[0] = 0
    bound_ref[DOCUMENTS] = length
    for d in range(1, DOCUMENTS):

        def halve(_, span):
            low, high = span
            middle = (low + high) // 2
            below = segment_ref[jnp.minimum(middle, length - 1)] < d
            inside = low < high
            return (
                jnp.where(jnp.logical_and(inside, below), middle + 1, low),
                jnp.where(jnp.logical_and(inside, jnp.logical_not(below)), middle, high),
            )

        low, _ = lax.fori_loop(0, length.bit_length(), halve, (0, length))
        bound_ref[d] = low


def find_window(segment_ref, bound_ref, qb):
    length = segment_ref.shape[0]
    first = segment_ref[qb * BLK]
    last = segment_ref[qb * BLK + BLK - 1]
    start = bound_ref[first] // 128 * 128
    count = (bound_ref[last + 1] - start + BLK - 1) // BLK
    return jnp.minimum(start, length - count * BLK), count


def each_tile(count, step):
    def two(i, _):
        step(i * (2 * BLK), 2 * BLK)
        return 0

    lax.fori_loop(0, count // 2, two, 0)

    @pl.when(count % 2 == 1)
    def _():
        step((count - 1) * BLK, BLK)


def make_marks(row_ref, mark_query, mark_key):
    length = mark_key.shape[0]
    step = 512
    for b in range(length // step):
        rows = slice(b * step, (b + 1) * step)
        column = jnp.broadcast_to(row_ref[0:1, rows], (128, step)).T
        lane = lax.broadcasted_iota(jnp.int32, (step, 128), 1) % 64
        same = lane == column
        line = lax.broadcasted_iota(jnp.int32, (128, step), 0) % 64
        mark_query[:, rows] = jnp.where(line == row_ref[0:1, rows], 1.0, 0.0).astype(jnp.bfloat16)
        apart = jnp.logical_and(lane < DOCUMENTS, jnp.logical_not(same))
        mark_key[rows, :] = jnp.where(apart, BIG, 0.0).astype(jnp.bfloat16)


def forward_kernel(place_ref, segment_ref, row_ref, tokens_ref, weights_ref, bias_ref, *refs):
    mine_ref, other_ref, lse_ref, qkv_ref, q2, k2, vt, acc, top, tot, keep, mark_query, mark_key, bound_ref = refs
    length = qkv_ref.shape[0]
    blocks = length // BLK
    part = length // 4

    @pl.when(pl.program_id(0) == 0)
    def _():
        find_bounds(segment_ref, bound_ref)
        make_marks(row_ref, mark_query, mark_key)

    low = lax.broadcasted_iota(jnp.int32, (part, 128), 1) < 64
    for b in range(4):
        src = part_rows(place_ref, b, part)
        dst = slice(b * part, (b + 1) * part)
        made = dot_nn(tokens_ref[src, :], weights_ref[...])
        lanes = pl.ds(pl.multiple_of(place_ref[4] * (128 * pl.num_programs(0)) + pl.program_id(0) * 128, 128), 128)
        q = ((made[:, 0:128] + bias_ref[0:1, lanes]) * 0.125).astype(jnp.bfloat16)
        k = made[:, 128:256].astype(jnp.bfloat16)
        v = (made[:, 256:384] + bias_ref[1:2, lanes]).astype(jnp.bfloat16)
        qkv_ref[src, 0:128] = q
        qkv_ref[src, 128:256] = k
        qkv_ref[src, 256:384] = v
        nohk = mark_key[dst, :]
        turned = q.T
        q2[0, 0:64, dst] = turned[0:64]
        q2[0, 64:128, dst] = mark_query[64:128, dst]
        q2[1, 0:64, dst] = mark_query[0:64, dst]
        q2[1, 64:128, dst] = turned[64:128]
        k2[0, dst, :] = jnp.where(low, k, nohk)
        k2[1, dst, :] = jnp.where(low, nohk, k)
        vt[:, dst] = v.T
    lse_ref[...] = jnp.zeros_like(lse_ref)

    def row(qb, _):
        qs = pl.ds(pl.multiple_of(qb * BLK, BLK), BLK)
        start, count = find_window(segment_ref, bound_ref, qb)
        top[...] = jnp.full_like(top, -1.0e30)

        def fold(tile, function):
            return function(tile.reshape(tile.shape[0] // 8, 8, BLK), axis=0)

        def highest(first, size):
            keys = pl.ds(pl.multiple_of(start + first, 128), size)
            for h in range(2):
                st = dot_nn(k2[h, keys, :], q2[h, :, qs])
                keep[h, pl.ds(pl.multiple_of(first, BLK), size), :] = st
                top[h] = jnp.maximum(top[h], fold(st, jnp.max))

        def weigh(first, size, largest):
            keys = pl.ds(pl.multiple_of(start + first, 128), size)
            for h in range(2):
                rows = slice(64 * h, 64 * h + 64)
                st = keep[h, pl.ds(pl.multiple_of(first, BLK), size), :]
                p = jnp.exp(st - largest[h])
                tot[h] = tot[h] + fold(p, jnp.sum)
                acc[rows, :] = acc[rows, :] + dot_nn(vt[rows, keys], p.astype(jnp.bfloat16))

        def paired(step):
            each_tile(count, step)

        paired(highest)
        largest = [jnp.max(top[h], axis=0, keepdims=True) for h in range(2)]
        acc[...] = jnp.zeros_like(acc)
        tot[...] = jnp.zeros_like(tot)
        paired(lambda first, size: weigh(first, size, largest))
        for h in range(2):
            rows = slice(64 * h, 64 * h + 64)
            total = jnp.sum(tot[h], axis=0, keepdims=True)
            acc[rows, :] = acc[rows, :] / total
            lse_ref[h : h + 1, qs] = largest[h] + jnp.log(total)
        where = place_ref[qb * BLK // part] + qb * BLK % part
        result = acc[...].T.astype(jnp.bfloat16)

        @pl.when(where < 2 * part)
        def _():
            mine_ref[pl.ds(pl.multiple_of(where, BLK), BLK), :] = result

        @pl.when(where >= 2 * part)
        def _():
            other_ref[pl.ds(pl.multiple_of(where - 2 * part, BLK), BLK), :] = result

        return 0

    lax.fori_loop(0, blocks, row, 0)


def attention(place, segments, tokens, weights, biases):
    length, depth = tokens.shape
    width = weights.shape[1]
    pairs = width // 384
    rows = length // 2
    return pl.pallas_call(
        forward_kernel,
        out_shape=(
            jax.ShapeDtypeStruct((rows, pairs * 128), jnp.bfloat16),
            jax.ShapeDtypeStruct((rows, pairs * 128), jnp.bfloat16),
            jax.ShapeDtypeStruct((pairs * 8, length), jnp.float32),
            jax.ShapeDtypeStruct((length, width), jnp.bfloat16),
        ),
        grid_spec=pltpu.PrefetchScalarGridSpec(
            num_scalar_prefetch=2,
            grid=(pairs,),
            in_specs=[
                pl.BlockSpec((1, length), lambda p, *_: (0, 0)),
                pl.BlockSpec((length, depth), lambda p, *_: (0, 0)),
                pl.BlockSpec((depth, 384), lambda p, *_: (0, p)),
                pl.BlockSpec(biases.shape, lambda p, *_: (0, 0)),
            ],
            out_specs=[
                pl.BlockSpec((rows, 128), lambda p, *_: (0, p)),
                pl.BlockSpec((rows, 128), lambda p, *_: (0, p)),
                pl.BlockSpec((8, length), lambda p, *_: (p, 0)),
                pl.BlockSpec((length, 384), lambda p, *_: (0, p)),
            ],
            scratch_shapes=[
                pltpu.VMEM((2, 128, length), jnp.bfloat16),
                pltpu.VMEM((2, length, 128), jnp.bfloat16),
                pltpu.VMEM((128, length), jnp.bfloat16),
                pltpu.VMEM((128, BLK), jnp.float32),
                pltpu.VMEM((2, 8, BLK), jnp.float32),
                pltpu.VMEM((2, 8, BLK), jnp.float32),
                pltpu.VMEM((2, length, BLK), jnp.float32),
                pltpu.VMEM((128, length), jnp.bfloat16),
                pltpu.VMEM((length, 128), jnp.bfloat16),
                pltpu.SMEM((DOCUMENTS + 1,), jnp.int32),
            ],
        ),
        compiler_params=pltpu.CompilerParams(dimension_semantics=("arbitrary",), vmem_limit_bytes=60 << 20),
        cost_estimate=pl.CostEstimate(flops=pairs * 40_000_000_000, bytes_accessed=pairs * 3_000_000, transcendentals=pairs * 4_000_000),
        name="attention_forward",
    )(place, segments, segments.reshape(1, length), tokens, weights, biases)


def backward_kernel(
    place_ref,
    segment_ref,
    qkv_ref,
    ctx_mine_ref,
    ctx_other_ref,
    do_mine_ref,
    do_other_ref,
    lse_ref,
    row_ref,
    out_ref,
    sum_ref,
    q2,
    k2,
    q0,
    d0,
    dt,
    v0,
    kt,
    dk,
    dv,
    dqt,
    delta,
    mark_query,
    mark_key,
    bound_ref,
):
    length = qkv_ref.shape[0]
    blocks = length // BLK
    part = length // 4

    @pl.when(pl.program_id(0) == 0)
    def _():
        find_bounds(segment_ref, bound_ref)
        make_marks(row_ref, mark_query, mark_key)

    low = lax.broadcasted_iota(jnp.int32, (part, 128), 1) < 64

    def prepare(b, do, ctx):
        src = part_rows(place_ref, b, part)
        dst = slice(b * part, (b + 1) * part)
        q, k = qkv_ref[src, 0:128], qkv_ref[src, 128:256]
        zero = jnp.zeros_like(q)
        nohk = mark_key[dst, :]
        turned = q.T
        q2[0, 0:64, dst] = turned[0:64]
        q2[0, 64:128, dst] = mark_query[64:128, dst]
        q2[1, 0:64, dst] = mark_query[0:64, dst]
        q2[1, 64:128, dst] = turned[64:128]
        k2[0, dst, :] = jnp.where(low, k, nohk)
        k2[1, dst, :] = jnp.where(low, nohk, k)
        q0[0, dst, :] = jnp.where(low, q, zero)
        q0[1, dst, :] = jnp.where(low, zero, q)
        d0[0, dst, :] = jnp.where(low, do, zero)
        d0[1, dst, :] = jnp.where(low, zero, do)
        turned = do.T
        blank = jnp.zeros((64, part), jnp.bfloat16)
        dt[0, 0:64, dst] = turned[0:64]
        dt[0, 64:128, dst] = blank
        dt[1, 0:64, dst] = blank
        dt[1, 64:128, dst] = turned[64:128]
        v0[dst, :] = qkv_ref[src, 256:384]
        kt[:, dst] = k.T
        prod = turned.astype(jnp.float32) * ctx.T.astype(jnp.float32)
        delta[0:1, dst] = jnp.sum(prod[0:64], axis=0, keepdims=True)
        delta[1:2, dst] = jnp.sum(prod[64:128], axis=0, keepdims=True)

    for b in range(4):

        @pl.when(place_ref[b] < 2 * part)
        def _():
            rows = part_rows(place_ref, b, part)
            prepare(b, do_mine_ref[rows, :], ctx_mine_ref[rows, :])

        @pl.when(place_ref[b] >= 2 * part)
        def _():
            rows = pl.ds(pl.multiple_of(place_ref[b] - 2 * part, 128), part)
            prepare(b, do_other_ref[rows, :], ctx_other_ref[rows, :])

    dk[...] = jnp.zeros_like(dk)
    dv[...] = jnp.zeros_like(dv)
    dqt[...] = jnp.zeros_like(dqt)

    def row(qb, _):
        qs = pl.ds(pl.multiple_of(qb * BLK, BLK), BLK)
        start, count = find_window(segment_ref, bound_ref, qb)

        def tile(first, size):
            ks = pl.ds(pl.multiple_of(start + first, 128), size)
            weights, grads = [], []
            for h in range(2):
                st = dot_nn(k2[h, ks, :], q2[h, :, qs])
                w = jnp.exp(st - lse_ref[h : h + 1, qs])
                gw = dot_nn(v0[ks, :], dt[h, :, qs])
                weights.append(w.astype(jnp.bfloat16))
                grads.append((w * (gw - delta[h : h + 1, qs])).astype(jnp.bfloat16))
            dv[ks, :] += dot_nn(jnp.concatenate(weights, axis=1), jnp.concatenate([d0[0, qs, :], d0[1, qs, :]], axis=0))
            dk[ks, :] += dot_nn(jnp.concatenate(grads, axis=1), jnp.concatenate([q0[0, qs, :], q0[1, qs, :]], axis=0))
            for h in range(2):
                rows = slice(64 * h, 64 * h + 64)
                dqt[rows, qs] += dot_nn(kt[rows, ks], grads[h])

        each_tile(count, tile)
        return 0

    lax.fori_loop(0, blocks, row, 0)
    sums = [jnp.zeros((1, 128), jnp.float32) for _ in range(3)]
    for b in range(4):
        dst = part_rows(place_ref, b, part)
        src = slice(b * part, (b + 1) * part)
        pieces = ((dqt[:, src].T * 0.125).astype(jnp.bfloat16), dk[src, :].astype(jnp.bfloat16), dv[src, :].astype(jnp.bfloat16))
        for i, piece in enumerate(pieces):
            out_ref[dst, 128 * i : 128 * i + 128] = piece
            sums[i] = sums[i] + jnp.sum(piece.astype(jnp.float32), axis=0, keepdims=True)
    sum_ref[...] = jnp.zeros_like(sum_ref)
    for i in range(3):
        sum_ref[0:1, 128 * i : 128 * i + 128] = sums[i]


def attention_back(place, segments, qkv, ctx_mine, ctx_other, do_mine, do_other, lse):
    length, width = qkv.shape
    pairs = width // 384
    rows = length // 2
    half = lambda: pltpu.VMEM((2, length, 128), jnp.bfloat16)
    turned = lambda: pltpu.VMEM((2, 128, length), jnp.bfloat16)
    column = pl.BlockSpec((rows, 128), lambda p, *_: (0, p))
    return pl.pallas_call(
        backward_kernel,
        out_shape=(
            jax.ShapeDtypeStruct((length, width), jnp.bfloat16),
            jax.ShapeDtypeStruct((pairs * 8, 384), jnp.float32),
        ),
        grid_spec=pltpu.PrefetchScalarGridSpec(
            num_scalar_prefetch=2,
            grid=(pairs,),
            in_specs=[
                pl.BlockSpec((length, 384), lambda p, *_: (0, p)),
                column,
                column,
                column,
                column,
                pl.BlockSpec((8, length), lambda p, *_: (p, 0)),
                pl.BlockSpec((1, length), lambda p, *_: (0, 0)),
            ],
            out_specs=[
                pl.BlockSpec((length, 384), lambda p, *_: (0, p)),
                pl.BlockSpec((8, 384), lambda p, *_: (p, 0)),
            ],
            scratch_shapes=[
                turned(),
                half(),
                half(),
                half(),
                turned(),
                pltpu.VMEM((length, 128), jnp.bfloat16),
                pltpu.VMEM((128, length), jnp.bfloat16),
                pltpu.VMEM((length, 128), jnp.float32),
                pltpu.VMEM((length, 128), jnp.float32),
                pltpu.VMEM((128, length), jnp.float32),
                pltpu.VMEM((8, length), jnp.float32),
                pltpu.VMEM((128, length), jnp.bfloat16),
                pltpu.VMEM((length, 128), jnp.bfloat16),
                pltpu.SMEM((DOCUMENTS + 1,), jnp.int32),
            ],
        ),
        compiler_params=pltpu.CompilerParams(dimension_semantics=("arbitrary",), vmem_limit_bytes=60 << 20),
        cost_estimate=pl.CostEstimate(flops=pairs * 20_000_000_000, bytes_accessed=pairs * 5_000_000, transcendentals=pairs * 4_000_000),
        name="attention_backward",
    )(place, segments, qkv, ctx_mine, ctx_other, do_mine, do_other, lse, segments.reshape(1, length))


MESH_ID = pl.DeviceIdType.MESH
WIDE = 5


def place_of():
    return tuple(lax.axis_index(name) for name in ("z", "x", "y", "core"))


def sizes_of():
    return lax.axis_size("z"), lax.axis_size("x")


def partner(**moved):
    z, x, y, core = place_of()
    return (moved.get("z", z), moved.get("x", x), moved.get("y", y), moved.get("core", core))


def greet(with_grid):
    z, x, y, core = place_of()
    size_z, size_x = sizes_of()
    peers = [partner(y=1 - y), partner(core=1 - core)]
    if with_grid:
        peers += [partner(z=lax.rem(z + k, size_z)) for k in range(1, size_z)]
        peers += [partner(x=lax.rem(x + j, size_x)) for j in range(1, size_x)]
    barrier = pltpu.get_barrier_semaphore()
    for peer in peers:
        pl.semaphore_signal(barrier, inc=1, device_id=peer, device_id_type=MESH_ID)
    pl.semaphore_wait(barrier, len(peers))


def remote(src, dst, send, recv, peer):
    return pltpu.make_async_remote_copy(
        src_ref=src, dst_ref=dst, send_sem=send, recv_sem=recv, device_id=peer, device_id_type=MESH_ID
    )


def entry_kernel(size_z, size_x, count, *refs):
    tokens, cotangent, wq, wk, wv, w_inner, w_output, w_outer = refs[:8]
    vectors = refs[8 : 8 + count]
    tokens_all, cotangent_all, weights_all, inner_all, outer_all, rows_out, inner_out = refs[8 + count : 15 + count]
    raw = refs[15 + count : 15 + 2 * count]
    stage, cot_stage, wbuf, ibuf, obuf, pack, ipack, opack, vpack, vectors_all = refs[15 + 2 * count : 25 + 2 * count]
    local_sem, load_sem, tsend, trecv, zsend, zrecv, xsend, xrecv, osend, orecv = refs[25 + 2 * count :]
    z, x, y, core = place_of()
    half = pack.shape[1] // 3
    pairs = half // 128
    chunks = w_inner.shape[1] // CHUNK
    me = z * size_x + x
    columns = [lax.rem(x + j, size_x) for j in range(size_x)]

    mine = pl.ds(pl.multiple_of(core * half, 128), half)
    loads = [pltpu.make_async_copy(w.at[:, mine], wbuf.at[i], load_sem.at[i]) for i, w in enumerate((wq, wk, wv))]
    loads += [pltpu.make_async_copy(v, r, load_sem.at[3 + i]) for i, (v, r) in enumerate(zip(vectors, raw))]
    late = [
        pltpu.make_async_copy(
            w_inner.at[:, pl.ds(pl.multiple_of(c * CHUNK + core * half, 128), half)],
            ibuf.at[:, pl.ds(c * half, half)],
            load_sem.at[3 + count + c],
        )
        for c in range(chunks)
    ]
    late.append(pltpu.make_async_copy(w_output.at[:, mine], ibuf.at[:, pl.ds(chunks * half, half)], load_sem.at[3 + count + chunks]))
    late.append(pltpu.make_async_copy(w_outer.at[:, mine], obuf, load_sem.at[4 + count + chunks]))
    load = pltpu.make_async_copy(tokens.at[y], stage, local_sem.at[0])
    cot_load = pltpu.make_async_copy(cotangent.at[y], cot_stage, local_sem.at[4])
    for copy in loads + late + [load, cot_load]:
        copy.start()
    vpack[...] = jnp.zeros_like(vpack)
    for copy in loads:
        copy.wait()
    for i, vector in enumerate(raw):
        vpack[i : i + 1, 0 : vector.shape[1]] = vector[...].astype(jnp.bfloat16).astype(jnp.float32)
    for i in range(3):
        for p in range(pairs):
            pack[:, (3 * p + i) * 128 : (3 * p + i + 1) * 128] = wbuf[i, :, p * 128 : (p + 1) * 128].astype(jnp.bfloat16)
    vectors_all[me] = vpack[...]
    greet(True)

    across = remote(tokens.at[1 - y], tokens_all.at[1], tsend.at[0], trecv.at[0], partner(y=1 - y))
    across.start()
    beside = remote(tokens.at[y], tokens_all.at[2], tsend.at[1], trecv.at[1], partner(core=1 - core))

    packs = (pack, vpack, ipack)

    def home(stream, origin):
        if stream == 2:
            return inner_all.at[origin]
        return (weights_all, vectors_all)[stream].at[origin * size_x + x]

    def z_move(stream, way, t):
        step = 1 - 2 * way
        origin = z - step * (t - 1)
        src = packs[stream] if t == 1 else home(stream, origin)
        peer = partner(z=lax.rem(z + step + size_z, size_z))
        return remote(src, home(stream, origin), zsend.at[stream, way, t - 1], zrecv.at[stream, way, t - 1], peer)

    def sends(way, t):
        step = 1 - 2 * way
        origin, target = z - step * (t - 1), z + step
        inside = lambda v: jnp.logical_and(v >= 0, v < size_z)
        return jnp.logical_and(inside(origin), inside(target))

    def receives(way, t):
        origin = z - (1 - 2 * way) * t
        return jnp.logical_and(origin >= 0, origin < size_z)

    def x_moves(index, origin, own):
        moves = []
        for j in range(1, size_x):
            for stream in range(2):
                src = packs[stream] if own else home(stream, origin)
                moves.append(
                    remote(
                        src,
                        home(stream, origin),
                        xsend.at[stream, index, j - 1],
                        xrecv.at[stream, index, j - 1],
                        partner(x=columns[j]),
                    )
                )
        return moves

    def start_z(streams, t):
        for way in range(2):

            @pl.when(sends(way, t))
            def _():
                for stream in streams:
                    z_move(stream, way, t).start()

    for move in x_moves(0, z, True):
        move.start()
    start_z((0, 1), 1)
    beside.start()
    for copy in late:
        copy.wait()
    ipack[...] = ibuf[...].astype(jnp.bfloat16)
    opack[...] = obuf[...].astype(jnp.bfloat16)
    start_z((2,), 1)
    outer_moves = [
        remote(opack, outer_all.at[x], osend.at[j - 1], orecv.at[j - 1], partner(x=columns[j])) for j in range(1, size_x)
    ]
    keeps = [
        pltpu.make_async_copy(pack, weights_all.at[me], local_sem.at[1]),
        pltpu.make_async_copy(ipack, inner_all.at[z], local_sem.at[2]),
        pltpu.make_async_copy(opack, outer_all.at[x], local_sem.at[6]),
    ]
    load.wait()
    keeps.append(pltpu.make_async_copy(stage, tokens_all.at[0], local_sem.at[3]))
    cot_load.wait()
    keeps.append(pltpu.make_async_copy(cot_stage, cotangent_all.at[0], local_sem.at[5]))
    for keep in keeps:
        keep.start()

    def arrive(streams, t, sideways):
        for way in range(2):

            @pl.when(receives(way, t))
            def _():
                origin = z - (1 - 2 * way) * t
                for stream in streams:
                    slot = home(stream, origin)
                    remote(
                        slot, slot, zsend.at[stream, way, t - 1], zrecv.at[stream, way, t - 1], partner(core=1 - core)
                    ).wait_recv()
                if sideways:
                    for move in x_moves(1 + way * (size_z - 1) + t - 1, origin, False):
                        move.start()

    onward = remote(tokens_all.at[1], tokens_all.at[3], tsend.at[2], trecv.at[2], partner(core=1 - core))
    later = remote(cotangent.at[1 - y], cotangent_all.at[1], tsend.at[3], trecv.at[3], partner(y=1 - y))
    for t in range(1, size_z):
        arrive((0, 1), t, True)
        if t < size_z - 1:
            start_z((0, 1), t + 1)
        if t == 1:
            for move in outer_moves:
                move.start()
        arrive((2,), t, False)
        if t < size_z - 1:
            start_z((2,), t + 1)
        if t == min(2, size_z - 1):
            across.wait_recv()
            onward.start()
            later.start()

    for move in x_moves(0, z, True):
        move.wait()
    for t in range(1, size_z):
        for way in range(2):

            @pl.when(receives(way, t))
            def _():
                origin = z - (1 - 2 * way) * t
                for move in x_moves(1 + way * (size_z - 1) + t - 1, origin, False):
                    move.wait()

            @pl.when(sends(way, t))
            def _():
                for stream in range(3):
                    z_move(stream, way, t).wait_send()

    short = min(vector.shape[1] for vector in raw)
    longest = vpack.shape[1]
    for s in range(size_z * size_x):
        rows_out[:, s * short : (s + 1) * short] = vectors_all[s, :, 0:short]
        inner_out[:, s * longest : (s + 1) * longest] = vectors_all[s, WIDE : WIDE + 1, :]
    for move in outer_moves:
        move.wait()
    across.wait_send()
    beside.wait()
    onward.wait()
    later.wait()
    for keep in keeps:
        keep.wait()


def entry(size_z, size_x, tokens, cotangent, wq, wk, wv, w_inner, w_output, w_outer, vectors):
    _, part, width = tokens.shape
    rows = wq.shape[0]
    half = width // 2
    lanes = 3 * half
    hidden = w_inner.shape[1]
    long = w_outer.shape[0]
    mixed_lanes = hidden // 2 + half
    chunks = hidden // CHUNK
    longest = max(v.shape[0] for v in vectors)
    shards = size_z * size_x
    count = len(vectors)
    anywhere, vmem = pl.BlockSpec(memory_space=pl.ANY), pl.BlockSpec(memory_space=pltpu.VMEM)
    dma = pltpu.SemaphoreType.DMA
    low, high = jnp.bfloat16, jnp.float32
    side = size_x - 1
    return pl.pallas_call(
        lambda *refs: entry_kernel(size_z, size_x, count, *refs),
        out_shape=(
            jax.ShapeDtypeStruct((4, part, width), low),
            jax.ShapeDtypeStruct((2, part, width), low),
            jax.ShapeDtypeStruct((shards, rows, lanes), low),
            jax.ShapeDtypeStruct((size_z, rows, mixed_lanes), low),
            jax.ShapeDtypeStruct((size_x, long, half), low),
            jax.ShapeDtypeStruct((16, width), high),
            jax.ShapeDtypeStruct((1, shards * longest), high),
        ),
        in_specs=[anywhere] * (8 + count),
        out_specs=(anywhere,) * 5 + (vmem,) * 2,
        scratch_shapes=[pltpu.VMEM((1, v.shape[0]), v.dtype) for v in vectors]
        + [
            pltpu.VMEM((part, width), low),
            pltpu.VMEM((part, width), low),
            pltpu.VMEM((3, rows, half), high),
            pltpu.VMEM((rows, mixed_lanes), high),
            pltpu.VMEM((long, half), high),
            pltpu.VMEM((rows, lanes), low),
            pltpu.VMEM((rows, mixed_lanes), low),
            pltpu.VMEM((long, half), low),
            pltpu.VMEM((16, longest), high),
            pltpu.VMEM((shards, 16, longest), high),
            dma((7,)),
            dma((5 + count + chunks,)),
            dma((4,)),
            dma((4,)),
            dma((3, 2, size_z - 1)),
            dma((3, 2, size_z - 1)),
            dma((2, 2 * size_z - 1, side)),
            dma((2, 2 * size_z - 1, side)),
            dma((side,)),
            dma((side,)),
        ],
        compiler_params=pltpu.CompilerParams(collective_id=0, has_side_effects=True, vmem_limit_bytes=66_000_000),
        name="entry",
    )(tokens, cotangent, wq, wk, wv, w_inner, w_output, w_outer, *[v.reshape(1, -1) for v in vectors])


def exit_kernel(size_z, size_x, shapes, *refs):
    z, x, y, core = place_of()
    names = list(shapes)
    grads_hbm, inputs_hbm, weights_hbm, base_hbm, output_term, dense_sums, inner_sums, head_sums = refs[:8]
    inner_in = refs[8 : 8 + size_z]
    outer_in = refs[8 + size_z : 8 + size_z + size_x]
    refs = refs[8 + size_z + size_x :]
    results = refs[:8]
    token_grads, grad_query, grad_key, grad_value, grad_output, grad_inner, grad_outer, vector_sums = refs[8:16]
    grads, inputs, turned, weights, base, terms, other_rows, recv_rows, send_rows, far_rows, odd = refs[16:27]
    inner_buf, outer_buf, vector_rows, vector_terms, store_sem = refs[27:32]
    load_sem, tsend, trecv, osend, orecv = refs[32:37]
    refs = refs[37:]
    made = (token_grads, grad_query, grad_key, grad_value, grad_output, grad_inner, grad_outer, vector_sums)
    stores = [pltpu.make_async_copy(a, b, store_sem.at[i]) for i, (a, b) in enumerate(zip(made, results))]
    xin, xsend, xrecv, xout = {}, {}, {}, {}
    zout, zin, zsend, zrecv = {}, {}, {}, {}
    ybuf, ysend, yrecv, cbuf, csend, crecv = {}, {}, {}, {}, {}, {}
    refs = list(refs)
    for name in names:
        ybuf[name], ysend[name], yrecv[name], cbuf[name], csend[name], crecv[name] = [refs.pop(0) for _ in range(6)]
        if name != "outer":
            xin[name], xsend[name], xrecv[name] = [refs.pop(0) for _ in range(3)]
        if name != "inner":
            zout[name], zin[name], zsend[name], zrecv[name] = [refs.pop(0) for _ in range(4)]
    xout["inner"] = refs.pop(0)

    shards, rows, lanes = terms.shape
    half = lanes // 3
    width = 2 * half
    pairs = half // 128
    hidden = grad_inner.shape[1]
    part = token_grads.shape[1]
    local = 2 * part
    low, high = jnp.bfloat16, jnp.float32
    mine = pl.ds(pl.multiple_of(core * half, 128), half)
    theirs = pl.ds(pl.multiple_of((1 - core) * half, 128), half)
    order = sorted(range(size_z), key=lambda k: -min(k, size_z - k))
    far_order = [k for k in order if k > 0]
    columns = [lax.rem(x + j, size_x) for j in range(size_x)]

    def slot_of(k, j):
        return lax.rem(z + k, size_z) * size_x + columns[j]

    loads = {}
    for i, src in enumerate(inner_in):
        loads["inner", i] = pltpu.make_async_copy(src, inner_buf.at[i], load_sem.at[i])
    for i, src in enumerate(outer_in):
        loads["outer", i] = pltpu.make_async_copy(src, outer_buf.at[i], load_sem.at[size_z + i])
    for i, (name, src, dst) in enumerate(
        (("inputs", inputs_hbm, inputs), ("grads", grads_hbm, grads), ("weights", weights_hbm, weights), ("base", base_hbm, base))
    ):
        loads[name] = pltpu.make_async_copy(src, dst, load_sem.at[size_z + size_x + i])
    for load in loads.values():
        load.start()
    greet(True)

    core_peer, y_peer = partner(core=1 - core), partner(y=1 - y)
    outputs = remote(output_term.at[:, :, theirs], odd, osend, orecv, core_peer)
    outputs.start()
    sideways = {}
    along = {}
    kept = {}

    def send_x(name, n, k, j, src, dst):
        move = remote(src, dst, xsend[name].at[n, k, j - 1], xrecv[name].at[n, k, j - 1], partner(x=columns[j]))
        move.start()
        sideways.setdefault((name, k, j), []).append(move)

    def send_z(name, k):
        move = remote(
            zout[name].at[k - 1],
            zin[name].at[k - 1],
            zsend[name].at[k - 1],
            zrecv[name].at[k - 1],
            partner(z=lax.rem(z + k, size_z)),
        )
        move.start()
        along[name, k] = move

    vector_rows[...] = jnp.zeros_like(vector_rows)
    for i, row in enumerate((7, 8, 6, 3, 4, 2)):
        vector_rows[row : row + 1, :] = jnp.sum(dense_sums[8 * i : 8 * i + 8, :], axis=0, keepdims=True)
    for p in range(pairs):
        place = pl.ds(pl.multiple_of(core * half + p * 128, 128), 128)
        vector_rows[0:1, place] = head_sums[8 * p : 8 * p + 1, 0:128]
        vector_rows[1:2, place] = head_sums[8 * p : 8 * p + 1, 256:384]
    inner_row = jnp.sum(inner_sums[...], axis=0, keepdims=True)
    vector_terms[...] = jnp.zeros_like(vector_terms)
    longest = vector_terms.shape[2]
    for s in range(shards):
        vector_terms[s, :, 0:rows] = vector_rows[:, s * rows : (s + 1) * rows]
        vector_terms[s, WIDE : WIDE + 1, :] = inner_row[:, s * longest : (s + 1) * longest]
    for k in order:
        for j in range(1, size_x):
            send_x("vec", 0, k, j, vector_terms.at[slot_of(k, j)], xin["vec"].at[j - 1, k])

    for i in range(size_z):
        loads["inner", i].wait()
    for j in range(size_x):
        total = inner_buf[0, columns[j]].astype(high)
        for i in range(1, size_z):
            total = total + inner_buf[i, columns[j]].astype(high)
        if j == 0:
            kept["inner"] = total
        else:
            xout["inner"][j - 1] = total.astype(low)
            send_x("inner", 0, 0, j, xout["inner"].at[j - 1], xin["inner"].at[j - 1, 0])

    for i in range(size_x):
        loads["outer", i].wait()
    for k in order:
        target = lax.rem(z + k, size_z)
        total = outer_buf[0, target].astype(high)
        for i in range(1, size_x):
            total = total + outer_buf[i, target].astype(high)
        if k == 0:
            kept["outer"] = total
        else:
            zout["outer"][k - 1] = total.astype(low)
            send_z("outer", k)

    loads["inputs"].wait()
    for b in range(4):
        turned[:, b * part : (b + 1) * part] = inputs[b * part : (b + 1) * part, :].T
    loads["grads"].wait()
    group = 4
    for p in range(pairs):
        block = slice(p * 384, (p + 1) * 384)

        def some(m, _):
            value = dot_nn(turned[pl.ds(pl.multiple_of(m * group * rows, group * rows), group * rows), :], grads[:, block])
            terms[pl.ds(m * group, group), :, block] = value.reshape(group, rows, 384).astype(low)
            return 0

        lax.fori_loop(0, shards // group, some, 0)
        for k in order:
            for j in range(1, size_x):
                send_x("qkv", p, k, j, terms.at[slot_of(k, j), :, block], xin["qkv"].at[j - 1, k, :, block])

    loads["weights"].wait()
    strip = 256

    def product(first):
        at = pl.ds(pl.multiple_of(first, strip), strip)
        return dot_nt(grads[at, :], weights[...])

    def other_strip(i, _):
        other_rows[pl.ds(pl.multiple_of(i * strip, strip), strip), :] = product(local + i * strip).astype(low)
        return 0

    lax.fori_loop(0, local // strip, other_strip, 0)
    halves = remote(other_rows, recv_rows, tsend.at[0], trecv.at[0], core_peer)
    halves.start()
    outputs.wait()
    for k in order:
        for j in range(1, size_x):
            slot = slot_of(k, j)
            odd[slot] = (odd[slot].astype(high) + output_term[slot, :, mine].astype(high)).astype(low)
            send_x("out", 0, k, j, odd.at[slot], xin["out"].at[j - 1, k])
    loads["base"].wait()

    def own_strip(i, _):
        at = pl.ds(pl.multiple_of(i * strip, strip), strip)
        base[at, :] = base[at, :] + product(i * strip)
        return 0

    lax.fori_loop(0, local // strip, own_strip, 0)
    halves.wait()
    send_rows[...] = (base[part:local, :] + recv_rows[part:local, :].astype(high)).astype(low)
    back = remote(send_rows, far_rows, tsend.at[1], trecv.at[1], y_peer)
    back.start()
    token_grads[y] = base[0:part, :] + recv_rows[0:part, :].astype(high)

    across = {}
    swapped = {}

    def step_y(name):
        move = remote(ybuf[name].at[0], ybuf[name].at[1], ysend[name], yrecv[name], y_peer)
        move.start()
        across[name] = move

    def step_core(name):
        across[name].wait()
        cbuf[name][0] = ybuf[name][0].astype(high) + ybuf[name][1].astype(high)
        move = remote(cbuf[name].at[0], cbuf[name].at[1], csend[name], crecv[name], core_peer)
        move.start()
        swapped[name] = move

    def finish_x(name):
        for k in order:
            slot = slot_of(k, 0)
            if name == "qkv":
                total = terms[slot].astype(high)
            elif name == "out":
                total = odd[slot].astype(high) + output_term[slot, :, mine].astype(high)
            else:
                total = vector_terms[slot]
            for j in range(1, size_x):
                for move in sideways[name, k, j]:
                    move.wait()
                total = total + xin[name][j - 1, k].astype(high)
            if k == 0:
                kept[name] = total
            else:
                zout[name][k - 1] = total.astype(zout[name].dtype)
                send_z(name, k)

    def finish_z(name):
        total = kept[name]
        for k in far_order:
            along[name, k].wait()
            total = total + zin[name][k - 1].astype(high)
        ybuf[name][0] = total.astype(ybuf[name].dtype)
        step_y(name)

    total = kept["inner"]
    for j in range(1, size_x):
        for move in sideways["inner", 0, j]:
            move.wait()
        total = total + xin["inner"][j - 1, 0].astype(high)
    ybuf["inner"][0] = total.astype(low)
    step_y("inner")
    finish_x("vec")
    finish_x("qkv")
    finish_z("outer")
    step_core("inner")
    finish_x("out")
    finish_z("vec")
    step_core("outer")
    finish_z("qkv")
    finish_z("out")
    back.wait()
    token_grads[1 - y] = far_rows[...].astype(high)
    stores[0].start()
    step_core("vec")

    def finish_core(name):
        swapped[name].wait()
        return cbuf[name]

    buf = finish_core("inner")
    chunks = hidden // CHUNK
    for i in range(2):
        owner = core if i == 0 else 1 - core
        for c in range(chunks):
            place = pl.ds(pl.multiple_of(c * CHUNK + owner * half, 128), half)
            grad_inner[:, place] = buf[i, :, c * half : (c + 1) * half]
    stores[5].start()
    buf = finish_core("outer")
    for i in range(2):
        owner = core if i == 0 else 1 - core
        grad_outer[:, pl.ds(pl.multiple_of(owner * half, 128), half)] = buf[i]
    stores[6].start()
    step_core("qkv")
    step_core("out")
    buf = finish_core("vec")
    vector_sums[...] = buf[0] + buf[1]
    stores[7].start()
    buf = finish_core("qkv")
    for i in range(2):
        owner = core if i == 0 else 1 - core
        for p in range(pairs):
            place = pl.ds(pl.multiple_of(owner * half + p * 128, 128), 128)
            for n, out in enumerate((grad_query, grad_key, grad_value)):
                out[:, place] = buf[i, :, (3 * p + n) * 128 : (3 * p + n + 1) * 128]
    for i in (1, 2, 3):
        stores[i].start()
    buf = finish_core("out")
    for i in range(2):
        owner = core if i == 0 else 1 - core
        grad_output[:, pl.ds(pl.multiple_of(owner * half, 128), half)] = buf[i]
    stores[4].start()
    for store in stores:
        store.wait()


def deliver_kernel(count, *refs):
    sources, vectors, outs, sem = refs[:count], refs[count], refs[count + 1 : -1], refs[-1]
    copies = [pltpu.make_async_copy(src, dst, sem.at[i]) for i, (src, dst) in enumerate(zip(sources, outs))]
    for copy in copies:
        copy.start()
    for i, out in enumerate(outs[count:]):
        out[...] = vectors[i : i + 1, 0 : out.shape[1]]
    for copy in copies:
        copy.wait()


def deliver(matrices, vectors, sizes):
    count = len(matrices)
    vmem, anywhere = pl.BlockSpec(memory_space=pltpu.VMEM), pl.BlockSpec(memory_space=pl.ANY)
    return pl.pallas_call(
        lambda *refs: deliver_kernel(count, *refs),
        out_shape=tuple(jax.ShapeDtypeStruct(m.shape, m.dtype) for m in matrices)
        + tuple(jax.ShapeDtypeStruct((1, size), jnp.float32) for size in sizes),
        in_specs=[vmem] * (count + 1),
        out_specs=(anywhere,) * count + (vmem,) * len(sizes),
        scratch_shapes=[pltpu.SemaphoreType.DMA((count,))],
        compiler_params=pltpu.CompilerParams(vmem_limit_bytes=60_000_000),
        name="deliver",
    )(*matrices, vectors)


def exit_call(size_z, size_x, grads, inputs, weights, base, output_term, dense_sums, inner_sums, head_sums, inner_terms, outer_terms):
    shards, rows, width = output_term.shape
    lanes = grads.shape[1]
    half = width // 2
    pairs = half // 128
    length = inputs.shape[0]
    local = length // 2
    part = local // 2
    long = outer_terms[0].shape[1]
    hidden = 2 * inner_terms[0].shape[2]
    vmem, anywhere = pl.BlockSpec(memory_space=pltpu.VMEM), pl.BlockSpec(memory_space=pl.ANY)
    dma = pltpu.SemaphoreType.DMA
    side = size_x - 1
    low, high = jnp.bfloat16, jnp.float32
    vector_shape = (16, hidden // shards)
    shapes = {
        "vec": (vector_shape, high, 1),
        "qkv": ((rows, lanes), low, pairs),
        "out": ((rows, half), low, 1),
        "inner": ((rows, hidden // 2), low, 1),
        "outer": ((long, half), low, 1),
    }
    matrix = jax.ShapeDtypeStruct((rows, width), high)
    results = (
        jax.ShapeDtypeStruct((2, part, width), high),
        matrix,
        matrix,
        matrix,
        matrix,
        jax.ShapeDtypeStruct((rows, hidden), high),
        jax.ShapeDtypeStruct((long, width), high),
        jax.ShapeDtypeStruct(vector_shape, high),
    )
    scratch = [pltpu.VMEM(r.shape, r.dtype) for r in results] + [
        pltpu.VMEM((length, lanes), low),
        pltpu.VMEM((length, width), low),
        pltpu.VMEM((width, length), low),
        pltpu.VMEM((width, lanes), low),
        pltpu.VMEM((local, width), high),
        pltpu.VMEM((shards, rows, lanes), low),
        pltpu.VMEM((local, width), low),
        pltpu.VMEM((local, width), low),
        pltpu.VMEM((part, width), low),
        pltpu.VMEM((part, width), low),
        pltpu.VMEM((shards, rows, half), low),
        pltpu.VMEM((size_z,) + inner_terms[0].shape, low),
        pltpu.VMEM((size_x,) + outer_terms[0].shape, low),
        pltpu.VMEM((16, width), high),
        pltpu.VMEM((shards,) + vector_shape, high),
        dma((len(results),)),
        dma((size_z + size_x + 4,)),
        dma((2,)),
        dma((2,)),
        dma,
        dma,
    ]
    for name, (shape, kind, sends) in shapes.items():
        scratch += [pltpu.VMEM((2,) + shape, kind), dma, dma, pltpu.VMEM((2,) + shape, high), dma, dma]
        stages = 1 if name == "inner" else size_z
        if name != "outer":
            scratch += [pltpu.VMEM((side, stages) + shape, kind), dma((sends, stages, side)), dma((sends, stages, side))]
        if name != "inner":
            scratch += [pltpu.VMEM((size_z - 1,) + shape, kind)] * 2 + [dma((size_z - 1,))] * 2
    scratch.append(pltpu.VMEM((side, rows, hidden // 2), low))
    return pl.pallas_call(
        lambda *refs: exit_kernel(size_z, size_x, shapes, *refs),
        out_shape=results,
        in_specs=[anywhere] * 4 + [vmem] * 4 + [anywhere] * (size_z + size_x),
        out_specs=(anywhere,) * len(results),
        scratch_shapes=scratch,
        compiler_params=pltpu.CompilerParams(collective_id=1, has_side_effects=True, vmem_limit_bytes=67_000_000),
        name="exit",
    )(grads, inputs, weights, base, output_term, dense_sums, inner_sums, head_sums, *inner_terms, *outer_terms)


TILE = 256
CHUNK = 768


def dot_nt(a, b):
    return lax.dot_general(a, b, (((1,), (1,)), ((), ())), preferred_element_type=jnp.float32)


def row_mean(value):
    return jnp.sum(value, axis=-1, keepdims=True) * (1.0 / value.shape[-1])


def standardize(hidden):
    centred = hidden - row_mean(hidden)
    reciprocal = lax.rsqrt(row_mean(centred * centred) + EPS)
    return centred * reciprocal, reciprocal


def column_sum(value):
    return jnp.sum(value.reshape(value.shape[0] // 8, 8, value.shape[1]), axis=0)


def dense_kernel(
    size_z,
    size_x,
    tokens_ref,
    mine_ref,
    other_hbm,
    cot_ref,
    vectors_ref,
    bias_inner_ref,
    *refs,
):
    inner_parts, outer_parts = refs[:size_x], refs[size_x : size_x + size_z]
    refs = refs[size_x + size_z :]
    mixed_ref, pre_first_ref, grad_mine_ref, grad_far_hbm, sums_ref, inner_sum_ref, grad_output_ref = refs[:7]
    inner_terms = refs[7 : 7 + size_z]
    outer_terms = refs[7 + size_z : 7 + size_z + size_x]
    refs = refs[7 + size_z + size_x :]
    w_output, w_inner, w_outer, a_output, a_inner, a_outer, grad_out_buf = refs[:7]
    context, first_low, turned_low, normed, first, slope, active, work = refs[7:15]
    send_inner, send_outer, recv_inner, recv_outer = refs[15:19]
    far_rows, grad_send, swap_send, swap_recv = refs[19:23]
    load_sem, share_send, share_recv, send_sem, recv_sem, store_sem = refs[23:]
    step, steps = pl.program_id(0), pl.num_programs(0)
    core_here = lax.axis_index("core")
    width, hidden = w_inner.shape
    half = width // 2
    chunks = hidden // CHUNK
    shards = size_z * size_x
    z, x, y, _ = place_of()
    twin = partner(core=1 - lax.axis_index("core"))

    shard = width // shards
    long = hidden // shards
    group = CHUNK // long // size_x

    def columns_of(first, owner):
        return pl.ds(pl.multiple_of(first + owner * half, 128), half)

    def start_piece(i, src, dst):
        pltpu.make_async_copy(src, dst, load_sem.at[i]).start()
        remote(src, dst, share_send.at[i], share_recv.at[i], twin).start()

    def start_rows(i, lane, ref, first):
        for j in range(size_x):
            for at in range(size_z):
                slot = at * size_x + lax.rem(x - j + size_x, size_x)
                rows = pl.ds(pl.multiple_of(slot * shard, shard), shard)
                start_piece(i, inner_parts[j].at[at, :, pl.ds(lane, half)], ref.at[rows, columns_of(first, core_here)])

    def start_loads():
        start_rows(0, hidden // 2, w_output, 0)
        for c in range(chunks):
            start_rows(1 + 2 * c, c * half, w_inner, c * CHUNK)
            for at in range(c * group, (c + 1) * group):
                for k in range(size_z):

                    @pl.when(lax.rem(z - k + size_z, size_z) == at)
                    def _():
                        for column in range(size_x):
                            rows = pl.ds((at * size_x + column) * long, long)
                            start_piece(2 + 2 * c, outer_parts[k].at[column], w_outer.at[rows, columns_of(0, core_here)])

    def wait_load(i, ref, rows, first):
        own, far = ref.at[rows, columns_of(first, core_here)], ref.at[rows, columns_of(first, 1 - core_here)]
        pltpu.make_async_copy(own, own, load_sem.at[i]).wait()
        remote(own, far, share_send.at[i], share_recv.at[i], twin).wait()

    @pl.when(step == 0)
    def _():
        barrier = pltpu.get_barrier_semaphore()
        pl.semaphore_signal(barrier, inc=1, device_id=twin, device_id_type=MESH_ID)
        pl.semaphore_wait(barrier, 1)
        remote(other_hbm, far_rows, swap_send.at[0], swap_recv.at[0], twin).start()
        start_loads()
        a_output[...] = jnp.zeros_like(a_output)
        a_inner[...] = jnp.zeros_like(a_inner)
        a_outer[...] = jnp.zeros_like(a_outer)
        sums_ref[...] = jnp.zeros_like(sums_ref)
        inner_sum_ref[...] = jnp.zeros_like(inner_sum_ref)

    def vector(i):
        row = (2, 3, 4, 6, 7, 8)[i]
        return vectors_ref[row : row + 1, :]

    def add_sum(i, value):
        sums_ref[8 * i : 8 * i + 8, :] += column_sum(value)

    context[:, pl.ds(pl.multiple_of(core_here * half, 128), half)] = mine_ref[...]

    context_move = remote(other_hbm, far_rows, swap_send.at[0], swap_recv.at[0], twin)

    @pl.when(step == 0)
    def _():
        context_move.wait()

    here = pl.ds(pl.multiple_of(step * TILE, TILE), TILE)
    context[:, pl.ds(pl.multiple_of((1 - core_here) * half, 128), half)] = far_rows[here, :]

    @pl.when(step == 0)
    def _():
        wait_load(0, w_output, slice(None), 0)

    hidden_rows = tokens_ref[...].astype(jnp.float32) + (dot_nn(context[...], w_output[...]) + vector(0))
    normed[...], first_recip = standardize(hidden_rows)
    first[...] = normed[...] * vector(1) + vector(2)
    first_low[...] = first[...].astype(jnp.bfloat16)
    turned_low[...] = first_low[...].T
    work[...] = jnp.broadcast_to(vector(3), work.shape)

    def part(c):
        return pl.ds(pl.multiple_of(c * CHUNK, CHUNK), CHUNK)

    def exchange(c):
        return (
            remote(send_inner.at[c], recv_inner.at[c], send_sem.at[0, c], recv_sem.at[0, c], twin),
            remote(send_outer.at[c], recv_outer.at[c], send_sem.at[1, c], recv_sem.at[1, c], twin),
        )

    def forward(c):
        @pl.when(step == 0)
        def _():
            wait_load(1 + 2 * c, w_inner, slice(None), c * CHUNK)

        u = dot_nn(first_low[...], w_inner[:, part(c)]) + bias_inner_ref[0:1, part(c)]
        cdf = 0.5 * (1.0 + lax.erf(u * ROOT_HALF))
        slope[:, part(c)] = cdf + u * jnp.exp(-0.5 * u * u) * INV_ROOT_TAU
        active[:, part(c)] = (u * cdf).astype(jnp.bfloat16)

        @pl.when(step == 0)
        def _():
            wait_load(2 + 2 * c, w_outer, part(c), 0)

        work[...] += dot_nn(active[:, part(c)], w_outer[part(c), :])

    for c in range(chunks):
        forward(c)
    second, second_recip = standardize(first[...] + work[...])
    mixed_ref[...] = (second * vector(4) + vector(5)).astype(jnp.bfloat16)
    upstream = cot_ref[...].astype(jnp.float32)
    add_sum(0, upstream * second)
    add_sum(1, upstream)
    scaled = upstream * vector(4)
    pre_second = second_recip * (scaled - row_mean(scaled) - second * row_mean(scaled * second))
    grad_outer = pre_second.astype(jnp.bfloat16)
    add_sum(2, grad_outer.astype(jnp.float32))
    work[...] = pre_second
    grad_out_buf[...] = grad_outer

    def backward(c, _):
        grad_out = grad_out_buf[...]
        grad = dot_nt(grad_out, w_outer[part(c), :])
        grad_inner = (grad * slope[:, part(c)]).astype(jnp.bfloat16)
        inner_sum_ref[:, part(c)] += column_sum(grad_inner.astype(jnp.float32))
        a_outer[part(c), :] += dot_nn(active[:, part(c)].T, grad_out)
        a_inner[:, part(c)] += dot_nn(turned_low[...], grad_inner)
        work[...] += dot_nt(grad_inner, w_inner[:, part(c)])

        @pl.when(step == steps - 1)
        def _():
            theirs = pl.multiple_of(c * CHUNK + (1 - core_here) * half, 128)
            send_inner[c] = a_inner[:, pl.ds(theirs, half)].astype(jnp.bfloat16)
            send_outer[c] = a_outer[part(c), pl.ds(pl.multiple_of((1 - core_here) * half, 128), half)].astype(jnp.bfloat16)
            for move in exchange(c):
                move.start()

        return 0

    lax.fori_loop(0, chunks, backward, 0)
    grad_first = work[...]
    add_sum(3, grad_first * normed[...])
    add_sum(4, grad_first)
    scaled = grad_first * vector(1)
    pre_first = first_recip * (scaled - row_mean(scaled) - normed[...] * row_mean(scaled * normed[...]))
    pre_first_ref[...] = pre_first
    grad_attended = pre_first.astype(jnp.bfloat16)
    add_sum(5, grad_attended.astype(jnp.float32))
    a_output[...] += dot_nn(context[...].T, grad_attended)
    context[...] = dot_nt(grad_attended, w_output[...]).astype(jnp.bfloat16)
    grad_mine_ref[...] = context[:, pl.ds(pl.multiple_of(core_here * half, 128), half)]

    def grad_move(t):
        rows = pl.ds(pl.multiple_of(t * TILE, TILE), TILE)
        return remote(grad_send.at[t], grad_far_hbm.at[rows, :], swap_send.at[1 + t], swap_recv.at[1 + t], twin)

    grad_send[step] = context[:, pl.ds(pl.multiple_of((1 - core_here) * half, 128), half)]
    grad_move(step).start()

    @pl.when(step == steps - 1)
    def _():
        grad_output_ref[...] = a_output[...].astype(jnp.bfloat16)

        def inner_out(c):
            copies = []
            for k in range(size_z):
                for column in range(size_x):
                    slot = lax.rem(z + k, size_z) * size_x + column
                    src = send_inner.at[c, pl.ds(pl.multiple_of(slot * shard, shard), shard), :]
                    copies.append(
                        pltpu.make_async_copy(src, inner_terms[k].at[column, :, pl.ds(c * half, half)], store_sem.at[0, c])
                    )
            return copies

        def outer_out(c):
            copies = []
            for i in range(group):
                for j in range(size_x):
                    src = send_outer.at[c, pl.ds(pl.multiple_of((i * size_x + lax.rem(x + j, size_x)) * long, long), long), :]
                    copies.append(pltpu.make_async_copy(src, outer_terms[j].at[c * group + i], store_sem.at[1, c]))
            return copies

        for c in range(chunks):
            ours = pl.multiple_of(c * CHUNK + core_here * half, 128)
            first_move, second_move = exchange(c)
            first_move.wait()
            send_inner[c] = (a_inner[:, pl.ds(ours, half)] + recv_inner[c].astype(jnp.float32)).astype(jnp.bfloat16)
            for copy in inner_out(c):
                copy.start()
            second_move.wait()
            columns = pl.ds(pl.multiple_of(core_here * half, 128), half)
            send_outer[c] = (a_outer[part(c), columns] + recv_outer[c].astype(jnp.float32)).astype(jnp.bfloat16)
            for copy in outer_out(c):
                copy.start()
        for t in range(grad_send.shape[0]):
            grad_move(t).wait()
        for c in range(chunks):
            pltpu.make_async_copy(send_inner.at[c], send_inner.at[c], store_sem.at[0, c]).wait()
            pltpu.make_async_copy(send_outer.at[c], send_outer.at[c], store_sem.at[1, c]).wait()


def dense_layer(size_z, size_x, tokens, mine, other, cotangent, vectors, bias_inner, inner_parts, outer_parts):
    local, half = mine.shape
    width = 2 * half
    hidden = bias_inner.shape[1]
    steps = local // TILE
    shards = size_z * size_x
    chunks = hidden // CHUNK
    low, high = jnp.bfloat16, jnp.float32
    tile = pl.BlockSpec((TILE, width), lambda t, *_: (t, 0))
    half_tile = pl.BlockSpec((TILE, half), lambda t, *_: (t, 0))
    anywhere = pl.BlockSpec(memory_space=pl.ANY)

    def whole(shape):
        return pl.BlockSpec(shape, lambda t, *_: (0, 0))

    inner_shape = jax.ShapeDtypeStruct((size_x, width // shards, hidden // 2), low)
    outer_shape = jax.ShapeDtypeStruct((size_z, hidden // shards, half), low)
    halves = pltpu.VMEM((chunks, width, half), low)
    dma = pltpu.SemaphoreType.DMA
    return pl.pallas_call(
        lambda *refs: dense_kernel(size_z, size_x, *refs),
        out_shape=(
            jax.ShapeDtypeStruct((local, width), low),
            jax.ShapeDtypeStruct((local, width), high),
            jax.ShapeDtypeStruct((local, half), low),
            jax.ShapeDtypeStruct((local, half), low),
            jax.ShapeDtypeStruct((48, width), high),
            jax.ShapeDtypeStruct((8, hidden), high),
            jax.ShapeDtypeStruct((width, width), low),
        )
        + (inner_shape,) * size_z
        + (outer_shape,) * size_x,
        grid_spec=pltpu.PrefetchScalarGridSpec(
            num_scalar_prefetch=0,
            grid=(steps,),
            in_specs=[
                tile,
                half_tile,
                anywhere,
                tile,
                whole((16, width)),
                whole((1, hidden)),
            ]
            + [anywhere] * (size_x + size_z),
            out_specs=[
                tile,
                tile,
                half_tile,
                anywhere,
                whole((48, width)),
                whole((8, hidden)),
                whole((width, width)),
            ]
            + [anywhere] * (size_z + size_x),
            scratch_shapes=[
                pltpu.VMEM((width, width), low),
                pltpu.VMEM((width, hidden), low),
                pltpu.VMEM((hidden, width), low),
                pltpu.VMEM((width, width), high),
                pltpu.VMEM((width, hidden), high),
                pltpu.VMEM((hidden, width), high),
                pltpu.VMEM((TILE, width), low),
                pltpu.VMEM((TILE, width), low),
                pltpu.VMEM((TILE, width), low),
                pltpu.VMEM((width, TILE), low),
                pltpu.VMEM((TILE, width), high),
                pltpu.VMEM((TILE, width), high),
                pltpu.VMEM((TILE, hidden), high),
                pltpu.VMEM((TILE, hidden), low),
                pltpu.VMEM((TILE, width), high),
                halves,
                halves,
                halves,
                halves,
                pltpu.VMEM((local, half), low),
                pltpu.VMEM((steps, TILE, half), low),
                dma((1 + steps,)),
                dma((1 + steps,)),
                dma((1 + 2 * chunks,)),
                dma((1 + 2 * chunks,)),
                dma((1 + 2 * chunks,)),
                dma((2, chunks)),
                dma((2, chunks)),
                dma((2, chunks)),
            ],
        ),
        compiler_params=pltpu.CompilerParams(
            dimension_semantics=("arbitrary",), vmem_limit_bytes=67_000_000, collective_id=3, has_side_effects=True
        ),
        cost_estimate=pl.CostEstimate(flops=32_000_000_000, bytes_accessed=40_000_000, transcendentals=6_000_000),
        name="dense_layer",
    )(tokens, mine, other, cotangent, vectors, bias_inner, *inner_parts, *outer_parts)


def lowered(piece):
    return piece.astype(jnp.bfloat16)


def widen(piece):
    return piece.astype(jnp.float32)


def matmul(left, right):
    return jnp.dot(left, right, preferred_element_type=jnp.float32)


def matmul_tn(left, right):
    return lax.dot_general(
        left, right, (((0,), (0,)), ((), ())), preferred_element_type=jnp.float32
    )


def matmul_nt(left, right):
    return lax.dot_general(
        left, right, (((1,), (1,)), ((), ())), preferred_element_type=jnp.float32
    )


def normalize(hidden, norm_gain, norm_shift):
    centred = hidden - jnp.mean(hidden, axis=-1, keepdims=True)
    reciprocal = lax.rsqrt(jnp.mean(centred * centred, axis=-1, keepdims=True) + EPS)
    normed = centred * reciprocal
    return (normed * norm_gain + norm_shift, normed, reciprocal)


def normalize_back(upstream, normed, reciprocal, norm_gain):
    scaled = upstream * norm_gain
    result = reciprocal * (
        scaled
        - jnp.mean(scaled, axis=-1, keepdims=True)
        - normed * jnp.mean(scaled * normed, axis=-1, keepdims=True)
    )
    return (result, jnp.sum(upstream * normed, axis=0), jnp.sum(upstream, axis=0))


def gelu_value(values_in):
    return 0.5 * values_in * (1.0 + lax.erf(values_in * ROOT_HALF))


def gelu_slope(values_in):
    return (
        0.5 * (1.0 + lax.erf(values_in * ROOT_HALF))
        + values_in * jnp.exp(-0.5 * values_in * values_in) * INV_ROOT_TAU
    )


def shift(piece, axis, step):
    size = lax.axis_size(axis)
    return lax.ppermute(piece, axis, [(i, (i + step) % size) for i in range(size)])


def swap(piece, axis):
    return lax.ppermute(piece, axis, [(0, 1), (1, 0)])


def pick(piece, index, axis=0):
    return lax.dynamic_index_in_dim(piece, index, axis, keepdims=False)


def in_order(first_is_zero, own, other, axis):
    return jnp.where(
        first_is_zero,
        jnp.concatenate([own, other], axis),
        jnp.concatenate([other, own], axis),
    )


def collect(piece):
    size_z, size_x = lax.axis_size("z"), lax.axis_size("x")
    z, x = lax.axis_index("z"), lax.axis_index("x")
    along_z = [piece] + [shift(piece, "z", k) for k in range(1, size_z)]
    whole = jnp.zeros((size_z, size_x) + piece.shape, piece.dtype)
    zeros = (0,) * piece.ndim
    for j in range(size_x):
        for k in range(size_z):
            arrived = along_z[k] if j == 0 else shift(along_z[k], "x", j)
            place = ((z - k) % size_z, (x - j) % size_x) + zeros
            whole = lax.dynamic_update_slice(whole, arrived[None, None], place)
    return whole.reshape((size_z * size_x,) + piece.shape)


def reduce_owned(terms):
    size_z, size_x = lax.axis_size("z"), lax.axis_size("x")
    z, x = lax.axis_index("z"), lax.axis_index("x")
    terms = terms.reshape((size_z, size_x) + terms.shape[1:])
    total = widen(pick(terms, x, 1))
    for j in range(1, size_x):
        total = total + widen(shift(pick(terms, (x + j) % size_x, 1), "x", j))
    terms = lowered(total)
    total = widen(pick(terms, z))
    for k in range(1, size_z):
        total = total + widen(shift(pick(terms, (z + k) % size_z), "z", k))
    terms = lowered(total)
    return widen(terms) + widen(swap(terms, "y"))


def plain_body(
    tokens,
    segment_ids,
    w_query,
    w_key,
    w_value,
    w_output,
    b_query,
    b_value,
    b_output,
    first_gain,
    first_shift,
    w_inner,
    b_inner,
    w_outer,
    b_outer,
    second_gain,
    second_shift,
    cotangent,
):
    core, y = lax.axis_index("core"), lax.axis_index("y")
    shards = lax.axis_size("z") * lax.axis_size("x")
    sequences, part, width = tokens.shape
    half = width // 2
    pairs = half // 128
    hidden = w_inner.shape[1]
    local = 2 * part
    own_rows = w_query.shape[0]
    unit_half = hidden // shards // 2

    def columns(matrix):
        return lowered(lax.dynamic_slice_in_dim(matrix, core * half, half, 1))

    vectors = (b_query, b_value, b_output, first_gain, first_shift, b_inner, b_outer, second_gain, second_shift)
    flat = jnp.concatenate([lowered(v) for v in vectors])
    lanes = 3 * half
    extra = -(-flat.shape[0] // lanes)
    flat = jnp.pad(flat, (0, extra * lanes - flat.shape[0])).reshape(extra, lanes)
    weights = jnp.stack([columns(w).reshape(own_rows, pairs, 128) for w in (w_query, w_key, w_value)], axis=2)
    early = collect(jnp.concatenate([weights.reshape(own_rows, lanes), flat], axis=0))

    mine = pick(tokens, y)
    arrived = swap(pick(tokens, 1 - y), "y")
    mine_other, arrived_other = swap(mine, "core"), swap(arrived, "core")
    inputs_all = jnp.concatenate([mine, arrived, mine_other, arrived_other], axis=0)
    inputs = jnp.concatenate([mine, arrived], axis=0)

    inner_piece = lowered(pick(w_inner.reshape(own_rows, shards, 2, unit_half), core, 2)).reshape(own_rows, hidden // 2)
    late = collect(jnp.concatenate([columns(w_output), inner_piece], axis=1)).reshape(width, half + hidden // 2)
    outer_own = collect(lowered(lax.dynamic_slice_in_dim(w_outer, core * unit_half, unit_half, 0))).reshape(hidden // 2, width)
    output_own, inner_own = late[:, :half], late[:, half:]
    output_other, inner_other, outer_other = swap(output_own, "core"), swap(inner_own, "core"), swap(outer_own, "core")
    full_output = in_order(core == 0, output_own, output_other, 1)
    cotangent_mine = pick(cotangent, y)
    cotangent_arrived = swap(pick(cotangent, 1 - y), "y")

    full_early = early[:, :own_rows].reshape(width, lanes)
    flat_all = early[:, own_rows:].reshape(shards, extra * lanes)
    sizes = [v.shape[0] for v in vectors]
    gathered, at = [], 0
    for size in sizes:
        gathered.append(flat_all[:, at : at + size].reshape(shards * size))
        at += size
    bias_query, bias_value, bias_output, gain_first, shift_first, bias_inner, bias_outer, gain_second, shift_second = [
        widen(v) for v in gathered
    ]
    spot = jnp.arange(5, dtype=jnp.int32)
    place = jnp.where(spot < 4, ((spot % 2 != core) * 2 + (spot // 2 != y) * 1) * part, core)
    segments = pick(segment_ids, y)
    biases = jnp.concatenate([bias_query[None], bias_value[None], jnp.zeros((14, width), jnp.float32)], axis=0)
    heads_mine, heads_other, logsum, projected = attention(place, segments, inputs_all, full_early, biases)
    context = in_order(core == 0, heads_mine, swap(heads_other, "core"), 1)

    attended = matmul(context, full_output) + bias_output
    first, first_normed, first_recip = normalize(widen(inputs) + attended, gain_first, shift_first)
    first_low = lowered(first)
    biases = bias_inner.reshape(shards, 2, unit_half)
    halves = ((inner_own, outer_own, pick(biases, core, 1)), (inner_other, outer_other, pick(biases, 1 - core, 1)))
    outer, kept = bias_outer, []
    for inner_weight, outer_weight, bias in halves:
        inner = matmul(first_low, inner_weight) + bias.reshape(hidden // 2)
        active = lowered(gelu_value(inner))
        outer = outer + matmul(active, outer_weight)
        kept.append((inner, active))
    mixed, second_normed, second_recip = normalize(first + outer, gain_second, shift_second)
    mixed = lowered(mixed)

    upstream = widen(jnp.concatenate([cotangent_mine, cotangent_arrived], axis=0))
    pre_second, grad_second_gain, grad_second_shift = normalize_back(upstream, second_normed, second_recip, gain_second)
    grad_outer = lowered(pre_second)
    grad_b_outer = jnp.sum(widen(grad_outer), axis=0)
    grad_first, inner_grads, outer_grads, bias_grads = pre_second, [], [], []
    for (inner, active), (inner_weight, outer_weight, _) in zip(kept, halves):
        grad_inner = lowered(matmul_nt(grad_outer, outer_weight) * gelu_slope(inner))
        outer_grads.append(lowered(matmul_tn(active, grad_outer)))
        inner_grads.append(lowered(matmul_tn(first_low, grad_inner)))
        bias_grads.append(jnp.sum(widen(grad_inner), axis=0).reshape(shards, 1, unit_half))
        grad_first = grad_first + matmul_nt(grad_inner, inner_weight)
    grad_b_inner = in_order(core == 0, bias_grads[0], bias_grads[1], 1).reshape(hidden)
    pre_first, grad_first_gain, grad_first_shift = normalize_back(grad_first, first_normed, first_recip, gain_first)
    grad_attended = lowered(pre_first)
    grad_b_output = jnp.sum(widen(grad_attended), axis=0)
    grad_w_output = lowered(matmul_tn(context, grad_attended))
    grad_context = lowered(matmul_nt(grad_attended, full_output))
    context_mine = lax.dynamic_slice_in_dim(grad_context, core * half, half, 1)
    context_other = lax.dynamic_slice_in_dim(grad_context, (1 - core) * half, half, 1)
    upstream_other = swap(context_other, "core")

    def core_sum(own, other):
        return lowered(widen(own) + widen(swap(other, "core")))

    outer_term = core_sum(*outer_grads)
    inner_term = core_sum(*inner_grads)
    output_term = core_sum(
        lax.dynamic_slice_in_dim(grad_w_output, core * half, half, 1),
        lax.dynamic_slice_in_dim(grad_w_output, (1 - core) * half, half, 1),
    )
    outer_done = reduce_owned(outer_term.reshape(shards, unit_half, width))
    late_done = reduce_owned(jnp.concatenate([output_term, inner_term], axis=1).reshape(shards, own_rows, half + hidden // 2))

    grads, sums = attention_back(place, segments, projected, heads_mine, heads_other, context_mine, upstream_other, logsum)
    grad_early = lowered(matmul_tn(inputs_all, grads))
    partial = matmul_nt(grads, full_early)
    sums = sums.reshape(pairs, 8, 3, 128)[:, 0]
    blank = jnp.zeros((width,), jnp.float32)
    grad_b_query = lax.dynamic_update_slice(blank, sums[:, 0].reshape(half), (core * half,))
    grad_b_value = lax.dynamic_update_slice(blank, sums[:, 2].reshape(half), (core * half,))
    vector_grads = (
        grad_b_query,
        grad_b_value,
        grad_b_output,
        grad_first_gain,
        grad_first_shift,
        grad_b_inner,
        grad_b_outer,
        grad_second_gain,
        grad_second_shift,
    )
    flat_grads = jnp.concatenate([v.reshape(shards, -1) for v in vector_grads], axis=1)
    flat_grads = jnp.pad(flat_grads, ((0, 0), (0, extra * lanes - flat_grads.shape[1])))
    early_term = jnp.concatenate(
        [grad_early.reshape(shards, own_rows, lanes), lowered(flat_grads).reshape(shards, extra, lanes)], axis=1
    )
    early_done = reduce_owned(early_term)

    grad_inputs = pre_first + partial[:local] + widen(swap(lowered(partial[local:]), "core"))
    returned = widen(swap(lowered(grad_inputs[part:]), "y"))
    grad_tokens = in_order(y == 0, grad_inputs[None, :part], returned[None], 0)
    mixed_out = in_order(y == 0, mixed[None, :part], swap(mixed[part:], "y")[None], 0)

    def both(piece):
        return widen(swap(lowered(piece), "core"))

    early_matrix = early_done[:own_rows]
    early_full = in_order(
        core == 0, early_matrix.reshape(own_rows, pairs, 3, 128)[None], both(early_matrix).reshape(own_rows, pairs, 3, 128)[None], 0
    )
    early_full = early_full.transpose(3, 1, 0, 2, 4).reshape(3, own_rows, width)
    late_other = both(late_done)
    output_full = in_order(core == 0, late_done[:, :half], late_other[:, :half], 1)
    inner_full = in_order(
        core == 0,
        late_done[:, half:].reshape(own_rows, shards, 1, unit_half),
        late_other[:, half:].reshape(own_rows, shards, 1, unit_half),
        2,
    ).reshape(own_rows, hidden)
    outer_full = in_order(core == 0, outer_done, both(outer_done), 0)
    vector_part = early_done[own_rows:]
    vector_sums = (vector_part + swap(vector_part, "core")).reshape(extra * lanes)
    out_vectors, at = [], 0
    for size in sizes:
        out_vectors.append(vector_sums[at : at + size])
        at += size
    (
        done_b_query,
        done_b_value,
        done_b_output,
        done_first_gain,
        done_first_shift,
        done_b_inner,
        done_b_outer,
        done_second_gain,
        done_second_shift,
    ) = out_vectors
    return (
        mixed_out,
        grad_tokens,
        early_full[0],
        early_full[1],
        early_full[2],
        output_full,
        done_b_query,
        done_b_value,
        done_b_output,
        done_first_gain,
        done_first_shift,
        inner_full,
        done_b_inner,
        outer_full,
        done_b_outer,
        done_second_gain,
        done_second_shift,
    )


def body(
    tokens,
    segment_ids,
    w_query,
    w_key,
    w_value,
    w_output,
    b_query,
    b_value,
    b_output,
    first_gain,
    first_shift,
    w_inner,
    b_inner,
    w_outer,
    b_outer,
    second_gain,
    second_shift,
    cotangent,
):
    core, y = lax.axis_index("core"), lax.axis_index("y")
    size_z, size_x = lax.axis_size("z"), lax.axis_size("x")
    shards = size_z * size_x
    sequences, part, width = tokens.shape
    half = width // 2
    pairs = half // 128
    hidden = w_inner.shape[1]
    local = 2 * part
    own_rows = w_query.shape[0]
    lanes = 3 * half

    vectors = (b_query, b_value, b_output, first_gain, first_shift, b_inner, b_outer, second_gain, second_shift)
    sizes = [v.shape[0] for v in vectors]
    tokens_all, cotangent_all, early, inner_own, outer_own, rows, inner_row = entry(
        size_z, size_x, tokens, cotangent, w_query, w_key, w_value, w_inner, w_output, w_outer, vectors
    )
    inner_parts = [inner_own] + [shift(inner_own, "x", j) for j in range(1, size_x)]
    outer_parts = [outer_own] + [shift(outer_own, "z", k) for k in range(1, size_z)]
    inputs_all = tokens_all.reshape(4 * part, width)
    full_early = early.reshape(width, lanes)
    spot = jnp.arange(5, dtype=jnp.int32)
    place = jnp.where(spot < 4, ((spot % 2 != core) * 2 + (spot // 2 != y) * 1) * part, core)
    segments = pick(segment_ids, y)
    context_mine, context_other, logsum, projected = attention(place, segments, inputs_all, full_early, rows)
    made = dense_layer(
        size_z,
        size_x,
        inputs_all,
        context_mine,
        context_other,
        cotangent_all.reshape(local, width),
        rows,
        inner_row,
        inner_parts,
        outer_parts,
    )
    mixed, pre_first, upstream_mine, upstream_other, dense_sums, inner_sums, grad_w_output = made[:7]
    inner_terms = [made[7]] + [shift(made[7 + k], "z", k) for k in range(1, size_z)]
    outer_terms = [made[7 + size_z]] + [shift(made[7 + size_z + j], "x", j) for j in range(1, size_x)]
    mixed_out = in_order(y == 0, mixed[None, :part], swap(mixed[part:], "y")[None], 0)

    grads, sums = attention_back(place, segments, projected, context_mine, context_other, upstream_mine, upstream_other, logsum)
    made = exit_call(
        size_z,
        size_x,
        grads,
        inputs_all,
        full_early,
        pre_first,
        grad_w_output.reshape(shards, own_rows, width),
        dense_sums,
        inner_sums,
        sums,
        inner_terms,
        outer_terms,
    )
    grad_tokens, grad_query, grad_key, grad_value, grad_output, grad_inner_full, grad_outer_full, *done = deliver(
        made[:7], made[7], sizes
    )
    done = [v.reshape(size) for v, size in zip(done, sizes)]
    return (
        mixed_out,
        grad_tokens,
        grad_query,
        grad_key,
        grad_value,
        grad_output,
        *done[:5],
        grad_inner_full,
        done[5],
        grad_outer_full,
        *done[6:],
    )


def layer(*arrays):
    if arrays[2].shape[0] % 32 == 0 and lax.axis_size("x") > 1:
        return body(*arrays)
    return plain_body(*arrays)


def solution(mesh):
    outer, inner = mesh.devices.shape
    size_z = 1
    while size_z * size_z < outer:
        size_z *= 2
    split = Mesh(mesh.devices.reshape(size_z, outer // size_z, inner // 2, 2), ("z", "x", "y", "core"))
    dp, seq = ("z", "x"), ("y", "core")
    activation, matrix, vector = P(dp, seq, None), P(dp, None), P(dp)
    return jax.shard_map(
        layer,
        mesh=split,
        in_specs=(
            activation,
            matrix,
            matrix,
            matrix,
            matrix,
            matrix,
            vector,
            vector,
            vector,
            vector,
            vector,
            matrix,
            vector,
            matrix,
            vector,
            vector,
            vector,
            activation,
        ),
        out_specs=(
            activation,
            activation,
            matrix,
            matrix,
            matrix,
            matrix,
            vector,
            vector,
            vector,
            vector,
            vector,
            matrix,
            vector,
            matrix,
            vector,
            vector,
            vector,
        ),
        check_vma=False,
    )
```

```python
import jax
import jax.numpy as jnp
from jax import lax
from jax.experimental import pallas as pl
from jax.experimental.pallas import tpu as pltpu
from jax.sharding import Mesh
from jax.sharding import PartitionSpec as P


HD = 64
EPS = 1e-12
ROOT_HALF = 0.7071067811865476
INV_ROOT_TAU = 0.3989422804014327

BLK = 256
BIG = -1.0e9
DOCUMENTS = 4


def dot_nn(a, b):
    return jnp.dot(a, b, preferred_element_type=jnp.float32)


def local_start(b, part):
    core, y = lax.axis_index("core"), lax.axis_index("y")
    return (jnp.where(b % 2 == core, 0, 2) + jnp.where(b // 2 == y, 0, 1)) * part


def part_rows(b, part):
    return pl.ds(pl.multiple_of(local_start(b, part), 128), part)


def find_bounds(segment_ref, bound_ref):
    length = segment_ref.shape[1]
    y = lax.axis_index("y")
    bound_ref[0] = 0
    bound_ref[DOCUMENTS] = length
    for d in range(1, DOCUMENTS):

        def halve(_, span):
            low, high = span
            middle = (low + high) // 2
            below = segment_ref[y, jnp.minimum(middle, length - 1)] < d
            inside = low < high
            return (
                jnp.where(jnp.logical_and(inside, below), middle + 1, low),
                jnp.where(jnp.logical_and(inside, jnp.logical_not(below)), middle, high),
            )

        low, _ = lax.fori_loop(0, length.bit_length(), halve, (0, length))
        bound_ref[d] = low


def find_window(segment_ref, bound_ref, qb):
    length = segment_ref.shape[1]
    y = lax.axis_index("y")
    first = segment_ref[y, qb * BLK]
    last = segment_ref[y, qb * BLK + BLK - 1]
    start = bound_ref[first] // 128 * 128
    count = (bound_ref[last + 1] - start + BLK - 1) // BLK
    return jnp.minimum(start, length - count * BLK), count


def each_tile(count, step):
    def two(i, _):
        step(i * (2 * BLK), 2 * BLK)
        return 0

    lax.fori_loop(0, count // 2, two, 0)

    @pl.when(count % 2 == 1)
    def _():
        step((count - 1) * BLK, BLK)


def make_marks(row_ref, mark_query, mark_key):
    length = mark_key.shape[0]
    y = lax.axis_index("y")
    step = 512
    for b in range(length // step):
        rows = slice(b * step, (b + 1) * step)
        column = jnp.broadcast_to(row_ref[pl.ds(y, 1), rows], (128, step)).T
        lane = lax.broadcasted_iota(jnp.int32, (step, 128), 1) % 64
        same = lane == column
        line = lax.broadcasted_iota(jnp.int32, (128, step), 0) % 64
        mark_query[:, rows] = jnp.where(line == row_ref[pl.ds(y, 1), rows], 1.0, 0.0).astype(jnp.bfloat16)
        apart = jnp.logical_and(lane < DOCUMENTS, jnp.logical_not(same))
        mark_key[rows, :] = jnp.where(apart, BIG, 0.0).astype(jnp.bfloat16)


def forward_kernel(segment_ref, row_ref, tokens_ref, weights_ref, bias_ref, *refs):
    mine_ref, other_ref, lse_ref, qkv_ref, q2, k2, vt, acc, top, tot, keep, mark_query, mark_key, bound_ref = refs
    length = qkv_ref.shape[0]
    blocks = length // BLK
    part = length // 4

    @pl.when(pl.program_id(0) == 0)
    def _():
        find_bounds(segment_ref, bound_ref)
        make_marks(row_ref, mark_query, mark_key)

    low = lax.broadcasted_iota(jnp.int32, (part, 128), 1) < 64
    for b in range(4):
        src = part_rows(b, part)
        dst = slice(b * part, (b + 1) * part)
        made = dot_nn(tokens_ref[src, :], weights_ref[...])
        lanes = pl.ds(pl.multiple_of(lax.axis_index("core") * (128 * pl.num_programs(0)) + pl.program_id(0) * 128, 128), 128)
        q = ((made[:, 0:128] + bias_ref[0:1, lanes]) * 0.125).astype(jnp.bfloat16)
        k = made[:, 128:256].astype(jnp.bfloat16)
        v = (made[:, 256:384] + bias_ref[1:2, lanes]).astype(jnp.bfloat16)
        qkv_ref[src, 0:128] = q
        qkv_ref[src, 128:256] = k
        qkv_ref[src, 256:384] = v
        nohk = mark_key[dst, :]
        turned = q.T
        q2[0, 0:64, dst] = turned[0:64]
        q2[0, 64:128, dst] = mark_query[64:128, dst]
        q2[1, 0:64, dst] = mark_query[0:64, dst]
        q2[1, 64:128, dst] = turned[64:128]
        k2[0, dst, :] = jnp.where(low, k, nohk)
        k2[1, dst, :] = jnp.where(low, nohk, k)
        vt[:, dst] = v.T
    lse_ref[...] = jnp.zeros_like(lse_ref)

    def row(qb, _):
        qs = pl.ds(pl.multiple_of(qb * BLK, BLK), BLK)
        start, count = find_window(segment_ref, bound_ref, qb)
        top[...] = jnp.full_like(top, -1.0e30)

        def fold(tile, function):
            return function(tile.reshape(tile.shape[0] // 8, 8, BLK), axis=0)

        def highest(first, size):
            keys = pl.ds(pl.multiple_of(start + first, 128), size)
            for h in range(2):
                st = dot_nn(k2[h, keys, :], q2[h, :, qs])
                keep[h, pl.ds(pl.multiple_of(first, BLK), size), :] = st
                top[h] = jnp.maximum(top[h], fold(st, jnp.max))

        def weigh(first, size, largest):
            keys = pl.ds(pl.multiple_of(start + first, 128), size)
            for h in range(2):
                rows = slice(64 * h, 64 * h + 64)
                st = keep[h, pl.ds(pl.multiple_of(first, BLK), size), :]
                p = jnp.exp(st - largest[h])
                tot[h] = tot[h] + fold(p, jnp.sum)
                acc[rows, :] = acc[rows, :] + dot_nn(vt[rows, keys], p.astype(jnp.bfloat16))

        def paired(step):
            each_tile(count, step)

        paired(highest)
        largest = [jnp.max(top[h], axis=0, keepdims=True) for h in range(2)]
        acc[...] = jnp.zeros_like(acc)
        tot[...] = jnp.zeros_like(tot)
        paired(lambda first, size: weigh(first, size, largest))
        for h in range(2):
            rows = slice(64 * h, 64 * h + 64)
            total = jnp.sum(tot[h], axis=0, keepdims=True)
            acc[rows, :] = acc[rows, :] / total
            lse_ref[h : h + 1, qs] = largest[h] + jnp.log(total)
        where = local_start(qb * BLK // part, part) + qb * BLK % part
        result = acc[...].T.astype(jnp.bfloat16)

        @pl.when(where < 2 * part)
        def _():
            mine_ref[pl.ds(pl.multiple_of(where, BLK), BLK), :] = result

        @pl.when(where >= 2 * part)
        def _():
            other_ref[pl.ds(pl.multiple_of(where - 2 * part, BLK), BLK), :] = result

        return 0

    lax.fori_loop(0, blocks, row, 0)


def attention(segments, tokens, weights, biases):
    length, depth = tokens.shape
    width = weights.shape[1]
    pairs = width // 384
    rows = length // 2
    return pl.pallas_call(
        forward_kernel,
        out_shape=(
            jax.ShapeDtypeStruct((rows, pairs * 128), jnp.bfloat16),
            jax.ShapeDtypeStruct((rows, pairs * 128), jnp.bfloat16),
            jax.ShapeDtypeStruct((pairs * 8, length), jnp.float32),
            jax.ShapeDtypeStruct((length, width), jnp.bfloat16),
        ),
        grid_spec=pltpu.PrefetchScalarGridSpec(
            num_scalar_prefetch=1,
            grid=(pairs,),
            in_specs=[
                pl.BlockSpec(segments.shape, lambda p, *_: (0, 0)),
                pl.BlockSpec((length, depth), lambda p, *_: (0, 0)),
                pl.BlockSpec((depth, 384), lambda p, *_: (0, p)),
                pl.BlockSpec(biases.shape, lambda p, *_: (0, 0)),
            ],
            out_specs=[
                pl.BlockSpec((rows, 128), lambda p, *_: (0, p)),
                pl.BlockSpec((rows, 128), lambda p, *_: (0, p)),
                pl.BlockSpec((8, length), lambda p, *_: (p, 0)),
                pl.BlockSpec((length, 384), lambda p, *_: (0, p)),
            ],
            scratch_shapes=[
                pltpu.VMEM((2, 128, length), jnp.bfloat16),
                pltpu.VMEM((2, length, 128), jnp.bfloat16),
                pltpu.VMEM((128, length), jnp.bfloat16),
                pltpu.VMEM((128, BLK), jnp.float32),
                pltpu.VMEM((2, 8, BLK), jnp.float32),
                pltpu.VMEM((2, 8, BLK), jnp.float32),
                pltpu.VMEM((2, length, BLK), jnp.float32),
                pltpu.VMEM((128, length), jnp.bfloat16),
                pltpu.VMEM((length, 128), jnp.bfloat16),
                pltpu.SMEM((DOCUMENTS + 1,), jnp.int32),
            ],
        ),
        compiler_params=pltpu.CompilerParams(dimension_semantics=("arbitrary",), vmem_limit_bytes=60 << 20),
        cost_estimate=pl.CostEstimate(flops=pairs * 40_000_000_000, bytes_accessed=pairs * 3_000_000, transcendentals=pairs * 4_000_000),
        name="attention_forward",
    )(segments, segments, tokens, weights, biases)


def backward_kernel(
    segment_ref,
    qkv_ref,
    ctx_mine_ref,
    ctx_other_ref,
    do_mine_ref,
    do_other_ref,
    lse_ref,
    row_ref,
    out_ref,
    sum_ref,
    q2,
    k2,
    q0,
    d0,
    dt,
    v0,
    kt,
    dk,
    dv,
    dqt,
    delta,
    mark_query,
    mark_key,
    bound_ref,
):
    length = qkv_ref.shape[0]
    blocks = length // BLK
    part = length // 4

    @pl.when(pl.program_id(0) == 0)
    def _():
        find_bounds(segment_ref, bound_ref)
        make_marks(row_ref, mark_query, mark_key)

    low = lax.broadcasted_iota(jnp.int32, (part, 128), 1) < 64

    def prepare(b, do, ctx):
        src = part_rows(b, part)
        dst = slice(b * part, (b + 1) * part)
        q, k = qkv_ref[src, 0:128], qkv_ref[src, 128:256]
        zero = jnp.zeros_like(q)
        nohk = mark_key[dst, :]
        turned = q.T
        q2[0, 0:64, dst] = turned[0:64]
        q2[0, 64:128, dst] = mark_query[64:128, dst]
        q2[1, 0:64, dst] = mark_query[0:64, dst]
        q2[1, 64:128, dst] = turned[64:128]
        k2[0, dst, :] = jnp.where(low, k, nohk)
        k2[1, dst, :] = jnp.where(low, nohk, k)
        q0[0, dst, :] = jnp.where(low, q, zero)
        q0[1, dst, :] = jnp.where(low, zero, q)
        d0[0, dst, :] = jnp.where(low, do, zero)
        d0[1, dst, :] = jnp.where(low, zero, do)
        turned = do.T
        blank = jnp.zeros((64, part), jnp.bfloat16)
        dt[0, 0:64, dst] = turned[0:64]
        dt[0, 64:128, dst] = blank
        dt[1, 0:64, dst] = blank
        dt[1, 64:128, dst] = turned[64:128]
        v0[dst, :] = qkv_ref[src, 256:384]
        kt[:, dst] = k.T
        prod = turned.astype(jnp.float32) * ctx.T.astype(jnp.float32)
        delta[0:1, dst] = jnp.sum(prod[0:64], axis=0, keepdims=True)
        delta[1:2, dst] = jnp.sum(prod[64:128], axis=0, keepdims=True)

    for b in range(4):

        @pl.when(local_start(b, part) < 2 * part)
        def _():
            rows = part_rows(b, part)
            prepare(b, do_mine_ref[rows, :], ctx_mine_ref[rows, :])

        @pl.when(local_start(b, part) >= 2 * part)
        def _():
            rows = pl.ds(pl.multiple_of(local_start(b, part) - 2 * part, 128), part)
            prepare(b, do_other_ref[rows, :], ctx_other_ref[rows, :])

    dk[...] = jnp.zeros_like(dk)
    dv[...] = jnp.zeros_like(dv)
    dqt[...] = jnp.zeros_like(dqt)

    def row(qb, _):
        qs = pl.ds(pl.multiple_of(qb * BLK, BLK), BLK)
        start, count = find_window(segment_ref, bound_ref, qb)

        def tile(first, size):
            ks = pl.ds(pl.multiple_of(start + first, 128), size)
            weights, grads = [], []
            for h in range(2):
                st = dot_nn(k2[h, ks, :], q2[h, :, qs])
                w = jnp.exp(st - lse_ref[h : h + 1, qs])
                gw = dot_nn(v0[ks, :], dt[h, :, qs])
                weights.append(w.astype(jnp.bfloat16))
                grads.append((w * (gw - delta[h : h + 1, qs])).astype(jnp.bfloat16))
            dv[ks, :] += dot_nn(jnp.concatenate(weights, axis=1), jnp.concatenate([d0[0, qs, :], d0[1, qs, :]], axis=0))
            dk[ks, :] += dot_nn(jnp.concatenate(grads, axis=1), jnp.concatenate([q0[0, qs, :], q0[1, qs, :]], axis=0))
            for h in range(2):
                rows = slice(64 * h, 64 * h + 64)
                dqt[rows, qs] += dot_nn(kt[rows, ks], grads[h])

        each_tile(count, tile)
        return 0

    lax.fori_loop(0, blocks, row, 0)
    sums = [jnp.zeros((1, 128), jnp.float32) for _ in range(3)]
    for b in range(4):
        dst = part_rows(b, part)
        src = slice(b * part, (b + 1) * part)
        pieces = ((dqt[:, src].T * 0.125).astype(jnp.bfloat16), dk[src, :].astype(jnp.bfloat16), dv[src, :].astype(jnp.bfloat16))
        for i, piece in enumerate(pieces):
            out_ref[dst, 128 * i : 128 * i + 128] = piece
            sums[i] = sums[i] + jnp.sum(piece.astype(jnp.float32), axis=0, keepdims=True)
    sum_ref[...] = jnp.zeros_like(sum_ref)
    for i in range(3):
        sum_ref[0:1, 128 * i : 128 * i + 128] = sums[i]


def attention_back(segments, qkv, ctx_mine, ctx_other, do_mine, do_other, lse):
    length, width = qkv.shape
    pairs = width // 384
    rows = length // 2
    half = lambda: pltpu.VMEM((2, length, 128), jnp.bfloat16)
    turned = lambda: pltpu.VMEM((2, 128, length), jnp.bfloat16)
    column = pl.BlockSpec((rows, 128), lambda p, *_: (0, p))
    return pl.pallas_call(
        backward_kernel,
        out_shape=(
            jax.ShapeDtypeStruct((length, width), jnp.bfloat16),
            jax.ShapeDtypeStruct((pairs * 8, 384), jnp.float32),
        ),
        grid_spec=pltpu.PrefetchScalarGridSpec(
            num_scalar_prefetch=1,
            grid=(pairs,),
            in_specs=[
                pl.BlockSpec((length, 384), lambda p, *_: (0, p)),
                column,
                column,
                column,
                column,
                pl.BlockSpec((8, length), lambda p, *_: (p, 0)),
                pl.BlockSpec(segments.shape, lambda p, *_: (0, 0)),
            ],
            out_specs=[
                pl.BlockSpec((length, 384), lambda p, *_: (0, p)),
                pl.BlockSpec((8, 384), lambda p, *_: (p, 0)),
            ],
            scratch_shapes=[
                turned(),
                half(),
                half(),
                half(),
                turned(),
                pltpu.VMEM((length, 128), jnp.bfloat16),
                pltpu.VMEM((128, length), jnp.bfloat16),
                pltpu.VMEM((length, 128), jnp.float32),
                pltpu.VMEM((length, 128), jnp.float32),
                pltpu.VMEM((128, length), jnp.float32),
                pltpu.VMEM((8, length), jnp.float32),
                pltpu.VMEM((128, length), jnp.bfloat16),
                pltpu.VMEM((length, 128), jnp.bfloat16),
                pltpu.SMEM((DOCUMENTS + 1,), jnp.int32),
            ],
        ),
        compiler_params=pltpu.CompilerParams(dimension_semantics=("arbitrary",), vmem_limit_bytes=60 << 20),
        cost_estimate=pl.CostEstimate(flops=pairs * 20_000_000_000, bytes_accessed=pairs * 5_000_000, transcendentals=pairs * 4_000_000),
        name="attention_backward",
    )(segments, qkv, ctx_mine, ctx_other, do_mine, do_other, lse, segments)


MESH_ID = pl.DeviceIdType.MESH
WIDE = 5


def place_of():
    return tuple(lax.axis_index(name) for name in ("z", "x", "y", "core"))


def sizes_of():
    return lax.axis_size("z"), lax.axis_size("x")


def partner(**moved):
    z, x, y, core = place_of()
    return (moved.get("z", z), moved.get("x", x), moved.get("y", y), moved.get("core", core))


def greet(with_grid):
    z, x, y, core = place_of()
    size_z, size_x = sizes_of()
    peers = [partner(y=1 - y), partner(core=1 - core)]
    if with_grid:
        peers += [partner(z=lax.rem(z + k, size_z)) for k in range(1, size_z)]
        peers += [partner(x=lax.rem(x + j, size_x)) for j in range(1, size_x)]
    barrier = pltpu.get_barrier_semaphore()
    for peer in peers:
        pl.semaphore_signal(barrier, inc=1, device_id=peer, device_id_type=MESH_ID)
    pl.semaphore_wait(barrier, len(peers))


def remote(src, dst, send, recv, peer):
    return pltpu.make_async_remote_copy(
        src_ref=src, dst_ref=dst, send_sem=send, recv_sem=recv, device_id=peer, device_id_type=MESH_ID
    )


def entry_kernel(size_z, size_x, count, *refs):
    tokens, cotangent, wq, wk, wv, w_inner, w_output, w_outer = refs[:8]
    vectors = refs[8 : 8 + count]
    tokens_all, cotangent_send, weights_all, inner_all, outer_all, rows_out, inner_out = refs[8 + count : 15 + count]
    raw = refs[15 + count : 15 + 2 * count]
    stage, cot_stage, wbuf, ibuf, obuf, pack, ipack, opack, vpack, vectors_all = refs[15 + 2 * count : 25 + 2 * count]
    local_sem, load_sem, tsend, trecv, zsend, zrecv, xsend, xrecv, ysend, yrecv, osend, orecv = refs[25 + 2 * count :]
    z, x, y, core = place_of()
    half = pack.shape[1] // 3
    pairs = half // 128
    chunks = w_inner.shape[1] // CHUNK
    me = z * size_x + x
    columns = [lax.rem(x + j, size_x) for j in range(size_x)]

    mine = pl.ds(pl.multiple_of(core * half, 128), half)
    loads = [pltpu.make_async_copy(w.at[:, mine], wbuf.at[i], load_sem.at[i]) for i, w in enumerate((wq, wk, wv))]
    loads += [pltpu.make_async_copy(v, r, load_sem.at[3 + i]) for i, (v, r) in enumerate(zip(vectors, raw))]
    late = [
        pltpu.make_async_copy(
            w_inner.at[:, pl.ds(pl.multiple_of(c * CHUNK + core * half, 128), half)],
            ibuf.at[:, pl.ds(c * half, half)],
            load_sem.at[3 + count + c],
        )
        for c in range(chunks)
    ]
    late.append(pltpu.make_async_copy(w_output.at[:, mine], ibuf.at[:, pl.ds(chunks * half, half)], load_sem.at[3 + count + chunks]))
    late.append(pltpu.make_async_copy(w_outer.at[:, mine], obuf, load_sem.at[4 + count + chunks]))
    load = pltpu.make_async_copy(tokens.at[y], stage, local_sem.at[0])
    cot_load = pltpu.make_async_copy(cotangent.at[1 - y], cot_stage, local_sem.at[4])
    for copy in loads + late + [load, cot_load]:
        copy.start()
    vpack[...] = jnp.zeros_like(vpack)
    for copy in loads:
        copy.wait()
    for i, vector in enumerate(raw):
        vpack[i : i + 1, 0 : vector.shape[1]] = vector[...].astype(jnp.bfloat16).astype(jnp.float32)
    for i in range(3):
        for p in range(pairs):
            pack[:, (3 * p + i) * 128 : (3 * p + i + 1) * 128] = wbuf[i, :, p * 128 : (p + 1) * 128].astype(jnp.bfloat16)
    vectors_all[me] = vpack[...]
    greet(True)

    across = remote(tokens.at[1 - y], tokens_all.at[1], tsend.at[0], trecv.at[0], partner(y=1 - y))
    across.start()
    beside = remote(tokens.at[y], tokens_all.at[2], tsend.at[1], trecv.at[1], partner(core=1 - core))

    rows = ipack.shape[0]

    def share(owner):
        return pl.ds(pl.multiple_of(owner * (rows // 2), rows // 2), rows // 2)

    packs = (pack, vpack, ipack.at[share(y), :])

    def y_move(index, origin):
        slot = home(2, origin)
        return remote(slot, slot, ysend.at[index], yrecv.at[index], partner(y=1 - y))

    def home(stream, origin):
        if stream == 2:
            return inner_all.at[origin, share(y), :]
        return (weights_all, vectors_all)[stream].at[origin * size_x + x]

    def z_move(stream, way, t):
        step = 1 - 2 * way
        origin = z - step * (t - 1)
        src = packs[stream] if t == 1 else home(stream, origin)
        peer = partner(z=lax.rem(z + step + size_z, size_z))
        return remote(src, home(stream, origin), zsend.at[stream, way, t - 1], zrecv.at[stream, way, t - 1], peer)

    def sends(way, t):
        step = 1 - 2 * way
        origin, target = z - step * (t - 1), z + step
        inside = lambda v: jnp.logical_and(v >= 0, v < size_z)
        return jnp.logical_and(inside(origin), inside(target))

    def receives(way, t):
        origin = z - (1 - 2 * way) * t
        return jnp.logical_and(origin >= 0, origin < size_z)

    def x_moves(index, origin, own):
        moves = []
        for j in range(1, size_x):
            for stream in range(2):
                src = packs[stream] if own else home(stream, origin)
                moves.append(
                    remote(
                        src,
                        home(stream, origin),
                        xsend.at[stream, index, j - 1],
                        xrecv.at[stream, index, j - 1],
                        partner(x=columns[j]),
                    )
                )
        return moves

    def start_z(streams, t):
        for way in range(2):

            @pl.when(sends(way, t))
            def _():
                for stream in streams:
                    z_move(stream, way, t).start()

    for move in x_moves(0, z, True):
        move.start()
    start_z((0, 1), 1)
    beside.start()
    for copy in late:
        copy.wait()
    ipack[...] = ibuf[...].astype(jnp.bfloat16)
    opack[...] = obuf[...].astype(jnp.bfloat16)
    start_z((2,), 1)
    outer_moves = [
        remote(opack, outer_all.at[x], osend.at[j - 1], orecv.at[j - 1], partner(x=columns[j])) for j in range(1, size_x)
    ]
    keeps = [
        pltpu.make_async_copy(pack, weights_all.at[me], local_sem.at[1]),
        pltpu.make_async_copy(ipack, inner_all.at[z], local_sem.at[2]),
        pltpu.make_async_copy(opack, outer_all.at[x], local_sem.at[6]),
    ]
    load.wait()
    keeps.append(pltpu.make_async_copy(stage, tokens_all.at[0], local_sem.at[3]))
    cot_load.wait()
    keeps.append(pltpu.make_async_copy(cot_stage, cotangent_send, local_sem.at[5]))
    for keep in keeps:
        keep.start()

    def arrive(streams, t, sideways):
        for way in range(2):

            @pl.when(receives(way, t))
            def _():
                origin = z - (1 - 2 * way) * t
                for stream in streams:
                    slot = home(stream, origin)
                    remote(
                        slot, slot, zsend.at[stream, way, t - 1], zrecv.at[stream, way, t - 1], partner(core=1 - core)
                    ).wait_recv()
                if sideways:
                    for move in x_moves(1 + way * (size_z - 1) + t - 1, origin, False):
                        move.start()
                else:
                    y_move(way * (size_z - 1) + t - 1, origin).start()

    onward = remote(tokens_all.at[1], tokens_all.at[3], tsend.at[2], trecv.at[2], partner(core=1 - core))
    for t in range(1, size_z):
        arrive((0, 1), t, True)
        if t < size_z - 1:
            start_z((0, 1), t + 1)
        if t == 1:
            for move in outer_moves:
                move.start()
        arrive((2,), t, False)
        if t < size_z - 1:
            start_z((2,), t + 1)
        if t == min(2, size_z - 1):
            across.wait_recv()
            onward.start()

    for move in x_moves(0, z, True):
        move.wait()
    for t in range(1, size_z):
        for way in range(2):

            @pl.when(receives(way, t))
            def _():
                origin = z - (1 - 2 * way) * t
                for move in x_moves(1 + way * (size_z - 1) + t - 1, origin, False):
                    move.wait()
                y_move(way * (size_z - 1) + t - 1, origin).wait()

            @pl.when(sends(way, t))
            def _():
                for stream in range(3):
                    z_move(stream, way, t).wait_send()

    short = min(vector.shape[1] for vector in raw)
    longest = vpack.shape[1]
    for s in range(size_z * size_x):
        rows_out[:, s * short : (s + 1) * short] = vectors_all[s, :, 0:short]
        inner_out[:, s * longest : (s + 1) * longest] = vectors_all[s, WIDE : WIDE + 1, :]
    for move in outer_moves:
        move.wait()
    across.wait_send()
    beside.wait()
    onward.wait()
    for keep in keeps:
        keep.wait()


def entry(size_z, size_x, tokens, cotangent, wq, wk, wv, w_inner, w_output, w_outer, vectors):
    _, part, width = tokens.shape
    rows = wq.shape[0]
    half = width // 2
    lanes = 3 * half
    hidden = w_inner.shape[1]
    long = w_outer.shape[0]
    mixed_lanes = hidden // 2 + half
    chunks = hidden // CHUNK
    longest = max(v.shape[0] for v in vectors)
    shards = size_z * size_x
    count = len(vectors)
    anywhere, vmem = pl.BlockSpec(memory_space=pl.ANY), pl.BlockSpec(memory_space=pltpu.VMEM)
    dma = pltpu.SemaphoreType.DMA
    low, high = jnp.bfloat16, jnp.float32
    side = size_x - 1
    return pl.pallas_call(
        lambda *refs: entry_kernel(size_z, size_x, count, *refs),
        out_shape=(
            jax.ShapeDtypeStruct((4, part, width), low),
            jax.ShapeDtypeStruct((part, width), low),
            jax.ShapeDtypeStruct((shards, rows, lanes), low),
            jax.ShapeDtypeStruct((size_z, rows, mixed_lanes), low),
            jax.ShapeDtypeStruct((size_x, long, half), low),
            jax.ShapeDtypeStruct((16, width), high),
            jax.ShapeDtypeStruct((1, shards * longest), high),
        ),
        in_specs=[anywhere] * (8 + count),
        out_specs=(anywhere,) * 5 + (vmem,) * 2,
        scratch_shapes=[pltpu.VMEM((1, v.shape[0]), v.dtype) for v in vectors]
        + [
            pltpu.VMEM((part, width), low),
            pltpu.VMEM((part, width), low),
            pltpu.VMEM((3, rows, half), high),
            pltpu.VMEM((rows, mixed_lanes), high),
            pltpu.VMEM((long, half), high),
            pltpu.VMEM((rows, lanes), low),
            pltpu.VMEM((rows, mixed_lanes), low),
            pltpu.VMEM((long, half), low),
            pltpu.VMEM((16, longest), high),
            pltpu.VMEM((shards, 16, longest), high),
            dma((7,)),
            dma((5 + count + chunks,)),
            dma((4,)),
            dma((4,)),
            dma((3, 2, size_z - 1)),
            dma((3, 2, size_z - 1)),
            dma((2, 2 * size_z - 1, side)),
            dma((2, 2 * size_z - 1, side)),
            dma((2 * size_z - 2,)),
            dma((2 * size_z - 2,)),
            dma((side,)),
            dma((side,)),
        ],
        compiler_params=pltpu.CompilerParams(collective_id=0, has_side_effects=True, vmem_limit_bytes=66_000_000),
        name="entry",
    )(tokens, cotangent, wq, wk, wv, w_inner, w_output, w_outer, *[v.reshape(1, -1) for v in vectors])


def exit_kernel(size_z, size_x, shapes, *refs):
    z, x, y, core = place_of()
    grads_hbm, inputs_hbm, weights_hbm, base_hbm, output_term, dense_sums, inner_sums, head_sums = refs[:8]
    inner_in = refs[8 : 8 + size_z]
    outer_in = refs[8 + size_z : 8 + size_z + size_x]
    refs = refs[8 + size_z + size_x :]
    results = refs[:8]
    made = refs[8:16]
    token_grads, grad_query, grad_key, grad_value, grad_output, grad_inner, grad_outer, vector_sums = made
    grads, inputs, turned, weights, base, terms, other_rows, recv_rows, send_rows, far_rows, odd = refs[16:27]
    inner_buf, outer_buf, vector_rows, vector_terms, inner_send, store_sem = refs[27:33]
    load_sem, tsend, trecv, osend, orecv = refs[33:38]
    refs = list(refs[38:])
    stores = [pltpu.make_async_copy(a, b, store_sem.at[i]) for i, (a, b) in enumerate(zip(made, results))]
    xin, xsend, xrecv = {}, {}, {}
    zout, zin, zsend, zrecv = {}, {}, {}, {}
    ybuf, ysend, yrecv, cbuf, csend, crecv = {}, {}, {}, {}, {}, {}
    for name in shapes:
        ybuf[name], ysend[name], yrecv[name], cbuf[name], csend[name], crecv[name] = [refs.pop(0) for _ in range(6)]
        if name != "outer":
            xin[name], xsend[name], xrecv[name] = [refs.pop(0) for _ in range(3)]
        if name != "inner":
            zout[name], zin[name], zsend[name], zrecv[name] = [refs.pop(0) for _ in range(4)]

    shards, rows, full = terms.shape
    half = full // 4
    lanes = 3 * half
    pairs = half // 128
    hidden = grad_inner.shape[1]
    part = token_grads.shape[1]
    local = 2 * part
    low, high = jnp.bfloat16, jnp.float32
    mine = pl.ds(pl.multiple_of(core * half, 128), half)
    theirs = pl.ds(pl.multiple_of((1 - core) * half, 128), half)
    columns = [lax.rem(x + j, size_x) for j in range(size_x)]
    steps = [(t, way) for t in range(1, size_z) for way in range(2)]
    core_peer, y_peer = partner(core=1 - core), partner(y=1 - y)

    loads = {}
    for i, src in enumerate(inner_in):
        loads["inner", i] = pltpu.make_async_copy(src, inner_buf.at[i], load_sem.at[i])
    for i, src in enumerate(outer_in):
        loads["outer", i] = pltpu.make_async_copy(src, outer_buf.at[i], load_sem.at[size_z + i])
    for i, (name, src, dst) in enumerate(
        (("inputs", inputs_hbm, inputs), ("grads", grads_hbm, grads), ("weights", weights_hbm, weights), ("base", base_hbm, base))
    ):
        loads[name] = pltpu.make_async_copy(src, dst, load_sem.at[size_z + size_x + i])
    for load in loads.values():
        load.start()

    def inside(v):
        return jnp.logical_and(v >= 0, v < size_z)

    def target_of(t, way):
        return z + (1 - 2 * way) * (size_z - t)

    def fed(way):
        return inside(z - (1 - 2 * way))

    def x_move(name, n, at, j, src, dst):
        return remote(src, dst, xsend[name].at[n, at, j - 1], xrecv[name].at[n, at, j - 1], partner(x=columns[j]))

    def x_pieces(name, at):
        source = vector_terms if name == "vec" else terms
        return [
            x_move(name, 0, at, j, source.at[at * size_x + columns[j]], xin[name].at[j - 1, at]) for j in range(1, size_x)
        ]

    def send_x(name):
        for t, way in steps:

            @pl.when(inside(target_of(t, way)))
            def _():
                for move in x_pieces(name, target_of(t, way)):
                    move.start()

        for move in x_pieces(name, z):
            move.start()

    def own_part(name, at):
        if name == "outer":
            total = outer_buf[0, at].astype(high)
            for i in range(1, size_x):
                total = total + outer_buf[i, at].astype(high)
            return [(slice(None), total)]
        slot = at * size_x + x
        if name == "vec":
            total = vector_terms[slot]
            for move in x_pieces("vec", at):
                move.wait()
            for j in range(1, size_x):
                total = total + xin["vec"][j - 1, at]
            return [(slice(None), total)]
        for move in x_pieces(name, at):
            move.wait()
        total = terms[slot].astype(high)
        for j in range(1, size_x):
            total = total + xin[name][j - 1, at].astype(high)
        return [(slice(None), total)]

    def z_move(name, t, way):
        peer = partner(z=lax.rem(z + 1 - 2 * way + size_z, size_z))
        return remote(
            zout[name].at[way, t - 1], zin[name].at[way, t - 1], zsend[name].at[way, t - 1], zrecv[name].at[way, t - 1], peer
        )

    def step_z(name, t):
        for way in range(2):

            @pl.when(inside(target_of(t, way)))
            def _():
                pieces = own_part(name, target_of(t, way))
                if t > 1:

                    @pl.when(fed(way))
                    def _():
                        z_move(name, t - 1, way).wait_recv()

                for span, total in pieces:
                    if t > 1:
                        before = zin[name][way, t - 2, :, span].astype(high)
                        total = total + jnp.where(fed(way), before, 0.0)
                    zout[name][way, t - 1, :, span] = total.astype(zout[name].dtype)
                z_move(name, t, way).start()

    across, swapped = {}, {}

    def step_y(name):
        across[name] = remote(ybuf[name].at[0], ybuf[name].at[1], ysend[name], yrecv[name], y_peer)
        across[name].start()

    def finish_z(name):
        pieces = own_part(name, z)
        last = size_z - 1
        for way in range(2):

            @pl.when(fed(way))
            def _():
                z_move(name, last, way).wait_recv()

        for span, total in pieces:
            for way in range(2):
                before = zin[name][way, last - 1, :, span].astype(high)
                total = total + jnp.where(fed(way), before, 0.0)
            ybuf[name][0, :, span] = total.astype(ybuf[name].dtype)
        step_y(name)

    def step_core(name):
        across[name].wait()
        cbuf[name][0] = ybuf[name][0].astype(high) + ybuf[name][1].astype(high)
        swapped[name] = remote(cbuf[name].at[0], cbuf[name].at[1], csend[name], crecv[name], core_peer)
        swapped[name].start()

    def finish_core(name):
        swapped[name].wait()
        return cbuf[name]

    vector_rows[...] = jnp.zeros_like(vector_rows)
    for i, row in enumerate((7, 8, 6, 3, 4, 2)):
        vector_rows[row : row + 1, :] = jnp.sum(dense_sums[8 * i : 8 * i + 8, :], axis=0, keepdims=True)
    for p in range(pairs):
        place = pl.ds(pl.multiple_of(core * half + p * 128, 128), 128)
        vector_rows[0:1, place] = head_sums[8 * p : 8 * p + 1, 0:128]
        vector_rows[1:2, place] = head_sums[8 * p : 8 * p + 1, 256:384]
    inner_row = jnp.sum(inner_sums[...], axis=0, keepdims=True)
    vector_terms[...] = jnp.zeros_like(vector_terms)
    for name in zin:
        if name == "vec":
            zin[name][...] = jnp.zeros_like(zin[name])
    longest = vector_terms.shape[2]
    for s in range(shards):
        vector_terms[s, :, 0:rows] = vector_rows[:, s * rows : (s + 1) * rows]
        vector_terms[s, WIDE : WIDE + 1, :] = inner_row[:, s * longest : (s + 1) * longest]
    greet(True)

    outputs = remote(output_term.at[:, :, theirs], odd, osend, orecv, core_peer)
    outputs.start()
    send_x("vec")
    for i in range(size_z):
        loads["inner", i].wait()
    inner_moves = []
    for j in range(1, size_x):
        total = inner_buf[0, columns[j]].astype(high)
        for i in range(1, size_z):
            total = total + inner_buf[i, columns[j]].astype(high)
        inner_send[j - 1] = total.astype(low)
        move = x_move("inner", 0, 0, j, inner_send.at[j - 1], xin["inner"].at[j - 1, 0])
        move.start()
        inner_moves.append(move)
    for i in range(size_x):
        loads["outer", i].wait()
    step_z("outer", 1)

    strip = 256

    def product(first):
        at = pl.ds(pl.multiple_of(first, strip), strip)
        return dot_nt(grads[at, :], weights[...])

    def token_rows(first):
        def other_strip(i, _):
            at = pl.ds(pl.multiple_of(first + i * strip, strip), strip)
            other_rows[at, :] = product(local + first + i * strip).astype(low)
            return 0

        def own_strip(i, _):
            at = pl.ds(pl.multiple_of(first + i * strip, strip), strip)
            base[at, :] = base[at, :] + product(first + i * strip)
            return 0

        lax.fori_loop(0, part // strip, other_strip, 0)
        span = pl.ds(first, part)
        move = remote(other_rows.at[span, :], recv_rows.at[span, :], tsend.at[first // part], trecv.at[first // part], core_peer)
        move.start()
        lax.fori_loop(0, part // strip, own_strip, 0)
        return move

    loads["inputs"].wait()
    for b in range(4):
        turned[:, b * part : (b + 1) * part] = inputs[b * part : (b + 1) * part, :].T
    group = 4
    loads["grads"].wait()
    for p in range(pairs):
        block = slice(p * 384, (p + 1) * 384)

        def some(m, _):
            value = dot_nn(turned[pl.ds(pl.multiple_of(m * group * rows, group * rows), group * rows), :], grads[:, block])
            terms[pl.ds(m * group, group), :, block] = value.reshape(group, rows, 384).astype(low)
            return 0

        lax.fori_loop(0, shards // group, some, 0)
    outputs.wait()
    terms[:, :, lanes : lanes + half] = (odd[...].astype(high) + output_term[:, :, mine].astype(high)).astype(low)
    send_x("qkvo")
    for name in ("weights", "base"):
        loads[name].wait()
    halves = token_rows(part)
    halves.wait()
    send_rows[...] = (base[part:local, :] + recv_rows[part:local, :].astype(high)).astype(low)
    back = remote(send_rows, far_rows, tsend.at[2], trecv.at[2], y_peer)
    back.start()

    step_z("outer", 2)
    halves = token_rows(0)
    for t in range(3, size_z):
        step_z("outer", t)
    step_z("vec", 1)
    step_z("qkvo", 1)

    total = inner_buf[0, x].astype(high)
    for i in range(1, size_z):
        total = total + inner_buf[i, x].astype(high)
    for j in range(1, size_x):
        inner_moves[j - 1].wait()
        total = total + xin["inner"][j - 1, 0].astype(high)
    ybuf["inner"][0] = total.astype(low)
    step_y("inner")
    finish_z("outer")
    step_z("vec", 2)
    step_z("qkvo", 2)
    halves.wait()
    token_grads[y] = base[0:part, :] + recv_rows[0:part, :].astype(high)
    step_core("inner")
    for t in range(3, size_z):
        step_z("vec", t)
        step_z("qkvo", t)
    step_core("outer")
    finish_z("vec")
    back.wait()
    token_grads[1 - y] = far_rows[...].astype(high)
    stores[0].start()
    chunks = hidden // CHUNK
    buf = finish_core("inner")
    for i in range(2):
        owner = core if i == 0 else 1 - core
        for c in range(chunks):
            place = pl.ds(pl.multiple_of(c * CHUNK + owner * half, 128), half)
            grad_inner[:, place] = buf[i, :, c * half : (c + 1) * half]
    stores[5].start()
    buf = finish_core("outer")
    for i in range(2):
        owner = core if i == 0 else 1 - core
        grad_outer[:, pl.ds(pl.multiple_of(owner * half, 128), half)] = buf[i]
    stores[6].start()
    finish_z("qkvo")
    step_core("vec")
    step_core("qkvo")
    for name in zout:
        for t, way in steps:

            @pl.when(inside(target_of(t, way)))
            def _():
                z_move(name, t, way).wait_send()

    buf = finish_core("vec")
    vector_sums[...] = buf[0] + buf[1]
    stores[7].start()
    buf = finish_core("qkvo")
    for i in range(2):
        owner = core if i == 0 else 1 - core
        for p in range(pairs):
            place = pl.ds(pl.multiple_of(owner * half + p * 128, 128), 128)
            for n, out in enumerate((grad_query, grad_key, grad_value)):
                out[:, place] = buf[i, :, (3 * p + n) * 128 : (3 * p + n + 1) * 128]
        grad_output[:, pl.ds(pl.multiple_of(owner * half, 128), half)] = buf[i, :, lanes : lanes + half]
    for i in range(1, 5):
        stores[i].start()
    for store in stores:
        store.wait()


def deliver_kernel(count, mixed_mine, mixed_far, *refs):
    matrices, vectors = refs[:count], refs[count]
    mixed = refs[count + 1]
    outs = refs[count + 2 : 2 * count + 2]
    smalls = refs[2 * count + 2 : -(count + 4)]
    stage, bufs, in_sem, out_sem = refs[-(count + 4) : -(count + 2)], refs[-(count + 2) : -2], refs[-2], refs[-1]
    y = lax.axis_index("y")
    moves = [(mixed_mine, stage[0], mixed.at[y]), (mixed_far, stage[1], mixed.at[1 - y])]
    for src, buf, dst in zip(matrices, bufs, outs):
        if len(src.shape) == 3:
            moves += [(src.at[i], buf.at[i], dst.at[i]) for i in range(src.shape[0])]
        else:
            moves.append((src, buf, dst))
    first = [pltpu.make_async_copy(src, buf, in_sem.at[i]) for i, (src, buf, _) in enumerate(moves)]
    second = [pltpu.make_async_copy(buf, dst, out_sem.at[i]) for i, (_, buf, dst) in enumerate(moves)]
    for copy in first:
        copy.start()
    for i, small in enumerate(smalls):
        small[...] = vectors[i : i + 1, 0 : small.shape[1]]
    for arrived, leaving in zip(first, second):
        arrived.wait()
        leaving.start()
    for copy in second:
        copy.wait()


def deliver(mixed_mine, mixed_far, matrices, vectors, sizes):
    count = len(matrices)
    vmem, anywhere = pl.BlockSpec(memory_space=pltpu.VMEM), pl.BlockSpec(memory_space=pl.ANY)
    moves = count + 4
    return pl.pallas_call(
        lambda *refs: deliver_kernel(count, *refs),
        out_shape=(jax.ShapeDtypeStruct((2,) + mixed_mine.shape, mixed_mine.dtype),)
        + tuple(jax.ShapeDtypeStruct(m.shape, m.dtype) for m in matrices)
        + tuple(jax.ShapeDtypeStruct((1, size), jnp.float32) for size in sizes),
        in_specs=[anywhere] * (2 + count) + [vmem],
        out_specs=(anywhere,) * (count + 1) + (vmem,) * len(sizes),
        scratch_shapes=[pltpu.VMEM(mixed_mine.shape, mixed_mine.dtype)] * 2
        + [pltpu.VMEM(m.shape, m.dtype) for m in matrices]
        + [pltpu.SemaphoreType.DMA((moves,))] * 2,
        compiler_params=pltpu.CompilerParams(vmem_limit_bytes=60_000_000),
        name="deliver",
    )(mixed_mine, mixed_far, *matrices, vectors)


def exit_call(size_z, size_x, grads, inputs, weights, base, output_term, dense_sums, inner_sums, head_sums, inner_terms, outer_terms):
    shards, rows, width = output_term.shape
    lanes = grads.shape[1]
    half = width // 2
    pairs = half // 128
    length = inputs.shape[0]
    local = length // 2
    part = local // 2
    long = outer_terms[0].shape[1]
    hidden = 2 * inner_terms[0].shape[2]
    vmem, anywhere = pl.BlockSpec(memory_space=pltpu.VMEM), pl.BlockSpec(memory_space=pl.ANY)
    dma = pltpu.SemaphoreType.DMA
    side = size_x - 1
    full = lanes + half
    low, high = jnp.bfloat16, jnp.float32
    vector_shape = (16, hidden // shards)
    shapes = {
        "vec": (vector_shape, high, 1),
        "qkvo": ((rows, full), low, 1),
        "inner": ((rows, hidden // 2), low, 1),
        "outer": ((long, half), low, 1),
    }
    matrix = jax.ShapeDtypeStruct((rows, width), high)
    results = (
        jax.ShapeDtypeStruct((2, part, width), high),
        matrix,
        matrix,
        matrix,
        matrix,
        jax.ShapeDtypeStruct((rows, hidden), high),
        jax.ShapeDtypeStruct((long, width), high),
        jax.ShapeDtypeStruct(vector_shape, high),
    )
    scratch = [pltpu.VMEM(r.shape, r.dtype) for r in results] + [
        pltpu.VMEM((length, lanes), low),
        pltpu.VMEM((length, width), low),
        pltpu.VMEM((width, length), low),
        pltpu.VMEM((width, lanes), low),
        pltpu.VMEM((local, width), high),
        pltpu.VMEM((shards, rows, full), low),
        pltpu.VMEM((local, width), low),
        pltpu.VMEM((local, width), low),
        pltpu.VMEM((part, width), low),
        pltpu.VMEM((part, width), low),
        pltpu.VMEM((shards, rows, half), low),
        pltpu.VMEM((size_z,) + inner_terms[0].shape, low),
        pltpu.VMEM((size_x,) + outer_terms[0].shape, low),
        pltpu.VMEM((16, width), high),
        pltpu.VMEM((shards,) + vector_shape, high),
        pltpu.VMEM((side, rows, hidden // 2), low),
        dma((len(results),)),
        dma((size_z + size_x + 4,)),
        dma((3,)),
        dma((3,)),
        dma,
        dma,
    ]
    for name, (shape, kind, sends) in shapes.items():
        scratch += [pltpu.VMEM((2,) + shape, kind), dma, dma, pltpu.VMEM((2,) + shape, high), dma, dma]
        stages = 1 if name == "inner" else size_z
        if name != "outer":
            scratch += [pltpu.VMEM((side, stages) + shape, kind), dma((sends, stages, side)), dma((sends, stages, side))]
        if name != "inner":
            scratch += [pltpu.VMEM((2, size_z - 1) + shape, kind)] * 2 + [dma((2, size_z - 1))] * 2
    return pl.pallas_call(
        lambda *refs: exit_kernel(size_z, size_x, shapes, *refs),
        out_shape=results,
        in_specs=[anywhere] * 4 + [vmem] * 4 + [anywhere] * (size_z + size_x),
        out_specs=(anywhere,) * len(results),
        scratch_shapes=scratch,
        compiler_params=pltpu.CompilerParams(collective_id=1, has_side_effects=True, vmem_limit_bytes=67_000_000),
        name="exit",
    )(grads, inputs, weights, base, output_term, dense_sums, inner_sums, head_sums, *inner_terms, *outer_terms)


TILE = 256
CHUNK = 768


def dot_nt(a, b):
    return lax.dot_general(a, b, (((1,), (1,)), ((), ())), preferred_element_type=jnp.float32)


def row_mean(value):
    return jnp.sum(value, axis=-1, keepdims=True) * (1.0 / value.shape[-1])


def standardize(hidden):
    centred = hidden - row_mean(hidden)
    reciprocal = lax.rsqrt(row_mean(centred * centred) + EPS)
    return centred * reciprocal, reciprocal


def column_sum(value):
    return jnp.sum(value.reshape(value.shape[0] // 8, 8, value.shape[1]), axis=0)


def dense_kernel(
    size_z,
    size_x,
    tokens_ref,
    mine_ref,
    other_hbm,
    cot_hbm,
    cot_far_hbm,
    vectors_ref,
    bias_inner_ref,
    *refs,
):
    inner_parts, outer_parts = refs[:size_x], refs[size_x : size_x + size_z]
    refs = refs[size_x + size_z :]
    mixed_ref, mixed_send_ref, pre_first_ref, grad_mine_ref, grad_far_hbm, sums_ref, inner_sum_ref, grad_output_ref = refs[:8]
    inner_terms = refs[8 : 8 + size_z]
    outer_terms = refs[8 + size_z : 8 + size_z + size_x]
    refs = refs[8 + size_z + size_x :]
    w_output, w_inner, w_outer, a_output, a_inner, a_outer, grad_out_buf = refs[:7]
    context, first_low, turned_low, normed, first, slope, active, work = refs[7:15]
    send_inner, send_outer, recv_inner, recv_outer = refs[15:19]
    far_rows, grad_send, ready, cotangent, cot_sem, swap_send, swap_recv = refs[19:26]
    load_sem, share_send, share_recv, send_sem, recv_sem, store_sem = refs[26:]
    step, steps = pl.program_id(0), pl.num_programs(0)
    core_here = lax.axis_index("core")
    width, hidden = w_inner.shape
    half = width // 2
    chunks = hidden // CHUNK
    shards = size_z * size_x
    z, x, y, _ = place_of()
    twin = partner(core=1 - lax.axis_index("core"))
    near = cotangent.shape[0] // 2
    cot_loads = (
        pltpu.make_async_copy(cot_hbm.at[y], cotangent.at[pl.ds(0, near), :], cot_sem.at[0]),
        pltpu.make_async_copy(cot_far_hbm, cotangent.at[pl.ds(near, near), :], cot_sem.at[1]),
    )

    shard = width // shards
    long = hidden // shards
    group = CHUNK // long // size_x

    def columns_of(first, owner):
        return pl.ds(pl.multiple_of(first + owner * half, 128), half)

    def start_piece(i, src, dst):
        pltpu.make_async_copy(src, dst, load_sem.at[i]).start()
        remote(src, dst, share_send.at[i], share_recv.at[i], twin).start()

    def start_rows(i, lane, ref, first):
        for j in range(size_x):
            for at in range(size_z):
                slot = at * size_x + lax.rem(x - j + size_x, size_x)
                rows = pl.ds(pl.multiple_of(slot * shard, shard), shard)
                start_piece(i, inner_parts[j].at[at, :, pl.ds(lane, half)], ref.at[rows, columns_of(first, core_here)])

    def start_loads():
        start_rows(0, hidden // 2, w_output, 0)
        for c in range(chunks):
            start_rows(1 + 2 * c, c * half, w_inner, c * CHUNK)
            for at in range(c * group, (c + 1) * group):
                for k in range(size_z):

                    @pl.when(lax.rem(z - k + size_z, size_z) == at)
                    def _():
                        for column in range(size_x):
                            rows = pl.ds((at * size_x + column) * long, long)
                            start_piece(2 + 2 * c, outer_parts[k].at[column], w_outer.at[rows, columns_of(0, core_here)])

    def wait_load(i, ref, rows, first):
        own, far = ref.at[rows, columns_of(first, core_here)], ref.at[rows, columns_of(first, 1 - core_here)]
        pltpu.make_async_copy(own, own, load_sem.at[i]).wait()
        remote(own, far, share_send.at[i], share_recv.at[i], twin).wait()

    @pl.when(step == 0)
    def _():
        barrier = pltpu.get_barrier_semaphore()
        pl.semaphore_signal(barrier, inc=1, device_id=twin, device_id_type=MESH_ID)
        pl.semaphore_wait(barrier, 1)
        remote(other_hbm, far_rows, swap_send.at[0], swap_recv.at[0], twin).start()
        start_loads()
        for load in cot_loads:
            load.start()
        a_output[...] = jnp.zeros_like(a_output)
        a_inner[...] = jnp.zeros_like(a_inner)
        a_outer[...] = jnp.zeros_like(a_outer)
        sums_ref[...] = jnp.zeros_like(sums_ref)
        inner_sum_ref[...] = jnp.zeros_like(inner_sum_ref)

    def vector(i):
        row = (2, 3, 4, 6, 7, 8)[i]
        return vectors_ref[row : row + 1, :]

    def add_sum(i, value):
        sums_ref[8 * i : 8 * i + 8, :] += column_sum(value)

    context[:, pl.ds(pl.multiple_of(core_here * half, 128), half)] = mine_ref[...]

    context_move = remote(other_hbm, far_rows, swap_send.at[0], swap_recv.at[0], twin)

    @pl.when(step == 0)
    def _():
        context_move.wait()

    here = pl.ds(pl.multiple_of(step * TILE, TILE), TILE)
    context[:, pl.ds(pl.multiple_of((1 - core_here) * half, 128), half)] = far_rows[here, :]

    @pl.when(step == 0)
    def _():
        wait_load(0, w_output, slice(None), 0)

    hidden_rows = tokens_ref[...].astype(jnp.float32) + (dot_nn(context[...], w_output[...]) + vector(0))
    normed[...], first_recip = standardize(hidden_rows)
    first[...] = normed[...] * vector(1) + vector(2)
    first_low[...] = first[...].astype(jnp.bfloat16)
    turned_low[...] = first_low[...].T
    work[...] = jnp.broadcast_to(vector(3), work.shape)

    def part(c):
        return pl.ds(c * CHUNK, CHUNK)

    def exchange(c):
        return (
            remote(send_inner.at[c], recv_inner.at[c], send_sem.at[0, c], recv_sem.at[0, c], twin),
            remote(send_outer.at[c], recv_outer.at[c], send_sem.at[1, c], recv_sem.at[1, c], twin),
        )

    def wait_inner(c):
        @pl.when(step == 0)
        def _():
            wait_load(1 + 2 * c, w_inner, slice(None), c * CHUNK)

    def ahead(c):
        ready[c % 2] = dot_nn(first_low[...], w_inner[:, part(c)])

    wait_inner(0)
    ahead(0)
    for c in range(chunks):
        if c + 1 < chunks:
            wait_inner(c + 1)

        @pl.when(step == 0)
        def _():
            wait_load(2 + 2 * c, w_outer, part(c), 0)

        if c + 1 < chunks:
            ahead(c + 1)
        u = ready[c % 2] + bias_inner_ref[0:1, part(c)]
        cdf = 0.5 * (1.0 + lax.erf(u * ROOT_HALF))
        slope[:, part(c)] = cdf + u * jnp.exp(-0.5 * u * u) * INV_ROOT_TAU
        acted = (u * cdf).astype(jnp.bfloat16)
        active[:, part(c)] = acted
        work[...] += dot_nn(acted, w_outer[part(c), :])

    second, second_recip = standardize(first[...] + work[...])
    mixed = (second * vector(4) + vector(5)).astype(jnp.bfloat16)

    @pl.when(step < steps // 2)
    def _():
        mixed_ref[...] = mixed

    @pl.when(step >= steps // 2)
    def _():
        mixed_send_ref[...] = mixed


    @pl.when(step == 0)
    def _():
        for load in cot_loads:
            load.wait()

    upstream = cotangent[pl.ds(pl.multiple_of(step * TILE, TILE), TILE), :].astype(jnp.float32)
    add_sum(0, upstream * second)
    add_sum(1, upstream)
    scaled = upstream * vector(4)
    pre_second = second_recip * (scaled - row_mean(scaled) - second * row_mean(scaled * second))
    grad_outer = pre_second.astype(jnp.bfloat16)
    add_sum(2, grad_outer.astype(jnp.float32))
    work[...] = pre_second
    grad_out_buf[...] = grad_outer

    def behind(c):
        ready[c % 2] = dot_nt(grad_out_buf[...], w_outer[part(c), :])

    behind(0)
    for c in range(chunks):
        if c + 1 < chunks:
            behind(c + 1)
        grad_inner = (ready[c % 2] * slope[:, part(c)]).astype(jnp.bfloat16)
        inner_sum_ref[:, part(c)] += column_sum(grad_inner.astype(jnp.float32))
        a_outer[part(c), :] += dot_nn(active[:, part(c)].T, grad_out_buf[...])
        a_inner[:, part(c)] += dot_nn(turned_low[...], grad_inner)
        work[...] += dot_nt(grad_inner, w_inner[:, part(c)])

        @pl.when(step == steps - 1)
        def _():
            theirs = pl.multiple_of(c * CHUNK + (1 - core_here) * half, 128)
            send_inner[c] = a_inner[:, pl.ds(theirs, half)].astype(jnp.bfloat16)
            send_outer[c] = a_outer[part(c), pl.ds(pl.multiple_of((1 - core_here) * half, 128), half)].astype(jnp.bfloat16)
            for move in exchange(c):
                move.start()

    grad_first = work[...]
    add_sum(3, grad_first * normed[...])
    add_sum(4, grad_first)
    scaled = grad_first * vector(1)
    pre_first = first_recip * (scaled - row_mean(scaled) - normed[...] * row_mean(scaled * normed[...]))
    pre_first_ref[...] = pre_first
    grad_attended = pre_first.astype(jnp.bfloat16)
    add_sum(5, grad_attended.astype(jnp.float32))
    a_output[...] += dot_nn(context[...].T, grad_attended)
    context[...] = dot_nt(grad_attended, w_output[...]).astype(jnp.bfloat16)
    grad_mine_ref[...] = context[:, pl.ds(pl.multiple_of(core_here * half, 128), half)]

    def grad_move(t):
        rows = pl.ds(pl.multiple_of(t * TILE, TILE), TILE)
        return remote(grad_send.at[t], grad_far_hbm.at[rows, :], swap_send.at[1 + t], swap_recv.at[1 + t], twin)

    grad_send[step] = context[:, pl.ds(pl.multiple_of((1 - core_here) * half, 128), half)]
    grad_move(step).start()

    @pl.when(step == steps - 1)
    def _():
        grad_output_ref[...] = a_output[...].astype(jnp.bfloat16)

        def inner_out(c):
            copies = []
            for k in range(size_z):
                for column in range(size_x):
                    slot = lax.rem(z + k, size_z) * size_x + column
                    src = send_inner.at[c, pl.ds(pl.multiple_of(slot * shard, shard), shard), :]
                    copies.append(
                        pltpu.make_async_copy(src, inner_terms[k].at[column, :, pl.ds(c * half, half)], store_sem.at[0, c])
                    )
            return copies

        def outer_out(c):
            copies = []
            for i in range(group):
                for j in range(size_x):
                    src = send_outer.at[c, pl.ds(pl.multiple_of((i * size_x + lax.rem(x + j, size_x)) * long, long), long), :]
                    copies.append(pltpu.make_async_copy(src, outer_terms[j].at[c * group + i], store_sem.at[1, c]))
            return copies

        for c in range(chunks):
            ours = pl.multiple_of(c * CHUNK + core_here * half, 128)
            first_move, second_move = exchange(c)
            first_move.wait()
            send_inner[c] = (a_inner[:, pl.ds(ours, half)] + recv_inner[c].astype(jnp.float32)).astype(jnp.bfloat16)
            for copy in inner_out(c):
                copy.start()
            second_move.wait()
            columns = pl.ds(pl.multiple_of(core_here * half, 128), half)
            send_outer[c] = (a_outer[part(c), columns] + recv_outer[c].astype(jnp.float32)).astype(jnp.bfloat16)
            for copy in outer_out(c):
                copy.start()
        for t in range(grad_send.shape[0]):
            grad_move(t).wait()
        for c in range(chunks):
            pltpu.make_async_copy(send_inner.at[c], send_inner.at[c], store_sem.at[0, c]).wait()
            pltpu.make_async_copy(send_outer.at[c], send_outer.at[c], store_sem.at[1, c]).wait()


def dense_layer(size_z, size_x, tokens, mine, other, cotangent, cotangent_far, vectors, bias_inner, inner_parts, outer_parts):
    local, half = mine.shape
    width = 2 * half
    hidden = bias_inner.shape[1]
    steps = local // TILE
    shards = size_z * size_x
    chunks = hidden // CHUNK
    low, high = jnp.bfloat16, jnp.float32
    tile = pl.BlockSpec((TILE, width), lambda t, *_: (t, 0))
    half_tile = pl.BlockSpec((TILE, half), lambda t, *_: (t, 0))
    anywhere = pl.BlockSpec(memory_space=pl.ANY)

    def whole(shape):
        return pl.BlockSpec(shape, lambda t, *_: (0, 0))

    inner_shape = jax.ShapeDtypeStruct((size_x, width // shards, hidden // 2), low)
    outer_shape = jax.ShapeDtypeStruct((size_z, hidden // shards, half), low)
    halves = pltpu.VMEM((chunks, width, half), low)
    dma = pltpu.SemaphoreType.DMA
    return pl.pallas_call(
        lambda *refs: dense_kernel(size_z, size_x, *refs),
        out_shape=(
            jax.ShapeDtypeStruct((local // 2, width), low),
            jax.ShapeDtypeStruct((local // 2, width), low),
            jax.ShapeDtypeStruct((local, width), high),
            jax.ShapeDtypeStruct((local, half), low),
            jax.ShapeDtypeStruct((local, half), low),
            jax.ShapeDtypeStruct((48, width), high),
            jax.ShapeDtypeStruct((8, hidden), high),
            jax.ShapeDtypeStruct((width, width), low),
        )
        + (inner_shape,) * size_z
        + (outer_shape,) * size_x,
        grid_spec=pltpu.PrefetchScalarGridSpec(
            num_scalar_prefetch=0,
            grid=(steps,),
            in_specs=[
                tile,
                half_tile,
                anywhere,
                anywhere,
                anywhere,
                whole((16, width)),
                whole((1, hidden)),
            ]
            + [anywhere] * (size_x + size_z),
            out_specs=[
                pl.BlockSpec((TILE, width), lambda t: (jnp.minimum(t, steps // 2 - 1), 0)),
                pl.BlockSpec((TILE, width), lambda t: (jnp.maximum(t - steps // 2, 0), 0)),
                tile,
                half_tile,
                anywhere,
                whole((48, width)),
                whole((8, hidden)),
                whole((width, width)),
            ]
            + [anywhere] * (size_z + size_x),
            scratch_shapes=[
                pltpu.VMEM((width, width), low),
                pltpu.VMEM((width, hidden), low),
                pltpu.VMEM((hidden, width), low),
                pltpu.VMEM((width, width), high),
                pltpu.VMEM((width, hidden), high),
                pltpu.VMEM((hidden, width), high),
                pltpu.VMEM((TILE, width), low),
                pltpu.VMEM((TILE, width), low),
                pltpu.VMEM((TILE, width), low),
                pltpu.VMEM((width, TILE), low),
                pltpu.VMEM((TILE, width), high),
                pltpu.VMEM((TILE, width), high),
                pltpu.VMEM((TILE, hidden), high),
                pltpu.VMEM((TILE, hidden), low),
                pltpu.VMEM((TILE, width), high),
                halves,
                halves,
                halves,
                halves,
                pltpu.VMEM((local, half), low),
                pltpu.VMEM((steps, TILE, half), low),
                pltpu.VMEM((2, TILE, CHUNK), high),
                pltpu.VMEM((local, width), low),
                dma((2,)),
                dma((1 + steps,)),
                dma((1 + steps,)),
                dma((1 + 2 * chunks,)),
                dma((1 + 2 * chunks,)),
                dma((1 + 2 * chunks,)),
                dma((2, chunks)),
                dma((2, chunks)),
                dma((2, chunks)),
            ],
        ),
        compiler_params=pltpu.CompilerParams(
            dimension_semantics=("arbitrary",), vmem_limit_bytes=67_000_000, collective_id=3, has_side_effects=True
        ),
        cost_estimate=pl.CostEstimate(flops=32_000_000_000, bytes_accessed=40_000_000, transcendentals=6_000_000),
        name="dense_layer",
    )(tokens, mine, other, cotangent, cotangent_far, vectors, bias_inner, *inner_parts, *outer_parts)


def lowered(piece):
    return piece.astype(jnp.bfloat16)


def widen(piece):
    return piece.astype(jnp.float32)


def matmul(left, right):
    return jnp.dot(left, right, preferred_element_type=jnp.float32)


def matmul_tn(left, right):
    return lax.dot_general(
        left, right, (((0,), (0,)), ((), ())), preferred_element_type=jnp.float32
    )


def matmul_nt(left, right):
    return lax.dot_general(
        left, right, (((1,), (1,)), ((), ())), preferred_element_type=jnp.float32
    )


def normalize(hidden, norm_gain, norm_shift):
    centred = hidden - jnp.mean(hidden, axis=-1, keepdims=True)
    reciprocal = lax.rsqrt(jnp.mean(centred * centred, axis=-1, keepdims=True) + EPS)
    normed = centred * reciprocal
    return (normed * norm_gain + norm_shift, normed, reciprocal)


def normalize_back(upstream, normed, reciprocal, norm_gain):
    scaled = upstream * norm_gain
    result = reciprocal * (
        scaled
        - jnp.mean(scaled, axis=-1, keepdims=True)
        - normed * jnp.mean(scaled * normed, axis=-1, keepdims=True)
    )
    return (result, jnp.sum(upstream * normed, axis=0), jnp.sum(upstream, axis=0))


def gelu_value(values_in):
    return 0.5 * values_in * (1.0 + lax.erf(values_in * ROOT_HALF))


def gelu_slope(values_in):
    return (
        0.5 * (1.0 + lax.erf(values_in * ROOT_HALF))
        + values_in * jnp.exp(-0.5 * values_in * values_in) * INV_ROOT_TAU
    )


def shift(piece, axis, step):
    size = lax.axis_size(axis)
    return lax.ppermute(piece, axis, [(i, (i + step) % size) for i in range(size)])


def swap(piece, axis):
    return lax.ppermute(piece, axis, [(0, 1), (1, 0)])


def pick(piece, index, axis=0):
    return lax.dynamic_index_in_dim(piece, index, axis, keepdims=False)


def in_order(first_is_zero, own, other, axis):
    return jnp.where(
        first_is_zero,
        jnp.concatenate([own, other], axis),
        jnp.concatenate([other, own], axis),
    )


def collect(piece):
    size_z, size_x = lax.axis_size("z"), lax.axis_size("x")
    z, x = lax.axis_index("z"), lax.axis_index("x")
    along_z = [piece] + [shift(piece, "z", k) for k in range(1, size_z)]
    whole = jnp.zeros((size_z, size_x) + piece.shape, piece.dtype)
    zeros = (0,) * piece.ndim
    for j in range(size_x):
        for k in range(size_z):
            arrived = along_z[k] if j == 0 else shift(along_z[k], "x", j)
            place = ((z - k) % size_z, (x - j) % size_x) + zeros
            whole = lax.dynamic_update_slice(whole, arrived[None, None], place)
    return whole.reshape((size_z * size_x,) + piece.shape)


def reduce_owned(terms):
    size_z, size_x = lax.axis_size("z"), lax.axis_size("x")
    z, x = lax.axis_index("z"), lax.axis_index("x")
    terms = terms.reshape((size_z, size_x) + terms.shape[1:])
    total = widen(pick(terms, x, 1))
    for j in range(1, size_x):
        total = total + widen(shift(pick(terms, (x + j) % size_x, 1), "x", j))
    terms = lowered(total)
    total = widen(pick(terms, z))
    for k in range(1, size_z):
        total = total + widen(shift(pick(terms, (z + k) % size_z), "z", k))
    terms = lowered(total)
    return widen(terms) + widen(swap(terms, "y"))


def plain_body(
    tokens,
    segment_ids,
    w_query,
    w_key,
    w_value,
    w_output,
    b_query,
    b_value,
    b_output,
    first_gain,
    first_shift,
    w_inner,
    b_inner,
    w_outer,
    b_outer,
    second_gain,
    second_shift,
    cotangent,
):
    core, y = lax.axis_index("core"), lax.axis_index("y")
    shards = lax.axis_size("z") * lax.axis_size("x")
    sequences, part, width = tokens.shape
    half = width // 2
    pairs = half // 128
    hidden = w_inner.shape[1]
    local = 2 * part
    own_rows = w_query.shape[0]
    unit_half = hidden // shards // 2

    def columns(matrix):
        return lowered(lax.dynamic_slice_in_dim(matrix, core * half, half, 1))

    vectors = (b_query, b_value, b_output, first_gain, first_shift, b_inner, b_outer, second_gain, second_shift)
    flat = jnp.concatenate([lowered(v) for v in vectors])
    lanes = 3 * half
    extra = -(-flat.shape[0] // lanes)
    flat = jnp.pad(flat, (0, extra * lanes - flat.shape[0])).reshape(extra, lanes)
    weights = jnp.stack([columns(w).reshape(own_rows, pairs, 128) for w in (w_query, w_key, w_value)], axis=2)
    early = collect(jnp.concatenate([weights.reshape(own_rows, lanes), flat], axis=0))

    mine = pick(tokens, y)
    arrived = swap(pick(tokens, 1 - y), "y")
    mine_other, arrived_other = swap(mine, "core"), swap(arrived, "core")
    inputs_all = jnp.concatenate([mine, arrived, mine_other, arrived_other], axis=0)
    inputs = jnp.concatenate([mine, arrived], axis=0)

    inner_piece = lowered(pick(w_inner.reshape(own_rows, shards, 2, unit_half), core, 2)).reshape(own_rows, hidden // 2)
    late = collect(jnp.concatenate([columns(w_output), inner_piece], axis=1)).reshape(width, half + hidden // 2)
    outer_own = collect(lowered(lax.dynamic_slice_in_dim(w_outer, core * unit_half, unit_half, 0))).reshape(hidden // 2, width)
    output_own, inner_own = late[:, :half], late[:, half:]
    output_other, inner_other, outer_other = swap(output_own, "core"), swap(inner_own, "core"), swap(outer_own, "core")
    full_output = in_order(core == 0, output_own, output_other, 1)
    cotangent_mine = pick(cotangent, y)
    cotangent_arrived = swap(pick(cotangent, 1 - y), "y")

    full_early = early[:, :own_rows].reshape(width, lanes)
    flat_all = early[:, own_rows:].reshape(shards, extra * lanes)
    sizes = [v.shape[0] for v in vectors]
    gathered, at = [], 0
    for size in sizes:
        gathered.append(flat_all[:, at : at + size].reshape(shards * size))
        at += size
    bias_query, bias_value, bias_output, gain_first, shift_first, bias_inner, bias_outer, gain_second, shift_second = [
        widen(v) for v in gathered
    ]
    biases = jnp.concatenate([bias_query[None], bias_value[None], jnp.zeros((14, width), jnp.float32)], axis=0)
    heads_mine, heads_other, logsum, projected = attention(segment_ids, inputs_all, full_early, biases)
    context = in_order(core == 0, heads_mine, swap(heads_other, "core"), 1)

    attended = matmul(context, full_output) + bias_output
    first, first_normed, first_recip = normalize(widen(inputs) + attended, gain_first, shift_first)
    first_low = lowered(first)
    biases = bias_inner.reshape(shards, 2, unit_half)
    halves = ((inner_own, outer_own, pick(biases, core, 1)), (inner_other, outer_other, pick(biases, 1 - core, 1)))
    outer, kept = bias_outer, []
    for inner_weight, outer_weight, bias in halves:
        inner = matmul(first_low, inner_weight) + bias.reshape(hidden // 2)
        active = lowered(gelu_value(inner))
        outer = outer + matmul(active, outer_weight)
        kept.append((inner, active))
    mixed, second_normed, second_recip = normalize(first + outer, gain_second, shift_second)
    mixed = lowered(mixed)

    upstream = widen(jnp.concatenate([cotangent_mine, cotangent_arrived], axis=0))
    pre_second, grad_second_gain, grad_second_shift = normalize_back(upstream, second_normed, second_recip, gain_second)
    grad_outer = lowered(pre_second)
    grad_b_outer = jnp.sum(widen(grad_outer), axis=0)
    grad_first, inner_grads, outer_grads, bias_grads = pre_second, [], [], []
    for (inner, active), (inner_weight, outer_weight, _) in zip(kept, halves):
        grad_inner = lowered(matmul_nt(grad_outer, outer_weight) * gelu_slope(inner))
        outer_grads.append(lowered(matmul_tn(active, grad_outer)))
        inner_grads.append(lowered(matmul_tn(first_low, grad_inner)))
        bias_grads.append(jnp.sum(widen(grad_inner), axis=0).reshape(shards, 1, unit_half))
        grad_first = grad_first + matmul_nt(grad_inner, inner_weight)
    grad_b_inner = in_order(core == 0, bias_grads[0], bias_grads[1], 1).reshape(hidden)
    pre_first, grad_first_gain, grad_first_shift = normalize_back(grad_first, first_normed, first_recip, gain_first)
    grad_attended = lowered(pre_first)
    grad_b_output = jnp.sum(widen(grad_attended), axis=0)
    grad_w_output = lowered(matmul_tn(context, grad_attended))
    grad_context = lowered(matmul_nt(grad_attended, full_output))
    context_mine = lax.dynamic_slice_in_dim(grad_context, core * half, half, 1)
    context_other = lax.dynamic_slice_in_dim(grad_context, (1 - core) * half, half, 1)
    upstream_other = swap(context_other, "core")

    def core_sum(own, other):
        return lowered(widen(own) + widen(swap(other, "core")))

    outer_term = core_sum(*outer_grads)
    inner_term = core_sum(*inner_grads)
    output_term = core_sum(
        lax.dynamic_slice_in_dim(grad_w_output, core * half, half, 1),
        lax.dynamic_slice_in_dim(grad_w_output, (1 - core) * half, half, 1),
    )
    outer_done = reduce_owned(outer_term.reshape(shards, unit_half, width))
    late_done = reduce_owned(jnp.concatenate([output_term, inner_term], axis=1).reshape(shards, own_rows, half + hidden // 2))

    grads, sums = attention_back(segment_ids, projected, heads_mine, heads_other, context_mine, upstream_other, logsum)
    grad_early = lowered(matmul_tn(inputs_all, grads))
    partial = matmul_nt(grads, full_early)
    sums = sums.reshape(pairs, 8, 3, 128)[:, 0]
    blank = jnp.zeros((width,), jnp.float32)
    grad_b_query = lax.dynamic_update_slice(blank, sums[:, 0].reshape(half), (core * half,))
    grad_b_value = lax.dynamic_update_slice(blank, sums[:, 2].reshape(half), (core * half,))
    vector_grads = (
        grad_b_query,
        grad_b_value,
        grad_b_output,
        grad_first_gain,
        grad_first_shift,
        grad_b_inner,
        grad_b_outer,
        grad_second_gain,
        grad_second_shift,
    )
    flat_grads = jnp.concatenate([v.reshape(shards, -1) for v in vector_grads], axis=1)
    flat_grads = jnp.pad(flat_grads, ((0, 0), (0, extra * lanes - flat_grads.shape[1])))
    early_term = jnp.concatenate(
        [grad_early.reshape(shards, own_rows, lanes), lowered(flat_grads).reshape(shards, extra, lanes)], axis=1
    )
    early_done = reduce_owned(early_term)

    grad_inputs = pre_first + partial[:local] + widen(swap(lowered(partial[local:]), "core"))
    returned = widen(swap(lowered(grad_inputs[part:]), "y"))
    grad_tokens = in_order(y == 0, grad_inputs[None, :part], returned[None], 0)
    mixed_out = in_order(y == 0, mixed[None, :part], swap(mixed[part:], "y")[None], 0)

    def both(piece):
        return widen(swap(lowered(piece), "core"))

    early_matrix = early_done[:own_rows]
    early_full = in_order(
        core == 0, early_matrix.reshape(own_rows, pairs, 3, 128)[None], both(early_matrix).reshape(own_rows, pairs, 3, 128)[None], 0
    )
    early_full = early_full.transpose(3, 1, 0, 2, 4).reshape(3, own_rows, width)
    late_other = both(late_done)
    output_full = in_order(core == 0, late_done[:, :half], late_other[:, :half], 1)
    inner_full = in_order(
        core == 0,
        late_done[:, half:].reshape(own_rows, shards, 1, unit_half),
        late_other[:, half:].reshape(own_rows, shards, 1, unit_half),
        2,
    ).reshape(own_rows, hidden)
    outer_full = in_order(core == 0, outer_done, both(outer_done), 0)
    vector_part = early_done[own_rows:]
    vector_sums = (vector_part + swap(vector_part, "core")).reshape(extra * lanes)
    out_vectors, at = [], 0
    for size in sizes:
        out_vectors.append(vector_sums[at : at + size])
        at += size
    (
        done_b_query,
        done_b_value,
        done_b_output,
        done_first_gain,
        done_first_shift,
        done_b_inner,
        done_b_outer,
        done_second_gain,
        done_second_shift,
    ) = out_vectors
    return (
        mixed_out,
        grad_tokens,
        early_full[0],
        early_full[1],
        early_full[2],
        output_full,
        done_b_query,
        done_b_value,
        done_b_output,
        done_first_gain,
        done_first_shift,
        inner_full,
        done_b_inner,
        outer_full,
        done_b_outer,
        done_second_gain,
        done_second_shift,
    )


def body(
    tokens,
    segment_ids,
    w_query,
    w_key,
    w_value,
    w_output,
    b_query,
    b_value,
    b_output,
    first_gain,
    first_shift,
    w_inner,
    b_inner,
    w_outer,
    b_outer,
    second_gain,
    second_shift,
    cotangent,
):
    core, y = lax.axis_index("core"), lax.axis_index("y")
    size_z, size_x = lax.axis_size("z"), lax.axis_size("x")
    shards = size_z * size_x
    sequences, part, width = tokens.shape
    half = width // 2
    pairs = half // 128
    hidden = w_inner.shape[1]
    local = 2 * part
    own_rows = w_query.shape[0]
    lanes = 3 * half

    vectors = (b_query, b_value, b_output, first_gain, first_shift, b_inner, b_outer, second_gain, second_shift)
    sizes = [v.shape[0] for v in vectors]
    tokens_all, cotangent_send, early, inner_own, outer_own, rows, inner_row = entry(
        size_z, size_x, tokens, cotangent, w_query, w_key, w_value, w_inner, w_output, w_outer, vectors
    )
    cotangent_far = swap(cotangent_send, "y")
    inner_parts = [inner_own] + [shift(inner_own, "x", j) for j in range(1, size_x)]
    outer_parts = [outer_own] + [shift(outer_own, "z", k) for k in range(1, size_z)]
    inputs_all = tokens_all.reshape(4 * part, width)
    full_early = early.reshape(width, lanes)
    context_mine, context_other, logsum, projected = attention(segment_ids, inputs_all, full_early, rows)
    made = dense_layer(
        size_z,
        size_x,
        inputs_all,
        context_mine,
        context_other,
        cotangent,
        cotangent_far,
        rows,
        inner_row,
        inner_parts,
        outer_parts,
    )
    mixed, mixed_send, pre_first, upstream_mine, upstream_other, dense_sums, inner_sums, grad_w_output = made[:8]
    inner_terms = [made[8]] + [shift(made[8 + k], "z", k) for k in range(1, size_z)]
    outer_terms = [made[8 + size_z]] + [shift(made[8 + size_z + j], "x", j) for j in range(1, size_x)]
    mixed_far = swap(mixed_send, "y")
    grads, sums = attention_back(segment_ids, projected, context_mine, context_other, upstream_mine, upstream_other, logsum)
    made = exit_call(
        size_z,
        size_x,
        grads,
        inputs_all,
        full_early,
        pre_first,
        grad_w_output.reshape(shards, own_rows, width),
        dense_sums,
        inner_sums,
        sums,
        inner_terms,
        outer_terms,
    )
    mixed_out, grad_tokens, grad_query, grad_key, grad_value, grad_output, grad_inner_full, grad_outer_full, *done = deliver(
        mixed, mixed_far, made[:7], made[7], sizes
    )
    done = [v.reshape(size) for v, size in zip(done, sizes)]
    return (
        mixed_out,
        grad_tokens,
        grad_query,
        grad_key,
        grad_value,
        grad_output,
        *done[:5],
        grad_inner_full,
        done[5],
        grad_outer_full,
        *done[6:],
    )


def layer(*arrays):
    if arrays[2].shape[0] % 32 == 0 and lax.axis_size("x") > 1:
        return body(*arrays)
    return plain_body(*arrays)


def solution(mesh):
    outer, inner = mesh.devices.shape
    size_z = 1
    while size_z * size_z < outer:
        size_z *= 2
    split = Mesh(mesh.devices.reshape(size_z, outer // size_z, inner // 2, 2), ("z", "x", "y", "core"))
    dp, seq = ("z", "x"), ("y", "core")
    activation, matrix, vector = P(dp, seq, None), P(dp, None), P(dp)
    return jax.shard_map(
        layer,
        mesh=split,
        in_specs=(
            activation,
            matrix,
            matrix,
            matrix,
            matrix,
            matrix,
            vector,
            vector,
            vector,
            vector,
            vector,
            matrix,
            vector,
            matrix,
            vector,
            vector,
            vector,
            activation,
        ),
        out_specs=(
            activation,
            activation,
            matrix,
            matrix,
            matrix,
            matrix,
            vector,
            vector,
            vector,
            vector,
            vector,
            matrix,
            vector,
            matrix,
            vector,
            vector,
            vector,
        ),
        check_vma=False,
    )
```

```python
import jax
import jax.numpy as jnp
from jax import lax
from jax.experimental import pallas as pl
from jax.experimental.pallas import tpu as pltpu
from jax.sharding import Mesh
from jax.sharding import PartitionSpec as P


HD = 64
EPS = 1e-12
ROOT_HALF = 0.7071067811865476
INV_ROOT_TAU = 0.3989422804014327

BLK = 256
BIG = -1.0e9
DOCUMENTS = 4


def dot_nn(a, b):
    return jnp.dot(a, b, preferred_element_type=jnp.float32)


def local_start(b, part):
    core, y = lax.axis_index("core"), lax.axis_index("y")
    return (jnp.where(b % 2 == core, 0, 2) + jnp.where(b // 2 == y, 0, 1)) * part


def part_rows(b, part):
    return pl.ds(pl.multiple_of(local_start(b, part), 128), part)


def find_bounds(segment_ref, bound_ref):
    length = segment_ref.shape[1]
    y = lax.axis_index("y")
    bound_ref[0] = 0
    bound_ref[DOCUMENTS] = length
    for d in range(1, DOCUMENTS):

        def halve(_, span):
            low, high = span
            middle = (low + high) // 2
            below = segment_ref[y, jnp.minimum(middle, length - 1)] < d
            inside = low < high
            return (
                jnp.where(jnp.logical_and(inside, below), middle + 1, low),
                jnp.where(jnp.logical_and(inside, jnp.logical_not(below)), middle, high),
            )

        low, _ = lax.fori_loop(0, length.bit_length(), halve, (0, length))
        bound_ref[d] = low


def find_window(segment_ref, bound_ref, qb):
    length = segment_ref.shape[1]
    y = lax.axis_index("y")
    first = segment_ref[y, qb * BLK]
    last = segment_ref[y, qb * BLK + BLK - 1]
    start = bound_ref[first] // 128 * 128
    count = (bound_ref[last + 1] - start + BLK - 1) // BLK
    return jnp.minimum(start, length - count * BLK), count


def each_tile(count, step):
    def two(i, _):
        step(i * (2 * BLK), 2 * BLK)
        return 0

    lax.fori_loop(0, count // 2, two, 0)

    @pl.when(count % 2 == 1)
    def _():
        step((count - 1) * BLK, BLK)


def make_marks(row_ref, mark_query, mark_key):
    length = mark_key.shape[0]
    y = lax.axis_index("y")
    step = 512
    for b in range(length // step):
        rows = slice(b * step, (b + 1) * step)
        column = jnp.broadcast_to(row_ref[pl.ds(y, 1), rows], (128, step)).T
        lane = lax.broadcasted_iota(jnp.int32, (step, 128), 1) % 64
        same = lane == column
        line = lax.broadcasted_iota(jnp.int32, (128, step), 0) % 64
        mark_query[:, rows] = jnp.where(line == row_ref[pl.ds(y, 1), rows], 1.0, 0.0).astype(jnp.bfloat16)
        apart = jnp.logical_and(lane < DOCUMENTS, jnp.logical_not(same))
        mark_key[rows, :] = jnp.where(apart, BIG, 0.0).astype(jnp.bfloat16)


def forward_kernel(segment_ref, row_ref, tokens_ref, weights_ref, bias_ref, *refs):
    mine_ref, other_ref, lse_ref, qkv_ref, q2, k2, vt, acc, top, tot, keep, mark_query, mark_key, bound_ref = refs
    length = qkv_ref.shape[0]
    blocks = length // BLK
    part = length // 4

    @pl.when(pl.program_id(0) == 0)
    def _():
        find_bounds(segment_ref, bound_ref)
        make_marks(row_ref, mark_query, mark_key)

    low = lax.broadcasted_iota(jnp.int32, (part, 128), 1) < 64
    for b in range(4):
        src = part_rows(b, part)
        dst = slice(b * part, (b + 1) * part)
        made = dot_nn(tokens_ref[src, :], weights_ref[...])
        lanes = pl.ds(pl.multiple_of(lax.axis_index("core") * (128 * pl.num_programs(0)) + pl.program_id(0) * 128, 128), 128)
        q = ((made[:, 0:128] + bias_ref[0:1, lanes]) * 0.125).astype(jnp.bfloat16)
        k = made[:, 128:256].astype(jnp.bfloat16)
        v = (made[:, 256:384] + bias_ref[1:2, lanes]).astype(jnp.bfloat16)
        qkv_ref[src, 0:128] = q
        qkv_ref[src, 128:256] = k
        qkv_ref[src, 256:384] = v
        nohk = mark_key[dst, :]
        turned = q.T
        q2[0, 0:64, dst] = turned[0:64]
        q2[0, 64:128, dst] = mark_query[64:128, dst]
        q2[1, 0:64, dst] = mark_query[0:64, dst]
        q2[1, 64:128, dst] = turned[64:128]
        k2[0, dst, :] = jnp.where(low, k, nohk)
        k2[1, dst, :] = jnp.where(low, nohk, k)
        vt[:, dst] = v.T
    lse_ref[...] = jnp.zeros_like(lse_ref)

    def row(qb, _):
        qs = pl.ds(pl.multiple_of(qb * BLK, BLK), BLK)
        start, count = find_window(segment_ref, bound_ref, qb)
        top[...] = jnp.full_like(top, -1.0e30)

        def fold(tile, function):
            return function(tile.reshape(tile.shape[0] // 8, 8, BLK), axis=0)

        def highest(first, size):
            keys = pl.ds(pl.multiple_of(start + first, 128), size)
            for h in range(2):
                st = dot_nn(k2[h, keys, :], q2[h, :, qs])
                keep[h, pl.ds(pl.multiple_of(first, BLK), size), :] = st
                top[h] = jnp.maximum(top[h], fold(st, jnp.max))

        def weigh(first, size, largest):
            keys = pl.ds(pl.multiple_of(start + first, 128), size)
            for h in range(2):
                rows = slice(64 * h, 64 * h + 64)
                st = keep[h, pl.ds(pl.multiple_of(first, BLK), size), :]
                p = jnp.exp(st - largest[h])
                tot[h] = tot[h] + fold(p, jnp.sum)
                acc[rows, :] = acc[rows, :] + dot_nn(vt[rows, keys], p.astype(jnp.bfloat16))

        def paired(step):
            each_tile(count, step)

        paired(highest)
        largest = [jnp.max(top[h], axis=0, keepdims=True) for h in range(2)]
        acc[...] = jnp.zeros_like(acc)
        tot[...] = jnp.zeros_like(tot)
        paired(lambda first, size: weigh(first, size, largest))
        for h in range(2):
            rows = slice(64 * h, 64 * h + 64)
            total = jnp.sum(tot[h], axis=0, keepdims=True)
            acc[rows, :] = acc[rows, :] / total
            lse_ref[h : h + 1, qs] = largest[h] + jnp.log(total)
        where = local_start(qb * BLK // part, part) + qb * BLK % part
        result = acc[...].T.astype(jnp.bfloat16)

        @pl.when(where < 2 * part)
        def _():
            mine_ref[pl.ds(pl.multiple_of(where, BLK), BLK), :] = result

        @pl.when(where >= 2 * part)
        def _():
            other_ref[pl.ds(pl.multiple_of(where - 2 * part, BLK), BLK), :] = result

        return 0

    lax.fori_loop(0, blocks, row, 0)


def attention(segments, tokens, weights, biases):
    length, depth = tokens.shape
    width = weights.shape[1]
    pairs = width // 384
    rows = length // 2
    return pl.pallas_call(
        forward_kernel,
        out_shape=(
            jax.ShapeDtypeStruct((rows, pairs * 128), jnp.bfloat16),
            jax.ShapeDtypeStruct((rows, pairs * 128), jnp.bfloat16),
            jax.ShapeDtypeStruct((pairs * 8, length), jnp.float32),
            jax.ShapeDtypeStruct((length, width), jnp.bfloat16),
        ),
        grid_spec=pltpu.PrefetchScalarGridSpec(
            num_scalar_prefetch=1,
            grid=(pairs,),
            in_specs=[
                pl.BlockSpec(segments.shape, lambda p, *_: (0, 0)),
                pl.BlockSpec((length, depth), lambda p, *_: (0, 0)),
                pl.BlockSpec((depth, 384), lambda p, *_: (0, p)),
                pl.BlockSpec(biases.shape, lambda p, *_: (0, 0)),
            ],
            out_specs=[
                pl.BlockSpec((rows, 128), lambda p, *_: (0, p)),
                pl.BlockSpec((rows, 128), lambda p, *_: (0, p)),
                pl.BlockSpec((8, length), lambda p, *_: (p, 0)),
                pl.BlockSpec((length, 384), lambda p, *_: (0, p)),
            ],
            scratch_shapes=[
                pltpu.VMEM((2, 128, length), jnp.bfloat16),
                pltpu.VMEM((2, length, 128), jnp.bfloat16),
                pltpu.VMEM((128, length), jnp.bfloat16),
                pltpu.VMEM((128, BLK), jnp.float32),
                pltpu.VMEM((2, 8, BLK), jnp.float32),
                pltpu.VMEM((2, 8, BLK), jnp.float32),
                pltpu.VMEM((2, length, BLK), jnp.float32),
                pltpu.VMEM((128, length), jnp.bfloat16),
                pltpu.VMEM((length, 128), jnp.bfloat16),
                pltpu.SMEM((DOCUMENTS + 1,), jnp.int32),
            ],
        ),
        compiler_params=pltpu.CompilerParams(dimension_semantics=("arbitrary",), vmem_limit_bytes=60 << 20),
        cost_estimate=pl.CostEstimate(flops=pairs * 40_000_000_000, bytes_accessed=pairs * 3_000_000, transcendentals=pairs * 4_000_000),
        name="attention_forward",
    )(segments, segments, tokens, weights, biases)


def backward_kernel(
    segment_ref,
    qkv_ref,
    ctx_mine_ref,
    ctx_other_ref,
    do_mine_ref,
    do_other_ref,
    lse_ref,
    row_ref,
    out_ref,
    sum_ref,
    q2,
    k2,
    q0,
    d0,
    dt,
    v0,
    kt,
    dk,
    dv,
    dqt,
    delta,
    mark_query,
    mark_key,
    bound_ref,
):
    length = qkv_ref.shape[0]
    blocks = length // BLK
    part = length // 4

    @pl.when(pl.program_id(0) == 0)
    def _():
        find_bounds(segment_ref, bound_ref)
        make_marks(row_ref, mark_query, mark_key)

    low = lax.broadcasted_iota(jnp.int32, (part, 128), 1) < 64

    def prepare(b, do, ctx):
        src = part_rows(b, part)
        dst = slice(b * part, (b + 1) * part)
        q, k = qkv_ref[src, 0:128], qkv_ref[src, 128:256]
        zero = jnp.zeros_like(q)
        nohk = mark_key[dst, :]
        turned = q.T
        q2[0, 0:64, dst] = turned[0:64]
        q2[0, 64:128, dst] = mark_query[64:128, dst]
        q2[1, 0:64, dst] = mark_query[0:64, dst]
        q2[1, 64:128, dst] = turned[64:128]
        k2[0, dst, :] = jnp.where(low, k, nohk)
        k2[1, dst, :] = jnp.where(low, nohk, k)
        q0[0, dst, :] = jnp.where(low, q, zero)
        q0[1, dst, :] = jnp.where(low, zero, q)
        d0[0, dst, :] = jnp.where(low, do, zero)
        d0[1, dst, :] = jnp.where(low, zero, do)
        turned = do.T
        blank = jnp.zeros((64, part), jnp.bfloat16)
        dt[0, 0:64, dst] = turned[0:64]
        dt[0, 64:128, dst] = blank
        dt[1, 0:64, dst] = blank
        dt[1, 64:128, dst] = turned[64:128]
        v0[dst, :] = qkv_ref[src, 256:384]
        kt[:, dst] = k.T
        prod = turned.astype(jnp.float32) * ctx.T.astype(jnp.float32)
        delta[0:1, dst] = jnp.sum(prod[0:64], axis=0, keepdims=True)
        delta[1:2, dst] = jnp.sum(prod[64:128], axis=0, keepdims=True)

    for b in range(4):

        @pl.when(local_start(b, part) < 2 * part)
        def _():
            rows = part_rows(b, part)
            prepare(b, do_mine_ref[rows, :], ctx_mine_ref[rows, :])

        @pl.when(local_start(b, part) >= 2 * part)
        def _():
            rows = pl.ds(pl.multiple_of(local_start(b, part) - 2 * part, 128), part)
            prepare(b, do_other_ref[rows, :], ctx_other_ref[rows, :])

    dk[...] = jnp.zeros_like(dk)
    dv[...] = jnp.zeros_like(dv)
    dqt[...] = jnp.zeros_like(dqt)

    def row(qb, _):
        qs = pl.ds(pl.multiple_of(qb * BLK, BLK), BLK)
        start, count = find_window(segment_ref, bound_ref, qb)

        def tile(first, size):
            ks = pl.ds(pl.multiple_of(start + first, 128), size)
            weights, grads = [], []
            for h in range(2):
                st = dot_nn(k2[h, ks, :], q2[h, :, qs])
                w = jnp.exp(st - lse_ref[h : h + 1, qs])
                gw = dot_nn(v0[ks, :], dt[h, :, qs])
                weights.append(w.astype(jnp.bfloat16))
                grads.append((w * (gw - delta[h : h + 1, qs])).astype(jnp.bfloat16))
            dv[ks, :] += dot_nn(jnp.concatenate(weights, axis=1), jnp.concatenate([d0[0, qs, :], d0[1, qs, :]], axis=0))
            dk[ks, :] += dot_nn(jnp.concatenate(grads, axis=1), jnp.concatenate([q0[0, qs, :], q0[1, qs, :]], axis=0))
            for h in range(2):
                rows = slice(64 * h, 64 * h + 64)
                dqt[rows, qs] += dot_nn(kt[rows, ks], grads[h])

        each_tile(count, tile)
        return 0

    lax.fori_loop(0, blocks, row, 0)
    sums = [jnp.zeros((1, 128), jnp.float32) for _ in range(3)]
    for b in range(4):
        dst = part_rows(b, part)
        src = slice(b * part, (b + 1) * part)
        pieces = ((dqt[:, src].T * 0.125).astype(jnp.bfloat16), dk[src, :].astype(jnp.bfloat16), dv[src, :].astype(jnp.bfloat16))
        for i, piece in enumerate(pieces):
            out_ref[dst, 128 * i : 128 * i + 128] = piece
            sums[i] = sums[i] + jnp.sum(piece.astype(jnp.float32), axis=0, keepdims=True)
    sum_ref[...] = jnp.zeros_like(sum_ref)
    for i in range(3):
        sum_ref[0:1, 128 * i : 128 * i + 128] = sums[i]


def attention_back(segments, qkv, ctx_mine, ctx_other, do_mine, do_other, lse):
    length, width = qkv.shape
    pairs = width // 384
    rows = length // 2
    half = lambda: pltpu.VMEM((2, length, 128), jnp.bfloat16)
    turned = lambda: pltpu.VMEM((2, 128, length), jnp.bfloat16)
    column = pl.BlockSpec((rows, 128), lambda p, *_: (0, p))
    return pl.pallas_call(
        backward_kernel,
        out_shape=(
            jax.ShapeDtypeStruct((length, width), jnp.bfloat16),
            jax.ShapeDtypeStruct((pairs * 8, 384), jnp.float32),
        ),
        grid_spec=pltpu.PrefetchScalarGridSpec(
            num_scalar_prefetch=1,
            grid=(pairs,),
            in_specs=[
                pl.BlockSpec((length, 384), lambda p, *_: (0, p)),
                column,
                column,
                column,
                column,
                pl.BlockSpec((8, length), lambda p, *_: (p, 0)),
                pl.BlockSpec(segments.shape, lambda p, *_: (0, 0)),
            ],
            out_specs=[
                pl.BlockSpec((length, 384), lambda p, *_: (0, p)),
                pl.BlockSpec((8, 384), lambda p, *_: (p, 0)),
            ],
            scratch_shapes=[
                turned(),
                half(),
                half(),
                half(),
                turned(),
                pltpu.VMEM((length, 128), jnp.bfloat16),
                pltpu.VMEM((128, length), jnp.bfloat16),
                pltpu.VMEM((length, 128), jnp.float32),
                pltpu.VMEM((length, 128), jnp.float32),
                pltpu.VMEM((128, length), jnp.float32),
                pltpu.VMEM((8, length), jnp.float32),
                pltpu.VMEM((128, length), jnp.bfloat16),
                pltpu.VMEM((length, 128), jnp.bfloat16),
                pltpu.SMEM((DOCUMENTS + 1,), jnp.int32),
            ],
        ),
        compiler_params=pltpu.CompilerParams(dimension_semantics=("arbitrary",), vmem_limit_bytes=60 << 20),
        cost_estimate=pl.CostEstimate(flops=pairs * 20_000_000_000, bytes_accessed=pairs * 5_000_000, transcendentals=pairs * 4_000_000),
        name="attention_backward",
    )(segments, qkv, ctx_mine, ctx_other, do_mine, do_other, lse, segments)


MESH_ID = pl.DeviceIdType.MESH
WIDE = 5


def place_of():
    return tuple(lax.axis_index(name) for name in ("z", "x", "y", "core"))


def sizes_of():
    return lax.axis_size("z"), lax.axis_size("x")


def partner(**moved):
    z, x, y, core = place_of()
    return (moved.get("z", z), moved.get("x", x), moved.get("y", y), moved.get("core", core))


def greet(with_grid):
    z, x, y, core = place_of()
    size_z, size_x = sizes_of()
    peers = [partner(y=1 - y), partner(core=1 - core)]
    if with_grid:
        peers += [partner(z=lax.rem(z + k, size_z)) for k in range(1, size_z)]
        peers += [partner(x=lax.rem(x + j, size_x)) for j in range(1, size_x)]
    barrier = pltpu.get_barrier_semaphore()
    for peer in peers:
        pl.semaphore_signal(barrier, inc=1, device_id=peer, device_id_type=MESH_ID)
    pl.semaphore_wait(barrier, len(peers))


def remote(src, dst, send, recv, peer):
    return pltpu.make_async_remote_copy(
        src_ref=src, dst_ref=dst, send_sem=send, recv_sem=recv, device_id=peer, device_id_type=MESH_ID
    )


def entry_kernel(size_z, size_x, count, *refs):
    tokens, cotangent, wq, wk, wv, w_inner, w_output, w_outer = refs[:8]
    vectors = refs[8 : 8 + count]
    tokens_all, cotangent_send, weights_all, inner_all, outer_all, rows_out, inner_out = refs[8 + count : 15 + count]
    raw = refs[15 + count : 15 + 2 * count]
    stage, cot_stage, wbuf, ibuf, obuf, pack, ipack, opack, vpack, vectors_all = refs[15 + 2 * count : 25 + 2 * count]
    local_sem, load_sem, tsend, trecv, zsend, zrecv, xsend, xrecv, ysend, yrecv, osend, orecv = refs[25 + 2 * count :]
    z, x, y, core = place_of()
    half = pack.shape[1] // 3
    pairs = half // 128
    chunks = w_inner.shape[1] // CHUNK
    me = z * size_x + x
    columns = [lax.rem(x + j, size_x) for j in range(size_x)]

    mine = pl.ds(pl.multiple_of(core * half, 128), half)
    loads = [pltpu.make_async_copy(w.at[:, mine], wbuf.at[i], load_sem.at[i]) for i, w in enumerate((wq, wk, wv))]
    loads += [pltpu.make_async_copy(v, r, load_sem.at[3 + i]) for i, (v, r) in enumerate(zip(vectors, raw))]
    late = [
        pltpu.make_async_copy(
            w_inner.at[:, pl.ds(pl.multiple_of(c * CHUNK + core * half, 128), half)],
            ibuf.at[:, pl.ds(c * half, half)],
            load_sem.at[3 + count + c],
        )
        for c in range(chunks)
    ]
    late.append(pltpu.make_async_copy(w_output.at[:, mine], ibuf.at[:, pl.ds(chunks * half, half)], load_sem.at[3 + count + chunks]))
    late.append(pltpu.make_async_copy(w_outer.at[:, mine], obuf, load_sem.at[4 + count + chunks]))
    load = pltpu.make_async_copy(tokens.at[y], stage, local_sem.at[0])
    cot_load = pltpu.make_async_copy(cotangent.at[1 - y], cot_stage, local_sem.at[4])
    for copy in loads + late + [load, cot_load]:
        copy.start()
    vpack[...] = jnp.zeros_like(vpack)
    for copy in loads:
        copy.wait()
    for i, vector in enumerate(raw):
        size = vector.shape[0]
        vpack[i : i + 1, 0:size] = vector[...].reshape(1, size).astype(jnp.bfloat16).astype(jnp.float32)
    for i in range(3):
        for p in range(pairs):
            pack[:, (3 * p + i) * 128 : (3 * p + i + 1) * 128] = wbuf[i, :, p * 128 : (p + 1) * 128].astype(jnp.bfloat16)
    vectors_all[me] = vpack[...]
    greet(True)

    across = remote(tokens.at[1 - y], tokens_all.at[1], tsend.at[0], trecv.at[0], partner(y=1 - y))
    across.start()
    beside = remote(tokens.at[y], tokens_all.at[2], tsend.at[1], trecv.at[1], partner(core=1 - core))

    rows = ipack.shape[0]

    def share(owner):
        return pl.ds(pl.multiple_of(owner * (rows // 2), rows // 2), rows // 2)

    packs = (pack, vpack, ipack.at[share(y), :])

    def y_move(index, origin):
        slot = home(2, origin)
        return remote(slot, slot, ysend.at[index], yrecv.at[index], partner(y=1 - y))

    def home(stream, origin):
        if stream == 2:
            return inner_all.at[origin, share(y), :]
        return (weights_all, vectors_all)[stream].at[origin * size_x + x]

    def z_move(stream, way, t):
        step = 1 - 2 * way
        origin = z - step * (t - 1)
        src = packs[stream] if t == 1 else home(stream, origin)
        peer = partner(z=lax.rem(z + step + size_z, size_z))
        return remote(src, home(stream, origin), zsend.at[stream, way, t - 1], zrecv.at[stream, way, t - 1], peer)

    def sends(way, t):
        step = 1 - 2 * way
        origin, target = z - step * (t - 1), z + step
        inside = lambda v: jnp.logical_and(v >= 0, v < size_z)
        return jnp.logical_and(inside(origin), inside(target))

    def receives(way, t):
        origin = z - (1 - 2 * way) * t
        return jnp.logical_and(origin >= 0, origin < size_z)

    def x_moves(index, origin, own):
        moves = []
        for j in range(1, size_x):
            for stream in range(2):
                src = packs[stream] if own else home(stream, origin)
                moves.append(
                    remote(
                        src,
                        home(stream, origin),
                        xsend.at[stream, index, j - 1],
                        xrecv.at[stream, index, j - 1],
                        partner(x=columns[j]),
                    )
                )
        return moves

    def start_z(streams, t):
        for way in range(2):

            @pl.when(sends(way, t))
            def _():
                for stream in streams:
                    z_move(stream, way, t).start()

    for move in x_moves(0, z, True):
        move.start()
    start_z((0, 1), 1)
    beside.start()
    for copy in late:
        copy.wait()
    ipack[...] = ibuf[...].astype(jnp.bfloat16)
    opack[...] = obuf[...].astype(jnp.bfloat16)
    start_z((2,), 1)
    outer_moves = [
        remote(opack, outer_all.at[x], osend.at[j - 1], orecv.at[j - 1], partner(x=columns[j])) for j in range(1, size_x)
    ]
    keeps = [
        pltpu.make_async_copy(pack, weights_all.at[me], local_sem.at[1]),
        pltpu.make_async_copy(ipack, inner_all.at[z], local_sem.at[2]),
        pltpu.make_async_copy(opack, outer_all.at[x], local_sem.at[6]),
    ]
    load.wait()
    keeps.append(pltpu.make_async_copy(stage, tokens_all.at[0], local_sem.at[3]))
    cot_load.wait()
    keeps.append(pltpu.make_async_copy(cot_stage, cotangent_send, local_sem.at[5]))
    for keep in keeps:
        keep.start()

    def arrive(streams, t, sideways):
        for way in range(2):

            @pl.when(receives(way, t))
            def _():
                origin = z - (1 - 2 * way) * t
                for stream in streams:
                    slot = home(stream, origin)
                    remote(
                        slot, slot, zsend.at[stream, way, t - 1], zrecv.at[stream, way, t - 1], partner(core=1 - core)
                    ).wait_recv()
                if sideways:
                    for move in x_moves(1 + way * (size_z - 1) + t - 1, origin, False):
                        move.start()
                else:
                    y_move(way * (size_z - 1) + t - 1, origin).start()

    onward = remote(tokens_all.at[1], tokens_all.at[3], tsend.at[2], trecv.at[2], partner(core=1 - core))
    for t in range(1, size_z):
        arrive((0, 1), t, True)
        if t < size_z - 1:
            start_z((0, 1), t + 1)
        if t == 1:
            for move in outer_moves:
                move.start()
        arrive((2,), t, False)
        if t < size_z - 1:
            start_z((2,), t + 1)
        if t == min(2, size_z - 1):
            across.wait_recv()
            onward.start()

    for move in x_moves(0, z, True):
        move.wait()
    for t in range(1, size_z):
        for way in range(2):

            @pl.when(receives(way, t))
            def _():
                origin = z - (1 - 2 * way) * t
                for move in x_moves(1 + way * (size_z - 1) + t - 1, origin, False):
                    move.wait()
                y_move(way * (size_z - 1) + t - 1, origin).wait()

            @pl.when(sends(way, t))
            def _():
                for stream in range(3):
                    z_move(stream, way, t).wait_send()

    short = min(vector.shape[0] for vector in raw)
    longest = vpack.shape[1]
    for s in range(size_z * size_x):
        rows_out[:, s * short : (s + 1) * short] = vectors_all[s, :, 0:short]
        inner_out[:, s * longest : (s + 1) * longest] = vectors_all[s, WIDE : WIDE + 1, :]
    for move in outer_moves:
        move.wait()
    across.wait_send()
    beside.wait()
    onward.wait()
    for keep in keeps:
        keep.wait()


def entry(size_z, size_x, tokens, cotangent, wq, wk, wv, w_inner, w_output, w_outer, vectors):
    _, part, width = tokens.shape
    rows = wq.shape[0]
    half = width // 2
    lanes = 3 * half
    hidden = w_inner.shape[1]
    long = w_outer.shape[0]
    mixed_lanes = hidden // 2 + half
    chunks = hidden // CHUNK
    longest = max(v.shape[0] for v in vectors)
    shards = size_z * size_x
    count = len(vectors)
    anywhere, vmem = pl.BlockSpec(memory_space=pl.ANY), pl.BlockSpec(memory_space=pltpu.VMEM)
    dma = pltpu.SemaphoreType.DMA
    low, high = jnp.bfloat16, jnp.float32
    side = size_x - 1
    return pl.pallas_call(
        lambda *refs: entry_kernel(size_z, size_x, count, *refs),
        out_shape=(
            jax.ShapeDtypeStruct((4, part, width), low),
            jax.ShapeDtypeStruct((part, width), low),
            jax.ShapeDtypeStruct((shards, rows, lanes), low),
            jax.ShapeDtypeStruct((size_z, rows, mixed_lanes), low),
            jax.ShapeDtypeStruct((size_x, long, half), low),
            jax.ShapeDtypeStruct((16, width), high),
            jax.ShapeDtypeStruct((1, shards * longest), high),
        ),
        in_specs=[anywhere] * (8 + count),
        out_specs=(anywhere,) * 5 + (vmem,) * 2,
        scratch_shapes=[pltpu.VMEM(v.shape, v.dtype) for v in vectors]
        + [
            pltpu.VMEM((part, width), low),
            pltpu.VMEM((part, width), low),
            pltpu.VMEM((3, rows, half), high),
            pltpu.VMEM((rows, mixed_lanes), high),
            pltpu.VMEM((long, half), high),
            pltpu.VMEM((rows, lanes), low),
            pltpu.VMEM((rows, mixed_lanes), low),
            pltpu.VMEM((long, half), low),
            pltpu.VMEM((16, longest), high),
            pltpu.VMEM((shards, 16, longest), high),
            dma((7,)),
            dma((5 + count + chunks,)),
            dma((4,)),
            dma((4,)),
            dma((3, 2, size_z - 1)),
            dma((3, 2, size_z - 1)),
            dma((2, 2 * size_z - 1, side)),
            dma((2, 2 * size_z - 1, side)),
            dma((2 * size_z - 2,)),
            dma((2 * size_z - 2,)),
            dma((side,)),
            dma((side,)),
        ],
        compiler_params=pltpu.CompilerParams(collective_id=0, has_side_effects=True, vmem_limit_bytes=66_000_000),
        name="entry",
    )(tokens, cotangent, wq, wk, wv, w_inner, w_output, w_outer, *vectors)


def exit_kernel(size_z, size_x, shapes, *refs):
    z, x, y, core = place_of()
    grads_hbm, inputs_hbm, weights_hbm, base_hbm, output_term, dense_sums, inner_sums, head_sums = refs[:8]
    inner_in = refs[8 : 8 + size_z]
    outer_in = refs[8 + size_z : 8 + size_z + size_x]
    refs = refs[8 + size_z + size_x :]
    made = refs[:8]
    token_grads, grad_query, grad_key, grad_value, grad_output, grad_inner, grad_outer, vector_sums = made
    grads, inputs, turned, weights, base, terms_a, terms_b, other_rows, recv_rows, send_rows, far_rows, odd = refs[8:20]
    inner_buf, outer_buf, vector_rows, vector_terms, inner_send = refs[20:25]
    load_sem, tsend, trecv, osend, orecv = refs[25:30]
    refs = list(refs[30:])
    terms = {"qa": terms_a, "qb": terms_b}
    xin, xsend, xrecv = {}, {}, {}
    zout, zin, zsend, zrecv = {}, {}, {}, {}
    ybuf, ysend, yrecv, cbuf, csend, crecv = {}, {}, {}, {}, {}, {}
    for name in shapes:
        ybuf[name], ysend[name], yrecv[name], cbuf[name], csend[name], crecv[name] = [refs.pop(0) for _ in range(6)]
        if name != "outer":
            xin[name], xsend[name], xrecv[name] = [refs.pop(0) for _ in range(3)]
        if name != "inner":
            zout[name], zin[name], zsend[name], zrecv[name] = [refs.pop(0) for _ in range(4)]

    shards, rows, half = odd.shape
    lanes = 3 * half
    pairs = half // 128
    hidden = grad_inner.shape[1]
    part = token_grads.shape[1]
    local = 2 * part
    low, high = jnp.bfloat16, jnp.float32
    mine = pl.ds(pl.multiple_of(core * half, 128), half)
    theirs = pl.ds(pl.multiple_of((1 - core) * half, 128), half)
    columns = [lax.rem(x + j, size_x) for j in range(size_x)]
    steps = [(t, way) for t in range(1, size_z) for way in range(2)]
    core_peer, y_peer = partner(core=1 - core), partner(y=1 - y)

    loads = {}
    for i, src in enumerate(inner_in):
        loads["inner", i] = pltpu.make_async_copy(src, inner_buf.at[i], load_sem.at[i])
    for i, src in enumerate(outer_in):
        loads["outer", i] = pltpu.make_async_copy(src, outer_buf.at[i], load_sem.at[size_z + i])
    for i, (name, src, dst) in enumerate(
        (("inputs", inputs_hbm, inputs), ("grads", grads_hbm, grads), ("weights", weights_hbm, weights), ("base", base_hbm, base))
    ):
        loads[name] = pltpu.make_async_copy(src, dst, load_sem.at[size_z + size_x + i])
    for load in loads.values():
        load.start()

    def inside(v):
        return jnp.logical_and(v >= 0, v < size_z)

    def target_of(t, way):
        return z + (1 - 2 * way) * (size_z - t)

    def fed(way):
        return inside(z - (1 - 2 * way))

    def x_move(name, n, at, j, src, dst):
        return remote(src, dst, xsend[name].at[n, at, j - 1], xrecv[name].at[n, at, j - 1], partner(x=columns[j]))

    def x_pieces(name, at):
        source = vector_terms if name == "vec" else terms[name]
        return [
            x_move(name, 0, at, j, source.at[at * size_x + columns[j]], xin[name].at[j - 1, at]) for j in range(1, size_x)
        ]

    def send_x(name):
        for t, way in steps:

            @pl.when(inside(target_of(t, way)))
            def _():
                for move in x_pieces(name, target_of(t, way)):
                    move.start()

        for move in x_pieces(name, z):
            move.start()

    def own_part(name, at):
        if name == "outer":
            total = outer_buf[0, at].astype(high)
            for i in range(1, size_x):
                total = total + outer_buf[i, at].astype(high)
            return [(slice(None), total)]
        slot = at * size_x + x
        if name == "vec":
            total = vector_terms[slot]
            for move in x_pieces("vec", at):
                move.wait()
            for j in range(1, size_x):
                total = total + xin["vec"][j - 1, at]
            return [(slice(None), total)]
        for move in x_pieces(name, at):
            move.wait()
        total = terms[name][slot].astype(high)
        for j in range(1, size_x):
            total = total + xin[name][j - 1, at].astype(high)
        return [(slice(None), total)]

    def z_move(name, t, way):
        peer = partner(z=lax.rem(z + 1 - 2 * way + size_z, size_z))
        return remote(
            zout[name].at[way, t - 1], zin[name].at[way, t - 1], zsend[name].at[way, t - 1], zrecv[name].at[way, t - 1], peer
        )

    def step_z(name, t):
        for way in range(2):

            @pl.when(inside(target_of(t, way)))
            def _():
                pieces = own_part(name, target_of(t, way))
                if t > 1:

                    @pl.when(fed(way))
                    def _():
                        z_move(name, t - 1, way).wait_recv()

                for span, total in pieces:
                    if t > 1:
                        before = zin[name][way, t - 2, :, span].astype(high)
                        total = total + jnp.where(fed(way), before, 0.0)
                    zout[name][way, t - 1, :, span] = total.astype(zout[name].dtype)
                z_move(name, t, way).start()

    across, swapped = {}, {}

    def step_y(name):
        across[name] = remote(ybuf[name].at[0], ybuf[name].at[1], ysend[name], yrecv[name], y_peer)
        across[name].start()

    def finish_z(name):
        pieces = own_part(name, z)
        last = size_z - 1
        for way in range(2):

            @pl.when(fed(way))
            def _():
                z_move(name, last, way).wait_recv()

        for span, total in pieces:
            for way in range(2):
                before = zin[name][way, last - 1, :, span].astype(high)
                total = total + jnp.where(fed(way), before, 0.0)
            ybuf[name][0, :, span] = total.astype(ybuf[name].dtype)
        step_y(name)

    def step_core(name):
        across[name].wait()
        cbuf[name][0] = ybuf[name][0].astype(high) + ybuf[name][1].astype(high)
        swapped[name] = remote(cbuf[name].at[0], cbuf[name].at[1], csend[name], crecv[name], core_peer)
        swapped[name].start()

    def finish_core(name):
        swapped[name].wait()
        return cbuf[name]

    vector_rows[...] = jnp.zeros_like(vector_rows)
    for i, row in enumerate((7, 8, 6, 3, 4, 2)):
        vector_rows[row : row + 1, :] = jnp.sum(dense_sums[8 * i : 8 * i + 8, :], axis=0, keepdims=True)
    for p in range(pairs):
        place = pl.ds(pl.multiple_of(core * half + p * 128, 128), 128)
        vector_rows[0:1, place] = head_sums[8 * p : 8 * p + 1, 0:128]
        vector_rows[1:2, place] = head_sums[8 * p : 8 * p + 1, 256:384]
    inner_row = jnp.sum(inner_sums[...], axis=0, keepdims=True)
    vector_terms[...] = jnp.zeros_like(vector_terms)
    for name in zin:
        if name == "vec":
            zin[name][...] = jnp.zeros_like(zin[name])
    longest = vector_terms.shape[2]
    for s in range(shards):
        vector_terms[s, :, 0:rows] = vector_rows[:, s * rows : (s + 1) * rows]
        vector_terms[s, WIDE : WIDE + 1, :] = inner_row[:, s * longest : (s + 1) * longest]
    greet(True)

    outputs = remote(output_term.at[:, :, theirs], odd, osend, orecv, core_peer)
    outputs.start()
    send_x("vec")
    for i in range(size_z):
        loads["inner", i].wait()
    inner_moves = []
    for j in range(1, size_x):
        total = inner_buf[0, columns[j]].astype(high)
        for i in range(1, size_z):
            total = total + inner_buf[i, columns[j]].astype(high)
        inner_send[j - 1] = total.astype(low)
        move = x_move("inner", 0, 0, j, inner_send.at[j - 1], xin["inner"].at[j - 1, 0])
        move.start()
        inner_moves.append(move)
    for i in range(size_x):
        loads["outer", i].wait()
    step_z("outer", 1)

    strip = 256

    def product(first):
        at = pl.ds(pl.multiple_of(first, strip), strip)
        return dot_nt(grads[at, :], weights[...])

    def token_rows(first):
        def other_strip(i, _):
            at = pl.ds(pl.multiple_of(first + i * strip, strip), strip)
            other_rows[at, :] = product(local + first + i * strip).astype(low)
            return 0

        def own_strip(i, _):
            at = pl.ds(pl.multiple_of(first + i * strip, strip), strip)
            base[at, :] = base[at, :] + product(first + i * strip)
            return 0

        lax.fori_loop(0, part // strip, other_strip, 0)
        span = pl.ds(first, part)
        move = remote(other_rows.at[span, :], recv_rows.at[span, :], tsend.at[first // part], trecv.at[first // part], core_peer)
        move.start()
        lax.fori_loop(0, part // strip, own_strip, 0)
        return move

    loads["inputs"].wait()
    for b in range(4):
        turned[:, b * part : (b + 1) * part] = inputs[b * part : (b + 1) * part, :].T
    group = 4
    loads["grads"].wait()
    for p in range(pairs):
        block = slice(p * 384, (p + 1) * 384)
        where = slice(p % 2 * 384, p % 2 * 384 + 384)
        goal = terms_a if p < 2 else terms_b

        def some(m, _):
            value = dot_nn(turned[pl.ds(pl.multiple_of(m * group * rows, group * rows), group * rows), :], grads[:, block])
            goal[pl.ds(m * group, group), :, where] = value.reshape(group, rows, 384).astype(low)
            return 0

        lax.fori_loop(0, shards // group, some, 0)
        if p == 1:
            send_x("qa")
    outputs.wait()
    terms_b[:, :, half : 2 * half] = (odd[...].astype(high) + output_term[:, :, mine].astype(high)).astype(low)
    send_x("qb")
    for name in ("weights", "base"):
        loads[name].wait()
    halves = token_rows(part)
    halves.wait()
    send_rows[...] = (base[part:local, :] + recv_rows[part:local, :].astype(high)).astype(low)
    back = remote(send_rows, far_rows, tsend.at[2], trecv.at[2], y_peer)
    back.start()

    step_z("outer", 2)
    total = inner_buf[0, x].astype(high)
    for i in range(1, size_z):
        total = total + inner_buf[i, x].astype(high)
    for j in range(1, size_x):
        inner_moves[j - 1].wait()
        total = total + xin["inner"][j - 1, 0].astype(high)
    ybuf["inner"][0] = total.astype(low)
    step_y("inner")
    for t in range(3, size_z):
        step_z("outer", t)
    step_z("vec", 1)
    step_z("qa", 1)
    halves = token_rows(0)
    step_z("vec", 2)
    step_z("qa", 2)
    finish_z("outer")
    for t in range(3, size_z):
        step_z("vec", t)
        step_z("qa", t)
    step_z("qb", 1)
    halves.wait()
    token_grads[y] = base[0:part, :] + recv_rows[0:part, :].astype(high)
    step_core("inner")
    step_z("qb", 2)
    finish_z("qa")
    finish_z("vec")
    for t in range(3, size_z):
        step_z("qb", t)
    step_core("outer")
    back.wait()
    token_grads[1 - y] = far_rows[...].astype(high)
    chunks = hidden // CHUNK
    buf = finish_core("inner")
    for i in range(2):
        owner = core if i == 0 else 1 - core
        for c in range(chunks):
            place = pl.ds(pl.multiple_of(c * CHUNK + owner * half, 128), half)
            grad_inner[:, place] = buf[i, :, c * half : (c + 1) * half]
    buf = finish_core("outer")
    for i in range(2):
        owner = core if i == 0 else 1 - core
        grad_outer[:, pl.ds(pl.multiple_of(owner * half, 128), half)] = buf[i]
    finish_z("qb")
    step_core("vec")
    step_core("qa")

    def spread(name):
        buf = finish_core(name)
        for i in range(2):
            owner = core if i == 0 else 1 - core
            for p in (0, 1) if name == "qa" else (2,):
                place = pl.ds(pl.multiple_of(owner * half + p * 128, 128), 128)
                for n, out in enumerate((grad_query, grad_key, grad_value)):
                    at = (3 * (p % 2) + n) * 128
                    out[:, place] = buf[i, :, at : at + 128]
            if name == "qb":
                grad_output[:, pl.ds(pl.multiple_of(owner * half, 128), half)] = buf[i, :, half : 2 * half]

    for name in zout:
        for t, way in steps:

            @pl.when(inside(target_of(t, way)))
            def _():
                z_move(name, t, way).wait_send()

    buf = finish_core("vec")
    vector_sums[...] = buf[0] + buf[1]
    spread("qa")
    step_core("qb")
    spread("qb")


def deliver_kernel(count, mixed_mine, mixed_far, *refs):
    matrices, vectors, mixed = refs[:count], refs[count], refs[count + 1]
    outs = refs[count + 2 : 2 * count + 2]
    smalls = refs[2 * count + 2 : -4]
    stage, in_sem, out_sem = refs[-4:-2], refs[-2], refs[-1]
    y = lax.axis_index("y")
    loads = [pltpu.make_async_copy(src, stage[i], in_sem.at[i]) for i, src in enumerate((mixed_mine, mixed_far))]
    copies = [pltpu.make_async_copy(src, dst, out_sem.at[i]) for i, (src, dst) in enumerate(zip(matrices, outs))]
    for copy in loads + copies:
        copy.start()
    for i, small in enumerate(smalls):
        small[...] = vectors[i : i + 1, 0 : small.shape[0]].reshape(small.shape)
    for i, place in enumerate((y, 1 - y)):
        loads[i].wait()
        copies.append(pltpu.make_async_copy(stage[i], mixed.at[place], out_sem.at[count + i]))
        copies[-1].start()
    for copy in copies:
        copy.wait()


def deliver(mixed_mine, mixed_far, matrices, vectors, sizes):
    count = len(matrices)
    vmem, anywhere = pl.BlockSpec(memory_space=pltpu.VMEM), pl.BlockSpec(memory_space=pl.ANY)
    return pl.pallas_call(
        lambda *refs: deliver_kernel(count, *refs),
        out_shape=(jax.ShapeDtypeStruct((2,) + mixed_mine.shape, mixed_mine.dtype),)
        + tuple(jax.ShapeDtypeStruct(m.shape, m.dtype) for m in matrices)
        + tuple(jax.ShapeDtypeStruct((size,), jnp.float32) for size in sizes),
        in_specs=[anywhere] * 2 + [vmem] * (count + 1),
        out_specs=(anywhere,) * (count + 1) + (vmem,) * len(sizes),
        scratch_shapes=[pltpu.VMEM(mixed_mine.shape, mixed_mine.dtype)] * 2
        + [pltpu.SemaphoreType.DMA((2,)), pltpu.SemaphoreType.DMA((count + 2,))],
        compiler_params=pltpu.CompilerParams(vmem_limit_bytes=40_000_000),
        name="deliver",
    )(mixed_mine, mixed_far, *matrices, vectors)


def exit_call(size_z, size_x, grads, inputs, weights, base, output_term, dense_sums, inner_sums, head_sums, inner_terms, outer_terms):
    shards, rows, width = output_term.shape
    lanes = grads.shape[1]
    half = width // 2
    pairs = half // 128
    length = inputs.shape[0]
    local = length // 2
    part = local // 2
    long = outer_terms[0].shape[1]
    hidden = 2 * inner_terms[0].shape[2]
    vmem, anywhere = pl.BlockSpec(memory_space=pltpu.VMEM), pl.BlockSpec(memory_space=pl.ANY)
    dma = pltpu.SemaphoreType.DMA
    side = size_x - 1
    full = lanes + half
    low, high = jnp.bfloat16, jnp.float32
    vector_shape = (16, hidden // shards)
    shapes = {
        "vec": (vector_shape, high, 1),
        "qa": ((rows, width), low, 1),
        "qb": ((rows, width), low, 1),
        "inner": ((rows, hidden // 2), low, 1),
        "outer": ((long, half), low, 1),
    }
    matrix = jax.ShapeDtypeStruct((rows, width), high)
    results = (
        jax.ShapeDtypeStruct((2, part, width), high),
        matrix,
        matrix,
        matrix,
        matrix,
        jax.ShapeDtypeStruct((rows, hidden), high),
        jax.ShapeDtypeStruct((long, width), high),
        jax.ShapeDtypeStruct(vector_shape, high),
    )
    scratch = [
        pltpu.VMEM((length, lanes), low),
        pltpu.VMEM((length, width), low),
        pltpu.VMEM((width, length), low),
        pltpu.VMEM((width, lanes), low),
        pltpu.VMEM((local, width), high),
        pltpu.VMEM((shards, rows, width), low),
        pltpu.VMEM((shards, rows, width), low),
        pltpu.VMEM((local, width), low),
        pltpu.VMEM((local, width), low),
        pltpu.VMEM((part, width), low),
        pltpu.VMEM((part, width), low),
        pltpu.VMEM((shards, rows, half), low),
        pltpu.VMEM((size_z,) + inner_terms[0].shape, low),
        pltpu.VMEM((size_x,) + outer_terms[0].shape, low),
        pltpu.VMEM((16, width), high),
        pltpu.VMEM((shards,) + vector_shape, high),
        pltpu.VMEM((side, rows, hidden // 2), low),
        dma((size_z + size_x + 4,)),
        dma((3,)),
        dma((3,)),
        dma,
        dma,
    ]
    for name, (shape, kind, sends) in shapes.items():
        scratch += [pltpu.VMEM((2,) + shape, kind), dma, dma, pltpu.VMEM((2,) + shape, high), dma, dma]
        stages = 1 if name == "inner" else size_z
        if name != "outer":
            scratch += [pltpu.VMEM((side, stages) + shape, kind), dma((sends, stages, side)), dma((sends, stages, side))]
        if name != "inner":
            scratch += [pltpu.VMEM((2, size_z - 1) + shape, kind)] * 2 + [dma((2, size_z - 1))] * 2
    return pl.pallas_call(
        lambda *refs: exit_kernel(size_z, size_x, shapes, *refs),
        out_shape=tuple(pltpu.VMEM(r.shape, r.dtype) for r in results),
        in_specs=[anywhere] * 4 + [vmem] * 4 + [anywhere] * (size_z + size_x),
        out_specs=(vmem,) * len(results),
        scratch_shapes=scratch,
        compiler_params=pltpu.CompilerParams(collective_id=1, has_side_effects=True, vmem_limit_bytes=56_000_000),
        name="exit",
    )(grads, inputs, weights, base, output_term, dense_sums, inner_sums, head_sums, *inner_terms, *outer_terms)


TILE = 256
CHUNK = 768


def dot_nt(a, b):
    return lax.dot_general(a, b, (((1,), (1,)), ((), ())), preferred_element_type=jnp.float32)


def row_mean(value):
    return jnp.sum(value, axis=-1, keepdims=True) * (1.0 / value.shape[-1])


def standardize(hidden):
    centred = hidden - row_mean(hidden)
    reciprocal = lax.rsqrt(row_mean(centred * centred) + EPS)
    return centred * reciprocal, reciprocal


def column_sum(value):
    return jnp.sum(value.reshape(value.shape[0] // 8, 8, value.shape[1]), axis=0)


def dense_kernel(
    size_z,
    size_x,
    tokens_ref,
    mine_ref,
    other_hbm,
    cot_hbm,
    cot_far_hbm,
    vectors_ref,
    bias_inner_ref,
    *refs,
):
    inner_parts, outer_parts = refs[:size_x], refs[size_x : size_x + size_z]
    refs = refs[size_x + size_z :]
    mixed_ref, mixed_send_ref, pre_first_ref, grad_mine_ref, grad_far_hbm, sums_ref, inner_sum_ref, grad_output_ref = refs[:8]
    inner_terms = refs[8 : 8 + size_z]
    outer_terms = refs[8 + size_z : 8 + size_z + size_x]
    refs = refs[8 + size_z + size_x :]
    w_output, w_inner, w_outer, a_output, a_inner, a_outer, grad_out_buf = refs[:7]
    context, first_low, turned_low, normed, first, slope, active, work = refs[7:15]
    send_inner, send_outer, recv_inner, recv_outer = refs[15:19]
    far_rows, grad_send, ready, cotangent, cot_sem, swap_send, swap_recv = refs[19:26]
    load_sem, share_send, share_recv, send_sem, recv_sem, store_sem = refs[26:]
    step, steps = pl.program_id(0), pl.num_programs(0)
    core_here = lax.axis_index("core")
    width, hidden = w_inner.shape
    half = width // 2
    chunks = hidden // CHUNK
    shards = size_z * size_x
    z, x, y, _ = place_of()
    twin = partner(core=1 - lax.axis_index("core"))
    near = cotangent.shape[0] // 2
    cot_loads = (
        pltpu.make_async_copy(cot_hbm.at[y], cotangent.at[pl.ds(0, near), :], cot_sem.at[0]),
        pltpu.make_async_copy(cot_far_hbm, cotangent.at[pl.ds(near, near), :], cot_sem.at[1]),
    )

    shard = width // shards
    long = hidden // shards
    group = CHUNK // long // size_x

    def columns_of(first, owner):
        return pl.ds(pl.multiple_of(first + owner * half, 128), half)

    def start_piece(i, src, dst):
        pltpu.make_async_copy(src, dst, load_sem.at[i]).start()
        remote(src, dst, share_send.at[i], share_recv.at[i], twin).start()

    def start_rows(i, lane, ref, first):
        for j in range(size_x):
            for at in range(size_z):
                slot = at * size_x + lax.rem(x - j + size_x, size_x)
                rows = pl.ds(pl.multiple_of(slot * shard, shard), shard)
                start_piece(i, inner_parts[j].at[at, :, pl.ds(lane, half)], ref.at[rows, columns_of(first, core_here)])

    def start_loads():
        start_rows(0, hidden // 2, w_output, 0)
        for c in range(chunks):
            start_rows(1 + 2 * c, c * half, w_inner, c * CHUNK)
            for at in range(c * group, (c + 1) * group):
                for k in range(size_z):

                    @pl.when(lax.rem(z - k + size_z, size_z) == at)
                    def _():
                        for column in range(size_x):
                            rows = pl.ds((at * size_x + column) * long, long)
                            start_piece(2 + 2 * c, outer_parts[k].at[column], w_outer.at[rows, columns_of(0, core_here)])

    def wait_load(i, ref, rows, first):
        own, far = ref.at[rows, columns_of(first, core_here)], ref.at[rows, columns_of(first, 1 - core_here)]
        pltpu.make_async_copy(own, own, load_sem.at[i]).wait()
        remote(own, far, share_send.at[i], share_recv.at[i], twin).wait()

    @pl.when(step == 0)
    def _():
        barrier = pltpu.get_barrier_semaphore()
        pl.semaphore_signal(barrier, inc=1, device_id=twin, device_id_type=MESH_ID)
        pl.semaphore_wait(barrier, 1)
        remote(other_hbm, far_rows, swap_send.at[0], swap_recv.at[0], twin).start()
        start_loads()
        for load in cot_loads:
            load.start()
        a_output[...] = jnp.zeros_like(a_output)
        a_inner[...] = jnp.zeros_like(a_inner)
        a_outer[...] = jnp.zeros_like(a_outer)
        sums_ref[...] = jnp.zeros_like(sums_ref)
        inner_sum_ref[...] = jnp.zeros_like(inner_sum_ref)

    def vector(i):
        row = (2, 3, 4, 6, 7, 8)[i]
        return vectors_ref[row : row + 1, :]

    def add_sum(i, value):
        sums_ref[8 * i : 8 * i + 8, :] += column_sum(value)

    context[:, pl.ds(pl.multiple_of(core_here * half, 128), half)] = mine_ref[...]

    context_move = remote(other_hbm, far_rows, swap_send.at[0], swap_recv.at[0], twin)

    @pl.when(step == 0)
    def _():
        context_move.wait()

    here = pl.ds(pl.multiple_of(step * TILE, TILE), TILE)
    context[:, pl.ds(pl.multiple_of((1 - core_here) * half, 128), half)] = far_rows[here, :]

    @pl.when(step == 0)
    def _():
        wait_load(0, w_output, slice(None), 0)

    hidden_rows = tokens_ref[...].astype(jnp.float32) + (dot_nn(context[...], w_output[...]) + vector(0))
    normed[...], first_recip = standardize(hidden_rows)
    first[...] = normed[...] * vector(1) + vector(2)
    first_low[...] = first[...].astype(jnp.bfloat16)
    turned_low[...] = first_low[...].T
    work[...] = jnp.broadcast_to(vector(3), work.shape)

    def part(c):
        return pl.ds(c * CHUNK, CHUNK)

    def exchange(c):
        return (
            remote(send_inner.at[c], recv_inner.at[c], send_sem.at[0, c], recv_sem.at[0, c], twin),
            remote(send_outer.at[c], recv_outer.at[c], send_sem.at[1, c], recv_sem.at[1, c], twin),
        )

    def wait_inner(c):
        @pl.when(step == 0)
        def _():
            wait_load(1 + 2 * c, w_inner, slice(None), c * CHUNK)

    def ahead(c):
        ready[c % 2] = dot_nn(first_low[...], w_inner[:, part(c)])

    wait_inner(0)
    ahead(0)
    for c in range(chunks):
        if c + 1 < chunks:
            wait_inner(c + 1)

        @pl.when(step == 0)
        def _():
            wait_load(2 + 2 * c, w_outer, part(c), 0)

        if c + 1 < chunks:
            ahead(c + 1)
        u = ready[c % 2] + bias_inner_ref[0:1, part(c)]
        cdf = 0.5 * (1.0 + lax.erf(u * ROOT_HALF))
        slope[:, part(c)] = cdf + u * jnp.exp(-0.5 * u * u) * INV_ROOT_TAU
        acted = (u * cdf).astype(jnp.bfloat16)
        active[:, part(c)] = acted
        work[...] += dot_nn(acted, w_outer[part(c), :])

    second, second_recip = standardize(first[...] + work[...])
    mixed = (second * vector(4) + vector(5)).astype(jnp.bfloat16)

    @pl.when(step < steps // 2)
    def _():
        mixed_ref[...] = mixed

    @pl.when(step >= steps // 2)
    def _():
        mixed_send_ref[...] = mixed


    @pl.when(step == 0)
    def _():
        for load in cot_loads:
            load.wait()

    upstream = cotangent[pl.ds(pl.multiple_of(step * TILE, TILE), TILE), :].astype(jnp.float32)
    add_sum(0, upstream * second)
    add_sum(1, upstream)
    scaled = upstream * vector(4)
    pre_second = second_recip * (scaled - row_mean(scaled) - second * row_mean(scaled * second))
    grad_outer = pre_second.astype(jnp.bfloat16)
    add_sum(2, grad_outer.astype(jnp.float32))
    work[...] = pre_second
    grad_out_buf[...] = grad_outer

    def behind(c):
        ready[c % 2] = dot_nt(grad_out_buf[...], w_outer[part(c), :])

    behind(0)
    for c in range(chunks):
        if c + 1 < chunks:
            behind(c + 1)
        grad_inner = (ready[c % 2] * slope[:, part(c)]).astype(jnp.bfloat16)
        inner_sum_ref[:, part(c)] += column_sum(grad_inner.astype(jnp.float32))
        a_outer[part(c), :] += dot_nn(active[:, part(c)].T, grad_out_buf[...])
        a_inner[:, part(c)] += dot_nn(turned_low[...], grad_inner)
        work[...] += dot_nt(grad_inner, w_inner[:, part(c)])

        @pl.when(step == steps - 1)
        def _():
            theirs = pl.multiple_of(c * CHUNK + (1 - core_here) * half, 128)
            send_inner[c] = a_inner[:, pl.ds(theirs, half)].astype(jnp.bfloat16)
            send_outer[c] = a_outer[part(c), pl.ds(pl.multiple_of((1 - core_here) * half, 128), half)].astype(jnp.bfloat16)
            for move in exchange(c):
                move.start()

    grad_first = work[...]
    add_sum(3, grad_first * normed[...])
    add_sum(4, grad_first)
    scaled = grad_first * vector(1)
    pre_first = first_recip * (scaled - row_mean(scaled) - normed[...] * row_mean(scaled * normed[...]))
    pre_first_ref[...] = pre_first
    grad_attended = pre_first.astype(jnp.bfloat16)
    add_sum(5, grad_attended.astype(jnp.float32))
    a_output[...] += dot_nn(context[...].T, grad_attended)
    context[...] = dot_nt(grad_attended, w_output[...]).astype(jnp.bfloat16)
    grad_mine_ref[...] = context[:, pl.ds(pl.multiple_of(core_here * half, 128), half)]

    def grad_move(t):
        rows = pl.ds(pl.multiple_of(t * TILE, TILE), TILE)
        return remote(grad_send.at[t], grad_far_hbm.at[rows, :], swap_send.at[1 + t], swap_recv.at[1 + t], twin)

    grad_send[step] = context[:, pl.ds(pl.multiple_of((1 - core_here) * half, 128), half)]
    grad_move(step).start()

    @pl.when(step == steps - 1)
    def _():
        grad_output_ref[...] = a_output[...].astype(jnp.bfloat16)

        def inner_out(c):
            copies = []
            for k in range(size_z):
                for column in range(size_x):
                    slot = lax.rem(z + k, size_z) * size_x + column
                    src = send_inner.at[c, pl.ds(pl.multiple_of(slot * shard, shard), shard), :]
                    copies.append(
                        pltpu.make_async_copy(src, inner_terms[k].at[column, :, pl.ds(c * half, half)], store_sem.at[0, c])
                    )
            return copies

        def outer_out(c):
            copies = []
            for i in range(group):
                for j in range(size_x):
                    src = send_outer.at[c, pl.ds(pl.multiple_of((i * size_x + lax.rem(x + j, size_x)) * long, long), long), :]
                    copies.append(pltpu.make_async_copy(src, outer_terms[j].at[c * group + i], store_sem.at[1, c]))
            return copies

        for c in range(chunks):
            ours = pl.multiple_of(c * CHUNK + core_here * half, 128)
            first_move, second_move = exchange(c)
            first_move.wait()
            send_inner[c] = (a_inner[:, pl.ds(ours, half)] + recv_inner[c].astype(jnp.float32)).astype(jnp.bfloat16)
            for copy in inner_out(c):
                copy.start()
            second_move.wait()
            columns = pl.ds(pl.multiple_of(core_here * half, 128), half)
            send_outer[c] = (a_outer[part(c), columns] + recv_outer[c].astype(jnp.float32)).astype(jnp.bfloat16)
            for copy in outer_out(c):
                copy.start()
        for t in range(grad_send.shape[0]):
            grad_move(t).wait()
        for c in range(chunks):
            pltpu.make_async_copy(send_inner.at[c], send_inner.at[c], store_sem.at[0, c]).wait()
            pltpu.make_async_copy(send_outer.at[c], send_outer.at[c], store_sem.at[1, c]).wait()


def dense_layer(size_z, size_x, tokens, mine, other, cotangent, cotangent_far, vectors, bias_inner, inner_parts, outer_parts):
    local, half = mine.shape
    width = 2 * half
    hidden = bias_inner.shape[1]
    steps = local // TILE
    shards = size_z * size_x
    chunks = hidden // CHUNK
    low, high = jnp.bfloat16, jnp.float32
    tile = pl.BlockSpec((TILE, width), lambda t, *_: (t, 0))
    half_tile = pl.BlockSpec((TILE, half), lambda t, *_: (t, 0))
    anywhere = pl.BlockSpec(memory_space=pl.ANY)

    def whole(shape):
        return pl.BlockSpec(shape, lambda t, *_: (0, 0))

    inner_shape = jax.ShapeDtypeStruct((size_x, width // shards, hidden // 2), low)
    outer_shape = jax.ShapeDtypeStruct((size_z, hidden // shards, half), low)
    halves = pltpu.VMEM((chunks, width, half), low)
    dma = pltpu.SemaphoreType.DMA
    return pl.pallas_call(
        lambda *refs: dense_kernel(size_z, size_x, *refs),
        out_shape=(
            jax.ShapeDtypeStruct((local // 2, width), low),
            jax.ShapeDtypeStruct((local // 2, width), low),
            jax.ShapeDtypeStruct((local, width), high),
            jax.ShapeDtypeStruct((local, half), low),
            jax.ShapeDtypeStruct((local, half), low),
            jax.ShapeDtypeStruct((48, width), high),
            jax.ShapeDtypeStruct((8, hidden), high),
            jax.ShapeDtypeStruct((width, width), low),
        )
        + (inner_shape,) * size_z
        + (outer_shape,) * size_x,
        grid_spec=pltpu.PrefetchScalarGridSpec(
            num_scalar_prefetch=0,
            grid=(steps,),
            in_specs=[
                tile,
                half_tile,
                anywhere,
                anywhere,
                anywhere,
                whole((16, width)),
                whole((1, hidden)),
            ]
            + [anywhere] * (size_x + size_z),
            out_specs=[
                pl.BlockSpec((TILE, width), lambda t: (jnp.minimum(t, steps // 2 - 1), 0)),
                pl.BlockSpec((TILE, width), lambda t: (jnp.maximum(t - steps // 2, 0), 0)),
                tile,
                half_tile,
                anywhere,
                whole((48, width)),
                whole((8, hidden)),
                whole((width, width)),
            ]
            + [anywhere] * (size_z + size_x),
            scratch_shapes=[
                pltpu.VMEM((width, width), low),
                pltpu.VMEM((width, hidden), low),
                pltpu.VMEM((hidden, width), low),
                pltpu.VMEM((width, width), high),
                pltpu.VMEM((width, hidden), high),
                pltpu.VMEM((hidden, width), high),
                pltpu.VMEM((TILE, width), low),
                pltpu.VMEM((TILE, width), low),
                pltpu.VMEM((TILE, width), low),
                pltpu.VMEM((width, TILE), low),
                pltpu.VMEM((TILE, width), high),
                pltpu.VMEM((TILE, width), high),
                pltpu.VMEM((TILE, hidden), high),
                pltpu.VMEM((TILE, hidden), low),
                pltpu.VMEM((TILE, width), high),
                halves,
                halves,
                halves,
                halves,
                pltpu.VMEM((local, half), low),
                pltpu.VMEM((steps, TILE, half), low),
                pltpu.VMEM((2, TILE, CHUNK), high),
                pltpu.VMEM((local, width), low),
                dma((2,)),
                dma((1 + steps,)),
                dma((1 + steps,)),
                dma((1 + 2 * chunks,)),
                dma((1 + 2 * chunks,)),
                dma((1 + 2 * chunks,)),
                dma((2, chunks)),
                dma((2, chunks)),
                dma((2, chunks)),
            ],
        ),
        compiler_params=pltpu.CompilerParams(
            dimension_semantics=("arbitrary",), vmem_limit_bytes=67_000_000, collective_id=3, has_side_effects=True
        ),
        cost_estimate=pl.CostEstimate(flops=32_000_000_000, bytes_accessed=40_000_000, transcendentals=6_000_000),
        name="dense_layer",
    )(tokens, mine, other, cotangent, cotangent_far, vectors, bias_inner, *inner_parts, *outer_parts)


def lowered(piece):
    return piece.astype(jnp.bfloat16)


def widen(piece):
    return piece.astype(jnp.float32)


def matmul(left, right):
    return jnp.dot(left, right, preferred_element_type=jnp.float32)


def matmul_tn(left, right):
    return lax.dot_general(
        left, right, (((0,), (0,)), ((), ())), preferred_element_type=jnp.float32
    )


def matmul_nt(left, right):
    return lax.dot_general(
        left, right, (((1,), (1,)), ((), ())), preferred_element_type=jnp.float32
    )


def normalize(hidden, norm_gain, norm_shift):
    centred = hidden - jnp.mean(hidden, axis=-1, keepdims=True)
    reciprocal = lax.rsqrt(jnp.mean(centred * centred, axis=-1, keepdims=True) + EPS)
    normed = centred * reciprocal
    return (normed * norm_gain + norm_shift, normed, reciprocal)


def normalize_back(upstream, normed, reciprocal, norm_gain):
    scaled = upstream * norm_gain
    result = reciprocal * (
        scaled
        - jnp.mean(scaled, axis=-1, keepdims=True)
        - normed * jnp.mean(scaled * normed, axis=-1, keepdims=True)
    )
    return (result, jnp.sum(upstream * normed, axis=0), jnp.sum(upstream, axis=0))


def gelu_value(values_in):
    return 0.5 * values_in * (1.0 + lax.erf(values_in * ROOT_HALF))


def gelu_slope(values_in):
    return (
        0.5 * (1.0 + lax.erf(values_in * ROOT_HALF))
        + values_in * jnp.exp(-0.5 * values_in * values_in) * INV_ROOT_TAU
    )


def shift(piece, axis, step):
    size = lax.axis_size(axis)
    return lax.ppermute(piece, axis, [(i, (i + step) % size) for i in range(size)])


def swap(piece, axis):
    return lax.ppermute(piece, axis, [(0, 1), (1, 0)])


def pick(piece, index, axis=0):
    return lax.dynamic_index_in_dim(piece, index, axis, keepdims=False)


def in_order(first_is_zero, own, other, axis):
    return jnp.where(
        first_is_zero,
        jnp.concatenate([own, other], axis),
        jnp.concatenate([other, own], axis),
    )


def collect(piece):
    size_z, size_x = lax.axis_size("z"), lax.axis_size("x")
    z, x = lax.axis_index("z"), lax.axis_index("x")
    along_z = [piece] + [shift(piece, "z", k) for k in range(1, size_z)]
    whole = jnp.zeros((size_z, size_x) + piece.shape, piece.dtype)
    zeros = (0,) * piece.ndim
    for j in range(size_x):
        for k in range(size_z):
            arrived = along_z[k] if j == 0 else shift(along_z[k], "x", j)
            place = ((z - k) % size_z, (x - j) % size_x) + zeros
            whole = lax.dynamic_update_slice(whole, arrived[None, None], place)
    return whole.reshape((size_z * size_x,) + piece.shape)


def reduce_owned(terms):
    size_z, size_x = lax.axis_size("z"), lax.axis_size("x")
    z, x = lax.axis_index("z"), lax.axis_index("x")
    terms = terms.reshape((size_z, size_x) + terms.shape[1:])
    total = widen(pick(terms, x, 1))
    for j in range(1, size_x):
        total = total + widen(shift(pick(terms, (x + j) % size_x, 1), "x", j))
    terms = lowered(total)
    total = widen(pick(terms, z))
    for k in range(1, size_z):
        total = total + widen(shift(pick(terms, (z + k) % size_z), "z", k))
    terms = lowered(total)
    return widen(terms) + widen(swap(terms, "y"))


def plain_body(
    tokens,
    segment_ids,
    w_query,
    w_key,
    w_value,
    w_output,
    b_query,
    b_value,
    b_output,
    first_gain,
    first_shift,
    w_inner,
    b_inner,
    w_outer,
    b_outer,
    second_gain,
    second_shift,
    cotangent,
):
    core, y = lax.axis_index("core"), lax.axis_index("y")
    shards = lax.axis_size("z") * lax.axis_size("x")
    sequences, part, width = tokens.shape
    half = width // 2
    pairs = half // 128
    hidden = w_inner.shape[1]
    local = 2 * part
    own_rows = w_query.shape[0]
    unit_half = hidden // shards // 2

    def columns(matrix):
        return lowered(lax.dynamic_slice_in_dim(matrix, core * half, half, 1))

    vectors = (b_query, b_value, b_output, first_gain, first_shift, b_inner, b_outer, second_gain, second_shift)
    flat = jnp.concatenate([lowered(v) for v in vectors])
    lanes = 3 * half
    extra = -(-flat.shape[0] // lanes)
    flat = jnp.pad(flat, (0, extra * lanes - flat.shape[0])).reshape(extra, lanes)
    weights = jnp.stack([columns(w).reshape(own_rows, pairs, 128) for w in (w_query, w_key, w_value)], axis=2)
    early = collect(jnp.concatenate([weights.reshape(own_rows, lanes), flat], axis=0))

    mine = pick(tokens, y)
    arrived = swap(pick(tokens, 1 - y), "y")
    mine_other, arrived_other = swap(mine, "core"), swap(arrived, "core")
    inputs_all = jnp.concatenate([mine, arrived, mine_other, arrived_other], axis=0)
    inputs = jnp.concatenate([mine, arrived], axis=0)

    inner_piece = lowered(pick(w_inner.reshape(own_rows, shards, 2, unit_half), core, 2)).reshape(own_rows, hidden // 2)
    late = collect(jnp.concatenate([columns(w_output), inner_piece], axis=1)).reshape(width, half + hidden // 2)
    outer_own = collect(lowered(lax.dynamic_slice_in_dim(w_outer, core * unit_half, unit_half, 0))).reshape(hidden // 2, width)
    output_own, inner_own = late[:, :half], late[:, half:]
    output_other, inner_other, outer_other = swap(output_own, "core"), swap(inner_own, "core"), swap(outer_own, "core")
    full_output = in_order(core == 0, output_own, output_other, 1)
    cotangent_mine = pick(cotangent, y)
    cotangent_arrived = swap(pick(cotangent, 1 - y), "y")

    full_early = early[:, :own_rows].reshape(width, lanes)
    flat_all = early[:, own_rows:].reshape(shards, extra * lanes)
    sizes = [v.shape[0] for v in vectors]
    gathered, at = [], 0
    for size in sizes:
        gathered.append(flat_all[:, at : at + size].reshape(shards * size))
        at += size
    bias_query, bias_value, bias_output, gain_first, shift_first, bias_inner, bias_outer, gain_second, shift_second = [
        widen(v) for v in gathered
    ]
    biases = jnp.concatenate([bias_query[None], bias_value[None], jnp.zeros((14, width), jnp.float32)], axis=0)
    heads_mine, heads_other, logsum, projected = attention(segment_ids, inputs_all, full_early, biases)
    context = in_order(core == 0, heads_mine, swap(heads_other, "core"), 1)

    attended = matmul(context, full_output) + bias_output
    first, first_normed, first_recip = normalize(widen(inputs) + attended, gain_first, shift_first)
    first_low = lowered(first)
    biases = bias_inner.reshape(shards, 2, unit_half)
    halves = ((inner_own, outer_own, pick(biases, core, 1)), (inner_other, outer_other, pick(biases, 1 - core, 1)))
    outer, kept = bias_outer, []
    for inner_weight, outer_weight, bias in halves:
        inner = matmul(first_low, inner_weight) + bias.reshape(hidden // 2)
        active = lowered(gelu_value(inner))
        outer = outer + matmul(active, outer_weight)
        kept.append((inner, active))
    mixed, second_normed, second_recip = normalize(first + outer, gain_second, shift_second)
    mixed = lowered(mixed)

    upstream = widen(jnp.concatenate([cotangent_mine, cotangent_arrived], axis=0))
    pre_second, grad_second_gain, grad_second_shift = normalize_back(upstream, second_normed, second_recip, gain_second)
    grad_outer = lowered(pre_second)
    grad_b_outer = jnp.sum(widen(grad_outer), axis=0)
    grad_first, inner_grads, outer_grads, bias_grads = pre_second, [], [], []
    for (inner, active), (inner_weight, outer_weight, _) in zip(kept, halves):
        grad_inner = lowered(matmul_nt(grad_outer, outer_weight) * gelu_slope(inner))
        outer_grads.append(lowered(matmul_tn(active, grad_outer)))
        inner_grads.append(lowered(matmul_tn(first_low, grad_inner)))
        bias_grads.append(jnp.sum(widen(grad_inner), axis=0).reshape(shards, 1, unit_half))
        grad_first = grad_first + matmul_nt(grad_inner, inner_weight)
    grad_b_inner = in_order(core == 0, bias_grads[0], bias_grads[1], 1).reshape(hidden)
    pre_first, grad_first_gain, grad_first_shift = normalize_back(grad_first, first_normed, first_recip, gain_first)
    grad_attended = lowered(pre_first)
    grad_b_output = jnp.sum(widen(grad_attended), axis=0)
    grad_w_output = lowered(matmul_tn(context, grad_attended))
    grad_context = lowered(matmul_nt(grad_attended, full_output))
    context_mine = lax.dynamic_slice_in_dim(grad_context, core * half, half, 1)
    context_other = lax.dynamic_slice_in_dim(grad_context, (1 - core) * half, half, 1)
    upstream_other = swap(context_other, "core")

    def core_sum(own, other):
        return lowered(widen(own) + widen(swap(other, "core")))

    outer_term = core_sum(*outer_grads)
    inner_term = core_sum(*inner_grads)
    output_term = core_sum(
        lax.dynamic_slice_in_dim(grad_w_output, core * half, half, 1),
        lax.dynamic_slice_in_dim(grad_w_output, (1 - core) * half, half, 1),
    )
    outer_done = reduce_owned(outer_term.reshape(shards, unit_half, width))
    late_done = reduce_owned(jnp.concatenate([output_term, inner_term], axis=1).reshape(shards, own_rows, half + hidden // 2))

    grads, sums = attention_back(segment_ids, projected, heads_mine, heads_other, context_mine, upstream_other, logsum)
    grad_early = lowered(matmul_tn(inputs_all, grads))
    partial = matmul_nt(grads, full_early)
    sums = sums.reshape(pairs, 8, 3, 128)[:, 0]
    blank = jnp.zeros((width,), jnp.float32)
    grad_b_query = lax.dynamic_update_slice(blank, sums[:, 0].reshape(half), (core * half,))
    grad_b_value = lax.dynamic_update_slice(blank, sums[:, 2].reshape(half), (core * half,))
    vector_grads = (
        grad_b_query,
        grad_b_value,
        grad_b_output,
        grad_first_gain,
        grad_first_shift,
        grad_b_inner,
        grad_b_outer,
        grad_second_gain,
        grad_second_shift,
    )
    flat_grads = jnp.concatenate([v.reshape(shards, -1) for v in vector_grads], axis=1)
    flat_grads = jnp.pad(flat_grads, ((0, 0), (0, extra * lanes - flat_grads.shape[1])))
    early_term = jnp.concatenate(
        [grad_early.reshape(shards, own_rows, lanes), lowered(flat_grads).reshape(shards, extra, lanes)], axis=1
    )
    early_done = reduce_owned(early_term)

    grad_inputs = pre_first + partial[:local] + widen(swap(lowered(partial[local:]), "core"))
    returned = widen(swap(lowered(grad_inputs[part:]), "y"))
    grad_tokens = in_order(y == 0, grad_inputs[None, :part], returned[None], 0)
    mixed_out = in_order(y == 0, mixed[None, :part], swap(mixed[part:], "y")[None], 0)

    def both(piece):
        return widen(swap(lowered(piece), "core"))

    early_matrix = early_done[:own_rows]
    early_full = in_order(
        core == 0, early_matrix.reshape(own_rows, pairs, 3, 128)[None], both(early_matrix).reshape(own_rows, pairs, 3, 128)[None], 0
    )
    early_full = early_full.transpose(3, 1, 0, 2, 4).reshape(3, own_rows, width)
    late_other = both(late_done)
    output_full = in_order(core == 0, late_done[:, :half], late_other[:, :half], 1)
    inner_full = in_order(
        core == 0,
        late_done[:, half:].reshape(own_rows, shards, 1, unit_half),
        late_other[:, half:].reshape(own_rows, shards, 1, unit_half),
        2,
    ).reshape(own_rows, hidden)
    outer_full = in_order(core == 0, outer_done, both(outer_done), 0)
    vector_part = early_done[own_rows:]
    vector_sums = (vector_part + swap(vector_part, "core")).reshape(extra * lanes)
    out_vectors, at = [], 0
    for size in sizes:
        out_vectors.append(vector_sums[at : at + size])
        at += size
    (
        done_b_query,
        done_b_value,
        done_b_output,
        done_first_gain,
        done_first_shift,
        done_b_inner,
        done_b_outer,
        done_second_gain,
        done_second_shift,
    ) = out_vectors
    return (
        mixed_out,
        grad_tokens,
        early_full[0],
        early_full[1],
        early_full[2],
        output_full,
        done_b_query,
        done_b_value,
        done_b_output,
        done_first_gain,
        done_first_shift,
        inner_full,
        done_b_inner,
        outer_full,
        done_b_outer,
        done_second_gain,
        done_second_shift,
    )


def body(
    tokens,
    segment_ids,
    w_query,
    w_key,
    w_value,
    w_output,
    b_query,
    b_value,
    b_output,
    first_gain,
    first_shift,
    w_inner,
    b_inner,
    w_outer,
    b_outer,
    second_gain,
    second_shift,
    cotangent,
):
    core, y = lax.axis_index("core"), lax.axis_index("y")
    size_z, size_x = lax.axis_size("z"), lax.axis_size("x")
    shards = size_z * size_x
    sequences, part, width = tokens.shape
    half = width // 2
    pairs = half // 128
    hidden = w_inner.shape[1]
    local = 2 * part
    own_rows = w_query.shape[0]
    lanes = 3 * half

    vectors = (b_query, b_value, b_output, first_gain, first_shift, b_inner, b_outer, second_gain, second_shift)
    sizes = [v.shape[0] for v in vectors]
    tokens_all, cotangent_send, early, inner_own, outer_own, rows, inner_row = entry(
        size_z, size_x, tokens, cotangent, w_query, w_key, w_value, w_inner, w_output, w_outer, vectors
    )
    cotangent_far = swap(cotangent_send, "y")
    inner_parts = [inner_own] + [shift(inner_own, "x", j) for j in range(1, size_x)]
    outer_parts = [outer_own] + [shift(outer_own, "z", k) for k in range(1, size_z)]
    inputs_all = tokens_all.reshape(4 * part, width)
    full_early = early.reshape(width, lanes)
    context_mine, context_other, logsum, projected = attention(segment_ids, inputs_all, full_early, rows)
    made = dense_layer(
        size_z,
        size_x,
        inputs_all,
        context_mine,
        context_other,
        cotangent,
        cotangent_far,
        rows,
        inner_row,
        inner_parts,
        outer_parts,
    )
    mixed, mixed_send, pre_first, upstream_mine, upstream_other, dense_sums, inner_sums, grad_w_output = made[:8]
    inner_terms = [made[8]] + [shift(made[8 + k], "z", k) for k in range(1, size_z)]
    outer_terms = [made[8 + size_z]] + [shift(made[8 + size_z + j], "x", j) for j in range(1, size_x)]
    mixed_far = swap(mixed_send, "y")
    grads, sums = attention_back(segment_ids, projected, context_mine, context_other, upstream_mine, upstream_other, logsum)
    made = exit_call(
        size_z,
        size_x,
        grads,
        inputs_all,
        full_early,
        pre_first,
        grad_w_output.reshape(shards, own_rows, width),
        dense_sums,
        inner_sums,
        sums,
        inner_terms,
        outer_terms,
    )
    mixed_out, grad_tokens, grad_query, grad_key, grad_value, grad_output, grad_inner_full, grad_outer_full, *done = deliver(
        mixed, mixed_far, made[:7], made[7], sizes
    )
    return (
        mixed_out,
        grad_tokens,
        grad_query,
        grad_key,
        grad_value,
        grad_output,
        *done[:5],
        grad_inner_full,
        done[5],
        grad_outer_full,
        *done[6:],
    )


def layer(*arrays):
    if arrays[2].shape[0] % 32 == 0 and lax.axis_size("x") > 1:
        return body(*arrays)
    return plain_body(*arrays)


def solution(mesh):
    outer, inner = mesh.devices.shape
    size_z = 1
    while size_z * size_z < outer:
        size_z *= 2
    split = Mesh(mesh.devices.reshape(size_z, outer // size_z, inner // 2, 2), ("z", "x", "y", "core"))
    dp, seq = ("z", "x"), ("y", "core")
    activation, matrix, vector = P(dp, seq, None), P(dp, None), P(dp)
    return jax.shard_map(
        layer,
        mesh=split,
        in_specs=(
            activation,
            matrix,
            matrix,
            matrix,
            matrix,
            matrix,
            vector,
            vector,
            vector,
            vector,
            vector,
            matrix,
            vector,
            matrix,
            vector,
            vector,
            vector,
            activation,
        ),
        out_specs=(
            activation,
            activation,
            matrix,
            matrix,
            matrix,
            matrix,
            vector,
            vector,
            vector,
            vector,
            vector,
            matrix,
            vector,
            matrix,
            vector,
            vector,
            vector,
        ),
        check_vma=False,
    )
```

```python
import jax
import jax.numpy as jnp
from jax import lax
from jax.experimental import pallas as pl
from jax.experimental.pallas import tpu as pltpu
from jax.sharding import Mesh
from jax.sharding import PartitionSpec as P


HD = 64
EPS = 1e-12
ROOT_HALF = 0.7071067811865476
INV_ROOT_TAU = 0.3989422804014327

BLK = 256
BIG = -1.0e9
DOCUMENTS = 4


def dot_nn(a, b):
    return jnp.dot(a, b, preferred_element_type=jnp.float32)


def local_start(b, part):
    core, y = lax.axis_index("core"), lax.axis_index("y")
    return (jnp.where(b % 2 == core, 0, 2) + jnp.where(b // 2 == y, 0, 1)) * part


def part_rows(b, part):
    return pl.ds(pl.multiple_of(local_start(b, part), 128), part)


def find_bounds(segment_ref, bound_ref):
    length = segment_ref.shape[1]
    y = lax.axis_index("y")
    bound_ref[0] = 0
    bound_ref[DOCUMENTS] = length
    for d in range(1, DOCUMENTS):

        def halve(_, span):
            low, high = span
            middle = (low + high) // 2
            below = segment_ref[y, jnp.minimum(middle, length - 1)] < d
            inside = low < high
            return (
                jnp.where(jnp.logical_and(inside, below), middle + 1, low),
                jnp.where(jnp.logical_and(inside, jnp.logical_not(below)), middle, high),
            )

        low, _ = lax.fori_loop(0, length.bit_length(), halve, (0, length))
        bound_ref[d] = low


def find_window(segment_ref, bound_ref, qb):
    length = segment_ref.shape[1]
    y = lax.axis_index("y")
    first = segment_ref[y, qb * BLK]
    last = segment_ref[y, qb * BLK + BLK - 1]
    start = bound_ref[first] // 128 * 128
    count = (bound_ref[last + 1] - start + BLK - 1) // BLK
    return jnp.minimum(start, length - count * BLK), count


def each_tile(count, step):
    def two(i, _):
        step(i * (2 * BLK), 2 * BLK)
        return 0

    lax.fori_loop(0, count // 2, two, 0)

    @pl.when(count % 2 == 1)
    def _():
        step((count - 1) * BLK, BLK)


def make_marks(row_ref, mark_query, mark_key):
    length = mark_key.shape[0]
    y = lax.axis_index("y")
    step = 512
    for b in range(length // step):
        rows = slice(b * step, (b + 1) * step)
        column = jnp.broadcast_to(row_ref[pl.ds(y, 1), rows], (128, step)).T
        lane = lax.broadcasted_iota(jnp.int32, (step, 128), 1) % 64
        same = lane == column
        line = lax.broadcasted_iota(jnp.int32, (128, step), 0) % 64
        mark_query[:, rows] = jnp.where(line == row_ref[pl.ds(y, 1), rows], 1.0, 0.0).astype(jnp.bfloat16)
        apart = jnp.logical_and(lane < DOCUMENTS, jnp.logical_not(same))
        mark_key[rows, :] = jnp.where(apart, BIG, 0.0).astype(jnp.bfloat16)


def forward_kernel(segment_ref, row_ref, tokens_ref, weights_ref, bias_ref, *refs):
    mine_ref, other_ref, lse_ref, qkv_ref, q2, k2, vt, acc, top, tot, keep, mark_query, mark_key, bound_ref = refs
    length = qkv_ref.shape[0]
    blocks = length // BLK
    part = length // 4

    @pl.when(pl.program_id(0) == 0)
    def _():
        find_bounds(segment_ref, bound_ref)
        make_marks(row_ref, mark_query, mark_key)

    low = lax.broadcasted_iota(jnp.int32, (part, 128), 1) < 64
    for b in range(4):
        src = part_rows(b, part)
        dst = slice(b * part, (b + 1) * part)
        made = dot_nn(tokens_ref[src, :], weights_ref[...])
        lanes = pl.ds(pl.multiple_of(lax.axis_index("core") * (128 * pl.num_programs(0)) + pl.program_id(0) * 128, 128), 128)
        q = ((made[:, 0:128] + bias_ref[0:1, lanes]) * 0.125).astype(jnp.bfloat16)
        k = made[:, 128:256].astype(jnp.bfloat16)
        v = (made[:, 256:384] + bias_ref[1:2, lanes]).astype(jnp.bfloat16)
        qkv_ref[src, 0:128] = q
        qkv_ref[src, 128:256] = k
        qkv_ref[src, 256:384] = v
        nohk = mark_key[dst, :]
        turned = q.T
        q2[0, 0:64, dst] = turned[0:64]
        q2[0, 64:128, dst] = mark_query[64:128, dst]
        q2[1, 0:64, dst] = mark_query[0:64, dst]
        q2[1, 64:128, dst] = turned[64:128]
        k2[0, dst, :] = jnp.where(low, k, nohk)
        k2[1, dst, :] = jnp.where(low, nohk, k)
        vt[:, dst] = v.T
    lse_ref[...] = jnp.zeros_like(lse_ref)

    def row(qb, _):
        qs = pl.ds(pl.multiple_of(qb * BLK, BLK), BLK)
        start, count = find_window(segment_ref, bound_ref, qb)
        top[...] = jnp.full_like(top, -1.0e30)

        def fold(tile, function):
            return function(tile.reshape(tile.shape[0] // 8, 8, BLK), axis=0)

        def highest(first, size):
            keys = pl.ds(pl.multiple_of(start + first, 128), size)
            for h in range(2):
                st = dot_nn(k2[h, keys, :], q2[h, :, qs])
                keep[h, pl.ds(pl.multiple_of(first, BLK), size), :] = st
                top[h] = jnp.maximum(top[h], fold(st, jnp.max))

        def weigh(first, size, largest):
            keys = pl.ds(pl.multiple_of(start + first, 128), size)
            for h in range(2):
                rows = slice(64 * h, 64 * h + 64)
                st = keep[h, pl.ds(pl.multiple_of(first, BLK), size), :]
                p = jnp.exp(st - largest[h])
                tot[h] = tot[h] + fold(p, jnp.sum)
                acc[rows, :] = acc[rows, :] + dot_nn(vt[rows, keys], p.astype(jnp.bfloat16))

        def paired(step):
            each_tile(count, step)

        paired(highest)
        largest = [jnp.max(top[h], axis=0, keepdims=True) for h in range(2)]
        acc[...] = jnp.zeros_like(acc)
        tot[...] = jnp.zeros_like(tot)
        paired(lambda first, size: weigh(first, size, largest))
        for h in range(2):
            rows = slice(64 * h, 64 * h + 64)
            total = jnp.sum(tot[h], axis=0, keepdims=True)
            acc[rows, :] = acc[rows, :] / total
            lse_ref[h : h + 1, qs] = largest[h] + jnp.log(total)
        where = local_start(qb * BLK // part, part) + qb * BLK % part
        result = acc[...].T.astype(jnp.bfloat16)

        @pl.when(where < 2 * part)
        def _():
            mine_ref[pl.ds(pl.multiple_of(where, BLK), BLK), :] = result

        @pl.when(where >= 2 * part)
        def _():
            other_ref[pl.ds(pl.multiple_of(where - 2 * part, BLK), BLK), :] = result

        return 0

    lax.fori_loop(0, blocks, row, 0)


def attention(segments, tokens, weights, biases):
    length, depth = tokens.shape
    width = weights.shape[1]
    pairs = width // 384
    rows = length // 2
    return pl.pallas_call(
        forward_kernel,
        out_shape=(
            jax.ShapeDtypeStruct((rows, pairs * 128), jnp.bfloat16),
            jax.ShapeDtypeStruct((rows, pairs * 128), jnp.bfloat16),
            jax.ShapeDtypeStruct((pairs * 8, length), jnp.float32),
            jax.ShapeDtypeStruct((length, width), jnp.bfloat16),
        ),
        grid_spec=pltpu.PrefetchScalarGridSpec(
            num_scalar_prefetch=1,
            grid=(pairs,),
            in_specs=[
                pl.BlockSpec(segments.shape, lambda p, *_: (0, 0)),
                pl.BlockSpec((length, depth), lambda p, *_: (0, 0)),
                pl.BlockSpec((depth, 384), lambda p, *_: (0, p)),
                pl.BlockSpec(biases.shape, lambda p, *_: (0, 0)),
            ],
            out_specs=[
                pl.BlockSpec((rows, 128), lambda p, *_: (0, p)),
                pl.BlockSpec((rows, 128), lambda p, *_: (0, p)),
                pl.BlockSpec((8, length), lambda p, *_: (p, 0)),
                pl.BlockSpec((length, 384), lambda p, *_: (0, p)),
            ],
            scratch_shapes=[
                pltpu.VMEM((2, 128, length), jnp.bfloat16),
                pltpu.VMEM((2, length, 128), jnp.bfloat16),
                pltpu.VMEM((128, length), jnp.bfloat16),
                pltpu.VMEM((128, BLK), jnp.float32),
                pltpu.VMEM((2, 8, BLK), jnp.float32),
                pltpu.VMEM((2, 8, BLK), jnp.float32),
                pltpu.VMEM((2, length, BLK), jnp.float32),
                pltpu.VMEM((128, length), jnp.bfloat16),
                pltpu.VMEM((length, 128), jnp.bfloat16),
                pltpu.SMEM((DOCUMENTS + 1,), jnp.int32),
            ],
        ),
        compiler_params=pltpu.CompilerParams(dimension_semantics=("arbitrary",), vmem_limit_bytes=60 << 20),
        cost_estimate=pl.CostEstimate(flops=pairs * 40_000_000_000, bytes_accessed=pairs * 3_000_000, transcendentals=pairs * 4_000_000),
        name="attention_forward",
    )(segments, segments, tokens, weights, biases)


def backward_kernel(
    segment_ref,
    qkv_ref,
    ctx_mine_ref,
    ctx_other_ref,
    do_mine_ref,
    do_other_ref,
    lse_ref,
    row_ref,
    out_ref,
    sum_ref,
    q2,
    k2,
    q0,
    d0,
    dt,
    v0,
    kt,
    dk,
    dv,
    dqt,
    delta,
    mark_query,
    mark_key,
    bound_ref,
):
    length = qkv_ref.shape[0]
    blocks = length // BLK
    part = length // 4

    @pl.when(pl.program_id(0) == 0)
    def _():
        find_bounds(segment_ref, bound_ref)
        make_marks(row_ref, mark_query, mark_key)

    low = lax.broadcasted_iota(jnp.int32, (part, 128), 1) < 64

    def prepare(b, do, ctx):
        src = part_rows(b, part)
        dst = slice(b * part, (b + 1) * part)
        q, k = qkv_ref[src, 0:128], qkv_ref[src, 128:256]
        zero = jnp.zeros_like(q)
        nohk = mark_key[dst, :]
        turned = q.T
        q2[0, 0:64, dst] = turned[0:64]
        q2[0, 64:128, dst] = mark_query[64:128, dst]
        q2[1, 0:64, dst] = mark_query[0:64, dst]
        q2[1, 64:128, dst] = turned[64:128]
        k2[0, dst, :] = jnp.where(low, k, nohk)
        k2[1, dst, :] = jnp.where(low, nohk, k)
        q0[0, dst, :] = jnp.where(low, q, zero)
        q0[1, dst, :] = jnp.where(low, zero, q)
        d0[0, dst, :] = jnp.where(low, do, zero)
        d0[1, dst, :] = jnp.where(low, zero, do)
        turned = do.T
        blank = jnp.zeros((64, part), jnp.bfloat16)
        dt[0, 0:64, dst] = turned[0:64]
        dt[0, 64:128, dst] = blank
        dt[1, 0:64, dst] = blank
        dt[1, 64:128, dst] = turned[64:128]
        v0[dst, :] = qkv_ref[src, 256:384]
        kt[:, dst] = k.T
        prod = turned.astype(jnp.float32) * ctx.T.astype(jnp.float32)
        delta[0:1, dst] = jnp.sum(prod[0:64], axis=0, keepdims=True)
        delta[1:2, dst] = jnp.sum(prod[64:128], axis=0, keepdims=True)

    for b in range(4):

        @pl.when(local_start(b, part) < 2 * part)
        def _():
            rows = part_rows(b, part)
            prepare(b, do_mine_ref[rows, :], ctx_mine_ref[rows, :])

        @pl.when(local_start(b, part) >= 2 * part)
        def _():
            rows = pl.ds(pl.multiple_of(local_start(b, part) - 2 * part, 128), part)
            prepare(b, do_other_ref[rows, :], ctx_other_ref[rows, :])

    dk[...] = jnp.zeros_like(dk)
    dv[...] = jnp.zeros_like(dv)
    dqt[...] = jnp.zeros_like(dqt)

    def row(qb, _):
        qs = pl.ds(pl.multiple_of(qb * BLK, BLK), BLK)
        start, count = find_window(segment_ref, bound_ref, qb)

        def tile(first, size):
            ks = pl.ds(pl.multiple_of(start + first, 128), size)
            weights, grads = [], []
            for h in range(2):
                st = dot_nn(k2[h, ks, :], q2[h, :, qs])
                w = jnp.exp(st - lse_ref[h : h + 1, qs])
                gw = dot_nn(v0[ks, :], dt[h, :, qs])
                weights.append(w.astype(jnp.bfloat16))
                grads.append((w * (gw - delta[h : h + 1, qs])).astype(jnp.bfloat16))
            dv[ks, :] += dot_nn(jnp.concatenate(weights, axis=1), jnp.concatenate([d0[0, qs, :], d0[1, qs, :]], axis=0))
            dk[ks, :] += dot_nn(jnp.concatenate(grads, axis=1), jnp.concatenate([q0[0, qs, :], q0[1, qs, :]], axis=0))
            for h in range(2):
                rows = slice(64 * h, 64 * h + 64)
                dqt[rows, qs] += dot_nn(kt[rows, ks], grads[h])

        each_tile(count, tile)
        return 0

    lax.fori_loop(0, blocks, row, 0)
    sums = [jnp.zeros((1, 128), jnp.float32) for _ in range(3)]
    for b in range(4):
        dst = part_rows(b, part)
        src = slice(b * part, (b + 1) * part)
        pieces = ((dqt[:, src].T * 0.125).astype(jnp.bfloat16), dk[src, :].astype(jnp.bfloat16), dv[src, :].astype(jnp.bfloat16))
        for i, piece in enumerate(pieces):
            out_ref[dst, 128 * i : 128 * i + 128] = piece
            sums[i] = sums[i] + jnp.sum(piece.astype(jnp.float32), axis=0, keepdims=True)
    sum_ref[...] = jnp.zeros_like(sum_ref)
    for i in range(3):
        sum_ref[0:1, 128 * i : 128 * i + 128] = sums[i]


def attention_back(segments, qkv, ctx_mine, ctx_other, do_mine, do_other, lse):
    length, width = qkv.shape
    pairs = width // 384
    rows = length // 2
    half = lambda: pltpu.VMEM((2, length, 128), jnp.bfloat16)
    turned = lambda: pltpu.VMEM((2, 128, length), jnp.bfloat16)
    column = pl.BlockSpec((rows, 128), lambda p, *_: (0, p))
    return pl.pallas_call(
        backward_kernel,
        out_shape=(
            jax.ShapeDtypeStruct((length, width), jnp.bfloat16),
            jax.ShapeDtypeStruct((pairs * 8, 384), jnp.float32),
        ),
        grid_spec=pltpu.PrefetchScalarGridSpec(
            num_scalar_prefetch=1,
            grid=(pairs,),
            in_specs=[
                pl.BlockSpec((length, 384), lambda p, *_: (0, p)),
                column,
                column,
                column,
                column,
                pl.BlockSpec((8, length), lambda p, *_: (p, 0)),
                pl.BlockSpec(segments.shape, lambda p, *_: (0, 0)),
            ],
            out_specs=[
                pl.BlockSpec((length, 384), lambda p, *_: (0, p)),
                pl.BlockSpec((8, 384), lambda p, *_: (p, 0)),
            ],
            scratch_shapes=[
                turned(),
                half(),
                half(),
                half(),
                turned(),
                pltpu.VMEM((length, 128), jnp.bfloat16),
                pltpu.VMEM((128, length), jnp.bfloat16),
                pltpu.VMEM((length, 128), jnp.float32),
                pltpu.VMEM((length, 128), jnp.float32),
                pltpu.VMEM((128, length), jnp.float32),
                pltpu.VMEM((8, length), jnp.float32),
                pltpu.VMEM((128, length), jnp.bfloat16),
                pltpu.VMEM((length, 128), jnp.bfloat16),
                pltpu.SMEM((DOCUMENTS + 1,), jnp.int32),
            ],
        ),
        compiler_params=pltpu.CompilerParams(dimension_semantics=("arbitrary",), vmem_limit_bytes=60 << 20),
        cost_estimate=pl.CostEstimate(flops=pairs * 20_000_000_000, bytes_accessed=pairs * 5_000_000, transcendentals=pairs * 4_000_000),
        name="attention_backward",
    )(segments, qkv, ctx_mine, ctx_other, do_mine, do_other, lse, segments)


MESH_ID = pl.DeviceIdType.MESH
WIDE = 5


def place_of():
    return tuple(lax.axis_index(name) for name in ("z", "x", "y", "core"))


def sizes_of():
    return lax.axis_size("z"), lax.axis_size("x")


def partner(**moved):
    z, x, y, core = place_of()
    return (moved.get("z", z), moved.get("x", x), moved.get("y", y), moved.get("core", core))


def greet(with_grid):
    z, x, y, core = place_of()
    size_z, size_x = sizes_of()
    peers = [partner(y=1 - y), partner(core=1 - core)]
    if with_grid:
        peers += [partner(z=lax.rem(z + k, size_z)) for k in range(1, size_z)]
        peers += [partner(x=lax.rem(x + j, size_x)) for j in range(1, size_x)]
    barrier = pltpu.get_barrier_semaphore()
    for peer in peers:
        pl.semaphore_signal(barrier, inc=1, device_id=peer, device_id_type=MESH_ID)
    pl.semaphore_wait(barrier, len(peers))


def remote(src, dst, send, recv, peer):
    return pltpu.make_async_remote_copy(
        src_ref=src, dst_ref=dst, send_sem=send, recv_sem=recv, device_id=peer, device_id_type=MESH_ID
    )


def entry_kernel(size_z, size_x, count, *refs):
    tokens, cotangent, wq, wk, wv, w_inner, w_output, w_outer = refs[:8]
    vectors = refs[8 : 8 + count]
    tokens_all, cotangent_send, weights_all, inner_all, outer_all, rows_out, inner_out = refs[8 + count : 15 + count]
    raw = refs[15 + count : 15 + 2 * count]
    stage, cot_stage, wbuf, ibuf, obuf, pack, ipack, opack, vpack, vectors_all = refs[15 + 2 * count : 25 + 2 * count]
    local_sem, load_sem, tsend, trecv, zsend, zrecv, xsend, xrecv, ysend, yrecv, osend, orecv = refs[25 + 2 * count :]
    z, x, y, core = place_of()
    half = pack.shape[1] // 3
    pairs = half // 128
    chunks = w_inner.shape[1] // CHUNK
    me = z * size_x + x
    columns = [lax.rem(x + j, size_x) for j in range(size_x)]

    mine = pl.ds(pl.multiple_of(core * half, 128), half)
    loads = [pltpu.make_async_copy(w.at[:, mine], wbuf.at[i], load_sem.at[i]) for i, w in enumerate((wq, wk, wv))]
    loads += [pltpu.make_async_copy(v, r, load_sem.at[3 + i]) for i, (v, r) in enumerate(zip(vectors, raw))]
    late = [
        pltpu.make_async_copy(
            w_inner.at[:, pl.ds(pl.multiple_of(c * CHUNK + core * half, 128), half)],
            ibuf.at[:, pl.ds(c * half, half)],
            load_sem.at[3 + count + c],
        )
        for c in range(chunks)
    ]
    late.append(pltpu.make_async_copy(w_output.at[:, mine], ibuf.at[:, pl.ds(chunks * half, half)], load_sem.at[3 + count + chunks]))
    late.append(pltpu.make_async_copy(w_outer.at[:, mine], obuf, load_sem.at[4 + count + chunks]))
    load = pltpu.make_async_copy(tokens.at[y], stage, local_sem.at[0])
    cot_load = pltpu.make_async_copy(cotangent.at[1 - y], cot_stage, local_sem.at[4])
    for copy in loads + late + [load, cot_load]:
        copy.start()
    vpack[...] = jnp.zeros_like(vpack)
    for copy in loads:
        copy.wait()
    for i, vector in enumerate(raw):
        size = vector.shape[0]
        vpack[i : i + 1, 0:size] = vector[...].reshape(1, size).astype(jnp.bfloat16).astype(jnp.float32)
    for i in range(3):
        for p in range(pairs):
            pack[:, (3 * p + i) * 128 : (3 * p + i + 1) * 128] = wbuf[i, :, p * 128 : (p + 1) * 128].astype(jnp.bfloat16)
    vectors_all[me] = vpack[...]
    greet(True)

    across = remote(tokens.at[1 - y], tokens_all.at[1], tsend.at[0], trecv.at[0], partner(y=1 - y))
    across.start()
    beside = remote(tokens.at[y], tokens_all.at[2], tsend.at[1], trecv.at[1], partner(core=1 - core))

    rows = ipack.shape[0]

    def share(owner):
        return pl.ds(pl.multiple_of(owner * (rows // 2), rows // 2), rows // 2)

    packs = (pack, vpack, ipack.at[share(y), :])

    def y_move(index, origin):
        slot = home(2, origin)
        return remote(slot, slot, ysend.at[index], yrecv.at[index], partner(y=1 - y))

    def home(stream, origin):
        if stream == 2:
            return inner_all.at[origin, share(y), :]
        return (weights_all, vectors_all)[stream].at[origin * size_x + x]

    def z_move(stream, way, t):
        step = 1 - 2 * way
        origin = z - step * (t - 1)
        src = packs[stream] if t == 1 else home(stream, origin)
        peer = partner(z=lax.rem(z + step + size_z, size_z))
        return remote(src, home(stream, origin), zsend.at[stream, way, t - 1], zrecv.at[stream, way, t - 1], peer)

    def sends(way, t):
        step = 1 - 2 * way
        origin, target = z - step * (t - 1), z + step
        inside = lambda v: jnp.logical_and(v >= 0, v < size_z)
        return jnp.logical_and(inside(origin), inside(target))

    def receives(way, t):
        origin = z - (1 - 2 * way) * t
        return jnp.logical_and(origin >= 0, origin < size_z)

    def x_moves(index, origin, own):
        moves = []
        for j in range(1, size_x):
            for stream in range(2):
                src = packs[stream] if own else home(stream, origin)
                moves.append(
                    remote(
                        src,
                        home(stream, origin),
                        xsend.at[stream, index, j - 1],
                        xrecv.at[stream, index, j - 1],
                        partner(x=columns[j]),
                    )
                )
        return moves

    def start_z(streams, t):
        for way in range(2):

            @pl.when(sends(way, t))
            def _():
                for stream in streams:
                    z_move(stream, way, t).start()

    for move in x_moves(0, z, True):
        move.start()
    start_z((0, 1), 1)
    beside.start()
    for copy in late:
        copy.wait()
    ipack[...] = ibuf[...].astype(jnp.bfloat16)
    opack[...] = obuf[...].astype(jnp.bfloat16)
    start_z((2,), 1)
    outer_moves = [
        remote(opack, outer_all.at[x], osend.at[j - 1], orecv.at[j - 1], partner(x=columns[j])) for j in range(1, size_x)
    ]
    keeps = [
        pltpu.make_async_copy(pack, weights_all.at[me], local_sem.at[1]),
        pltpu.make_async_copy(ipack, inner_all.at[z], local_sem.at[2]),
        pltpu.make_async_copy(opack, outer_all.at[x], local_sem.at[6]),
    ]
    load.wait()
    keeps.append(pltpu.make_async_copy(stage, tokens_all.at[0], local_sem.at[3]))
    cot_load.wait()
    keeps.append(pltpu.make_async_copy(cot_stage, cotangent_send, local_sem.at[5]))
    for keep in keeps:
        keep.start()

    def arrive(streams, t, sideways):
        for way in range(2):

            @pl.when(receives(way, t))
            def _():
                origin = z - (1 - 2 * way) * t
                for stream in streams:
                    slot = home(stream, origin)
                    remote(
                        slot, slot, zsend.at[stream, way, t - 1], zrecv.at[stream, way, t - 1], partner(core=1 - core)
                    ).wait_recv()
                if sideways:
                    for move in x_moves(1 + way * (size_z - 1) + t - 1, origin, False):
                        move.start()
                else:
                    y_move(way * (size_z - 1) + t - 1, origin).start()

    onward = remote(tokens_all.at[1], tokens_all.at[3], tsend.at[2], trecv.at[2], partner(core=1 - core))
    for t in range(1, size_z):
        arrive((0, 1), t, True)
        if t < size_z - 1:
            start_z((0, 1), t + 1)
        if t == 1:
            for move in outer_moves:
                move.start()
        arrive((2,), t, False)
        if t < size_z - 1:
            start_z((2,), t + 1)
        if t == min(2, size_z - 1):
            across.wait_recv()
            onward.start()

    for move in x_moves(0, z, True):
        move.wait()
    for t in range(1, size_z):
        for way in range(2):

            @pl.when(receives(way, t))
            def _():
                origin = z - (1 - 2 * way) * t
                for move in x_moves(1 + way * (size_z - 1) + t - 1, origin, False):
                    move.wait()
                y_move(way * (size_z - 1) + t - 1, origin).wait()

            @pl.when(sends(way, t))
            def _():
                for stream in range(3):
                    z_move(stream, way, t).wait_send()

    short = min(vector.shape[0] for vector in raw)
    longest = vpack.shape[1]
    for s in range(size_z * size_x):
        rows_out[:, s * short : (s + 1) * short] = vectors_all[s, :, 0:short]
        inner_out[:, s * longest : (s + 1) * longest] = vectors_all[s, WIDE : WIDE + 1, :]
    for move in outer_moves:
        move.wait()
    across.wait_send()
    beside.wait()
    onward.wait()
    for keep in keeps:
        keep.wait()


def entry(size_z, size_x, tokens, cotangent, wq, wk, wv, w_inner, w_output, w_outer, vectors):
    _, part, width = tokens.shape
    rows = wq.shape[0]
    half = width // 2
    lanes = 3 * half
    hidden = w_inner.shape[1]
    long = w_outer.shape[0]
    mixed_lanes = hidden // 2 + half
    chunks = hidden // CHUNK
    longest = max(v.shape[0] for v in vectors)
    shards = size_z * size_x
    count = len(vectors)
    anywhere, vmem = pl.BlockSpec(memory_space=pl.ANY), pl.BlockSpec(memory_space=pltpu.VMEM)
    dma = pltpu.SemaphoreType.DMA
    low, high = jnp.bfloat16, jnp.float32
    side = size_x - 1
    return pl.pallas_call(
        lambda *refs: entry_kernel(size_z, size_x, count, *refs),
        out_shape=(
            jax.ShapeDtypeStruct((4, part, width), low),
            jax.ShapeDtypeStruct((part, width), low),
            jax.ShapeDtypeStruct((shards, rows, lanes), low),
            jax.ShapeDtypeStruct((size_z, rows, mixed_lanes), low),
            jax.ShapeDtypeStruct((size_x, long, half), low),
            jax.ShapeDtypeStruct((16, width), high),
            jax.ShapeDtypeStruct((1, shards * longest), high),
        ),
        in_specs=[anywhere] * (8 + count),
        out_specs=(anywhere,) * 5 + (vmem,) * 2,
        scratch_shapes=[pltpu.VMEM(v.shape, v.dtype) for v in vectors]
        + [
            pltpu.VMEM((part, width), low),
            pltpu.VMEM((part, width), low),
            pltpu.VMEM((3, rows, half), high),
            pltpu.VMEM((rows, mixed_lanes), high),
            pltpu.VMEM((long, half), high),
            pltpu.VMEM((rows, lanes), low),
            pltpu.VMEM((rows, mixed_lanes), low),
            pltpu.VMEM((long, half), low),
            pltpu.VMEM((16, longest), high),
            pltpu.VMEM((shards, 16, longest), high),
            dma((7,)),
            dma((5 + count + chunks,)),
            dma((4,)),
            dma((4,)),
            dma((3, 2, size_z - 1)),
            dma((3, 2, size_z - 1)),
            dma((2, 2 * size_z - 1, side)),
            dma((2, 2 * size_z - 1, side)),
            dma((2 * size_z - 2,)),
            dma((2 * size_z - 2,)),
            dma((side,)),
            dma((side,)),
        ],
        compiler_params=pltpu.CompilerParams(collective_id=0, has_side_effects=True, vmem_limit_bytes=66_000_000),
        name="entry",
    )(tokens, cotangent, wq, wk, wv, w_inner, w_output, w_outer, *vectors)


def exit_kernel(size_z, size_x, shapes, *refs):
    z, x, y, core = place_of()
    grads_hbm, inputs_hbm, weights_hbm, base_hbm, output_term, dense_sums, inner_sums, head_sums = refs[:8]
    inner_in = refs[8 : 8 + size_z]
    outer_in = refs[8 + size_z : 8 + size_z + size_x]
    refs = refs[8 + size_z + size_x :]
    made = refs[:8]
    token_grads, grad_query, grad_key, grad_value, grad_output, grad_inner, grad_outer, vector_sums = made
    grads, inputs, turned, weights, base, terms_a, terms_b, other_rows, recv_rows, send_rows, far_rows, odd = refs[8:20]
    inner_buf, outer_buf, vector_rows, vector_terms, inner_send = refs[20:25]
    load_sem, tsend, trecv, osend, orecv = refs[25:30]
    refs = list(refs[30:])
    terms = {"qa": terms_a, "qb": terms_b}
    xin, xsend, xrecv = {}, {}, {}
    zout, zin, zsend, zrecv = {}, {}, {}, {}
    ybuf, ysend, yrecv, cbuf, csend, crecv = {}, {}, {}, {}, {}, {}
    for name in shapes:
        ybuf[name], ysend[name], yrecv[name], cbuf[name], csend[name], crecv[name] = [refs.pop(0) for _ in range(6)]
        if name != "outer":
            xin[name], xsend[name], xrecv[name] = [refs.pop(0) for _ in range(3)]
        if name != "inner":
            zout[name], zin[name], zsend[name], zrecv[name] = [refs.pop(0) for _ in range(4)]

    shards, rows, half = odd.shape
    lanes = 3 * half
    pairs = half // 128
    hidden = grad_inner.shape[1]
    part = token_grads.shape[1]
    local = 2 * part
    low, high = jnp.bfloat16, jnp.float32
    mine = pl.ds(pl.multiple_of(core * half, 128), half)
    theirs = pl.ds(pl.multiple_of((1 - core) * half, 128), half)
    columns = [lax.rem(x + j, size_x) for j in range(size_x)]
    steps = [(t, way) for t in range(1, size_z) for way in range(2)]
    core_peer, y_peer = partner(core=1 - core), partner(y=1 - y)

    loads = {}
    for i, src in enumerate(inner_in):
        loads["inner", i] = pltpu.make_async_copy(src, inner_buf.at[i], load_sem.at[i])
    for i, src in enumerate(outer_in):
        loads["outer", i] = pltpu.make_async_copy(src, outer_buf.at[i], load_sem.at[size_z + i])
    for i, (name, src, dst) in enumerate(
        (("grads", grads_hbm, grads), ("weights", weights_hbm, weights), ("base", base_hbm, base), ("inputs", inputs_hbm, inputs))
    ):
        loads[name] = pltpu.make_async_copy(src, dst, load_sem.at[size_z + size_x + i])
    for load in loads.values():
        load.start()

    def inside(v):
        return jnp.logical_and(v >= 0, v < size_z)

    def target_of(t, way):
        return z + (1 - 2 * way) * (size_z - t)

    def fed(way):
        return inside(z - (1 - 2 * way))

    def x_move(name, n, at, j, src, dst):
        return remote(src, dst, xsend[name].at[n, at, j - 1], xrecv[name].at[n, at, j - 1], partner(x=columns[j]))

    def x_pieces(name, at):
        source = vector_terms if name == "vec" else terms[name]
        return [
            x_move(name, 0, at, j, source.at[at * size_x + columns[j]], xin[name].at[j - 1, at]) for j in range(1, size_x)
        ]

    def send_own(name):
        for move in x_pieces(name, z):
            move.start()

    def send_far(name):
        for t, way in steps:

            @pl.when(inside(target_of(t, way)))
            def _():
                for move in x_pieces(name, target_of(t, way)):
                    move.start()

    def own_part(name, at):
        if name == "outer":
            total = outer_buf[0, at].astype(high)
            for i in range(1, size_x):
                total = total + outer_buf[i, at].astype(high)
            return [(slice(None), total)]
        slot = at * size_x + x
        if name == "vec":
            total = vector_terms[slot]
            for move in x_pieces("vec", at):
                move.wait()
            for j in range(1, size_x):
                total = total + xin["vec"][j - 1, at]
            return [(slice(None), total)]
        for move in x_pieces(name, at):
            move.wait()
        total = terms[name][slot].astype(high)
        for j in range(1, size_x):
            total = total + xin[name][j - 1, at].astype(high)
        return [(slice(None), total)]

    def z_move(name, t, way):
        peer = partner(z=lax.rem(z + 1 - 2 * way + size_z, size_z))
        return remote(
            zout[name].at[way, t - 1], zin[name].at[way, t - 1], zsend[name].at[way, t - 1], zrecv[name].at[way, t - 1], peer
        )

    def step_z(name, t):
        for way in range(2):

            @pl.when(inside(target_of(t, way)))
            def _():
                pieces = own_part(name, target_of(t, way))
                if t > 1:

                    @pl.when(fed(way))
                    def _():
                        z_move(name, t - 1, way).wait_recv()

                for span, total in pieces:
                    if t > 1:
                        before = zin[name][way, t - 2, :, span].astype(high)
                        total = total + jnp.where(fed(way), before, 0.0)
                    zout[name][way, t - 1, :, span] = total.astype(zout[name].dtype)
                z_move(name, t, way).start()

    across, swapped = {}, {}

    def step_y(name):
        across[name] = remote(ybuf[name].at[0], ybuf[name].at[1], ysend[name], yrecv[name], y_peer)
        across[name].start()

    def finish_z(name):
        pieces = own_part(name, z)
        last = size_z - 1
        for way in range(2):

            @pl.when(fed(way))
            def _():
                z_move(name, last, way).wait_recv()

        for span, total in pieces:
            for way in range(2):
                before = zin[name][way, last - 1, :, span].astype(high)
                total = total + jnp.where(fed(way), before, 0.0)
            ybuf[name][0, :, span] = total.astype(ybuf[name].dtype)
        step_y(name)

    def step_core(name):
        across[name].wait()
        cbuf[name][0] = ybuf[name][0].astype(high) + ybuf[name][1].astype(high)
        swapped[name] = remote(cbuf[name].at[0], cbuf[name].at[1], csend[name], crecv[name], core_peer)
        swapped[name].start()

    def finish_core(name):
        swapped[name].wait()
        return cbuf[name]

    vector_rows[...] = jnp.zeros_like(vector_rows)
    for i, row in enumerate((7, 8, 6, 3, 4, 2)):
        vector_rows[row : row + 1, :] = jnp.sum(dense_sums[8 * i : 8 * i + 8, :], axis=0, keepdims=True)
    for p in range(pairs):
        place = pl.ds(pl.multiple_of(core * half + p * 128, 128), 128)
        vector_rows[0:1, place] = head_sums[8 * p : 8 * p + 1, 0:128]
        vector_rows[1:2, place] = head_sums[8 * p : 8 * p + 1, 256:384]
    inner_row = jnp.sum(inner_sums[...], axis=0, keepdims=True)
    vector_terms[...] = jnp.zeros_like(vector_terms)
    for name in zin:
        if name == "vec":
            zin[name][...] = jnp.zeros_like(zin[name])
    longest = vector_terms.shape[2]
    for s in range(shards):
        vector_terms[s, :, 0:rows] = vector_rows[:, s * rows : (s + 1) * rows]
        vector_terms[s, WIDE : WIDE + 1, :] = inner_row[:, s * longest : (s + 1) * longest]
    greet(True)

    outputs = remote(output_term.at[:, :, theirs], odd, osend, orecv, core_peer)
    outputs.start()
    send_far("vec")
    send_own("vec")
    for i in range(size_z):
        loads["inner", i].wait()
    inner_moves = []
    for j in range(1, size_x):
        total = inner_buf[0, columns[j]].astype(high)
        for i in range(1, size_z):
            total = total + inner_buf[i, columns[j]].astype(high)
        inner_send[j - 1] = total.astype(low)
        move = x_move("inner", 0, 0, j, inner_send.at[j - 1], xin["inner"].at[j - 1, 0])
        move.start()
        inner_moves.append(move)
    for i in range(size_x):
        loads["outer", i].wait()
    step_z("outer", 1)

    strip = 256

    def product(first):
        at = pl.ds(pl.multiple_of(first, strip), strip)
        return dot_nt(grads[at, :], weights[...])

    def token_rows(first):
        def other_strip(i, _):
            at = pl.ds(pl.multiple_of(first + i * strip, strip), strip)
            other_rows[at, :] = product(local + first + i * strip).astype(low)
            return 0

        def own_strip(i, _):
            at = pl.ds(pl.multiple_of(first + i * strip, strip), strip)
            base[at, :] = base[at, :] + product(first + i * strip)
            return 0

        lax.fori_loop(0, part // strip, other_strip, 0)
        span = pl.ds(first, part)
        move = remote(other_rows.at[span, :], recv_rows.at[span, :], tsend.at[first // part], trecv.at[first // part], core_peer)
        move.start()
        lax.fori_loop(0, part // strip, own_strip, 0)
        return move

    for name in ("grads", "weights", "base"):
        loads[name].wait()
    halves = token_rows(part)
    halves.wait()
    send_rows[...] = (base[part:local, :] + recv_rows[part:local, :].astype(high)).astype(low)
    back = remote(send_rows, far_rows, tsend.at[2], trecv.at[2], y_peer)
    back.start()

    step_z("outer", 2)
    loads["inputs"].wait()
    for b in range(4):
        turned[:, b * part : (b + 1) * part] = inputs[b * part : (b + 1) * part, :].T
    group = 4
    for p in range(pairs):
        block = slice(p * 384, (p + 1) * 384)
        where = slice(p % 2 * 384, p % 2 * 384 + 384)
        goal = terms_a if p < 2 else terms_b

        def some(m, _):
            value = dot_nn(turned[pl.ds(pl.multiple_of(m * group * rows, group * rows), group * rows), :], grads[:, block])
            goal[pl.ds(m * group, group), :, where] = value.reshape(group, rows, 384).astype(low)
            return 0

        lax.fori_loop(0, shards // group, some, 0)
        if p == 1:
            send_far("qa")
    outputs.wait()
    terms_b[:, :, half : 2 * half] = (odd[...].astype(high) + output_term[:, :, mine].astype(high)).astype(low)
    send_far("qb")
    send_own("qa")
    send_own("qb")
    total = inner_buf[0, x].astype(high)
    for i in range(1, size_z):
        total = total + inner_buf[i, x].astype(high)
    for j in range(1, size_x):
        inner_moves[j - 1].wait()
        total = total + xin["inner"][j - 1, 0].astype(high)
    ybuf["inner"][0] = total.astype(low)
    step_y("inner")
    for t in range(3, size_z):
        step_z("outer", t)
    step_z("vec", 1)
    step_z("qa", 1)
    halves = token_rows(0)
    step_z("vec", 2)
    step_z("qa", 2)
    finish_z("outer")
    for t in range(3, size_z):
        step_z("vec", t)
        step_z("qa", t)
    step_z("qb", 1)
    halves.wait()
    token_grads[y] = base[0:part, :] + recv_rows[0:part, :].astype(high)
    step_core("inner")
    step_z("qb", 2)
    for t in range(3, size_z):
        step_z("qb", t)
    finish_z("qa")
    finish_z("vec")
    step_core("outer")
    back.wait()
    token_grads[1 - y] = far_rows[...].astype(high)
    chunks = hidden // CHUNK
    buf = finish_core("inner")
    for i in range(2):
        owner = core if i == 0 else 1 - core
        for c in range(chunks):
            place = pl.ds(pl.multiple_of(c * CHUNK + owner * half, 128), half)
            grad_inner[:, place] = buf[i, :, c * half : (c + 1) * half]
    buf = finish_core("outer")
    for i in range(2):
        owner = core if i == 0 else 1 - core
        grad_outer[:, pl.ds(pl.multiple_of(owner * half, 128), half)] = buf[i]
    finish_z("qb")
    step_core("vec")
    step_core("qa")

    def spread(name):
        buf = finish_core(name)
        for i in range(2):
            owner = core if i == 0 else 1 - core
            for p in (0, 1) if name == "qa" else (2,):
                place = pl.ds(pl.multiple_of(owner * half + p * 128, 128), 128)
                for n, out in enumerate((grad_query, grad_key, grad_value)):
                    at = (3 * (p % 2) + n) * 128
                    out[:, place] = buf[i, :, at : at + 128]
            if name == "qb":
                grad_output[:, pl.ds(pl.multiple_of(owner * half, 128), half)] = buf[i, :, half : 2 * half]

    for name in zout:
        for t, way in steps:

            @pl.when(inside(target_of(t, way)))
            def _():
                z_move(name, t, way).wait_send()

    buf = finish_core("vec")
    vector_sums[...] = buf[0] + buf[1]
    spread("qa")
    step_core("qb")
    spread("qb")


def deliver_kernel(count, mixed_mine, mixed_far, *refs):
    matrices, vectors, mixed = refs[:count], refs[count], refs[count + 1]
    outs = refs[count + 2 : 2 * count + 2]
    smalls = refs[2 * count + 2 : -4]
    stage, in_sem, out_sem = refs[-4:-2], refs[-2], refs[-1]
    y = lax.axis_index("y")
    loads = [pltpu.make_async_copy(src, stage[i], in_sem.at[i]) for i, src in enumerate((mixed_mine, mixed_far))]
    copies = [pltpu.make_async_copy(src, dst, out_sem.at[i]) for i, (src, dst) in enumerate(zip(matrices, outs))]
    for copy in loads + copies:
        copy.start()
    for i, small in enumerate(smalls):
        small[...] = vectors[i : i + 1, 0 : small.shape[0]].reshape(small.shape)
    for i, place in enumerate((y, 1 - y)):
        loads[i].wait()
        copies.append(pltpu.make_async_copy(stage[i], mixed.at[place], out_sem.at[count + i]))
        copies[-1].start()
    for copy in copies:
        copy.wait()


def deliver(mixed_mine, mixed_far, matrices, vectors, sizes):
    count = len(matrices)
    vmem, anywhere = pl.BlockSpec(memory_space=pltpu.VMEM), pl.BlockSpec(memory_space=pl.ANY)
    return pl.pallas_call(
        lambda *refs: deliver_kernel(count, *refs),
        out_shape=(jax.ShapeDtypeStruct((2,) + mixed_mine.shape, mixed_mine.dtype),)
        + tuple(jax.ShapeDtypeStruct(m.shape, m.dtype) for m in matrices)
        + tuple(jax.ShapeDtypeStruct((size,), jnp.float32) for size in sizes),
        in_specs=[anywhere] * 2 + [vmem] * (count + 1),
        out_specs=(anywhere,) * (count + 1) + (vmem,) * len(sizes),
        scratch_shapes=[pltpu.VMEM(mixed_mine.shape, mixed_mine.dtype)] * 2
        + [pltpu.SemaphoreType.DMA((2,)), pltpu.SemaphoreType.DMA((count + 2,))],
        compiler_params=pltpu.CompilerParams(vmem_limit_bytes=40_000_000),
        name="deliver",
    )(mixed_mine, mixed_far, *matrices, vectors)


def exit_call(size_z, size_x, grads, inputs, weights, base, output_term, dense_sums, inner_sums, head_sums, inner_terms, outer_terms):
    shards, rows, width = output_term.shape
    lanes = grads.shape[1]
    half = width // 2
    pairs = half // 128
    length = inputs.shape[0]
    local = length // 2
    part = local // 2
    long = outer_terms[0].shape[1]
    hidden = 2 * inner_terms[0].shape[2]
    vmem, anywhere = pl.BlockSpec(memory_space=pltpu.VMEM), pl.BlockSpec(memory_space=pl.ANY)
    dma = pltpu.SemaphoreType.DMA
    side = size_x - 1
    full = lanes + half
    low, high = jnp.bfloat16, jnp.float32
    vector_shape = (16, hidden // shards)
    shapes = {
        "vec": (vector_shape, high, 1),
        "qa": ((rows, width), low, 1),
        "qb": ((rows, width), low, 1),
        "inner": ((rows, hidden // 2), low, 1),
        "outer": ((long, half), low, 1),
    }
    matrix = jax.ShapeDtypeStruct((rows, width), high)
    results = (
        jax.ShapeDtypeStruct((2, part, width), high),
        matrix,
        matrix,
        matrix,
        matrix,
        jax.ShapeDtypeStruct((rows, hidden), high),
        jax.ShapeDtypeStruct((long, width), high),
        jax.ShapeDtypeStruct(vector_shape, high),
    )
    scratch = [
        pltpu.VMEM((length, lanes), low),
        pltpu.VMEM((length, width), low),
        pltpu.VMEM((width, length), low),
        pltpu.VMEM((width, lanes), low),
        pltpu.VMEM((local, width), high),
        pltpu.VMEM((shards, rows, width), low),
        pltpu.VMEM((shards, rows, width), low),
        pltpu.VMEM((local, width), low),
        pltpu.VMEM((local, width), low),
        pltpu.VMEM((part, width), low),
        pltpu.VMEM((part, width), low),
        pltpu.VMEM((shards, rows, half), low),
        pltpu.VMEM((size_z,) + inner_terms[0].shape, low),
        pltpu.VMEM((size_x,) + outer_terms[0].shape, low),
        pltpu.VMEM((16, width), high),
        pltpu.VMEM((shards,) + vector_shape, high),
        pltpu.VMEM((side, rows, hidden // 2), low),
        dma((size_z + size_x + 4,)),
        dma((3,)),
        dma((3,)),
        dma,
        dma,
    ]
    for name, (shape, kind, sends) in shapes.items():
        scratch += [pltpu.VMEM((2,) + shape, kind), dma, dma, pltpu.VMEM((2,) + shape, high), dma, dma]
        stages = 1 if name == "inner" else size_z
        if name != "outer":
            scratch += [pltpu.VMEM((side, stages) + shape, kind), dma((sends, stages, side)), dma((sends, stages, side))]
        if name != "inner":
            scratch += [pltpu.VMEM((2, size_z - 1) + shape, kind)] * 2 + [dma((2, size_z - 1))] * 2
    return pl.pallas_call(
        lambda *refs: exit_kernel(size_z, size_x, shapes, *refs),
        out_shape=tuple(pltpu.VMEM(r.shape, r.dtype) for r in results),
        in_specs=[anywhere] * 4 + [vmem] * 4 + [anywhere] * (size_z + size_x),
        out_specs=(vmem,) * len(results),
        scratch_shapes=scratch,
        compiler_params=pltpu.CompilerParams(collective_id=1, has_side_effects=True, vmem_limit_bytes=56_000_000),
        name="exit",
    )(grads, inputs, weights, base, output_term, dense_sums, inner_sums, head_sums, *inner_terms, *outer_terms)


TILE = 256
CHUNK = 768


def dot_nt(a, b):
    return lax.dot_general(a, b, (((1,), (1,)), ((), ())), preferred_element_type=jnp.float32)


def row_mean(value):
    return jnp.sum(value, axis=-1, keepdims=True) * (1.0 / value.shape[-1])


def standardize(hidden):
    centred = hidden - row_mean(hidden)
    reciprocal = lax.rsqrt(row_mean(centred * centred) + EPS)
    return centred * reciprocal, reciprocal


def column_sum(value):
    return jnp.sum(value.reshape(value.shape[0] // 8, 8, value.shape[1]), axis=0)


def dense_kernel(
    size_z,
    size_x,
    tokens_ref,
    mine_ref,
    other_hbm,
    cot_hbm,
    cot_far_hbm,
    vectors_ref,
    bias_inner_ref,
    *refs,
):
    inner_parts, outer_parts = refs[:size_x], refs[size_x : size_x + size_z]
    refs = refs[size_x + size_z :]
    mixed_ref, mixed_send_ref, pre_first_ref, grad_mine_ref, grad_far_hbm, sums_ref, inner_sum_ref, grad_output_ref = refs[:8]
    inner_terms = refs[8 : 8 + size_z]
    outer_terms = refs[8 + size_z : 8 + size_z + size_x]
    refs = refs[8 + size_z + size_x :]
    w_output, w_inner, w_outer, a_output, a_inner, a_outer, grad_out_buf = refs[:7]
    context, first_low, turned_low, normed, first, slope, active, work = refs[7:15]
    send_inner, send_outer, recv_inner, recv_outer = refs[15:19]
    far_rows, grad_send, ready, cotangent, cot_sem, swap_send, swap_recv = refs[19:26]
    load_sem, share_send, share_recv, send_sem, recv_sem, store_sem = refs[26:]
    step, steps = pl.program_id(0), pl.num_programs(0)
    core_here = lax.axis_index("core")
    width, hidden = w_inner.shape
    half = width // 2
    chunks = hidden // CHUNK
    shards = size_z * size_x
    z, x, y, _ = place_of()
    twin = partner(core=1 - lax.axis_index("core"))
    near = cotangent.shape[0] // 2
    cot_loads = (
        pltpu.make_async_copy(cot_hbm.at[y], cotangent.at[pl.ds(0, near), :], cot_sem.at[0]),
        pltpu.make_async_copy(cot_far_hbm, cotangent.at[pl.ds(near, near), :], cot_sem.at[1]),
    )

    shard = width // shards
    long = hidden // shards
    group = CHUNK // long // size_x

    def columns_of(first, owner):
        return pl.ds(pl.multiple_of(first + owner * half, 128), half)

    def start_piece(i, src, dst):
        pltpu.make_async_copy(src, dst, load_sem.at[i]).start()
        remote(src, dst, share_send.at[i], share_recv.at[i], twin).start()

    def start_rows(i, lane, ref, first):
        for j in range(size_x):
            for at in range(size_z):
                slot = at * size_x + lax.rem(x - j + size_x, size_x)
                rows = pl.ds(pl.multiple_of(slot * shard, shard), shard)
                start_piece(i, inner_parts[j].at[at, :, pl.ds(lane, half)], ref.at[rows, columns_of(first, core_here)])

    def start_loads():
        start_rows(0, hidden // 2, w_output, 0)
        for c in range(chunks):
            start_rows(1 + 2 * c, c * half, w_inner, c * CHUNK)
            for at in range(c * group, (c + 1) * group):
                for k in range(size_z):

                    @pl.when(lax.rem(z - k + size_z, size_z) == at)
                    def _():
                        for column in range(size_x):
                            rows = pl.ds((at * size_x + column) * long, long)
                            start_piece(2 + 2 * c, outer_parts[k].at[column], w_outer.at[rows, columns_of(0, core_here)])

    def wait_load(i, ref, rows, first):
        own, far = ref.at[rows, columns_of(first, core_here)], ref.at[rows, columns_of(first, 1 - core_here)]
        pltpu.make_async_copy(own, own, load_sem.at[i]).wait()
        remote(own, far, share_send.at[i], share_recv.at[i], twin).wait()

    @pl.when(step == 0)
    def _():
        barrier = pltpu.get_barrier_semaphore()
        pl.semaphore_signal(barrier, inc=1, device_id=twin, device_id_type=MESH_ID)
        pl.semaphore_wait(barrier, 1)
        remote(other_hbm, far_rows, swap_send.at[0], swap_recv.at[0], twin).start()
        start_loads()
        for load in cot_loads:
            load.start()
        a_output[...] = jnp.zeros_like(a_output)
        a_inner[...] = jnp.zeros_like(a_inner)
        a_outer[...] = jnp.zeros_like(a_outer)
        sums_ref[...] = jnp.zeros_like(sums_ref)
        inner_sum_ref[...] = jnp.zeros_like(inner_sum_ref)

    def vector(i):
        row = (2, 3, 4, 6, 7, 8)[i]
        return vectors_ref[row : row + 1, :]

    def add_sum(i, value):
        sums_ref[8 * i : 8 * i + 8, :] += column_sum(value)

    context[:, pl.ds(pl.multiple_of(core_here * half, 128), half)] = mine_ref[...]

    context_move = remote(other_hbm, far_rows, swap_send.at[0], swap_recv.at[0], twin)

    @pl.when(step == 0)
    def _():
        context_move.wait()

    here = pl.ds(pl.multiple_of(step * TILE, TILE), TILE)
    context[:, pl.ds(pl.multiple_of((1 - core_here) * half, 128), half)] = far_rows[here, :]

    @pl.when(step == 0)
    def _():
        wait_load(0, w_output, slice(None), 0)

    hidden_rows = tokens_ref[...].astype(jnp.float32) + (dot_nn(context[...], w_output[...]) + vector(0))
    normed[...], first_recip = standardize(hidden_rows)
    first[...] = normed[...] * vector(1) + vector(2)
    first_low[...] = first[...].astype(jnp.bfloat16)
    turned_low[...] = first_low[...].T
    work[...] = jnp.broadcast_to(vector(3), work.shape)

    def part(c):
        return pl.ds(c * CHUNK, CHUNK)

    def exchange(c):
        return (
            remote(send_inner.at[c], recv_inner.at[c], send_sem.at[0, c], recv_sem.at[0, c], twin),
            remote(send_outer.at[c], recv_outer.at[c], send_sem.at[1, c], recv_sem.at[1, c], twin),
        )

    def wait_inner(c):
        @pl.when(step == 0)
        def _():
            wait_load(1 + 2 * c, w_inner, slice(None), c * CHUNK)

    def ahead(c):
        ready[c % 2] = dot_nn(first_low[...], w_inner[:, part(c)])

    wait_inner(0)
    ahead(0)
    for c in range(chunks):
        if c + 1 < chunks:
            wait_inner(c + 1)

        @pl.when(step == 0)
        def _():
            wait_load(2 + 2 * c, w_outer, part(c), 0)

        if c + 1 < chunks:
            ahead(c + 1)
        u = ready[c % 2] + bias_inner_ref[0:1, part(c)]
        cdf = 0.5 * (1.0 + lax.erf(u * ROOT_HALF))
        slope[:, part(c)] = cdf + u * jnp.exp(-0.5 * u * u) * INV_ROOT_TAU
        acted = (u * cdf).astype(jnp.bfloat16)
        active[:, part(c)] = acted
        work[...] += dot_nn(acted, w_outer[part(c), :])

    second, second_recip = standardize(first[...] + work[...])
    mixed = (second * vector(4) + vector(5)).astype(jnp.bfloat16)

    @pl.when(step < steps // 2)
    def _():
        mixed_ref[...] = mixed

    @pl.when(step >= steps // 2)
    def _():
        mixed_send_ref[...] = mixed


    @pl.when(step == 0)
    def _():
        for load in cot_loads:
            load.wait()

    upstream = cotangent[pl.ds(pl.multiple_of(step * TILE, TILE), TILE), :].astype(jnp.float32)
    add_sum(0, upstream * second)
    add_sum(1, upstream)
    scaled = upstream * vector(4)
    pre_second = second_recip * (scaled - row_mean(scaled) - second * row_mean(scaled * second))
    grad_outer = pre_second.astype(jnp.bfloat16)
    add_sum(2, grad_outer.astype(jnp.float32))
    work[...] = pre_second
    grad_out_buf[...] = grad_outer

    def behind(c):
        ready[c % 2] = dot_nt(grad_out_buf[...], w_outer[part(c), :])

    behind(0)
    for c in range(chunks):
        if c + 1 < chunks:
            behind(c + 1)
        grad_inner = (ready[c % 2] * slope[:, part(c)]).astype(jnp.bfloat16)
        inner_sum_ref[:, part(c)] += column_sum(grad_inner.astype(jnp.float32))
        a_outer[part(c), :] += dot_nn(active[:, part(c)].T, grad_out_buf[...])
        a_inner[:, part(c)] += dot_nn(turned_low[...], grad_inner)
        work[...] += dot_nt(grad_inner, w_inner[:, part(c)])

        @pl.when(step == steps - 1)
        def _():
            theirs = pl.multiple_of(c * CHUNK + (1 - core_here) * half, 128)
            send_inner[c] = a_inner[:, pl.ds(theirs, half)].astype(jnp.bfloat16)
            send_outer[c] = a_outer[part(c), pl.ds(pl.multiple_of((1 - core_here) * half, 128), half)].astype(jnp.bfloat16)
            for move in exchange(c):
                move.start()

    grad_first = work[...]
    add_sum(3, grad_first * normed[...])
    add_sum(4, grad_first)
    scaled = grad_first * vector(1)
    pre_first = first_recip * (scaled - row_mean(scaled) - normed[...] * row_mean(scaled * normed[...]))
    pre_first_ref[...] = pre_first
    grad_attended = pre_first.astype(jnp.bfloat16)
    add_sum(5, grad_attended.astype(jnp.float32))
    a_output[...] += dot_nn(context[...].T, grad_attended)
    context[...] = dot_nt(grad_attended, w_output[...]).astype(jnp.bfloat16)
    grad_mine_ref[...] = context[:, pl.ds(pl.multiple_of(core_here * half, 128), half)]

    def grad_move(t):
        rows = pl.ds(pl.multiple_of(t * TILE, TILE), TILE)
        return remote(grad_send.at[t], grad_far_hbm.at[rows, :], swap_send.at[1 + t], swap_recv.at[1 + t], twin)

    grad_send[step] = context[:, pl.ds(pl.multiple_of((1 - core_here) * half, 128), half)]
    grad_move(step).start()

    @pl.when(step == steps - 1)
    def _():
        grad_output_ref[...] = a_output[...].astype(jnp.bfloat16)

        def inner_out(c):
            copies = []
            for k in range(size_z):
                for column in range(size_x):
                    slot = lax.rem(z + k, size_z) * size_x + column
                    src = send_inner.at[c, pl.ds(pl.multiple_of(slot * shard, shard), shard), :]
                    copies.append(
                        pltpu.make_async_copy(src, inner_terms[k].at[column, :, pl.ds(c * half, half)], store_sem.at[0, c])
                    )
            return copies

        def outer_out(c):
            copies = []
            for i in range(group):
                for j in range(size_x):
                    src = send_outer.at[c, pl.ds(pl.multiple_of((i * size_x + lax.rem(x + j, size_x)) * long, long), long), :]
                    copies.append(pltpu.make_async_copy(src, outer_terms[j].at[c * group + i], store_sem.at[1, c]))
            return copies

        for c in range(chunks):
            ours = pl.multiple_of(c * CHUNK + core_here * half, 128)
            first_move, second_move = exchange(c)
            first_move.wait()
            send_inner[c] = (a_inner[:, pl.ds(ours, half)] + recv_inner[c].astype(jnp.float32)).astype(jnp.bfloat16)
            for copy in inner_out(c):
                copy.start()
            second_move.wait()
            columns = pl.ds(pl.multiple_of(core_here * half, 128), half)
            send_outer[c] = (a_outer[part(c), columns] + recv_outer[c].astype(jnp.float32)).astype(jnp.bfloat16)
            for copy in outer_out(c):
                copy.start()
        for t in range(grad_send.shape[0]):
            grad_move(t).wait()
        for c in range(chunks):
            pltpu.make_async_copy(send_inner.at[c], send_inner.at[c], store_sem.at[0, c]).wait()
            pltpu.make_async_copy(send_outer.at[c], send_outer.at[c], store_sem.at[1, c]).wait()


def dense_layer(size_z, size_x, tokens, mine, other, cotangent, cotangent_far, vectors, bias_inner, inner_parts, outer_parts):
    local, half = mine.shape
    width = 2 * half
    hidden = bias_inner.shape[1]
    steps = local // TILE
    shards = size_z * size_x
    chunks = hidden // CHUNK
    low, high = jnp.bfloat16, jnp.float32
    tile = pl.BlockSpec((TILE, width), lambda t, *_: (t, 0))
    half_tile = pl.BlockSpec((TILE, half), lambda t, *_: (t, 0))
    anywhere = pl.BlockSpec(memory_space=pl.ANY)

    def whole(shape):
        return pl.BlockSpec(shape, lambda t, *_: (0, 0))

    inner_shape = jax.ShapeDtypeStruct((size_x, width // shards, hidden // 2), low)
    outer_shape = jax.ShapeDtypeStruct((size_z, hidden // shards, half), low)
    halves = pltpu.VMEM((chunks, width, half), low)
    dma = pltpu.SemaphoreType.DMA
    return pl.pallas_call(
        lambda *refs: dense_kernel(size_z, size_x, *refs),
        out_shape=(
            jax.ShapeDtypeStruct((local // 2, width), low),
            jax.ShapeDtypeStruct((local // 2, width), low),
            jax.ShapeDtypeStruct((local, width), high),
            jax.ShapeDtypeStruct((local, half), low),
            jax.ShapeDtypeStruct((local, half), low),
            jax.ShapeDtypeStruct((48, width), high),
            jax.ShapeDtypeStruct((8, hidden), high),
            jax.ShapeDtypeStruct((width, width), low),
        )
        + (inner_shape,) * size_z
        + (outer_shape,) * size_x,
        grid_spec=pltpu.PrefetchScalarGridSpec(
            num_scalar_prefetch=0,
            grid=(steps,),
            in_specs=[
                tile,
                half_tile,
                anywhere,
                anywhere,
                anywhere,
                whole((16, width)),
                whole((1, hidden)),
            ]
            + [anywhere] * (size_x + size_z),
            out_specs=[
                pl.BlockSpec((TILE, width), lambda t: (jnp.minimum(t, steps // 2 - 1), 0)),
                pl.BlockSpec((TILE, width), lambda t: (jnp.maximum(t - steps // 2, 0), 0)),
                tile,
                half_tile,
                anywhere,
                whole((48, width)),
                whole((8, hidden)),
                whole((width, width)),
            ]
            + [anywhere] * (size_z + size_x),
            scratch_shapes=[
                pltpu.VMEM((width, width), low),
                pltpu.VMEM((width, hidden), low),
                pltpu.VMEM((hidden, width), low),
                pltpu.VMEM((width, width), high),
                pltpu.VMEM((width, hidden), high),
                pltpu.VMEM((hidden, width), high),
                pltpu.VMEM((TILE, width), low),
                pltpu.VMEM((TILE, width), low),
                pltpu.VMEM((TILE, width), low),
                pltpu.VMEM((width, TILE), low),
                pltpu.VMEM((TILE, width), high),
                pltpu.VMEM((TILE, width), high),
                pltpu.VMEM((TILE, hidden), high),
                pltpu.VMEM((TILE, hidden), low),
                pltpu.VMEM((TILE, width), high),
                halves,
                halves,
                halves,
                halves,
                pltpu.VMEM((local, half), low),
                pltpu.VMEM((steps, TILE, half), low),
                pltpu.VMEM((2, TILE, CHUNK), high),
                pltpu.VMEM((local, width), low),
                dma((2,)),
                dma((1 + steps,)),
                dma((1 + steps,)),
                dma((1 + 2 * chunks,)),
                dma((1 + 2 * chunks,)),
                dma((1 + 2 * chunks,)),
                dma((2, chunks)),
                dma((2, chunks)),
                dma((2, chunks)),
            ],
        ),
        compiler_params=pltpu.CompilerParams(
            dimension_semantics=("arbitrary",), vmem_limit_bytes=67_000_000, collective_id=3, has_side_effects=True
        ),
        cost_estimate=pl.CostEstimate(flops=32_000_000_000, bytes_accessed=40_000_000, transcendentals=6_000_000),
        name="dense_layer",
    )(tokens, mine, other, cotangent, cotangent_far, vectors, bias_inner, *inner_parts, *outer_parts)


def lowered(piece):
    return piece.astype(jnp.bfloat16)


def widen(piece):
    return piece.astype(jnp.float32)


def matmul(left, right):
    return jnp.dot(left, right, preferred_element_type=jnp.float32)


def matmul_tn(left, right):
    return lax.dot_general(
        left, right, (((0,), (0,)), ((), ())), preferred_element_type=jnp.float32
    )


def matmul_nt(left, right):
    return lax.dot_general(
        left, right, (((1,), (1,)), ((), ())), preferred_element_type=jnp.float32
    )


def normalize(hidden, norm_gain, norm_shift):
    centred = hidden - jnp.mean(hidden, axis=-1, keepdims=True)
    reciprocal = lax.rsqrt(jnp.mean(centred * centred, axis=-1, keepdims=True) + EPS)
    normed = centred * reciprocal
    return (normed * norm_gain + norm_shift, normed, reciprocal)


def normalize_back(upstream, normed, reciprocal, norm_gain):
    scaled = upstream * norm_gain
    result = reciprocal * (
        scaled
        - jnp.mean(scaled, axis=-1, keepdims=True)
        - normed * jnp.mean(scaled * normed, axis=-1, keepdims=True)
    )
    return (result, jnp.sum(upstream * normed, axis=0), jnp.sum(upstream, axis=0))


def gelu_value(values_in):
    return 0.5 * values_in * (1.0 + lax.erf(values_in * ROOT_HALF))


def gelu_slope(values_in):
    return (
        0.5 * (1.0 + lax.erf(values_in * ROOT_HALF))
        + values_in * jnp.exp(-0.5 * values_in * values_in) * INV_ROOT_TAU
    )


def shift(piece, axis, step):
    size = lax.axis_size(axis)
    return lax.ppermute(piece, axis, [(i, (i + step) % size) for i in range(size)])


def swap(piece, axis):
    return lax.ppermute(piece, axis, [(0, 1), (1, 0)])


def pick(piece, index, axis=0):
    return lax.dynamic_index_in_dim(piece, index, axis, keepdims=False)


def in_order(first_is_zero, own, other, axis):
    return jnp.where(
        first_is_zero,
        jnp.concatenate([own, other], axis),
        jnp.concatenate([other, own], axis),
    )


def collect(piece):
    size_z, size_x = lax.axis_size("z"), lax.axis_size("x")
    z, x = lax.axis_index("z"), lax.axis_index("x")
    along_z = [piece] + [shift(piece, "z", k) for k in range(1, size_z)]
    whole = jnp.zeros((size_z, size_x) + piece.shape, piece.dtype)
    zeros = (0,) * piece.ndim
    for j in range(size_x):
        for k in range(size_z):
            arrived = along_z[k] if j == 0 else shift(along_z[k], "x", j)
            place = ((z - k) % size_z, (x - j) % size_x) + zeros
            whole = lax.dynamic_update_slice(whole, arrived[None, None], place)
    return whole.reshape((size_z * size_x,) + piece.shape)


def reduce_owned(terms):
    size_z, size_x = lax.axis_size("z"), lax.axis_size("x")
    z, x = lax.axis_index("z"), lax.axis_index("x")
    terms = terms.reshape((size_z, size_x) + terms.shape[1:])
    total = widen(pick(terms, x, 1))
    for j in range(1, size_x):
        total = total + widen(shift(pick(terms, (x + j) % size_x, 1), "x", j))
    terms = lowered(total)
    total = widen(pick(terms, z))
    for k in range(1, size_z):
        total = total + widen(shift(pick(terms, (z + k) % size_z), "z", k))
    terms = lowered(total)
    return widen(terms) + widen(swap(terms, "y"))


def plain_body(
    tokens,
    segment_ids,
    w_query,
    w_key,
    w_value,
    w_output,
    b_query,
    b_value,
    b_output,
    first_gain,
    first_shift,
    w_inner,
    b_inner,
    w_outer,
    b_outer,
    second_gain,
    second_shift,
    cotangent,
):
    core, y = lax.axis_index("core"), lax.axis_index("y")
    shards = lax.axis_size("z") * lax.axis_size("x")
    sequences, part, width = tokens.shape
    half = width // 2
    pairs = half // 128
    hidden = w_inner.shape[1]
    local = 2 * part
    own_rows = w_query.shape[0]
    unit_half = hidden // shards // 2

    def columns(matrix):
        return lowered(lax.dynamic_slice_in_dim(matrix, core * half, half, 1))

    vectors = (b_query, b_value, b_output, first_gain, first_shift, b_inner, b_outer, second_gain, second_shift)
    flat = jnp.concatenate([lowered(v) for v in vectors])
    lanes = 3 * half
    extra = -(-flat.shape[0] // lanes)
    flat = jnp.pad(flat, (0, extra * lanes - flat.shape[0])).reshape(extra, lanes)
    weights = jnp.stack([columns(w).reshape(own_rows, pairs, 128) for w in (w_query, w_key, w_value)], axis=2)
    early = collect(jnp.concatenate([weights.reshape(own_rows, lanes), flat], axis=0))

    mine = pick(tokens, y)
    arrived = swap(pick(tokens, 1 - y), "y")
    mine_other, arrived_other = swap(mine, "core"), swap(arrived, "core")
    inputs_all = jnp.concatenate([mine, arrived, mine_other, arrived_other], axis=0)
    inputs = jnp.concatenate([mine, arrived], axis=0)

    inner_piece = lowered(pick(w_inner.reshape(own_rows, shards, 2, unit_half), core, 2)).reshape(own_rows, hidden // 2)
    late = collect(jnp.concatenate([columns(w_output), inner_piece], axis=1)).reshape(width, half + hidden // 2)
    outer_own = collect(lowered(lax.dynamic_slice_in_dim(w_outer, core * unit_half, unit_half, 0))).reshape(hidden // 2, width)
    output_own, inner_own = late[:, :half], late[:, half:]
    output_other, inner_other, outer_other = swap(output_own, "core"), swap(inner_own, "core"), swap(outer_own, "core")
    full_output = in_order(core == 0, output_own, output_other, 1)
    cotangent_mine = pick(cotangent, y)
    cotangent_arrived = swap(pick(cotangent, 1 - y), "y")

    full_early = early[:, :own_rows].reshape(width, lanes)
    flat_all = early[:, own_rows:].reshape(shards, extra * lanes)
    sizes = [v.shape[0] for v in vectors]
    gathered, at = [], 0
    for size in sizes:
        gathered.append(flat_all[:, at : at + size].reshape(shards * size))
        at += size
    bias_query, bias_value, bias_output, gain_first, shift_first, bias_inner, bias_outer, gain_second, shift_second = [
        widen(v) for v in gathered
    ]
    biases = jnp.concatenate([bias_query[None], bias_value[None], jnp.zeros((14, width), jnp.float32)], axis=0)
    heads_mine, heads_other, logsum, projected = attention(segment_ids, inputs_all, full_early, biases)
    context = in_order(core == 0, heads_mine, swap(heads_other, "core"), 1)

    attended = matmul(context, full_output) + bias_output
    first, first_normed, first_recip = normalize(widen(inputs) + attended, gain_first, shift_first)
    first_low = lowered(first)
    biases = bias_inner.reshape(shards, 2, unit_half)
    halves = ((inner_own, outer_own, pick(biases, core, 1)), (inner_other, outer_other, pick(biases, 1 - core, 1)))
    outer, kept = bias_outer, []
    for inner_weight, outer_weight, bias in halves:
        inner = matmul(first_low, inner_weight) + bias.reshape(hidden // 2)
        active = lowered(gelu_value(inner))
        outer = outer + matmul(active, outer_weight)
        kept.append((inner, active))
    mixed, second_normed, second_recip = normalize(first + outer, gain_second, shift_second)
    mixed = lowered(mixed)

    upstream = widen(jnp.concatenate([cotangent_mine, cotangent_arrived], axis=0))
    pre_second, grad_second_gain, grad_second_shift = normalize_back(upstream, second_normed, second_recip, gain_second)
    grad_outer = lowered(pre_second)
    grad_b_outer = jnp.sum(widen(grad_outer), axis=0)
    grad_first, inner_grads, outer_grads, bias_grads = pre_second, [], [], []
    for (inner, active), (inner_weight, outer_weight, _) in zip(kept, halves):
        grad_inner = lowered(matmul_nt(grad_outer, outer_weight) * gelu_slope(inner))
        outer_grads.append(lowered(matmul_tn(active, grad_outer)))
        inner_grads.append(lowered(matmul_tn(first_low, grad_inner)))
        bias_grads.append(jnp.sum(widen(grad_inner), axis=0).reshape(shards, 1, unit_half))
        grad_first = grad_first + matmul_nt(grad_inner, inner_weight)
    grad_b_inner = in_order(core == 0, bias_grads[0], bias_grads[1], 1).reshape(hidden)
    pre_first, grad_first_gain, grad_first_shift = normalize_back(grad_first, first_normed, first_recip, gain_first)
    grad_attended = lowered(pre_first)
    grad_b_output = jnp.sum(widen(grad_attended), axis=0)
    grad_w_output = lowered(matmul_tn(context, grad_attended))
    grad_context = lowered(matmul_nt(grad_attended, full_output))
    context_mine = lax.dynamic_slice_in_dim(grad_context, core * half, half, 1)
    context_other = lax.dynamic_slice_in_dim(grad_context, (1 - core) * half, half, 1)
    upstream_other = swap(context_other, "core")

    def core_sum(own, other):
        return lowered(widen(own) + widen(swap(other, "core")))

    outer_term = core_sum(*outer_grads)
    inner_term = core_sum(*inner_grads)
    output_term = core_sum(
        lax.dynamic_slice_in_dim(grad_w_output, core * half, half, 1),
        lax.dynamic_slice_in_dim(grad_w_output, (1 - core) * half, half, 1),
    )
    outer_done = reduce_owned(outer_term.reshape(shards, unit_half, width))
    late_done = reduce_owned(jnp.concatenate([output_term, inner_term], axis=1).reshape(shards, own_rows, half + hidden // 2))

    grads, sums = attention_back(segment_ids, projected, heads_mine, heads_other, context_mine, upstream_other, logsum)
    grad_early = lowered(matmul_tn(inputs_all, grads))
    partial = matmul_nt(grads, full_early)
    sums = sums.reshape(pairs, 8, 3, 128)[:, 0]
    blank = jnp.zeros((width,), jnp.float32)
    grad_b_query = lax.dynamic_update_slice(blank, sums[:, 0].reshape(half), (core * half,))
    grad_b_value = lax.dynamic_update_slice(blank, sums[:, 2].reshape(half), (core * half,))
    vector_grads = (
        grad_b_query,
        grad_b_value,
        grad_b_output,
        grad_first_gain,
        grad_first_shift,
        grad_b_inner,
        grad_b_outer,
        grad_second_gain,
        grad_second_shift,
    )
    flat_grads = jnp.concatenate([v.reshape(shards, -1) for v in vector_grads], axis=1)
    flat_grads = jnp.pad(flat_grads, ((0, 0), (0, extra * lanes - flat_grads.shape[1])))
    early_term = jnp.concatenate(
        [grad_early.reshape(shards, own_rows, lanes), lowered(flat_grads).reshape(shards, extra, lanes)], axis=1
    )
    early_done = reduce_owned(early_term)

    grad_inputs = pre_first + partial[:local] + widen(swap(lowered(partial[local:]), "core"))
    returned = widen(swap(lowered(grad_inputs[part:]), "y"))
    grad_tokens = in_order(y == 0, grad_inputs[None, :part], returned[None], 0)
    mixed_out = in_order(y == 0, mixed[None, :part], swap(mixed[part:], "y")[None], 0)

    def both(piece):
        return widen(swap(lowered(piece), "core"))

    early_matrix = early_done[:own_rows]
    early_full = in_order(
        core == 0, early_matrix.reshape(own_rows, pairs, 3, 128)[None], both(early_matrix).reshape(own_rows, pairs, 3, 128)[None], 0
    )
    early_full = early_full.transpose(3, 1, 0, 2, 4).reshape(3, own_rows, width)
    late_other = both(late_done)
    output_full = in_order(core == 0, late_done[:, :half], late_other[:, :half], 1)
    inner_full = in_order(
        core == 0,
        late_done[:, half:].reshape(own_rows, shards, 1, unit_half),
        late_other[:, half:].reshape(own_rows, shards, 1, unit_half),
        2,
    ).reshape(own_rows, hidden)
    outer_full = in_order(core == 0, outer_done, both(outer_done), 0)
    vector_part = early_done[own_rows:]
    vector_sums = (vector_part + swap(vector_part, "core")).reshape(extra * lanes)
    out_vectors, at = [], 0
    for size in sizes:
        out_vectors.append(vector_sums[at : at + size])
        at += size
    (
        done_b_query,
        done_b_value,
        done_b_output,
        done_first_gain,
        done_first_shift,
        done_b_inner,
        done_b_outer,
        done_second_gain,
        done_second_shift,
    ) = out_vectors
    return (
        mixed_out,
        grad_tokens,
        early_full[0],
        early_full[1],
        early_full[2],
        output_full,
        done_b_query,
        done_b_value,
        done_b_output,
        done_first_gain,
        done_first_shift,
        inner_full,
        done_b_inner,
        outer_full,
        done_b_outer,
        done_second_gain,
        done_second_shift,
    )


def body(
    tokens,
    segment_ids,
    w_query,
    w_key,
    w_value,
    w_output,
    b_query,
    b_value,
    b_output,
    first_gain,
    first_shift,
    w_inner,
    b_inner,
    w_outer,
    b_outer,
    second_gain,
    second_shift,
    cotangent,
):
    core, y = lax.axis_index("core"), lax.axis_index("y")
    size_z, size_x = lax.axis_size("z"), lax.axis_size("x")
    shards = size_z * size_x
    sequences, part, width = tokens.shape
    half = width // 2
    pairs = half // 128
    hidden = w_inner.shape[1]
    local = 2 * part
    own_rows = w_query.shape[0]
    lanes = 3 * half

    vectors = (b_query, b_value, b_output, first_gain, first_shift, b_inner, b_outer, second_gain, second_shift)
    sizes = [v.shape[0] for v in vectors]
    tokens_all, cotangent_send, early, inner_own, outer_own, rows, inner_row = entry(
        size_z, size_x, tokens, cotangent, w_query, w_key, w_value, w_inner, w_output, w_outer, vectors
    )
    cotangent_far = swap(cotangent_send, "y")
    inner_parts = [inner_own] + [shift(inner_own, "x", j) for j in range(1, size_x)]
    outer_parts = [outer_own] + [shift(outer_own, "z", k) for k in range(1, size_z)]
    inputs_all = tokens_all.reshape(4 * part, width)
    full_early = early.reshape(width, lanes)
    context_mine, context_other, logsum, projected = attention(segment_ids, inputs_all, full_early, rows)
    made = dense_layer(
        size_z,
        size_x,
        inputs_all,
        context_mine,
        context_other,
        cotangent,
        cotangent_far,
        rows,
        inner_row,
        inner_parts,
        outer_parts,
    )
    mixed, mixed_send, pre_first, upstream_mine, upstream_other, dense_sums, inner_sums, grad_w_output = made[:8]
    inner_terms = [made[8]] + [shift(made[8 + k], "z", k) for k in range(1, size_z)]
    outer_terms = [made[8 + size_z]] + [shift(made[8 + size_z + j], "x", j) for j in range(1, size_x)]
    mixed_far = swap(mixed_send, "y")
    grads, sums = attention_back(segment_ids, projected, context_mine, context_other, upstream_mine, upstream_other, logsum)
    made = exit_call(
        size_z,
        size_x,
        grads,
        inputs_all,
        full_early,
        pre_first,
        grad_w_output.reshape(shards, own_rows, width),
        dense_sums,
        inner_sums,
        sums,
        inner_terms,
        outer_terms,
    )
    mixed_out, grad_tokens, grad_query, grad_key, grad_value, grad_output, grad_inner_full, grad_outer_full, *done = deliver(
        mixed, mixed_far, made[:7], made[7], sizes
    )
    return (
        mixed_out,
        grad_tokens,
        grad_query,
        grad_key,
        grad_value,
        grad_output,
        *done[:5],
        grad_inner_full,
        done[5],
        grad_outer_full,
        *done[6:],
    )


def layer(*arrays):
    if arrays[2].shape[0] % 32 == 0 and lax.axis_size("x") > 1:
        return body(*arrays)
    return plain_body(*arrays)


def solution(mesh):
    outer, inner = mesh.devices.shape
    size_z = 1
    while size_z * size_z < outer:
        size_z *= 2
    split = Mesh(mesh.devices.reshape(size_z, outer // size_z, inner // 2, 2), ("z", "x", "y", "core"))
    dp, seq = ("z", "x"), ("y", "core")
    activation, matrix, vector = P(dp, seq, None), P(dp, None), P(dp)
    return jax.shard_map(
        layer,
        mesh=split,
        in_specs=(
            activation,
            matrix,
            matrix,
            matrix,
            matrix,
            matrix,
            vector,
            vector,
            vector,
            vector,
            vector,
            matrix,
            vector,
            matrix,
            vector,
            vector,
            vector,
            activation,
        ),
        out_specs=(
            activation,
            activation,
            matrix,
            matrix,
            matrix,
            matrix,
            vector,
            vector,
            vector,
            vector,
            vector,
            matrix,
            vector,
            matrix,
            vector,
            vector,
            vector,
        ),
        check_vma=False,
    )
```

```python
import jax
import jax.numpy as jnp
from jax import lax
from jax.experimental import pallas as pl
from jax.experimental.pallas import tpu as pltpu
from jax.sharding import Mesh
from jax.sharding import PartitionSpec as P


HD = 64
EPS = 1e-12
ROOT_HALF = 0.7071067811865476
INV_ROOT_TAU = 0.3989422804014327

BLK = 256
BIG = -1.0e9
DOCUMENTS = 4


def dot_nn(a, b):
    return jnp.dot(a, b, preferred_element_type=jnp.float32)


def local_start(b, part):
    core, y = lax.axis_index("core"), lax.axis_index("y")
    return (jnp.where(b % 2 == core, 0, 2) + jnp.where(b // 2 == y, 0, 1)) * part


def part_rows(b, part):
    return pl.ds(pl.multiple_of(local_start(b, part), 128), part)


def find_bounds(segment_ref, bound_ref):
    length = segment_ref.shape[1]
    y = lax.axis_index("y")
    bound_ref[0] = 0
    bound_ref[DOCUMENTS] = length
    for d in range(1, DOCUMENTS):

        def halve(_, span):
            low, high = span
            middle = (low + high) // 2
            below = segment_ref[y, jnp.minimum(middle, length - 1)] < d
            inside = low < high
            return (
                jnp.where(jnp.logical_and(inside, below), middle + 1, low),
                jnp.where(jnp.logical_and(inside, jnp.logical_not(below)), middle, high),
            )

        low, _ = lax.fori_loop(0, length.bit_length(), halve, (0, length))
        bound_ref[d] = low


def find_window(segment_ref, bound_ref, qb):
    length = segment_ref.shape[1]
    y = lax.axis_index("y")
    first = segment_ref[y, qb * BLK]
    last = segment_ref[y, qb * BLK + BLK - 1]
    start = bound_ref[first] // 128 * 128
    count = (bound_ref[last + 1] - start + BLK - 1) // BLK
    return jnp.minimum(start, length - count * BLK), count


def each_tile(count, step):
    def two(i, _):
        step(i * (2 * BLK), 2 * BLK)
        return 0

    lax.fori_loop(0, count // 2, two, 0)

    @pl.when(count % 2 == 1)
    def _():
        step((count - 1) * BLK, BLK)


def make_marks(row_ref, mark_query, mark_key):
    length = mark_key.shape[0]
    y = lax.axis_index("y")
    step = 512
    for b in range(length // step):
        rows = slice(b * step, (b + 1) * step)
        column = jnp.broadcast_to(row_ref[pl.ds(y, 1), rows], (128, step)).T
        lane = lax.broadcasted_iota(jnp.int32, (step, 128), 1) % 64
        same = lane == column
        line = lax.broadcasted_iota(jnp.int32, (128, step), 0) % 64
        mark_query[:, rows] = jnp.where(line == row_ref[pl.ds(y, 1), rows], 1.0, 0.0).astype(jnp.bfloat16)
        apart = jnp.logical_and(lane < DOCUMENTS, jnp.logical_not(same))
        mark_key[rows, :] = jnp.where(apart, BIG, 0.0).astype(jnp.bfloat16)


def forward_kernel(segment_ref, row_ref, tokens_ref, weights_ref, bias_ref, *refs):
    mine_ref, other_ref, lse_ref, qkv_ref, q2, k2, vt, acc, top, tot, keep, mark_query, mark_key, bound_ref = refs
    length = qkv_ref.shape[0]
    blocks = length // BLK
    part = length // 4

    @pl.when(pl.program_id(0) == 0)
    def _():
        find_bounds(segment_ref, bound_ref)
        make_marks(row_ref, mark_query, mark_key)

    low = lax.broadcasted_iota(jnp.int32, (part, 128), 1) < 64
    for b in range(4):
        src = part_rows(b, part)
        dst = slice(b * part, (b + 1) * part)
        made = dot_nn(tokens_ref[src, :], weights_ref[...])
        lanes = pl.ds(pl.multiple_of(lax.axis_index("core") * (128 * pl.num_programs(0)) + pl.program_id(0) * 128, 128), 128)
        q = ((made[:, 0:128] + bias_ref[0:1, lanes]) * 0.125).astype(jnp.bfloat16)
        k = made[:, 128:256].astype(jnp.bfloat16)
        v = (made[:, 256:384] + bias_ref[1:2, lanes]).astype(jnp.bfloat16)
        qkv_ref[src, 0:128] = q
        qkv_ref[src, 128:256] = k
        qkv_ref[src, 256:384] = v
        nohk = mark_key[dst, :]
        turned = q.T
        q2[0, 0:64, dst] = turned[0:64]
        q2[0, 64:128, dst] = mark_query[64:128, dst]
        q2[1, 0:64, dst] = mark_query[0:64, dst]
        q2[1, 64:128, dst] = turned[64:128]
        k2[0, dst, :] = jnp.where(low, k, nohk)
        k2[1, dst, :] = jnp.where(low, nohk, k)
        vt[:, dst] = v.T
    lse_ref[...] = jnp.zeros_like(lse_ref)

    def row(qb, _):
        qs = pl.ds(pl.multiple_of(qb * BLK, BLK), BLK)
        start, count = find_window(segment_ref, bound_ref, qb)
        top[...] = jnp.full_like(top, -1.0e30)

        def fold(tile, function):
            return function(tile.reshape(tile.shape[0] // 8, 8, BLK), axis=0)

        def highest(first, size):
            keys = pl.ds(pl.multiple_of(start + first, 128), size)
            for h in range(2):
                st = dot_nn(k2[h, keys, :], q2[h, :, qs])
                keep[h, pl.ds(pl.multiple_of(first, BLK), size), :] = st
                top[h] = jnp.maximum(top[h], fold(st, jnp.max))

        def weigh(first, size, largest):
            keys = pl.ds(pl.multiple_of(start + first, 128), size)
            for h in range(2):
                rows = slice(64 * h, 64 * h + 64)
                st = keep[h, pl.ds(pl.multiple_of(first, BLK), size), :]
                p = jnp.exp(st - largest[h])
                tot[h] = tot[h] + fold(p, jnp.sum)
                acc[rows, :] = acc[rows, :] + dot_nn(vt[rows, keys], p.astype(jnp.bfloat16))

        def paired(step):
            each_tile(count, step)

        paired(highest)
        largest = [jnp.max(top[h], axis=0, keepdims=True) for h in range(2)]
        acc[...] = jnp.zeros_like(acc)
        tot[...] = jnp.zeros_like(tot)
        paired(lambda first, size: weigh(first, size, largest))
        for h in range(2):
            rows = slice(64 * h, 64 * h + 64)
            total = jnp.sum(tot[h], axis=0, keepdims=True)
            acc[rows, :] = acc[rows, :] / total
            lse_ref[h : h + 1, qs] = largest[h] + jnp.log(total)
        where = local_start(qb * BLK // part, part) + qb * BLK % part
        result = acc[...].T.astype(jnp.bfloat16)

        @pl.when(where < 2 * part)
        def _():
            mine_ref[pl.ds(pl.multiple_of(where, BLK), BLK), :] = result

        @pl.when(where >= 2 * part)
        def _():
            other_ref[pl.ds(pl.multiple_of(where - 2 * part, BLK), BLK), :] = result

        return 0

    lax.fori_loop(0, blocks, row, 0)


def attention(segments, tokens, weights, biases):
    length, depth = tokens.shape
    width = weights.shape[1]
    pairs = width // 384
    rows = length // 2
    return pl.pallas_call(
        forward_kernel,
        out_shape=(
            jax.ShapeDtypeStruct((rows, pairs * 128), jnp.bfloat16),
            jax.ShapeDtypeStruct((rows, pairs * 128), jnp.bfloat16),
            jax.ShapeDtypeStruct((pairs * 8, length), jnp.float32),
            jax.ShapeDtypeStruct((length, width), jnp.bfloat16),
        ),
        grid_spec=pltpu.PrefetchScalarGridSpec(
            num_scalar_prefetch=1,
            grid=(pairs,),
            in_specs=[
                pl.BlockSpec(segments.shape, lambda p, *_: (0, 0)),
                pl.BlockSpec((length, depth), lambda p, *_: (0, 0)),
                pl.BlockSpec((depth, 384), lambda p, *_: (0, p)),
                pl.BlockSpec(biases.shape, lambda p, *_: (0, 0)),
            ],
            out_specs=[
                pl.BlockSpec((rows, 128), lambda p, *_: (0, p)),
                pl.BlockSpec((rows, 128), lambda p, *_: (0, p)),
                pl.BlockSpec((8, length), lambda p, *_: (p, 0)),
                pl.BlockSpec((length, 384), lambda p, *_: (0, p)),
            ],
            scratch_shapes=[
                pltpu.VMEM((2, 128, length), jnp.bfloat16),
                pltpu.VMEM((2, length, 128), jnp.bfloat16),
                pltpu.VMEM((128, length), jnp.bfloat16),
                pltpu.VMEM((128, BLK), jnp.float32),
                pltpu.VMEM((2, 8, BLK), jnp.float32),
                pltpu.VMEM((2, 8, BLK), jnp.float32),
                pltpu.VMEM((2, length, BLK), jnp.float32),
                pltpu.VMEM((128, length), jnp.bfloat16),
                pltpu.VMEM((length, 128), jnp.bfloat16),
                pltpu.SMEM((DOCUMENTS + 1,), jnp.int32),
            ],
        ),
        compiler_params=pltpu.CompilerParams(dimension_semantics=("arbitrary",), vmem_limit_bytes=60 << 20),
        cost_estimate=pl.CostEstimate(flops=pairs * 40_000_000_000, bytes_accessed=pairs * 3_000_000, transcendentals=pairs * 4_000_000),
        name="attention_forward",
    )(segments, segments, tokens, weights, biases)


def backward_kernel(
    segment_ref,
    qkv_ref,
    ctx_mine_ref,
    ctx_other_ref,
    do_mine_ref,
    do_other_ref,
    lse_ref,
    row_ref,
    out_ref,
    sum_ref,
    q2,
    k2,
    q0,
    d0,
    dt,
    v0,
    kt,
    dk,
    dv,
    dqt,
    delta,
    mark_query,
    mark_key,
    bound_ref,
):
    length = qkv_ref.shape[0]
    blocks = length // BLK
    part = length // 4

    @pl.when(pl.program_id(0) == 0)
    def _():
        find_bounds(segment_ref, bound_ref)
        make_marks(row_ref, mark_query, mark_key)

    low = lax.broadcasted_iota(jnp.int32, (part, 128), 1) < 64

    def prepare(b, do, ctx):
        src = part_rows(b, part)
        dst = slice(b * part, (b + 1) * part)
        q, k = qkv_ref[src, 0:128], qkv_ref[src, 128:256]
        zero = jnp.zeros_like(q)
        nohk = mark_key[dst, :]
        turned = q.T
        q2[0, 0:64, dst] = turned[0:64]
        q2[0, 64:128, dst] = mark_query[64:128, dst]
        q2[1, 0:64, dst] = mark_query[0:64, dst]
        q2[1, 64:128, dst] = turned[64:128]
        k2[0, dst, :] = jnp.where(low, k, nohk)
        k2[1, dst, :] = jnp.where(low, nohk, k)
        q0[0, dst, :] = jnp.where(low, q, zero)
        q0[1, dst, :] = jnp.where(low, zero, q)
        d0[0, dst, :] = jnp.where(low, do, zero)
        d0[1, dst, :] = jnp.where(low, zero, do)
        turned = do.T
        blank = jnp.zeros((64, part), jnp.bfloat16)
        dt[0, 0:64, dst] = turned[0:64]
        dt[0, 64:128, dst] = blank
        dt[1, 0:64, dst] = blank
        dt[1, 64:128, dst] = turned[64:128]
        v0[dst, :] = qkv_ref[src, 256:384]
        kt[:, dst] = k.T
        prod = turned.astype(jnp.float32) * ctx.T.astype(jnp.float32)
        delta[0:1, dst] = jnp.sum(prod[0:64], axis=0, keepdims=True)
        delta[1:2, dst] = jnp.sum(prod[64:128], axis=0, keepdims=True)

    for b in range(4):

        @pl.when(local_start(b, part) < 2 * part)
        def _():
            rows = part_rows(b, part)
            prepare(b, do_mine_ref[rows, :], ctx_mine_ref[rows, :])

        @pl.when(local_start(b, part) >= 2 * part)
        def _():
            rows = pl.ds(pl.multiple_of(local_start(b, part) - 2 * part, 128), part)
            prepare(b, do_other_ref[rows, :], ctx_other_ref[rows, :])

    dk[...] = jnp.zeros_like(dk)
    dv[...] = jnp.zeros_like(dv)
    dqt[...] = jnp.zeros_like(dqt)

    def row(qb, _):
        qs = pl.ds(pl.multiple_of(qb * BLK, BLK), BLK)
        start, count = find_window(segment_ref, bound_ref, qb)

        def tile(first, size):
            ks = pl.ds(pl.multiple_of(start + first, 128), size)
            weights, grads = [], []
            for h in range(2):
                st = dot_nn(k2[h, ks, :], q2[h, :, qs])
                w = jnp.exp(st - lse_ref[h : h + 1, qs])
                gw = dot_nn(v0[ks, :], dt[h, :, qs])
                weights.append(w.astype(jnp.bfloat16))
                grads.append((w * (gw - delta[h : h + 1, qs])).astype(jnp.bfloat16))
            dv[ks, :] += dot_nn(jnp.concatenate(weights, axis=1), jnp.concatenate([d0[0, qs, :], d0[1, qs, :]], axis=0))
            dk[ks, :] += dot_nn(jnp.concatenate(grads, axis=1), jnp.concatenate([q0[0, qs, :], q0[1, qs, :]], axis=0))
            for h in range(2):
                rows = slice(64 * h, 64 * h + 64)
                dqt[rows, qs] += dot_nn(kt[rows, ks], grads[h])

        each_tile(count, tile)
        return 0

    lax.fori_loop(0, blocks, row, 0)
    sums = [jnp.zeros((1, 128), jnp.float32) for _ in range(3)]
    for b in range(4):
        dst = part_rows(b, part)
        src = slice(b * part, (b + 1) * part)
        pieces = ((dqt[:, src].T * 0.125).astype(jnp.bfloat16), dk[src, :].astype(jnp.bfloat16), dv[src, :].astype(jnp.bfloat16))
        for i, piece in enumerate(pieces):
            out_ref[dst, 128 * i : 128 * i + 128] = piece
            sums[i] = sums[i] + jnp.sum(piece.astype(jnp.float32), axis=0, keepdims=True)
    sum_ref[...] = jnp.zeros_like(sum_ref)
    for i in range(3):
        sum_ref[0:1, 128 * i : 128 * i + 128] = sums[i]


def attention_back(segments, qkv, ctx_mine, ctx_other, do_mine, do_other, lse):
    length, width = qkv.shape
    pairs = width // 384
    rows = length // 2
    half = lambda: pltpu.VMEM((2, length, 128), jnp.bfloat16)
    turned = lambda: pltpu.VMEM((2, 128, length), jnp.bfloat16)
    column = pl.BlockSpec((rows, 128), lambda p, *_: (0, p))
    return pl.pallas_call(
        backward_kernel,
        out_shape=(
            jax.ShapeDtypeStruct((length, width), jnp.bfloat16),
            jax.ShapeDtypeStruct((pairs * 8, 384), jnp.float32),
        ),
        grid_spec=pltpu.PrefetchScalarGridSpec(
            num_scalar_prefetch=1,
            grid=(pairs,),
            in_specs=[
                pl.BlockSpec((length, 384), lambda p, *_: (0, p)),
                column,
                column,
                column,
                column,
                pl.BlockSpec((8, length), lambda p, *_: (p, 0)),
                pl.BlockSpec(segments.shape, lambda p, *_: (0, 0)),
            ],
            out_specs=[
                pl.BlockSpec((length, 384), lambda p, *_: (0, p)),
                pl.BlockSpec((8, 384), lambda p, *_: (p, 0)),
            ],
            scratch_shapes=[
                turned(),
                half(),
                half(),
                half(),
                turned(),
                pltpu.VMEM((length, 128), jnp.bfloat16),
                pltpu.VMEM((128, length), jnp.bfloat16),
                pltpu.VMEM((length, 128), jnp.float32),
                pltpu.VMEM((length, 128), jnp.float32),
                pltpu.VMEM((128, length), jnp.float32),
                pltpu.VMEM((8, length), jnp.float32),
                pltpu.VMEM((128, length), jnp.bfloat16),
                pltpu.VMEM((length, 128), jnp.bfloat16),
                pltpu.SMEM((DOCUMENTS + 1,), jnp.int32),
            ],
        ),
        compiler_params=pltpu.CompilerParams(dimension_semantics=("arbitrary",), vmem_limit_bytes=60 << 20),
        cost_estimate=pl.CostEstimate(flops=pairs * 20_000_000_000, bytes_accessed=pairs * 5_000_000, transcendentals=pairs * 4_000_000),
        name="attention_backward",
    )(segments, qkv, ctx_mine, ctx_other, do_mine, do_other, lse, segments)


MESH_ID = pl.DeviceIdType.MESH
WIDE = 5


def place_of():
    return tuple(lax.axis_index(name) for name in ("z", "x", "y", "core"))


def sizes_of():
    return lax.axis_size("z"), lax.axis_size("x")


def partner(**moved):
    z, x, y, core = place_of()
    return (moved.get("z", z), moved.get("x", x), moved.get("y", y), moved.get("core", core))


def greet(with_grid):
    z, x, y, core = place_of()
    size_z, size_x = sizes_of()
    peers = [partner(y=1 - y), partner(core=1 - core)]
    if with_grid:
        peers += [partner(z=lax.rem(z + k, size_z)) for k in range(1, size_z)]
        peers += [partner(x=lax.rem(x + j, size_x)) for j in range(1, size_x)]
    barrier = pltpu.get_barrier_semaphore()
    for peer in peers:
        pl.semaphore_signal(barrier, inc=1, device_id=peer, device_id_type=MESH_ID)
    pl.semaphore_wait(barrier, len(peers))


def remote(src, dst, send, recv, peer):
    return pltpu.make_async_remote_copy(
        src_ref=src, dst_ref=dst, send_sem=send, recv_sem=recv, device_id=peer, device_id_type=MESH_ID
    )


def entry_kernel(size_z, size_x, count, *refs):
    tokens, cotangent, wq, wk, wv, w_inner, w_output, w_outer = refs[:8]
    vectors = refs[8 : 8 + count]
    tokens_all, cotangent_send, weights_all, inner_all, outer_all, rows_out, inner_out = refs[8 + count : 15 + count]
    raw = refs[15 + count : 15 + 2 * count]
    stage, cot_stage, wbuf, ibuf, obuf, pack, ipack, opack, vpack, vectors_all = refs[15 + 2 * count : 25 + 2 * count]
    local_sem, load_sem, tsend, trecv, zsend, zrecv, xsend, xrecv, ysend, yrecv, osend, orecv = refs[25 + 2 * count :]
    z, x, y, core = place_of()
    half = pack.shape[1] // 3
    pairs = half // 128
    chunks = w_inner.shape[1] // CHUNK
    me = z * size_x + x
    columns = [lax.rem(x + j, size_x) for j in range(size_x)]

    mine = pl.ds(pl.multiple_of(core * half, 128), half)
    loads = [pltpu.make_async_copy(w.at[:, mine], wbuf.at[i], load_sem.at[i]) for i, w in enumerate((wq, wk, wv))]
    loads += [pltpu.make_async_copy(v, r, load_sem.at[3 + i]) for i, (v, r) in enumerate(zip(vectors, raw))]
    late = [
        pltpu.make_async_copy(
            w_inner.at[:, pl.ds(pl.multiple_of(c * CHUNK + core * half, 128), half)],
            ibuf.at[:, pl.ds(c * half, half)],
            load_sem.at[3 + count + c],
        )
        for c in range(chunks)
    ]
    late.append(pltpu.make_async_copy(w_output.at[:, mine], ibuf.at[:, pl.ds(chunks * half, half)], load_sem.at[3 + count + chunks]))
    late.append(pltpu.make_async_copy(w_outer.at[:, mine], obuf, load_sem.at[4 + count + chunks]))
    load = pltpu.make_async_copy(tokens.at[y], stage, local_sem.at[0])
    cot_load = pltpu.make_async_copy(cotangent.at[1 - y], cot_stage, local_sem.at[4])
    for copy in loads + late + [load, cot_load]:
        copy.start()
    vpack[...] = jnp.zeros_like(vpack)
    for copy in loads:
        copy.wait()
    for i, vector in enumerate(raw):
        size = vector.shape[0]
        vpack[i : i + 1, 0:size] = vector[...].reshape(1, size).astype(jnp.bfloat16).astype(jnp.float32)
    for i in range(3):
        for p in range(pairs):
            pack[:, (3 * p + i) * 128 : (3 * p + i + 1) * 128] = wbuf[i, :, p * 128 : (p + 1) * 128].astype(jnp.bfloat16)
    vectors_all[me] = vpack[...]
    greet(True)

    across = remote(tokens.at[1 - y], tokens_all.at[1], tsend.at[0], trecv.at[0], partner(y=1 - y))
    across.start()
    beside = remote(tokens.at[y], tokens_all.at[2], tsend.at[1], trecv.at[1], partner(core=1 - core))

    rows = ipack.shape[0]

    def share(owner):
        return pl.ds(pl.multiple_of(owner * (rows // 2), rows // 2), rows // 2)

    packs = (pack, vpack, ipack.at[share(y), :])

    def y_move(index, origin):
        slot = home(2, origin)
        return remote(slot, slot, ysend.at[index], yrecv.at[index], partner(y=1 - y))

    def home(stream, origin):
        if stream == 2:
            return inner_all.at[origin, share(y), :]
        return (weights_all, vectors_all)[stream].at[origin * size_x + x]

    def z_move(stream, way, t):
        step = 1 - 2 * way
        origin = z - step * (t - 1)
        src = packs[stream] if t == 1 else home(stream, origin)
        peer = partner(z=lax.rem(z + step + size_z, size_z))
        return remote(src, home(stream, origin), zsend.at[stream, way, t - 1], zrecv.at[stream, way, t - 1], peer)

    def sends(way, t):
        step = 1 - 2 * way
        origin, target = z - step * (t - 1), z + step
        inside = lambda v: jnp.logical_and(v >= 0, v < size_z)
        return jnp.logical_and(inside(origin), inside(target))

    def receives(way, t):
        origin = z - (1 - 2 * way) * t
        return jnp.logical_and(origin >= 0, origin < size_z)

    def x_moves(index, origin, own):
        moves = []
        for j in range(1, size_x):
            for stream in range(2):
                src = packs[stream] if own else home(stream, origin)
                moves.append(
                    remote(
                        src,
                        home(stream, origin),
                        xsend.at[stream, index, j - 1],
                        xrecv.at[stream, index, j - 1],
                        partner(x=columns[j]),
                    )
                )
        return moves

    def start_z(streams, t):
        for way in range(2):

            @pl.when(sends(way, t))
            def _():
                for stream in streams:
                    z_move(stream, way, t).start()

    for move in x_moves(0, z, True):
        move.start()
    start_z((0, 1), 1)
    beside.start()
    for copy in late:
        copy.wait()
    ipack[...] = ibuf[...].astype(jnp.bfloat16)
    opack[...] = obuf[...].astype(jnp.bfloat16)
    start_z((2,), 1)
    outer_moves = [
        remote(opack, outer_all.at[x], osend.at[j - 1], orecv.at[j - 1], partner(x=columns[j])) for j in range(1, size_x)
    ]
    keeps = [
        pltpu.make_async_copy(pack, weights_all.at[me], local_sem.at[1]),
        pltpu.make_async_copy(ipack, inner_all.at[z], local_sem.at[2]),
        pltpu.make_async_copy(opack, outer_all.at[x], local_sem.at[6]),
    ]
    load.wait()
    keeps.append(pltpu.make_async_copy(stage, tokens_all.at[0], local_sem.at[3]))
    cot_load.wait()
    keeps.append(pltpu.make_async_copy(cot_stage, cotangent_send, local_sem.at[5]))
    for keep in keeps:
        keep.start()

    def arrive(streams, t, sideways):
        for way in range(2):

            @pl.when(receives(way, t))
            def _():
                origin = z - (1 - 2 * way) * t
                for stream in streams:
                    slot = home(stream, origin)
                    remote(
                        slot, slot, zsend.at[stream, way, t - 1], zrecv.at[stream, way, t - 1], partner(core=1 - core)
                    ).wait_recv()
                if sideways:
                    for move in x_moves(1 + way * (size_z - 1) + t - 1, origin, False):
                        move.start()
                else:
                    y_move(way * (size_z - 1) + t - 1, origin).start()

    onward = remote(tokens_all.at[1], tokens_all.at[3], tsend.at[2], trecv.at[2], partner(core=1 - core))
    for t in range(1, size_z):
        arrive((0, 1), t, True)
        if t < size_z - 1:
            start_z((0, 1), t + 1)
        if t == 1:
            for move in outer_moves:
                move.start()
        arrive((2,), t, False)
        if t < size_z - 1:
            start_z((2,), t + 1)
        if t == min(2, size_z - 1):
            across.wait_recv()
            onward.start()

    for move in x_moves(0, z, True):
        move.wait()
    for t in range(1, size_z):
        for way in range(2):

            @pl.when(receives(way, t))
            def _():
                origin = z - (1 - 2 * way) * t
                for move in x_moves(1 + way * (size_z - 1) + t - 1, origin, False):
                    move.wait()
                y_move(way * (size_z - 1) + t - 1, origin).wait()

            @pl.when(sends(way, t))
            def _():
                for stream in range(3):
                    z_move(stream, way, t).wait_send()

    short = min(vector.shape[0] for vector in raw)
    longest = vpack.shape[1]
    for s in range(size_z * size_x):
        rows_out[:, s * short : (s + 1) * short] = vectors_all[s, :, 0:short]
        inner_out[:, s * longest : (s + 1) * longest] = vectors_all[s, WIDE : WIDE + 1, :]
    for move in outer_moves:
        move.wait()
    across.wait_send()
    beside.wait()
    onward.wait()
    for keep in keeps:
        keep.wait()


def entry(size_z, size_x, tokens, cotangent, wq, wk, wv, w_inner, w_output, w_outer, vectors):
    _, part, width = tokens.shape
    rows = wq.shape[0]
    half = width // 2
    lanes = 3 * half
    hidden = w_inner.shape[1]
    long = w_outer.shape[0]
    mixed_lanes = hidden // 2 + half
    chunks = hidden // CHUNK
    longest = max(v.shape[0] for v in vectors)
    shards = size_z * size_x
    count = len(vectors)
    anywhere, vmem = pl.BlockSpec(memory_space=pl.ANY), pl.BlockSpec(memory_space=pltpu.VMEM)
    dma = pltpu.SemaphoreType.DMA
    low, high = jnp.bfloat16, jnp.float32
    side = size_x - 1
    return pl.pallas_call(
        lambda *refs: entry_kernel(size_z, size_x, count, *refs),
        out_shape=(
            jax.ShapeDtypeStruct((4, part, width), low),
            jax.ShapeDtypeStruct((part, width), low),
            jax.ShapeDtypeStruct((shards, rows, lanes), low),
            jax.ShapeDtypeStruct((size_z, rows, mixed_lanes), low),
            jax.ShapeDtypeStruct((size_x, long, half), low),
            jax.ShapeDtypeStruct((16, width), high),
            jax.ShapeDtypeStruct((1, shards * longest), high),
        ),
        in_specs=[anywhere] * (8 + count),
        out_specs=(anywhere,) * 5 + (vmem,) * 2,
        scratch_shapes=[pltpu.VMEM(v.shape, v.dtype) for v in vectors]
        + [
            pltpu.VMEM((part, width), low),
            pltpu.VMEM((part, width), low),
            pltpu.VMEM((3, rows, half), high),
            pltpu.VMEM((rows, mixed_lanes), high),
            pltpu.VMEM((long, half), high),
            pltpu.VMEM((rows, lanes), low),
            pltpu.VMEM((rows, mixed_lanes), low),
            pltpu.VMEM((long, half), low),
            pltpu.VMEM((16, longest), high),
            pltpu.VMEM((shards, 16, longest), high),
            dma((7,)),
            dma((5 + count + chunks,)),
            dma((4,)),
            dma((4,)),
            dma((3, 2, size_z - 1)),
            dma((3, 2, size_z - 1)),
            dma((2, 2 * size_z - 1, side)),
            dma((2, 2 * size_z - 1, side)),
            dma((2 * size_z - 2,)),
            dma((2 * size_z - 2,)),
            dma((side,)),
            dma((side,)),
        ],
        compiler_params=pltpu.CompilerParams(collective_id=0, has_side_effects=True, vmem_limit_bytes=66_000_000),
        name="entry",
    )(tokens, cotangent, wq, wk, wv, w_inner, w_output, w_outer, *vectors)


def exit_kernel(size_z, size_x, shapes, *refs):
    z, x, y, core = place_of()
    grads_hbm, inputs_hbm, weights_hbm, base_hbm, output_term, dense_sums, inner_sums, head_sums = refs[:8]
    inner_in = refs[8 : 8 + size_z]
    outer_in = refs[8 + size_z : 8 + size_z + size_x]
    refs = refs[8 + size_z + size_x :]
    made = refs[:8]
    token_grads, grad_query, grad_key, grad_value, grad_output, grad_inner, grad_outer, vector_sums = made
    grads, inputs, turned, weights, base, terms_a, terms_b, other_rows, recv_rows, send_rows, far_rows, odd = refs[8:20]
    inner_buf, outer_buf, vector_rows, vector_terms, inner_send = refs[20:25]
    load_sem, tsend, trecv, osend, orecv = refs[25:30]
    refs = list(refs[30:])
    terms = {"qa": terms_a, "qb": terms_b}
    xin, xsend, xrecv = {}, {}, {}
    zout, zin, zsend, zrecv = {}, {}, {}, {}
    ybuf, ysend, yrecv, cbuf, csend, crecv = {}, {}, {}, {}, {}, {}
    for name in shapes:
        ybuf[name], ysend[name], yrecv[name], cbuf[name], csend[name], crecv[name] = [refs.pop(0) for _ in range(6)]
        if name != "outer":
            xin[name], xsend[name], xrecv[name] = [refs.pop(0) for _ in range(3)]
        if name != "inner":
            zout[name], zin[name], zsend[name], zrecv[name] = [refs.pop(0) for _ in range(4)]

    shards, rows, half = odd.shape
    lanes = 3 * half
    pairs = half // 128
    hidden = grad_inner.shape[1]
    part = token_grads.shape[1]
    local = 2 * part
    low, high = jnp.bfloat16, jnp.float32
    mine = pl.ds(pl.multiple_of(core * half, 128), half)
    theirs = pl.ds(pl.multiple_of((1 - core) * half, 128), half)
    columns = [lax.rem(x + j, size_x) for j in range(size_x)]
    steps = [(t, way) for t in range(1, size_z) for way in range(2)]
    core_peer, y_peer = partner(core=1 - core), partner(y=1 - y)

    loads = {}
    for i, src in enumerate(inner_in):
        loads["inner", i] = pltpu.make_async_copy(src, inner_buf.at[i], load_sem.at[i])
    for i, src in enumerate(outer_in):
        loads["outer", i] = pltpu.make_async_copy(src, outer_buf.at[i], load_sem.at[size_z + i])
    for i, (name, src, dst) in enumerate(
        (("grads", grads_hbm, grads), ("weights", weights_hbm, weights), ("base", base_hbm, base), ("inputs", inputs_hbm, inputs))
    ):
        loads[name] = pltpu.make_async_copy(src, dst, load_sem.at[size_z + size_x + i])
    for load in loads.values():
        load.start()

    def inside(v):
        return jnp.logical_and(v >= 0, v < size_z)

    def target_of(t, way):
        return z + (1 - 2 * way) * (size_z - t)

    def fed(way):
        return inside(z - (1 - 2 * way))

    def x_move(name, n, at, j, src, dst):
        return remote(src, dst, xsend[name].at[n, at, j - 1], xrecv[name].at[n, at, j - 1], partner(x=columns[j]))

    def x_pieces(name, at):
        source = vector_terms if name == "vec" else terms[name]
        return [
            x_move(name, 0, at, j, source.at[at * size_x + columns[j]], xin[name].at[j - 1, at]) for j in range(1, size_x)
        ]

    def send_own(name):
        for move in x_pieces(name, z):
            move.start()

    def send_far(name):
        for t, way in steps:

            @pl.when(inside(target_of(t, way)))
            def _():
                for move in x_pieces(name, target_of(t, way)):
                    move.start()

    def own_part(name, at):
        if name == "outer":
            total = outer_buf[0, at].astype(high)
            for i in range(1, size_x):
                total = total + outer_buf[i, at].astype(high)
            return [(slice(None), total)]
        slot = at * size_x + x
        if name == "vec":
            total = vector_terms[slot]
            for move in x_pieces("vec", at):
                move.wait()
            for j in range(1, size_x):
                total = total + xin["vec"][j - 1, at]
            return [(slice(None), total)]
        for move in x_pieces(name, at):
            move.wait()
        total = terms[name][slot].astype(high)
        for j in range(1, size_x):
            total = total + xin[name][j - 1, at].astype(high)
        return [(slice(None), total)]

    def z_move(name, t, way):
        peer = partner(z=lax.rem(z + 1 - 2 * way + size_z, size_z))
        return remote(
            zout[name].at[way, t - 1], zin[name].at[way, t - 1], zsend[name].at[way, t - 1], zrecv[name].at[way, t - 1], peer
        )

    def step_z(name, t):
        for way in range(2):

            @pl.when(inside(target_of(t, way)))
            def _():
                pieces = own_part(name, target_of(t, way))
                if t > 1:

                    @pl.when(fed(way))
                    def _():
                        z_move(name, t - 1, way).wait_recv()

                for span, total in pieces:
                    if t > 1:
                        before = zin[name][way, t - 2, :, span].astype(high)
                        total = total + jnp.where(fed(way), before, 0.0)
                    zout[name][way, t - 1, :, span] = total.astype(zout[name].dtype)
                z_move(name, t, way).start()

    across, swapped = {}, {}

    def step_y(name):
        across[name] = remote(ybuf[name].at[0], ybuf[name].at[1], ysend[name], yrecv[name], y_peer)
        across[name].start()

    def finish_z(name):
        pieces = own_part(name, z)
        last = size_z - 1
        for way in range(2):

            @pl.when(fed(way))
            def _():
                z_move(name, last, way).wait_recv()

        for span, total in pieces:
            for way in range(2):
                before = zin[name][way, last - 1, :, span].astype(high)
                total = total + jnp.where(fed(way), before, 0.0)
            ybuf[name][0, :, span] = total.astype(ybuf[name].dtype)
        step_y(name)

    def step_core(name):
        across[name].wait()
        cbuf[name][0] = ybuf[name][0].astype(high) + ybuf[name][1].astype(high)
        swapped[name] = remote(cbuf[name].at[0], cbuf[name].at[1], csend[name], crecv[name], core_peer)
        swapped[name].start()

    def finish_core(name):
        swapped[name].wait()
        return cbuf[name]

    greet(True)

    outputs = remote(output_term.at[:, :, theirs], odd, osend, orecv, core_peer)
    outputs.start()
    for i in range(size_z):
        loads["inner", i].wait()
    inner_moves = []
    for j in range(1, size_x):
        total = inner_buf[0, columns[j]].astype(high)
        for i in range(1, size_z):
            total = total + inner_buf[i, columns[j]].astype(high)
        inner_send[j - 1] = total.astype(low)
        move = x_move("inner", 0, 0, j, inner_send.at[j - 1], xin["inner"].at[j - 1, 0])
        move.start()
        inner_moves.append(move)
    for i in range(size_x):
        loads["outer", i].wait()
    step_z("outer", 1)

    strip = 256

    def product(first):
        at = pl.ds(pl.multiple_of(first, strip), strip)
        return dot_nt(grads[at, :], weights[...])

    def token_move(first):
        at = pl.ds(pl.multiple_of(first, strip), strip)
        n = first // strip
        return remote(other_rows.at[at, :], recv_rows.at[at, :], tsend.at[n], trecv.at[n], core_peer)

    def back_move(i):
        at = pl.ds(pl.multiple_of(i * strip, strip), strip)
        n = local // strip + i
        return remote(send_rows.at[at, :], far_rows.at[at, :], tsend.at[n], trecv.at[n], y_peer)

    def token_rows(first):
        def other_strip(i, _):
            at = pl.ds(pl.multiple_of(first + i * strip, strip), strip)
            other_rows[at, :] = product(local + first + i * strip).astype(low)
            token_move(first + i * strip).start()
            return 0

        def own_strip(i, _):
            at = pl.ds(pl.multiple_of(first + i * strip, strip), strip)
            base[at, :] = base[at, :] + product(first + i * strip)
            if first == part:
                token_move(first + i * strip).wait()
                rows_out = pl.ds(pl.multiple_of(i * strip, strip), strip)
                send_rows[rows_out, :] = (base[at, :] + recv_rows[at, :].astype(high)).astype(low)
                back_move(i).start()
            return 0

        lax.fori_loop(0, part // strip, other_strip, 0)
        lax.fori_loop(0, part // strip, own_strip, 0)

    for name in ("grads", "weights", "base"):
        loads[name].wait()
    token_rows(part)

    vector_rows[...] = jnp.zeros_like(vector_rows)
    for i, row in enumerate((7, 8, 6, 3, 4, 2)):
        vector_rows[row : row + 1, :] = jnp.sum(dense_sums[8 * i : 8 * i + 8, :], axis=0, keepdims=True)
    for p in range(pairs):
        place = pl.ds(pl.multiple_of(core * half + p * 128, 128), 128)
        vector_rows[0:1, place] = head_sums[8 * p : 8 * p + 1, 0:128]
        vector_rows[1:2, place] = head_sums[8 * p : 8 * p + 1, 256:384]
    inner_row = jnp.sum(inner_sums[...], axis=0, keepdims=True)
    vector_terms[...] = jnp.zeros_like(vector_terms)
    longest = vector_terms.shape[2]
    for s in range(shards):
        vector_terms[s, :, 0:rows] = vector_rows[:, s * rows : (s + 1) * rows]
        vector_terms[s, WIDE : WIDE + 1, :] = inner_row[:, s * longest : (s + 1) * longest]
    send_far("vec")
    send_own("vec")
    step_z("outer", 2)
    loads["inputs"].wait()
    for b in range(4):
        turned[:, b * part : (b + 1) * part] = inputs[b * part : (b + 1) * part, :].T
    group = 4
    for p in range(pairs):
        block = slice(p * 384, (p + 1) * 384)
        where = slice(p % 2 * 384, p % 2 * 384 + 384)
        goal = terms_a if p < 2 else terms_b

        def some(m, _):
            value = dot_nn(turned[pl.ds(pl.multiple_of(m * group * rows, group * rows), group * rows), :], grads[:, block])
            goal[pl.ds(m * group, group), :, where] = value.reshape(group, rows, 384).astype(low)
            return 0

        lax.fori_loop(0, shards // group, some, 0)
        if p == 1:
            send_far("qa")
    outputs.wait()
    terms_b[:, :, half : 2 * half] = (odd[...].astype(high) + output_term[:, :, mine].astype(high)).astype(low)
    send_far("qb")
    send_own("qa")
    send_own("qb")
    total = inner_buf[0, x].astype(high)
    for i in range(1, size_z):
        total = total + inner_buf[i, x].astype(high)
    for j in range(1, size_x):
        inner_moves[j - 1].wait()
        total = total + xin["inner"][j - 1, 0].astype(high)
    ybuf["inner"][0] = total.astype(low)
    step_y("inner")
    for t in range(3, size_z):
        step_z("outer", t)
    step_z("vec", 1)
    step_z("qa", 1)
    token_rows(0)
    step_z("vec", 2)
    step_z("qa", 2)
    finish_z("outer")
    for t in range(3, size_z):
        step_z("vec", t)
        step_z("qa", t)
    step_z("qb", 1)
    for i in range(part // strip):
        token_move(i * strip).wait()
    token_grads[y] = base[0:part, :] + recv_rows[0:part, :].astype(high)
    step_core("inner")
    step_z("qb", 2)
    for t in range(3, size_z):
        step_z("qb", t)
    finish_z("qa")
    finish_z("vec")
    step_core("outer")
    for i in range(part // strip):
        back_move(i).wait()
    token_grads[1 - y] = far_rows[...].astype(high)
    chunks = hidden // CHUNK
    buf = finish_core("inner")
    for i in range(2):
        owner = core if i == 0 else 1 - core
        for c in range(chunks):
            place = pl.ds(pl.multiple_of(c * CHUNK + owner * half, 128), half)
            grad_inner[:, place] = buf[i, :, c * half : (c + 1) * half]
    buf = finish_core("outer")
    for i in range(2):
        owner = core if i == 0 else 1 - core
        grad_outer[:, pl.ds(pl.multiple_of(owner * half, 128), half)] = buf[i]
    finish_z("qb")
    step_core("vec")
    step_core("qa")

    def spread(name):
        buf = finish_core(name)
        for i in range(2):
            owner = core if i == 0 else 1 - core
            for p in (0, 1) if name == "qa" else (2,):
                place = pl.ds(pl.multiple_of(owner * half + p * 128, 128), 128)
                for n, out in enumerate((grad_query, grad_key, grad_value)):
                    at = (3 * (p % 2) + n) * 128
                    out[:, place] = buf[i, :, at : at + 128]
            if name == "qb":
                grad_output[:, pl.ds(pl.multiple_of(owner * half, 128), half)] = buf[i, :, half : 2 * half]

    for name in zout:
        for t, way in steps:

            @pl.when(inside(target_of(t, way)))
            def _():
                z_move(name, t, way).wait_send()

    buf = finish_core("vec")
    vector_sums[...] = buf[0] + buf[1]
    spread("qa")
    step_core("qb")
    spread("qb")


def deliver_kernel(count, mixed_mine, mixed_far, *refs):
    matrices, vectors, mixed = refs[:count], refs[count], refs[count + 1]
    outs = refs[count + 2 : 2 * count + 2]
    smalls = refs[2 * count + 2 : -4]
    stage, in_sem, out_sem = refs[-4:-2], refs[-2], refs[-1]
    y = lax.axis_index("y")
    loads = [pltpu.make_async_copy(src, stage[i], in_sem.at[i]) for i, src in enumerate((mixed_mine, mixed_far))]
    copies = [pltpu.make_async_copy(src, dst, out_sem.at[i]) for i, (src, dst) in enumerate(zip(matrices, outs))]
    for copy in loads + copies:
        copy.start()
    for i, small in enumerate(smalls):
        small[...] = vectors[i : i + 1, 0 : small.shape[0]].reshape(small.shape)
    for i, place in enumerate((y, 1 - y)):
        loads[i].wait()
        copies.append(pltpu.make_async_copy(stage[i], mixed.at[place], out_sem.at[count + i]))
        copies[-1].start()
    for copy in copies:
        copy.wait()


def deliver(mixed_mine, mixed_far, matrices, vectors, sizes):
    count = len(matrices)
    vmem, anywhere = pl.BlockSpec(memory_space=pltpu.VMEM), pl.BlockSpec(memory_space=pl.ANY)
    return pl.pallas_call(
        lambda *refs: deliver_kernel(count, *refs),
        out_shape=(jax.ShapeDtypeStruct((2,) + mixed_mine.shape, mixed_mine.dtype),)
        + tuple(jax.ShapeDtypeStruct(m.shape, m.dtype) for m in matrices)
        + tuple(jax.ShapeDtypeStruct((size,), jnp.float32) for size in sizes),
        in_specs=[anywhere] * 2 + [vmem] * (count + 1),
        out_specs=(anywhere,) * (count + 1) + (vmem,) * len(sizes),
        scratch_shapes=[pltpu.VMEM(mixed_mine.shape, mixed_mine.dtype)] * 2
        + [pltpu.SemaphoreType.DMA((2,)), pltpu.SemaphoreType.DMA((count + 2,))],
        compiler_params=pltpu.CompilerParams(vmem_limit_bytes=40_000_000),
        name="deliver",
    )(mixed_mine, mixed_far, *matrices, vectors)


def exit_call(size_z, size_x, grads, inputs, weights, base, output_term, dense_sums, inner_sums, head_sums, inner_terms, outer_terms):
    shards, rows, width = output_term.shape
    lanes = grads.shape[1]
    half = width // 2
    pairs = half // 128
    length = inputs.shape[0]
    local = length // 2
    part = local // 2
    long = outer_terms[0].shape[1]
    hidden = 2 * inner_terms[0].shape[2]
    vmem, anywhere = pl.BlockSpec(memory_space=pltpu.VMEM), pl.BlockSpec(memory_space=pl.ANY)
    dma = pltpu.SemaphoreType.DMA
    side = size_x - 1
    full = lanes + half
    low, high = jnp.bfloat16, jnp.float32
    vector_shape = (16, hidden // shards)
    shapes = {
        "vec": (vector_shape, high, 1),
        "qa": ((rows, width), low, 1),
        "qb": ((rows, width), low, 1),
        "inner": ((rows, hidden // 2), low, 1),
        "outer": ((long, half), low, 1),
    }
    matrix = jax.ShapeDtypeStruct((rows, width), high)
    results = (
        jax.ShapeDtypeStruct((2, part, width), high),
        matrix,
        matrix,
        matrix,
        matrix,
        jax.ShapeDtypeStruct((rows, hidden), high),
        jax.ShapeDtypeStruct((long, width), high),
        jax.ShapeDtypeStruct(vector_shape, high),
    )
    scratch = [
        pltpu.VMEM((length, lanes), low),
        pltpu.VMEM((length, width), low),
        pltpu.VMEM((width, length), low),
        pltpu.VMEM((width, lanes), low),
        pltpu.VMEM((local, width), high),
        pltpu.VMEM((shards, rows, width), low),
        pltpu.VMEM((shards, rows, width), low),
        pltpu.VMEM((local, width), low),
        pltpu.VMEM((local, width), low),
        pltpu.VMEM((part, width), low),
        pltpu.VMEM((part, width), low),
        pltpu.VMEM((shards, rows, half), low),
        pltpu.VMEM((size_z,) + inner_terms[0].shape, low),
        pltpu.VMEM((size_x,) + outer_terms[0].shape, low),
        pltpu.VMEM((16, width), high),
        pltpu.VMEM((shards,) + vector_shape, high),
        pltpu.VMEM((side, rows, hidden // 2), low),
        dma((size_z + size_x + 4,)),
        dma((local // 256 + part // 256,)),
        dma((local // 256 + part // 256,)),
        dma,
        dma,
    ]
    for name, (shape, kind, sends) in shapes.items():
        scratch += [pltpu.VMEM((2,) + shape, kind), dma, dma, pltpu.VMEM((2,) + shape, high), dma, dma]
        stages = 1 if name == "inner" else size_z
        if name != "outer":
            scratch += [pltpu.VMEM((side, stages) + shape, kind), dma((sends, stages, side)), dma((sends, stages, side))]
        if name != "inner":
            scratch += [pltpu.VMEM((2, size_z - 1) + shape, kind)] * 2 + [dma((2, size_z - 1))] * 2
    return pl.pallas_call(
        lambda *refs: exit_kernel(size_z, size_x, shapes, *refs),
        out_shape=tuple(pltpu.VMEM(r.shape, r.dtype) for r in results),
        in_specs=[anywhere] * 4 + [vmem] * 4 + [anywhere] * (size_z + size_x),
        out_specs=(vmem,) * len(results),
        scratch_shapes=scratch,
        compiler_params=pltpu.CompilerParams(collective_id=1, has_side_effects=True, vmem_limit_bytes=56_000_000),
        name="exit",
    )(grads, inputs, weights, base, output_term, dense_sums, inner_sums, head_sums, *inner_terms, *outer_terms)


TILE = 256
CHUNK = 768


def dot_nt(a, b):
    return lax.dot_general(a, b, (((1,), (1,)), ((), ())), preferred_element_type=jnp.float32)


def row_mean(value):
    return jnp.sum(value, axis=-1, keepdims=True) * (1.0 / value.shape[-1])


def standardize(hidden):
    centred = hidden - row_mean(hidden)
    reciprocal = lax.rsqrt(row_mean(centred * centred) + EPS)
    return centred * reciprocal, reciprocal


def column_sum(value):
    return jnp.sum(value.reshape(value.shape[0] // 8, 8, value.shape[1]), axis=0)


def dense_kernel(
    size_z,
    size_x,
    tokens_ref,
    mine_ref,
    other_hbm,
    cot_hbm,
    cot_far_hbm,
    vectors_ref,
    bias_inner_ref,
    *refs,
):
    inner_parts, outer_parts = refs[:size_x], refs[size_x : size_x + size_z]
    refs = refs[size_x + size_z :]
    mixed_ref, mixed_send_ref, pre_first_ref, grad_mine_ref, grad_far_hbm, sums_ref, inner_sum_ref, grad_output_ref = refs[:8]
    inner_terms = refs[8 : 8 + size_z]
    outer_terms = refs[8 + size_z : 8 + size_z + size_x]
    refs = refs[8 + size_z + size_x :]
    w_output, w_inner, w_outer, a_output, a_inner, a_outer, grad_out_buf = refs[:7]
    context, first_low, turned_low, normed, first, slope, active, work = refs[7:15]
    send_inner, send_outer, recv_inner, recv_outer = refs[15:19]
    far_rows, grad_send, ready, cotangent, cot_sem, swap_send, swap_recv = refs[19:26]
    load_sem, share_send, share_recv, send_sem, recv_sem, store_sem = refs[26:]
    step, steps = pl.program_id(0), pl.num_programs(0)
    core_here = lax.axis_index("core")
    width, hidden = w_inner.shape
    half = width // 2
    chunks = hidden // CHUNK
    shards = size_z * size_x
    z, x, y, _ = place_of()
    twin = partner(core=1 - lax.axis_index("core"))
    near = cotangent.shape[0] // 2
    cot_loads = (
        pltpu.make_async_copy(cot_hbm.at[y], cotangent.at[pl.ds(0, near), :], cot_sem.at[0]),
        pltpu.make_async_copy(cot_far_hbm, cotangent.at[pl.ds(near, near), :], cot_sem.at[1]),
    )

    shard = width // shards
    long = hidden // shards
    group = CHUNK // long // size_x

    def columns_of(first, owner):
        return pl.ds(pl.multiple_of(first + owner * half, 128), half)

    def start_piece(i, src, dst):
        pltpu.make_async_copy(src, dst, load_sem.at[i]).start()
        remote(src, dst, share_send.at[i], share_recv.at[i], twin).start()

    def start_rows(i, lane, ref, first):
        for j in range(size_x):
            for at in range(size_z):
                slot = at * size_x + lax.rem(x - j + size_x, size_x)
                rows = pl.ds(pl.multiple_of(slot * shard, shard), shard)
                start_piece(i, inner_parts[j].at[at, :, pl.ds(lane, half)], ref.at[rows, columns_of(first, core_here)])

    def start_loads():
        start_rows(0, hidden // 2, w_output, 0)
        for c in range(chunks):
            start_rows(1 + 2 * c, c * half, w_inner, c * CHUNK)
            for at in range(c * group, (c + 1) * group):
                for k in range(size_z):

                    @pl.when(lax.rem(z - k + size_z, size_z) == at)
                    def _():
                        for column in range(size_x):
                            rows = pl.ds((at * size_x + column) * long, long)
                            start_piece(2 + 2 * c, outer_parts[k].at[column], w_outer.at[rows, columns_of(0, core_here)])

    def wait_load(i, ref, rows, first):
        own, far = ref.at[rows, columns_of(first, core_here)], ref.at[rows, columns_of(first, 1 - core_here)]
        pltpu.make_async_copy(own, own, load_sem.at[i]).wait()
        remote(own, far, share_send.at[i], share_recv.at[i], twin).wait()

    @pl.when(step == 0)
    def _():
        barrier = pltpu.get_barrier_semaphore()
        pl.semaphore_signal(barrier, inc=1, device_id=twin, device_id_type=MESH_ID)
        pl.semaphore_wait(barrier, 1)
        remote(other_hbm, far_rows, swap_send.at[0], swap_recv.at[0], twin).start()
        start_loads()
        for load in cot_loads:
            load.start()
        a_output[...] = jnp.zeros_like(a_output)
        a_inner[...] = jnp.zeros_like(a_inner)
        a_outer[...] = jnp.zeros_like(a_outer)
        sums_ref[...] = jnp.zeros_like(sums_ref)
        inner_sum_ref[...] = jnp.zeros_like(inner_sum_ref)

    def vector(i):
        row = (2, 3, 4, 6, 7, 8)[i]
        return vectors_ref[row : row + 1, :]

    def add_sum(i, value):
        sums_ref[8 * i : 8 * i + 8, :] += column_sum(value)

    context[:, pl.ds(pl.multiple_of(core_here * half, 128), half)] = mine_ref[...]

    context_move = remote(other_hbm, far_rows, swap_send.at[0], swap_recv.at[0], twin)

    @pl.when(step == 0)
    def _():
        context_move.wait()

    here = pl.ds(pl.multiple_of(step * TILE, TILE), TILE)
    context[:, pl.ds(pl.multiple_of((1 - core_here) * half, 128), half)] = far_rows[here, :]

    @pl.when(step == 0)
    def _():
        wait_load(0, w_output, slice(None), 0)

    hidden_rows = tokens_ref[...].astype(jnp.float32) + (dot_nn(context[...], w_output[...]) + vector(0))
    normed[...], first_recip = standardize(hidden_rows)
    first[...] = normed[...] * vector(1) + vector(2)
    first_low[...] = first[...].astype(jnp.bfloat16)
    turned_low[...] = first_low[...].T
    work[...] = jnp.broadcast_to(vector(3), work.shape)

    def part(c):
        return pl.ds(c * CHUNK, CHUNK)

    def exchange(c):
        return (
            remote(send_inner.at[c], recv_inner.at[c], send_sem.at[0, c], recv_sem.at[0, c], twin),
            remote(send_outer.at[c], recv_outer.at[c], send_sem.at[1, c], recv_sem.at[1, c], twin),
        )

    def wait_inner(c):
        @pl.when(step == 0)
        def _():
            wait_load(1 + 2 * c, w_inner, slice(None), c * CHUNK)

    def ahead(c):
        ready[c % 2] = dot_nn(first_low[...], w_inner[:, part(c)])

    wait_inner(0)
    ahead(0)
    for c in range(chunks):
        if c + 1 < chunks:
            wait_inner(c + 1)

        @pl.when(step == 0)
        def _():
            wait_load(2 + 2 * c, w_outer, part(c), 0)

        if c + 1 < chunks:
            ahead(c + 1)
        u = ready[c % 2] + bias_inner_ref[0:1, part(c)]
        cdf = 0.5 * (1.0 + lax.erf(u * ROOT_HALF))
        slope[:, part(c)] = cdf + u * jnp.exp(-0.5 * u * u) * INV_ROOT_TAU
        acted = (u * cdf).astype(jnp.bfloat16)
        active[:, part(c)] = acted
        work[...] += dot_nn(acted, w_outer[part(c), :])

    second, second_recip = standardize(first[...] + work[...])
    mixed = (second * vector(4) + vector(5)).astype(jnp.bfloat16)

    @pl.when(step < steps // 2)
    def _():
        mixed_ref[...] = mixed

    @pl.when(step >= steps // 2)
    def _():
        mixed_send_ref[...] = mixed


    @pl.when(step == 0)
    def _():
        for load in cot_loads:
            load.wait()

    upstream = cotangent[pl.ds(pl.multiple_of(step * TILE, TILE), TILE), :].astype(jnp.float32)
    add_sum(0, upstream * second)
    add_sum(1, upstream)
    scaled = upstream * vector(4)
    pre_second = second_recip * (scaled - row_mean(scaled) - second * row_mean(scaled * second))
    grad_outer = pre_second.astype(jnp.bfloat16)
    add_sum(2, grad_outer.astype(jnp.float32))
    work[...] = pre_second
    grad_out_buf[...] = grad_outer

    def behind(c):
        ready[c % 2] = dot_nt(grad_out_buf[...], w_outer[part(c), :])

    behind(0)
    for c in range(chunks):
        if c + 1 < chunks:
            behind(c + 1)
        grad_inner = (ready[c % 2] * slope[:, part(c)]).astype(jnp.bfloat16)
        inner_sum_ref[:, part(c)] += column_sum(grad_inner.astype(jnp.float32))
        a_outer[part(c), :] += dot_nn(active[:, part(c)].T, grad_out_buf[...])
        a_inner[:, part(c)] += dot_nn(turned_low[...], grad_inner)
        work[...] += dot_nt(grad_inner, w_inner[:, part(c)])

        @pl.when(step == steps - 1)
        def _():
            theirs = pl.multiple_of(c * CHUNK + (1 - core_here) * half, 128)
            send_inner[c] = a_inner[:, pl.ds(theirs, half)].astype(jnp.bfloat16)
            send_outer[c] = a_outer[part(c), pl.ds(pl.multiple_of((1 - core_here) * half, 128), half)].astype(jnp.bfloat16)
            for move in exchange(c):
                move.start()

    grad_first = work[...]
    add_sum(3, grad_first * normed[...])
    add_sum(4, grad_first)
    scaled = grad_first * vector(1)
    pre_first = first_recip * (scaled - row_mean(scaled) - normed[...] * row_mean(scaled * normed[...]))
    pre_first_ref[...] = pre_first
    grad_attended = pre_first.astype(jnp.bfloat16)
    add_sum(5, grad_attended.astype(jnp.float32))
    a_output[...] += dot_nn(context[...].T, grad_attended)
    context[...] = dot_nt(grad_attended, w_output[...]).astype(jnp.bfloat16)
    grad_mine_ref[...] = context[:, pl.ds(pl.multiple_of(core_here * half, 128), half)]

    def grad_move(t):
        rows = pl.ds(pl.multiple_of(t * TILE, TILE), TILE)
        return remote(grad_send.at[t], grad_far_hbm.at[rows, :], swap_send.at[1 + t], swap_recv.at[1 + t], twin)

    grad_send[step] = context[:, pl.ds(pl.multiple_of((1 - core_here) * half, 128), half)]
    grad_move(step).start()

    @pl.when(step == steps - 1)
    def _():
        grad_output_ref[...] = a_output[...].astype(jnp.bfloat16)

        def inner_out(c):
            copies = []
            for k in range(size_z):
                for column in range(size_x):
                    slot = lax.rem(z + k, size_z) * size_x + column
                    src = send_inner.at[c, pl.ds(pl.multiple_of(slot * shard, shard), shard), :]
                    copies.append(
                        pltpu.make_async_copy(src, inner_terms[k].at[column, :, pl.ds(c * half, half)], store_sem.at[0, c])
                    )
            return copies

        def outer_out(c):
            copies = []
            for i in range(group):
                for j in range(size_x):
                    src = send_outer.at[c, pl.ds(pl.multiple_of((i * size_x + lax.rem(x + j, size_x)) * long, long), long), :]
                    copies.append(pltpu.make_async_copy(src, outer_terms[j].at[c * group + i], store_sem.at[1, c]))
            return copies

        for c in range(chunks):
            ours = pl.multiple_of(c * CHUNK + core_here * half, 128)
            first_move, second_move = exchange(c)
            first_move.wait()
            send_inner[c] = (a_inner[:, pl.ds(ours, half)] + recv_inner[c].astype(jnp.float32)).astype(jnp.bfloat16)
            for copy in inner_out(c):
                copy.start()
            second_move.wait()
            columns = pl.ds(pl.multiple_of(core_here * half, 128), half)
            send_outer[c] = (a_outer[part(c), columns] + recv_outer[c].astype(jnp.float32)).astype(jnp.bfloat16)
            for copy in outer_out(c):
                copy.start()
        for t in range(grad_send.shape[0]):
            grad_move(t).wait()
        for c in range(chunks):
            pltpu.make_async_copy(send_inner.at[c], send_inner.at[c], store_sem.at[0, c]).wait()
            pltpu.make_async_copy(send_outer.at[c], send_outer.at[c], store_sem.at[1, c]).wait()


def dense_layer(size_z, size_x, tokens, mine, other, cotangent, cotangent_far, vectors, bias_inner, inner_parts, outer_parts):
    local, half = mine.shape
    width = 2 * half
    hidden = bias_inner.shape[1]
    steps = local // TILE
    shards = size_z * size_x
    chunks = hidden // CHUNK
    low, high = jnp.bfloat16, jnp.float32
    tile = pl.BlockSpec((TILE, width), lambda t, *_: (t, 0))
    half_tile = pl.BlockSpec((TILE, half), lambda t, *_: (t, 0))
    anywhere = pl.BlockSpec(memory_space=pl.ANY)

    def whole(shape):
        return pl.BlockSpec(shape, lambda t, *_: (0, 0))

    inner_shape = jax.ShapeDtypeStruct((size_x, width // shards, hidden // 2), low)
    outer_shape = jax.ShapeDtypeStruct((size_z, hidden // shards, half), low)
    halves = pltpu.VMEM((chunks, width, half), low)
    dma = pltpu.SemaphoreType.DMA
    return pl.pallas_call(
        lambda *refs: dense_kernel(size_z, size_x, *refs),
        out_shape=(
            jax.ShapeDtypeStruct((local // 2, width), low),
            jax.ShapeDtypeStruct((local // 2, width), low),
            jax.ShapeDtypeStruct((local, width), high),
            jax.ShapeDtypeStruct((local, half), low),
            jax.ShapeDtypeStruct((local, half), low),
            jax.ShapeDtypeStruct((48, width), high),
            jax.ShapeDtypeStruct((8, hidden), high),
            jax.ShapeDtypeStruct((width, width), low),
        )
        + (inner_shape,) * size_z
        + (outer_shape,) * size_x,
        grid_spec=pltpu.PrefetchScalarGridSpec(
            num_scalar_prefetch=0,
            grid=(steps,),
            in_specs=[
                tile,
                half_tile,
                anywhere,
                anywhere,
                anywhere,
                whole((16, width)),
                whole((1, hidden)),
            ]
            + [anywhere] * (size_x + size_z),
            out_specs=[
                pl.BlockSpec((TILE, width), lambda t: (jnp.minimum(t, steps // 2 - 1), 0)),
                pl.BlockSpec((TILE, width), lambda t: (jnp.maximum(t - steps // 2, 0), 0)),
                tile,
                half_tile,
                anywhere,
                whole((48, width)),
                whole((8, hidden)),
                whole((width, width)),
            ]
            + [anywhere] * (size_z + size_x),
            scratch_shapes=[
                pltpu.VMEM((width, width), low),
                pltpu.VMEM((width, hidden), low),
                pltpu.VMEM((hidden, width), low),
                pltpu.VMEM((width, width), high),
                pltpu.VMEM((width, hidden), high),
                pltpu.VMEM((hidden, width), high),
                pltpu.VMEM((TILE, width), low),
                pltpu.VMEM((TILE, width), low),
                pltpu.VMEM((TILE, width), low),
                pltpu.VMEM((width, TILE), low),
                pltpu.VMEM((TILE, width), high),
                pltpu.VMEM((TILE, width), high),
                pltpu.VMEM((TILE, hidden), high),
                pltpu.VMEM((TILE, hidden), low),
                pltpu.VMEM((TILE, width), high),
                halves,
                halves,
                halves,
                halves,
                pltpu.VMEM((local, half), low),
                pltpu.VMEM((steps, TILE, half), low),
                pltpu.VMEM((2, TILE, CHUNK), high),
                pltpu.VMEM((local, width), low),
                dma((2,)),
                dma((1 + steps,)),
                dma((1 + steps,)),
                dma((1 + 2 * chunks,)),
                dma((1 + 2 * chunks,)),
                dma((1 + 2 * chunks,)),
                dma((2, chunks)),
                dma((2, chunks)),
                dma((2, chunks)),
            ],
        ),
        compiler_params=pltpu.CompilerParams(
            dimension_semantics=("arbitrary",), vmem_limit_bytes=67_000_000, collective_id=3, has_side_effects=True
        ),
        cost_estimate=pl.CostEstimate(flops=32_000_000_000, bytes_accessed=40_000_000, transcendentals=6_000_000),
        name="dense_layer",
    )(tokens, mine, other, cotangent, cotangent_far, vectors, bias_inner, *inner_parts, *outer_parts)


def lowered(piece):
    return piece.astype(jnp.bfloat16)


def widen(piece):
    return piece.astype(jnp.float32)


def matmul(left, right):
    return jnp.dot(left, right, preferred_element_type=jnp.float32)


def matmul_tn(left, right):
    return lax.dot_general(
        left, right, (((0,), (0,)), ((), ())), preferred_element_type=jnp.float32
    )


def matmul_nt(left, right):
    return lax.dot_general(
        left, right, (((1,), (1,)), ((), ())), preferred_element_type=jnp.float32
    )


def normalize(hidden, norm_gain, norm_shift):
    centred = hidden - jnp.mean(hidden, axis=-1, keepdims=True)
    reciprocal = lax.rsqrt(jnp.mean(centred * centred, axis=-1, keepdims=True) + EPS)
    normed = centred * reciprocal
    return (normed * norm_gain + norm_shift, normed, reciprocal)


def normalize_back(upstream, normed, reciprocal, norm_gain):
    scaled = upstream * norm_gain
    result = reciprocal * (
        scaled
        - jnp.mean(scaled, axis=-1, keepdims=True)
        - normed * jnp.mean(scaled * normed, axis=-1, keepdims=True)
    )
    return (result, jnp.sum(upstream * normed, axis=0), jnp.sum(upstream, axis=0))


def gelu_value(values_in):
    return 0.5 * values_in * (1.0 + lax.erf(values_in * ROOT_HALF))


def gelu_slope(values_in):
    return (
        0.5 * (1.0 + lax.erf(values_in * ROOT_HALF))
        + values_in * jnp.exp(-0.5 * values_in * values_in) * INV_ROOT_TAU
    )


def shift(piece, axis, step):
    size = lax.axis_size(axis)
    return lax.ppermute(piece, axis, [(i, (i + step) % size) for i in range(size)])


def swap(piece, axis):
    return lax.ppermute(piece, axis, [(0, 1), (1, 0)])


def pick(piece, index, axis=0):
    return lax.dynamic_index_in_dim(piece, index, axis, keepdims=False)


def in_order(first_is_zero, own, other, axis):
    return jnp.where(
        first_is_zero,
        jnp.concatenate([own, other], axis),
        jnp.concatenate([other, own], axis),
    )


def collect(piece):
    size_z, size_x = lax.axis_size("z"), lax.axis_size("x")
    z, x = lax.axis_index("z"), lax.axis_index("x")
    along_z = [piece] + [shift(piece, "z", k) for k in range(1, size_z)]
    whole = jnp.zeros((size_z, size_x) + piece.shape, piece.dtype)
    zeros = (0,) * piece.ndim
    for j in range(size_x):
        for k in range(size_z):
            arrived = along_z[k] if j == 0 else shift(along_z[k], "x", j)
            place = ((z - k) % size_z, (x - j) % size_x) + zeros
            whole = lax.dynamic_update_slice(whole, arrived[None, None], place)
    return whole.reshape((size_z * size_x,) + piece.shape)


def reduce_owned(terms):
    size_z, size_x = lax.axis_size("z"), lax.axis_size("x")
    z, x = lax.axis_index("z"), lax.axis_index("x")
    terms = terms.reshape((size_z, size_x) + terms.shape[1:])
    total = widen(pick(terms, x, 1))
    for j in range(1, size_x):
        total = total + widen(shift(pick(terms, (x + j) % size_x, 1), "x", j))
    terms = lowered(total)
    total = widen(pick(terms, z))
    for k in range(1, size_z):
        total = total + widen(shift(pick(terms, (z + k) % size_z), "z", k))
    terms = lowered(total)
    return widen(terms) + widen(swap(terms, "y"))


def plain_body(
    tokens,
    segment_ids,
    w_query,
    w_key,
    w_value,
    w_output,
    b_query,
    b_value,
    b_output,
    first_gain,
    first_shift,
    w_inner,
    b_inner,
    w_outer,
    b_outer,
    second_gain,
    second_shift,
    cotangent,
):
    core, y = lax.axis_index("core"), lax.axis_index("y")
    shards = lax.axis_size("z") * lax.axis_size("x")
    sequences, part, width = tokens.shape
    half = width // 2
    pairs = half // 128
    hidden = w_inner.shape[1]
    local = 2 * part
    own_rows = w_query.shape[0]
    unit_half = hidden // shards // 2

    def columns(matrix):
        return lowered(lax.dynamic_slice_in_dim(matrix, core * half, half, 1))

    vectors = (b_query, b_value, b_output, first_gain, first_shift, b_inner, b_outer, second_gain, second_shift)
    flat = jnp.concatenate([lowered(v) for v in vectors])
    lanes = 3 * half
    extra = -(-flat.shape[0] // lanes)
    flat = jnp.pad(flat, (0, extra * lanes - flat.shape[0])).reshape(extra, lanes)
    weights = jnp.stack([columns(w).reshape(own_rows, pairs, 128) for w in (w_query, w_key, w_value)], axis=2)
    early = collect(jnp.concatenate([weights.reshape(own_rows, lanes), flat], axis=0))

    mine = pick(tokens, y)
    arrived = swap(pick(tokens, 1 - y), "y")
    mine_other, arrived_other = swap(mine, "core"), swap(arrived, "core")
    inputs_all = jnp.concatenate([mine, arrived, mine_other, arrived_other], axis=0)
    inputs = jnp.concatenate([mine, arrived], axis=0)

    inner_piece = lowered(pick(w_inner.reshape(own_rows, shards, 2, unit_half), core, 2)).reshape(own_rows, hidden // 2)
    late = collect(jnp.concatenate([columns(w_output), inner_piece], axis=1)).reshape(width, half + hidden // 2)
    outer_own = collect(lowered(lax.dynamic_slice_in_dim(w_outer, core * unit_half, unit_half, 0))).reshape(hidden // 2, width)
    output_own, inner_own = late[:, :half], late[:, half:]
    output_other, inner_other, outer_other = swap(output_own, "core"), swap(inner_own, "core"), swap(outer_own, "core")
    full_output = in_order(core == 0, output_own, output_other, 1)
    cotangent_mine = pick(cotangent, y)
    cotangent_arrived = swap(pick(cotangent, 1 - y), "y")

    full_early = early[:, :own_rows].reshape(width, lanes)
    flat_all = early[:, own_rows:].reshape(shards, extra * lanes)
    sizes = [v.shape[0] for v in vectors]
    gathered, at = [], 0
    for size in sizes:
        gathered.append(flat_all[:, at : at + size].reshape(shards * size))
        at += size
    bias_query, bias_value, bias_output, gain_first, shift_first, bias_inner, bias_outer, gain_second, shift_second = [
        widen(v) for v in gathered
    ]
    biases = jnp.concatenate([bias_query[None], bias_value[None], jnp.zeros((14, width), jnp.float32)], axis=0)
    heads_mine, heads_other, logsum, projected = attention(segment_ids, inputs_all, full_early, biases)
    context = in_order(core == 0, heads_mine, swap(heads_other, "core"), 1)

    attended = matmul(context, full_output) + bias_output
    first, first_normed, first_recip = normalize(widen(inputs) + attended, gain_first, shift_first)
    first_low = lowered(first)
    biases = bias_inner.reshape(shards, 2, unit_half)
    halves = ((inner_own, outer_own, pick(biases, core, 1)), (inner_other, outer_other, pick(biases, 1 - core, 1)))
    outer, kept = bias_outer, []
    for inner_weight, outer_weight, bias in halves:
        inner = matmul(first_low, inner_weight) + bias.reshape(hidden // 2)
        active = lowered(gelu_value(inner))
        outer = outer + matmul(active, outer_weight)
        kept.append((inner, active))
    mixed, second_normed, second_recip = normalize(first + outer, gain_second, shift_second)
    mixed = lowered(mixed)

    upstream = widen(jnp.concatenate([cotangent_mine, cotangent_arrived], axis=0))
    pre_second, grad_second_gain, grad_second_shift = normalize_back(upstream, second_normed, second_recip, gain_second)
    grad_outer = lowered(pre_second)
    grad_b_outer = jnp.sum(widen(grad_outer), axis=0)
    grad_first, inner_grads, outer_grads, bias_grads = pre_second, [], [], []
    for (inner, active), (inner_weight, outer_weight, _) in zip(kept, halves):
        grad_inner = lowered(matmul_nt(grad_outer, outer_weight) * gelu_slope(inner))
        outer_grads.append(lowered(matmul_tn(active, grad_outer)))
        inner_grads.append(lowered(matmul_tn(first_low, grad_inner)))
        bias_grads.append(jnp.sum(widen(grad_inner), axis=0).reshape(shards, 1, unit_half))
        grad_first = grad_first + matmul_nt(grad_inner, inner_weight)
    grad_b_inner = in_order(core == 0, bias_grads[0], bias_grads[1], 1).reshape(hidden)
    pre_first, grad_first_gain, grad_first_shift = normalize_back(grad_first, first_normed, first_recip, gain_first)
    grad_attended = lowered(pre_first)
    grad_b_output = jnp.sum(widen(grad_attended), axis=0)
    grad_w_output = lowered(matmul_tn(context, grad_attended))
    grad_context = lowered(matmul_nt(grad_attended, full_output))
    context_mine = lax.dynamic_slice_in_dim(grad_context, core * half, half, 1)
    context_other = lax.dynamic_slice_in_dim(grad_context, (1 - core) * half, half, 1)
    upstream_other = swap(context_other, "core")

    def core_sum(own, other):
        return lowered(widen(own) + widen(swap(other, "core")))

    outer_term = core_sum(*outer_grads)
    inner_term = core_sum(*inner_grads)
    output_term = core_sum(
        lax.dynamic_slice_in_dim(grad_w_output, core * half, half, 1),
        lax.dynamic_slice_in_dim(grad_w_output, (1 - core) * half, half, 1),
    )
    outer_done = reduce_owned(outer_term.reshape(shards, unit_half, width))
    late_done = reduce_owned(jnp.concatenate([output_term, inner_term], axis=1).reshape(shards, own_rows, half + hidden // 2))

    grads, sums = attention_back(segment_ids, projected, heads_mine, heads_other, context_mine, upstream_other, logsum)
    grad_early = lowered(matmul_tn(inputs_all, grads))
    partial = matmul_nt(grads, full_early)
    sums = sums.reshape(pairs, 8, 3, 128)[:, 0]
    blank = jnp.zeros((width,), jnp.float32)
    grad_b_query = lax.dynamic_update_slice(blank, sums[:, 0].reshape(half), (core * half,))
    grad_b_value = lax.dynamic_update_slice(blank, sums[:, 2].reshape(half), (core * half,))
    vector_grads = (
        grad_b_query,
        grad_b_value,
        grad_b_output,
        grad_first_gain,
        grad_first_shift,
        grad_b_inner,
        grad_b_outer,
        grad_second_gain,
        grad_second_shift,
    )
    flat_grads = jnp.concatenate([v.reshape(shards, -1) for v in vector_grads], axis=1)
    flat_grads = jnp.pad(flat_grads, ((0, 0), (0, extra * lanes - flat_grads.shape[1])))
    early_term = jnp.concatenate(
        [grad_early.reshape(shards, own_rows, lanes), lowered(flat_grads).reshape(shards, extra, lanes)], axis=1
    )
    early_done = reduce_owned(early_term)

    grad_inputs = pre_first + partial[:local] + widen(swap(lowered(partial[local:]), "core"))
    returned = widen(swap(lowered(grad_inputs[part:]), "y"))
    grad_tokens = in_order(y == 0, grad_inputs[None, :part], returned[None], 0)
    mixed_out = in_order(y == 0, mixed[None, :part], swap(mixed[part:], "y")[None], 0)

    def both(piece):
        return widen(swap(lowered(piece), "core"))

    early_matrix = early_done[:own_rows]
    early_full = in_order(
        core == 0, early_matrix.reshape(own_rows, pairs, 3, 128)[None], both(early_matrix).reshape(own_rows, pairs, 3, 128)[None], 0
    )
    early_full = early_full.transpose(3, 1, 0, 2, 4).reshape(3, own_rows, width)
    late_other = both(late_done)
    output_full = in_order(core == 0, late_done[:, :half], late_other[:, :half], 1)
    inner_full = in_order(
        core == 0,
        late_done[:, half:].reshape(own_rows, shards, 1, unit_half),
        late_other[:, half:].reshape(own_rows, shards, 1, unit_half),
        2,
    ).reshape(own_rows, hidden)
    outer_full = in_order(core == 0, outer_done, both(outer_done), 0)
    vector_part = early_done[own_rows:]
    vector_sums = (vector_part + swap(vector_part, "core")).reshape(extra * lanes)
    out_vectors, at = [], 0
    for size in sizes:
        out_vectors.append(vector_sums[at : at + size])
        at += size
    (
        done_b_query,
        done_b_value,
        done_b_output,
        done_first_gain,
        done_first_shift,
        done_b_inner,
        done_b_outer,
        done_second_gain,
        done_second_shift,
    ) = out_vectors
    return (
        mixed_out,
        grad_tokens,
        early_full[0],
        early_full[1],
        early_full[2],
        output_full,
        done_b_query,
        done_b_value,
        done_b_output,
        done_first_gain,
        done_first_shift,
        inner_full,
        done_b_inner,
        outer_full,
        done_b_outer,
        done_second_gain,
        done_second_shift,
    )


def body(
    tokens,
    segment_ids,
    w_query,
    w_key,
    w_value,
    w_output,
    b_query,
    b_value,
    b_output,
    first_gain,
    first_shift,
    w_inner,
    b_inner,
    w_outer,
    b_outer,
    second_gain,
    second_shift,
    cotangent,
):
    core, y = lax.axis_index("core"), lax.axis_index("y")
    size_z, size_x = lax.axis_size("z"), lax.axis_size("x")
    shards = size_z * size_x
    sequences, part, width = tokens.shape
    half = width // 2
    pairs = half // 128
    hidden = w_inner.shape[1]
    local = 2 * part
    own_rows = w_query.shape[0]
    lanes = 3 * half

    vectors = (b_query, b_value, b_output, first_gain, first_shift, b_inner, b_outer, second_gain, second_shift)
    sizes = [v.shape[0] for v in vectors]
    tokens_all, cotangent_send, early, inner_own, outer_own, rows, inner_row = entry(
        size_z, size_x, tokens, cotangent, w_query, w_key, w_value, w_inner, w_output, w_outer, vectors
    )
    cotangent_far = swap(cotangent_send, "y")
    inner_parts = [inner_own] + [shift(inner_own, "x", j) for j in range(1, size_x)]
    outer_parts = [outer_own] + [shift(outer_own, "z", k) for k in range(1, size_z)]
    inputs_all = tokens_all.reshape(4 * part, width)
    full_early = early.reshape(width, lanes)
    context_mine, context_other, logsum, projected = attention(segment_ids, inputs_all, full_early, rows)
    made = dense_layer(
        size_z,
        size_x,
        inputs_all,
        context_mine,
        context_other,
        cotangent,
        cotangent_far,
        rows,
        inner_row,
        inner_parts,
        outer_parts,
    )
    mixed, mixed_send, pre_first, upstream_mine, upstream_other, dense_sums, inner_sums, grad_w_output = made[:8]
    inner_terms = [made[8]] + [shift(made[8 + k], "z", k) for k in range(1, size_z)]
    outer_terms = [made[8 + size_z]] + [shift(made[8 + size_z + j], "x", j) for j in range(1, size_x)]
    mixed_far = swap(mixed_send, "y")
    grads, sums = attention_back(segment_ids, projected, context_mine, context_other, upstream_mine, upstream_other, logsum)
    made = exit_call(
        size_z,
        size_x,
        grads,
        inputs_all,
        full_early,
        pre_first,
        grad_w_output.reshape(shards, own_rows, width),
        dense_sums,
        inner_sums,
        sums,
        inner_terms,
        outer_terms,
    )
    mixed_out, grad_tokens, grad_query, grad_key, grad_value, grad_output, grad_inner_full, grad_outer_full, *done = deliver(
        mixed, mixed_far, made[:7], made[7], sizes
    )
    return (
        mixed_out,
        grad_tokens,
        grad_query,
        grad_key,
        grad_value,
        grad_output,
        *done[:5],
        grad_inner_full,
        done[5],
        grad_outer_full,
        *done[6:],
    )


def layer(*arrays):
    if arrays[2].shape[0] % 32 == 0 and lax.axis_size("x") > 1:
        return body(*arrays)
    return plain_body(*arrays)


def solution(mesh):
    outer, inner = mesh.devices.shape
    size_z = 1
    while size_z * size_z < outer:
        size_z *= 2
    split = Mesh(mesh.devices.reshape(size_z, outer // size_z, inner // 2, 2), ("z", "x", "y", "core"))
    dp, seq = ("z", "x"), ("y", "core")
    activation, matrix, vector = P(dp, seq, None), P(dp, None), P(dp)
    return jax.shard_map(
        layer,
        mesh=split,
        in_specs=(
            activation,
            matrix,
            matrix,
            matrix,
            matrix,
            matrix,
            vector,
            vector,
            vector,
            vector,
            vector,
            matrix,
            vector,
            matrix,
            vector,
            vector,
            vector,
            activation,
        ),
        out_specs=(
            activation,
            activation,
            matrix,
            matrix,
            matrix,
            matrix,
            vector,
            vector,
            vector,
            vector,
            vector,
            matrix,
            vector,
            matrix,
            vector,
            vector,
            vector,
        ),
        check_vma=False,
    )
```
